32 devices in a mesh: dp: 4 (over x, core), seq: 2 (over y), tensor: 4 (over z).
Axes of the slice: x: 2, y: 2, z: 4, core: 2. Of those that a mesh axis runs over, the one named last changes fastest.
Arguments:
- tokens: bfloat16 [2048, 4096], P(('dp', 'seq')), may hold values from -6 to 6
- seg_ids: int32 [2048], P('dp'), may hold values from 0 to 15, as said below
- gain_attn: bfloat16 [4096], P(('dp', 'seq')), may hold values from 0.5 to 1.5
- w_query: bfloat16 [4096, 4096], P(('dp', 'seq'), 'tensor'), may hold values from -1.5 to 1.5
- kv_weight: bfloat16 [4096, 512], P(('dp', 'seq')), may hold values from -1.5 to 1.5
- w_out: bfloat16 [4096, 4096], P('tensor', ('dp', 'seq')), may hold values from -0.375 to 0.375
- gain_ffn: bfloat16 [4096], P(('dp', 'seq')), may hold values from 0.5 to 1.5
- w_gate: bfloat16 [4096, 12288], P(('dp', 'seq'), 'tensor'), may hold values from -0.09375 to 0.09375
- w_up: bfloat16 [4096, 12288], P(('dp', 'seq'), 'tensor'), may hold values from -0.09375 to 0.09375
- w_down: bfloat16 [12288, 4096], P('tensor', ('dp', 'seq')), may hold values from -0.0546875 to 0.0546875
- d_out: bfloat16 [2048, 4096], P(('dp', 'seq')), may hold values from -6 to 6
Outputs:
- out: bfloat16 [2048, 4096], P(('dp', 'seq'))
- d_tokens: float32 [2048, 4096], P(('dp', 'seq'))
- d_gain_attn: float32 [4096], P(('dp', 'seq'))
- d_w_query: float32 [4096, 4096], P(('dp', 'seq'), 'tensor')
- d_kv_weight: float32 [4096, 512], P(('dp', 'seq'))
- d_w_out: float32 [4096, 4096], P('tensor', ('dp', 'seq'))
- d_gain_ffn: float32 [4096], P(('dp', 'seq'))
- d_w_gate: float32 [4096, 12288], P(('dp', 'seq'), 'tensor')
- d_w_up: float32 [4096, 12288], P(('dp', 'seq'), 'tensor')
- d_w_down: float32 [12288, 4096], P('tensor', ('dp', 'seq'))
The draws below stay inside these ranges and needn't reach their ends.
Inputs may be any that keep to these rules, and one draw needn't show every extreme that they name: `seg_ids`: within each group of 512 tokens g (from 0) the ids never fall, take values from 4 g to 4 g + 3 and start at 4 g; some group other than the last holds one sequence.
All inputs are finite; a program needn't handle non-finite values.
Results may differ from the reference program's by a relative error of at most 0.02.
Values may be sent and summed in bfloat16 or wider, within the bound.
A program may use at most 384 MiB of HBM per device.

```python
import math
import jax
import jax.numpy as jnp
from jax import lax

D = 4096
H = 16
HD = 256
FF = 12288
GROUP = 512
TOKENS = 2048


def draw_kv_weight(key, part):
    values = jax.random.normal(jax.random.fold_in(key, 102), (D, HD), jnp.float32) / math.sqrt(D)
    key_part = jax.random.normal(jax.random.fold_in(key, 103), (D, HD), jnp.float32) / math.sqrt(D)
    joined = jnp.concatenate([key_part, values], axis=1)
    return jnp.clip(joined, -1.5, 1.5).astype(jnp.bfloat16)


def draw_w_query(key, part):
    drawn = jax.random.normal(jax.random.fold_in(key, 104), (D, H * HD), jnp.float32) / math.sqrt(D)
    return jnp.clip(drawn, -1.5, 1.5).astype(jnp.bfloat16)


def draw_seg_ids(key, part):
    groups = TOKENS // GROUP
    cuts = jax.random.randint(jax.random.fold_in(key, 201), (groups, 3), 1, GROUP)
    live = jax.random.randint(jax.random.fold_in(key, 202), (groups, 3), 0, 2)
    single = jax.random.randint(jax.random.fold_in(key, 203), (), 0, groups - 1)
    group_index = jnp.arange(groups, dtype=jnp.int32)
    live = jnp.where(group_index[:, None] == groups - 1, 1, live)
    live = jnp.where(group_index[:, None] == single, 0, live)
    cuts = jnp.where(live == 1, cuts, GROUP)
    spots = jnp.arange(GROUP, dtype=jnp.int32)
    local = jnp.sum((cuts[:, None, :] <= spots[None, :, None]).astype(jnp.int32), axis=-1)
    ids = group_index[:, None] * 4 + local
    return ids.reshape(-1).astype(jnp.int32)


def block_scale(own_key, extent, shards, least, high):
    def one(axis_at, blocks):
        steps = jax.random.uniform(jax.random.fold_in(jax.random.fold_in(own_key, 6), axis_at), (blocks,), jnp.float32, least / len(shards), high / len(shards))
        return jnp.repeat(jnp.exp(steps), extent[axis_at] // blocks).reshape((-1,) + (1,) * (len(extent) - axis_at - 1))

    factor_of = one(*shards[0])
    for cut in shards[1:]:
        factor_of = factor_of * one(*cut)
    return factor_of


def centred(stream_key, extent, width, reach, split=(), held_as=jnp.bfloat16):
    loudness = block_scale(stream_key, extent, split, -0.22, 0.18) if split else 1.0
    drawn = jax.random.normal(stream_key, extent, jnp.float32) * width * loudness
    return jnp.minimum(jnp.maximum(drawn, -reach), reach).astype(held_as)


def setup_inputs(seed: int = 0) -> dict:
    key_list = jax.random.split(jax.random.key(seed), 12)
    tokens = centred(key_list[0], (TOKENS, D), 1.0, 6.0, ((0, 8),))
    seg_ids = draw_seg_ids(jax.random.fold_in(key_list[11], 71), 0)
    gain_attn = jnp.clip(1.0 + 0.1 * jax.random.normal(key_list[2], (D,), jnp.float32), 0.5, 1.5).astype(jnp.bfloat16)
    w_query = draw_w_query(jax.random.fold_in(key_list[11], 71), 0)
    kv_weight = draw_kv_weight(jax.random.fold_in(key_list[11], 71), 0)
    w_out = centred(key_list[5], (H * HD, D), (H * HD // 16) ** -0.5, 0.375, ((0, 4), (1, 8)))
    gain_ffn = jnp.clip(1.0 + 0.1 * jax.random.normal(key_list[6], (D,), jnp.float32), 0.5, 1.5).astype(jnp.bfloat16)
    w_gate = centred(key_list[7], (D, FF), D ** -0.5, 0.09375, ((0, 8), (1, 4)))
    w_up = centred(key_list[8], (D, FF), D ** -0.5, 0.09375, ((0, 8), (1, 4)))
    w_down = centred(key_list[9], (FF, D), FF ** -0.5, 0.0546875, ((0, 4), (1, 8)))
    d_out = centred(key_list[10], (TOKENS, D), 1.0, 6.0, ((0, 8),))
    return {"tokens": tokens, "seg_ids": seg_ids, "gain_attn": gain_attn, "w_query": w_query, "kv_weight": kv_weight, "w_out": w_out, "gain_ffn": gain_ffn, "w_gate": w_gate, "w_up": w_up, "w_down": w_down, "d_out": d_out}


EPS = 1e-06
NEG = -1e+30

@jax.custom_vjp
def low(v):
    return lax.optimization_barrier(v.astype(jnp.bfloat16)).astype(jnp.float32)

@jax.custom_vjp
def low_back(v):
    return v

def low_keep(v):
    return (low(v), None)

def low_pass(kept, grad):
    return (grad,)

def back_keep(v):
    return (v, None)

def back_low(kept, grad):
    return (low(grad),)
low.defvjp(low_keep, low_pass)
low_back.defvjp(back_keep, back_low)

def place_tables(segs):
    length = segs.shape[0]
    index = jnp.arange(length, dtype=jnp.int32)
    flags = jnp.concatenate([jnp.ones((1,), dtype=bool), segs[1:] != segs[:-1]])
    starts = lax.cummax(jnp.where(flags, index, jnp.zeros_like(index)), axis=0)
    places = (index - starts).astype(jnp.int32)
    half_size = HD // 2
    freqs = jnp.exp(jnp.arange(half_size, dtype=jnp.float32) * (-math.log(10000.0) / half_size))
    angles = places.astype(jnp.float32)[:, None] * freqs[None, :]
    return (places, jnp.cos(angles), jnp.sin(angles))

def rotate(vector, cos_table, sin_table):
    half_size = vector.shape[-1] // 2
    leading = vector[..., :half_size]
    trailing = vector[..., half_size:]
    return jnp.concatenate([leading * cos_table - trailing * sin_table, trailing * cos_table + leading * sin_table], axis=-1)

def forward(tokens, gain_one, query_w, kv_w, out_w, gain_two, gate_w, up_w, down_w, segs):
    highest = lax.Precision.HIGHEST
    length = tokens.shape[0]
    places, cos_table, sin_table = place_tables(segs)
    rms_one = lax.rsqrt(lax.optimization_barrier(jnp.mean(tokens * tokens, axis=-1, keepdims=True)) + EPS)
    act_one = low(tokens * rms_one * gain_one)
    query_pre = low_back(jnp.dot(act_one, query_w, precision=highest))
    kv_pre = low_back(jnp.dot(act_one, kv_w, precision=highest))
    queries = low(rotate(query_pre.reshape(length, H, HD), cos_table[:, None, :], sin_table[:, None, :]) * (1.0 / math.sqrt(HD)))
    keys = low(rotate(kv_pre[:, :HD], cos_table, sin_table))
    values = low(kv_pre[:, HD:])
    scores = low_back(jnp.einsum('rhd,kd->hrk', queries, keys, precision=highest))
    allowed = (segs[:, None] == segs[None, :]) & (places[:, None] >= places[None, :])
    scores = jnp.where(allowed[None], scores, NEG)
    probs = jax.nn.softmax(scores, axis=-1)
    mixed = jnp.einsum('hrk,kd->rhd', low(probs), values, precision=highest).reshape(length, H * HD)
    mixed = low(low_back(mixed))
    attn = low_back(jnp.dot(mixed, out_w, precision=highest))
    resid = tokens + attn
    rms_two = lax.rsqrt(lax.optimization_barrier(jnp.mean(resid * resid, axis=-1, keepdims=True)) + EPS)
    act_two = low(resid * rms_two * gain_two)
    gate = low_back(jnp.dot(act_two, gate_w, precision=highest))
    up_val = low_back(jnp.dot(act_two, up_w, precision=highest))
    hidden = low(jax.nn.gelu(gate, approximate=True) * up_val)
    return resid + jnp.dot(hidden, down_w, precision=highest)

def reference(tokens, seg_ids, gain_attn, w_query, kv_weight, w_out, gain_ffn, w_gate, w_up, w_down, d_out):
    params = tuple((item.astype(jnp.float32) for item in (gain_attn, w_query, kv_weight, w_out, gain_ffn, w_gate, w_up, w_down)))
    groups = TOKENS // GROUP

    def per_group(carry, inputs):
        group_tok, group_seg, group_cot = inputs

        def local_fwd(tok_in, *weights):
            return forward(tok_in, *weights, group_seg)
        result, pullback = jax.vjp(local_fwd, group_tok, *params)
        grads = pullback(group_cot)
        carry = tuple((acc + new for acc, new in zip(carry, grads[1:])))
        return (carry, (result.astype(jnp.bfloat16), grads[0]))
    init = tuple((jnp.zeros_like(item) for item in params))
    inputs = (tokens.astype(jnp.float32).reshape(groups, GROUP, D), seg_ids.reshape(groups, GROUP), d_out.astype(jnp.float32).reshape(groups, GROUP, D))
    totals, (outputs, d_toks) = lax.scan(per_group, init, inputs)
    return (outputs.reshape(TOKENS, D), d_toks.reshape(TOKENS, D), totals[0], totals[1], totals[2], totals[3], totals[4], totals[5], totals[6], totals[7])
```

```python
import math

import jax
import jax.numpy as jnp
from jax import lax
from jax.sharding import PartitionSpec as P

HD = 256


EPS = 1e-06
NEG = -1e30


def place_tables(segs):
    length = segs.shape[0]
    index = jnp.arange(length, dtype=jnp.int32)
    flags = jnp.concatenate([jnp.ones((1,), dtype=bool), segs[1:] != segs[:-1]])
    starts = lax.cummax(jnp.where(flags, index, jnp.zeros_like(index)), axis=0)
    places = index - starts
    half_size = HD // 2
    freqs = jnp.exp(jnp.arange(half_size, dtype=jnp.float32) * (-math.log(10000.0) / half_size))
    angles = places.astype(jnp.float32)[:, None] * freqs[None, :]
    return (places, jnp.cos(angles), jnp.sin(angles))


def rotate(vector, cos_table, sin_table):
    half_size = vector.shape[-1] // 2
    leading = vector[..., :half_size]
    trailing = vector[..., half_size:]
    return jnp.concatenate(
        [leading * cos_table - trailing * sin_table, trailing * cos_table + leading * sin_table],
        axis=-1,
    )


def rotate_back(vector, cos_table, sin_table):
    half_size = vector.shape[-1] // 2
    leading = vector[..., :half_size]
    trailing = vector[..., half_size:]
    return jnp.concatenate(
        [leading * cos_table + trailing * sin_table, trailing * cos_table - leading * sin_table],
        axis=-1,
    )


def matmul(left, right):
    return jnp.dot(left, right, preferred_element_type=jnp.float32)


def matmul_nt(left, right):
    return lax.dot_general(
        left, right, (((1,), (1,)), ((), ())), preferred_element_type=jnp.float32
    )


def matmul_tn(left, right):
    return lax.dot_general(
        left, right, (((0,), (0,)), ((), ())), preferred_element_type=jnp.float32
    )


def gelu_tanh(values):
    return jax.nn.gelu(values, approximate=True)


def norm_back(d_act, normed, rms_val, gain_val):
    scaled = d_act * gain_val
    return rms_val * (scaled - normed * jnp.mean(scaled * normed, axis=-1, keepdims=True))


def weights_move(
    tokens, seg_ids, gain_attn, w_query, kv_weight, w_out, gain_ffn, w_gate, w_up, w_down, d_out
):
    rows = tokens.shape[0]
    scale_factor = 1.0 / math.sqrt(HD)
    offset = lax.axis_index("seq") * rows
    places, cos_table, sin_table = place_tables(seg_ids)
    own_places = lax.dynamic_slice_in_dim(places, offset, rows, 0)
    own_segs = lax.dynamic_slice_in_dim(seg_ids, offset, rows, 0)
    own_cos = lax.dynamic_slice_in_dim(cos_table, offset, rows, 0)
    own_sin = lax.dynamic_slice_in_dim(sin_table, offset, rows, 0)
    allowed = (own_segs[:, None] == seg_ids[None, :]) & (own_places[:, None] >= places[None, :])
    full_query, full_out, full_kv, full_gain_one = (
        lax.all_gather(w_query, ("dp", "seq"), axis=0, tiled=True),
        lax.all_gather(w_out, ("dp", "seq"), axis=1, tiled=True),
        lax.all_gather(kv_weight, ("dp", "seq"), axis=0, tiled=True),
        lax.all_gather(gain_attn, ("dp", "seq"), axis=0, tiled=True),
    )
    gain_one = full_gain_one.astype(jnp.float32)
    inputs = tokens.astype(jnp.float32)
    rms_one = lax.rsqrt(jnp.mean(inputs * inputs, axis=-1, keepdims=True) + EPS)
    norm_one = inputs * rms_one
    act_one = (norm_one * gain_one).astype(jnp.bfloat16)
    query_pre = matmul(act_one, full_query)
    heads = query_pre.shape[1] // HD
    kv_pre = matmul(act_one, full_kv)
    queries = (
        rotate(query_pre.reshape(rows, heads, HD), own_cos[:, None, :], own_sin[:, None, :])
        * scale_factor
    ).astype(jnp.bfloat16)
    own_kv = jnp.concatenate(
        [rotate(kv_pre[:, :HD], own_cos, own_sin), kv_pre[:, HD:]], axis=1
    ).astype(jnp.bfloat16)
    all_kv = lax.all_gather(own_kv, "seq", axis=0, tiled=True)
    keys = all_kv[:, :HD]
    values_all = all_kv[:, HD:]
    scores = jnp.einsum("rhd,kd->hrk", queries, keys, preferred_element_type=jnp.float32)
    scores = jnp.where(allowed[None], scores, NEG)
    top_score = jnp.max(scores, axis=-1, keepdims=True)
    expd = jnp.exp(scores - top_score)
    total = jnp.sum(expd, axis=-1, keepdims=True)
    log_total = top_score + jnp.log(total)
    probs_low = (expd / total).astype(jnp.bfloat16)
    mixed = (
        jnp.einsum("hrk,kd->rhd", probs_low, values_all, preferred_element_type=jnp.float32)
        .reshape(rows, heads * HD)
        .astype(jnp.bfloat16)
    )
    attn = lax.psum(matmul(mixed, full_out), "tensor")
    resid = inputs + attn
    full_gate, full_up, full_down, full_gain_two = (
        lax.all_gather(w_gate, ("dp", "seq"), axis=0, tiled=True),
        lax.all_gather(w_up, ("dp", "seq"), axis=0, tiled=True),
        lax.all_gather(w_down, ("dp", "seq"), axis=1, tiled=True),
        lax.all_gather(gain_ffn, ("dp", "seq"), axis=0, tiled=True),
    )
    gain_two = full_gain_two.astype(jnp.float32)
    rms_two = lax.rsqrt(jnp.mean(resid * resid, axis=-1, keepdims=True) + EPS)
    norm_two = resid * rms_two
    act_two = (norm_two * gain_two).astype(jnp.bfloat16)
    gate = matmul(act_two, full_gate)
    up_val = matmul(act_two, full_up)
    gelu_val, gelu_pull = jax.vjp(gelu_tanh, gate)
    hidden = (gelu_val * up_val).astype(jnp.bfloat16)
    ffn = lax.psum(matmul(hidden, full_down).astype(jnp.bfloat16), "tensor").astype(jnp.float32)
    out = (resid + ffn).astype(jnp.bfloat16)
    back_gate, back_up, back_down = (
        lax.all_gather(w_gate, ("dp", "seq"), axis=0, tiled=True),
        lax.all_gather(w_up, ("dp", "seq"), axis=0, tiled=True),
        lax.all_gather(w_down, ("dp", "seq"), axis=1, tiled=True),
    )
    d_hidden = matmul_nt(d_out, back_down)
    grad_down = matmul_tn(hidden, d_out)
    d_gate = gelu_pull(d_hidden * up_val)[0].astype(jnp.bfloat16)
    d_up = (d_hidden * gelu_val).astype(jnp.bfloat16)
    grad_gate = matmul_tn(act_two, d_gate)
    grad_up = matmul_tn(act_two, d_up)
    d_act_two = lax.psum(matmul_nt(d_gate, back_gate) + matmul_nt(d_up, back_up), "tensor")
    grad_gain_two = jnp.sum(d_act_two * norm_two, axis=0)
    d_resid = d_out.astype(jnp.float32) + norm_back(d_act_two, norm_two, rms_two, gain_two)
    ffn_grads = (
        lax.psum_scatter(
            grad_gate.astype(jnp.bfloat16), ("dp", "seq"), scatter_dimension=0, tiled=True
        ).astype(jnp.float32),
        lax.psum_scatter(
            grad_up.astype(jnp.bfloat16), ("dp", "seq"), scatter_dimension=0, tiled=True
        ).astype(jnp.float32),
        lax.psum_scatter(
            grad_down.astype(jnp.bfloat16), ("dp", "seq"), scatter_dimension=1, tiled=True
        ).astype(jnp.float32),
        lax.psum_scatter(
            grad_gain_two.astype(jnp.bfloat16), ("dp", "seq"), scatter_dimension=0, tiled=True
        ).astype(jnp.float32),
    )
    back_query, back_out, back_kv = (
        lax.all_gather(w_query, ("dp", "seq"), axis=0, tiled=True),
        lax.all_gather(w_out, ("dp", "seq"), axis=1, tiled=True),
        lax.all_gather(kv_weight, ("dp", "seq"), axis=0, tiled=True),
    )
    d_attn = d_resid.astype(jnp.bfloat16)
    grad_out = matmul_tn(mixed, d_attn)
    d_mixed = matmul_nt(d_attn, back_out).astype(jnp.bfloat16).reshape(rows, heads, HD)
    scores_again = jnp.einsum("rhd,kd->hrk", queries, keys, preferred_element_type=jnp.float32)
    probs = jnp.where(allowed[None], jnp.exp(scores_again - log_total), 0.0)
    d_probs = jnp.einsum("rhd,kd->hrk", d_mixed, values_all, preferred_element_type=jnp.float32)
    delta = jnp.sum(probs * d_probs, axis=-1, keepdims=True)
    d_scores = (probs * (d_probs - delta)).astype(jnp.bfloat16)
    d_queries = (
        jnp.einsum("hrk,kd->rhd", d_scores, keys, preferred_element_type=jnp.float32) * scale_factor
    )
    d_query_pre = (
        rotate_back(d_queries, own_cos[:, None, :], own_sin[:, None, :])
        .reshape(rows, heads * HD)
        .astype(jnp.bfloat16)
    )
    d_keys_part = jnp.einsum("hrk,rhd->kd", d_scores, queries, preferred_element_type=jnp.float32)
    d_values_part = jnp.einsum(
        "hrk,rhd->kd", probs.astype(jnp.bfloat16), d_mixed, preferred_element_type=jnp.float32
    )
    own_kv_grad = lax.psum_scatter(
        jnp.concatenate([d_keys_part, d_values_part], axis=1).astype(jnp.bfloat16),
        "seq",
        scatter_dimension=0,
        tiled=True,
    )
    d_act_query = matmul_nt(d_query_pre, back_query)
    d_act_sum, kv_grad = (
        lax.psum(d_act_query.astype(jnp.bfloat16), "tensor").astype(jnp.float32),
        lax.psum(own_kv_grad, "tensor").astype(jnp.float32),
    )
    d_kv_pre = jnp.concatenate(
        [rotate_back(kv_grad[:, :HD], own_cos, own_sin), kv_grad[:, HD:]], axis=1
    ).astype(jnp.bfloat16)
    d_act_one = d_act_sum + matmul_nt(d_kv_pre, back_kv)
    grad_query = matmul_tn(act_one, d_query_pre)
    grad_kv = matmul_tn(act_one, d_kv_pre)
    grad_gain_one = jnp.sum(d_act_one * norm_one, axis=0)
    d_tokens = d_resid + norm_back(d_act_one, norm_one, rms_one, gain_one)
    attn_grads = (
        lax.psum_scatter(
            grad_query.astype(jnp.bfloat16), ("dp", "seq"), scatter_dimension=0, tiled=True
        ).astype(jnp.float32),
        lax.psum_scatter(
            grad_out.astype(jnp.bfloat16), ("dp", "seq"), scatter_dimension=1, tiled=True
        ).astype(jnp.float32),
        lax.psum_scatter(
            grad_kv.astype(jnp.bfloat16), ("dp", "seq"), scatter_dimension=0, tiled=True
        ).astype(jnp.float32),
        lax.psum_scatter(
            grad_gain_one.astype(jnp.bfloat16), ("dp", "seq"), scatter_dimension=0, tiled=True
        ).astype(jnp.float32),
    )
    return (
        out,
        d_tokens,
        attn_grads[3],
        attn_grads[0],
        attn_grads[2],
        attn_grads[1],
        ffn_grads[3],
        ffn_grads[0],
        ffn_grads[1],
        ffn_grads[2],
    )


AXES = ("dp", "seq")
LANES = 128


def gather_rows(block):
    return lax.all_gather(block, AXES, axis=0, tiled=True)


def scatter_rows(block):
    return lax.psum_scatter(block, AXES, scatter_dimension=0, tiled=True)


def to_columns(block):
    return lax.all_to_all(block, AXES, split_axis=1, concat_axis=0, tiled=True)


def lane_sums(values):
    return jnp.sum(values.reshape(values.shape[0], -1, LANES), axis=1)


def to_tokens(partial, rest, parts, rows):
    depth = lax.axis_size("tensor")
    width = partial.shape[1]
    share = rows // depth
    summed = lax.psum_scatter(
        partial.astype(jnp.bfloat16).reshape(parts, depth, share, width),
        "tensor",
        scatter_dimension=1,
        tiled=False,
    )
    own_rest = lax.dynamic_index_in_dim(
        rest.reshape(parts, depth, share, width), lax.axis_index("tensor"), 1, keepdims=False
    )
    whole = (summed.astype(jnp.float32) + own_rest).astype(jnp.bfloat16)
    moved = lax.all_to_all(whole, AXES, split_axis=0, concat_axis=0, tiled=True)
    by_row = jnp.transpose(moved, (1, 0, 2)).reshape(share, parts * width)
    return lax.all_gather(by_row, "tensor", axis=0, tiled=True)


def acts_move(
    tokens, seg_ids, gain_attn, w_query, kv_weight, w_out, gain_ffn, w_gate, w_up, w_down, d_out
):
    low = jnp.bfloat16
    rows, width = tokens.shape
    seqs = lax.axis_size("seq")
    parts = lax.axis_size("dp") * seqs
    scale_factor = 1.0 / math.sqrt(HD)
    offset = lax.axis_index("seq") * rows
    places, cos_table, sin_table = place_tables(seg_ids)
    own_places = lax.dynamic_slice_in_dim(places, offset, rows, 0)
    own_segs = lax.dynamic_slice_in_dim(seg_ids, offset, rows, 0)
    own_cos = lax.dynamic_slice_in_dim(cos_table, offset, rows, 0)
    own_sin = lax.dynamic_slice_in_dim(sin_table, offset, rows, 0)
    allowed = (own_segs[:, None] == seg_ids[None, :]) & (own_places[:, None] >= places[None, :])
    gain_one = gain_attn.astype(jnp.float32)
    gain_two = gain_ffn.astype(jnp.float32)
    qw = w_query.shape[1]
    heads = qw // HD
    ff = w_gate.shape[1]

    x_low = to_columns(tokens)
    g_low = to_columns(d_out)
    x_col = x_low.astype(jnp.float32)
    own_x = tokens.astype(jnp.float32)
    rms_one = lax.rsqrt(jnp.mean(own_x * own_x, axis=-1, keepdims=True) + EPS)
    act_one = (x_col * gain_one).astype(low)
    qkv = scatter_rows(
        jnp.concatenate([matmul(act_one, w_query), matmul(act_one, kv_weight)], axis=1).astype(low)
    )
    qkv = qkv.astype(jnp.float32) * rms_one
    queries = (
        rotate(qkv[:, :qw].reshape(rows, heads, HD), own_cos[:, None, :], own_sin[:, None, :])
        * scale_factor
    ).astype(low)
    rms_high = rms_one.astype(low)
    rms_rest = (rms_one - rms_high.astype(jnp.float32)).astype(low)
    half = (rows, LANES // 2)
    own_kv = jnp.concatenate(
        [
            rotate(qkv[:, qw : qw + HD], own_cos, own_sin).astype(low),
            qkv[:, qw + HD :].astype(low),
            jnp.broadcast_to(rms_high, half),
            jnp.broadcast_to(rms_rest, half),
        ],
        axis=1,
    )
    all_kv = lax.all_gather(own_kv, "seq", axis=0, tiled=True)
    keys = all_kv[:, :HD]
    values_all = all_kv[:, HD : 2 * HD]
    rms_group = all_kv[:, 2 * HD : 2 * HD + 1].astype(jnp.float32) + all_kv[
        :, 2 * HD + LANES // 2 : 2 * HD + LANES // 2 + 1
    ].astype(jnp.float32)
    scores = jnp.einsum("rhd,kd->hrk", queries, keys, preferred_element_type=jnp.float32)
    scores = jnp.where(allowed[None], scores, NEG)
    top_score = jnp.max(scores, axis=-1, keepdims=True)
    expd = jnp.exp(scores - top_score)
    total = jnp.sum(expd, axis=-1, keepdims=True)
    probs = expd / total
    probs_low = probs.astype(low)
    mixed = (
        jnp.einsum("hrk,kd->rhd", probs_low, values_all, preferred_element_type=jnp.float32)
        .reshape(rows, heads * HD)
        .astype(low)
    )
    mixed_all = gather_rows(mixed)
    attn = lax.psum(matmul(mixed_all, w_out).astype(low), "tensor")
    d_hidden = scatter_rows(matmul_nt(g_low, w_down).astype(low)).astype(jnp.float32)
    resid = x_col + attn.astype(jnp.float32)
    act_two = (resid * gain_two).astype(low)
    both = scatter_rows(
        jnp.concatenate(
            [matmul(act_two, w_gate), matmul(act_two, w_up), lane_sums(resid * resid)], axis=1
        ).astype(low)
    ).astype(jnp.float32)
    mean_two = jnp.sum(both[:, 2 * ff :], axis=-1, keepdims=True) / width
    rms_two = lax.rsqrt(mean_two + EPS)
    gate = both[:, :ff] * rms_two
    up_val = both[:, ff : 2 * ff] * rms_two
    gelu_val, gelu_pull = jax.vjp(gelu_tanh, gate)
    hidden = (gelu_val * up_val).astype(low)
    d_gate = gelu_pull(d_hidden * up_val)[0]
    d_up = d_hidden * gelu_val
    dots_two = lane_sums(d_gate * gate + d_up * up_val) * (rms_two * rms_two / width)
    back = gather_rows(
        jnp.concatenate(
            [(d_gate * rms_two).astype(low), (d_up * rms_two).astype(low), dots_two.astype(low)],
            axis=1,
        )
    )
    hidden_all = gather_rows(hidden)
    d_gate_all = back[:, :ff]
    d_up_all = back[:, ff : 2 * ff]
    dot_two = jnp.sum(back[:, 2 * ff :].astype(jnp.float32), axis=-1, keepdims=True)
    d_act_two = matmul_nt(d_gate_all, w_gate) + matmul_nt(d_up_all, w_up)
    grad_gain_two = jnp.sum(d_act_two * resid, axis=0)
    d_norm = lax.psum((d_act_two * gain_two - resid * dot_two).astype(low), "tensor")
    d_resid = g_low.astype(jnp.float32) + d_norm.astype(jnp.float32)
    d_attn = d_resid.astype(low)
    d_mixed = scatter_rows(matmul_nt(d_attn, w_out).astype(low)).reshape(rows, heads, HD)
    grad_gate = matmul_tn(act_two, d_gate_all)
    grad_up = matmul_tn(act_two, d_up_all)
    grad_down = matmul_tn(hidden_all, g_low)
    out = to_tokens(matmul(hidden_all, w_down), resid, parts, rows)
    grad_out = matmul_tn(mixed_all, d_attn)

    d_probs = jnp.einsum("rhd,kd->hrk", d_mixed, values_all, preferred_element_type=jnp.float32)
    delta = jnp.sum(probs * d_probs, axis=-1, keepdims=True)
    d_scores = (probs * (d_probs - delta)).astype(low)
    d_queries = (
        jnp.einsum("hrk,kd->rhd", d_scores, keys, preferred_element_type=jnp.float32) * scale_factor
    )
    d_query_pre = (
        rotate_back(d_queries, own_cos[:, None, :], own_sin[:, None, :]).reshape(rows, heads * HD)
        * rms_one
    ).astype(low)
    query_dots = lane_sums(
        (d_queries * queries.astype(jnp.float32)).reshape(rows, heads * HD)
    ) * (rms_one * rms_one / (width * scale_factor))
    d_keys = jnp.einsum("hrk,rhd->kd", d_scores, queries, preferred_element_type=jnp.float32)
    d_values = jnp.einsum("hrk,rhd->kd", probs_low, d_mixed, preferred_element_type=jnp.float32)
    kv_dots = lane_sums(
        jnp.concatenate(
            [d_keys * keys.astype(jnp.float32), d_values * values_all.astype(jnp.float32)], axis=1
        )
    ) * (rms_group * rms_group / width)
    d_kv = jnp.concatenate(
        [
            rotate_back(d_keys, cos_table, sin_table) * rms_group,
            d_values * rms_group,
            kv_dots,
        ],
        axis=1,
    ).astype(low)
    kvw = d_kv.shape[1]
    pieces = [d_kv[at * rows : (at + 1) * rows] for at in range(seqs)]
    home = gather_rows(
        jnp.concatenate([d_query_pre, query_dots.astype(low)] + pieces, axis=1)
    )
    d_query_all = home[:, :qw]
    kv_parts = home[:, qw + LANES :].reshape(parts // seqs, seqs, rows, seqs, kvw)
    kv_sum = jnp.sum(kv_parts.astype(jnp.float32), axis=1)
    kv_sum = jnp.transpose(kv_sum, (0, 2, 1, 3)).reshape(parts * rows, kvw)
    d_kv_all = kv_sum[:, : 2 * HD].astype(low)
    dot_one = jnp.sum(
        home[:, qw : qw + LANES].astype(jnp.float32) + kv_sum[:, 2 * HD :], axis=-1, keepdims=True
    )
    d_act_one = matmul_nt(d_query_all, w_query) + matmul_nt(d_kv_all, kv_weight)
    grad_gain_one = jnp.sum(d_act_one * x_col, axis=0)
    d_tokens = to_tokens(d_act_one * gain_one - x_col * dot_one, d_resid, parts, rows)
    grad_query = matmul_tn(act_one, d_query_all)
    grad_kv = lax.psum(matmul_tn(act_one, d_kv_all).astype(low), "tensor").astype(jnp.float32)
    gains = lax.psum(jnp.stack([grad_gain_one, grad_gain_two]), "tensor")
    return (
        out,
        d_tokens.astype(jnp.float32),
        gains[0],
        grad_query,
        grad_kv,
        grad_out,
        gains[1],
        grad_gate,
        grad_up,
        grad_down,
    )


def solution(mesh):
    in_specs = (
        P(("dp", "seq"), None),
        P("dp"),
        P(("dp", "seq")),
        P(("dp", "seq"), "tensor"),
        P(("dp", "seq"), None),
        P("tensor", ("dp", "seq")),
        P(("dp", "seq")),
        P(("dp", "seq"), "tensor"),
        P(("dp", "seq"), "tensor"),
        P("tensor", ("dp", "seq")),
        P(("dp", "seq"), None),
    )
    out_specs = (
        P(("dp", "seq"), None),
        P(("dp", "seq"), None),
        P(("dp", "seq")),
        P(("dp", "seq"), "tensor"),
        P(("dp", "seq"), None),
        P("tensor", ("dp", "seq")),
        P(("dp", "seq")),
        P(("dp", "seq"), "tensor"),
        P(("dp", "seq"), "tensor"),
        P("tensor", ("dp", "seq")),
    )

    def shards(*arrays):
        tokens = arrays[0]
        count = tokens.shape[0] * mesh.shape["dp"] * mesh.shape["seq"]
        plan = acts_move if count <= tokens.shape[1] else weights_move
        return plan(*arrays)

    return jax.shard_map(shards, mesh=mesh, in_specs=in_specs, out_specs=out_specs, check_vma=False)
```

```python
import functools
import math

import jax
import jax.numpy as jnp
from jax import lax
from jax.experimental import pallas as pl
from jax.experimental.pallas import tpu as pltpu
from jax.sharding import PartitionSpec as P

HD = 256


EPS = 1e-06
NEG = -1e30


def place_tables(segs):
    length = segs.shape[0]
    index = jnp.arange(length, dtype=jnp.int32)
    flags = jnp.concatenate([jnp.ones((1,), dtype=bool), segs[1:] != segs[:-1]])
    starts = lax.cummax(jnp.where(flags, index, jnp.zeros_like(index)), axis=0)
    places = index - starts
    half_size = HD // 2
    freqs = jnp.exp(jnp.arange(half_size, dtype=jnp.float32) * (-math.log(10000.0) / half_size))
    angles = places.astype(jnp.float32)[:, None] * freqs[None, :]
    return (places, jnp.cos(angles), jnp.sin(angles))


def rotate(vector, cos_table, sin_table):
    half_size = vector.shape[-1] // 2
    leading = vector[..., :half_size]
    trailing = vector[..., half_size:]
    return jnp.concatenate(
        [leading * cos_table - trailing * sin_table, trailing * cos_table + leading * sin_table],
        axis=-1,
    )


def rotate_back(vector, cos_table, sin_table):
    half_size = vector.shape[-1] // 2
    leading = vector[..., :half_size]
    trailing = vector[..., half_size:]
    return jnp.concatenate(
        [leading * cos_table + trailing * sin_table, trailing * cos_table - leading * sin_table],
        axis=-1,
    )


def matmul(left, right):
    return jnp.dot(left, right, preferred_element_type=jnp.float32)


def matmul_nt(left, right):
    return lax.dot_general(
        left, right, (((1,), (1,)), ((), ())), preferred_element_type=jnp.float32
    )


def matmul_tn(left, right):
    return lax.dot_general(
        left, right, (((0,), (0,)), ((), ())), preferred_element_type=jnp.float32
    )


def gelu_tanh(values):
    return jax.nn.gelu(values, approximate=True)


def norm_back(d_act, normed, rms_val, gain_val):
    scaled = d_act * gain_val
    return rms_val * (scaled - normed * jnp.mean(scaled * normed, axis=-1, keepdims=True))


def weights_move(
    tokens, seg_ids, gain_attn, w_query, kv_weight, w_out, gain_ffn, w_gate, w_up, w_down, d_out
):
    rows = tokens.shape[0]
    scale_factor = 1.0 / math.sqrt(HD)
    offset = lax.axis_index("seq") * rows
    places, cos_table, sin_table = place_tables(seg_ids)
    own_places = lax.dynamic_slice_in_dim(places, offset, rows, 0)
    own_segs = lax.dynamic_slice_in_dim(seg_ids, offset, rows, 0)
    own_cos = lax.dynamic_slice_in_dim(cos_table, offset, rows, 0)
    own_sin = lax.dynamic_slice_in_dim(sin_table, offset, rows, 0)
    allowed = (own_segs[:, None] == seg_ids[None, :]) & (own_places[:, None] >= places[None, :])
    full_query, full_out, full_kv, full_gain_one = (
        lax.all_gather(w_query, ("dp", "seq"), axis=0, tiled=True),
        lax.all_gather(w_out, ("dp", "seq"), axis=1, tiled=True),
        lax.all_gather(kv_weight, ("dp", "seq"), axis=0, tiled=True),
        lax.all_gather(gain_attn, ("dp", "seq"), axis=0, tiled=True),
    )
    gain_one = full_gain_one.astype(jnp.float32)
    inputs = tokens.astype(jnp.float32)
    rms_one = lax.rsqrt(jnp.mean(inputs * inputs, axis=-1, keepdims=True) + EPS)
    norm_one = inputs * rms_one
    act_one = (norm_one * gain_one).astype(jnp.bfloat16)
    query_pre = matmul(act_one, full_query)
    heads = query_pre.shape[1] // HD
    kv_pre = matmul(act_one, full_kv)
    queries = (
        rotate(query_pre.reshape(rows, heads, HD), own_cos[:, None, :], own_sin[:, None, :])
        * scale_factor
    ).astype(jnp.bfloat16)
    own_kv = jnp.concatenate(
        [rotate(kv_pre[:, :HD], own_cos, own_sin), kv_pre[:, HD:]], axis=1
    ).astype(jnp.bfloat16)
    all_kv = lax.all_gather(own_kv, "seq", axis=0, tiled=True)
    keys = all_kv[:, :HD]
    values_all = all_kv[:, HD:]
    scores = jnp.einsum("rhd,kd->hrk", queries, keys, preferred_element_type=jnp.float32)
    scores = jnp.where(allowed[None], scores, NEG)
    top_score = jnp.max(scores, axis=-1, keepdims=True)
    expd = jnp.exp(scores - top_score)
    total = jnp.sum(expd, axis=-1, keepdims=True)
    log_total = top_score + jnp.log(total)
    probs_low = (expd / total).astype(jnp.bfloat16)
    mixed = (
        jnp.einsum("hrk,kd->rhd", probs_low, values_all, preferred_element_type=jnp.float32)
        .reshape(rows, heads * HD)
        .astype(jnp.bfloat16)
    )
    attn = lax.psum(matmul(mixed, full_out), "tensor")
    resid = inputs + attn
    full_gate, full_up, full_down, full_gain_two = (
        lax.all_gather(w_gate, ("dp", "seq"), axis=0, tiled=True),
        lax.all_gather(w_up, ("dp", "seq"), axis=0, tiled=True),
        lax.all_gather(w_down, ("dp", "seq"), axis=1, tiled=True),
        lax.all_gather(gain_ffn, ("dp", "seq"), axis=0, tiled=True),
    )
    gain_two = full_gain_two.astype(jnp.float32)
    rms_two = lax.rsqrt(jnp.mean(resid * resid, axis=-1, keepdims=True) + EPS)
    norm_two = resid * rms_two
    act_two = (norm_two * gain_two).astype(jnp.bfloat16)
    gate = matmul(act_two, full_gate)
    up_val = matmul(act_two, full_up)
    gelu_val, gelu_pull = jax.vjp(gelu_tanh, gate)
    hidden = (gelu_val * up_val).astype(jnp.bfloat16)
    ffn = lax.psum(matmul(hidden, full_down).astype(jnp.bfloat16), "tensor").astype(jnp.float32)
    out = (resid + ffn).astype(jnp.bfloat16)
    back_gate, back_up, back_down = (
        lax.all_gather(w_gate, ("dp", "seq"), axis=0, tiled=True),
        lax.all_gather(w_up, ("dp", "seq"), axis=0, tiled=True),
        lax.all_gather(w_down, ("dp", "seq"), axis=1, tiled=True),
    )
    d_hidden = matmul_nt(d_out, back_down)
    grad_down = matmul_tn(hidden, d_out)
    d_gate = gelu_pull(d_hidden * up_val)[0].astype(jnp.bfloat16)
    d_up = (d_hidden * gelu_val).astype(jnp.bfloat16)
    grad_gate = matmul_tn(act_two, d_gate)
    grad_up = matmul_tn(act_two, d_up)
    d_act_two = lax.psum(matmul_nt(d_gate, back_gate) + matmul_nt(d_up, back_up), "tensor")
    grad_gain_two = jnp.sum(d_act_two * norm_two, axis=0)
    d_resid = d_out.astype(jnp.float32) + norm_back(d_act_two, norm_two, rms_two, gain_two)
    ffn_grads = (
        lax.psum_scatter(
            grad_gate.astype(jnp.bfloat16), ("dp", "seq"), scatter_dimension=0, tiled=True
        ).astype(jnp.float32),
        lax.psum_scatter(
            grad_up.astype(jnp.bfloat16), ("dp", "seq"), scatter_dimension=0, tiled=True
        ).astype(jnp.float32),
        lax.psum_scatter(
            grad_down.astype(jnp.bfloat16), ("dp", "seq"), scatter_dimension=1, tiled=True
        ).astype(jnp.float32),
        lax.psum_scatter(
            grad_gain_two.astype(jnp.bfloat16), ("dp", "seq"), scatter_dimension=0, tiled=True
        ).astype(jnp.float32),
    )
    back_query, back_out, back_kv = (
        lax.all_gather(w_query, ("dp", "seq"), axis=0, tiled=True),
        lax.all_gather(w_out, ("dp", "seq"), axis=1, tiled=True),
        lax.all_gather(kv_weight, ("dp", "seq"), axis=0, tiled=True),
    )
    d_attn = d_resid.astype(jnp.bfloat16)
    grad_out = matmul_tn(mixed, d_attn)
    d_mixed = matmul_nt(d_attn, back_out).astype(jnp.bfloat16).reshape(rows, heads, HD)
    scores_again = jnp.einsum("rhd,kd->hrk", queries, keys, preferred_element_type=jnp.float32)
    probs = jnp.where(allowed[None], jnp.exp(scores_again - log_total), 0.0)
    d_probs = jnp.einsum("rhd,kd->hrk", d_mixed, values_all, preferred_element_type=jnp.float32)
    delta = jnp.sum(probs * d_probs, axis=-1, keepdims=True)
    d_scores = (probs * (d_probs - delta)).astype(jnp.bfloat16)
    d_queries = (
        jnp.einsum("hrk,kd->rhd", d_scores, keys, preferred_element_type=jnp.float32) * scale_factor
    )
    d_query_pre = (
        rotate_back(d_queries, own_cos[:, None, :], own_sin[:, None, :])
        .reshape(rows, heads * HD)
        .astype(jnp.bfloat16)
    )
    d_keys_part = jnp.einsum("hrk,rhd->kd", d_scores, queries, preferred_element_type=jnp.float32)
    d_values_part = jnp.einsum(
        "hrk,rhd->kd", probs.astype(jnp.bfloat16), d_mixed, preferred_element_type=jnp.float32
    )
    own_kv_grad = lax.psum_scatter(
        jnp.concatenate([d_keys_part, d_values_part], axis=1).astype(jnp.bfloat16),
        "seq",
        scatter_dimension=0,
        tiled=True,
    )
    d_act_query = matmul_nt(d_query_pre, back_query)
    d_act_sum, kv_grad = (
        lax.psum(d_act_query.astype(jnp.bfloat16), "tensor").astype(jnp.float32),
        lax.psum(own_kv_grad, "tensor").astype(jnp.float32),
    )
    d_kv_pre = jnp.concatenate(
        [rotate_back(kv_grad[:, :HD], own_cos, own_sin), kv_grad[:, HD:]], axis=1
    ).astype(jnp.bfloat16)
    d_act_one = d_act_sum + matmul_nt(d_kv_pre, back_kv)
    grad_query = matmul_tn(act_one, d_query_pre)
    grad_kv = matmul_tn(act_one, d_kv_pre)
    grad_gain_one = jnp.sum(d_act_one * norm_one, axis=0)
    d_tokens = d_resid + norm_back(d_act_one, norm_one, rms_one, gain_one)
    attn_grads = (
        lax.psum_scatter(
            grad_query.astype(jnp.bfloat16), ("dp", "seq"), scatter_dimension=0, tiled=True
        ).astype(jnp.float32),
        lax.psum_scatter(
            grad_out.astype(jnp.bfloat16), ("dp", "seq"), scatter_dimension=1, tiled=True
        ).astype(jnp.float32),
        lax.psum_scatter(
            grad_kv.astype(jnp.bfloat16), ("dp", "seq"), scatter_dimension=0, tiled=True
        ).astype(jnp.float32),
        lax.psum_scatter(
            grad_gain_one.astype(jnp.bfloat16), ("dp", "seq"), scatter_dimension=0, tiled=True
        ).astype(jnp.float32),
    )
    return (
        out,
        d_tokens,
        attn_grads[3],
        attn_grads[0],
        attn_grads[2],
        attn_grads[1],
        ffn_grads[3],
        ffn_grads[0],
        ffn_grads[1],
        ffn_grads[2],
    )


MESH = pl.DeviceIdType.MESH
VMEM_LIMIT = 66000 * 1024


class Place:
    def __init__(self):
        self.dp = lax.axis_index("dp")
        self.seq = lax.axis_index("seq")
        self.z = lax.axis_index("tensor")
        self.core = lax.rem(self.dp, 2)
        self.chip = lax.div(self.dp, 2)

    def device(self, across, other):
        chip = (self.chip + across) % 2
        seq = (self.seq + across // 2) % 2
        core = (self.core + other) % 2
        return chip * 2 + core, seq, self.z

    def shard(self, across, other):
        dp, seq, _ = self.device(across, other)
        return dp * 2 + seq


def greet(peers):
    barrier = pltpu.get_barrier_semaphore()
    for peer in peers:
        pl.semaphore_signal(barrier, inc=1, device_id=peer, device_id_type=MESH)
    pl.semaphore_wait(barrier, len(peers))


def remote(src, dst, send, recv, peer):
    return pltpu.make_async_remote_copy(
        src_ref=src, dst_ref=dst, send_sem=send, recv_sem=recv, device_id=peer, device_id_type=MESH
    )


def scatter_kernel(rows, width, counts, nt, shared, act, *refs):
    w0 = refs[0]
    w1 = w0 if shared else refs[1]
    tiny, out, tiny_all, held, sib_out, sib_in, from_x, from_y, sib_send, sib_recv = refs[1 if shared else 2 :][:10]
    x_send, x_recv, y_send, y_recv, tiny_send, tiny_recv = refs[-6:]
    here = Place()
    sib, xdev, ydev = here.device(0, 1), here.device(1, 0), here.device(2, 0)
    peers = [here.device(a, o) for a in range(4) for o in range(2) if a + o > 0]
    greet(peers)
    weights = (w0, w1)

    def tiny_copy(at):
        across, other = (at + 1) // 2, (at + 1) % 2
        return remote(tiny.at[here.shard(across, other)], tiny_all.at[here.shard(0, 0)],
                      tiny_send.at[at], tiny_recv.at[at], peers[at])

    for at in range(7):
        tiny_copy(at).start()
    tiny_all[here.shard(0, 0)] = tiny[here.shard(0, 0)]
    half_cols = counts * width
    stages = (((3, 0), (3, 1)), ((1, 0), (2, 1)), ((0, 0), (0, 1)), ((1, 1), (2, 0)))

    def product(across, other, half, at):
        row = pl.multiple_of(here.shard(across, other) * rows, rows)
        first = half * half_cols if shared else 0
        cols = pl.ds(pl.multiple_of(first + at * width, width), width)
        block = act[pl.ds(row, rows), :]
        if nt:
            return lax.dot_general(block, weights[half][cols, :], (((1,), (1,)), ((), ())),
                                   preferred_element_type=jnp.float32)
        return jnp.dot(block, weights[half][:, cols], preferred_element_type=jnp.float32)

    def to_sib(stage, stream, at):
        return remote(sib_out.at[stage, stream, at], sib_in.at[stage, stream, at],
                      sib_send.at[stage, stream, at], sib_recv.at[stage, stream, at], sib)

    def to_x(step, at, stage):
        return remote(held.at[stage, 0, at], from_x.at[step, at], x_send.at[step, at],
                      x_recv.at[step, at], xdev)

    def to_y(step, at, stage):
        return remote(held.at[stage, 1, at], from_y.at[step, at], y_send.at[step, at],
                      y_recv.at[step, at], ydev)

    step_of = {0: 0, 1: 1, 3: 2}

    for stage, streams in enumerate(stages):
        def compute(at, stage=stage, streams=streams):
            for stream, (across, half) in enumerate(streams):
                sib_out[stage, stream, at] = product(across, 1, half, at).astype(jnp.bfloat16)
                held[stage, stream, at] = product(across, 0, half, at).astype(jnp.bfloat16)

        def finish(at, stage=stage):
            for stream in range(2):
                to_sib(stage, stream, at).wait_recv()
                total = held[stage, stream, at].astype(jnp.float32) + sib_in[
                    stage, stream, at].astype(jnp.float32)
                if stage == 3:
                    if stream == 0:
                        to_y(0, at, 0).wait_recv()
                        total += from_y[0, at].astype(jnp.float32)
                    else:
                        to_x(0, at, 0).wait_recv()
                        total += from_x[0, at].astype(jnp.float32)
                if stage == 2:
                    cols = pl.ds(pl.multiple_of(stream * half_cols + at * width, width), width)
                    out[:, cols] = total
                else:
                    held[stage, stream, at] = total.astype(jnp.bfloat16)
            if stage != 2:
                to_x(step_of[stage], at, stage).start()
                to_y(step_of[stage], at, stage).start()

        def body(at, _, compute=compute, finish=finish, stage=stage):
            compute(at)
            for stream in range(2):
                to_sib(stage, stream, at).start()

            @pl.when(at > 0)
            def _():
                finish(at - 1)
            return 0

        lax.fori_loop(0, counts, body, 0)
        finish(counts - 1)

    def last(at, _):
        for half in range(2):
            cols = pl.ds(pl.multiple_of(half * half_cols + at * width, width), width)
            xs, ys = (1, 2) if half == 0 else (2, 1)
            to_x(xs, at, 0).wait_recv()
            to_y(ys, at, 0).wait_recv()
            out[:, cols] += from_x[xs, at].astype(jnp.float32) + from_y[ys, at].astype(jnp.float32)
        for stage in range(4):
            for stream in range(2):
                to_sib(stage, stream, at).wait_send()
        for step in range(3):
            to_x(step, at, 0).wait_send()
            to_y(step, at, 0).wait_send()
        return 0

    lax.fori_loop(0, counts, last, 0)
    for at in range(7):
        tiny_copy(at).wait()


def scatter_product(act, weights, tiny, width, nt, cid):
    total, depth = act.shape
    rows = total // 8
    shared = len(weights) == 1
    half = weights[0].shape[0 if nt else 1] // (2 if shared else 1)
    counts = half // width
    low = jnp.bfloat16
    dma = pltpu.SemaphoreType.DMA
    vm = pl.BlockSpec(memory_space=pltpu.VMEM)
    return pl.pallas_call(
        functools.partial(scatter_kernel, rows, width, counts, nt, shared),
        out_shape=(
            jax.ShapeDtypeStruct((rows, 2 * half), jnp.float32),
            jax.ShapeDtypeStruct(tiny.shape, jnp.float32),
        ),
        in_specs=[vm] * (2 + len(weights)),
        out_specs=(vm, vm),
        scratch_shapes=[
            pltpu.VMEM((4, 2, counts, rows, width), low),
            pltpu.VMEM((4, 2, counts, rows, width), low),
            pltpu.VMEM((4, 2, counts, rows, width), low),
            pltpu.VMEM((3, counts, rows, width), low),
            pltpu.VMEM((3, counts, rows, width), low),
            dma((4, 2, counts)), dma((4, 2, counts)),
            dma((3, counts)), dma((3, counts)), dma((3, counts)), dma((3, counts)),
            dma((7,)), dma((7,)),
        ],
        compiler_params=pltpu.CompilerParams(collective_id=cid, has_side_effects=True,
                                             vmem_limit_bytes=VMEM_LIMIT),
        name=f"scatter_product_{cid}",
    )(act, *weights, tiny)


def line_kernel(chunk, counts, own, out, from_end, mine, from_mid, end_send, end_recv, mid_send, mid_recv,
                back_send, back_recv):
    here = Place()
    z = here.z
    outer = jnp.logical_or(z == 0, z == 3)
    mate = z + 1 - 2 * (z % 2)
    other = 3 - z
    mate_dev = (here.dp, here.seq, mate)
    other_dev = (here.dp, here.seq, other)

    def rows(at):
        return pl.ds(pl.multiple_of(at * chunk, chunk), chunk)

    def up(at):
        return remote(own.at[rows(at), :], from_end.at[at], end_send.at[at], end_recv.at[at], mate_dev)

    def over(at):
        return remote(mine.at[at], from_mid.at[at], mid_send.at[at], mid_recv.at[at], other_dev)

    def down(at):
        return remote(out.at[rows(at), :], out.at[rows(at), :], back_send.at[at], back_recv.at[at], mate_dev)

    barrier = pltpu.get_barrier_semaphore()
    pl.semaphore_signal(barrier, inc=1, device_id=mate_dev, device_id_type=MESH)

    @pl.when(outer)
    def _():
        pl.semaphore_wait(barrier, 1)

        def send(at, _):
            up(at).start()
            return 0

        def take(at, _):
            up(at).wait_send()
            down(at).wait_recv()
            return 0

        lax.fori_loop(0, counts, send, 0)
        lax.fori_loop(0, counts, take, 0)

    @pl.when(jnp.logical_not(outer))
    def _():
        pl.semaphore_signal(barrier, inc=1, device_id=other_dev, device_id_type=MESH)
        pl.semaphore_wait(barrier, 2)

        def second(at):
            over(at).wait_recv()
            out[rows(at), :] = (mine[at].astype(jnp.float32) + from_mid[at].astype(jnp.float32)).astype(out.dtype)
            down(at).start()

        def first(at, _):
            up(at).wait_recv()
            mine[at] = (own[rows(at), :].astype(jnp.float32) + from_end[at].astype(jnp.float32)).astype(mine.dtype)
            over(at).start()

            @pl.when(at > 1)
            def _():
                second(at - 2)
            return 0

        lax.fori_loop(0, counts, first, 0)
        second(counts - 2)
        second(counts - 1)

        def drain(at, _):
            over(at).wait_send()
            down(at).wait_send()
            return 0

        lax.fori_loop(0, counts, drain, 0)


def line_sum(own, cid, counts=16):
    total, width = own.shape
    chunk = total // counts
    low = own.dtype
    dma = pltpu.SemaphoreType.DMA
    vm = pl.BlockSpec(memory_space=pltpu.VMEM)
    buf = pltpu.VMEM((counts, chunk, width), low)
    return pl.pallas_call(
        functools.partial(line_kernel, chunk, counts),
        out_shape=jax.ShapeDtypeStruct((total, width), low),
        in_specs=[vm],
        out_specs=vm,
        scratch_shapes=[buf, buf, buf] + [dma((counts,))] * 6,
        compiler_params=pltpu.CompilerParams(collective_id=cid, has_side_effects=True,
                                             vmem_limit_bytes=VMEM_LIMIT),
        name=f"line_sum_{cid}",
    )(own)


def gather_kernel(rows, width, counts, act_t, w0, w1, g0, g1, tiny, d_act, gw0, gw1, tiny_all, got,
                  x_send, x_recv, y_send, y_recv, sib_send, sib_recv, tiny_send, tiny_recv):
    here = Place()
    sib, xdev, ydev = here.device(0, 1), here.device(1, 0), here.device(2, 0)
    peers = [here.device(a, o) for a in range(4) for o in range(2) if a + o > 0]
    greet(peers)
    core = here.core
    own, weights, grads = (g0, g1), (w0, w1), (gw0, gw1)
    stages = (((1, 0), (2, 1)), ((1, 1), (2, 0)), ((3, 1), (3, 0)))

    def part(half, at):
        return own[half].at[:, pl.ds(pl.multiple_of(at * width, width), width)]

    def x_copy(step, at):
        src = part(step, at) if step < 2 else got.at[2, core, 1, at]
        dst = got.at[1, core, step, at] if step < 2 else got.at[3, core, 1, at]
        return remote(src, dst, x_send.at[step, at], x_recv.at[step, at], xdev)

    def y_copy(step, at):
        src = part(1 - step, at) if step < 2 else got.at[1, core, 0, at]
        dst = got.at[2, core, 1 - step, at] if step < 2 else got.at[3, core, 0, at]
        return remote(src, dst, y_send.at[step, at], y_recv.at[step, at], ydev)

    def sib_copy(stage, stream, at):
        if stage == 3:
            src, (across, half) = part(stream, at), (0, stream)
        else:
            across, half = stages[stage][stream]
            src = got.at[across, core, half, at]
        return remote(src, got.at[across, core, half, at], sib_send.at[stage, stream, at],
                      sib_recv.at[stage, stream, at], sib)

    def tiny_copy(at, peer):
        return remote(tiny, tiny_all.at[here.shard(0, 0)], tiny_send.at[at], tiny_recv.at[at], peer)

    def begin(at, _):
        x_copy(0, at).start()
        y_copy(0, at).start()
        return 0

    def begin_sib(at, _):
        sib_copy(3, 0, at).start()
        sib_copy(3, 1, at).start()
        return 0

    for at, peer in enumerate(peers):
        tiny_copy(at, peer).start()
    lax.fori_loop(0, counts, begin, 0)
    lax.fori_loop(0, counts, begin_sib, 0)
    tiny_all[here.shard(0, 0)] = tiny[...]
    d_act[...] = jnp.zeros_like(d_act)

    def blocks(across, half, at, mine):
        cols = pl.ds(pl.multiple_of(at * width, width), width)
        gained = None
        for other in range(2):
            row = pl.ds(pl.multiple_of(here.shard(across, other) * rows, rows), rows)
            if mine and other == 0:
                block = own[half][:, cols]
            else:
                block = got[across, (core + other) % 2, half, at]
            d_act[row, :] += lax.dot_general(block, weights[half][:, cols], (((1,), (1,)), ((), ())),
                                             preferred_element_type=jnp.float32)
            more = jnp.dot(act_t[:, row], block, preferred_element_type=jnp.float32)
            gained = more if gained is None else gained + more
        if mine:
            grads[half][:, cols] = gained
        else:
            grads[half][:, cols] += gained

    def own_step(at, _):
        for half in range(2):
            sib_copy(3, half, at).wait_recv()
            blocks(0, half, at, True)
        return 0

    lax.fori_loop(0, counts, own_step, 0)

    def work(stage, at):
        for stream, (across, half) in enumerate(stages[stage]):
            sib_copy(stage, stream, at).wait_recv()
            blocks(across, half, at, False)

    for stage in range(3):
        def body(at, _, stage=stage):
            x_copy(stage, at).wait_recv()
            sib_copy(stage, 0, at).start()
            y_copy(stage, at).wait_recv()
            sib_copy(stage, 1, at).start()
            if stage < 2:
                x_copy(stage + 1, at).start()
                y_copy(stage + 1, at).start()

            @pl.when(at > 0)
            def _():
                work(stage, at - 1)
            return 0

        lax.fori_loop(0, counts, body, 0)
        work(stage, counts - 1)

    def drain(at, _):
        for step in range(3):
            x_copy(step, at).wait_send()
            y_copy(step, at).wait_send()
        for stage in range(4):
            sib_copy(stage, 0, at).wait_send()
            sib_copy(stage, 1, at).wait_send()
        return 0

    lax.fori_loop(0, counts, drain, 0)
    for at, peer in enumerate(peers):
        tiny_copy(at, peer).wait()


def gather_product(act_t, w0, w1, g0, g1, tiny, width, cid):
    depth, total = act_t.shape
    rows, half = g0.shape
    counts = half // width
    low = jnp.bfloat16
    dma = pltpu.SemaphoreType.DMA
    vm = pl.BlockSpec(memory_space=pltpu.VMEM)
    f32 = jnp.float32
    return pl.pallas_call(
        functools.partial(gather_kernel, rows, width, counts),
        out_shape=(
            jax.ShapeDtypeStruct((total, depth), f32),
            jax.ShapeDtypeStruct((depth, half), f32),
            jax.ShapeDtypeStruct((depth, half), f32),
            jax.ShapeDtypeStruct((8,) + tiny.shape, f32),
        ),
        in_specs=[vm] * 6,
        out_specs=(vm,) * 4,
        scratch_shapes=[
            pltpu.VMEM((4, 2, 2, counts, rows, width), low),
            dma((3, counts)), dma((3, counts)), dma((3, counts)), dma((3, counts)),
            dma((4, 2, counts)), dma((4, 2, counts)), dma((7,)), dma((7,)),
        ],
        compiler_params=pltpu.CompilerParams(collective_id=cid, has_side_effects=True,
                                             vmem_limit_bytes=VMEM_LIMIT),
        name=f"gather_product_{cid}",
    )(act_t, w0, w1, g0, g1, tiny)


def turn_kernel(rows, cols, back, src, out, own_sem, send, recv):
    here = Place()
    peers = [(a, o) for a in (3, 1, 2, 0) for o in range(2) if a + o > 0]
    greet([here.device(a, o) for a, o in peers])

    def by_row(ref, shard):
        return ref.at[pl.ds(pl.multiple_of(shard * rows, rows), rows), :]

    def by_col(ref, shard):
        return ref.at[:, pl.ds(pl.multiple_of(shard * cols, cols), cols)]

    take, put = (by_row, by_col) if back else (by_col, by_row)
    me = here.shard(0, 0)

    def copy(at):
        across, other = peers[at]
        return remote(take(src, here.shard(across, other)), put(out, me), send.at[at], recv.at[at],
                      here.device(across, other))

    for at in range(7):
        copy(at).start()
    own = pltpu.make_async_copy(take(src, me), put(out, me), own_sem)
    own.start()
    own.wait()
    for at in range(7):
        copy(at).wait()


def turn(src, back, cid):
    rows, cols = (src.shape[0] // 8, src.shape[1]) if back else (src.shape[0], src.shape[1] // 8)
    shape = (rows, 8 * cols) if back else (8 * rows, cols)
    dma = pltpu.SemaphoreType.DMA
    vm = pl.BlockSpec(memory_space=pltpu.VMEM)
    return pl.pallas_call(
        functools.partial(turn_kernel, rows, cols, back),
        out_shape=jax.ShapeDtypeStruct(shape, src.dtype),
        in_specs=[vm],
        out_specs=vm,
        scratch_shapes=[dma(()), dma((7,)), dma((7,))],
        compiler_params=pltpu.CompilerParams(collective_id=cid, has_side_effects=True,
                                             vmem_limit_bytes=VMEM_LIMIT),
        name=f"turn_{cid}",
    )(src)


AXES = ("dp", "seq")
LANES = 128


def gather_rows(block):
    return lax.all_gather(block, AXES, axis=0, tiled=True)


def lane_sums(values):
    return jnp.sum(values.reshape(values.shape[0], -1, LANES), axis=1)


def pack_rows(values):
    parts = values.reshape(8, -1, LANES)
    return jnp.pad(parts, ((0, 0), (0, 8 - parts.shape[1]), (0, 0)))


def acts_move(
    tokens, seg_ids, gain_attn, w_query, kv_weight, w_out, gain_ffn, w_gate, w_up, w_down, d_out
):
    low = jnp.bfloat16
    rows, width = tokens.shape
    seqs = lax.axis_size("seq")
    parts = lax.axis_size("dp") * seqs
    scale_factor = 1.0 / math.sqrt(HD)
    offset = lax.axis_index("seq") * rows
    places, cos_table, sin_table = place_tables(seg_ids)
    own_places = lax.dynamic_slice_in_dim(places, offset, rows, 0)
    own_segs = lax.dynamic_slice_in_dim(seg_ids, offset, rows, 0)
    own_cos = lax.dynamic_slice_in_dim(cos_table, offset, rows, 0)
    own_sin = lax.dynamic_slice_in_dim(sin_table, offset, rows, 0)
    allowed = (own_segs[:, None] == seg_ids[None, :]) & (own_places[:, None] >= places[None, :])
    gain_one = gain_attn.astype(jnp.float32)
    gain_two = gain_ffn.astype(jnp.float32)
    qw = w_query.shape[1]
    heads = qw // HD
    ff = w_gate.shape[1]

    none = jnp.zeros((8, 8, LANES), jnp.float32)
    x_low = turn(tokens, False, 1)
    g_low = turn(d_out, False, 2)
    x_col = x_low.astype(jnp.float32)
    own_x = tokens.astype(jnp.float32)
    rms_one = lax.rsqrt(jnp.mean(own_x * own_x, axis=-1, keepdims=True) + EPS)
    act_one = (x_col * gain_one).astype(low)
    w_qkv = jnp.concatenate([w_query, kv_weight], axis=1)
    qkv = scatter_product(act_one, (w_qkv,), none, 256, False, 3)[0] * rms_one
    queries = (
        rotate(qkv[:, :qw].reshape(rows, heads, HD), own_cos[:, None, :], own_sin[:, None, :])
        * scale_factor
    ).astype(low)
    rms_high = rms_one.astype(low)
    rms_rest = (rms_one - rms_high.astype(jnp.float32)).astype(low)
    half = (rows, LANES // 2)
    own_kv = jnp.concatenate(
        [
            rotate(qkv[:, qw : qw + HD], own_cos, own_sin).astype(low),
            qkv[:, qw + HD :].astype(low),
            jnp.broadcast_to(rms_high, half),
            jnp.broadcast_to(rms_rest, half),
        ],
        axis=1,
    )
    all_kv = lax.all_gather(own_kv, "seq", axis=0, tiled=True)
    keys = all_kv[:, :HD]
    values_all = all_kv[:, HD : 2 * HD]
    rms_group = all_kv[:, 2 * HD : 2 * HD + 1].astype(jnp.float32) + all_kv[
        :, 2 * HD + LANES // 2 : 2 * HD + LANES // 2 + 1
    ].astype(jnp.float32)
    scores = jnp.einsum("rhd,kd->hrk", queries, keys, preferred_element_type=jnp.float32)
    scores = jnp.where(allowed[None], scores, NEG)
    top_score = jnp.max(scores, axis=-1, keepdims=True)
    expd = jnp.exp(scores - top_score)
    total = jnp.sum(expd, axis=-1, keepdims=True)
    probs = expd / total
    probs_low = probs.astype(low)
    mixed = (
        jnp.einsum("hrk,kd->rhd", probs_low, values_all, preferred_element_type=jnp.float32)
        .reshape(rows, heads * HD)
        .astype(low)
    )
    mixed_all = gather_rows(mixed)
    attn = line_sum(matmul(mixed_all, w_out).astype(low), 4)
    d_hidden = scatter_product(g_low, (w_down,), none, 512, True, 5)[0]
    resid = x_col + attn.astype(jnp.float32)
    act_two = (resid * gain_two).astype(low)
    squares = pack_rows(jnp.sum(resid * resid, axis=-1))
    both, squares_all = scatter_product(act_two, (w_gate, w_up), squares, 512, False, 6)
    mean_two = jnp.sum(squares_all[:, : rows // LANES], axis=0).reshape(rows, 1) / width
    rms_two = lax.rsqrt(mean_two + EPS)
    gate = both[:, :ff] * rms_two
    up_val = both[:, ff : 2 * ff] * rms_two
    gelu_val, gelu_pull = jax.vjp(gelu_tanh, gate)
    hidden = (gelu_val * up_val).astype(low)
    d_gate = gelu_pull(d_hidden * up_val)[0]
    d_up = d_hidden * gelu_val
    dots_two = jnp.sum(d_gate * gate + d_up * up_val, axis=-1, keepdims=True) * (
        rms_two * rms_two / width
    )
    dots_own = jnp.pad(dots_two.reshape(-1, LANES), ((0, 8 - rows // LANES), (0, 0)))
    d_act_two, grad_gate, grad_up, dots_all = gather_product(
        act_two.T,
        w_gate,
        w_up,
        (d_gate * rms_two).astype(low),
        (d_up * rms_two).astype(low),
        dots_own,
        512,
        7,
    )
    hidden_all = gather_rows(hidden)
    dot_two = dots_all[:, : rows // LANES].reshape(parts * rows, 1)
    grad_gain_two = jnp.sum(d_act_two * resid, axis=0)
    d_norm = line_sum((d_act_two * gain_two - resid * dot_two).astype(low), 8)
    d_resid = g_low.astype(jnp.float32) + d_norm.astype(jnp.float32)
    d_attn = d_resid.astype(low)
    d_mixed = scatter_product(d_attn, (w_out,), none, 256, True, 9)[0]
    d_mixed = d_mixed.astype(low).reshape(rows, heads, HD)
    grad_down = matmul_tn(hidden_all, g_low)
    ffn = lax.psum(matmul(hidden_all, w_down).astype(low), "tensor")
    out = turn((resid + ffn.astype(jnp.float32)).astype(low), True, 10)
    grad_out = matmul_tn(mixed_all, d_attn)

    d_probs = jnp.einsum("rhd,kd->hrk", d_mixed, values_all, preferred_element_type=jnp.float32)
    delta = jnp.sum(probs * d_probs, axis=-1, keepdims=True)
    d_scores = (probs * (d_probs - delta)).astype(low)
    d_queries = (
        jnp.einsum("hrk,kd->rhd", d_scores, keys, preferred_element_type=jnp.float32) * scale_factor
    )
    d_query_pre = (
        rotate_back(d_queries, own_cos[:, None, :], own_sin[:, None, :]).reshape(rows, heads * HD)
        * rms_one
    ).astype(low)
    query_dots = lane_sums(
        (d_queries * queries.astype(jnp.float32)).reshape(rows, heads * HD)
    ) * (rms_one * rms_one / (width * scale_factor))
    d_keys = jnp.einsum("hrk,rhd->kd", d_scores, queries, preferred_element_type=jnp.float32)
    d_values = jnp.einsum("hrk,rhd->kd", probs_low, d_mixed, preferred_element_type=jnp.float32)
    kv_dots = lane_sums(
        jnp.concatenate(
            [d_keys * keys.astype(jnp.float32), d_values * values_all.astype(jnp.float32)], axis=1
        )
    ) * (rms_group * rms_group / width)
    d_kv = jnp.concatenate(
        [
            rotate_back(d_keys, cos_table, sin_table) * rms_group,
            d_values * rms_group,
            kv_dots,
        ],
        axis=1,
    ).astype(low)
    kvw = d_kv.shape[1]
    pieces = [d_kv[at * rows : (at + 1) * rows] for at in range(seqs)]
    home = gather_rows(
        jnp.concatenate([d_query_pre, query_dots.astype(low)] + pieces, axis=1)
    )
    d_query_all = home[:, :qw]
    kv_parts = home[:, qw + LANES :].reshape(parts // seqs, seqs, rows, seqs, kvw)
    kv_sum = jnp.sum(kv_parts.astype(jnp.float32), axis=1)
    kv_sum = jnp.transpose(kv_sum, (0, 2, 1, 3)).reshape(parts * rows, kvw)
    d_kv_all = kv_sum[:, : 2 * HD].astype(low)
    dot_one = jnp.sum(
        home[:, qw : qw + LANES].astype(jnp.float32) + kv_sum[:, 2 * HD :], axis=-1, keepdims=True
    )
    d_act_one = matmul_nt(d_query_all, w_query) + matmul_nt(d_kv_all, kv_weight)
    grad_gain_one = jnp.sum(d_act_one * x_col, axis=0)
    d_norm_one = line_sum((d_act_one * gain_one - x_col * dot_one).astype(low), 11)
    d_tokens = turn((d_resid + d_norm_one.astype(jnp.float32)).astype(low), True, 12)
    grad_query = matmul_tn(act_one, d_query_all)
    grad_kv = lax.psum(matmul_tn(act_one, d_kv_all).astype(low), "tensor").astype(jnp.float32)
    gains = lax.psum(jnp.stack([grad_gain_one, grad_gain_two]), "tensor")
    return (
        out,
        d_tokens.astype(jnp.float32),
        gains[0],
        grad_query,
        grad_kv,
        grad_out,
        gains[1],
        grad_gate,
        grad_up,
        grad_down,
    )


def solution(mesh):
    in_specs = (
        P(("dp", "seq"), None),
        P("dp"),
        P(("dp", "seq")),
        P(("dp", "seq"), "tensor"),
        P(("dp", "seq"), None),
        P("tensor", ("dp", "seq")),
        P(("dp", "seq")),
        P(("dp", "seq"), "tensor"),
        P(("dp", "seq"), "tensor"),
        P("tensor", ("dp", "seq")),
        P(("dp", "seq"), None),
    )
    out_specs = (
        P(("dp", "seq"), None),
        P(("dp", "seq"), None),
        P(("dp", "seq")),
        P(("dp", "seq"), "tensor"),
        P(("dp", "seq"), None),
        P("tensor", ("dp", "seq")),
        P(("dp", "seq")),
        P(("dp", "seq"), "tensor"),
        P(("dp", "seq"), "tensor"),
        P("tensor", ("dp", "seq")),
    )

    def shards(*arrays):
        tokens = arrays[0]
        sizes = tuple(mesh.shape[name] for name in ("dp", "seq", "tensor"))
        count = tokens.shape[0] * sizes[0] * sizes[1]
        plan = acts_move if sizes == (4, 2, 4) and count <= tokens.shape[1] else weights_move
        return plan(*arrays)

    return jax.shard_map(shards, mesh=mesh, in_specs=in_specs, out_specs=out_specs, check_vma=False)
```

```python
import functools
import math

import jax
import jax.numpy as jnp
from jax import lax
from jax.experimental import pallas as pl
from jax.experimental.pallas import tpu as pltpu
from jax.sharding import PartitionSpec as P

HD = 256


EPS = 1e-06
NEG = -1e30


def place_tables(segs):
    length = segs.shape[0]
    index = jnp.arange(length, dtype=jnp.int32)
    flags = jnp.concatenate([jnp.ones((1,), dtype=bool), segs[1:] != segs[:-1]])
    starts = lax.cummax(jnp.where(flags, index, jnp.zeros_like(index)), axis=0)
    places = index - starts
    half_size = HD // 2
    freqs = jnp.exp(jnp.arange(half_size, dtype=jnp.float32) * (-math.log(10000.0) / half_size))
    angles = places.astype(jnp.float32)[:, None] * freqs[None, :]
    return (places, jnp.cos(angles), jnp.sin(angles))


def rotate(vector, cos_table, sin_table):
    half_size = vector.shape[-1] // 2
    leading = vector[..., :half_size]
    trailing = vector[..., half_size:]
    return jnp.concatenate(
        [leading * cos_table - trailing * sin_table, trailing * cos_table + leading * sin_table],
        axis=-1,
    )


def rotate_back(vector, cos_table, sin_table):
    half_size = vector.shape[-1] // 2
    leading = vector[..., :half_size]
    trailing = vector[..., half_size:]
    return jnp.concatenate(
        [leading * cos_table + trailing * sin_table, trailing * cos_table - leading * sin_table],
        axis=-1,
    )


def matmul(left, right):
    return jnp.dot(left, right, preferred_element_type=jnp.float32)


def matmul_nt(left, right):
    return lax.dot_general(
        left, right, (((1,), (1,)), ((), ())), preferred_element_type=jnp.float32
    )


def matmul_tn(left, right):
    return lax.dot_general(
        left, right, (((0,), (0,)), ((), ())), preferred_element_type=jnp.float32
    )


def gelu_tanh(values):
    return jax.nn.gelu(values, approximate=True)


def norm_back(d_act, normed, rms_val, gain_val):
    scaled = d_act * gain_val
    return rms_val * (scaled - normed * jnp.mean(scaled * normed, axis=-1, keepdims=True))


def weights_move(
    tokens, seg_ids, gain_attn, w_query, kv_weight, w_out, gain_ffn, w_gate, w_up, w_down, d_out
):
    rows = tokens.shape[0]
    scale_factor = 1.0 / math.sqrt(HD)
    offset = lax.axis_index("seq") * rows
    places, cos_table, sin_table = place_tables(seg_ids)
    own_places = lax.dynamic_slice_in_dim(places, offset, rows, 0)
    own_segs = lax.dynamic_slice_in_dim(seg_ids, offset, rows, 0)
    own_cos = lax.dynamic_slice_in_dim(cos_table, offset, rows, 0)
    own_sin = lax.dynamic_slice_in_dim(sin_table, offset, rows, 0)
    allowed = (own_segs[:, None] == seg_ids[None, :]) & (own_places[:, None] >= places[None, :])
    full_query, full_out, full_kv, full_gain_one = (
        lax.all_gather(w_query, ("dp", "seq"), axis=0, tiled=True),
        lax.all_gather(w_out, ("dp", "seq"), axis=1, tiled=True),
        lax.all_gather(kv_weight, ("dp", "seq"), axis=0, tiled=True),
        lax.all_gather(gain_attn, ("dp", "seq"), axis=0, tiled=True),
    )
    gain_one = full_gain_one.astype(jnp.float32)
    inputs = tokens.astype(jnp.float32)
    rms_one = lax.rsqrt(jnp.mean(inputs * inputs, axis=-1, keepdims=True) + EPS)
    norm_one = inputs * rms_one
    act_one = (norm_one * gain_one).astype(jnp.bfloat16)
    query_pre = matmul(act_one, full_query)
    heads = query_pre.shape[1] // HD
    kv_pre = matmul(act_one, full_kv)
    queries = (
        rotate(query_pre.reshape(rows, heads, HD), own_cos[:, None, :], own_sin[:, None, :])
        * scale_factor
    ).astype(jnp.bfloat16)
    own_kv = jnp.concatenate(
        [rotate(kv_pre[:, :HD], own_cos, own_sin), kv_pre[:, HD:]], axis=1
    ).astype(jnp.bfloat16)
    all_kv = lax.all_gather(own_kv, "seq", axis=0, tiled=True)
    keys = all_kv[:, :HD]
    values_all = all_kv[:, HD:]
    scores = jnp.einsum("rhd,kd->hrk", queries, keys, preferred_element_type=jnp.float32)
    scores = jnp.where(allowed[None], scores, NEG)
    top_score = jnp.max(scores, axis=-1, keepdims=True)
    expd = jnp.exp(scores - top_score)
    total = jnp.sum(expd, axis=-1, keepdims=True)
    log_total = top_score + jnp.log(total)
    probs_low = (expd / total).astype(jnp.bfloat16)
    mixed = (
        jnp.einsum("hrk,kd->rhd", probs_low, values_all, preferred_element_type=jnp.float32)
        .reshape(rows, heads * HD)
        .astype(jnp.bfloat16)
    )
    attn = lax.psum(matmul(mixed, full_out), "tensor")
    resid = inputs + attn
    full_gate, full_up, full_down, full_gain_two = (
        lax.all_gather(w_gate, ("dp", "seq"), axis=0, tiled=True),
        lax.all_gather(w_up, ("dp", "seq"), axis=0, tiled=True),
        lax.all_gather(w_down, ("dp", "seq"), axis=1, tiled=True),
        lax.all_gather(gain_ffn, ("dp", "seq"), axis=0, tiled=True),
    )
    gain_two = full_gain_two.astype(jnp.float32)
    rms_two = lax.rsqrt(jnp.mean(resid * resid, axis=-1, keepdims=True) + EPS)
    norm_two = resid * rms_two
    act_two = (norm_two * gain_two).astype(jnp.bfloat16)
    gate = matmul(act_two, full_gate)
    up_val = matmul(act_two, full_up)
    gelu_val, gelu_pull = jax.vjp(gelu_tanh, gate)
    hidden = (gelu_val * up_val).astype(jnp.bfloat16)
    ffn = lax.psum(matmul(hidden, full_down).astype(jnp.bfloat16), "tensor").astype(jnp.float32)
    out = (resid + ffn).astype(jnp.bfloat16)
    back_gate, back_up, back_down = (
        lax.all_gather(w_gate, ("dp", "seq"), axis=0, tiled=True),
        lax.all_gather(w_up, ("dp", "seq"), axis=0, tiled=True),
        lax.all_gather(w_down, ("dp", "seq"), axis=1, tiled=True),
    )
    d_hidden = matmul_nt(d_out, back_down)
    grad_down = matmul_tn(hidden, d_out)
    d_gate = gelu_pull(d_hidden * up_val)[0].astype(jnp.bfloat16)
    d_up = (d_hidden * gelu_val).astype(jnp.bfloat16)
    grad_gate = matmul_tn(act_two, d_gate)
    grad_up = matmul_tn(act_two, d_up)
    d_act_two = lax.psum(matmul_nt(d_gate, back_gate) + matmul_nt(d_up, back_up), "tensor")
    grad_gain_two = jnp.sum(d_act_two * norm_two, axis=0)
    d_resid = d_out.astype(jnp.float32) + norm_back(d_act_two, norm_two, rms_two, gain_two)
    ffn_grads = (
        lax.psum_scatter(
            grad_gate.astype(jnp.bfloat16), ("dp", "seq"), scatter_dimension=0, tiled=True
        ).astype(jnp.float32),
        lax.psum_scatter(
            grad_up.astype(jnp.bfloat16), ("dp", "seq"), scatter_dimension=0, tiled=True
        ).astype(jnp.float32),
        lax.psum_scatter(
            grad_down.astype(jnp.bfloat16), ("dp", "seq"), scatter_dimension=1, tiled=True
        ).astype(jnp.float32),
        lax.psum_scatter(
            grad_gain_two.astype(jnp.bfloat16), ("dp", "seq"), scatter_dimension=0, tiled=True
        ).astype(jnp.float32),
    )
    back_query, back_out, back_kv = (
        lax.all_gather(w_query, ("dp", "seq"), axis=0, tiled=True),
        lax.all_gather(w_out, ("dp", "seq"), axis=1, tiled=True),
        lax.all_gather(kv_weight, ("dp", "seq"), axis=0, tiled=True),
    )
    d_attn = d_resid.astype(jnp.bfloat16)
    grad_out = matmul_tn(mixed, d_attn)
    d_mixed = matmul_nt(d_attn, back_out).astype(jnp.bfloat16).reshape(rows, heads, HD)
    scores_again = jnp.einsum("rhd,kd->hrk", queries, keys, preferred_element_type=jnp.float32)
    probs = jnp.where(allowed[None], jnp.exp(scores_again - log_total), 0.0)
    d_probs = jnp.einsum("rhd,kd->hrk", d_mixed, values_all, preferred_element_type=jnp.float32)
    delta = jnp.sum(probs * d_probs, axis=-1, keepdims=True)
    d_scores = (probs * (d_probs - delta)).astype(jnp.bfloat16)
    d_queries = (
        jnp.einsum("hrk,kd->rhd", d_scores, keys, preferred_element_type=jnp.float32) * scale_factor
    )
    d_query_pre = (
        rotate_back(d_queries, own_cos[:, None, :], own_sin[:, None, :])
        .reshape(rows, heads * HD)
        .astype(jnp.bfloat16)
    )
    d_keys_part = jnp.einsum("hrk,rhd->kd", d_scores, queries, preferred_element_type=jnp.float32)
    d_values_part = jnp.einsum(
        "hrk,rhd->kd", probs.astype(jnp.bfloat16), d_mixed, preferred_element_type=jnp.float32
    )
    own_kv_grad = lax.psum_scatter(
        jnp.concatenate([d_keys_part, d_values_part], axis=1).astype(jnp.bfloat16),
        "seq",
        scatter_dimension=0,
        tiled=True,
    )
    d_act_query = matmul_nt(d_query_pre, back_query)
    d_act_sum, kv_grad = (
        lax.psum(d_act_query.astype(jnp.bfloat16), "tensor").astype(jnp.float32),
        lax.psum(own_kv_grad, "tensor").astype(jnp.float32),
    )
    d_kv_pre = jnp.concatenate(
        [rotate_back(kv_grad[:, :HD], own_cos, own_sin), kv_grad[:, HD:]], axis=1
    ).astype(jnp.bfloat16)
    d_act_one = d_act_sum + matmul_nt(d_kv_pre, back_kv)
    grad_query = matmul_tn(act_one, d_query_pre)
    grad_kv = matmul_tn(act_one, d_kv_pre)
    grad_gain_one = jnp.sum(d_act_one * norm_one, axis=0)
    d_tokens = d_resid + norm_back(d_act_one, norm_one, rms_one, gain_one)
    attn_grads = (
        lax.psum_scatter(
            grad_query.astype(jnp.bfloat16), ("dp", "seq"), scatter_dimension=0, tiled=True
        ).astype(jnp.float32),
        lax.psum_scatter(
            grad_out.astype(jnp.bfloat16), ("dp", "seq"), scatter_dimension=1, tiled=True
        ).astype(jnp.float32),
        lax.psum_scatter(
            grad_kv.astype(jnp.bfloat16), ("dp", "seq"), scatter_dimension=0, tiled=True
        ).astype(jnp.float32),
        lax.psum_scatter(
            grad_gain_one.astype(jnp.bfloat16), ("dp", "seq"), scatter_dimension=0, tiled=True
        ).astype(jnp.float32),
    )
    return (
        out,
        d_tokens,
        attn_grads[3],
        attn_grads[0],
        attn_grads[2],
        attn_grads[1],
        ffn_grads[3],
        ffn_grads[0],
        ffn_grads[1],
        ffn_grads[2],
    )


MESH = pl.DeviceIdType.MESH
VMEM_LIMIT = 66000 * 1024


class Place:
    def __init__(self):
        self.dp = lax.axis_index("dp")
        self.seq = lax.axis_index("seq")
        self.z = lax.axis_index("tensor")
        self.core = lax.rem(self.dp, 2)
        self.chip = lax.div(self.dp, 2)

    def device(self, across, other):
        chip = (self.chip + across) % 2
        seq = (self.seq + across // 2) % 2
        core = (self.core + other) % 2
        return chip * 2 + core, seq, self.z

    def shard(self, across, other):
        dp, seq, _ = self.device(across, other)
        return dp * 2 + seq


def greet(peers, line=None):
    barrier = pltpu.get_barrier_semaphore()
    for peer in peers:
        pl.semaphore_signal(barrier, inc=1, device_id=peer, device_id_type=MESH)
    if line is None:
        pl.semaphore_wait(barrier, len(peers))
        return
    pl.semaphore_signal(barrier, inc=1, device_id=line.mate, device_id_type=MESH)

    @pl.when(line.inner == 1)
    def _():
        pl.semaphore_signal(barrier, inc=1, device_id=line.other, device_id_type=MESH)

    pl.semaphore_wait(barrier, len(peers) + 1 + line.inner)


def remote(src, dst, send, recv, peer):
    return pltpu.make_async_remote_copy(
        src_ref=src, dst_ref=dst, send_sem=send, recv_sem=recv, device_id=peer, device_id_type=MESH
    )


class Line:
    def __init__(self, here, counts, refs, place=None):
        self.own, self.out, self.from_end, self.mine, self.from_mid = refs[:5]
        self.sems = refs[5:11]
        self.counts = counts
        self.chunk = self.own.shape[0] // counts
        self.place = place
        z = here.z
        self.inner = ((z + 1) // 2) % 2
        self.mate = (here.dp, here.seq, z + 1 - 2 * (z % 2))
        self.other = (here.dp, here.seq, 3 - z)

    def rows(self, at):
        at = at if self.place is None else self.place(at)
        return pl.ds(pl.multiple_of(at * self.chunk, self.chunk), self.chunk)

    def up(self, at):
        return remote(self.own.at[self.rows(at), :], self.from_end.at[at], self.sems[0].at[at],
                      self.sems[1].at[at], self.mate)

    def over(self, at):
        return remote(self.mine.at[at], self.from_mid.at[at], self.sems[2].at[at], self.sems[3].at[at],
                      self.other)

    def down(self, at):
        rows = self.rows(at)
        return remote(self.out.at[rows, :], self.out.at[rows, :], self.sems[4].at[at],
                      self.sems[5].at[at], self.mate)

    def begin(self):
        @pl.when(self.inner == 0)
        def _():
            def send(at, _):
                self.up(at).start()
                return 0

            lax.fori_loop(0, self.counts, send, 0)

    def first(self, at):
        rows = self.rows(at)
        self.up(at).wait_recv()
        total = self.own[rows, :].astype(jnp.float32) + self.from_end[at].astype(jnp.float32)
        self.mine[at] = total.astype(self.mine.dtype)
        self.over(at).start()

    def second(self, at):
        rows = self.rows(at)
        self.over(at).wait_recv()
        total = self.mine[at].astype(jnp.float32) + self.from_mid[at].astype(jnp.float32)
        self.out[rows, :] = total.astype(self.out.dtype)
        self.down(at).start()

    def step(self, at):
        @pl.when(jnp.logical_and(self.inner == 1, at < self.counts))
        def _():
            self.first(at)

        @pl.when(jnp.logical_and(self.inner == 1, jnp.logical_and(at > 1, at < self.counts + 2)))
        def _():
            self.second(at - 2)

    def end(self, done=0):
        def rest(at, _):
            self.step(at)
            return 0

        lax.fori_loop(min(done, self.counts + 2), self.counts + 2, rest, 0)

        @pl.when(self.inner == 0)
        def _():
            def take(at, _):
                self.up(at).wait_send()
                self.down(at).wait_recv()
                return 0

            lax.fori_loop(0, self.counts, take, 0)

        @pl.when(self.inner == 1)
        def _():
            def drain(at, _):
                self.over(at).wait_send()
                self.down(at).wait_send()
                return 0

            lax.fori_loop(0, self.counts, drain, 0)


def line_scratch(counts, shape, low):
    buf = pltpu.VMEM((counts, shape[0] // counts, shape[1]), low)
    return [buf, buf, buf] + [pltpu.SemaphoreType.DMA((counts,))] * 6


def scatter_kernel(rows, width, counts, nt, shared, line_counts, act, *refs):
    refs = list(refs)
    here = Place()
    w0 = refs.pop(0)
    w1 = w0 if shared else refs.pop(0)
    tiny = refs.pop(0)
    line_own = refs.pop(0) if line_counts else None
    out, tiny_all = refs.pop(0), refs.pop(0)
    line = None
    if line_counts:
        line = Line(here, line_counts, [line_own, refs.pop(0)] + refs[13:])
    held, sib_out, sib_in, from_x, from_y, sib_send, sib_recv = refs[:7]
    x_send, x_recv, y_send, y_recv, tiny_send, tiny_recv = refs[7:13]
    sib, xdev, ydev = here.device(0, 1), here.device(1, 0), here.device(2, 0)
    peers = [here.device(a, o) for a in range(4) for o in range(2) if a + o > 0]
    greet(peers, line)
    if line:
        line.begin()
    weights = (w0, w1)

    def tiny_copy(at):
        across, other = (at + 1) // 2, (at + 1) % 2
        return remote(tiny.at[here.shard(across, other)], tiny_all.at[here.shard(0, 0)],
                      tiny_send.at[at], tiny_recv.at[at], peers[at])

    for at in range(7):
        tiny_copy(at).start()
    tiny_all[here.shard(0, 0)] = tiny[here.shard(0, 0)]
    half_cols = counts * width
    stages = (((3, 0), (3, 1)), ((1, 0), (2, 1)), ((0, 0), (0, 1)), ((1, 1), (2, 0)))

    def product(across, other, half, at):
        row = pl.multiple_of(here.shard(across, other) * rows, rows)
        first = half * half_cols if shared else 0
        cols = pl.ds(pl.multiple_of(first + at * width, width), width)
        block = act[pl.ds(row, rows), :]
        if nt:
            return lax.dot_general(block, weights[half][cols, :], (((1,), (1,)), ((), ())),
                                   preferred_element_type=jnp.float32)
        return jnp.dot(block, weights[half][:, cols], preferred_element_type=jnp.float32)

    def to_sib(stage, stream, at):
        return remote(sib_out.at[stage, stream, at], sib_in.at[stage, stream, at],
                      sib_send.at[stage, stream, at], sib_recv.at[stage, stream, at], sib)

    def to_x(step, at, stage):
        return remote(held.at[stage, 0, at], from_x.at[step, at], x_send.at[step, at],
                      x_recv.at[step, at], xdev)

    def to_y(step, at, stage):
        return remote(held.at[stage, 1, at], from_y.at[step, at], y_send.at[step, at],
                      y_recv.at[step, at], ydev)

    step_of = {0: 0, 1: 1, 3: 2}

    for order, (stage, streams) in enumerate(enumerate(stages)):
        def compute(at, stage=stage, streams=streams):
            for stream, (across, half) in enumerate(streams):
                sib_out[stage, stream, at] = product(across, 1, half, at).astype(jnp.bfloat16)
                held[stage, stream, at] = product(across, 0, half, at).astype(jnp.bfloat16)

        def finish(at, stage=stage):
            for stream in range(2):
                to_sib(stage, stream, at).wait_recv()
                total = held[stage, stream, at].astype(jnp.float32) + sib_in[
                    stage, stream, at].astype(jnp.float32)
                if stage == 3:
                    if stream == 0:
                        to_y(0, at, 0).wait_recv()
                        total += from_y[0, at].astype(jnp.float32)
                    else:
                        to_x(0, at, 0).wait_recv()
                        total += from_x[0, at].astype(jnp.float32)
                if stage == 2:
                    cols = pl.ds(pl.multiple_of(stream * half_cols + at * width, width), width)
                    out[:, cols] = total
                else:
                    held[stage, stream, at] = total.astype(jnp.bfloat16)
            if stage != 2:
                to_x(step_of[stage], at, stage).start()
                to_y(step_of[stage], at, stage).start()

        def body(at, _, compute=compute, finish=finish, stage=stage, order=0):
            compute(at)
            for stream in range(2):
                to_sib(stage, stream, at).start()

            @pl.when(at > 0)
            def _():
                finish(at - 1)

            if line:
                line.step(order * counts + at)
            return 0

        lax.fori_loop(0, counts, functools.partial(body, order=order), 0)
        finish(counts - 1)
    if line:
        line.end(4 * counts)

    def last(at, _):
        for half in range(2):
            cols = pl.ds(pl.multiple_of(half * half_cols + at * width, width), width)
            xs, ys = (1, 2) if half == 0 else (2, 1)
            to_x(xs, at, 0).wait_recv()
            to_y(ys, at, 0).wait_recv()
            out[:, cols] += from_x[xs, at].astype(jnp.float32) + from_y[ys, at].astype(jnp.float32)
        for stage in range(4):
            for stream in range(2):
                to_sib(stage, stream, at).wait_send()
        for step in range(3):
            to_x(step, at, 0).wait_send()
            to_y(step, at, 0).wait_send()
        return 0

    lax.fori_loop(0, counts, last, 0)
    for at in range(7):
        tiny_copy(at).wait()


def scatter_product(act, weights, tiny, width, nt, cid, line=None, line_counts=16):
    total, depth = act.shape
    rows = total // 8
    shared = len(weights) == 1
    half = weights[0].shape[0 if nt else 1] // (2 if shared else 1)
    counts = half // width
    low = jnp.bfloat16
    dma = pltpu.SemaphoreType.DMA
    vm = pl.BlockSpec(memory_space=pltpu.VMEM)
    out_shape = [
        jax.ShapeDtypeStruct((rows, 2 * half), jnp.float32),
        jax.ShapeDtypeStruct(tiny.shape, jnp.float32),
    ]
    scratch = [
        pltpu.VMEM((4, 2, counts, rows, width), low),
        pltpu.VMEM((4, 2, counts, rows, width), low),
        pltpu.VMEM((4, 2, counts, rows, width), low),
        pltpu.VMEM((3, counts, rows, width), low),
        pltpu.VMEM((3, counts, rows, width), low),
        dma((4, 2, counts)), dma((4, 2, counts)),
        dma((3, counts)), dma((3, counts)), dma((3, counts)), dma((3, counts)),
        dma((7,)), dma((7,)),
    ]
    operands = [act, *weights, tiny]
    if line is not None:
        operands.append(line)
        out_shape.append(jax.ShapeDtypeStruct(line.shape, line.dtype))
        scratch += line_scratch(line_counts, line.shape, line.dtype)
    return pl.pallas_call(
        functools.partial(scatter_kernel, rows, width, counts, nt, shared,
                          0 if line is None else line_counts),
        out_shape=out_shape,
        in_specs=[vm] * len(operands),
        out_specs=[vm] * len(out_shape),
        scratch_shapes=scratch,
        compiler_params=pltpu.CompilerParams(collective_id=cid, has_side_effects=True,
                                             vmem_limit_bytes=VMEM_LIMIT),
        name=f"scatter_product_{cid}",
    )(*operands)


def gather_kernel(rows, width, counts, down, give_cols, n_own, n_out, line_counts, act, *refs):
    refs = list(refs)
    here = Place()
    weights = [refs.pop(0) for _ in range(n_own)]
    payload = [refs.pop(0) for _ in range(n_own)]
    give = refs.pop(0) if give_cols else None
    tiny = refs.pop(0)
    line_own = refs.pop(0) if line_counts else None
    sums = refs.pop(0)
    grads = [refs.pop(0) for _ in range(n_out)]
    tiny_all = refs.pop(0)
    line_out = refs.pop(0) if line_counts else None
    got, x_send, x_recv, y_send, y_recv, sib_send, sib_recv, tiny_send, tiny_recv, own_sem = refs[:10]
    refs = refs[10:]
    if give_cols:
        taken, give_sems = refs[:2]
        refs = refs[2:]
    line = Line(here, line_counts, [line_own, line_out] + refs) if line_counts else None
    sib, xdev, ydev = here.device(0, 1), here.device(1, 0), here.device(2, 0)
    peers = [here.device(a, o) for a in range(4) for o in range(2) if a + o > 0]
    core = here.core
    half_cols = counts * width

    def part(half, at):
        first = half * half_cols if n_own == 1 else 0
        return pl.ds(pl.multiple_of(first + at * width, width), width)

    def weight(half):
        return weights[half if n_own > 1 else 0]

    def own_copy(half, at):
        src = payload[half if n_own > 1 else 0].at[:, part(half, at)]
        return pltpu.make_async_copy(src, got.at[0, core, half, at], own_sem.at[half, at])

    for half in range(2):
        for at in range(counts):
            own_copy(half, at).start()
    greet(peers, line)
    stages = (((1, 0), (2, 1)), ((1, 1), (2, 0)), ((3, 1), (3, 0)))

    def x_copy(step, at):
        src = got.at[0, core, step, at] if step < 2 else got.at[2, core, 1, at]
        dst = got.at[1, core, step, at] if step < 2 else got.at[3, core, 1, at]
        return remote(src, dst, x_send.at[step, at], x_recv.at[step, at], xdev)

    def y_copy(step, at):
        src = got.at[0, core, 1 - step, at] if step < 2 else got.at[1, core, 0, at]
        dst = got.at[2, core, 1 - step, at] if step < 2 else got.at[3, core, 0, at]
        return remote(src, dst, y_send.at[step, at], y_recv.at[step, at], ydev)

    def sib_copy(stage, stream, at):
        across, half = (0, stream) if stage == 3 else stages[stage][stream]
        slot = got.at[across, core, half, at]
        return remote(slot, slot, sib_send.at[stage, stream, at], sib_recv.at[stage, stream, at], sib)

    def tiny_copy(at):
        return remote(tiny, tiny_all.at[here.shard(0, 0)], tiny_send.at[at], tiny_recv.at[at], peers[at])

    if give_cols:
        given = remote(give, taken, give_sems.at[0], give_sems.at[1], ydev)
        given.start()
    if line:
        line.begin()
    for at in range(counts):
        for half in range(2):
            own_copy(half, at).wait()
    if give_cols:
        given.wait()
        for at in range(give_cols // width):
            slot = counts - give_cols // width + at
            more = taken[:, at * width : (at + 1) * width].astype(jnp.float32)
            got[0, core, 1, slot] = (got[0, core, 1, slot].astype(jnp.float32) + more).astype(got.dtype)
    sums[...] = jnp.zeros_like(sums)
    for at in range(counts):
        x_copy(0, at).start()
        y_copy(0, at).start()
    for at in range(counts):
        sib_copy(3, 0, at).start()
        sib_copy(3, 1, at).start()
    for at in range(7):
        tiny_copy(at).start()
    tiny_all[here.shard(0, 0)] = tiny[...]

    def blocks(across, half, at, fresh):
        gained = None
        cols = part(half, at)
        for other in range(2):
            row = pl.ds(pl.multiple_of(here.shard(across, other) * rows, rows), rows)
            block = got[across, (core + other) % 2, half, at]
            if down:
                sums[row, :] += jnp.dot(block, weight(half)[cols, :], preferred_element_type=jnp.float32)
                more = lax.dot_general(block, act[row, :], (((0,), (0,)), ((), ())),
                                       preferred_element_type=jnp.float32)
            else:
                sums[row, :] += lax.dot_general(block, weight(half)[:, cols], (((1,), (1,)), ((), ())),
                                                preferred_element_type=jnp.float32)
                more = jnp.dot(act[:, row], block, preferred_element_type=jnp.float32)
            gained = more if gained is None else gained + more
        grad = grads[half if n_out > 1 else 0]
        where = (cols, slice(None)) if down else (slice(None), cols)
        if fresh:
            grad[where] = gained
        else:
            grad[where] += gained

    def own_step(at, _):
        for half in range(2):
            sib_copy(3, half, at).wait_recv()
            blocks(0, half, at, True)
        if line:
            line.step(at)
        return 0

    lax.fori_loop(0, counts, own_step, 0)

    def work(stage, at):
        for stream, (across, half) in enumerate(stages[stage]):
            sib_copy(stage, stream, at).wait_recv()
            blocks(across, half, at, False)

    for stage in range(3):
        def body(at, _, stage=stage):
            x_copy(stage, at).wait_recv()
            sib_copy(stage, 0, at).start()
            y_copy(stage, at).wait_recv()
            sib_copy(stage, 1, at).start()
            if stage < 2:
                x_copy(stage + 1, at).start()
                y_copy(stage + 1, at).start()

            @pl.when(at > 0)
            def _():
                work(stage, at - 1)

            if line:
                line.step((stage + 1) * counts + at)
            return 0

        lax.fori_loop(0, counts, body, 0)
        work(stage, counts - 1)
    if line:
        line.end(4 * counts)

    def drain(at, _):
        for step in range(3):
            x_copy(step, at).wait_send()
            y_copy(step, at).wait_send()
        for stage in range(4):
            sib_copy(stage, 0, at).wait_send()
            sib_copy(stage, 1, at).wait_send()
        return 0

    lax.fori_loop(0, counts, drain, 0)
    for at in range(7):
        tiny_copy(at).wait()


def gather_product(act, weights, payload, tiny, width, down, cid, give=None, line=None, line_counts=16):
    total, depth = act.shape if down else act.shape[::-1]
    rows = payload[0].shape[0]
    half = payload[0].shape[1] // (2 if len(payload) == 1 else 1)
    counts = half // width
    low = jnp.bfloat16
    f32 = jnp.float32
    dma = pltpu.SemaphoreType.DMA
    vm = pl.BlockSpec(memory_space=pltpu.VMEM)
    hbm = pl.BlockSpec(memory_space=pl.ANY)
    out_shape = [jax.ShapeDtypeStruct((total, depth), f32)]
    out_shape += [jax.ShapeDtypeStruct(w.shape, f32) for w in weights]
    out_shape.append(jax.ShapeDtypeStruct((8,) + tiny.shape, f32))
    scratch = [
        pltpu.VMEM((4, 2, 2, counts, rows, width), low),
        dma((3, counts)), dma((3, counts)), dma((3, counts)), dma((3, counts)),
        dma((4, 2, counts)), dma((4, 2, counts)), dma((7,)), dma((7,)), dma((2, counts)),
    ]
    operands = [act, *weights, *payload]
    specs = [vm] * (1 + len(weights)) + [hbm] * len(payload)
    if give is not None:
        operands.append(give)
        specs.append(vm)
        scratch += [pltpu.VMEM(give.shape, low), dma((2,))]
    operands.append(tiny)
    specs.append(vm)
    if line is not None:
        operands.append(line)
        specs.append(vm)
        out_shape.append(jax.ShapeDtypeStruct(line.shape, line.dtype))
        scratch += line_scratch(line_counts, line.shape, line.dtype)
    return pl.pallas_call(
        functools.partial(gather_kernel, rows, width, counts, down,
                          0 if give is None else give.shape[1], len(weights), len(weights),
                          0 if line is None else line_counts),
        out_shape=out_shape,
        in_specs=specs,
        out_specs=[vm] * len(out_shape),
        scratch_shapes=scratch,
        compiler_params=pltpu.CompilerParams(collective_id=cid, has_side_effects=True,
                                             vmem_limit_bytes=VMEM_LIMIT),
        name=f"gather_product_{cid}",
    )(*operands)


def turn_kernel(rows, cols, back, src, out, own_sem, send, recv):
    here = Place()
    peers = [(a, o) for a in (3, 1, 2, 0) for o in range(2) if a + o > 0]
    greet([here.device(a, o) for a, o in peers])

    def by_row(ref, shard):
        return ref.at[pl.ds(pl.multiple_of(shard * rows, rows), rows), :]

    def by_col(ref, shard):
        return ref.at[:, pl.ds(pl.multiple_of(shard * cols, cols), cols)]

    take, put = (by_row, by_col) if back else (by_col, by_row)
    me = here.shard(0, 0)

    def copy(at):
        across, other = peers[at]
        return remote(take(src, here.shard(across, other)), put(out, me), send.at[at], recv.at[at],
                      here.device(across, other))

    for at in range(7):
        copy(at).start()
    own = pltpu.make_async_copy(take(src, me), put(out, me), own_sem)
    own.start()
    own.wait()
    for at in range(7):
        copy(at).wait()


def turn(src, back, cid):
    rows, cols = (src.shape[0] // 8, src.shape[1]) if back else (src.shape[0], src.shape[1] // 8)
    shape = (rows, 8 * cols) if back else (8 * rows, cols)
    dma = pltpu.SemaphoreType.DMA
    vm = pl.BlockSpec(memory_space=pltpu.VMEM)
    return pl.pallas_call(
        functools.partial(turn_kernel, rows, cols, back),
        out_shape=jax.ShapeDtypeStruct(shape, src.dtype),
        in_specs=[vm],
        out_specs=vm,
        scratch_shapes=[dma(()), dma((7,)), dma((7,))],
        compiler_params=pltpu.CompilerParams(collective_id=cid, has_side_effects=True,
                                             vmem_limit_bytes=VMEM_LIMIT),
        name=f"turn_{cid}",
    )(src)


def close_kernel(rows, cols, per, own, rest, other_own, out, other_out, summed, ready, local_sem, other_send,
                 other_recv, put_send, put_recv, *line_refs):
    here = Place()
    me = here.shard(0, 0)
    counts = 8 * per

    def target(at):
        turn_at = at // per
        return 3 - turn_at // 2, 1 - turn_at % 2

    def place(at):
        across, other = target(at)
        return here.shard(across, other) * per + at % per

    line = Line(here, counts, [own, summed] + list(line_refs), place)
    peers = [(a, o) for a in (3, 2, 1, 0) for o in (1, 0) if a + o > 0]
    greet([here.device(a, o) for a, o in peers], line)
    line.begin()
    columns = pl.ds(pl.multiple_of(me * cols, cols), cols)

    def turn_copy(at):
        across, other = peers[at]
        src = other_own.at[pl.ds(pl.multiple_of(here.shard(across, other) * rows, rows), rows), :]
        return remote(src, other_out.at[:, columns], other_send.at[at], other_recv.at[at],
                      here.device(across, other))

    for at in range(7):
        turn_copy(at).start()
    mine = pltpu.make_async_copy(other_own.at[pl.ds(pl.multiple_of(me * rows, rows), rows), :],
                                 other_out.at[:, columns], local_sem)
    mine.start()
    chunk = line.chunk

    def put(at):
        across, other = target(at)
        dst = out.at[pl.ds(pl.multiple_of(at % per * chunk, chunk), chunk), columns]
        return remote(ready.at[at], dst, put_send.at[at], put_recv.at[at], here.device(across, other))

    def emit(at):
        total = rest[line.rows(at), :] + summed[line.rows(at), :].astype(jnp.float32)

        @pl.when(at < 7 * per)
        def _():
            ready[at] = total.astype(ready.dtype)
            put(at).start()

        @pl.when(at >= 7 * per)
        def _():
            out[pl.ds(pl.multiple_of(at % per * chunk, chunk), chunk), columns] = total.astype(out.dtype)

    @pl.when(line.inner == 1)
    def _():
        def both(at, _):
            line.step(at)

            @pl.when(at > 1)
            def _():
                emit(at - 2)
            return 0

        lax.fori_loop(0, counts + 2, both, 0)

        def drain(at, _):
            line.over(at).wait_send()
            line.down(at).wait_send()
            return 0

        lax.fori_loop(0, counts, drain, 0)

    @pl.when(line.inner == 0)
    def _():
        def take(at, _):
            line.up(at).wait_send()
            line.down(at).wait_recv()
            emit(at)
            return 0

        lax.fori_loop(0, counts, take, 0)

    mine.wait()
    for at in range(7):
        turn_copy(at).wait()

    def finish(at, _):
        put(at).wait()
        return 0

    lax.fori_loop(0, 7 * per, finish, 0)


def close(own, rest, other_own, cid, per=2):
    total, cols = own.shape
    rows = total // 8
    low = own.dtype
    dma = pltpu.SemaphoreType.DMA
    vm = pl.BlockSpec(memory_space=pltpu.VMEM)
    whole = jax.ShapeDtypeStruct((rows, 8 * cols), low)
    counts = 8 * per
    return pl.pallas_call(
        functools.partial(close_kernel, rows, cols, per),
        out_shape=[whole, whole],
        in_specs=[vm] * 3,
        out_specs=[vm] * 2,
        scratch_shapes=[
            pltpu.VMEM((total, cols), low),
            pltpu.VMEM((7 * per, rows // per, cols), low),
            dma(()), dma((7,)), dma((7,)), dma((7 * per,)), dma((7 * per,)),
        ] + line_scratch(counts, own.shape, low),
        compiler_params=pltpu.CompilerParams(collective_id=cid, has_side_effects=True,
                                             vmem_limit_bytes=VMEM_LIMIT),
        name=f"close_{cid}",
    )(own, rest, other_own)


AXES = ("dp", "seq")
LANES = 128


def gather_rows(block):
    return lax.all_gather(block, AXES, axis=0, tiled=True)


def pack_rows(values):
    parts = values.reshape(8, -1, LANES)
    return jnp.pad(parts, ((0, 0), (0, 8 - parts.shape[1]), (0, 0)))


def acts_move(
    tokens, seg_ids, gain_attn, w_query, kv_weight, w_out, gain_ffn, w_gate, w_up, w_down, d_out
):
    low = jnp.bfloat16
    rows, width = tokens.shape
    seqs = lax.axis_size("seq")
    parts = lax.axis_size("dp") * seqs
    scale_factor = 1.0 / math.sqrt(HD)
    offset = lax.axis_index("seq") * rows
    places, cos_table, sin_table = place_tables(seg_ids)
    own_places = lax.dynamic_slice_in_dim(places, offset, rows, 0)
    own_segs = lax.dynamic_slice_in_dim(seg_ids, offset, rows, 0)
    own_cos = lax.dynamic_slice_in_dim(cos_table, offset, rows, 0)
    own_sin = lax.dynamic_slice_in_dim(sin_table, offset, rows, 0)
    allowed = (own_segs[:, None] == seg_ids[None, :]) & (own_places[:, None] >= places[None, :])
    gain_one = gain_attn.astype(jnp.float32)
    gain_two = gain_ffn.astype(jnp.float32)
    qw = w_query.shape[1]
    heads = qw // HD
    ff = w_gate.shape[1]

    none = jnp.zeros((8, 8, LANES), jnp.float32)
    x_low = turn(tokens, False, 1)
    g_low = turn(d_out, False, 2)
    x_col = x_low.astype(jnp.float32)
    own_x = tokens.astype(jnp.float32)
    rms_one = lax.rsqrt(jnp.mean(own_x * own_x, axis=-1, keepdims=True) + EPS)
    act_one = (x_col * gain_one).astype(low)
    w_qkv = jnp.concatenate([w_query, kv_weight], axis=1)
    qkv = scatter_product(act_one, (w_qkv,), none, 256, False, 3)[0] * rms_one
    queries = (
        rotate(qkv[:, :qw].reshape(rows, heads, HD), own_cos[:, None, :], own_sin[:, None, :])
        * scale_factor
    ).astype(low)
    rms_high = rms_one.astype(low)
    rms_rest = (rms_one - rms_high.astype(jnp.float32)).astype(low)
    half = (rows, LANES // 2)
    own_kv = jnp.concatenate(
        [
            rotate(qkv[:, qw : qw + HD], own_cos, own_sin).astype(low),
            qkv[:, qw + HD :].astype(low),
            jnp.broadcast_to(rms_high, half),
            jnp.broadcast_to(rms_rest, half),
        ],
        axis=1,
    )
    all_kv = lax.all_gather(own_kv, "seq", axis=0, tiled=True)
    keys = all_kv[:, :HD]
    values_all = all_kv[:, HD : 2 * HD]
    rms_group = all_kv[:, 2 * HD : 2 * HD + 1].astype(jnp.float32) + all_kv[
        :, 2 * HD + LANES // 2 : 2 * HD + LANES // 2 + 1
    ].astype(jnp.float32)
    scores = jnp.einsum("rhd,kd->hrk", queries, keys, preferred_element_type=jnp.float32)
    scores = jnp.where(allowed[None], scores, NEG)
    top_score = jnp.max(scores, axis=-1, keepdims=True)
    expd = jnp.exp(scores - top_score)
    total = jnp.sum(expd, axis=-1, keepdims=True)
    probs = expd / total
    probs_low = probs.astype(low)
    mixed = (
        jnp.einsum("hrk,kd->rhd", probs_low, values_all, preferred_element_type=jnp.float32)
        .reshape(rows, heads * HD)
        .astype(low)
    )
    mixed_all = gather_rows(mixed)
    d_hidden, _, attn = scatter_product(
        g_low, (w_down,), none, 512, True, 4, line=matmul(mixed_all, w_out).astype(low)
    )
    resid = x_col + attn.astype(jnp.float32)
    act_two = (resid * gain_two).astype(low)
    squares = pack_rows(jnp.sum(resid * resid, axis=-1))
    both, squares_all = scatter_product(act_two, (w_gate, w_up), squares, 512, False, 6)
    mean_two = jnp.sum(squares_all[:, : rows // LANES], axis=0).reshape(rows, 1) / width
    rms_two = lax.rsqrt(mean_two + EPS)
    gate = both[:, :ff] * rms_two
    up_val = both[:, ff : 2 * ff] * rms_two
    gelu_val, gelu_pull = jax.vjp(gelu_tanh, gate)
    hidden = (gelu_val * up_val).astype(low)
    d_gate = gelu_pull(d_hidden * up_val)[0]
    d_up = d_hidden * gelu_val
    dots_two = jnp.sum(d_gate * gate + d_up * up_val, axis=-1, keepdims=True) * (
        rms_two * rms_two / width
    )
    dots_own = jnp.pad(dots_two.reshape(-1, LANES), ((0, 8 - rows // LANES), (0, 0)))
    d_act_two, grad_gate, grad_up, dots_all = gather_product(
        act_two.T,
        (w_gate, w_up),
        ((d_gate * rms_two).astype(low), (d_up * rms_two).astype(low)),
        dots_own,
        512,
        False,
        7,
    )
    dot_two = dots_all[:, : rows // LANES].reshape(parts * rows, 1)
    grad_gain_two = jnp.sum(d_act_two * resid, axis=0)
    ffn, grad_down, _, d_norm = gather_product(
        g_low,
        (w_down,),
        (hidden,),
        none[0],
        256,
        True,
        8,
        line=(d_act_two * gain_two - resid * dot_two).astype(low),
    )
    d_resid = g_low.astype(jnp.float32) + d_norm.astype(jnp.float32)
    d_attn = d_resid.astype(low)
    d_mixed = scatter_product(d_attn, (w_out,), none, 256, True, 9)[0]
    d_mixed = d_mixed.astype(low).reshape(rows, heads, HD)
    grad_out = matmul_tn(mixed_all, d_attn)

    d_probs = jnp.einsum("rhd,kd->hrk", d_mixed, values_all, preferred_element_type=jnp.float32)
    delta = jnp.sum(probs * d_probs, axis=-1, keepdims=True)
    d_scores = (probs * (d_probs - delta)).astype(low)
    d_queries = (
        jnp.einsum("hrk,kd->rhd", d_scores, keys, preferred_element_type=jnp.float32) * scale_factor
    )
    d_query_pre = (
        rotate_back(d_queries, own_cos[:, None, :], own_sin[:, None, :]).reshape(rows, heads * HD)
        * rms_one
    ).astype(low)
    query_dots = jnp.sum(
        (d_queries * queries.astype(jnp.float32)).reshape(rows, heads * HD), axis=1, keepdims=True
    ) * (rms_one * rms_one / (width * scale_factor))
    d_keys = jnp.einsum("hrk,rhd->kd", d_scores, queries, preferred_element_type=jnp.float32)
    d_values = jnp.einsum("hrk,rhd->kd", probs_low, d_mixed, preferred_element_type=jnp.float32)
    kv_dots = jnp.sum(
        d_keys * keys.astype(jnp.float32) + d_values * values_all.astype(jnp.float32),
        axis=1,
        keepdims=True,
    ) * (rms_group * rms_group / width)
    d_kv = jnp.concatenate(
        [rotate_back(d_keys, cos_table, sin_table) * rms_group, d_values * rms_group], axis=1
    ).astype(low)
    away = rows - offset
    own_dots = query_dots + lax.dynamic_slice_in_dim(kv_dots, offset, rows, 0)
    dots_one = jnp.concatenate(
        [
            own_dots.reshape(-1, LANES),
            lax.dynamic_slice_in_dim(kv_dots, away, rows, 0).reshape(-1, LANES),
        ]
    )
    tiles = rows // LANES
    d_act_one, grad_qkv, dots_all, ffn_sum = gather_product(
        act_one.T,
        (w_qkv,),
        (jnp.concatenate([d_query_pre, lax.dynamic_slice_in_dim(d_kv, offset, rows, 0)], axis=1),),
        jnp.pad(dots_one, ((0, 8 - 2 * tiles), (0, 0))),
        256,
        False,
        11,
        give=lax.dynamic_slice_in_dim(d_kv, away, rows, 0),
        line=ffn.astype(low),
    )
    pairs = dots_all.reshape(parts // 2, 2, 8, LANES)
    dot_one = (pairs[:, :, :tiles] + pairs[:, ::-1, tiles : 2 * tiles]).reshape(parts * rows, 1)
    grad_gain_one = jnp.sum(d_act_one * x_col, axis=0)
    d_tokens, out = close(
        (d_act_one * gain_one - x_col * dot_one).astype(low),
        d_resid,
        (resid + ffn_sum.astype(jnp.float32)).astype(low),
        12,
    )
    grad_query = grad_qkv[:, :qw]
    sums = jnp.concatenate(
        [grad_qkv[:, qw:], jnp.stack([grad_gain_one, grad_gain_two]), jnp.zeros((14, width // parts))]
    )
    sums = lax.psum(sums.astype(low), "tensor").astype(jnp.float32)
    grad_kv = sums[: width // parts]
    gains = sums[width // parts :]
    return (
        out,
        d_tokens.astype(jnp.float32),
        gains[0],
        grad_query,
        grad_kv,
        grad_out,
        gains[1],
        grad_gate,
        grad_up,
        grad_down,
    )


def solution(mesh):
    in_specs = (
        P(("dp", "seq"), None),
        P("dp"),
        P(("dp", "seq")),
        P(("dp", "seq"), "tensor"),
        P(("dp", "seq"), None),
        P("tensor", ("dp", "seq")),
        P(("dp", "seq")),
        P(("dp", "seq"), "tensor"),
        P(("dp", "seq"), "tensor"),
        P("tensor", ("dp", "seq")),
        P(("dp", "seq"), None),
    )
    out_specs = (
        P(("dp", "seq"), None),
        P(("dp", "seq"), None),
        P(("dp", "seq")),
        P(("dp", "seq"), "tensor"),
        P(("dp", "seq"), None),
        P("tensor", ("dp", "seq")),
        P(("dp", "seq")),
        P(("dp", "seq"), "tensor"),
        P(("dp", "seq"), "tensor"),
        P("tensor", ("dp", "seq")),
    )

    def shards(*arrays):
        tokens = arrays[0]
        sizes = tuple(mesh.shape[name] for name in ("dp", "seq", "tensor"))
        count = tokens.shape[0] * sizes[0] * sizes[1]
        plan = acts_move if sizes == (4, 2, 4) and count <= tokens.shape[1] else weights_move
        return plan(*arrays)

    return jax.shard_map(shards, mesh=mesh, in_specs=in_specs, out_specs=out_specs, check_vma=False)
```

```python
import functools
import math

import jax
import jax.numpy as jnp
from jax import lax
from jax.experimental import pallas as pl
from jax.experimental.pallas import tpu as pltpu
from jax.sharding import PartitionSpec as P

HD = 256


EPS = 1e-06
NEG = -1e30


def place_tables(segs):
    length = segs.shape[0]
    index = jnp.arange(length, dtype=jnp.int32)
    flags = jnp.concatenate([jnp.ones((1,), dtype=bool), segs[1:] != segs[:-1]])
    starts = lax.cummax(jnp.where(flags, index, jnp.zeros_like(index)), axis=0)
    places = index - starts
    half_size = HD // 2
    freqs = jnp.exp(jnp.arange(half_size, dtype=jnp.float32) * (-math.log(10000.0) / half_size))
    angles = places.astype(jnp.float32)[:, None] * freqs[None, :]
    return (places, jnp.cos(angles), jnp.sin(angles))


def rotate(vector, cos_table, sin_table):
    half_size = vector.shape[-1] // 2
    leading = vector[..., :half_size]
    trailing = vector[..., half_size:]
    return jnp.concatenate(
        [leading * cos_table - trailing * sin_table, trailing * cos_table + leading * sin_table],
        axis=-1,
    )


def rotate_back(vector, cos_table, sin_table):
    half_size = vector.shape[-1] // 2
    leading = vector[..., :half_size]
    trailing = vector[..., half_size:]
    return jnp.concatenate(
        [leading * cos_table + trailing * sin_table, trailing * cos_table - leading * sin_table],
        axis=-1,
    )


def matmul(left, right):
    return jnp.dot(left, right, preferred_element_type=jnp.float32)


def matmul_nt(left, right):
    return lax.dot_general(
        left, right, (((1,), (1,)), ((), ())), preferred_element_type=jnp.float32
    )


def matmul_tn(left, right):
    return lax.dot_general(
        left, right, (((0,), (0,)), ((), ())), preferred_element_type=jnp.float32
    )


def gelu_tanh(values):
    return jax.nn.gelu(values, approximate=True)


def norm_back(d_act, normed, rms_val, gain_val):
    scaled = d_act * gain_val
    return rms_val * (scaled - normed * jnp.mean(scaled * normed, axis=-1, keepdims=True))


def weights_move(
    tokens, seg_ids, gain_attn, w_query, kv_weight, w_out, gain_ffn, w_gate, w_up, w_down, d_out
):
    rows = tokens.shape[0]
    scale_factor = 1.0 / math.sqrt(HD)
    offset = lax.axis_index("seq") * rows
    places, cos_table, sin_table = place_tables(seg_ids)
    own_places = lax.dynamic_slice_in_dim(places, offset, rows, 0)
    own_segs = lax.dynamic_slice_in_dim(seg_ids, offset, rows, 0)
    own_cos = lax.dynamic_slice_in_dim(cos_table, offset, rows, 0)
    own_sin = lax.dynamic_slice_in_dim(sin_table, offset, rows, 0)
    allowed = (own_segs[:, None] == seg_ids[None, :]) & (own_places[:, None] >= places[None, :])
    full_query, full_out, full_kv, full_gain_one = (
        lax.all_gather(w_query, ("dp", "seq"), axis=0, tiled=True),
        lax.all_gather(w_out, ("dp", "seq"), axis=1, tiled=True),
        lax.all_gather(kv_weight, ("dp", "seq"), axis=0, tiled=True),
        lax.all_gather(gain_attn, ("dp", "seq"), axis=0, tiled=True),
    )
    gain_one = full_gain_one.astype(jnp.float32)
    inputs = tokens.astype(jnp.float32)
    rms_one = lax.rsqrt(jnp.mean(inputs * inputs, axis=-1, keepdims=True) + EPS)
    norm_one = inputs * rms_one
    act_one = (norm_one * gain_one).astype(jnp.bfloat16)
    query_pre = matmul(act_one, full_query)
    heads = query_pre.shape[1] // HD
    kv_pre = matmul(act_one, full_kv)
    queries = (
        rotate(query_pre.reshape(rows, heads, HD), own_cos[:, None, :], own_sin[:, None, :])
        * scale_factor
    ).astype(jnp.bfloat16)
    own_kv = jnp.concatenate(
        [rotate(kv_pre[:, :HD], own_cos, own_sin), kv_pre[:, HD:]], axis=1
    ).astype(jnp.bfloat16)
    all_kv = lax.all_gather(own_kv, "seq", axis=0, tiled=True)
    keys = all_kv[:, :HD]
    values_all = all_kv[:, HD:]
    scores = jnp.einsum("rhd,kd->hrk", queries, keys, preferred_element_type=jnp.float32)
    scores = jnp.where(allowed[None], scores, NEG)
    top_score = jnp.max(scores, axis=-1, keepdims=True)
    expd = jnp.exp(scores - top_score)
    total = jnp.sum(expd, axis=-1, keepdims=True)
    log_total = top_score + jnp.log(total)
    probs_low = (expd / total).astype(jnp.bfloat16)
    mixed = (
        jnp.einsum("hrk,kd->rhd", probs_low, values_all, preferred_element_type=jnp.float32)
        .reshape(rows, heads * HD)
        .astype(jnp.bfloat16)
    )
    attn = lax.psum(matmul(mixed, full_out), "tensor")
    resid = inputs + attn
    full_gate, full_up, full_down, full_gain_two = (
        lax.all_gather(w_gate, ("dp", "seq"), axis=0, tiled=True),
        lax.all_gather(w_up, ("dp", "seq"), axis=0, tiled=True),
        lax.all_gather(w_down, ("dp", "seq"), axis=1, tiled=True),
        lax.all_gather(gain_ffn, ("dp", "seq"), axis=0, tiled=True),
    )
    gain_two = full_gain_two.astype(jnp.float32)
    rms_two = lax.rsqrt(jnp.mean(resid * resid, axis=-1, keepdims=True) + EPS)
    norm_two = resid * rms_two
    act_two = (norm_two * gain_two).astype(jnp.bfloat16)
    gate = matmul(act_two, full_gate)
    up_val = matmul(act_two, full_up)
    gelu_val, gelu_pull = jax.vjp(gelu_tanh, gate)
    hidden = (gelu_val * up_val).astype(jnp.bfloat16)
    ffn = lax.psum(matmul(hidden, full_down).astype(jnp.bfloat16), "tensor").astype(jnp.float32)
    out = (resid + ffn).astype(jnp.bfloat16)
    back_gate, back_up, back_down = (
        lax.all_gather(w_gate, ("dp", "seq"), axis=0, tiled=True),
        lax.all_gather(w_up, ("dp", "seq"), axis=0, tiled=True),
        lax.all_gather(w_down, ("dp", "seq"), axis=1, tiled=True),
    )
    d_hidden = matmul_nt(d_out, back_down)
    grad_down = matmul_tn(hidden, d_out)
    d_gate = gelu_pull(d_hidden * up_val)[0].astype(jnp.bfloat16)
    d_up = (d_hidden * gelu_val).astype(jnp.bfloat16)
    grad_gate = matmul_tn(act_two, d_gate)
    grad_up = matmul_tn(act_two, d_up)
    d_act_two = lax.psum(matmul_nt(d_gate, back_gate) + matmul_nt(d_up, back_up), "tensor")
    grad_gain_two = jnp.sum(d_act_two * norm_two, axis=0)
    d_resid = d_out.astype(jnp.float32) + norm_back(d_act_two, norm_two, rms_two, gain_two)
    ffn_grads = (
        lax.psum_scatter(
            grad_gate.astype(jnp.bfloat16), ("dp", "seq"), scatter_dimension=0, tiled=True
        ).astype(jnp.float32),
        lax.psum_scatter(
            grad_up.astype(jnp.bfloat16), ("dp", "seq"), scatter_dimension=0, tiled=True
        ).astype(jnp.float32),
        lax.psum_scatter(
            grad_down.astype(jnp.bfloat16), ("dp", "seq"), scatter_dimension=1, tiled=True
        ).astype(jnp.float32),
        lax.psum_scatter(
            grad_gain_two.astype(jnp.bfloat16), ("dp", "seq"), scatter_dimension=0, tiled=True
        ).astype(jnp.float32),
    )
    back_query, back_out, back_kv = (
        lax.all_gather(w_query, ("dp", "seq"), axis=0, tiled=True),
        lax.all_gather(w_out, ("dp", "seq"), axis=1, tiled=True),
        lax.all_gather(kv_weight, ("dp", "seq"), axis=0, tiled=True),
    )
    d_attn = d_resid.astype(jnp.bfloat16)
    grad_out = matmul_tn(mixed, d_attn)
    d_mixed = matmul_nt(d_attn, back_out).astype(jnp.bfloat16).reshape(rows, heads, HD)
    scores_again = jnp.einsum("rhd,kd->hrk", queries, keys, preferred_element_type=jnp.float32)
    probs = jnp.where(allowed[None], jnp.exp(scores_again - log_total), 0.0)
    d_probs = jnp.einsum("rhd,kd->hrk", d_mixed, values_all, preferred_element_type=jnp.float32)
    delta = jnp.sum(probs * d_probs, axis=-1, keepdims=True)
    d_scores = (probs * (d_probs - delta)).astype(jnp.bfloat16)
    d_queries = (
        jnp.einsum("hrk,kd->rhd", d_scores, keys, preferred_element_type=jnp.float32) * scale_factor
    )
    d_query_pre = (
        rotate_back(d_queries, own_cos[:, None, :], own_sin[:, None, :])
        .reshape(rows, heads * HD)
        .astype(jnp.bfloat16)
    )
    d_keys_part = jnp.einsum("hrk,rhd->kd", d_scores, queries, preferred_element_type=jnp.float32)
    d_values_part = jnp.einsum(
        "hrk,rhd->kd", probs.astype(jnp.bfloat16), d_mixed, preferred_element_type=jnp.float32
    )
    own_kv_grad = lax.psum_scatter(
        jnp.concatenate([d_keys_part, d_values_part], axis=1).astype(jnp.bfloat16),
        "seq",
        scatter_dimension=0,
        tiled=True,
    )
    d_act_query = matmul_nt(d_query_pre, back_query)
    d_act_sum, kv_grad = (
        lax.psum(d_act_query.astype(jnp.bfloat16), "tensor").astype(jnp.float32),
        lax.psum(own_kv_grad, "tensor").astype(jnp.float32),
    )
    d_kv_pre = jnp.concatenate(
        [rotate_back(kv_grad[:, :HD], own_cos, own_sin), kv_grad[:, HD:]], axis=1
    ).astype(jnp.bfloat16)
    d_act_one = d_act_sum + matmul_nt(d_kv_pre, back_kv)
    grad_query = matmul_tn(act_one, d_query_pre)
    grad_kv = matmul_tn(act_one, d_kv_pre)
    grad_gain_one = jnp.sum(d_act_one * norm_one, axis=0)
    d_tokens = d_resid + norm_back(d_act_one, norm_one, rms_one, gain_one)
    attn_grads = (
        lax.psum_scatter(
            grad_query.astype(jnp.bfloat16), ("dp", "seq"), scatter_dimension=0, tiled=True
        ).astype(jnp.float32),
        lax.psum_scatter(
            grad_out.astype(jnp.bfloat16), ("dp", "seq"), scatter_dimension=1, tiled=True
        ).astype(jnp.float32),
        lax.psum_scatter(
            grad_kv.astype(jnp.bfloat16), ("dp", "seq"), scatter_dimension=0, tiled=True
        ).astype(jnp.float32),
        lax.psum_scatter(
            grad_gain_one.astype(jnp.bfloat16), ("dp", "seq"), scatter_dimension=0, tiled=True
        ).astype(jnp.float32),
    )
    return (
        out,
        d_tokens,
        attn_grads[3],
        attn_grads[0],
        attn_grads[2],
        attn_grads[1],
        ffn_grads[3],
        ffn_grads[0],
        ffn_grads[1],
        ffn_grads[2],
    )


MESH = pl.DeviceIdType.MESH
VMEM_LIMIT = 66000 * 1024


class Place:
    def __init__(self):
        self.dp = lax.axis_index("dp")
        self.seq = lax.axis_index("seq")
        self.z = lax.axis_index("tensor")
        self.core = lax.rem(self.dp, 2)
        self.chip = lax.div(self.dp, 2)

    def device(self, across, other):
        chip = (self.chip + across) % 2
        seq = (self.seq + across // 2) % 2
        core = (self.core + other) % 2
        return chip * 2 + core, seq, self.z

    def shard(self, across, other):
        dp, seq, _ = self.device(across, other)
        return dp * 2 + seq


def greet(here, peers, line=False):
    barrier = pltpu.get_barrier_semaphore()
    peers = list(peers)
    if line:
        peers += [(here.dp, here.seq, (here.z + step) % 4) for step in range(1, 4)]
    for peer in peers:
        pl.semaphore_signal(barrier, inc=1, device_id=peer, device_id_type=MESH)
    pl.semaphore_wait(barrier, len(peers))


def remote(src, dst, send, recv, peer):
    return pltpu.make_async_remote_copy(
        src_ref=src, dst_ref=dst, send_sem=send, recv_sem=recv, device_id=peer, device_id_type=MESH
    )


class Line:
    def __init__(self, here, counts, refs, place=None):
        self.own, self.out, self.from_end, self.mine, self.from_mid = refs[:5]
        self.sems = refs[5:11]
        self.counts = counts
        self.chunk = self.own.shape[0] // counts
        self.place = place
        z = here.z
        self.inner = ((z + 1) // 2) % 2
        self.mate = (here.dp, here.seq, z + 1 - 2 * (z % 2))
        self.other = (here.dp, here.seq, 3 - z)

    def rows(self, at):
        at = at if self.place is None else self.place(at)
        return pl.ds(pl.multiple_of(at * self.chunk, self.chunk), self.chunk)

    def up(self, at):
        return remote(self.own.at[self.rows(at), :], self.from_end.at[at], self.sems[0].at[at],
                      self.sems[1].at[at], self.mate)

    def over(self, at):
        return remote(self.mine.at[at], self.from_mid.at[at], self.sems[2].at[at], self.sems[3].at[at],
                      self.other)

    def down(self, at):
        rows = self.rows(at)
        return remote(self.out.at[rows, :], self.out.at[rows, :], self.sems[4].at[at],
                      self.sems[5].at[at], self.mate)

    def begin(self):
        @pl.when(self.inner == 0)
        def _():
            def send(at, _):
                self.up(at).start()
                return 0

            lax.fori_loop(0, self.counts, send, 0)

    def first(self, at):
        rows = self.rows(at)
        self.up(at).wait_recv()
        total = self.own[rows, :].astype(jnp.float32) + self.from_end[at].astype(jnp.float32)
        self.mine[at] = total.astype(self.mine.dtype)
        self.over(at).start()

    def second(self, at):
        rows = self.rows(at)
        self.over(at).wait_recv()
        total = self.mine[at].astype(jnp.float32) + self.from_mid[at].astype(jnp.float32)
        self.out[rows, :] = total.astype(self.out.dtype)
        self.down(at).start()

    def step(self, at):
        @pl.when(jnp.logical_and(self.inner == 1, at < self.counts))
        def _():
            self.first(at)

        @pl.when(jnp.logical_and(self.inner == 1, jnp.logical_and(at > 1, at < self.counts + 2)))
        def _():
            self.second(at - 2)

    def end(self, done=0):
        def rest(at, _):
            self.step(at)
            return 0

        lax.fori_loop(min(done, self.counts + 2), self.counts + 2, rest, 0)

        @pl.when(self.inner == 0)
        def _():
            def take(at, _):
                self.up(at).wait_send()
                self.down(at).wait_recv()
                return 0

            lax.fori_loop(0, self.counts, take, 0)

        @pl.when(self.inner == 1)
        def _():
            def drain(at, _):
                self.over(at).wait_send()
                self.down(at).wait_send()
                return 0

            lax.fori_loop(0, self.counts, drain, 0)


def line_scratch(counts, shape, low):
    buf = pltpu.VMEM((counts, shape[0] // counts, shape[1]), low)
    return [buf, buf, buf] + [pltpu.SemaphoreType.DMA((counts,))] * 6


def turned(at):
    return 3 - at // 2, 1 - at % 2


def slice_peers(here):
    return [here.device(*turned(at)) for at in range(7)]


def kernel_call(kernel, out_shape, operands, specs, scratch, cid, name):
    vm = pl.BlockSpec(memory_space=pltpu.VMEM)
    return pl.pallas_call(
        kernel,
        out_shape=out_shape,
        in_specs=specs,
        out_specs=[vm] * len(out_shape),
        scratch_shapes=scratch,
        compiler_params=pltpu.CompilerParams(
            collective_id=cid, has_side_effects=True, vmem_limit_bytes=VMEM_LIMIT
        ),
        name=f"{name}_{cid}",
    )(*operands)


class Tiny:
    def __init__(self, here, src, dst, sems, spread):
        self.here, self.src, self.dst, self.sems, self.spread = here, src, dst, sems, spread
        self.peers = slice_peers(here)
        self.me = here.shard(0, 0)

    def tile(self, shard):
        return self.src.at[shard] if self.spread else self.src

    def copy(self, at):
        return remote(self.tile(self.here.shard(*turned(at))), self.dst.at[self.me], self.sems[0].at[at],
                      self.sems[1].at[at], self.peers[at])

    def begin(self):
        for at in range(7):
            self.copy(at).start()
        self.dst[self.me] = self.tile(self.me)[...]

    def end(self):
        for at in range(7):
            self.copy(at).wait()


class Reduce:
    def __init__(self, here, counts, width, product, out, refs):
        self.counts, self.width, self.product, self.out = counts, width, product, out
        self.held, self.sib_out, self.sib_in, self.from_x, self.from_y = refs[:5]
        self.sib_sems, self.x_sems, self.y_sems = refs[5:7], refs[7:9], refs[9:11]
        self.sib, self.xdev, self.ydev = here.device(0, 1), here.device(1, 0), here.device(2, 0)
        self.stages = (((3, 0), (3, 1)), ((1, 0), (2, 1)), ((0, 0), (0, 1)), ((1, 1), (2, 0)))

    def to_sib(self, stage, stream, at):
        spot = (stage, stream, at)
        return remote(self.sib_out.at[spot], self.sib_in.at[spot], self.sib_sems[0].at[spot],
                      self.sib_sems[1].at[spot], self.sib)

    def to_x(self, step, at, stage=0):
        return remote(self.held.at[stage, 0, at], self.from_x.at[step, at], self.x_sems[0].at[step, at],
                      self.x_sems[1].at[step, at], self.xdev)

    def to_y(self, step, at, stage=0):
        return remote(self.held.at[stage, 1, at], self.from_y.at[step, at], self.y_sems[0].at[step, at],
                      self.y_sems[1].at[step, at], self.ydev)

    def cols(self, half, at):
        return pl.ds(pl.multiple_of((half * self.counts + at) * self.width, self.width), self.width)

    def compute(self, stage, at):
        for stream, (across, half) in enumerate(self.stages[stage]):
            self.sib_out[stage, stream, at] = self.product(across, 1, half, at).astype(jnp.bfloat16)
            self.held[stage, stream, at] = self.product(across, 0, half, at).astype(jnp.bfloat16)
        for stream in range(2):
            self.to_sib(stage, stream, at).start()

    def finish(self, stage, at):
        for stream in range(2):
            self.to_sib(stage, stream, at).wait_recv()
            total = self.held[stage, stream, at].astype(jnp.float32)
            total += self.sib_in[stage, stream, at].astype(jnp.float32)
            if stage == 3 and stream == 0:
                self.to_y(0, at).wait_recv()
                total += self.from_y[0, at].astype(jnp.float32)
            if stage == 3 and stream == 1:
                self.to_x(0, at).wait_recv()
                total += self.from_x[0, at].astype(jnp.float32)
            if stage == 2:
                self.out[:, self.cols(stream, at)] = total
            else:
                self.held[stage, stream, at] = total.astype(jnp.bfloat16)
        if stage != 2:
            step = (0, 1, None, 2)[stage]
            self.to_x(step, at, stage).start()
            self.to_y(step, at, stage).start()

    def run(self, line=None):
        for stage in range(4):
            def body(at, _, stage=stage):
                self.compute(stage, at)

                @pl.when(at > 0)
                def _():
                    self.finish(stage, at - 1)

                if line:
                    line.step(stage * self.counts + at)
                return 0

            lax.fori_loop(0, self.counts, body, 0)
            self.finish(stage, self.counts - 1)

    def end(self):
        def last(at, _):
            for half in range(2):
                xs, ys = (1, 2) if half == 0 else (2, 1)
                self.to_x(xs, at).wait_recv()
                self.to_y(ys, at).wait_recv()
                self.out[:, self.cols(half, at)] += self.from_x[xs, at].astype(
                    jnp.float32) + self.from_y[ys, at].astype(jnp.float32)
            for stage in range(4):
                for stream in range(2):
                    self.to_sib(stage, stream, at).wait_send()
            for step in range(3):
                self.to_x(step, at).wait_send()
                self.to_y(step, at).wait_send()
            return 0

        lax.fori_loop(0, self.counts, last, 0)


def reduce_scratch(counts, rows, width):
    low, dma = jnp.bfloat16, pltpu.SemaphoreType.DMA
    block = pltpu.VMEM((4, 2, counts, rows, width), low)
    landed = pltpu.VMEM((3, counts, rows, width), low)
    return [block] * 3 + [landed] * 2 + [dma((4, 2, counts))] * 2 + [dma((3, counts))] * 4


class Spread:
    def __init__(self, here, counts, refs):
        self.counts = counts
        self.got = refs[0]
        self.x_sems, self.y_sems, self.sib_sems = refs[1:3], refs[3:5], refs[5:7]
        self.core = here.core
        self.sib, self.xdev, self.ydev = here.device(0, 1), here.device(1, 0), here.device(2, 0)
        self.stages = (((1, 0), (2, 1)), ((1, 1), (2, 0)), ((3, 1), (3, 0)))

    def slot(self, across, half, at):
        return self.got.at[across, self.core, half, at]

    def x_copy(self, step, at):
        src = self.slot(0, step, at) if step < 2 else self.slot(2, 1, at)
        dst = self.slot(1, step, at) if step < 2 else self.slot(3, 1, at)
        return remote(src, dst, self.x_sems[0].at[step, at], self.x_sems[1].at[step, at], self.xdev)

    def y_copy(self, step, at):
        src = self.slot(0, 1 - step, at) if step < 2 else self.slot(1, 0, at)
        dst = self.slot(2, 1 - step, at) if step < 2 else self.slot(3, 0, at)
        return remote(src, dst, self.y_sems[0].at[step, at], self.y_sems[1].at[step, at], self.ydev)

    def sib_copy(self, stage, stream, at):
        across, half = (0, stream) if stage == 3 else self.stages[stage][stream]
        slot = self.slot(across, half, at)
        spot = (stage, stream, at)
        return remote(slot, slot, self.sib_sems[0].at[spot], self.sib_sems[1].at[spot], self.sib)

    def begin(self):
        for at in range(self.counts):
            self.x_copy(0, at).start()
            self.y_copy(0, at).start()
        for at in range(self.counts):
            self.sib_copy(3, 0, at).start()
            self.sib_copy(3, 1, at).start()

    def run(self, blocks, line=None, done=0):
        def own(at, _):
            for half in range(2):
                self.sib_copy(3, half, at).wait_recv()
                blocks(0, half, at, True)
            if line:
                line.step(done + at)
            return 0

        lax.fori_loop(0, self.counts, own, 0)

        def work(stage, at):
            for stream, (across, half) in enumerate(self.stages[stage]):
                self.sib_copy(stage, stream, at).wait_recv()
                blocks(across, half, at, False)

        for stage in range(3):
            def body(at, _, stage=stage):
                self.x_copy(stage, at).wait_recv()
                self.sib_copy(stage, 0, at).start()
                self.y_copy(stage, at).wait_recv()
                self.sib_copy(stage, 1, at).start()
                if stage < 2:
                    self.x_copy(stage + 1, at).start()
                    self.y_copy(stage + 1, at).start()

                @pl.when(at > 0)
                def _():
                    work(stage, at - 1)

                if line:
                    line.step(done + (stage + 1) * self.counts + at)
                return 0

            lax.fori_loop(0, self.counts, body, 0)
            work(stage, self.counts - 1)

    def end(self):
        def drain(at, _):
            for step in range(3):
                self.x_copy(step, at).wait_send()
                self.y_copy(step, at).wait_send()
            for stage in range(4):
                self.sib_copy(stage, 0, at).wait_send()
                self.sib_copy(stage, 1, at).wait_send()
            return 0

        lax.fori_loop(0, self.counts, drain, 0)


def spread_scratch(counts, rows, width):
    dma = pltpu.SemaphoreType.DMA
    return [pltpu.VMEM((4, 2, 2, counts, rows, width), jnp.bfloat16)] + [dma((3, counts))] * 4 + [
        dma((4, 2, counts))] * 2


def row_span(here, across, other, rows):
    return pl.ds(pl.multiple_of(here.shard(across, other) * rows, rows), rows)


def dot_nt(left, right):
    return lax.dot_general(left, right, (((1,), (1,)), ((), ())), preferred_element_type=jnp.float32)


def dot_tn(left, right):
    return lax.dot_general(left, right, (((0,), (0,)), ((), ())), preferred_element_type=jnp.float32)


def dot_nn(left, right):
    return jnp.dot(left, right, preferred_element_type=jnp.float32)


def products(here, act, weight_of, nt, rows, width, half_cols, shared):
    def product(across, other, half, at):
        first = half * half_cols if shared else 0
        cols = pl.ds(pl.multiple_of(first + at * width, width), width)
        block = act[row_span(here, across, other, rows), :]
        weight = weight_of(half)
        return dot_nt(block, weight[cols, :]) if nt else dot_nn(block, weight[:, cols])

    return product


def scatter_kernel(rows, width, counts, nt, shared, line_counts, act, *refs):
    refs = list(refs)
    here = Place()
    w0 = refs.pop(0)
    w1 = w0 if shared else refs.pop(0)
    tiny_own = refs.pop(0)
    line_own = refs.pop(0) if line_counts else None
    out, tiny_all = refs.pop(0), refs.pop(0)
    line = None
    if line_counts:
        line = Line(here, line_counts, [line_own, refs.pop(0)] + refs[13:])
    weights = (w0, w1)
    product = products(here, act, lambda half: weights[half], nt, rows, width, counts * width, shared)
    total = Reduce(here, counts, width, product, out, refs[:11])
    tiny = Tiny(here, tiny_own, tiny_all, refs[11:13], True)
    greet(here, tiny.peers, line is not None)
    if line:
        line.begin()
    tiny.begin()
    total.run(line)
    if line:
        line.end(4 * counts)
    total.end()
    tiny.end()


def scatter_product(act, weights, tiny, width, nt, cid, line=None, line_counts=16):
    total, depth = act.shape
    rows = total // 8
    shared = len(weights) == 1
    half = weights[0].shape[0 if nt else 1] // (2 if shared else 1)
    counts = half // width
    dma = pltpu.SemaphoreType.DMA
    vm = pl.BlockSpec(memory_space=pltpu.VMEM)
    out_shape = [
        jax.ShapeDtypeStruct((rows, 2 * half), jnp.float32),
        jax.ShapeDtypeStruct(tiny.shape, jnp.float32),
    ]
    scratch = reduce_scratch(counts, rows, width) + [dma((7,))] * 2
    operands = [act, *weights, tiny]
    if line is not None:
        operands.append(line)
        out_shape.append(jax.ShapeDtypeStruct(line.shape, line.dtype))
        scratch += line_scratch(line_counts, line.shape, line.dtype)
    kernel = functools.partial(scatter_kernel, rows, width, counts, nt, shared,
                               0 if line is None else line_counts)
    return kernel_call(kernel, out_shape, operands, [vm] * len(operands), scratch, cid, "scatter_product")


def gather_kernel(rows, width, counts, down, n_own, line_counts, act, *refs):
    refs = list(refs)
    here = Place()
    weights = [refs.pop(0) for _ in range(n_own)]
    payload = [refs.pop(0) for _ in range(n_own)]
    tiny_own = refs.pop(0)
    line_own = refs.pop(0) if line_counts else None
    sums = refs.pop(0)
    grads = [refs.pop(0) for _ in range(n_own)]
    tiny_all = refs.pop(0)
    line_out = refs.pop(0) if line_counts else None
    spread = Spread(here, counts, refs[:7])
    tiny = Tiny(here, tiny_own, tiny_all, refs[7:9], False)
    own_sem = refs[9]
    line = Line(here, line_counts, [line_own, line_out] + refs[10:]) if line_counts else None
    got, core = spread.got, here.core

    def part(half, at):
        first = half * counts * width if n_own == 1 else 0
        return pl.ds(pl.multiple_of(first + at * width, width), width)

    def own_copy(half, at):
        src = payload[half if n_own > 1 else 0].at[:, part(half, at)]
        return pltpu.make_async_copy(src, got.at[0, core, half, at], own_sem.at[half, at])

    for half in range(2):
        for at in range(counts):
            own_copy(half, at).start()
    greet(here, tiny.peers, line is not None)
    if line:
        line.begin()
    for at in range(counts):
        for half in range(2):
            own_copy(half, at).wait()
    spread.begin()
    tiny.begin()
    sums[...] = jnp.zeros_like(sums)

    def blocks(across, half, at, fresh):
        gained = None
        cols = part(half, at)
        weight = weights[half if n_own > 1 else 0]
        for other in range(2):
            row = row_span(here, across, other, rows)
            block = got[across, (core + other) % 2, half, at]
            if down:
                sums[row, :] += dot_nn(block, weight[cols, :])
                more = dot_tn(block, act[row, :])
            else:
                sums[row, :] += dot_nt(block, weight[:, cols])
                more = dot_nn(act[:, row], block)
            gained = more if gained is None else gained + more
        grad = grads[half if n_own > 1 else 0]
        where = (cols, slice(None)) if down else (slice(None), cols)
        if fresh:
            grad[where] = gained
        else:
            grad[where] += gained

    spread.run(blocks, line)
    if line:
        line.end(4 * counts)
    spread.end()
    tiny.end()


def gather_product(act, weights, payload, tiny, width, down, cid, line=None, line_counts=16):
    total, depth = act.shape if down else act.shape[::-1]
    rows = payload[0].shape[0]
    half = payload[0].shape[1] // (2 if len(payload) == 1 else 1)
    counts = half // width
    f32 = jnp.float32
    dma = pltpu.SemaphoreType.DMA
    vm = pl.BlockSpec(memory_space=pltpu.VMEM)
    hbm = pl.BlockSpec(memory_space=pl.ANY)
    out_shape = [jax.ShapeDtypeStruct((total, depth), f32)]
    out_shape += [jax.ShapeDtypeStruct(w.shape, f32) for w in weights]
    out_shape.append(jax.ShapeDtypeStruct((8,) + tiny.shape, f32))
    scratch = spread_scratch(counts, rows, width) + [dma((7,))] * 2 + [dma((2, counts))]
    operands = [act, *weights, *payload, tiny]
    specs = [vm] * (1 + len(weights)) + [hbm] * len(payload) + [vm]
    if line is not None:
        operands.append(line)
        specs.append(vm)
        out_shape.append(jax.ShapeDtypeStruct(line.shape, line.dtype))
        scratch += line_scratch(line_counts, line.shape, line.dtype)
    kernel = functools.partial(gather_kernel, rows, width, counts, down, len(weights),
                               0 if line is None else line_counts)
    return kernel_call(kernel, out_shape, operands, specs, scratch, cid, "gather_product")


def attend_kernel(rows, heads, cols, qkv, rms, cos, sin, mask, w_out, cot, tiny_own, part, mixed_all, g_col, kv,
                  probs, queries, tiny_pair, *refs):
    here = Place()
    spread = Spread(here, heads // 2, refs[:7])
    sums, pair_sems, turn_send, turn_recv, local_sem = refs[7:12]
    got, core = spread.got, here.core
    greet(here, slice_peers(here))
    me = here.shard(0, 0)

    def turn_copy(at):
        across, other = turned(at)
        first = pl.multiple_of(here.shard(across, other) * cols, cols)
        return remote(cot.at[:, pl.ds(first, cols)], g_col.at[pl.ds(pl.multiple_of(me * rows, rows), rows), :],
                      turn_send.at[at], turn_recv.at[at], here.device(across, other))

    own_turn = pltpu.make_async_copy(cot.at[:, pl.ds(pl.multiple_of(me * cols, cols), cols)],
                                     g_col.at[pl.ds(pl.multiple_of(me * rows, rows), rows), :], local_sem)
    own_turn.start()
    half = HD // 2
    scale = 1.0 / math.sqrt(HD)
    wide = heads * HD

    def rotated(first):
        lead = qkv[:, first : first + half] * rms[...]
        trail = qkv[:, first + half : first + HD] * rms[...]
        return lead * cos[...] - trail * sin[...], trail * cos[...] + lead * sin[...]

    low_k, high_k = rotated(wide)
    kv[0, :, :half] = low_k.astype(kv.dtype)
    kv[0, :, half:HD] = high_k.astype(kv.dtype)
    for at in range(2):
        first = HD + at * half
        kv[0, :, first : first + half] = (qkv[:, wide + first : wide + first + half] * rms[...]).astype(kv.dtype)
    tiny_pair[0] = tiny_own[...]
    pair = remote(kv.at[0], kv.at[1], pair_sems.at[0], pair_sems.at[1], spread.ydev)
    tiny = remote(tiny_own, tiny_pair.at[1], pair_sems.at[2], pair_sems.at[3], spread.ydev)
    for head in range(heads):
        if head == 1:
            pair.start()
            tiny.start()
            turn_copy(2 * (3 - 1)).start()
            turn_copy(2 * (3 - 1) + 1).start()
        lead, trail = rotated(head * HD)
        queries[:, head * HD : head * HD + half] = (lead * scale).astype(queries.dtype)
        queries[:, head * HD + half : (head + 1) * HD] = (trail * scale).astype(queries.dtype)
    pair.wait()
    for at in range(7):
        if at // 2 != 2:
            turn_copy(at).start()

    def one_head(head, _):
        query = queries[:, pl.ds(pl.multiple_of(head * HD, HD), HD)]
        scores = jnp.concatenate([dot_nt(query, kv[0, :, :HD]), dot_nt(query, kv[1, :, :HD])], axis=1)
        scores = jnp.where(mask[...] > 0, scores, NEG)
        expd = jnp.exp(scores - jnp.max(scores, axis=-1, keepdims=True))
        prob = expd / jnp.sum(expd, axis=-1, keepdims=True)
        probs[head] = prob
        prob_low = prob.astype(jnp.bfloat16)
        mixed = dot_nn(prob_low[:, :rows], kv[0, :, HD:]) + dot_nn(prob_low[:, rows:], kv[1, :, HD:])
        got[0, core, head // (heads // 2), head % (heads // 2)] = mixed.astype(got.dtype)
        return 0

    lax.fori_loop(0, heads, one_head, 0)
    sums[...] = jnp.zeros_like(sums)
    spread.begin()

    def blocks(across, half_at, at, fresh):
        span = pl.ds(pl.multiple_of((half_at * (heads // 2) + at) * HD, HD), HD)
        for other in range(2):
            row = row_span(here, across, other, rows)
            block = got[across, (core + other) % 2, half_at, at]
            mixed_all[row, span] = block
            sums[row, :] += dot_nn(block, w_out[span, :])

    spread.run(blocks)
    part[...] = sums[...].astype(part.dtype)
    spread.end()
    tiny.wait()
    own_turn.wait()
    for at in range(7):
        turn_copy(at).wait()


def attend(qkv, rms, cos, sin, mask, w_out, cot, tiny, cid):
    rows = qkv.shape[0]
    wide, cols = w_out.shape
    heads = wide // HD
    low, f32 = jnp.bfloat16, jnp.float32
    dma = pltpu.SemaphoreType.DMA
    vm = pl.BlockSpec(memory_space=pltpu.VMEM)
    out_shape = [
        jax.ShapeDtypeStruct((8 * rows, cols), low),
        jax.ShapeDtypeStruct((8 * rows, wide), low),
        jax.ShapeDtypeStruct((8 * rows, cols), low),
        jax.ShapeDtypeStruct((2, rows, 2 * HD), low),
        jax.ShapeDtypeStruct((heads, rows, 2 * rows), f32),
        jax.ShapeDtypeStruct((rows, wide), low),
        jax.ShapeDtypeStruct((2,) + tiny.shape, f32),
    ]
    scratch = spread_scratch(heads // 2, rows, HD) + [
        pltpu.VMEM((8 * rows, cols), f32), dma((4,)), dma((7,)), dma((7,)), dma(())]
    kernel = functools.partial(attend_kernel, rows, heads, cols)
    return kernel_call(kernel, out_shape, [qkv, rms, cos, sin, mask, w_out, cot, tiny], [vm] * 8, scratch, cid,
                       "attend")


def home_kernel(rows, heads, line_counts, d_attn, w_out, queries, kv, probs, rms, cos, sin, act_t, w_qkv, line_own,
                sums, grad, tiny_all, line_out, *refs):
    here = Place()
    width = HD
    counts, out_counts = heads // 2, (heads + 2) // 2
    refs = list(refs)
    total_refs, refs = refs[:11], refs[11:]
    spread = Spread(here, out_counts, refs[:7])
    d_mixed, tiny_own, d_kv, give, taken, give_sems, tiny_send, tiny_recv = refs[7:15]
    line = Line(here, line_counts, [line_own, line_out] + refs[15:])
    tiny = Tiny(here, tiny_own, tiny_all, (tiny_send, tiny_recv), False)
    got, core = spread.got, here.core
    product = products(here, d_attn, lambda half: w_out, True, rows, width, counts * width, True)
    total = Reduce(here, counts, width, product, d_mixed, total_refs)
    greet(here, tiny.peers, True)
    line.begin()
    total.run(line)
    done = 4 * counts
    total.end()
    half = HD // 2
    scale = 1.0 / math.sqrt(HD)
    depth = w_qkv.shape[0] * 8
    d_kv[...] = jnp.zeros_like(d_kv)

    def one_head(head, dots):
        span = pl.ds(pl.multiple_of(head * HD, HD), HD)
        query = queries[:, span]
        cot = d_mixed[:, span].astype(jnp.bfloat16)
        prob = probs[head]
        d_prob = jnp.concatenate([dot_nt(cot, kv[0, :, HD:]), dot_nt(cot, kv[1, :, HD:])], axis=1)
        delta = jnp.sum(prob * d_prob, axis=-1, keepdims=True)
        d_score = (prob * (d_prob - delta)).astype(jnp.bfloat16)
        prob_low = prob.astype(jnp.bfloat16)
        d_query = (dot_nn(d_score[:, :rows], kv[0, :, :HD]) + dot_nn(d_score[:, rows:], kv[1, :, :HD])) * scale
        for side in range(2):
            keys = slice(side * rows, (side + 1) * rows)
            d_kv[side, :, :HD] += dot_tn(d_score[:, keys], query)
            d_kv[side, :, HD:] += dot_tn(prob_low[:, keys], cot)
        dots = dots + jnp.sum(d_query * query.astype(jnp.float32), axis=-1, keepdims=True)
        lead, trail = d_query[:, :half], d_query[:, half:]
        slot = got.at[0, core, head // out_counts, head % out_counts]
        slot[:, :half] = ((lead * cos[0] + trail * sin[0]) * rms[0]).astype(got.dtype)
        slot[:, half:] = ((trail * cos[0] - lead * sin[0]) * rms[0]).astype(got.dtype)

        @pl.when(done + head < line_counts + 2)
        def _():
            line.step(done + head)
        return dots

    dots = lax.fori_loop(0, heads, one_head, jnp.zeros((rows, 1), jnp.float32))
    done += heads
    eye = (lax.broadcasted_iota(jnp.int32, (LANES, LANES), 0) ==
           lax.broadcasted_iota(jnp.int32, (LANES, LANES), 1)).astype(jnp.float32)
    tiny_own[...] = jnp.zeros_like(tiny_own)
    for side in (1, 0):
        d_key, d_value = d_kv[side, :, :HD], d_kv[side, :, HD:]
        own = jnp.sum(d_key * kv[side, :, :HD].astype(jnp.float32) +
                      d_value * kv[side, :, HD:].astype(jnp.float32), axis=-1, keepdims=True)
        if side == 0:
            own = own + dots * (1.0 / scale)
        own = own * (rms[side] * rms[side] * (1.0 / depth))
        for at in range(rows // LANES):
            tile = own[at * LANES : (at + 1) * LANES, :] * eye
            spot = side * (rows // LANES) + at
            tiny_own[spot : spot + 1, :] = jnp.sum(tile, axis=0, keepdims=True)
        lead, trail = d_key[:, :half], d_key[:, half:]
        parts = [(lead * cos[side] + trail * sin[side]) * rms[side],
                 (trail * cos[side] - lead * sin[side]) * rms[side],
                 d_value[:, :half] * rms[side], d_value[:, half:] * rms[side]]
        for at, value in enumerate(parts):
            if side == 1:
                give[:, at * half : (at + 1) * half] = value.astype(give.dtype)
            else:
                d_kv[0, :, at * half : (at + 1) * half] = value
    given = remote(give, taken, give_sems.at[0], give_sems.at[1], spread.ydev)
    given.start()
    sums[...] = jnp.zeros_like(sums)
    given.wait()
    for at in range(2):
        span = slice(at * HD, (at + 1) * HD)
        value = d_kv[0, :, span] + taken[:, span].astype(jnp.float32)
        got[0, core, 1, out_counts - 2 + at] = value.astype(got.dtype)
    tiny.begin()
    spread.begin()

    def blocks(across, half_at, at, fresh):
        span = pl.ds(pl.multiple_of((half_at * out_counts + at) * width, width), width)
        gained = None
        for other in range(2):
            row = row_span(here, across, other, rows)
            block = got[across, (core + other) % 2, half_at, at]
            sums[row, :] += dot_nt(block, w_qkv[:, span])
            more = dot_nn(act_t[:, row], block)
            gained = more if gained is None else gained + more
        if fresh:
            grad[:, span] = gained
        else:
            grad[:, span] += gained

    spread.run(blocks, line, done)
    line.end(done + 4 * out_counts)
    spread.end()
    tiny.end()


def home(d_attn, w_out, queries, kv, probs, rms, cos, sin, act_t, w_qkv, line, cid, line_counts=16):
    total, cols = d_attn.shape
    rows = total // 8
    wide = w_out.shape[0]
    heads = wide // HD
    low, f32 = jnp.bfloat16, jnp.float32
    dma = pltpu.SemaphoreType.DMA
    vm = pl.BlockSpec(memory_space=pltpu.VMEM)
    out_shape = [
        jax.ShapeDtypeStruct((total, cols), f32),
        jax.ShapeDtypeStruct(w_qkv.shape, f32),
        jax.ShapeDtypeStruct((8, 8, LANES), f32),
        jax.ShapeDtypeStruct(line.shape, line.dtype),
    ]
    scratch = reduce_scratch(heads // 2, rows, HD) + spread_scratch((heads + 2) // 2, rows, HD)
    scratch += [
        pltpu.VMEM((rows, wide), f32),
        pltpu.VMEM((8, LANES), f32),
        pltpu.VMEM((2, rows, 2 * HD), f32),
        pltpu.VMEM((rows, 2 * HD), low),
        pltpu.VMEM((rows, 2 * HD), low),
        dma((2,)), dma((7,)), dma((7,)),
    ] + line_scratch(line_counts, line.shape, low)
    operands = [d_attn, w_out, queries, kv, probs, rms, cos, sin, act_t, w_qkv, line]
    kernel = functools.partial(home_kernel, rows, heads, line_counts)
    return kernel_call(kernel, out_shape, operands, [vm] * len(operands), scratch, cid, "home")


def turn_kernel(rows, cols, back, src, out, own_sem, send, recv):
    here = Place()
    peers = [(a, o) for a in (3, 1, 2, 0) for o in range(2) if a + o > 0]
    greet(here, [here.device(a, o) for a, o in peers])

    def by_row(ref, shard):
        return ref.at[pl.ds(pl.multiple_of(shard * rows, rows), rows), :]

    def by_col(ref, shard):
        return ref.at[:, pl.ds(pl.multiple_of(shard * cols, cols), cols)]

    take, put = (by_row, by_col) if back else (by_col, by_row)
    me = here.shard(0, 0)

    def copy(at):
        across, other = peers[at]
        return remote(take(src, here.shard(across, other)), put(out, me), send.at[at], recv.at[at],
                      here.device(across, other))

    for at in range(7):
        copy(at).start()
    own = pltpu.make_async_copy(take(src, me), put(out, me), own_sem)
    own.start()
    own.wait()
    for at in range(7):
        copy(at).wait()


def turn(src, back, cid):
    rows, cols = (src.shape[0] // 8, src.shape[1]) if back else (src.shape[0], src.shape[1] // 8)
    shape = (rows, 8 * cols) if back else (8 * rows, cols)
    dma = pltpu.SemaphoreType.DMA
    vm = pl.BlockSpec(memory_space=pltpu.VMEM)
    return pl.pallas_call(
        functools.partial(turn_kernel, rows, cols, back),
        out_shape=jax.ShapeDtypeStruct(shape, src.dtype),
        in_specs=[vm],
        out_specs=vm,
        scratch_shapes=[dma(()), dma((7,)), dma((7,))],
        compiler_params=pltpu.CompilerParams(collective_id=cid, has_side_effects=True,
                                             vmem_limit_bytes=VMEM_LIMIT),
        name=f"turn_{cid}",
    )(src)

def close_kernel(rows, cols, per, extra, own, rest, other_own, tile, out, other_out, summed, tiles, ready, local_sem,
                 other_send, other_recv, put_send, put_recv, tile_send, tile_recv, *line_refs):
    here = Place()
    me = here.shard(0, 0)
    counts = 8 * per

    def target(at):
        turn_at = at // per
        return 3 - turn_at // 2, 1 - turn_at % 2

    def place(at):
        across, other = target(jnp.minimum(at, counts - 1))
        return jnp.where(at < counts, here.shard(across, other) * per + at % per, at)

    line = Line(here, counts + extra, [own, summed] + list(line_refs), place)
    peers = [turned(at) for at in range(7)]
    greet(here, slice_peers(here), True)
    line.begin()

    def tile_copy(step):
        return remote(tile, tiles.at[here.z], tile_send.at[step], tile_recv.at[step],
                      (here.dp, here.seq, (here.z + step + 1) % 4))

    for step in range(3):
        tile_copy(step).start()
    tiles[here.z] = tile[...]
    columns = pl.ds(pl.multiple_of(me * cols, cols), cols)

    def turn_copy(at):
        across, other = peers[at]
        src = other_own.at[pl.ds(pl.multiple_of(here.shard(across, other) * rows, rows), rows), :]
        return remote(src, other_out.at[:, columns], other_send.at[at], other_recv.at[at],
                      here.device(across, other))

    for at in range(7):
        turn_copy(at).start()
    mine = pltpu.make_async_copy(other_own.at[pl.ds(pl.multiple_of(me * rows, rows), rows), :],
                                 other_out.at[:, columns], local_sem)
    mine.start()
    chunk = line.chunk

    def put(at):
        across, other = target(at)
        dst = out.at[pl.ds(pl.multiple_of(at % per * chunk, chunk), chunk), columns]
        return remote(ready.at[at], dst, put_send.at[at], put_recv.at[at], here.device(across, other))

    def emit(at):
        total = rest[line.rows(at), :] + summed[line.rows(at), :].astype(jnp.float32)

        @pl.when(at < 7 * per)
        def _():
            ready[at] = total.astype(ready.dtype)
            put(at).start()

        @pl.when(at >= 7 * per)
        def _():
            out[pl.ds(pl.multiple_of(at % per * chunk, chunk), chunk), columns] = total.astype(out.dtype)

    @pl.when(line.inner == 1)
    def _():
        def both(at, _):
            line.step(at)

            @pl.when(jnp.logical_and(at > 1, at < counts + 2))
            def _():
                emit(at - 2)
            return 0

        lax.fori_loop(0, counts + extra + 2, both, 0)

        def drain(at, _):
            line.over(at).wait_send()
            line.down(at).wait_send()
            return 0

        lax.fori_loop(0, counts + extra, drain, 0)

    @pl.when(line.inner == 0)
    def _():
        def take(at, _):
            line.up(at).wait_send()
            line.down(at).wait_recv()

            @pl.when(at < counts)
            def _():
                emit(at)
            return 0

        lax.fori_loop(0, counts + extra, take, 0)

    mine.wait()
    for at in range(7):
        turn_copy(at).wait()

    def finish(at, _):
        put(at).wait()
        return 0

    lax.fori_loop(0, 7 * per, finish, 0)
    for step in range(3):
        tile_copy(step).wait()


def close(own, rest, other_own, tile, cid, per=2):
    total, cols = rest.shape
    rows = total // 8
    low = own.dtype
    dma = pltpu.SemaphoreType.DMA
    vm = pl.BlockSpec(memory_space=pltpu.VMEM)
    whole = jax.ShapeDtypeStruct((rows, 8 * cols), low)
    chunk = rows // per
    extra = (own.shape[0] - total) // chunk
    counts = 8 * per
    out_shape = [whole, whole, jax.ShapeDtypeStruct(own.shape, low), jax.ShapeDtypeStruct((4,) + tile.shape, tile.dtype)]
    scratch = [
        pltpu.VMEM((7 * per, chunk, cols), low),
        dma(()), dma((7,)), dma((7,)), dma((7 * per,)), dma((7 * per,)), dma((3,)), dma((3,)),
    ] + line_scratch(counts + extra, own.shape, low)
    kernel = functools.partial(close_kernel, rows, cols, per, extra)
    return kernel_call(kernel, out_shape, [own, rest, other_own, tile], [vm] * 4, scratch, cid, "close")


LANES = 128


def pack_rows(values):
    parts = values.reshape(8, -1, LANES)
    return jnp.pad(parts, ((0, 0), (0, 8 - parts.shape[1]), (0, 0)))


def acts_move(
    tokens, seg_ids, gain_attn, w_query, kv_weight, w_out, gain_ffn, w_gate, w_up, w_down, d_out
):
    low = jnp.bfloat16
    rows, width = tokens.shape
    seqs = lax.axis_size("seq")
    parts = lax.axis_size("dp") * seqs
    offset = lax.axis_index("seq") * rows
    places, cos_table, sin_table = place_tables(seg_ids)
    away = rows - offset

    def own_first(table):
        return jnp.stack(
            [
                lax.dynamic_slice_in_dim(table, offset, rows, 0),
                lax.dynamic_slice_in_dim(table, away, rows, 0),
            ]
        )

    pair_places = own_first(places)
    pair_segs = own_first(seg_ids)
    pair_cos = own_first(cos_table)
    pair_sin = own_first(sin_table)
    allowed = (pair_segs[0][:, None] == pair_segs.reshape(1, -1)) & (
        pair_places[0][:, None] >= pair_places.reshape(1, -1)
    )
    gain_one = gain_attn.astype(jnp.float32)
    gain_two = gain_ffn.astype(jnp.float32)
    qw = w_query.shape[1]
    ff = w_gate.shape[1]

    none = jnp.zeros((8, 8, LANES), jnp.float32)
    x_low = turn(tokens, False, 1)
    x_col = x_low.astype(jnp.float32)
    own_x = tokens.astype(jnp.float32)
    rms_one = lax.rsqrt(jnp.mean(own_x * own_x, axis=-1, keepdims=True) + EPS)
    act_one = (x_col * gain_one).astype(low)
    w_qkv = jnp.concatenate([w_query, kv_weight], axis=1)
    qkv = scatter_product(act_one, (w_qkv,), none, 256, False, 2)[0]
    tiles = rows // LANES
    attn_part, mixed_all, g_low, kv, probs, queries, rms_tiles = attend(
        qkv,
        jnp.broadcast_to(rms_one, (rows, LANES)),
        pair_cos[0],
        pair_sin[0],
        allowed.astype(jnp.float32),
        w_out,
        d_out,
        jnp.pad(rms_one.reshape(tiles, LANES), ((0, 8 - tiles), (0, 0))),
        3,
    )
    pair_rms = jnp.broadcast_to(rms_tiles[:, :tiles].reshape(2, rows, 1), (2, rows, LANES))
    d_hidden, _, attn = scatter_product(g_low, (w_down,), none, 512, True, 4, line=attn_part)
    resid = x_col + attn.astype(jnp.float32)
    act_two = (resid * gain_two).astype(low)
    squares = pack_rows(jnp.sum(resid * resid, axis=-1))
    both, squares_all = scatter_product(act_two, (w_gate, w_up), squares, 512, False, 6)
    mean_two = jnp.sum(squares_all[:, : rows // LANES], axis=0).reshape(rows, 1) / width
    rms_two = lax.rsqrt(mean_two + EPS)
    gate = both[:, :ff] * rms_two
    up_val = both[:, ff : 2 * ff] * rms_two
    gelu_val, gelu_pull = jax.vjp(gelu_tanh, gate)
    hidden = (gelu_val * up_val).astype(low)
    d_gate = gelu_pull(d_hidden * up_val)[0]
    d_up = d_hidden * gelu_val
    dots_two = jnp.sum(d_gate * gate + d_up * up_val, axis=-1, keepdims=True) * (
        rms_two * rms_two / width
    )
    dots_own = jnp.pad(dots_two.reshape(-1, LANES), ((0, 8 - rows // LANES), (0, 0)))
    d_act_two, grad_gate, grad_up, dots_all = gather_product(
        act_two.T,
        (w_gate, w_up),
        ((d_gate * rms_two).astype(low), (d_up * rms_two).astype(low)),
        dots_own,
        512,
        False,
        7,
    )
    dot_two = dots_all[:, : rows // LANES].reshape(parts * rows, 1)
    grad_gain_two = jnp.sum(d_act_two * resid, axis=0)
    ffn, grad_down, _, d_norm = gather_product(
        g_low,
        (w_down,),
        (hidden,),
        none[0],
        256,
        True,
        8,
        line=(d_act_two * gain_two - resid * dot_two).astype(low),
    )
    d_resid = g_low.astype(jnp.float32) + d_norm.astype(jnp.float32)
    d_attn = d_resid.astype(low)
    grad_out = matmul_tn(mixed_all, d_attn)

    d_act_one, grad_qkv, dots_all, ffn_sum = home(
        d_attn,
        w_out,
        queries,
        kv,
        probs,
        pair_rms,
        pair_cos,
        pair_sin,
        act_one.T,
        w_qkv,
        ffn.astype(low),
        9,
    )
    pairs = dots_all.reshape(parts // 2, 2, 8, LANES)
    dot_one = (pairs[:, :, :tiles] + pairs[:, ::-1, tiles : 2 * tiles]).reshape(parts * rows, 1)
    grad_gain_one = jnp.sum(d_act_one * x_col, axis=0)
    d_tokens, out, summed, gain_tiles = close(
        jnp.concatenate(
            [(d_act_one * gain_one - x_col * dot_one).astype(low), grad_qkv[:, qw:].astype(low)]
        ),
        d_resid,
        (resid + ffn_sum.astype(jnp.float32)).astype(low),
        jnp.stack([grad_gain_one, grad_gain_two]).reshape(8, LANES),
        10,
    )
    grad_query = grad_qkv[:, :qw]
    grad_kv = summed[parts * rows :].astype(jnp.float32)
    gains = jnp.sum(gain_tiles, axis=0).reshape(2, -1)
    return (
        out,
        d_tokens.astype(jnp.float32),
        gains[0],
        grad_query,
        grad_kv,
        grad_out,
        gains[1],
        grad_gate,
        grad_up,
        grad_down,
    )


def solution(mesh):
    in_specs = (
        P(("dp", "seq"), None),
        P("dp"),
        P(("dp", "seq")),
        P(("dp", "seq"), "tensor"),
        P(("dp", "seq"), None),
        P("tensor", ("dp", "seq")),
        P(("dp", "seq")),
        P(("dp", "seq"), "tensor"),
        P(("dp", "seq"), "tensor"),
        P("tensor", ("dp", "seq")),
        P(("dp", "seq"), None),
    )
    out_specs = (
        P(("dp", "seq"), None),
        P(("dp", "seq"), None),
        P(("dp", "seq")),
        P(("dp", "seq"), "tensor"),
        P(("dp", "seq"), None),
        P("tensor", ("dp", "seq")),
        P(("dp", "seq")),
        P(("dp", "seq"), "tensor"),
        P(("dp", "seq"), "tensor"),
        P("tensor", ("dp", "seq")),
    )

    def shards(*arrays):
        tokens = arrays[0]
        sizes = tuple(mesh.shape[name] for name in ("dp", "seq", "tensor"))
        count = tokens.shape[0] * sizes[0] * sizes[1]
        plan = acts_move if sizes == (4, 2, 4) and count <= tokens.shape[1] else weights_move
        return plan(*arrays)

    return jax.shard_map(shards, mesh=mesh, in_specs=in_specs, out_specs=out_specs, check_vma=False)
```

```python
import functools
import math

import jax
import jax.numpy as jnp
from jax import lax
from jax.experimental import pallas as pl
from jax.experimental.pallas import tpu as pltpu
from jax.sharding import PartitionSpec as P

HD = 256


EPS = 1e-06
NEG = -1e30


def place_tables(segs):
    length = segs.shape[0]
    index = jnp.arange(length, dtype=jnp.int32)
    flags = jnp.concatenate([jnp.ones((1,), dtype=bool), segs[1:] != segs[:-1]])
    starts = lax.cummax(jnp.where(flags, index, jnp.zeros_like(index)), axis=0)
    places = index - starts
    half_size = HD // 2
    freqs = jnp.exp(jnp.arange(half_size, dtype=jnp.float32) * (-math.log(10000.0) / half_size))
    angles = places.astype(jnp.float32)[:, None] * freqs[None, :]
    return (places, jnp.cos(angles), jnp.sin(angles))


def rotate(vector, cos_table, sin_table):
    half_size = vector.shape[-1] // 2
    leading = vector[..., :half_size]
    trailing = vector[..., half_size:]
    return jnp.concatenate(
        [leading * cos_table - trailing * sin_table, trailing * cos_table + leading * sin_table],
        axis=-1,
    )


def rotate_back(vector, cos_table, sin_table):
    half_size = vector.shape[-1] // 2
    leading = vector[..., :half_size]
    trailing = vector[..., half_size:]
    return jnp.concatenate(
        [leading * cos_table + trailing * sin_table, trailing * cos_table - leading * sin_table],
        axis=-1,
    )


def matmul(left, right):
    return jnp.dot(left, right, preferred_element_type=jnp.float32)


def matmul_nt(left, right):
    return lax.dot_general(
        left, right, (((1,), (1,)), ((), ())), preferred_element_type=jnp.float32
    )


def matmul_tn(left, right):
    return lax.dot_general(
        left, right, (((0,), (0,)), ((), ())), preferred_element_type=jnp.float32
    )


def gelu_tanh(values):
    return jax.nn.gelu(values, approximate=True)


def norm_back(d_act, normed, rms_val, gain_val):
    scaled = d_act * gain_val
    return rms_val * (scaled - normed * jnp.mean(scaled * normed, axis=-1, keepdims=True))


def weights_move(
    tokens, seg_ids, gain_attn, w_query, kv_weight, w_out, gain_ffn, w_gate, w_up, w_down, d_out
):
    rows = tokens.shape[0]
    scale_factor = 1.0 / math.sqrt(HD)
    offset = lax.axis_index("seq") * rows
    places, cos_table, sin_table = place_tables(seg_ids)
    own_places = lax.dynamic_slice_in_dim(places, offset, rows, 0)
    own_segs = lax.dynamic_slice_in_dim(seg_ids, offset, rows, 0)
    own_cos = lax.dynamic_slice_in_dim(cos_table, offset, rows, 0)
    own_sin = lax.dynamic_slice_in_dim(sin_table, offset, rows, 0)
    allowed = (own_segs[:, None] == seg_ids[None, :]) & (own_places[:, None] >= places[None, :])
    full_query, full_out, full_kv, full_gain_one = (
        lax.all_gather(w_query, ("dp", "seq"), axis=0, tiled=True),
        lax.all_gather(w_out, ("dp", "seq"), axis=1, tiled=True),
        lax.all_gather(kv_weight, ("dp", "seq"), axis=0, tiled=True),
        lax.all_gather(gain_attn, ("dp", "seq"), axis=0, tiled=True),
    )
    gain_one = full_gain_one.astype(jnp.float32)
    inputs = tokens.astype(jnp.float32)
    rms_one = lax.rsqrt(jnp.mean(inputs * inputs, axis=-1, keepdims=True) + EPS)
    norm_one = inputs * rms_one
    act_one = (norm_one * gain_one).astype(jnp.bfloat16)
    query_pre = matmul(act_one, full_query)
    heads = query_pre.shape[1] // HD
    kv_pre = matmul(act_one, full_kv)
    queries = (
        rotate(query_pre.reshape(rows, heads, HD), own_cos[:, None, :], own_sin[:, None, :])
        * scale_factor
    ).astype(jnp.bfloat16)
    own_kv = jnp.concatenate(
        [rotate(kv_pre[:, :HD], own_cos, own_sin), kv_pre[:, HD:]], axis=1
    ).astype(jnp.bfloat16)
    all_kv = lax.all_gather(own_kv, "seq", axis=0, tiled=True)
    keys = all_kv[:, :HD]
    values_all = all_kv[:, HD:]
    scores = jnp.einsum("rhd,kd->hrk", queries, keys, preferred_element_type=jnp.float32)
    scores = jnp.where(allowed[None], scores, NEG)
    top_score = jnp.max(scores, axis=-1, keepdims=True)
    expd = jnp.exp(scores - top_score)
    total = jnp.sum(expd, axis=-1, keepdims=True)
    log_total = top_score + jnp.log(total)
    probs_low = (expd / total).astype(jnp.bfloat16)
    mixed = (
        jnp.einsum("hrk,kd->rhd", probs_low, values_all, preferred_element_type=jnp.float32)
        .reshape(rows, heads * HD)
        .astype(jnp.bfloat16)
    )
    attn = lax.psum(matmul(mixed, full_out), "tensor")
    resid = inputs + attn
    full_gate, full_up, full_down, full_gain_two = (
        lax.all_gather(w_gate, ("dp", "seq"), axis=0, tiled=True),
        lax.all_gather(w_up, ("dp", "seq"), axis=0, tiled=True),
        lax.all_gather(w_down, ("dp", "seq"), axis=1, tiled=True),
        lax.all_gather(gain_ffn, ("dp", "seq"), axis=0, tiled=True),
    )
    gain_two = full_gain_two.astype(jnp.float32)
    rms_two = lax.rsqrt(jnp.mean(resid * resid, axis=-1, keepdims=True) + EPS)
    norm_two = resid * rms_two
    act_two = (norm_two * gain_two).astype(jnp.bfloat16)
    gate = matmul(act_two, full_gate)
    up_val = matmul(act_two, full_up)
    gelu_val, gelu_pull = jax.vjp(gelu_tanh, gate)
    hidden = (gelu_val * up_val).astype(jnp.bfloat16)
    ffn = lax.psum(matmul(hidden, full_down).astype(jnp.bfloat16), "tensor").astype(jnp.float32)
    out = (resid + ffn).astype(jnp.bfloat16)
    back_gate, back_up, back_down = (
        lax.all_gather(w_gate, ("dp", "seq"), axis=0, tiled=True),
        lax.all_gather(w_up, ("dp", "seq"), axis=0, tiled=True),
        lax.all_gather(w_down, ("dp", "seq"), axis=1, tiled=True),
    )
    d_hidden = matmul_nt(d_out, back_down)
    grad_down = matmul_tn(hidden, d_out)
    d_gate = gelu_pull(d_hidden * up_val)[0].astype(jnp.bfloat16)
    d_up = (d_hidden * gelu_val).astype(jnp.bfloat16)
    grad_gate = matmul_tn(act_two, d_gate)
    grad_up = matmul_tn(act_two, d_up)
    d_act_two = lax.psum(matmul_nt(d_gate, back_gate) + matmul_nt(d_up, back_up), "tensor")
    grad_gain_two = jnp.sum(d_act_two * norm_two, axis=0)
    d_resid = d_out.astype(jnp.float32) + norm_back(d_act_two, norm_two, rms_two, gain_two)
    ffn_grads = (
        lax.psum_scatter(
            grad_gate.astype(jnp.bfloat16), ("dp", "seq"), scatter_dimension=0, tiled=True
        ).astype(jnp.float32),
        lax.psum_scatter(
            grad_up.astype(jnp.bfloat16), ("dp", "seq"), scatter_dimension=0, tiled=True
        ).astype(jnp.float32),
        lax.psum_scatter(
            grad_down.astype(jnp.bfloat16), ("dp", "seq"), scatter_dimension=1, tiled=True
        ).astype(jnp.float32),
        lax.psum_scatter(
            grad_gain_two.astype(jnp.bfloat16), ("dp", "seq"), scatter_dimension=0, tiled=True
        ).astype(jnp.float32),
    )
    back_query, back_out, back_kv = (
        lax.all_gather(w_query, ("dp", "seq"), axis=0, tiled=True),
        lax.all_gather(w_out, ("dp", "seq"), axis=1, tiled=True),
        lax.all_gather(kv_weight, ("dp", "seq"), axis=0, tiled=True),
    )
    d_attn = d_resid.astype(jnp.bfloat16)
    grad_out = matmul_tn(mixed, d_attn)
    d_mixed = matmul_nt(d_attn, back_out).astype(jnp.bfloat16).reshape(rows, heads, HD)
    scores_again = jnp.einsum("rhd,kd->hrk", queries, keys, preferred_element_type=jnp.float32)
    probs = jnp.where(allowed[None], jnp.exp(scores_again - log_total), 0.0)
    d_probs = jnp.einsum("rhd,kd->hrk", d_mixed, values_all, preferred_element_type=jnp.float32)
    delta = jnp.sum(probs * d_probs, axis=-1, keepdims=True)
    d_scores = (probs * (d_probs - delta)).astype(jnp.bfloat16)
    d_queries = (
        jnp.einsum("hrk,kd->rhd", d_scores, keys, preferred_element_type=jnp.float32) * scale_factor
    )
    d_query_pre = (
        rotate_back(d_queries, own_cos[:, None, :], own_sin[:, None, :])
        .reshape(rows, heads * HD)
        .astype(jnp.bfloat16)
    )
    d_keys_part = jnp.einsum("hrk,rhd->kd", d_scores, queries, preferred_element_type=jnp.float32)
    d_values_part = jnp.einsum(
        "hrk,rhd->kd", probs.astype(jnp.bfloat16), d_mixed, preferred_element_type=jnp.float32
    )
    own_kv_grad = lax.psum_scatter(
        jnp.concatenate([d_keys_part, d_values_part], axis=1).astype(jnp.bfloat16),
        "seq",
        scatter_dimension=0,
        tiled=True,
    )
    d_act_query = matmul_nt(d_query_pre, back_query)
    d_act_sum, kv_grad = (
        lax.psum(d_act_query.astype(jnp.bfloat16), "tensor").astype(jnp.float32),
        lax.psum(own_kv_grad, "tensor").astype(jnp.float32),
    )
    d_kv_pre = jnp.concatenate(
        [rotate_back(kv_grad[:, :HD], own_cos, own_sin), kv_grad[:, HD:]], axis=1
    ).astype(jnp.bfloat16)
    d_act_one = d_act_sum + matmul_nt(d_kv_pre, back_kv)
    grad_query = matmul_tn(act_one, d_query_pre)
    grad_kv = matmul_tn(act_one, d_kv_pre)
    grad_gain_one = jnp.sum(d_act_one * norm_one, axis=0)
    d_tokens = d_resid + norm_back(d_act_one, norm_one, rms_one, gain_one)
    attn_grads = (
        lax.psum_scatter(
            grad_query.astype(jnp.bfloat16), ("dp", "seq"), scatter_dimension=0, tiled=True
        ).astype(jnp.float32),
        lax.psum_scatter(
            grad_out.astype(jnp.bfloat16), ("dp", "seq"), scatter_dimension=1, tiled=True
        ).astype(jnp.float32),
        lax.psum_scatter(
            grad_kv.astype(jnp.bfloat16), ("dp", "seq"), scatter_dimension=0, tiled=True
        ).astype(jnp.float32),
        lax.psum_scatter(
            grad_gain_one.astype(jnp.bfloat16), ("dp", "seq"), scatter_dimension=0, tiled=True
        ).astype(jnp.float32),
    )
    return (
        out,
        d_tokens,
        attn_grads[3],
        attn_grads[0],
        attn_grads[2],
        attn_grads[1],
        ffn_grads[3],
        ffn_grads[0],
        ffn_grads[1],
        ffn_grads[2],
    )


MESH = pl.DeviceIdType.MESH
VMEM_LIMIT = 66000 * 1024


class Place:
    def __init__(self):
        self.dp = lax.axis_index("dp")
        self.seq = lax.axis_index("seq")
        self.z = lax.axis_index("tensor")
        self.core = lax.rem(self.dp, 2)
        self.chip = lax.div(self.dp, 2)

    def device(self, across, other):
        chip = (self.chip + across) % 2
        seq = (self.seq + across // 2) % 2
        core = (self.core + other) % 2
        return chip * 2 + core, seq, self.z

    def shard(self, across, other):
        dp, seq, _ = self.device(across, other)
        return dp * 2 + seq


def greet(here, peers, line=False):
    barrier = pltpu.get_barrier_semaphore()
    peers = list(peers)
    if line:
        peers += [(here.dp, here.seq, (here.z + step) % 4) for step in range(1, 4)]
    for peer in peers:
        pl.semaphore_signal(barrier, inc=1, device_id=peer, device_id_type=MESH)
    pl.semaphore_wait(barrier, len(peers))


def remote(src, dst, send, recv, peer):
    return pltpu.make_async_remote_copy(
        src_ref=src, dst_ref=dst, send_sem=send, recv_sem=recv, device_id=peer, device_id_type=MESH
    )


class Line:
    def __init__(self, here, counts, refs, place=None):
        self.own, self.out, self.from_end, self.from_mid = refs[:4]
        self.sems = refs[4:10]
        self.counts = counts
        self.chunk = self.own.shape[0] // counts
        self.place = place
        z = here.z
        self.inner = ((z + 1) // 2) % 2
        self.mate = (here.dp, here.seq, z + 1 - 2 * (z % 2))
        self.other = (here.dp, here.seq, 3 - z)

    def rows(self, at):
        at = at if self.place is None else self.place(at)
        return pl.ds(pl.multiple_of(at * self.chunk, self.chunk), self.chunk)

    def up(self, at):
        return remote(self.own.at[self.rows(at), :], self.from_end.at[at], self.sems[0].at[at],
                      self.sems[1].at[at], self.mate)

    def over(self, at):
        return remote(self.out.at[self.rows(at), :], self.from_mid.at[at], self.sems[2].at[at],
                      self.sems[3].at[at], self.other)

    def down(self, at):
        rows = self.rows(at)
        return remote(self.out.at[rows, :], self.out.at[rows, :], self.sems[4].at[at],
                      self.sems[5].at[at], self.mate)

    def launch(self, first, count):
        @pl.when(self.inner == 0)
        def _():
            def send(at, _):
                self.up(first + at).start()
                return 0

            lax.fori_loop(0, count, send, 0)

    def begin(self):
        self.launch(0, self.counts)

    def first(self, at):
        rows = self.rows(at)
        self.up(at).wait_recv()
        total = self.own[rows, :].astype(jnp.float32) + self.from_end[at].astype(jnp.float32)
        self.out[rows, :] = total.astype(self.out.dtype)
        self.over(at).start()

    def second(self, at):
        rows = self.rows(at)
        self.over(at).wait()
        total = self.out[rows, :].astype(jnp.float32) + self.from_mid[at].astype(jnp.float32)
        self.out[rows, :] = total.astype(self.out.dtype)
        self.down(at).start()

    def step(self, at, start=0, count=None):
        count = self.counts if count is None else count

        @pl.when(jnp.logical_and(self.inner == 1, at < count))
        def _():
            self.first(start + at)

        @pl.when(jnp.logical_and(self.inner == 1, jnp.logical_and(at > 1, at < count + 2)))
        def _():
            self.second(start + at - 2)

    def steps(self, first, last, start=0, count=None):
        def rest(at, _):
            self.step(at, start, count)
            return 0

        lax.fori_loop(first, last, rest, 0)

    def settle(self):
        @pl.when(self.inner == 0)
        def _():
            def take(at, _):
                self.up(at).wait_send()
                self.down(at).wait_recv()
                return 0

            lax.fori_loop(0, self.counts, take, 0)

        @pl.when(self.inner == 1)
        def _():
            def drain(at, _):
                self.down(at).wait_send()
                return 0

            lax.fori_loop(0, self.counts, drain, 0)

    def end(self, done=0):
        self.steps(min(done, self.counts + 2), self.counts + 2)
        self.settle()


def line_scratch(counts, shape, low):
    buf = pltpu.VMEM((counts, shape[0] // counts, shape[1]), low)
    return [buf, buf] + [pltpu.SemaphoreType.DMA((counts,))] * 6


def turned(at):
    return 3 - at // 2, 1 - at % 2


def slice_peers(here):
    return [here.device(*turned(at)) for at in range(7)]


def kernel_call(kernel, out_shape, operands, specs, scratch, cid, name):
    vm = pl.BlockSpec(memory_space=pltpu.VMEM)
    return pl.pallas_call(
        kernel,
        out_shape=out_shape,
        in_specs=specs,
        out_specs=[vm] * len(out_shape),
        scratch_shapes=scratch,
        compiler_params=pltpu.CompilerParams(
            collective_id=cid, has_side_effects=True, vmem_limit_bytes=VMEM_LIMIT
        ),
        name=f"{name}_{cid}",
    )(*operands)


class Tiny:
    def __init__(self, here, src, dst, sems, spread):
        self.here, self.src, self.dst, self.sems, self.spread = here, src, dst, sems, spread
        self.peers = slice_peers(here)
        self.me = here.shard(0, 0)

    def tile(self, shard):
        return self.src.at[shard] if self.spread else self.src

    def copy(self, at):
        return remote(self.tile(self.here.shard(*turned(at))), self.dst.at[self.me], self.sems[0].at[at],
                      self.sems[1].at[at], self.peers[at])

    def begin(self):
        for at in range(7):
            self.copy(at).start()
        self.dst[self.me] = self.tile(self.me)[...]

    def end(self):
        for at in range(7):
            self.copy(at).wait()


class Reduce:
    def __init__(self, here, counts, width, product, out, refs):
        self.counts, self.width, self.product, self.out = counts, width, product, out
        self.held, self.sib_out, self.sib_in, self.from_x, self.from_y = refs[:5]
        self.sib_sems, self.x_sems, self.y_sems = refs[5:7], refs[7:9], refs[9:11]
        self.sib, self.xdev, self.ydev = here.device(0, 1), here.device(1, 0), here.device(2, 0)
        self.stages = (((3, 0), (3, 1)), ((1, 0), (2, 1)), ((0, 0), (0, 1)), ((1, 1), (2, 0)))

    def to_sib(self, stage, stream, at):
        spot = (stage, stream, at)
        return remote(self.sib_out.at[spot], self.sib_in.at[spot], self.sib_sems[0].at[spot],
                      self.sib_sems[1].at[spot], self.sib)

    def to_x(self, step, at, stage=0):
        return remote(self.held.at[stage, 0, at], self.from_x.at[step, at], self.x_sems[0].at[step, at],
                      self.x_sems[1].at[step, at], self.xdev)

    def to_y(self, step, at, stage=0):
        return remote(self.held.at[stage, 1, at], self.from_y.at[step, at], self.y_sems[0].at[step, at],
                      self.y_sems[1].at[step, at], self.ydev)

    def cols(self, half, at):
        return pl.ds(pl.multiple_of((half * self.counts + at) * self.width, self.width), self.width)

    def compute(self, stage, at):
        for stream, (across, half) in enumerate(self.stages[stage]):
            self.sib_out[stage, stream, at] = self.product(across, 1, half, at).astype(jnp.bfloat16)
            self.held[stage, stream, at] = self.product(across, 0, half, at).astype(jnp.bfloat16)
        for stream in range(2):
            self.to_sib(stage, stream, at).start()

    def finish(self, stage, at):
        for stream in range(2):
            self.to_sib(stage, stream, at).wait_recv()
            total = self.held[stage, stream, at].astype(jnp.float32)
            total += self.sib_in[stage, stream, at].astype(jnp.float32)
            if stage == 3 and stream == 0:
                self.to_y(0, at).wait_recv()
                total += self.from_y[0, at].astype(jnp.float32)
            if stage == 3 and stream == 1:
                self.to_x(0, at).wait_recv()
                total += self.from_x[0, at].astype(jnp.float32)
            if stage == 2:
                self.out[:, self.cols(stream, at)] = total
            else:
                self.held[stage, stream, at] = total.astype(jnp.bfloat16)
        if stage != 2:
            step = (0, 1, None, 2)[stage]
            self.to_x(step, at, stage).start()
            self.to_y(step, at, stage).start()

    def run(self, line=None):
        for stage in range(4):
            def body(at, _, stage=stage):
                self.compute(stage, at)

                @pl.when(at > 0)
                def _():
                    self.finish(stage, at - 1)

                if line:
                    line.step(stage * self.counts + at)
                return 0

            lax.fori_loop(0, self.counts, body, 0)
            self.finish(stage, self.counts - 1)

    def end(self):
        def last(at, _):
            for half in range(2):
                xs, ys = (1, 2) if half == 0 else (2, 1)
                self.to_x(xs, at).wait_recv()
                self.to_y(ys, at).wait_recv()
                self.out[:, self.cols(half, at)] += self.from_x[xs, at].astype(
                    jnp.float32) + self.from_y[ys, at].astype(jnp.float32)
            for stage in range(4):
                for stream in range(2):
                    self.to_sib(stage, stream, at).wait_send()
            for step in range(3):
                self.to_x(step, at).wait_send()
                self.to_y(step, at).wait_send()
            return 0

        lax.fori_loop(0, self.counts, last, 0)


def reduce_scratch(counts, rows, width):
    low, dma = jnp.bfloat16, pltpu.SemaphoreType.DMA
    block = pltpu.VMEM((4, 2, counts, rows, width), low)
    landed = pltpu.VMEM((3, counts, rows, width), low)
    return [block] * 3 + [landed] * 2 + [dma((4, 2, counts))] * 2 + [dma((3, counts))] * 4


class Spread:
    def __init__(self, here, counts, refs):
        self.counts = counts
        self.got = refs[0]
        self.x_sems, self.y_sems, self.sib_sems = refs[1:3], refs[3:5], refs[5:7]
        self.core = here.core
        self.sib, self.xdev, self.ydev = here.device(0, 1), here.device(1, 0), here.device(2, 0)
        self.stages = (((1, 0), (2, 1)), ((1, 1), (2, 0)), ((3, 1), (3, 0)))

    def slot(self, across, half, at):
        return self.got.at[across, self.core, half, at]

    def x_copy(self, step, at):
        src = self.slot(0, step, at) if step < 2 else self.slot(2, 1, at)
        dst = self.slot(1, step, at) if step < 2 else self.slot(3, 1, at)
        return remote(src, dst, self.x_sems[0].at[step, at], self.x_sems[1].at[step, at], self.xdev)

    def y_copy(self, step, at):
        src = self.slot(0, 1 - step, at) if step < 2 else self.slot(1, 0, at)
        dst = self.slot(2, 1 - step, at) if step < 2 else self.slot(3, 0, at)
        return remote(src, dst, self.y_sems[0].at[step, at], self.y_sems[1].at[step, at], self.ydev)

    def sib_copy(self, stage, stream, at):
        across, half = (0, stream) if stage == 3 else self.stages[stage][stream]
        slot = self.slot(across, half, at)
        spot = (stage, stream, at)
        return remote(slot, slot, self.sib_sems[0].at[spot], self.sib_sems[1].at[spot], self.sib)

    def begin(self):
        for at in range(self.counts):
            self.x_copy(0, at).start()
            self.y_copy(0, at).start()
        for at in range(self.counts):
            self.sib_copy(3, 0, at).start()
            self.sib_copy(3, 1, at).start()

    def run(self, blocks, line=None, hook=None, between=None):
        if hook is None:
            def hook(stage, at):
                if line:
                    line.step((stage + 1) * self.counts + at)

        def own(at, _):
            for half in range(2):
                self.sib_copy(3, half, at).wait_recv()
                blocks(0, half, at, True)
            hook(-1, at)
            return 0

        lax.fori_loop(0, self.counts, own, 0)
        if between:
            between(-1)

        def work(stage, at):
            for stream, (across, half) in enumerate(self.stages[stage]):
                self.sib_copy(stage, stream, at).wait_recv()
                blocks(across, half, at, False)

        for stage in range(3):
            def body(at, _, stage=stage):
                self.x_copy(stage, at).wait_recv()
                self.sib_copy(stage, 0, at).start()
                self.y_copy(stage, at).wait_recv()
                self.sib_copy(stage, 1, at).start()
                if stage < 2:
                    self.x_copy(stage + 1, at).start()
                    self.y_copy(stage + 1, at).start()

                @pl.when(at > 0)
                def _():
                    work(stage, at - 1)

                hook(stage, at)
                return 0

            lax.fori_loop(0, self.counts, body, 0)
            work(stage, self.counts - 1)
            if between:
                between(stage)

    def end(self):
        def drain(at, _):
            for step in range(3):
                self.x_copy(step, at).wait_send()
                self.y_copy(step, at).wait_send()
            for stage in range(4):
                self.sib_copy(stage, 0, at).wait_send()
                self.sib_copy(stage, 1, at).wait_send()
            return 0

        lax.fori_loop(0, self.counts, drain, 0)


def spread_scratch(counts, rows, width):
    dma = pltpu.SemaphoreType.DMA
    return [pltpu.VMEM((4, 2, 2, counts, rows, width), jnp.bfloat16)] + [dma((3, counts))] * 4 + [
        dma((4, 2, counts))] * 2


def row_span(here, across, other, rows):
    return pl.ds(pl.multiple_of(here.shard(across, other) * rows, rows), rows)


def dot_nt(left, right):
    return lax.dot_general(left, right, (((1,), (1,)), ((), ())), preferred_element_type=jnp.float32)


def dot_tn(left, right):
    return lax.dot_general(left, right, (((0,), (0,)), ((), ())), preferred_element_type=jnp.float32)


def dot_nn(left, right):
    return jnp.dot(left, right, preferred_element_type=jnp.float32)


def products(here, act, weight_of, nt, rows, width, half_cols, shared):
    def product(across, other, half, at):
        first = half * half_cols if shared else 0
        cols = pl.ds(pl.multiple_of(first + at * width, width), width)
        block = act[row_span(here, across, other, rows), :]
        weight = weight_of(half)
        return dot_nt(block, weight[cols, :]) if nt else dot_nn(block, weight[:, cols])

    return product


def scatter_kernel(rows, width, counts, nt, shared, line_counts, act, *refs):
    refs = list(refs)
    here = Place()
    w0 = refs.pop(0)
    w1 = w0 if shared else refs.pop(0)
    tiny_own = refs.pop(0)
    line_own = refs.pop(0) if line_counts else None
    out, tiny_all = refs.pop(0), refs.pop(0)
    line = None
    if line_counts:
        line = Line(here, line_counts, [line_own, refs.pop(0)] + refs[13:])
    weights = (w0, w1)
    product = products(here, act, lambda half: weights[half], nt, rows, width, counts * width, shared)
    total = Reduce(here, counts, width, product, out, refs[:11])
    tiny = Tiny(here, tiny_own, tiny_all, refs[11:13], True)
    greet(here, tiny.peers, line is not None)
    if line:
        line.begin()
    tiny.begin()
    total.run(line)
    if line:
        line.end(4 * counts)
    total.end()
    tiny.end()


def scatter_product(act, weights, tiny, width, nt, cid, line=None, line_counts=16):
    total, depth = act.shape
    rows = total // 8
    shared = len(weights) == 1
    half = weights[0].shape[0 if nt else 1] // (2 if shared else 1)
    counts = half // width
    dma = pltpu.SemaphoreType.DMA
    vm = pl.BlockSpec(memory_space=pltpu.VMEM)
    out_shape = [
        jax.ShapeDtypeStruct((rows, 2 * half), jnp.float32),
        jax.ShapeDtypeStruct(tiny.shape, jnp.float32),
    ]
    scratch = reduce_scratch(counts, rows, width) + [dma((7,))] * 2
    operands = [act, *weights, tiny]
    if line is not None:
        operands.append(line)
        out_shape.append(jax.ShapeDtypeStruct(line.shape, line.dtype))
        scratch += line_scratch(line_counts, line.shape, line.dtype)
    kernel = functools.partial(scatter_kernel, rows, width, counts, nt, shared,
                               0 if line is None else line_counts)
    return kernel_call(kernel, out_shape, operands, [vm] * len(operands), scratch, cid, "scatter_product")


def gather_kernel(rows, width, counts, down, n_own, line_counts, act, *refs):
    refs = list(refs)
    here = Place()
    weights = [refs.pop(0) for _ in range(n_own)]
    payload = [refs.pop(0) for _ in range(n_own)]
    tiny_own = refs.pop(0)
    line_own = refs.pop(0) if line_counts else None
    sums = refs.pop(0)
    grads = [refs.pop(0) for _ in range(n_own)]
    tiny_all = refs.pop(0)
    line_out = refs.pop(0) if line_counts else None
    spread = Spread(here, counts, refs[:7])
    tiny = Tiny(here, tiny_own, tiny_all, refs[7:9], False)
    own_sem = refs[9]
    line = Line(here, line_counts, [line_own, line_out] + refs[10:]) if line_counts else None
    got, core = spread.got, here.core

    def part(half, at):
        first = half * counts * width if n_own == 1 else 0
        return pl.ds(pl.multiple_of(first + at * width, width), width)

    def own_copy(half, at):
        src = payload[half if n_own > 1 else 0].at[:, part(half, at)]
        return pltpu.make_async_copy(src, got.at[0, core, half, at], own_sem.at[half, at])

    for half in range(2):
        for at in range(counts):
            own_copy(half, at).start()
    greet(here, tiny.peers, line is not None)
    if line:
        line.begin()
    for at in range(counts):
        for half in range(2):
            own_copy(half, at).wait()
    spread.begin()
    tiny.begin()
    sums[...] = jnp.zeros_like(sums)

    def blocks(across, half, at, fresh):
        gained = None
        cols = part(half, at)
        weight = weights[half if n_own > 1 else 0]
        for other in range(2):
            row = row_span(here, across, other, rows)
            block = got[across, (core + other) % 2, half, at]
            if down:
                sums[row, :] += dot_nn(block, weight[cols, :])
                more = dot_tn(block, act[row, :])
            else:
                sums[row, :] += dot_nt(block, weight[:, cols])
                more = dot_nn(act[:, row], block)
            gained = more if gained is None else gained + more
        grad = grads[half if n_own > 1 else 0]
        where = (cols, slice(None)) if down else (slice(None), cols)
        if fresh:
            grad[where] = gained
        else:
            grad[where] += gained

    spread.run(blocks, line)
    if line:
        line.end(4 * counts)
    spread.end()
    tiny.end()


def gather_product(act, weights, payload, tiny, width, down, cid, line=None, line_counts=16):
    total, depth = act.shape if down else act.shape[::-1]
    rows = payload[0].shape[0]
    half = payload[0].shape[1] // (2 if len(payload) == 1 else 1)
    counts = half // width
    f32 = jnp.float32
    dma = pltpu.SemaphoreType.DMA
    vm = pl.BlockSpec(memory_space=pltpu.VMEM)
    hbm = pl.BlockSpec(memory_space=pl.ANY)
    out_shape = [jax.ShapeDtypeStruct((total, depth), f32)]
    out_shape += [jax.ShapeDtypeStruct(w.shape, f32) for w in weights]
    out_shape.append(jax.ShapeDtypeStruct((8,) + tiny.shape, f32))
    scratch = spread_scratch(counts, rows, width) + [dma((7,))] * 2 + [dma((2, counts))]
    operands = [act, *weights, *payload, tiny]
    specs = [vm] * (1 + len(weights)) + [hbm] * len(payload) + [vm]
    if line is not None:
        operands.append(line)
        specs.append(vm)
        out_shape.append(jax.ShapeDtypeStruct(line.shape, line.dtype))
        scratch += line_scratch(line_counts, line.shape, line.dtype)
    kernel = functools.partial(gather_kernel, rows, width, counts, down, len(weights),
                               0 if line is None else line_counts)
    return kernel_call(kernel, out_shape, operands, specs, scratch, cid, "gather_product")


def attend_kernel(rows, heads, cols, qkv, rms, cos, sin, mask, w_out, cot, tiny_own, part, mixed_all, g_col, kv,
                  probs, queries, tiny_pair, *refs):
    here = Place()
    spread = Spread(here, heads // 2, refs[:7])
    sums, pair_sems, turn_send, turn_recv, local_sem = refs[7:12]
    got, core = spread.got, here.core
    greet(here, slice_peers(here))
    me = here.shard(0, 0)

    def turn_copy(at):
        across, other = turned(at)
        first = pl.multiple_of(here.shard(across, other) * cols, cols)
        return remote(cot.at[:, pl.ds(first, cols)], g_col.at[pl.ds(pl.multiple_of(me * rows, rows), rows), :],
                      turn_send.at[at], turn_recv.at[at], here.device(across, other))

    own_turn = pltpu.make_async_copy(cot.at[:, pl.ds(pl.multiple_of(me * cols, cols), cols)],
                                     g_col.at[pl.ds(pl.multiple_of(me * rows, rows), rows), :], local_sem)
    own_turn.start()
    half = HD // 2
    scale = 1.0 / math.sqrt(HD)
    wide = heads * HD

    def rotated(first):
        lead = qkv[:, first : first + half] * rms[...]
        trail = qkv[:, first + half : first + HD] * rms[...]
        return lead * cos[...] - trail * sin[...], trail * cos[...] + lead * sin[...]

    low_k, high_k = rotated(wide)
    kv[0, :, :half] = low_k.astype(kv.dtype)
    kv[0, :, half:HD] = high_k.astype(kv.dtype)
    for at in range(2):
        first = HD + at * half
        kv[0, :, first : first + half] = (qkv[:, wide + first : wide + first + half] * rms[...]).astype(kv.dtype)
    tiny_pair[0] = tiny_own[...]
    pair = remote(kv.at[0], kv.at[1], pair_sems.at[0], pair_sems.at[1], spread.ydev)
    tiny = remote(tiny_own, tiny_pair.at[1], pair_sems.at[2], pair_sems.at[3], spread.ydev)
    for head in range(heads):
        if head == 1:
            pair.start()
            tiny.start()
            turn_copy(2 * (3 - 1)).start()
            turn_copy(2 * (3 - 1) + 1).start()
        lead, trail = rotated(head * HD)
        queries[:, head * HD : head * HD + half] = (lead * scale).astype(queries.dtype)
        queries[:, head * HD + half : (head + 1) * HD] = (trail * scale).astype(queries.dtype)
    pair.wait()
    for at in range(7):
        if at // 2 != 2:
            turn_copy(at).start()

    def one_head(head, _):
        query = queries[:, pl.ds(pl.multiple_of(head * HD, HD), HD)]
        scores = jnp.concatenate([dot_nt(query, kv[0, :, :HD]), dot_nt(query, kv[1, :, :HD])], axis=1)
        scores = jnp.where(mask[...] > 0, scores, NEG)
        expd = jnp.exp(scores - jnp.max(scores, axis=-1, keepdims=True))
        prob = expd / jnp.sum(expd, axis=-1, keepdims=True)
        probs[head] = prob
        prob_low = prob.astype(jnp.bfloat16)
        mixed = dot_nn(prob_low[:, :rows], kv[0, :, HD:]) + dot_nn(prob_low[:, rows:], kv[1, :, HD:])
        got[0, core, head // (heads // 2), head % (heads // 2)] = mixed.astype(got.dtype)
        return 0

    lax.fori_loop(0, heads, one_head, 0)
    sums[...] = jnp.zeros_like(sums)
    spread.begin()

    def blocks(across, half_at, at, fresh):
        span = pl.ds(pl.multiple_of((half_at * (heads // 2) + at) * HD, HD), HD)
        for other in range(2):
            row = row_span(here, across, other, rows)
            block = got[across, (core + other) % 2, half_at, at]
            mixed_all[row, span] = block
            sums[row, :] += dot_nn(block, w_out[span, :])

    spread.run(blocks)
    part[...] = sums[...].astype(part.dtype)
    spread.end()
    tiny.wait()
    own_turn.wait()
    for at in range(7):
        turn_copy(at).wait()


def attend(qkv, rms, cos, sin, mask, w_out, cot, tiny, cid):
    rows = qkv.shape[0]
    wide, cols = w_out.shape
    heads = wide // HD
    low, f32 = jnp.bfloat16, jnp.float32
    dma = pltpu.SemaphoreType.DMA
    vm = pl.BlockSpec(memory_space=pltpu.VMEM)
    out_shape = [
        jax.ShapeDtypeStruct((8 * rows, cols), low),
        jax.ShapeDtypeStruct((8 * rows, wide), low),
        jax.ShapeDtypeStruct((8 * rows, cols), low),
        jax.ShapeDtypeStruct((2, rows, 2 * HD), low),
        jax.ShapeDtypeStruct((heads, rows, 2 * rows), f32),
        jax.ShapeDtypeStruct((rows, wide), low),
        jax.ShapeDtypeStruct((2,) + tiny.shape, f32),
    ]
    scratch = spread_scratch(heads // 2, rows, HD) + [
        pltpu.VMEM((8 * rows, cols), f32), dma((4,)), dma((7,)), dma((7,)), dma(())]
    kernel = functools.partial(attend_kernel, rows, heads, cols)
    return kernel_call(kernel, out_shape, [qkv, rms, cos, sin, mask, w_out, cot, tiny], [vm] * 8, scratch, cid,
                       "attend")


def tail_kernel(rows, heads, per, d_attn, w_out, queries, kv, probs, rms, cos, sin, act_t, w_qkv, ffn, x_low,
                resid, gain, gain_grad, d_tok, out, grad, kv_sum, gain_tiles, *refs):
    here = Place()
    width = HD
    counts, out_counts = heads // 2, (heads + 2) // 2
    refs = list(refs)
    line_counts = 8 * per
    cols = d_attn.shape[1]
    extra = cols // (rows // per)

    def take(count):
        taken_refs = refs[:count]
        del refs[:count]
        return taken_refs

    total_refs = take(11)
    spread = Spread(here, out_counts, take(7))
    d_mixed, tiny_own, tiny_all, d_kv, give, taken, give_sems, tiny_send, tiny_recv = take(9)
    sums, gain_sum, tile, tile_send, tile_recv, put_sems, local_sems = take(7)

    def far(at):
        return turned(at // per)

    def near(at):
        return at // (2 * per), at // per % 2

    def place_ffn(at):
        return here.shard(*far(at)) * per + at % per

    def place_tok(at):
        return jnp.where(at < line_counts, here.shard(*near(jnp.minimum(at, line_counts - 1))) * per + at % per, at)

    ffn_sum = take(1)[0]
    line = Line(here, line_counts, [ffn, ffn_sum] + take(8), place_ffn)
    contrib, summed = take(2)
    line_tok = Line(here, line_counts + extra, [contrib, summed] + take(8), place_tok)
    tiny = Tiny(here, tiny_own, tiny_all, (tiny_send, tiny_recv), False)
    got, core = spread.got, here.core
    product = products(here, d_attn, lambda half: w_out, True, rows, width, counts * width, True)
    total = Reduce(here, counts, width, product, d_mixed, total_refs)
    greet(here, tiny.peers, True)
    line.begin()
    total.run(line)
    done = 4 * counts
    total.end()
    half = HD // 2
    scale = 1.0 / math.sqrt(HD)
    depth = w_qkv.shape[0] * 8
    d_kv[...] = jnp.zeros_like(d_kv)

    def one_head(head, dots):
        span = pl.ds(pl.multiple_of(head * HD, HD), HD)
        query = queries[:, span]
        cot = d_mixed[:, span].astype(jnp.bfloat16)
        prob = probs[head]
        d_prob = jnp.concatenate([dot_nt(cot, kv[0, :, HD:]), dot_nt(cot, kv[1, :, HD:])], axis=1)
        delta = jnp.sum(prob * d_prob, axis=-1, keepdims=True)
        d_score = (prob * (d_prob - delta)).astype(jnp.bfloat16)
        prob_low = prob.astype(jnp.bfloat16)
        d_query = (dot_nn(d_score[:, :rows], kv[0, :, :HD]) + dot_nn(d_score[:, rows:], kv[1, :, :HD])) * scale
        for side in range(2):
            keys = slice(side * rows, (side + 1) * rows)
            d_kv[side, :, :HD] += dot_tn(d_score[:, keys], query)
            d_kv[side, :, HD:] += dot_tn(prob_low[:, keys], cot)
        dots = dots + jnp.sum(d_query * query.astype(jnp.float32), axis=-1, keepdims=True)
        lead, trail = d_query[:, :half], d_query[:, half:]
        slot = got.at[0, core, head // out_counts, head % out_counts]
        slot[:, :half] = ((lead * cos[0] + trail * sin[0]) * rms[0]).astype(got.dtype)
        slot[:, half:] = ((trail * cos[0] - lead * sin[0]) * rms[0]).astype(got.dtype)

        line.step(done + head)
        return dots

    dots = lax.fori_loop(0, heads, one_head, jnp.zeros((rows, 1), jnp.float32))
    done += heads
    eye = (lax.broadcasted_iota(jnp.int32, (LANES, LANES), 0) ==
           lax.broadcasted_iota(jnp.int32, (LANES, LANES), 1)).astype(jnp.float32)
    tiny_own[...] = jnp.zeros_like(tiny_own)
    for side in (1, 0):
        d_key, d_value = d_kv[side, :, :HD], d_kv[side, :, HD:]
        own = jnp.sum(d_key * kv[side, :, :HD].astype(jnp.float32) +
                      d_value * kv[side, :, HD:].astype(jnp.float32), axis=-1, keepdims=True)
        if side == 0:
            own = own + dots * (1.0 / scale)
        own = own * (rms[side] * rms[side] * (1.0 / depth))
        for at in range(rows // LANES):
            spot_values = own[at * LANES : (at + 1) * LANES, :] * eye
            spot = side * (rows // LANES) + at
            tiny_own[spot : spot + 1, :] = jnp.sum(spot_values, axis=0, keepdims=True)
        lead, trail = d_key[:, :half], d_key[:, half:]
        parts = [(lead * cos[side] + trail * sin[side]) * rms[side],
                 (trail * cos[side] - lead * sin[side]) * rms[side],
                 d_value[:, :half] * rms[side], d_value[:, half:] * rms[side]]
        for at, value in enumerate(parts):
            if side == 1:
                give[:, at * half : (at + 1) * half] = value.astype(give.dtype)
            else:
                d_kv[0, :, at * half : (at + 1) * half] = value
    given = remote(give, taken, give_sems.at[0], give_sems.at[1], spread.ydev)
    given.start()
    sums[...] = jnp.zeros_like(sums)
    given.wait()
    for at in range(2):
        span = slice(at * HD, (at + 1) * HD)
        value = d_kv[0, :, span] + taken[:, span].astype(jnp.float32)
        got[0, core, 1, out_counts - 2 + at] = value.astype(got.dtype)
    tiny.begin()
    spread.begin()
    gain_sum[...] = jnp.zeros_like(gain_sum)

    def blocks(across, half_at, at, fresh):
        span = pl.ds(pl.multiple_of((half_at * out_counts + at) * width, width), width)
        gained = None
        for other in range(2):
            row = row_span(here, across, other, rows)
            block = got[across, (core + other) % 2, half_at, at]
            sums[row, :] += dot_nt(block, w_qkv[:, span])
            more = dot_nn(act_t[:, row], block)
            gained = more if gained is None else gained + more
        if fresh:
            grad[:, span] = gained
        else:
            grad[:, span] += gained

    def column(values):
        return jnp.sum(eye * values, axis=1, keepdims=True)

    def contribute(chip):
        def shard_rows(other, _):
            shard, partner = here.shard(chip, other), here.shard((chip + 2) % 4, other)
            for at in range(rows // LANES):
                row = pl.ds(pl.multiple_of(shard * rows + at * LANES, LANES), LANES)
                kept = rows // LANES + at
                dot = column(tiny_all[shard, at : at + 1, :] + tiny_all[partner, kept : kept + 1, :])
                value, x_rows = sums[row, :], x_low[row, :].astype(jnp.float32)
                contrib[row, :] = (value * gain[...] - x_rows * dot).astype(contrib.dtype)
                gain_sum[...] += jnp.sum(value * x_rows, axis=0, keepdims=True)
            return 0

        lax.fori_loop(0, 2, shard_rows, 0)
        line_tok.launch(2 * per * chip, 2 * per)

    first_part = 2 * per

    def hook(stage, at):
        if stage < 0:
            line.step(done + at)
        elif stage < 2:
            line_tok.step(stage * out_counts + at, 0, first_part)
        else:
            line_tok.step(at, first_part, line_counts + extra - first_part)

    def between(stage):
        if stage < 0:
            tiny.end()
            contribute(0)
            line.steps(min(done + out_counts, line_counts + 2), line_counts + 2)
        elif stage == 1:
            line_tok.steps(2 * out_counts, first_part + 2, 0, first_part)
            contribute(1)
            contribute(2)
        elif stage == 2:
            contribute(3)

    spread.run(blocks, hook=hook, between=between)
    for half_at in range(cols // (rows // per)):
        span = pl.ds(line_counts * (rows // per) + half_at * (rows // per), rows // per)
        source = slice(half_at * (rows // per), (half_at + 1) * (rows // per))
        contrib[span, :] = grad[source, heads * HD :].astype(contrib.dtype)
    line_tok.launch(line_counts, extra)
    for at in range(cols // LANES):
        tile[at : at + 1, :] = gain_sum[:, at * LANES : (at + 1) * LANES]
        spot = cols // LANES + at
        tile[spot : spot + 1, :] = gain_grad[:, at * LANES : (at + 1) * LANES]

    def tile_copy(step):
        return remote(tile, gain_tiles.at[here.z], tile_send.at[step], tile_recv.at[step],
                      (here.dp, here.seq, (here.z + step + 1) % 4))

    line.settle()
    me = here.shard(0, 0)
    columns = pl.ds(pl.multiple_of(me * cols, cols), cols)
    chunk = line.chunk

    def put(which, at):
        kind = (line, line_tok)[which]
        goal = here.device(*(far, near)[which](at))
        dst = (out, d_tok)[which].at[pl.ds(pl.multiple_of(at % per * chunk, chunk), chunk), columns]
        return remote(kind.from_end.at[at], dst, put_sems.at[which, 0, at], put_sems.at[which, 1, at], goal)

    def emit(which, at):
        kind = (line, line_tok)[which]
        row = kind.rows(at)
        base = (resid, d_attn)[which][row, :].astype(jnp.float32)
        kind.from_end[at] = (base + kind.out[row, :].astype(jnp.float32)).astype(out.dtype)

    def is_own(which, at):
        return at >= 7 * per if which == 0 else at < per

    def send(which, at):
        own = is_own(which, at)

        @pl.when(own)
        def _():
            dst = (out, d_tok)[which].at[pl.ds(pl.multiple_of(at % per * chunk, chunk), chunk), columns]
            pltpu.make_async_copy((line, line_tok)[which].from_end.at[at], dst, local_sems.at[which, at % per]).start()

        @pl.when(jnp.logical_not(own))
        def _():
            put(which, at).start()

    for step in range(3):
        tile_copy(step).start()
    gain_tiles[here.z] = tile[...]
    left = line_counts + extra - first_part

    @pl.when(line.inner == 1)
    def _():
        def early(at, _):
            emit(1, at)
            return 0

        lax.fori_loop(0, first_part, early, 0)

        def both(at, _):
            line_tok.step(at, first_part, left)
            spot = at - out_counts
            ready = first_part + at - out_counts

            @pl.when(jnp.logical_and(spot > 0, spot <= line_counts))
            def _():
                send(0, spot - 1)

            @pl.when(jnp.logical_and(spot > 0, spot <= first_part))
            def _():
                send(1, spot - 1)

            @pl.when(jnp.logical_and(ready > first_part, ready <= line_counts))
            def _():
                send(1, ready - 1)

            @pl.when(spot < line_counts)
            def _():
                emit(0, spot)

            @pl.when(ready < line_counts)
            def _():
                emit(1, ready)
            return 0

        lax.fori_loop(out_counts, out_counts + line_counts + 1, both, 0)
        line_tok.steps(out_counts + line_counts + 1, left + 2, first_part, left)

        def drain(at, _):
            line_tok.down(at).wait_send()
            return 0

        lax.fori_loop(0, line_counts + extra, drain, 0)

    @pl.when(line.inner == 0)
    def _():
        def arrive(at, _):
            line_tok.up(at).wait_send()
            line_tok.down(at).wait_recv()

            @pl.when(jnp.logical_and(at > 0, at <= line_counts))
            def _():
                send(0, at - 1)
                send(1, at - 1)

            @pl.when(at < line_counts)
            def _():
                emit(0, at)
                emit(1, at)
            return 0

        lax.fori_loop(0, line_counts + extra, arrive, 0)

    for half_at in range(extra):
        span = pl.ds((line_counts + half_at) * chunk, chunk)
        kv_sum[half_at * chunk : (half_at + 1) * chunk, :] = summed[span, :].astype(jnp.float32)
    spread.end()
    for which in range(2):
        def finish(at, _, which=which):
            @pl.when(jnp.logical_not(is_own(which, at)))
            def _():
                put(which, at).wait()
            return 0

        lax.fori_loop(0, line_counts, finish, 0)
        for at in range(per):
            dst = (out, d_tok)[which].at[at * chunk : (at + 1) * chunk, columns]
            spot = (7 * per if which == 0 else 0) + at
            pltpu.make_async_copy((line, line_tok)[which].from_end.at[spot], dst, local_sems.at[which, at]).wait()
    for step in range(3):
        tile_copy(step).wait()


def tail(d_attn, w_out, queries, kv, probs, rms, cos, sin, act_t, w_qkv, ffn, x_low, resid, gain, gain_grad, cid,
         per=2):
    total, cols = d_attn.shape
    rows = total // 8
    wide = w_out.shape[0]
    heads = wide // HD
    low, f32 = jnp.bfloat16, jnp.float32
    dma = pltpu.SemaphoreType.DMA
    vm = pl.BlockSpec(memory_space=pltpu.VMEM)
    counts = 8 * per
    chunk = rows // per
    extra = cols // chunk
    long = (total + cols, cols)
    out_shape = [
        jax.ShapeDtypeStruct((rows, 8 * cols), low),
        jax.ShapeDtypeStruct((rows, 8 * cols), low),
        jax.ShapeDtypeStruct(w_qkv.shape, f32),
        jax.ShapeDtypeStruct((cols, 2 * HD), f32),
        jax.ShapeDtypeStruct((4, 8, LANES), f32),
    ]
    scratch = reduce_scratch(heads // 2, rows, HD) + spread_scratch((heads + 2) // 2, rows, HD)
    scratch += [
        pltpu.VMEM((rows, wide), f32),
        pltpu.VMEM((8, LANES), f32),
        pltpu.VMEM((8, 8, LANES), f32),
        pltpu.VMEM((2, rows, 2 * HD), f32),
        pltpu.VMEM((rows, 2 * HD), low),
        pltpu.VMEM((rows, 2 * HD), low),
        dma((2,)), dma((7,)), dma((7,)),
        pltpu.VMEM((total, cols), f32),
        pltpu.VMEM((1, cols), f32),
        pltpu.VMEM((8, LANES), f32),
        dma((3,)), dma((3,)), dma((2, 2, counts)), dma((2, per)),
        pltpu.VMEM((total, cols), low),
    ] + line_scratch(counts, (total, cols), low)
    scratch += [pltpu.VMEM(long, low), pltpu.VMEM(long, low)] + line_scratch(counts + extra, long, low)
    operands = [d_attn, w_out, queries, kv, probs, rms, cos, sin, act_t, w_qkv, ffn, x_low, resid, gain, gain_grad]
    kernel = functools.partial(tail_kernel, rows, heads, per)
    return kernel_call(kernel, out_shape, operands, [vm] * len(operands), scratch, cid, "tail")


def turn_kernel(rows, cols, back, src, out, own_sem, send, recv):
    here = Place()
    peers = [(a, o) for a in (3, 1, 2, 0) for o in range(2) if a + o > 0]
    greet(here, [here.device(a, o) for a, o in peers])

    def by_row(ref, shard):
        return ref.at[pl.ds(pl.multiple_of(shard * rows, rows), rows), :]

    def by_col(ref, shard):
        return ref.at[:, pl.ds(pl.multiple_of(shard * cols, cols), cols)]

    take, put = (by_row, by_col) if back else (by_col, by_row)
    me = here.shard(0, 0)

    def copy(at):
        across, other = peers[at]
        return remote(take(src, here.shard(across, other)), put(out, me), send.at[at], recv.at[at],
                      here.device(across, other))

    for at in range(7):
        copy(at).start()
    own = pltpu.make_async_copy(take(src, me), put(out, me), own_sem)
    own.start()
    own.wait()
    for at in range(7):
        copy(at).wait()


def turn(src, back, cid):
    rows, cols = (src.shape[0] // 8, src.shape[1]) if back else (src.shape[0], src.shape[1] // 8)
    shape = (rows, 8 * cols) if back else (8 * rows, cols)
    dma = pltpu.SemaphoreType.DMA
    vm = pl.BlockSpec(memory_space=pltpu.VMEM)
    return pl.pallas_call(
        functools.partial(turn_kernel, rows, cols, back),
        out_shape=jax.ShapeDtypeStruct(shape, src.dtype),
        in_specs=[vm],
        out_specs=vm,
        scratch_shapes=[dma(()), dma((7,)), dma((7,))],
        compiler_params=pltpu.CompilerParams(collective_id=cid, has_side_effects=True,
                                             vmem_limit_bytes=VMEM_LIMIT),
        name=f"turn_{cid}",
    )(src)


LANES = 128


def pack_rows(values):
    parts = values.reshape(8, -1, LANES)
    return jnp.pad(parts, ((0, 0), (0, 8 - parts.shape[1]), (0, 0)))


def acts_move(
    tokens, seg_ids, gain_attn, w_query, kv_weight, w_out, gain_ffn, w_gate, w_up, w_down, d_out
):
    low = jnp.bfloat16
    rows, width = tokens.shape
    seqs = lax.axis_size("seq")
    parts = lax.axis_size("dp") * seqs
    offset = lax.axis_index("seq") * rows
    places, cos_table, sin_table = place_tables(seg_ids)
    away = rows - offset

    def own_first(table):
        return jnp.stack(
            [
                lax.dynamic_slice_in_dim(table, offset, rows, 0),
                lax.dynamic_slice_in_dim(table, away, rows, 0),
            ]
        )

    pair_places = own_first(places)
    pair_segs = own_first(seg_ids)
    pair_cos = own_first(cos_table)
    pair_sin = own_first(sin_table)
    allowed = (pair_segs[0][:, None] == pair_segs.reshape(1, -1)) & (
        pair_places[0][:, None] >= pair_places.reshape(1, -1)
    )
    gain_one = gain_attn.astype(jnp.float32)
    gain_two = gain_ffn.astype(jnp.float32)
    qw = w_query.shape[1]
    ff = w_gate.shape[1]

    none = jnp.zeros((8, 8, LANES), jnp.float32)
    x_low = turn(tokens, False, 1)
    x_col = x_low.astype(jnp.float32)
    own_x = tokens.astype(jnp.float32)
    rms_one = lax.rsqrt(jnp.mean(own_x * own_x, axis=-1, keepdims=True) + EPS)
    act_one = (x_col * gain_one).astype(low)
    w_qkv = jnp.concatenate([w_query, kv_weight], axis=1)
    qkv = scatter_product(act_one, (w_qkv,), none, 256, False, 2)[0]
    tiles = rows // LANES
    attn_part, mixed_all, g_low, kv, probs, queries, rms_tiles = attend(
        qkv,
        jnp.broadcast_to(rms_one, (rows, LANES)),
        pair_cos[0],
        pair_sin[0],
        allowed.astype(jnp.float32),
        w_out,
        d_out,
        jnp.pad(rms_one.reshape(tiles, LANES), ((0, 8 - tiles), (0, 0))),
        3,
    )
    pair_rms = jnp.broadcast_to(rms_tiles[:, :tiles].reshape(2, rows, 1), (2, rows, LANES))
    d_hidden, _, attn = scatter_product(g_low, (w_down,), none, 512, True, 4, line=attn_part)
    resid = x_col + attn.astype(jnp.float32)
    act_two = (resid * gain_two).astype(low)
    squares = pack_rows(jnp.sum(resid * resid, axis=-1))
    both, squares_all = scatter_product(act_two, (w_gate, w_up), squares, 512, False, 6)
    mean_two = jnp.sum(squares_all[:, : rows // LANES], axis=0).reshape(rows, 1) / width
    rms_two = lax.rsqrt(mean_two + EPS)
    gate = both[:, :ff] * rms_two
    up_val = both[:, ff : 2 * ff] * rms_two
    gelu_val, gelu_pull = jax.vjp(gelu_tanh, gate)
    hidden = (gelu_val * up_val).astype(low)
    d_gate = gelu_pull(d_hidden * up_val)[0]
    d_up = d_hidden * gelu_val
    dots_two = jnp.sum(d_gate * gate + d_up * up_val, axis=-1, keepdims=True) * (
        rms_two * rms_two / width
    )
    dots_own = jnp.pad(dots_two.reshape(-1, LANES), ((0, 8 - rows // LANES), (0, 0)))
    d_act_two, grad_gate, grad_up, dots_all = gather_product(
        act_two.T,
        (w_gate, w_up),
        ((d_gate * rms_two).astype(low), (d_up * rms_two).astype(low)),
        dots_own,
        512,
        False,
        7,
    )
    dot_two = dots_all[:, : rows // LANES].reshape(parts * rows, 1)
    grad_gain_two = jnp.sum(d_act_two * resid, axis=0)
    ffn, grad_down, _, d_norm = gather_product(
        g_low,
        (w_down,),
        (hidden,),
        none[0],
        256,
        True,
        8,
        line=(d_act_two * gain_two - resid * dot_two).astype(low),
    )
    d_resid = g_low.astype(jnp.float32) + d_norm.astype(jnp.float32)
    d_attn = d_resid.astype(low)
    grad_out = matmul_tn(mixed_all, d_attn)

    d_tokens, out, grad_qkv, grad_kv, gain_tiles = tail(
        d_attn,
        w_out,
        queries,
        kv,
        probs,
        pair_rms,
        pair_cos,
        pair_sin,
        act_one.T,
        w_qkv,
        ffn.astype(low),
        x_low,
        resid.astype(low),
        gain_one[None, :],
        grad_gain_two[None, :],
        9,
    )
    grad_query = grad_qkv[:, :qw]
    gains = jnp.sum(gain_tiles, axis=0).reshape(2, -1)
    return (
        out,
        d_tokens.astype(jnp.float32),
        gains[0],
        grad_query,
        grad_kv,
        grad_out,
        gains[1],
        grad_gate,
        grad_up,
        grad_down,
    )


def solution(mesh):
    in_specs = (
        P(("dp", "seq"), None),
        P("dp"),
        P(("dp", "seq")),
        P(("dp", "seq"), "tensor"),
        P(("dp", "seq"), None),
        P("tensor", ("dp", "seq")),
        P(("dp", "seq")),
        P(("dp", "seq"), "tensor"),
        P(("dp", "seq"), "tensor"),
        P("tensor", ("dp", "seq")),
        P(("dp", "seq"), None),
    )
    out_specs = (
        P(("dp", "seq"), None),
        P(("dp", "seq"), None),
        P(("dp", "seq")),
        P(("dp", "seq"), "tensor"),
        P(("dp", "seq"), None),
        P("tensor", ("dp", "seq")),
        P(("dp", "seq")),
        P(("dp", "seq"), "tensor"),
        P(("dp", "seq"), "tensor"),
        P("tensor", ("dp", "seq")),
    )

    def shards(*arrays):
        tokens = arrays[0]
        sizes = tuple(mesh.shape[name] for name in ("dp", "seq", "tensor"))
        count = tokens.shape[0] * sizes[0] * sizes[1]
        plan = acts_move if sizes == (4, 2, 4) and count <= tokens.shape[1] else weights_move
        return plan(*arrays)

    return jax.shard_map(shards, mesh=mesh, in_specs=in_specs, out_specs=out_specs, check_vma=False)
```

```python
import functools
import math

import jax
import jax.numpy as jnp
from jax import lax
from jax.experimental import pallas as pl
from jax.experimental.pallas import tpu as pltpu
from jax.sharding import PartitionSpec as P

HD = 256


EPS = 1e-06
NEG = -1e30


def place_tables(segs):
    length = segs.shape[0]
    index = jnp.arange(length, dtype=jnp.int32)
    flags = jnp.concatenate([jnp.ones((1,), dtype=bool), segs[1:] != segs[:-1]])
    starts = lax.cummax(jnp.where(flags, index, jnp.zeros_like(index)), axis=0)
    places = index - starts
    half_size = HD // 2
    freqs = jnp.exp(jnp.arange(half_size, dtype=jnp.float32) * (-math.log(10000.0) / half_size))
    angles = places.astype(jnp.float32)[:, None] * freqs[None, :]
    return (places, jnp.cos(angles), jnp.sin(angles))


def rotate(vector, cos_table, sin_table):
    half_size = vector.shape[-1] // 2
    leading = vector[..., :half_size]
    trailing = vector[..., half_size:]
    return jnp.concatenate(
        [leading * cos_table - trailing * sin_table, trailing * cos_table + leading * sin_table],
        axis=-1,
    )


def rotate_back(vector, cos_table, sin_table):
    half_size = vector.shape[-1] // 2
    leading = vector[..., :half_size]
    trailing = vector[..., half_size:]
    return jnp.concatenate(
        [leading * cos_table + trailing * sin_table, trailing * cos_table - leading * sin_table],
        axis=-1,
    )


def matmul(left, right):
    return jnp.dot(left, right, preferred_element_type=jnp.float32)


def matmul_nt(left, right):
    return lax.dot_general(
        left, right, (((1,), (1,)), ((), ())), preferred_element_type=jnp.float32
    )


def matmul_tn(left, right):
    return lax.dot_general(
        left, right, (((0,), (0,)), ((), ())), preferred_element_type=jnp.float32
    )


def gelu_tanh(values):
    return jax.nn.gelu(values, approximate=True)


def norm_back(d_act, normed, rms_val, gain_val):
    scaled = d_act * gain_val
    return rms_val * (scaled - normed * jnp.mean(scaled * normed, axis=-1, keepdims=True))


def weights_move(
    tokens, seg_ids, gain_attn, w_query, kv_weight, w_out, gain_ffn, w_gate, w_up, w_down, d_out
):
    rows = tokens.shape[0]
    scale_factor = 1.0 / math.sqrt(HD)
    offset = lax.axis_index("seq") * rows
    places, cos_table, sin_table = place_tables(seg_ids)
    own_places = lax.dynamic_slice_in_dim(places, offset, rows, 0)
    own_segs = lax.dynamic_slice_in_dim(seg_ids, offset, rows, 0)
    own_cos = lax.dynamic_slice_in_dim(cos_table, offset, rows, 0)
    own_sin = lax.dynamic_slice_in_dim(sin_table, offset, rows, 0)
    allowed = (own_segs[:, None] == seg_ids[None, :]) & (own_places[:, None] >= places[None, :])
    full_query, full_out, full_kv, full_gain_one = (
        lax.all_gather(w_query, ("dp", "seq"), axis=0, tiled=True),
        lax.all_gather(w_out, ("dp", "seq"), axis=1, tiled=True),
        lax.all_gather(kv_weight, ("dp", "seq"), axis=0, tiled=True),
        lax.all_gather(gain_attn, ("dp", "seq"), axis=0, tiled=True),
    )
    gain_one = full_gain_one.astype(jnp.float32)
    inputs = tokens.astype(jnp.float32)
    rms_one = lax.rsqrt(jnp.mean(inputs * inputs, axis=-1, keepdims=True) + EPS)
    norm_one = inputs * rms_one
    act_one = (norm_one * gain_one).astype(jnp.bfloat16)
    query_pre = matmul(act_one, full_query)
    heads = query_pre.shape[1] // HD
    kv_pre = matmul(act_one, full_kv)
    queries = (
        rotate(query_pre.reshape(rows, heads, HD), own_cos[:, None, :], own_sin[:, None, :])
        * scale_factor
    ).astype(jnp.bfloat16)
    own_kv = jnp.concatenate(
        [rotate(kv_pre[:, :HD], own_cos, own_sin), kv_pre[:, HD:]], axis=1
    ).astype(jnp.bfloat16)
    all_kv = lax.all_gather(own_kv, "seq", axis=0, tiled=True)
    keys = all_kv[:, :HD]
    values_all = all_kv[:, HD:]
    scores = jnp.einsum("rhd,kd->hrk", queries, keys, preferred_element_type=jnp.float32)
    scores = jnp.where(allowed[None], scores, NEG)
    top_score = jnp.max(scores, axis=-1, keepdims=True)
    expd = jnp.exp(scores - top_score)
    total = jnp.sum(expd, axis=-1, keepdims=True)
    log_total = top_score + jnp.log(total)
    probs_low = (expd / total).astype(jnp.bfloat16)
    mixed = (
        jnp.einsum("hrk,kd->rhd", probs_low, values_all, preferred_element_type=jnp.float32)
        .reshape(rows, heads * HD)
        .astype(jnp.bfloat16)
    )
    attn = lax.psum(matmul(mixed, full_out), "tensor")
    resid = inputs + attn
    full_gate, full_up, full_down, full_gain_two = (
        lax.all_gather(w_gate, ("dp", "seq"), axis=0, tiled=True),
        lax.all_gather(w_up, ("dp", "seq"), axis=0, tiled=True),
        lax.all_gather(w_down, ("dp", "seq"), axis=1, tiled=True),
        lax.all_gather(gain_ffn, ("dp", "seq"), axis=0, tiled=True),
    )
    gain_two = full_gain_two.astype(jnp.float32)
    rms_two = lax.rsqrt(jnp.mean(resid * resid, axis=-1, keepdims=True) + EPS)
    norm_two = resid * rms_two
    act_two = (norm_two * gain_two).astype(jnp.bfloat16)
    gate = matmul(act_two, full_gate)
    up_val = matmul(act_two, full_up)
    gelu_val, gelu_pull = jax.vjp(gelu_tanh, gate)
    hidden = (gelu_val * up_val).astype(jnp.bfloat16)
    ffn = lax.psum(matmul(hidden, full_down).astype(jnp.bfloat16), "tensor").astype(jnp.float32)
    out = (resid + ffn).astype(jnp.bfloat16)
    back_gate, back_up, back_down = (
        lax.all_gather(w_gate, ("dp", "seq"), axis=0, tiled=True),
        lax.all_gather(w_up, ("dp", "seq"), axis=0, tiled=True),
        lax.all_gather(w_down, ("dp", "seq"), axis=1, tiled=True),
    )
    d_hidden = matmul_nt(d_out, back_down)
    grad_down = matmul_tn(hidden, d_out)
    d_gate = gelu_pull(d_hidden * up_val)[0].astype(jnp.bfloat16)
    d_up = (d_hidden * gelu_val).astype(jnp.bfloat16)
    grad_gate = matmul_tn(act_two, d_gate)
    grad_up = matmul_tn(act_two, d_up)
    d_act_two = lax.psum(matmul_nt(d_gate, back_gate) + matmul_nt(d_up, back_up), "tensor")
    grad_gain_two = jnp.sum(d_act_two * norm_two, axis=0)
    d_resid = d_out.astype(jnp.float32) + norm_back(d_act_two, norm_two, rms_two, gain_two)
    ffn_grads = (
        lax.psum_scatter(
            grad_gate.astype(jnp.bfloat16), ("dp", "seq"), scatter_dimension=0, tiled=True
        ).astype(jnp.float32),
        lax.psum_scatter(
            grad_up.astype(jnp.bfloat16), ("dp", "seq"), scatter_dimension=0, tiled=True
        ).astype(jnp.float32),
        lax.psum_scatter(
            grad_down.astype(jnp.bfloat16), ("dp", "seq"), scatter_dimension=1, tiled=True
        ).astype(jnp.float32),
        lax.psum_scatter(
            grad_gain_two.astype(jnp.bfloat16), ("dp", "seq"), scatter_dimension=0, tiled=True
        ).astype(jnp.float32),
    )
    back_query, back_out, back_kv = (
        lax.all_gather(w_query, ("dp", "seq"), axis=0, tiled=True),
        lax.all_gather(w_out, ("dp", "seq"), axis=1, tiled=True),
        lax.all_gather(kv_weight, ("dp", "seq"), axis=0, tiled=True),
    )
    d_attn = d_resid.astype(jnp.bfloat16)
    grad_out = matmul_tn(mixed, d_attn)
    d_mixed = matmul_nt(d_attn, back_out).astype(jnp.bfloat16).reshape(rows, heads, HD)
    scores_again = jnp.einsum("rhd,kd->hrk", queries, keys, preferred_element_type=jnp.float32)
    probs = jnp.where(allowed[None], jnp.exp(scores_again - log_total), 0.0)
    d_probs = jnp.einsum("rhd,kd->hrk", d_mixed, values_all, preferred_element_type=jnp.float32)
    delta = jnp.sum(probs * d_probs, axis=-1, keepdims=True)
    d_scores = (probs * (d_probs - delta)).astype(jnp.bfloat16)
    d_queries = (
        jnp.einsum("hrk,kd->rhd", d_scores, keys, preferred_element_type=jnp.float32) * scale_factor
    )
    d_query_pre = (
        rotate_back(d_queries, own_cos[:, None, :], own_sin[:, None, :])
        .reshape(rows, heads * HD)
        .astype(jnp.bfloat16)
    )
    d_keys_part = jnp.einsum("hrk,rhd->kd", d_scores, queries, preferred_element_type=jnp.float32)
    d_values_part = jnp.einsum(
        "hrk,rhd->kd", probs.astype(jnp.bfloat16), d_mixed, preferred_element_type=jnp.float32
    )
    own_kv_grad = lax.psum_scatter(
        jnp.concatenate([d_keys_part, d_values_part], axis=1).astype(jnp.bfloat16),
        "seq",
        scatter_dimension=0,
        tiled=True,
    )
    d_act_query = matmul_nt(d_query_pre, back_query)
    d_act_sum, kv_grad = (
        lax.psum(d_act_query.astype(jnp.bfloat16), "tensor").astype(jnp.float32),
        lax.psum(own_kv_grad, "tensor").astype(jnp.float32),
    )
    d_kv_pre = jnp.concatenate(
        [rotate_back(kv_grad[:, :HD], own_cos, own_sin), kv_grad[:, HD:]], axis=1
    ).astype(jnp.bfloat16)
    d_act_one = d_act_sum + matmul_nt(d_kv_pre, back_kv)
    grad_query = matmul_tn(act_one, d_query_pre)
    grad_kv = matmul_tn(act_one, d_kv_pre)
    grad_gain_one = jnp.sum(d_act_one * norm_one, axis=0)
    d_tokens = d_resid + norm_back(d_act_one, norm_one, rms_one, gain_one)
    attn_grads = (
        lax.psum_scatter(
            grad_query.astype(jnp.bfloat16), ("dp", "seq"), scatter_dimension=0, tiled=True
        ).astype(jnp.float32),
        lax.psum_scatter(
            grad_out.astype(jnp.bfloat16), ("dp", "seq"), scatter_dimension=1, tiled=True
        ).astype(jnp.float32),
        lax.psum_scatter(
            grad_kv.astype(jnp.bfloat16), ("dp", "seq"), scatter_dimension=0, tiled=True
        ).astype(jnp.float32),
        lax.psum_scatter(
            grad_gain_one.astype(jnp.bfloat16), ("dp", "seq"), scatter_dimension=0, tiled=True
        ).astype(jnp.float32),
    )
    return (
        out,
        d_tokens,
        attn_grads[3],
        attn_grads[0],
        attn_grads[2],
        attn_grads[1],
        ffn_grads[3],
        ffn_grads[0],
        ffn_grads[1],
        ffn_grads[2],
    )


MESH = pl.DeviceIdType.MESH
VMEM_LIMIT = 66000 * 1024


class Place:
    def __init__(self):
        self.dp = lax.axis_index("dp")
        self.seq = lax.axis_index("seq")
        self.z = lax.axis_index("tensor")
        self.core = lax.rem(self.dp, 2)
        self.chip = lax.div(self.dp, 2)

    def device(self, across, other):
        chip = (self.chip + across) % 2
        seq = (self.seq + across // 2) % 2
        core = (self.core + other) % 2
        return chip * 2 + core, seq, self.z

    def shard(self, across, other):
        dp, seq, _ = self.device(across, other)
        return dp * 2 + seq


def greet(here, peers, line=False):
    barrier = pltpu.get_barrier_semaphore()
    peers = list(peers)
    if line:
        peers += [(here.dp, here.seq, (here.z + step) % 4) for step in range(1, 4)]
    for peer in peers:
        pl.semaphore_signal(barrier, inc=1, device_id=peer, device_id_type=MESH)
    pl.semaphore_wait(barrier, len(peers))


def remote(src, dst, send, recv, peer):
    return pltpu.make_async_remote_copy(
        src_ref=src, dst_ref=dst, send_sem=send, recv_sem=recv, device_id=peer, device_id_type=MESH
    )


class Line:
    def __init__(self, here, counts, refs, place=None):
        self.own, self.out, self.from_end, self.from_mid = refs[:4]
        self.sems = refs[4:10]
        self.counts = counts
        self.chunk = self.own.shape[0] // counts
        self.place = place
        z = here.z
        self.inner = ((z + 1) // 2) % 2
        self.mate = (here.dp, here.seq, z + 1 - 2 * (z % 2))
        self.other = (here.dp, here.seq, 3 - z)

    def rows(self, at):
        at = at if self.place is None else self.place(at)
        return pl.ds(pl.multiple_of(at * self.chunk, self.chunk), self.chunk)

    def up(self, at):
        return remote(self.own.at[self.rows(at), :], self.from_end.at[at], self.sems[0].at[at],
                      self.sems[1].at[at], self.mate)

    def over(self, at):
        return remote(self.out.at[self.rows(at), :], self.from_mid.at[at], self.sems[2].at[at],
                      self.sems[3].at[at], self.other)

    def down(self, at):
        rows = self.rows(at)
        return remote(self.out.at[rows, :], self.out.at[rows, :], self.sems[4].at[at],
                      self.sems[5].at[at], self.mate)

    def launch(self, first, count):
        @pl.when(self.inner == 0)
        def _():
            def send(at, _):
                self.up(first + at).start()
                return 0

            lax.fori_loop(0, count, send, 0)

    def begin(self):
        self.launch(0, self.counts)

    def first(self, at):
        rows = self.rows(at)
        self.up(at).wait_recv()
        total = self.own[rows, :].astype(jnp.float32) + self.from_end[at].astype(jnp.float32)
        self.out[rows, :] = total.astype(self.out.dtype)
        self.over(at).start()

    def second(self, at):
        rows = self.rows(at)
        self.over(at).wait()
        total = self.out[rows, :].astype(jnp.float32) + self.from_mid[at].astype(jnp.float32)
        self.out[rows, :] = total.astype(self.out.dtype)
        self.down(at).start()

    def step(self, at, start=0, count=None):
        count = self.counts if count is None else count

        @pl.when(jnp.logical_and(self.inner == 1, at < count))
        def _():
            self.first(start + at)

        @pl.when(jnp.logical_and(self.inner == 1, jnp.logical_and(at > 1, at < count + 2)))
        def _():
            self.second(start + at - 2)

    def steps(self, first, last, start=0, count=None):
        def rest(at, _):
            self.step(at, start, count)
            return 0

        lax.fori_loop(first, last, rest, 0)

    def settle(self):
        @pl.when(self.inner == 0)
        def _():
            def take(at, _):
                self.up(at).wait_send()
                self.down(at).wait_recv()
                return 0

            lax.fori_loop(0, self.counts, take, 0)

        @pl.when(self.inner == 1)
        def _():
            def drain(at, _):
                self.down(at).wait_send()
                return 0

            lax.fori_loop(0, self.counts, drain, 0)

    def end(self, done=0):
        self.steps(min(done, self.counts + 2), self.counts + 2)
        self.settle()


def line_scratch(counts, shape, low):
    buf = pltpu.VMEM((counts, shape[0] // counts, shape[1]), low)
    return [buf, buf] + [pltpu.SemaphoreType.DMA((counts,))] * 6


def turned(at):
    return 3 - at // 2, 1 - at % 2


def slice_peers(here):
    return [here.device(*turned(at)) for at in range(7)]


def kernel_call(kernel, out_shape, operands, specs, scratch, cid, name, out_specs=None):
    vm = pl.BlockSpec(memory_space=pltpu.VMEM)
    return pl.pallas_call(
        kernel,
        out_shape=out_shape,
        in_specs=specs,
        out_specs=out_specs or [vm] * len(out_shape),
        scratch_shapes=scratch,
        compiler_params=pltpu.CompilerParams(
            collective_id=cid, has_side_effects=True, vmem_limit_bytes=VMEM_LIMIT
        ),
        name=f"{name}_{cid}",
    )(*operands)


class Tiny:
    def __init__(self, here, src, dst, sems, spread):
        self.here, self.src, self.dst, self.sems, self.spread = here, src, dst, sems, spread
        self.peers = slice_peers(here)
        self.me = here.shard(0, 0)

    def tile(self, shard):
        return self.src.at[shard] if self.spread else self.src

    def copy(self, at):
        return remote(self.tile(self.here.shard(*turned(at))), self.dst.at[self.me], self.sems[0].at[at],
                      self.sems[1].at[at], self.peers[at])

    def begin(self):
        for at in range(7):
            self.copy(at).start()
        self.dst[self.me] = self.tile(self.me)[...]

    def end(self):
        for at in range(7):
            self.copy(at).wait()


class Reduce:
    def __init__(self, here, counts, product, refs, before=None):
        self.counts, self.product, self.before = counts, product, before
        self.held, self.sib_out, self.sib_in, self.from_x, self.from_y = refs[:5]
        self.sib_sems, self.x_sems, self.y_sems = refs[5:7], refs[7:9], refs[9:11]
        self.sib, self.xdev, self.ydev = here.device(0, 1), here.device(1, 0), here.device(2, 0)
        self.steps = 4 * counts
        self.ring = self.sib_out.shape[0]

    def streams(self, stage):
        far = stage // 3
        x_chip = jnp.where(stage == 0, 3, jnp.where(stage == 2, 0, 1))
        y_chip = jnp.where(stage == 0, 3, jnp.where(stage == 2, 0, 2))
        return (x_chip, far), (y_chip, 1 - far)

    def to_sib(self, step, stream):
        stage, at = step // self.counts, step % self.counts
        return remote(self.sib_out.at[step % self.ring, stream], self.sib_in.at[stage, stream, at],
                      self.sib_sems[0].at[stage, stream, at], self.sib_sems[1].at[stage, stream, at], self.sib)

    def to_x(self, hop, at, stage=0):
        return remote(self.held.at[stage, 0, at], self.from_x.at[hop, at], self.x_sems[0].at[hop, at],
                      self.x_sems[1].at[hop, at], self.xdev)

    def to_y(self, hop, at, stage=0):
        return remote(self.held.at[stage, 1, at], self.from_y.at[hop, at], self.y_sems[0].at[hop, at],
                      self.y_sems[1].at[hop, at], self.ydev)

    def compute(self, step):
        stage, at = step // self.counts, step % self.counts
        if self.before:
            for stop in range(3):
                @pl.when(step == stop * self.counts)
                def _():
                    self.before(stop)

        @pl.when(step >= self.ring)
        def _():
            for stream in range(2):
                self.to_sib(step - self.ring, stream).wait_send()

        for stream, (across, half) in enumerate(self.streams(stage)):
            self.sib_out[step % self.ring, stream] = self.product(across, 1, half, at).astype(jnp.bfloat16)
            self.held[stage, stream, at] = self.product(across, 0, half, at).astype(jnp.bfloat16)
        for stream in range(2):
            self.to_sib(step, stream).start()

    def finish(self, step):
        stage, at = step // self.counts, step % self.counts
        for stream in range(2):
            self.to_sib(step, stream).wait_recv()

        def total(stream):
            return self.held[stage, stream, at].astype(jnp.float32) + self.sib_in[stage, stream, at].astype(
                jnp.float32)

        @pl.when(stage < 3)
        def _():
            for stream in range(2):
                self.held[stage, stream, at] = total(stream).astype(jnp.bfloat16)

        @pl.when(stage == 3)
        def _():
            self.to_y(0, at).wait_recv()
            self.held[3, 0, at] = (total(0) + self.from_y[0, at].astype(jnp.float32)).astype(jnp.bfloat16)
            self.to_x(0, at).wait_recv()
            self.held[3, 1, at] = (total(1) + self.from_x[0, at].astype(jnp.float32)).astype(jnp.bfloat16)

        @pl.when(stage != 2)
        def _():
            hop = stage - stage // 3
            self.to_x(hop, at, stage).start()
            self.to_y(hop, at, stage).start()

    def run(self, line=None):
        def body(step, _):
            @pl.when(step < self.steps)
            def _():
                self.compute(step)

            @pl.when(step > 0)
            def _():
                self.finish(step - 1)

            if line:
                line.step(step)
            return 0

        lax.fori_loop(0, self.steps + 1, body, 0)
        return self.steps + 1

    def end(self, emit):
        def last(at, _):
            values = []
            for half in range(2):
                xs, ys = (1, 2) if half == 0 else (2, 1)
                self.to_x(xs, at).wait_recv()
                self.to_y(ys, at).wait_recv()
                values.append(self.held[2, half, at].astype(jnp.float32) + self.from_x[xs, at].astype(jnp.float32)
                              + self.from_y[ys, at].astype(jnp.float32))
            emit(at, *values)
            for hop in range(3):
                self.to_x(hop, at).wait_send()
                self.to_y(hop, at).wait_send()
            return 0

        lax.fori_loop(0, self.counts, last, 0)

        def drain(at, _):
            for stream in range(2):
                self.to_sib(self.steps - self.ring + at, stream).wait_send()
            return 0

        lax.fori_loop(0, self.ring, drain, 0)


def reduce_scratch(counts, rows, width, ring=4):
    low, dma = jnp.bfloat16, pltpu.SemaphoreType.DMA
    block = pltpu.VMEM((4, 2, counts, rows, width), low)
    landed = pltpu.VMEM((3, counts, rows, width), low)
    sent = pltpu.VMEM((ring, 2, rows, width), low)
    return [block, sent, block, landed, landed] + [dma((4, 2, counts))] * 2 + [dma((3, counts))] * 4


class Spread:
    def __init__(self, here, counts, refs):
        self.counts = counts
        self.got = refs[0]
        self.x_sems, self.y_sems, self.sib_sems = refs[1:3], refs[3:5], refs[5:7]
        self.core = here.core
        self.sib, self.xdev, self.ydev = here.device(0, 1), here.device(1, 0), here.device(2, 0)

    def slot(self, across, half, at):
        return self.got.at[across, self.core, half, at]

    def x_copy(self, hop, at):
        half = jnp.minimum(hop, 1)
        src = self.slot(2 * (hop // 2), half, at)
        dst = self.slot(1 + 2 * (hop // 2), half, at)
        return remote(src, dst, self.x_sems[0].at[hop, at], self.x_sems[1].at[hop, at], self.xdev)

    def y_copy(self, hop, at):
        half = 1 - jnp.minimum(hop, 1)
        src = self.slot(hop // 2, half, at)
        dst = self.slot(2 + hop // 2, half, at)
        return remote(src, dst, self.y_sems[0].at[hop, at], self.y_sems[1].at[hop, at], self.ydev)

    def streams(self, stage):
        some, last, late = jnp.minimum(stage, 1), stage // 3, stage // 2
        return (some + 2 * last, late), (2 * some + last, 1 - late)

    def sib_copy(self, stage, stream, at):
        across, half = self.streams(stage)[stream]
        slot = self.slot(across, half, at)
        spot = (stage, stream, at)
        return remote(slot, slot, self.sib_sems[0].at[spot], self.sib_sems[1].at[spot], self.sib)

    def begin(self):
        def first(at, _):
            self.x_copy(0, at).start()
            self.y_copy(0, at).start()
            return 0

        def own(at, _):
            self.sib_copy(0, 0, at).start()
            self.sib_copy(0, 1, at).start()
            return 0

        lax.fori_loop(0, self.counts, first, 0)
        lax.fori_loop(0, self.counts, own, 0)

    def run(self, blocks, hook=None, done=None):
        counts = self.counts

        def body(step, _):
            stage, at = step // counts, step % counts

            @pl.when(jnp.logical_and(stage > 0, stage < 4))
            def _():
                self.x_copy(stage - 1, at).wait_recv()
                self.sib_copy(stage, 0, at).start()
                self.y_copy(stage - 1, at).wait_recv()
                self.sib_copy(stage, 1, at).start()

            @pl.when(jnp.logical_and(stage > 0, stage < 3))
            def _():
                self.x_copy(stage, at).start()
                self.y_copy(stage, at).start()

            @pl.when(step > 0)
            def _():
                old, spot = (step - 1) // counts, (step - 1) % counts
                for stream, (across, half) in enumerate(self.streams(old)):
                    self.sib_copy(old, stream, spot).wait_recv()
                    blocks(across, half, spot)
                if done:
                    done(old, spot)

            if hook:
                hook(step)
            return 0

        lax.fori_loop(0, 4 * counts + 1, body, 0)
        return 4 * counts + 1

    def end(self):
        def drain(at, _):
            for hop in range(3):
                self.x_copy(hop, at).wait_send()
                self.y_copy(hop, at).wait_send()
            for stage in range(4):
                self.sib_copy(stage, 0, at).wait_send()
                self.sib_copy(stage, 1, at).wait_send()
            return 0

        lax.fori_loop(0, self.counts, drain, 0)


def spread_scratch(counts, rows, width):
    dma = pltpu.SemaphoreType.DMA
    return [pltpu.VMEM((4, 2, 2, counts, rows, width), jnp.bfloat16)] + [dma((3, counts))] * 4 + [
        dma((4, 2, counts))] * 2


def row_span(here, across, other, rows):
    return pl.ds(pl.multiple_of(here.shard(across, other) * rows, rows), rows)


def dot_nt(left, right):
    return lax.dot_general(left, right, (((1,), (1,)), ((), ())), preferred_element_type=jnp.float32)


def dot_tn(left, right):
    return lax.dot_general(left, right, (((0,), (0,)), ((), ())), preferred_element_type=jnp.float32)


def dot_nn(left, right):
    return jnp.dot(left, right, preferred_element_type=jnp.float32)


def products(here, act, weight, nt, rows, width, counts):
    def product(across, other, half, at):
        cols = pl.ds(pl.multiple_of((half * counts + at) * width, width), width)
        block = act[row_span(here, across, other, rows), :]
        return dot_nt(block, weight[cols, :]) if nt else dot_nn(block, weight[:, cols])

    return product


def diagonal():
    return (lax.broadcasted_iota(jnp.int32, (LANES, LANES), 0) ==
            lax.broadcasted_iota(jnp.int32, (LANES, LANES), 1)).astype(jnp.float32)


def to_tile(tile, first, column, eye):
    for at in range(column.shape[0] // LANES):
        spread = column[at * LANES : (at + 1) * LANES, :] * eye
        tile[first + at : first + at + 1, :] = jnp.sum(spread, axis=0, keepdims=True)


def from_tile(row, eye):
    return jnp.sum(eye * row, axis=1, keepdims=True)


def open_kernel(rows, width, counts, tokens, gain, w_query, kv_weight, qkv, x_low, act_t, w_qkv, rms, *refs):
    here = Place()
    cols = gain.shape[1]
    act, turn_send, turn_recv, local_sems = refs[:4]
    me = here.shard(0, 0)
    own_rows = pl.ds(pl.multiple_of(me * rows, rows), rows)

    def turn_copy(at):
        across, other = turned(at)
        first = pl.multiple_of(here.shard(across, other) * cols, cols)
        return remote(tokens.at[:, pl.ds(first, cols)], x_low.at[own_rows, :], turn_send.at[at], turn_recv.at[at],
                      here.device(across, other))

    wide = w_query.shape[1]
    local = [
        pltpu.make_async_copy(w_query, w_qkv.at[:, :wide], local_sems.at[0]),
        pltpu.make_async_copy(kv_weight, w_qkv.at[:, wide:], local_sems.at[1]),
        pltpu.make_async_copy(tokens.at[:, pl.ds(pl.multiple_of(me * cols, cols), cols)], x_low.at[own_rows, :],
                              local_sems.at[2]),
    ]
    for copy in local:
        copy.start()
    greet(here, slice_peers(here))
    for at in range(7):
        turn_copy(at).start()
    for copy in local:
        copy.wait()

    def squares(at, total):
        values = tokens[:, pl.ds(pl.multiple_of(at * cols, cols), cols)].astype(jnp.float32)
        return total + jnp.sum(values * values, axis=-1, keepdims=True)

    total = lax.fori_loop(0, 8, squares, jnp.zeros((rows, 1), jnp.float32))
    rms[...] = jnp.broadcast_to(lax.rsqrt(total / (8 * cols) + EPS), rms.shape)

    def prepare(first, count):
        def one(step, _):
            at = first + step
            span = row_span(here, *turned(at), rows)
            value = (x_low[span, :].astype(jnp.float32) * gain[...]).astype(act.dtype)
            act[span, :] = value
            return 0

        lax.fori_loop(0, count, one, 0)

    def before(stop):
        first, count = ((0, 2), (2, 4), (6, 2))[stop]
        for at in range(first, min(first + count, 7)):
            turn_copy(at).wait_recv()
        prepare(first, count)

    def flip():
        def one(shard, _):
            span = pl.ds(pl.multiple_of(shard * rows, rows), rows)
            act_t[:, span] = act[span, :].T
            return 0

        lax.fori_loop(0, 8, one, 0)

    product = products(here, act, w_qkv, False, rows, width, counts)
    total = Reduce(here, counts, product, refs[4:15], before)
    total.run()
    flip()

    def emit(at, first, second):
        for half, value in enumerate((first, second)):
            qkv[:, pl.ds(pl.multiple_of((half * counts + at) * width, width), width)] = value

    total.end(emit)
    for at in range(7):
        turn_copy(at).wait_send()


def opening(tokens, gain, w_query, kv_weight, cid, width=256):
    rows = tokens.shape[0]
    cols, wide = w_query.shape
    every = wide + kv_weight.shape[1]
    counts = every // (2 * width)
    low, f32 = jnp.bfloat16, jnp.float32
    dma = pltpu.SemaphoreType.DMA
    vm = pl.BlockSpec(memory_space=pltpu.VMEM)
    hbm = pl.BlockSpec(memory_space=pl.ANY)
    out_shape = [
        jax.ShapeDtypeStruct((rows, every), f32),
        jax.ShapeDtypeStruct((8 * rows, cols), low),
        jax.ShapeDtypeStruct((cols, 8 * rows), low),
        jax.ShapeDtypeStruct((cols, every), low),
        jax.ShapeDtypeStruct((rows, LANES), f32),
    ]
    scratch = [pltpu.VMEM((8 * rows, cols), low), dma((7,)), dma((7,)), dma((3,))]
    scratch += reduce_scratch(counts, rows, width)
    kernel = functools.partial(open_kernel, rows, width, counts)
    return kernel_call(kernel, out_shape, [tokens, gain, w_query, kv_weight], [vm, vm, hbm, hbm], scratch, cid, "open")


def scatter_kernel(rows, width, counts, line_counts, act, weight, line_own, out, line_out, *refs):
    here = Place()
    line = Line(here, line_counts, [line_own, line_out] + list(refs[11:]))
    product = products(here, act, weight, True, rows, width, counts)
    total = Reduce(here, counts, product, refs[:11])
    greet(here, slice_peers(here), True)
    line.begin()
    done = total.run(line)
    line.end(done)

    def emit(at, first, second):
        for half, value in enumerate((first, second)):
            out[:, pl.ds(pl.multiple_of((half * counts + at) * width, width), width)] = value

    total.end(emit)


def scatter_product(act, weight, width, cid, line, line_counts=16):
    rows = act.shape[0] // 8
    every = weight.shape[0]
    counts = every // (2 * width)
    vm = pl.BlockSpec(memory_space=pltpu.VMEM)
    out_shape = [
        jax.ShapeDtypeStruct((rows, every), jnp.float32),
        jax.ShapeDtypeStruct(line.shape, line.dtype),
    ]
    scratch = reduce_scratch(counts, rows, width) + line_scratch(line_counts, line.shape, line.dtype)
    kernel = functools.partial(scatter_kernel, rows, width, counts, line_counts)
    return kernel_call(kernel, out_shape, [act, weight, line], [vm] * 3, scratch, cid, "scatter_product")


def ffn_kernel(rows, width, counts, x_low, attn, gain, w_gate, w_up, d_hidden, hidden, d_gate, d_up, act_t, tile_out,
               *refs):
    here = Place()
    cols = gain.shape[1]
    act, weight, tiny_own, tiny_all, tiny_send, tiny_recv, dots, local_sems = refs[:8]
    tiny = Tiny(here, tiny_own, tiny_all, (tiny_send, tiny_recv), True)
    half_cols = counts * width
    local = [
        pltpu.make_async_copy(w_gate, weight.at[:, :half_cols], local_sems.at[0]),
        pltpu.make_async_copy(w_up, weight.at[:, half_cols:], local_sems.at[1]),
    ]
    for copy in local:
        copy.start()
    eye = diagonal()
    tiny_own[...] = jnp.zeros_like(tiny_own)

    def prepare(shard, _):
        for at in range(rows // LANES):
            span = pl.ds(pl.multiple_of(shard * rows + at * LANES, LANES), LANES)
            resid = x_low[span, :].astype(jnp.float32) + attn[span, :].astype(jnp.float32)
            act[span, :] = (resid * gain[...]).astype(act.dtype)
            square = jnp.sum(resid * resid, axis=-1, keepdims=True)
            tiny_own[shard, at : at + 1, :] = jnp.sum(square * eye, axis=0, keepdims=True)
        return 0

    lax.fori_loop(0, 8, prepare, 0)
    greet(here, slice_peers(here))
    tiny.begin()
    for copy in local:
        copy.wait()
    product = products(here, act, weight, False, rows, width, counts)
    total = Reduce(here, counts, product, refs[8:19])
    total.run()

    def flip(shard, _):
        span = pl.ds(pl.multiple_of(shard * rows, rows), rows)
        act_t[:, span] = act[span, :].T
        return 0

    lax.fori_loop(0, 8, flip, 0)
    tiny.end()
    tiles = rows // LANES
    mean = [from_tile(jnp.sum(tiny_all[:, at, :], axis=0, keepdims=True), eye) for at in range(tiles)]
    scale = lax.rsqrt(jnp.concatenate(mean, axis=0) / (8 * cols) + EPS)
    dots[...] = jnp.zeros_like(dots)
    coeff = math.sqrt(2.0 / math.pi)

    def emit(at, first, second):
        span = pl.ds(pl.multiple_of(at * width, width), width)
        gate, up = first * scale, second * scale
        inner = jnp.tanh(coeff * (gate + 0.044715 * (gate * gate * gate)))
        gelu = 0.5 * gate * (1.0 + inner)
        slope = 0.5 * (1.0 + inner) + 0.5 * gate * (1.0 - inner * inner) * (
            coeff * (1.0 + 3.0 * 0.044715 * gate * gate))
        cot = d_hidden[:, span]
        hidden[:, span] = (gelu * up).astype(hidden.dtype)
        back_gate, back_up = cot * up * slope, cot * gelu
        d_gate[:, span] = (back_gate * scale).astype(d_gate.dtype)
        d_up[:, span] = (back_up * scale).astype(d_up.dtype)
        dots[...] += jnp.sum(back_gate * gate + back_up * up, axis=-1, keepdims=True)

    total.end(emit)
    tile_out[...] = jnp.zeros_like(tile_out)
    to_tile(tile_out, 0, dots[...] * (scale * scale * (1.0 / (8 * cols))), eye)


def ffn_scatter(x_low, attn, gain, w_gate, w_up, d_hidden, cid, width=512):
    rows, half = d_hidden.shape
    cols = gain.shape[1]
    counts = half // width
    low, f32 = jnp.bfloat16, jnp.float32
    dma = pltpu.SemaphoreType.DMA
    vm = pl.BlockSpec(memory_space=pltpu.VMEM)
    hbm = pl.BlockSpec(memory_space=pl.ANY)
    out_shape = [jax.ShapeDtypeStruct((rows, half), low)] * 3 + [
        jax.ShapeDtypeStruct((cols, 8 * rows), low),
        jax.ShapeDtypeStruct((8, LANES), f32),
    ]
    scratch = [
        pltpu.VMEM((8 * rows, cols), low),
        pltpu.VMEM((cols, 2 * half), low),
        pltpu.VMEM((8, 8, LANES), f32),
        pltpu.VMEM((8, 8, LANES), f32),
        dma((7,)), dma((7,)),
        pltpu.VMEM((rows, 1), f32),
        dma((2,)),
    ] + reduce_scratch(counts, rows, width)
    kernel = functools.partial(ffn_kernel, rows, width, counts)
    return kernel_call(kernel, out_shape, [x_low, attn, gain, w_gate, w_up, d_hidden], [vm, vm, vm, hbm, hbm, vm],
                       scratch, cid, "ffn")


def load_own(spread, payload, width, counts, sems):
    copies = []
    for half in range(2):
        for at in range(counts):
            first = at * width + (half * counts * width if len(payload) == 1 else 0)
            src = payload[half % len(payload)].at[:, first : first + width]
            copies.append(pltpu.make_async_copy(src, spread.slot(0, half, at), sems.at[half, at]))
    return copies


def back_kernel(rows, width, counts, act_t, w_gate, w_up, d_gate, d_up, dots, x_low, attn, gain, contrib, gain_grad,
                grad_gate, grad_up, *refs):
    here = Place()
    spread = Spread(here, counts, refs[:7])
    tiny_all, tiny_send, tiny_recv, own_sems, weight, sums, grads, local_sems, out_sems = refs[7:16]
    tiny = Tiny(here, dots, tiny_all, (tiny_send, tiny_recv), False)
    half_cols = counts * width
    local = [
        pltpu.make_async_copy(w_gate, weight.at[:, :half_cols], local_sems.at[0]),
        pltpu.make_async_copy(w_up, weight.at[:, half_cols:], local_sems.at[1]),
    ]
    own = load_own(spread, (d_gate, d_up), width, counts, own_sems)
    for copy in own + local:
        copy.start()
    greet(here, tiny.peers)
    for copy in own:
        copy.wait()
    spread.begin()
    tiny.begin()
    sums[...] = jnp.zeros_like(sums)
    for copy in local:
        copy.wait()

    def columns(half, at):
        return pl.ds(pl.multiple_of((half * counts + at) * width, width), width)

    def clear(at, _):
        grads[:, columns(0, at)] = jnp.zeros((grads.shape[0], width), jnp.float32)
        return 0

    lax.fori_loop(0, 2 * counts, clear, 0)

    def blocks(across, half, at):
        cols = columns(half, at)
        gained = grads[:, cols]
        for other in range(2):
            row = row_span(here, across, other, rows)
            block = spread.got[across, (spread.core + other) % 2, half, at]
            sums[row, :] += dot_nt(block, weight[:, cols])
            gained = gained + dot_nn(act_t[:, row], block)
        grads[:, cols] = gained

    def leave(half, at):
        spot = pl.ds(pl.multiple_of(at * width, width), width)
        return pltpu.make_async_copy(grads.at[:, columns(half, at)], (grad_gate, grad_up)[half].at[:, spot],
                                     out_sems.at[half, at])

    def done(stage, at):
        @pl.when(stage == 3)
        def _():
            leave(0, at).start()
            leave(1, at).start()

    spread.run(blocks, done=done)
    tiny.end()
    eye = diagonal()
    gain_grad[...] = jnp.zeros_like(gain_grad)

    def close_shard(shard, _):
        for at in range(rows // LANES):
            span = pl.ds(pl.multiple_of(shard * rows + at * LANES, LANES), LANES)
            dot = from_tile(tiny_all[shard, at : at + 1, :], eye)
            resid = x_low[span, :].astype(jnp.float32) + attn[span, :].astype(jnp.float32)
            value = sums[span, :]
            contrib[span, :] = (value * gain[...] - resid * dot).astype(contrib.dtype)
            gain_grad[...] += jnp.sum(value * resid, axis=0, keepdims=True)
        return 0

    lax.fori_loop(0, 8, close_shard, 0)
    spread.end()

    def drain(at, _):
        leave(0, at).wait()
        leave(1, at).wait()
        return 0

    lax.fori_loop(0, counts, drain, 0)


def back_gather(act_t, w_gate, w_up, d_gate, d_up, dots, x_low, attn, gain, cid, width=512):
    cols, total = act_t.shape
    rows, half = d_gate.shape
    counts = half // width
    low, f32 = jnp.bfloat16, jnp.float32
    dma = pltpu.SemaphoreType.DMA
    vm = pl.BlockSpec(memory_space=pltpu.VMEM)
    hbm = pl.BlockSpec(memory_space=pl.ANY)
    out_shape = [
        jax.ShapeDtypeStruct((total, cols), low),
        jax.ShapeDtypeStruct((1, cols), f32),
        jax.ShapeDtypeStruct((cols, half), f32),
        jax.ShapeDtypeStruct((cols, half), f32),
    ]
    scratch = spread_scratch(counts, rows, width) + [
        pltpu.VMEM((8, 8, LANES), f32), dma((7,)), dma((7,)), dma((2, counts)),
        pltpu.VMEM((cols, 2 * half), low),
        pltpu.VMEM((total, cols), f32),
        pltpu.VMEM((cols, 2 * half), f32),
        dma((2,)), dma((2, counts)),
    ]
    operands = [act_t, w_gate, w_up, d_gate, d_up, dots, x_low, attn, gain]
    kernel = functools.partial(back_kernel, rows, width, counts)
    return kernel_call(kernel, out_shape, operands, [vm] + [hbm] * 4 + [vm] * 4, scratch, cid, "back",
                       [vm, vm, hbm, hbm])


def down_kernel(rows, width, counts, line_counts, cot, weight, hidden, line_own, ffn, d_attn, grad, *refs):
    here = Place()
    spread = Spread(here, counts, refs[:7])
    own_sems, sums, grads, out_sems, line_out = refs[7:12]
    line = Line(here, line_counts, [line_own, line_out] + list(refs[12:]))
    own = load_own(spread, (hidden,), width, counts, own_sems)
    for copy in own:
        copy.start()
    greet(here, slice_peers(here), True)
    line.begin()
    for copy in own:
        copy.wait()
    spread.begin()
    sums[...] = jnp.zeros_like(sums)
    grads[...] = jnp.zeros_like(grads)

    def columns(half, at):
        return pl.ds(pl.multiple_of((half * counts + at) * width, width), width)

    def blocks(across, half, at):
        cols = columns(half, at)
        gained = grads[cols, :]
        for other in range(2):
            row = row_span(here, across, other, rows)
            block = spread.got[across, (spread.core + other) % 2, half, at]
            sums[row, :] += dot_nn(block, weight[cols, :])
            gained = gained + dot_tn(block, cot[row, :])
        grads[cols, :] = gained

    def leave(half, at):
        cols = columns(half, at)
        return pltpu.make_async_copy(grads.at[cols, :], grad.at[cols, :], out_sems.at[half, at])

    def done(stage, at):
        @pl.when(stage == 3)
        def _():
            leave(0, at).start()
            leave(1, at).start()

    steps = spread.run(blocks, line.step, done)
    line.end(steps)

    def close_shard(shard, _):
        span = pl.ds(pl.multiple_of(shard * rows, rows), rows)
        ffn[span, :] = sums[span, :].astype(ffn.dtype)
        d_attn[span, :] = (cot[span, :].astype(jnp.float32) + line_out[span, :].astype(jnp.float32)).astype(
            d_attn.dtype)
        return 0

    lax.fori_loop(0, 8, close_shard, 0)
    spread.end()

    def drain(at, _):
        leave(0, at).wait()
        leave(1, at).wait()
        return 0

    lax.fori_loop(0, counts, drain, 0)


def down_gather(cot, weight, hidden, line, cid, width=256, line_counts=16):
    total, cols = cot.shape
    rows, every = hidden.shape
    counts = every // (2 * width)
    low, f32 = jnp.bfloat16, jnp.float32
    dma = pltpu.SemaphoreType.DMA
    vm = pl.BlockSpec(memory_space=pltpu.VMEM)
    hbm = pl.BlockSpec(memory_space=pl.ANY)
    out_shape = [
        jax.ShapeDtypeStruct((total, cols), low),
        jax.ShapeDtypeStruct((total, cols), low),
        jax.ShapeDtypeStruct(weight.shape, f32),
    ]
    scratch = spread_scratch(counts, rows, width) + [
        dma((2, counts)),
        pltpu.VMEM((total, cols), f32),
        pltpu.VMEM(weight.shape, f32),
        dma((2, counts)),
        pltpu.VMEM((total, cols), low),
    ] + line_scratch(line_counts, line.shape, low)
    kernel = functools.partial(down_kernel, rows, width, counts, line_counts)
    return kernel_call(kernel, out_shape, [cot, weight, hidden, line], [vm, vm, hbm, vm], scratch, cid, "down",
                       [vm, vm, hbm])


def attend_kernel(rows, heads, cols, qkv, rms, cos, sin, mask, w_out, cot, part, mixed_all, g_col, kv, probs, queries,
                  pair_rms, *refs):
    here = Place()
    spread = Spread(here, heads // 2, refs[:7])
    sums, pair_sems, turn_send, turn_recv, local_sem, tiny_own, tiny_pair = refs[7:14]
    got, core = spread.got, here.core
    greet(here, slice_peers(here))
    me = here.shard(0, 0)

    def turn_copy(at):
        across, other = turned(at)
        first = pl.multiple_of(here.shard(across, other) * cols, cols)
        return remote(cot.at[:, pl.ds(first, cols)], g_col.at[pl.ds(pl.multiple_of(me * rows, rows), rows), :],
                      turn_send.at[at], turn_recv.at[at], here.device(across, other))

    own_turn = pltpu.make_async_copy(cot.at[:, pl.ds(pl.multiple_of(me * cols, cols), cols)],
                                     g_col.at[pl.ds(pl.multiple_of(me * rows, rows), rows), :], local_sem)
    own_turn.start()
    half = HD // 2
    scale = 1.0 / math.sqrt(HD)
    wide = heads * HD

    def rotated(first):
        lead = qkv[:, first : first + half] * rms[...]
        trail = qkv[:, first + half : first + HD] * rms[...]
        return lead * cos[...] - trail * sin[...], trail * cos[...] + lead * sin[...]

    low_k, high_k = rotated(wide)
    kv[0, :, :half] = low_k.astype(kv.dtype)
    kv[0, :, half:HD] = high_k.astype(kv.dtype)
    for at in range(2):
        first = HD + at * half
        kv[0, :, first : first + half] = (qkv[:, wide + first : wide + first + half] * rms[...]).astype(kv.dtype)
    eye = diagonal()
    tiny_own[...] = jnp.zeros_like(tiny_own)
    to_tile(tiny_own, 0, rms[:, :1], eye)
    pair_rms[0] = rms[...]
    pair = remote(kv.at[0], kv.at[1], pair_sems.at[0], pair_sems.at[1], spread.ydev)
    tiny = remote(tiny_own, tiny_pair, pair_sems.at[2], pair_sems.at[3], spread.ydev)
    for head in range(heads):
        if head == 1:
            pair.start()
            tiny.start()
            turn_copy(2 * (3 - 1)).start()
            turn_copy(2 * (3 - 1) + 1).start()
        lead, trail = rotated(head * HD)
        queries[:, head * HD : head * HD + half] = (lead * scale).astype(queries.dtype)
        queries[:, head * HD + half : (head + 1) * HD] = (trail * scale).astype(queries.dtype)
    pair.wait()
    for at in range(7):
        if at // 2 != 2:
            turn_copy(at).start()

    def one_head(head, _):
        query = queries[:, pl.ds(pl.multiple_of(head * HD, HD), HD)]
        scores = jnp.concatenate([dot_nt(query, kv[0, :, :HD]), dot_nt(query, kv[1, :, :HD])], axis=1)
        scores = jnp.where(mask[...] > 0, scores, NEG)
        expd = jnp.exp(scores - jnp.max(scores, axis=-1, keepdims=True))
        prob = expd / jnp.sum(expd, axis=-1, keepdims=True)
        probs[head] = prob
        prob_low = prob.astype(jnp.bfloat16)
        mixed = dot_nn(prob_low[:, :rows], kv[0, :, HD:]) + dot_nn(prob_low[:, rows:], kv[1, :, HD:])
        got[0, core, head // (heads // 2), head % (heads // 2)] = mixed.astype(got.dtype)
        return 0

    lax.fori_loop(0, heads, one_head, 0)
    sums[...] = jnp.zeros_like(sums)
    spread.begin()

    def blocks(across, half_at, at):
        span = pl.ds(pl.multiple_of((half_at * (heads // 2) + at) * HD, HD), HD)
        for other in range(2):
            row = row_span(here, across, other, rows)
            block = got[across, (core + other) % 2, half_at, at]
            mixed_all[row, span] = block
            sums[row, :] += dot_nn(block, w_out[span, :])

    spread.run(blocks)
    part[...] = sums[...].astype(part.dtype)
    spread.end()
    tiny.wait()
    for at in range(rows // LANES):
        values = jnp.broadcast_to(from_tile(tiny_pair[at : at + 1, :], eye), (LANES, LANES))
        pair_rms[1, at * LANES : (at + 1) * LANES, :] = values
    own_turn.wait()
    for at in range(7):
        turn_copy(at).wait()


def attend(qkv, rms, cos, sin, mask, w_out, cot, cid):
    rows = qkv.shape[0]
    wide, cols = w_out.shape
    heads = wide // HD
    low, f32 = jnp.bfloat16, jnp.float32
    dma = pltpu.SemaphoreType.DMA
    vm = pl.BlockSpec(memory_space=pltpu.VMEM)
    out_shape = [
        jax.ShapeDtypeStruct((8 * rows, cols), low),
        jax.ShapeDtypeStruct((8 * rows, wide), low),
        jax.ShapeDtypeStruct((8 * rows, cols), low),
        jax.ShapeDtypeStruct((2, rows, 2 * HD), low),
        jax.ShapeDtypeStruct((heads, rows, 2 * rows), f32),
        jax.ShapeDtypeStruct((rows, wide), low),
        jax.ShapeDtypeStruct((2,) + rms.shape, f32),
    ]
    scratch = spread_scratch(heads // 2, rows, HD) + [
        pltpu.VMEM((8 * rows, cols), f32), dma((4,)), dma((7,)), dma((7,)), dma(()),
        pltpu.VMEM((8, LANES), f32), pltpu.VMEM((8, LANES), f32)]
    kernel = functools.partial(attend_kernel, rows, heads, cols)
    return kernel_call(kernel, out_shape, [qkv, rms, cos, sin, mask, w_out, cot], [vm] * 7, scratch, cid,
                       "attend")


def tail_kernel(rows, heads, per, d_attn, w_out, queries, kv, probs, rms, cos, sin, act_t, w_qkv, ffn, x_low,
                attn, gain, gain_grad, d_tok, out, grad, kv_sum, gain_tiles, *refs):
    here = Place()
    width = HD
    counts, out_counts = heads // 2, (heads + 2) // 2
    refs = list(refs)
    line_counts = 8 * per
    cols = d_attn.shape[1]
    extra = cols // (rows // per)

    def take(count):
        taken_refs = refs[:count]
        del refs[:count]
        return taken_refs

    total_refs = take(11)
    spread = Spread(here, out_counts, take(7))
    d_mixed, tiny_own, tiny_all, d_kv, give, taken, give_sems, tiny_send, tiny_recv = take(9)
    sums, gain_sum, tile, tile_send, tile_recv, put_sems, local_sems = take(7)

    def far(at):
        return turned(at // per)

    def near(at):
        return at // (2 * per), at // per % 2

    def place_ffn(at):
        return here.shard(*far(at)) * per + at % per

    def place_tok(at):
        return jnp.where(at < line_counts, here.shard(*near(jnp.minimum(at, line_counts - 1))) * per + at % per, at)

    ffn_sum = take(1)[0]
    line = Line(here, line_counts, [ffn, ffn_sum] + take(8), place_ffn)
    contrib, summed = take(2)
    line_tok = Line(here, line_counts + extra, [contrib, summed] + take(8), place_tok)
    tiny = Tiny(here, tiny_own, tiny_all, (tiny_send, tiny_recv), False)
    got, core = spread.got, here.core
    product = products(here, d_attn, w_out, True, rows, width, counts)
    total = Reduce(here, counts, product, total_refs)
    greet(here, tiny.peers, True)
    line.begin()
    done = total.run(line)

    def land(at, first, second):
        for half_at, value in enumerate((first, second)):
            d_mixed[:, pl.ds(pl.multiple_of((half_at * counts + at) * width, width), width)] = value

    total.end(land)
    half = HD // 2
    scale = 1.0 / math.sqrt(HD)
    depth = w_qkv.shape[0] * 8
    d_kv[...] = jnp.zeros_like(d_kv)

    def one_head(head, dots):
        span = pl.ds(pl.multiple_of(head * HD, HD), HD)
        query = queries[:, span]
        cot = d_mixed[:, span].astype(jnp.bfloat16)
        prob = probs[head]
        d_prob = jnp.concatenate([dot_nt(cot, kv[0, :, HD:]), dot_nt(cot, kv[1, :, HD:])], axis=1)
        delta = jnp.sum(prob * d_prob, axis=-1, keepdims=True)
        d_score = (prob * (d_prob - delta)).astype(jnp.bfloat16)
        prob_low = prob.astype(jnp.bfloat16)
        d_query = (dot_nn(d_score[:, :rows], kv[0, :, :HD]) + dot_nn(d_score[:, rows:], kv[1, :, :HD])) * scale
        for side in range(2):
            keys = slice(side * rows, (side + 1) * rows)
            d_kv[side, :, :HD] += dot_tn(d_score[:, keys], query)
            d_kv[side, :, HD:] += dot_tn(prob_low[:, keys], cot)
        dots = dots + jnp.sum(d_query * query.astype(jnp.float32), axis=-1, keepdims=True)
        lead, trail = d_query[:, :half], d_query[:, half:]
        slot = got.at[0, core, head // out_counts, head % out_counts]
        slot[:, :half] = ((lead * cos[0] + trail * sin[0]) * rms[0]).astype(got.dtype)
        slot[:, half:] = ((trail * cos[0] - lead * sin[0]) * rms[0]).astype(got.dtype)

        line.step(done + head)
        return dots

    dots = lax.fori_loop(0, heads, one_head, jnp.zeros((rows, 1), jnp.float32))
    done += heads
    eye = diagonal()
    tiny_own[...] = jnp.zeros_like(tiny_own)
    for side in (1, 0):
        d_key, d_value = d_kv[side, :, :HD], d_kv[side, :, HD:]
        own = jnp.sum(d_key * kv[side, :, :HD].astype(jnp.float32) +
                      d_value * kv[side, :, HD:].astype(jnp.float32), axis=-1, keepdims=True)
        if side == 0:
            own = own + dots * (1.0 / scale)
        own = own * (rms[side] * rms[side] * (1.0 / depth))
        to_tile(tiny_own, side * (rows // LANES), own, eye)
        lead, trail = d_key[:, :half], d_key[:, half:]
        parts = [(lead * cos[side] + trail * sin[side]) * rms[side],
                 (trail * cos[side] - lead * sin[side]) * rms[side],
                 d_value[:, :half] * rms[side], d_value[:, half:] * rms[side]]
        for at, value in enumerate(parts):
            if side == 1:
                give[:, at * half : (at + 1) * half] = value.astype(give.dtype)
            else:
                d_kv[0, :, at * half : (at + 1) * half] = value
    given = remote(give, taken, give_sems.at[0], give_sems.at[1], spread.ydev)
    given.start()
    sums[...] = jnp.zeros_like(sums)
    given.wait()
    for at in range(2):
        span = slice(at * HD, (at + 1) * HD)
        value = d_kv[0, :, span] + taken[:, span].astype(jnp.float32)
        got[0, core, 1, out_counts - 2 + at] = value.astype(got.dtype)
    tiny.begin()
    spread.begin()
    gain_sum[...] = jnp.zeros_like(gain_sum)

    grad[...] = jnp.zeros_like(grad)

    def blocks(across, half_at, at):
        span = pl.ds(pl.multiple_of((half_at * out_counts + at) * width, width), width)
        gained = grad[:, span]
        for other in range(2):
            row = row_span(here, across, other, rows)
            block = got[across, (core + other) % 2, half_at, at]
            sums[row, :] += dot_nt(block, w_qkv[:, span])
            gained = gained + dot_nn(act_t[:, row], block)
        grad[:, span] = gained

    def contribute(chip):
        def shard_rows(other, _):
            shard, partner = here.shard(chip, other), here.shard((chip + 2) % 4, other)
            for at in range(rows // LANES):
                row = pl.ds(pl.multiple_of(shard * rows + at * LANES, LANES), LANES)
                kept = rows // LANES + at
                dot = from_tile(tiny_all[shard, at : at + 1, :] + tiny_all[partner, kept : kept + 1, :], eye)
                value, x_rows = sums[row, :], x_low[row, :].astype(jnp.float32)
                contrib[row, :] = (value * gain[...] - x_rows * dot).astype(contrib.dtype)
                gain_sum[...] += jnp.sum(value * x_rows, axis=0, keepdims=True)
            return 0

        lax.fori_loop(0, 2, shard_rows, 0)
        line_tok.launch(2 * per * chip, 2 * per)

    first_part = 2 * per
    left = line_counts + extra - first_part
    line.steps(done, line_counts + 2)
    tiny.end()

    def hook(step):
        stage, at = step // out_counts, step % out_counts

        @pl.when(jnp.logical_and(stage > 0, stage < 3))
        def _():
            line_tok.step((stage - 1) * out_counts + at, 0, first_part)

        @pl.when(stage == 3)
        def _():
            line_tok.step(at, first_part, left)

    def complete(stage, at):
        @pl.when(jnp.logical_and(at == out_counts - 1, stage == 0))
        def _():
            contribute(0)

        @pl.when(jnp.logical_and(at == out_counts - 1, stage == 2))
        def _():
            lax.fori_loop(1, 3, lambda chip, _: (contribute(chip), 0)[1], 0)

        @pl.when(jnp.logical_and(at == out_counts - 1, stage == 3))
        def _():
            contribute(3)

    spread.run(blocks, hook, complete)
    for half_at in range(cols // (rows // per)):
        span = pl.ds(line_counts * (rows // per) + half_at * (rows // per), rows // per)
        source = slice(half_at * (rows // per), (half_at + 1) * (rows // per))
        contrib[span, :] = grad[source, heads * HD :].astype(contrib.dtype)
    line_tok.launch(line_counts, extra)
    for at in range(cols // LANES):
        tile[at : at + 1, :] = gain_sum[:, at * LANES : (at + 1) * LANES]
        spot = cols // LANES + at
        tile[spot : spot + 1, :] = gain_grad[:, at * LANES : (at + 1) * LANES]

    def tile_copy(step):
        return remote(tile, gain_tiles.at[here.z], tile_send.at[step], tile_recv.at[step],
                      (here.dp, here.seq, (here.z + step + 1) % 4))

    line.settle()
    me = here.shard(0, 0)
    columns = pl.ds(pl.multiple_of(me * cols, cols), cols)
    chunk = line.chunk

    def put(which, at):
        kind = (line, line_tok)[which]
        goal = here.device(*(far, near)[which](at))
        dst = (out, d_tok)[which].at[pl.ds(pl.multiple_of(at % per * chunk, chunk), chunk), columns]
        return remote(kind.from_end.at[at], dst, put_sems.at[which, 0, at], put_sems.at[which, 1, at], goal)

    def emit(which, at):
        kind = (line, line_tok)[which]
        row = kind.rows(at)
        base = (attn, d_attn)[which][row, :].astype(jnp.float32)
        if which == 0:
            base = base + x_low[row, :].astype(jnp.float32)
        kind.from_end[at] = (base + kind.out[row, :].astype(jnp.float32)).astype(out.dtype)

    def is_own(which, at):
        return at >= 7 * per if which == 0 else at < per

    def send(which, at):
        own = is_own(which, at)

        @pl.when(own)
        def _():
            dst = (out, d_tok)[which].at[pl.ds(pl.multiple_of(at % per * chunk, chunk), chunk), columns]
            pltpu.make_async_copy((line, line_tok)[which].from_end.at[at], dst, local_sems.at[which, at % per]).start()

        @pl.when(jnp.logical_not(own))
        def _():
            put(which, at).start()

    for step in range(3):
        tile_copy(step).start()
    gain_tiles[here.z] = tile[...]

    @pl.when(line.inner == 1)
    def _():
        def early(at, _):
            emit(1, at)
            return 0

        lax.fori_loop(0, first_part, early, 0)

        def both(at, _):
            line_tok.step(at, first_part, left)
            spot = at - out_counts
            ready = first_part + at - out_counts

            @pl.when(jnp.logical_and(spot > 0, spot <= line_counts))
            def _():
                send(0, spot - 1)

            @pl.when(jnp.logical_and(spot > 0, spot <= first_part))
            def _():
                send(1, spot - 1)

            @pl.when(jnp.logical_and(ready > first_part, ready <= line_counts))
            def _():
                send(1, ready - 1)

            @pl.when(spot < line_counts)
            def _():
                emit(0, spot)

            @pl.when(ready < line_counts)
            def _():
                emit(1, ready)
            return 0

        lax.fori_loop(out_counts, out_counts + line_counts + 1, both, 0)
        line_tok.steps(out_counts + line_counts + 1, left + 2, first_part, left)

        def drain(at, _):
            line_tok.down(at).wait_send()
            return 0

        lax.fori_loop(0, line_counts + extra, drain, 0)

    @pl.when(line.inner == 0)
    def _():
        def arrive(at, _):
            line_tok.up(at).wait_send()
            line_tok.down(at).wait_recv()

            @pl.when(jnp.logical_and(at > 0, at <= line_counts))
            def _():
                send(0, at - 1)
                send(1, at - 1)

            @pl.when(at < line_counts)
            def _():
                emit(0, at)
                emit(1, at)
            return 0

        lax.fori_loop(0, line_counts + extra, arrive, 0)

    for half_at in range(extra):
        span = pl.ds((line_counts + half_at) * chunk, chunk)
        kv_sum[half_at * chunk : (half_at + 1) * chunk, :] = summed[span, :].astype(jnp.float32)
    spread.end()
    for which in range(2):
        def finish(at, _, which=which):
            @pl.when(jnp.logical_not(is_own(which, at)))
            def _():
                put(which, at).wait()
            return 0

        lax.fori_loop(0, line_counts, finish, 0)
        for at in range(per):
            dst = (out, d_tok)[which].at[at * chunk : (at + 1) * chunk, columns]
            spot = (7 * per if which == 0 else 0) + at
            pltpu.make_async_copy((line, line_tok)[which].from_end.at[spot], dst, local_sems.at[which, at]).wait()
    for step in range(3):
        tile_copy(step).wait()


def tail(d_attn, w_out, queries, kv, probs, rms, cos, sin, act_t, w_qkv, ffn, x_low, attn, gain, gain_grad, cid,
         per=2):
    total, cols = d_attn.shape
    rows = total // 8
    wide = w_out.shape[0]
    heads = wide // HD
    low, f32 = jnp.bfloat16, jnp.float32
    dma = pltpu.SemaphoreType.DMA
    vm = pl.BlockSpec(memory_space=pltpu.VMEM)
    counts = 8 * per
    chunk = rows // per
    extra = cols // chunk
    long = (total + cols, cols)
    out_shape = [
        jax.ShapeDtypeStruct((rows, 8 * cols), low),
        jax.ShapeDtypeStruct((rows, 8 * cols), low),
        jax.ShapeDtypeStruct(w_qkv.shape, f32),
        jax.ShapeDtypeStruct((cols, 2 * HD), f32),
        jax.ShapeDtypeStruct((4, 8, LANES), f32),
    ]
    scratch = reduce_scratch(heads // 2, rows, HD) + spread_scratch((heads + 2) // 2, rows, HD)
    scratch += [
        pltpu.VMEM((rows, wide), f32),
        pltpu.VMEM((8, LANES), f32),
        pltpu.VMEM((8, 8, LANES), f32),
        pltpu.VMEM((2, rows, 2 * HD), f32),
        pltpu.VMEM((rows, 2 * HD), low),
        pltpu.VMEM((rows, 2 * HD), low),
        dma((2,)), dma((7,)), dma((7,)),
        pltpu.VMEM((total, cols), f32),
        pltpu.VMEM((1, cols), f32),
        pltpu.VMEM((8, LANES), f32),
        dma((3,)), dma((3,)), dma((2, 2, counts)), dma((2, per)),
        pltpu.VMEM((total, cols), low),
    ] + line_scratch(counts, (total, cols), low)
    scratch += [pltpu.VMEM(long, low), pltpu.VMEM(long, low)] + line_scratch(counts + extra, long, low)
    operands = [d_attn, w_out, queries, kv, probs, rms, cos, sin, act_t, w_qkv, ffn, x_low, attn, gain, gain_grad]
    kernel = functools.partial(tail_kernel, rows, heads, per)
    return kernel_call(kernel, out_shape, operands, [vm] * len(operands), scratch, cid, "tail")


LANES = 128


def acts_move(
    tokens, seg_ids, gain_attn, w_query, kv_weight, w_out, gain_ffn, w_gate, w_up, w_down, d_out
):
    rows = tokens.shape[0]
    offset = lax.axis_index("seq") * rows
    places, cos_table, sin_table = place_tables(seg_ids)
    away = rows - offset

    def own_first(table):
        return jnp.stack(
            [
                lax.dynamic_slice_in_dim(table, offset, rows, 0),
                lax.dynamic_slice_in_dim(table, away, rows, 0),
            ]
        )

    pair_places = own_first(places)
    pair_segs = own_first(seg_ids)
    pair_cos = own_first(cos_table)
    pair_sin = own_first(sin_table)
    allowed = (pair_segs[0][:, None] == pair_segs.reshape(1, -1)) & (
        pair_places[0][:, None] >= pair_places.reshape(1, -1)
    )
    gain_one = gain_attn.astype(jnp.float32)[None, :]
    gain_two = gain_ffn.astype(jnp.float32)[None, :]
    wide = w_query.shape[1]

    qkv, x_low, act_one_t, w_qkv, rms = opening(tokens, gain_one, w_query, kv_weight, 1)
    attn_part, mixed_all, g_low, kv, probs, queries, pair_rms = attend(
        qkv, rms, pair_cos[0], pair_sin[0], allowed.astype(jnp.float32), w_out, d_out, 2
    )
    d_hidden, attn = scatter_product(g_low, w_down, 512, 3, attn_part)
    hidden, d_gate, d_up, act_two_t, dots = ffn_scatter(x_low, attn, gain_two, w_gate, w_up, d_hidden, 4)
    contrib, grad_gain_two, grad_gate, grad_up = back_gather(
        act_two_t, w_gate, w_up, d_gate, d_up, dots, x_low, attn, gain_two, 5
    )
    ffn, d_attn, grad_down = down_gather(g_low, w_down, hidden, contrib, 6)
    grad_out = matmul_tn(mixed_all, d_attn)
    d_tokens, out, grad_qkv, grad_kv, gain_tiles = tail(
        d_attn,
        w_out,
        queries,
        kv,
        probs,
        pair_rms,
        pair_cos,
        pair_sin,
        act_one_t,
        w_qkv,
        ffn,
        x_low,
        attn,
        gain_one,
        grad_gain_two,
        7,
    )
    gains = jnp.sum(gain_tiles, axis=0).reshape(2, -1)
    return (
        out,
        d_tokens.astype(jnp.float32),
        gains[0],
        grad_qkv[:, :wide],
        grad_kv,
        grad_out,
        gains[1],
        grad_gate,
        grad_up,
        grad_down,
    )


def solution(mesh):
    in_specs = (
        P(("dp", "seq"), None),
        P("dp"),
        P(("dp", "seq")),
        P(("dp", "seq"), "tensor"),
        P(("dp", "seq"), None),
        P("tensor", ("dp", "seq")),
        P(("dp", "seq")),
        P(("dp", "seq"), "tensor"),
        P(("dp", "seq"), "tensor"),
        P("tensor", ("dp", "seq")),
        P(("dp", "seq"), None),
    )
    out_specs = (
        P(("dp", "seq"), None),
        P(("dp", "seq"), None),
        P(("dp", "seq")),
        P(("dp", "seq"), "tensor"),
        P(("dp", "seq"), None),
        P("tensor", ("dp", "seq")),
        P(("dp", "seq")),
        P(("dp", "seq"), "tensor"),
        P(("dp", "seq"), "tensor"),
        P("tensor", ("dp", "seq")),
    )

    def shards(*arrays):
        tokens = arrays[0]
        sizes = tuple(mesh.shape[name] for name in ("dp", "seq", "tensor"))
        count = tokens.shape[0] * sizes[0] * sizes[1]
        plan = acts_move if sizes == (4, 2, 4) and count <= tokens.shape[1] else weights_move
        return plan(*arrays)

    return jax.shard_map(shards, mesh=mesh, in_specs=in_specs, out_specs=out_specs, check_vma=False)
```

```python
import functools
import math

import jax
import jax.numpy as jnp
from jax import lax
from jax.experimental import pallas as pl
from jax.experimental.pallas import tpu as pltpu
from jax.sharding import PartitionSpec as P

HD = 256


EPS = 1e-06
NEG = -1e30


def place_tables(segs):
    length = segs.shape[0]
    index = jnp.arange(length, dtype=jnp.int32)
    flags = jnp.concatenate([jnp.ones((1,), dtype=bool), segs[1:] != segs[:-1]])
    starts = lax.cummax(jnp.where(flags, index, jnp.zeros_like(index)), axis=0)
    places = index - starts
    half_size = HD // 2
    freqs = jnp.exp(jnp.arange(half_size, dtype=jnp.float32) * (-math.log(10000.0) / half_size))
    angles = places.astype(jnp.float32)[:, None] * freqs[None, :]
    return (places, jnp.cos(angles), jnp.sin(angles))


def rotate(vector, cos_table, sin_table):
    half_size = vector.shape[-1] // 2
    leading = vector[..., :half_size]
    trailing = vector[..., half_size:]
    return jnp.concatenate(
        [leading * cos_table - trailing * sin_table, trailing * cos_table + leading * sin_table],
        axis=-1,
    )


def rotate_back(vector, cos_table, sin_table):
    half_size = vector.shape[-1] // 2
    leading = vector[..., :half_size]
    trailing = vector[..., half_size:]
    return jnp.concatenate(
        [leading * cos_table + trailing * sin_table, trailing * cos_table - leading * sin_table],
        axis=-1,
    )


def matmul(left, right):
    return jnp.dot(left, right, preferred_element_type=jnp.float32)


def matmul_nt(left, right):
    return lax.dot_general(
        left, right, (((1,), (1,)), ((), ())), preferred_element_type=jnp.float32
    )


def matmul_tn(left, right):
    return lax.dot_general(
        left, right, (((0,), (0,)), ((), ())), preferred_element_type=jnp.float32
    )


def gelu_tanh(values):
    return jax.nn.gelu(values, approximate=True)


def norm_back(d_act, normed, rms_val, gain_val):
    scaled = d_act * gain_val
    return rms_val * (scaled - normed * jnp.mean(scaled * normed, axis=-1, keepdims=True))


def weights_move(
    tokens, seg_ids, gain_attn, w_query, kv_weight, w_out, gain_ffn, w_gate, w_up, w_down, d_out
):
    rows = tokens.shape[0]
    scale_factor = 1.0 / math.sqrt(HD)
    offset = lax.axis_index("seq") * rows
    places, cos_table, sin_table = place_tables(seg_ids)
    own_places = lax.dynamic_slice_in_dim(places, offset, rows, 0)
    own_segs = lax.dynamic_slice_in_dim(seg_ids, offset, rows, 0)
    own_cos = lax.dynamic_slice_in_dim(cos_table, offset, rows, 0)
    own_sin = lax.dynamic_slice_in_dim(sin_table, offset, rows, 0)
    allowed = (own_segs[:, None] == seg_ids[None, :]) & (own_places[:, None] >= places[None, :])
    full_query, full_out, full_kv, full_gain_one = (
        lax.all_gather(w_query, ("dp", "seq"), axis=0, tiled=True),
        lax.all_gather(w_out, ("dp", "seq"), axis=1, tiled=True),
        lax.all_gather(kv_weight, ("dp", "seq"), axis=0, tiled=True),
        lax.all_gather(gain_attn, ("dp", "seq"), axis=0, tiled=True),
    )
    gain_one = full_gain_one.astype(jnp.float32)
    inputs = tokens.astype(jnp.float32)
    rms_one = lax.rsqrt(jnp.mean(inputs * inputs, axis=-1, keepdims=True) + EPS)
    norm_one = inputs * rms_one
    act_one = (norm_one * gain_one).astype(jnp.bfloat16)
    query_pre = matmul(act_one, full_query)
    heads = query_pre.shape[1] // HD
    kv_pre = matmul(act_one, full_kv)
    queries = (
        rotate(query_pre.reshape(rows, heads, HD), own_cos[:, None, :], own_sin[:, None, :])
        * scale_factor
    ).astype(jnp.bfloat16)
    own_kv = jnp.concatenate(
        [rotate(kv_pre[:, :HD], own_cos, own_sin), kv_pre[:, HD:]], axis=1
    ).astype(jnp.bfloat16)
    all_kv = lax.all_gather(own_kv, "seq", axis=0, tiled=True)
    keys = all_kv[:, :HD]
    values_all = all_kv[:, HD:]
    scores = jnp.einsum("rhd,kd->hrk", queries, keys, preferred_element_type=jnp.float32)
    scores = jnp.where(allowed[None], scores, NEG)
    top_score = jnp.max(scores, axis=-1, keepdims=True)
    expd = jnp.exp(scores - top_score)
    total = jnp.sum(expd, axis=-1, keepdims=True)
    log_total = top_score + jnp.log(total)
    probs_low = (expd / total).astype(jnp.bfloat16)
    mixed = (
        jnp.einsum("hrk,kd->rhd", probs_low, values_all, preferred_element_type=jnp.float32)
        .reshape(rows, heads * HD)
        .astype(jnp.bfloat16)
    )
    attn = lax.psum(matmul(mixed, full_out), "tensor")
    resid = inputs + attn
    full_gate, full_up, full_down, full_gain_two = (
        lax.all_gather(w_gate, ("dp", "seq"), axis=0, tiled=True),
        lax.all_gather(w_up, ("dp", "seq"), axis=0, tiled=True),
        lax.all_gather(w_down, ("dp", "seq"), axis=1, tiled=True),
        lax.all_gather(gain_ffn, ("dp", "seq"), axis=0, tiled=True),
    )
    gain_two = full_gain_two.astype(jnp.float32)
    rms_two = lax.rsqrt(jnp.mean(resid * resid, axis=-1, keepdims=True) + EPS)
    norm_two = resid * rms_two
    act_two = (norm_two * gain_two).astype(jnp.bfloat16)
    gate = matmul(act_two, full_gate)
    up_val = matmul(act_two, full_up)
    gelu_val, gelu_pull = jax.vjp(gelu_tanh, gate)
    hidden = (gelu_val * up_val).astype(jnp.bfloat16)
    ffn = lax.psum(matmul(hidden, full_down).astype(jnp.bfloat16), "tensor").astype(jnp.float32)
    out = (resid + ffn).astype(jnp.bfloat16)
    back_gate, back_up, back_down = (
        lax.all_gather(w_gate, ("dp", "seq"), axis=0, tiled=True),
        lax.all_gather(w_up, ("dp", "seq"), axis=0, tiled=True),
        lax.all_gather(w_down, ("dp", "seq"), axis=1, tiled=True),
    )
    d_hidden = matmul_nt(d_out, back_down)
    grad_down = matmul_tn(hidden, d_out)
    d_gate = gelu_pull(d_hidden * up_val)[0].astype(jnp.bfloat16)
    d_up = (d_hidden * gelu_val).astype(jnp.bfloat16)
    grad_gate = matmul_tn(act_two, d_gate)
    grad_up = matmul_tn(act_two, d_up)
    d_act_two = lax.psum(matmul_nt(d_gate, back_gate) + matmul_nt(d_up, back_up), "tensor")
    grad_gain_two = jnp.sum(d_act_two * norm_two, axis=0)
    d_resid = d_out.astype(jnp.float32) + norm_back(d_act_two, norm_two, rms_two, gain_two)
    ffn_grads = (
        lax.psum_scatter(
            grad_gate.astype(jnp.bfloat16), ("dp", "seq"), scatter_dimension=0, tiled=True
        ).astype(jnp.float32),
        lax.psum_scatter(
            grad_up.astype(jnp.bfloat16), ("dp", "seq"), scatter_dimension=0, tiled=True
        ).astype(jnp.float32),
        lax.psum_scatter(
            grad_down.astype(jnp.bfloat16), ("dp", "seq"), scatter_dimension=1, tiled=True
        ).astype(jnp.float32),
        lax.psum_scatter(
            grad_gain_two.astype(jnp.bfloat16), ("dp", "seq"), scatter_dimension=0, tiled=True
        ).astype(jnp.float32),
    )
    back_query, back_out, back_kv = (
        lax.all_gather(w_query, ("dp", "seq"), axis=0, tiled=True),
        lax.all_gather(w_out, ("dp", "seq"), axis=1, tiled=True),
        lax.all_gather(kv_weight, ("dp", "seq"), axis=0, tiled=True),
    )
    d_attn = d_resid.astype(jnp.bfloat16)
    grad_out = matmul_tn(mixed, d_attn)
    d_mixed = matmul_nt(d_attn, back_out).astype(jnp.bfloat16).reshape(rows, heads, HD)
    scores_again = jnp.einsum("rhd,kd->hrk", queries, keys, preferred_element_type=jnp.float32)
    probs = jnp.where(allowed[None], jnp.exp(scores_again - log_total), 0.0)
    d_probs = jnp.einsum("rhd,kd->hrk", d_mixed, values_all, preferred_element_type=jnp.float32)
    delta = jnp.sum(probs * d_probs, axis=-1, keepdims=True)
    d_scores = (probs * (d_probs - delta)).astype(jnp.bfloat16)
    d_queries = (
        jnp.einsum("hrk,kd->rhd", d_scores, keys, preferred_element_type=jnp.float32) * scale_factor
    )
    d_query_pre = (
        rotate_back(d_queries, own_cos[:, None, :], own_sin[:, None, :])
        .reshape(rows, heads * HD)
        .astype(jnp.bfloat16)
    )
    d_keys_part = jnp.einsum("hrk,rhd->kd", d_scores, queries, preferred_element_type=jnp.float32)
    d_values_part = jnp.einsum(
        "hrk,rhd->kd", probs.astype(jnp.bfloat16), d_mixed, preferred_element_type=jnp.float32
    )
    own_kv_grad = lax.psum_scatter(
        jnp.concatenate([d_keys_part, d_values_part], axis=1).astype(jnp.bfloat16),
        "seq",
        scatter_dimension=0,
        tiled=True,
    )
    d_act_query = matmul_nt(d_query_pre, back_query)
    d_act_sum, kv_grad = (
        lax.psum(d_act_query.astype(jnp.bfloat16), "tensor").astype(jnp.float32),
        lax.psum(own_kv_grad, "tensor").astype(jnp.float32),
    )
    d_kv_pre = jnp.concatenate(
        [rotate_back(kv_grad[:, :HD], own_cos, own_sin), kv_grad[:, HD:]], axis=1
    ).astype(jnp.bfloat16)
    d_act_one = d_act_sum + matmul_nt(d_kv_pre, back_kv)
    grad_query = matmul_tn(act_one, d_query_pre)
    grad_kv = matmul_tn(act_one, d_kv_pre)
    grad_gain_one = jnp.sum(d_act_one * norm_one, axis=0)
    d_tokens = d_resid + norm_back(d_act_one, norm_one, rms_one, gain_one)
    attn_grads = (
        lax.psum_scatter(
            grad_query.astype(jnp.bfloat16), ("dp", "seq"), scatter_dimension=0, tiled=True
        ).astype(jnp.float32),
        lax.psum_scatter(
            grad_out.astype(jnp.bfloat16), ("dp", "seq"), scatter_dimension=1, tiled=True
        ).astype(jnp.float32),
        lax.psum_scatter(
            grad_kv.astype(jnp.bfloat16), ("dp", "seq"), scatter_dimension=0, tiled=True
        ).astype(jnp.float32),
        lax.psum_scatter(
            grad_gain_one.astype(jnp.bfloat16), ("dp", "seq"), scatter_dimension=0, tiled=True
        ).astype(jnp.float32),
    )
    return (
        out,
        d_tokens,
        attn_grads[3],
        attn_grads[0],
        attn_grads[2],
        attn_grads[1],
        ffn_grads[3],
        ffn_grads[0],
        ffn_grads[1],
        ffn_grads[2],
    )


MESH = pl.DeviceIdType.MESH
VMEM_LIMIT = 66000 * 1024


class Place:
    def __init__(self):
        self.dp = lax.axis_index("dp")
        self.seq = lax.axis_index("seq")
        self.z = lax.axis_index("tensor")
        self.core = lax.rem(self.dp, 2)
        self.chip = lax.div(self.dp, 2)

    def device(self, across, other):
        chip = (self.chip + across) % 2
        seq = (self.seq + across // 2) % 2
        core = (self.core + other) % 2
        return chip * 2 + core, seq, self.z

    def shard(self, across, other):
        dp, seq, _ = self.device(across, other)
        return dp * 2 + seq


def greet(here, peers, line=False):
    barrier = pltpu.get_barrier_semaphore()
    peers = list(peers)
    if line:
        peers += [(here.dp, here.seq, (here.z + step) % 4) for step in range(1, 4)]
    for peer in peers:
        pl.semaphore_signal(barrier, inc=1, device_id=peer, device_id_type=MESH)
    pl.semaphore_wait(barrier, len(peers))


def remote(src, dst, send, recv, peer):
    return pltpu.make_async_remote_copy(
        src_ref=src, dst_ref=dst, send_sem=send, recv_sem=recv, device_id=peer, device_id_type=MESH
    )


class Line:
    def __init__(self, here, counts, refs, place=None):
        self.own, self.out, self.from_end, self.from_mid = refs[:4]
        self.sems = refs[4:10]
        self.counts = counts
        self.chunk = self.own.shape[0] // counts
        self.place = place
        z = here.z
        self.inner = ((z + 1) // 2) % 2
        self.mate = (here.dp, here.seq, z + 1 - 2 * (z % 2))
        self.other = (here.dp, here.seq, 3 - z)

    def rows(self, at):
        at = at if self.place is None else self.place(at)
        return pl.ds(pl.multiple_of(at * self.chunk, self.chunk), self.chunk)

    def up(self, at):
        return remote(self.own.at[self.rows(at), :], self.from_end.at[at], self.sems[0].at[at],
                      self.sems[1].at[at], self.mate)

    def over(self, at):
        return remote(self.out.at[self.rows(at), :], self.from_mid.at[at], self.sems[2].at[at],
                      self.sems[3].at[at], self.other)

    def down(self, at):
        rows = self.rows(at)
        return remote(self.out.at[rows, :], self.out.at[rows, :], self.sems[4].at[at],
                      self.sems[5].at[at], self.mate)

    def launch(self, first, count):
        @pl.when(self.inner == 0)
        def _():
            def send(at, _):
                self.up(first + at).start()
                return 0

            lax.fori_loop(0, count, send, 0)

    def begin(self):
        self.launch(0, self.counts)

    def first(self, at):
        rows = self.rows(at)
        self.up(at).wait_recv()
        total = self.own[rows, :].astype(jnp.float32) + self.from_end[at].astype(jnp.float32)
        self.out[rows, :] = total.astype(self.out.dtype)
        self.over(at).start()

    def second(self, at):
        rows = self.rows(at)
        self.over(at).wait()
        total = self.out[rows, :].astype(jnp.float32) + self.from_mid[at].astype(jnp.float32)
        self.out[rows, :] = total.astype(self.out.dtype)
        self.down(at).start()

    def step(self, at, start=0, count=None):
        count = self.counts if count is None else count

        @pl.when(jnp.logical_and(self.inner == 1, at < count))
        def _():
            self.first(start + at)

        @pl.when(jnp.logical_and(self.inner == 1, jnp.logical_and(at > 1, at < count + 2)))
        def _():
            self.second(start + at - 2)

    def steps(self, first, last, start=0, count=None):
        def rest(at, _):
            self.step(at, start, count)
            return 0

        lax.fori_loop(first, last, rest, 0)

    def settle(self):
        @pl.when(self.inner == 0)
        def _():
            def take(at, _):
                self.up(at).wait_send()
                self.down(at).wait_recv()
                return 0

            lax.fori_loop(0, self.counts, take, 0)

        @pl.when(self.inner == 1)
        def _():
            def drain(at, _):
                self.down(at).wait_send()
                return 0

            lax.fori_loop(0, self.counts, drain, 0)

    def end(self, done=0):
        self.steps(min(done, self.counts + 2), self.counts + 2)
        self.settle()


def line_scratch(counts, shape, low):
    buf = pltpu.VMEM((counts, shape[0] // counts, shape[1]), low)
    return [buf, buf] + [pltpu.SemaphoreType.DMA((counts,))] * 6


def turned(at):
    return 3 - at // 2, 1 - at % 2


def slice_peers(here):
    return [here.device(*turned(at)) for at in range(7)]


def kernel_call(kernel, out_shape, operands, specs, scratch, cid, name, out_specs=None):
    vm = pl.BlockSpec(memory_space=pltpu.VMEM)
    return pl.pallas_call(
        kernel,
        out_shape=out_shape,
        in_specs=specs,
        out_specs=out_specs or [vm] * len(out_shape),
        scratch_shapes=scratch,
        compiler_params=pltpu.CompilerParams(
            collective_id=cid, has_side_effects=True, vmem_limit_bytes=VMEM_LIMIT
        ),
        name=f"{name}_{cid}",
    )(*operands)


class Tiny:
    def __init__(self, here, src, dst, sems, spread):
        self.here, self.src, self.dst, self.sems, self.spread = here, src, dst, sems, spread
        self.peers = slice_peers(here)
        self.me = here.shard(0, 0)

    def tile(self, shard):
        return self.src.at[shard] if self.spread else self.src

    def copy(self, at):
        return remote(self.tile(self.here.shard(*turned(at))), self.dst.at[self.me], self.sems[0].at[at],
                      self.sems[1].at[at], self.peers[at])

    def begin(self):
        for at in range(7):
            self.copy(at).start()
        self.dst[self.me] = self.tile(self.me)[...]

    def end(self):
        for at in range(7):
            self.copy(at).wait()


class Reduce:
    def __init__(self, here, counts, product, refs, before=None):
        self.counts, self.product, self.before = counts, product, before
        self.held, self.sib_out, self.sib_in, self.from_x, self.from_y = refs[:5]
        self.sib_sems, self.x_sems, self.y_sems = refs[5:7], refs[7:9], refs[9:11]
        self.sib, self.xdev, self.ydev = here.device(0, 1), here.device(1, 0), here.device(2, 0)
        self.steps = 4 * counts
        self.ring = self.sib_out.shape[0]

    def streams(self, stage):
        far = stage // 3
        x_chip = jnp.where(stage == 0, 3, jnp.where(stage == 2, 0, 1))
        y_chip = jnp.where(stage == 0, 3, jnp.where(stage == 2, 0, 2))
        return (x_chip, far), (y_chip, 1 - far)

    def to_sib(self, step, stream):
        stage, at = step // self.counts, step % self.counts
        return remote(self.sib_out.at[step % self.ring, stream], self.sib_in.at[stage, stream, at],
                      self.sib_sems[0].at[stage, stream, at], self.sib_sems[1].at[stage, stream, at], self.sib)

    def to_x(self, hop, at, stage=0):
        return remote(self.held.at[stage, 0, at], self.from_x.at[hop, at], self.x_sems[0].at[hop, at],
                      self.x_sems[1].at[hop, at], self.xdev)

    def to_y(self, hop, at, stage=0):
        return remote(self.held.at[stage, 1, at], self.from_y.at[hop, at], self.y_sems[0].at[hop, at],
                      self.y_sems[1].at[hop, at], self.ydev)

    def compute(self, step):
        stage, at = step // self.counts, step % self.counts
        if self.before:
            for stop in range(3):
                @pl.when(step == stop * self.counts)
                def _():
                    self.before(stop)

        @pl.when(step >= self.ring)
        def _():
            for stream in range(2):
                self.to_sib(step - self.ring, stream).wait_send()

        for stream, (across, half) in enumerate(self.streams(stage)):
            self.sib_out[step % self.ring, stream] = self.product(across, 1, half, at).astype(jnp.bfloat16)
            self.held[stage, stream, at] = self.product(across, 0, half, at).astype(jnp.bfloat16)
        for stream in range(2):
            self.to_sib(step, stream).start()

    def finish(self, step):
        stage, at = step // self.counts, step % self.counts
        for stream in range(2):
            self.to_sib(step, stream).wait_recv()

        def total(stream):
            return self.held[stage, stream, at].astype(jnp.float32) + self.sib_in[stage, stream, at].astype(
                jnp.float32)

        @pl.when(stage < 3)
        def _():
            for stream in range(2):
                self.held[stage, stream, at] = total(stream).astype(jnp.bfloat16)

        @pl.when(stage == 3)
        def _():
            self.to_y(0, at).wait_recv()
            self.held[3, 0, at] = (total(0) + self.from_y[0, at].astype(jnp.float32)).astype(jnp.bfloat16)
            self.to_x(0, at).wait_recv()
            self.held[3, 1, at] = (total(1) + self.from_x[0, at].astype(jnp.float32)).astype(jnp.bfloat16)

        @pl.when(stage != 2)
        def _():
            hop = stage - stage // 3
            self.to_x(hop, at, stage).start()
            self.to_y(hop, at, stage).start()

    def run(self, hook=None):
        def body(step, _):
            @pl.when(step < self.steps)
            def _():
                self.compute(step)

            @pl.when(step > 0)
            def _():
                self.finish(step - 1)

            if hook:
                hook(step)
            return 0

        lax.fori_loop(0, self.steps + 1, body, 0)
        return self.steps + 1

    def end(self, emit):
        def last(at, _):
            values = []
            for half in range(2):
                xs, ys = (1, 2) if half == 0 else (2, 1)
                self.to_x(xs, at).wait_recv()
                self.to_y(ys, at).wait_recv()
                values.append(self.held[2, half, at].astype(jnp.float32) + self.from_x[xs, at].astype(jnp.float32)
                              + self.from_y[ys, at].astype(jnp.float32))
            emit(at, *values)
            for hop in range(3):
                self.to_x(hop, at).wait_send()
                self.to_y(hop, at).wait_send()
            return 0

        lax.fori_loop(0, self.counts, last, 0)

        def drain(at, _):
            for stream in range(2):
                self.to_sib(self.steps - self.ring + at, stream).wait_send()
            return 0

        lax.fori_loop(0, self.ring, drain, 0)


def reduce_scratch(counts, rows, width, ring=4):
    low, dma = jnp.bfloat16, pltpu.SemaphoreType.DMA
    block = pltpu.VMEM((4, 2, counts, rows, width), low)
    landed = pltpu.VMEM((3, counts, rows, width), low)
    sent = pltpu.VMEM((ring, 2, rows, width), low)
    return [block, sent, block, landed, landed] + [dma((4, 2, counts))] * 2 + [dma((3, counts))] * 4


class Spread:
    def __init__(self, here, counts, refs):
        self.counts = counts
        self.got = refs[0]
        self.x_sems, self.y_sems, self.sib_sems = refs[1:3], refs[3:5], refs[5:7]
        self.core = here.core
        self.sib, self.xdev, self.ydev = here.device(0, 1), here.device(1, 0), here.device(2, 0)

    def slot(self, across, half, at):
        return self.got.at[across, self.core, half, at]

    def x_copy(self, hop, at):
        half = jnp.minimum(hop, 1)
        src = self.slot(2 * (hop // 2), half, at)
        dst = self.slot(1 + 2 * (hop // 2), half, at)
        return remote(src, dst, self.x_sems[0].at[hop, at], self.x_sems[1].at[hop, at], self.xdev)

    def y_copy(self, hop, at):
        half = 1 - jnp.minimum(hop, 1)
        src = self.slot(hop // 2, half, at)
        dst = self.slot(2 + hop // 2, half, at)
        return remote(src, dst, self.y_sems[0].at[hop, at], self.y_sems[1].at[hop, at], self.ydev)

    def streams(self, stage):
        some, last, late = jnp.minimum(stage, 1), stage // 3, stage // 2
        return (some + 2 * last, late), (2 * some + last, 1 - late)

    def sib_copy(self, stage, stream, at):
        across, half = self.streams(stage)[stream]
        slot = self.slot(across, half, at)
        spot = (stage, stream, at)
        return remote(slot, slot, self.sib_sems[0].at[spot], self.sib_sems[1].at[spot], self.sib)

    def begin(self):
        def first(at, _):
            self.x_copy(0, at).start()
            self.y_copy(0, at).start()
            return 0

        def own(at, _):
            self.sib_copy(0, 0, at).start()
            self.sib_copy(0, 1, at).start()
            return 0

        lax.fori_loop(0, self.counts, first, 0)
        lax.fori_loop(0, self.counts, own, 0)

    def run(self, blocks, hook=None, done=None):
        counts = self.counts

        def body(step, _):
            stage, at = step // counts, step % counts

            @pl.when(jnp.logical_and(stage > 0, stage < 4))
            def _():
                self.x_copy(stage - 1, at).wait_recv()
                self.sib_copy(stage, 0, at).start()
                self.y_copy(stage - 1, at).wait_recv()
                self.sib_copy(stage, 1, at).start()

            @pl.when(jnp.logical_and(stage > 0, stage < 3))
            def _():
                self.x_copy(stage, at).start()
                self.y_copy(stage, at).start()

            @pl.when(step > 0)
            def _():
                old, spot = (step - 1) // counts, (step - 1) % counts
                for stream, (across, half) in enumerate(self.streams(old)):
                    self.sib_copy(old, stream, spot).wait_recv()
                    blocks(across, half, spot)
                if done:
                    done(old, spot)

            if hook:
                hook(step)
            return 0

        lax.fori_loop(0, 4 * counts + 1, body, 0)
        return 4 * counts + 1

    def end(self):
        def drain(at, _):
            for hop in range(3):
                self.x_copy(hop, at).wait_send()
                self.y_copy(hop, at).wait_send()
            for stage in range(4):
                self.sib_copy(stage, 0, at).wait_send()
                self.sib_copy(stage, 1, at).wait_send()
            return 0

        lax.fori_loop(0, self.counts, drain, 0)


def spread_scratch(counts, rows, width):
    dma = pltpu.SemaphoreType.DMA
    return [pltpu.VMEM((4, 2, 2, counts, rows, width), jnp.bfloat16)] + [dma((3, counts))] * 4 + [
        dma((4, 2, counts))] * 2


def row_span(here, across, other, rows):
    return pl.ds(pl.multiple_of(here.shard(across, other) * rows, rows), rows)


def dot_nt(left, right):
    return lax.dot_general(left, right, (((1,), (1,)), ((), ())), preferred_element_type=jnp.float32)


def dot_tn(left, right):
    return lax.dot_general(left, right, (((0,), (0,)), ((), ())), preferred_element_type=jnp.float32)


def dot_nn(left, right):
    return jnp.dot(left, right, preferred_element_type=jnp.float32)


def products(here, act, weight, nt, rows, width, counts):
    def product(across, other, half, at):
        cols = pl.ds(pl.multiple_of((half * counts + at) * width, width), width)
        block = act[row_span(here, across, other, rows), :]
        return dot_nt(block, weight[cols, :]) if nt else dot_nn(block, weight[:, cols])

    return product


def diagonal():
    return (lax.broadcasted_iota(jnp.int32, (LANES, LANES), 0) ==
            lax.broadcasted_iota(jnp.int32, (LANES, LANES), 1)).astype(jnp.float32)


def to_tile(tile, first, column, eye):
    for at in range(column.shape[0] // LANES):
        spread = column[at * LANES : (at + 1) * LANES, :] * eye
        tile[first + at : first + at + 1, :] = jnp.sum(spread, axis=0, keepdims=True)


def from_tile(row, eye):
    return jnp.sum(eye * row, axis=1, keepdims=True)


def make_tables(here, rows, segs, cos, sin, mask):
    eye = diagonal()
    tiles = rows // LANES
    freqs = jnp.exp(lax.broadcasted_iota(jnp.int32, (1, LANES), 1).astype(jnp.float32) * (-math.log(10000.0) / LANES))
    lane = lax.broadcasted_iota(jnp.int32, (1, LANES), 1)
    line = lax.broadcasted_iota(jnp.int32, (LANES, 1), 0)

    def row_of(side, at):
        return ((here.seq + side) % 2) * tiles + at

    for side in range(2):
        for at in range(tiles):
            row = row_of(side, at)
            ids = from_tile(segs[pl.ds(row, 1), :], eye)
            before = jnp.zeros((LANES, 1), jnp.float32)
            for other in range(2 * tiles):
                smaller = segs[other : other + 1, :] < ids
                before += jnp.sum(smaller.astype(jnp.float32), axis=-1, keepdims=True)
            index = row * LANES + line
            angles = (index.astype(jnp.float32) - before) * freqs
            span = slice(at * LANES, (at + 1) * LANES)
            cos[side, span, :] = jnp.cos(angles)
            sin[side, span, :] = jnp.sin(angles)
            if side == 0:
                for key_side in range(2):
                    for key_at in range(tiles):
                        key_row = row_of(key_side, key_at)
                        same = segs[pl.ds(key_row, 1), :] == ids
                        allowed = jnp.logical_and(same, key_row * LANES + lane <= index)
                        first = key_side * rows + key_at * LANES
                        mask[span, first : first + LANES] = allowed.astype(jnp.float32)


def open_kernel(rows, width, counts, tokens, gain, w_query, kv_weight, segs, qkv, x_low, act_t, w_qkv, rms, cos, sin,
                mask, *refs):
    here = Place()
    cols = gain.shape[1]
    act, turn_send, turn_recv, local_sems = refs[:4]
    me = here.shard(0, 0)
    own_rows = pl.ds(pl.multiple_of(me * rows, rows), rows)

    def turn_copy(at):
        across, other = turned(at)
        first = pl.multiple_of(here.shard(across, other) * cols, cols)
        return remote(tokens.at[:, pl.ds(first, cols)], x_low.at[own_rows, :], turn_send.at[at], turn_recv.at[at],
                      here.device(across, other))

    wide = w_query.shape[1]
    local = [
        pltpu.make_async_copy(w_query, w_qkv.at[:, :wide], local_sems.at[0]),
        pltpu.make_async_copy(kv_weight, w_qkv.at[:, wide:], local_sems.at[1]),
        pltpu.make_async_copy(tokens.at[:, pl.ds(pl.multiple_of(me * cols, cols), cols)], x_low.at[own_rows, :],
                              local_sems.at[2]),
    ]
    for copy in local:
        copy.start()
    greet(here, slice_peers(here))
    for at in range(7):
        turn_copy(at).start()
    for copy in local:
        copy.wait()

    def squares(at, total):
        values = tokens[:, pl.ds(pl.multiple_of(at * cols, cols), cols)].astype(jnp.float32)
        return total + jnp.sum(values * values, axis=-1, keepdims=True)

    total = lax.fori_loop(0, 8, squares, jnp.zeros((rows, 1), jnp.float32))
    rms[...] = jnp.broadcast_to(lax.rsqrt(total / (8 * cols) + EPS), rms.shape)
    make_tables(here, rows, segs, cos, sin, mask)

    def prepare(first, count):
        def one(step, _):
            at = first + step
            span = row_span(here, *turned(at), rows)
            value = (x_low[span, :].astype(jnp.float32) * gain[...]).astype(act.dtype)
            act[span, :] = value
            return 0

        lax.fori_loop(0, count, one, 0)

    def before(stop):
        first, count = ((0, 2), (2, 4), (6, 2))[stop]
        for at in range(first, min(first + count, 7)):
            turn_copy(at).wait_recv()
        prepare(first, count)

    def flip():
        def one(shard, _):
            span = pl.ds(pl.multiple_of(shard * rows, rows), rows)
            act_t[:, span] = act[span, :].T
            return 0

        lax.fori_loop(0, 8, one, 0)

    product = products(here, act, w_qkv, False, rows, width, counts)
    total = Reduce(here, counts, product, refs[4:15], before)
    total.run()
    flip()

    def emit(at, first, second):
        for half, value in enumerate((first, second)):
            qkv[:, pl.ds(pl.multiple_of((half * counts + at) * width, width), width)] = value

    total.end(emit)
    for at in range(7):
        turn_copy(at).wait_send()


def opening(tokens, gain, w_query, kv_weight, segs, cid, width=256):
    rows = tokens.shape[0]
    cols, wide = w_query.shape
    every = wide + kv_weight.shape[1]
    counts = every // (2 * width)
    low, f32 = jnp.bfloat16, jnp.float32
    dma = pltpu.SemaphoreType.DMA
    vm = pl.BlockSpec(memory_space=pltpu.VMEM)
    hbm = pl.BlockSpec(memory_space=pl.ANY)
    out_shape = [
        jax.ShapeDtypeStruct((rows, every), f32),
        jax.ShapeDtypeStruct((8 * rows, cols), low),
        jax.ShapeDtypeStruct((cols, 8 * rows), low),
        jax.ShapeDtypeStruct((cols, every), low),
        jax.ShapeDtypeStruct((rows, LANES), f32),
        jax.ShapeDtypeStruct((2, rows, LANES), f32),
        jax.ShapeDtypeStruct((2, rows, LANES), f32),
        jax.ShapeDtypeStruct((rows, 2 * rows), f32),
    ]
    scratch = [pltpu.VMEM((8 * rows, cols), low), dma((7,)), dma((7,)), dma((3,))]
    scratch += reduce_scratch(counts, rows, width)
    kernel = functools.partial(open_kernel, rows, width, counts)
    return kernel_call(kernel, out_shape, [tokens, gain, w_query, kv_weight, segs],
                       [vm, vm, hbm, hbm, vm], scratch, cid, "open")


def scatter_kernel(rows, width, counts, line_counts, act, weight, line_own, out, line_out, *refs):
    here = Place()
    line = Line(here, line_counts, [line_own, line_out] + list(refs[11:]))
    product = products(here, act, weight, True, rows, width, counts)
    total = Reduce(here, counts, product, refs[:11])
    greet(here, slice_peers(here), True)
    line.begin()
    done = total.run(line.step)
    line.end(done)

    def emit(at, first, second):
        for half, value in enumerate((first, second)):
            out[:, pl.ds(pl.multiple_of((half * counts + at) * width, width), width)] = value

    total.end(emit)


def scatter_product(act, weight, width, cid, line, line_counts=16):
    rows = act.shape[0] // 8
    every = weight.shape[0]
    counts = every // (2 * width)
    vm = pl.BlockSpec(memory_space=pltpu.VMEM)
    out_shape = [
        jax.ShapeDtypeStruct((rows, every), jnp.float32),
        jax.ShapeDtypeStruct(line.shape, line.dtype),
    ]
    scratch = reduce_scratch(counts, rows, width) + line_scratch(line_counts, line.shape, line.dtype)
    kernel = functools.partial(scatter_kernel, rows, width, counts, line_counts)
    return kernel_call(kernel, out_shape, [act, weight, line], [vm] * 3, scratch, cid, "scatter_product")


def ffn_kernel(rows, width, counts, x_low, attn, gain, w_gate, w_up, d_hidden, hidden, d_gate, d_up, act_t, tile_out,
               *refs):
    here = Place()
    cols = gain.shape[1]
    act, weight, tiny_own, tiny_all, tiny_send, tiny_recv, dots, local_sems = refs[:8]
    tiny = Tiny(here, tiny_own, tiny_all, (tiny_send, tiny_recv), True)
    half_cols = counts * width
    local = [
        pltpu.make_async_copy(w_gate, weight.at[:, :half_cols], local_sems.at[0]),
        pltpu.make_async_copy(w_up, weight.at[:, half_cols:], local_sems.at[1]),
    ]
    for copy in local:
        copy.start()
    eye = diagonal()
    tiny_own[...] = jnp.zeros_like(tiny_own)

    def prepare(shard, _):
        for at in range(rows // LANES):
            span = pl.ds(pl.multiple_of(shard * rows + at * LANES, LANES), LANES)
            resid = x_low[span, :].astype(jnp.float32) + attn[span, :].astype(jnp.float32)
            act[span, :] = (resid * gain[...]).astype(act.dtype)
            square = jnp.sum(resid * resid, axis=-1, keepdims=True)
            tiny_own[shard, at : at + 1, :] = jnp.sum(square * eye, axis=0, keepdims=True)
        return 0

    lax.fori_loop(0, 8, prepare, 0)
    greet(here, slice_peers(here))
    tiny.begin()
    for copy in local:
        copy.wait()
    product = products(here, act, weight, False, rows, width, counts)
    total = Reduce(here, counts, product, refs[8:19])
    total.run()

    def flip(shard, _):
        span = pl.ds(pl.multiple_of(shard * rows, rows), rows)
        act_t[:, span] = act[span, :].T
        return 0

    lax.fori_loop(0, 8, flip, 0)
    tiny.end()
    tiles = rows // LANES
    mean = [from_tile(jnp.sum(tiny_all[:, at, :], axis=0, keepdims=True), eye) for at in range(tiles)]
    scale = lax.rsqrt(jnp.concatenate(mean, axis=0) / (8 * cols) + EPS)
    dots[...] = jnp.zeros_like(dots)
    coeff = math.sqrt(2.0 / math.pi)

    def emit(at, first, second):
        span = pl.ds(pl.multiple_of(at * width, width), width)
        gate, up = first * scale, second * scale
        inner = jnp.tanh(coeff * (gate + 0.044715 * (gate * gate * gate)))
        gelu = 0.5 * gate * (1.0 + inner)
        slope = 0.5 * (1.0 + inner) + 0.5 * gate * (1.0 - inner * inner) * (
            coeff * (1.0 + 3.0 * 0.044715 * gate * gate))
        cot = d_hidden[:, span]
        hidden[:, span] = (gelu * up).astype(hidden.dtype)
        back_gate, back_up = cot * up * slope, cot * gelu
        d_gate[:, span] = (back_gate * scale).astype(d_gate.dtype)
        d_up[:, span] = (back_up * scale).astype(d_up.dtype)
        dots[...] += jnp.sum(back_gate * gate + back_up * up, axis=-1, keepdims=True)

    total.end(emit)
    tile_out[...] = jnp.zeros_like(tile_out)
    to_tile(tile_out, 0, dots[...] * (scale * scale * (1.0 / (8 * cols))), eye)


def ffn_scatter(x_low, attn, gain, w_gate, w_up, d_hidden, cid, width=512):
    rows, half = d_hidden.shape
    cols = gain.shape[1]
    counts = half // width
    low, f32 = jnp.bfloat16, jnp.float32
    dma = pltpu.SemaphoreType.DMA
    vm = pl.BlockSpec(memory_space=pltpu.VMEM)
    hbm = pl.BlockSpec(memory_space=pl.ANY)
    out_shape = [jax.ShapeDtypeStruct((rows, half), low)] * 3 + [
        jax.ShapeDtypeStruct((cols, 8 * rows), low),
        jax.ShapeDtypeStruct((8, LANES), f32),
    ]
    scratch = [
        pltpu.VMEM((8 * rows, cols), low),
        pltpu.VMEM((cols, 2 * half), low),
        pltpu.VMEM((8, 8, LANES), f32),
        pltpu.VMEM((8, 8, LANES), f32),
        dma((7,)), dma((7,)),
        pltpu.VMEM((rows, 1), f32),
        dma((2,)),
    ] + reduce_scratch(counts, rows, width)
    kernel = functools.partial(ffn_kernel, rows, width, counts)
    return kernel_call(kernel, out_shape, [x_low, attn, gain, w_gate, w_up, d_hidden], [vm, vm, vm, hbm, hbm, vm],
                       scratch, cid, "ffn")


def load_own(spread, payload, width, counts, sems):
    copies = []
    for half in range(2):
        for at in range(counts):
            first = at * width + (half * counts * width if len(payload) == 1 else 0)
            src = payload[half % len(payload)].at[:, first : first + width]
            copies.append(pltpu.make_async_copy(src, spread.slot(0, half, at), sems.at[half, at]))
    return copies


def back_kernel(rows, width, counts, act_t, w_gate, w_up, d_gate, d_up, dots, x_low, attn, gain, contrib, gain_grad,
                grad_gate, grad_up, *refs):
    here = Place()
    spread = Spread(here, counts, refs[:7])
    tiny_all, tiny_send, tiny_recv, own_sems, weight, sums, grads, staged, local_sems, out_sems = refs[7:17]
    tiny = Tiny(here, dots, tiny_all, (tiny_send, tiny_recv), False)
    half_cols = counts * width
    local = [
        pltpu.make_async_copy(w_gate, weight.at[:, :half_cols], local_sems.at[0]),
        pltpu.make_async_copy(w_up, weight.at[:, half_cols:], local_sems.at[1]),
    ]
    own = load_own(spread, (d_gate, d_up), width, counts, own_sems)
    for copy in own + local:
        copy.start()
    greet(here, tiny.peers)
    for copy in own:
        copy.wait()
    spread.begin()
    tiny.begin()
    sums[...] = jnp.zeros_like(sums)
    for copy in local:
        copy.wait()

    def columns(half, at):
        return pl.ds(pl.multiple_of((half * counts + at) * width, width), width)

    def clear(at, _):
        grads[:, columns(0, at)] = jnp.zeros((grads.shape[0], width), jnp.float32)
        return 0

    lax.fori_loop(0, 2 * counts, clear, 0)

    def blocks(across, half, at):
        cols = columns(half, at)
        gained = grads[:, cols]
        for other in range(2):
            row = row_span(here, across, other, rows)
            block = spread.got[across, (spread.core + other) % 2, half, at]
            sums[row, :] += dot_nt(block, weight[:, cols])
            gained = gained + dot_nn(act_t[:, row], block)
        grads[:, cols] = gained

    def leave(half, at):
        spot = pl.ds(pl.multiple_of(at * width, width), width)
        return pltpu.make_async_copy(staged.at[at % 2, half], (grad_gate, grad_up)[half].at[:, spot],
                                     out_sems.at[half, at])

    def done(stage, at):
        @pl.when(jnp.logical_and(stage == 3, at > 1))
        def _():
            leave(0, at - 2).wait()
            leave(1, at - 2).wait()

        @pl.when(stage == 3)
        def _():
            for half in range(2):
                staged[at % 2, half] = grads[:, columns(half, at)].astype(staged.dtype)
            leave(0, at).start()
            leave(1, at).start()

    spread.run(blocks, done=done)
    tiny.end()
    eye = diagonal()
    gain_grad[...] = jnp.zeros_like(gain_grad)

    def close_shard(shard, _):
        for at in range(rows // LANES):
            span = pl.ds(pl.multiple_of(shard * rows + at * LANES, LANES), LANES)
            dot = from_tile(tiny_all[shard, at : at + 1, :], eye)
            resid = x_low[span, :].astype(jnp.float32) + attn[span, :].astype(jnp.float32)
            value = sums[span, :]
            contrib[span, :] = (value * gain[...] - resid * dot).astype(contrib.dtype)
            gain_grad[...] += jnp.sum(value * resid, axis=0, keepdims=True)
        return 0

    lax.fori_loop(0, 8, close_shard, 0)
    spread.end()

    def drain(at, _):
        leave(0, at).wait()
        leave(1, at).wait()
        return 0

    lax.fori_loop(counts - 2, counts, drain, 0)


def back_gather(act_t, w_gate, w_up, d_gate, d_up, dots, x_low, attn, gain, cid, width=512):
    cols, total = act_t.shape
    rows, half = d_gate.shape
    counts = half // width
    low, f32 = jnp.bfloat16, jnp.float32
    dma = pltpu.SemaphoreType.DMA
    vm = pl.BlockSpec(memory_space=pltpu.VMEM)
    hbm = pl.BlockSpec(memory_space=pl.ANY)
    out_shape = [
        jax.ShapeDtypeStruct((total, cols), low),
        jax.ShapeDtypeStruct((1, cols), f32),
        jax.ShapeDtypeStruct((cols, half), low),
        jax.ShapeDtypeStruct((cols, half), low),
    ]
    scratch = spread_scratch(counts, rows, width) + [
        pltpu.VMEM((8, 8, LANES), f32), dma((7,)), dma((7,)), dma((2, counts)),
        pltpu.VMEM((cols, 2 * half), low),
        pltpu.VMEM((total, cols), f32),
        pltpu.VMEM((cols, 2 * half), f32),
        pltpu.VMEM((2, 2, cols, width), low),
        dma((2,)), dma((2, counts)),
    ]
    operands = [act_t, w_gate, w_up, d_gate, d_up, dots, x_low, attn, gain]
    kernel = functools.partial(back_kernel, rows, width, counts)
    return kernel_call(kernel, out_shape, operands, [vm] + [hbm] * 4 + [vm] * 4, scratch, cid, "back",
                       [vm, vm, hbm, hbm])


def down_kernel(rows, width, counts, line_counts, cot, weight, hidden, line_own, ffn, d_attn, grad, *refs):
    here = Place()
    spread = Spread(here, counts, refs[:7])
    own_sems, sums, grads, staged, out_sems, line_out = refs[7:13]
    line = Line(here, line_counts, [line_own, line_out] + list(refs[13:]))
    own = load_own(spread, (hidden,), width, counts, own_sems)
    for copy in own:
        copy.start()
    greet(here, slice_peers(here), True)
    line.begin()
    for copy in own:
        copy.wait()
    spread.begin()
    sums[...] = jnp.zeros_like(sums)
    grads[...] = jnp.zeros_like(grads)

    def columns(half, at):
        return pl.ds(pl.multiple_of((half * counts + at) * width, width), width)

    def blocks(across, half, at):
        cols = columns(half, at)
        gained = grads[cols, :]
        for other in range(2):
            row = row_span(here, across, other, rows)
            block = spread.got[across, (spread.core + other) % 2, half, at]
            sums[row, :] += dot_nn(block, weight[cols, :])
            gained = gained + dot_tn(block, cot[row, :])
        grads[cols, :] = gained

    def leave(half, at):
        return pltpu.make_async_copy(staged.at[at % 2, half], grad.at[columns(half, at), :], out_sems.at[half, at])

    def done(stage, at):
        @pl.when(jnp.logical_and(stage == 3, at > 1))
        def _():
            leave(0, at - 2).wait()
            leave(1, at - 2).wait()

        @pl.when(stage == 3)
        def _():
            for half in range(2):
                staged[at % 2, half] = grads[columns(half, at), :].astype(staged.dtype)
            leave(0, at).start()
            leave(1, at).start()

    steps = spread.run(blocks, line.step, done)
    line.end(steps)

    def close_shard(shard, _):
        span = pl.ds(pl.multiple_of(shard * rows, rows), rows)
        ffn[span, :] = sums[span, :].astype(ffn.dtype)
        d_attn[span, :] = (cot[span, :].astype(jnp.float32) + line_out[span, :].astype(jnp.float32)).astype(
            d_attn.dtype)
        return 0

    lax.fori_loop(0, 8, close_shard, 0)
    spread.end()

    def drain(at, _):
        leave(0, at).wait()
        leave(1, at).wait()
        return 0

    lax.fori_loop(counts - 2, counts, drain, 0)


def down_gather(cot, weight, hidden, line, cid, width=256, line_counts=16):
    total, cols = cot.shape
    rows, every = hidden.shape
    counts = every // (2 * width)
    low, f32 = jnp.bfloat16, jnp.float32
    dma = pltpu.SemaphoreType.DMA
    vm = pl.BlockSpec(memory_space=pltpu.VMEM)
    hbm = pl.BlockSpec(memory_space=pl.ANY)
    out_shape = [
        jax.ShapeDtypeStruct((total, cols), low),
        jax.ShapeDtypeStruct((total, cols), low),
        jax.ShapeDtypeStruct(weight.shape, low),
    ]
    scratch = spread_scratch(counts, rows, width) + [
        dma((2, counts)),
        pltpu.VMEM((total, cols), f32),
        pltpu.VMEM(weight.shape, f32),
        pltpu.VMEM((2, 2, width, cols), low),
        dma((2, counts)),
        pltpu.VMEM((total, cols), low),
    ] + line_scratch(line_counts, line.shape, low)
    kernel = functools.partial(down_kernel, rows, width, counts, line_counts)
    return kernel_call(kernel, out_shape, [cot, weight, hidden, line], [vm, vm, hbm, vm], scratch, cid, "down",
                       [vm, vm, hbm])


def attend_kernel(rows, heads, cols, qkv, rms, cos, sin, mask, w_out, cot, part, mixed_all, g_col, kv, probs, queries,
                  pair_rms, *refs):
    here = Place()
    spread = Spread(here, heads // 2, refs[:7])
    sums, pair_sems, turn_send, turn_recv, local_sem, tiny_own, tiny_pair = refs[7:14]
    got, core = spread.got, here.core
    greet(here, slice_peers(here))
    me = here.shard(0, 0)

    def turn_copy(at):
        across, other = turned(at)
        first = pl.multiple_of(here.shard(across, other) * cols, cols)
        return remote(cot.at[:, pl.ds(first, cols)], g_col.at[pl.ds(pl.multiple_of(me * rows, rows), rows), :],
                      turn_send.at[at], turn_recv.at[at], here.device(across, other))

    own_turn = pltpu.make_async_copy(cot.at[:, pl.ds(pl.multiple_of(me * cols, cols), cols)],
                                     g_col.at[pl.ds(pl.multiple_of(me * rows, rows), rows), :], local_sem)
    own_turn.start()
    half = HD // 2
    scale = 1.0 / math.sqrt(HD)
    wide = heads * HD

    def rotated(first):
        lead = qkv[:, first : first + half] * rms[...]
        trail = qkv[:, first + half : first + HD] * rms[...]
        return lead * cos[0] - trail * sin[0], trail * cos[0] + lead * sin[0]

    low_k, high_k = rotated(wide)
    kv[0, :, :half] = low_k.astype(kv.dtype)
    kv[0, :, half:HD] = high_k.astype(kv.dtype)
    for at in range(2):
        first = HD + at * half
        kv[0, :, first : first + half] = (qkv[:, wide + first : wide + first + half] * rms[...]).astype(kv.dtype)
    eye = diagonal()
    tiny_own[...] = jnp.zeros_like(tiny_own)
    to_tile(tiny_own, 0, rms[:, :1], eye)
    pair_rms[0] = rms[...]
    pair = remote(kv.at[0], kv.at[1], pair_sems.at[0], pair_sems.at[1], spread.ydev)
    tiny = remote(tiny_own, tiny_pair, pair_sems.at[2], pair_sems.at[3], spread.ydev)
    for head in range(heads):
        if head == 1:
            pair.start()
            tiny.start()
            turn_copy(2 * (3 - 1)).start()
            turn_copy(2 * (3 - 1) + 1).start()
        lead, trail = rotated(head * HD)
        queries[:, head * HD : head * HD + half] = (lead * scale).astype(queries.dtype)
        queries[:, head * HD + half : (head + 1) * HD] = (trail * scale).astype(queries.dtype)
    pair.wait()
    for at in range(7):
        if at // 2 != 2:
            turn_copy(at).start()

    def one_head(head, _):
        query = queries[:, pl.ds(pl.multiple_of(head * HD, HD), HD)]
        scores = jnp.concatenate([dot_nt(query, kv[0, :, :HD]), dot_nt(query, kv[1, :, :HD])], axis=1)
        scores = jnp.where(mask[...] > 0, scores, NEG)
        expd = jnp.exp(scores - jnp.max(scores, axis=-1, keepdims=True))
        prob = expd / jnp.sum(expd, axis=-1, keepdims=True)
        probs[head] = prob
        prob_low = prob.astype(jnp.bfloat16)
        mixed = dot_nn(prob_low[:, :rows], kv[0, :, HD:]) + dot_nn(prob_low[:, rows:], kv[1, :, HD:])
        got[0, core, head // (heads // 2), head % (heads // 2)] = mixed.astype(got.dtype)
        return 0

    lax.fori_loop(0, heads, one_head, 0)
    sums[...] = jnp.zeros_like(sums)
    spread.begin()

    def blocks(across, half_at, at):
        span = pl.ds(pl.multiple_of((half_at * (heads // 2) + at) * HD, HD), HD)
        for other in range(2):
            row = row_span(here, across, other, rows)
            block = got[across, (core + other) % 2, half_at, at]
            mixed_all[row, span] = block
            sums[row, :] += dot_nn(block, w_out[span, :])

    spread.run(blocks)
    part[...] = sums[...].astype(part.dtype)
    spread.end()
    tiny.wait()
    for at in range(rows // LANES):
        values = jnp.broadcast_to(from_tile(tiny_pair[at : at + 1, :], eye), (LANES, LANES))
        pair_rms[1, at * LANES : (at + 1) * LANES, :] = values
    own_turn.wait()
    for at in range(7):
        turn_copy(at).wait()


def attend(qkv, rms, cos, sin, mask, w_out, cot, cid):
    rows = qkv.shape[0]
    wide, cols = w_out.shape
    heads = wide // HD
    low, f32 = jnp.bfloat16, jnp.float32
    dma = pltpu.SemaphoreType.DMA
    vm = pl.BlockSpec(memory_space=pltpu.VMEM)
    out_shape = [
        jax.ShapeDtypeStruct((8 * rows, cols), low),
        jax.ShapeDtypeStruct((8 * rows, wide), low),
        jax.ShapeDtypeStruct((8 * rows, cols), low),
        jax.ShapeDtypeStruct((2, rows, 2 * HD), low),
        jax.ShapeDtypeStruct((heads, rows, 2 * rows), f32),
        jax.ShapeDtypeStruct((rows, wide), low),
        jax.ShapeDtypeStruct((2,) + rms.shape, f32),
    ]
    scratch = spread_scratch(heads // 2, rows, HD) + [
        pltpu.VMEM((8 * rows, cols), f32), dma((4,)), dma((7,)), dma((7,)), dma(()),
        pltpu.VMEM((8, LANES), f32), pltpu.VMEM((8, LANES), f32)]
    kernel = functools.partial(attend_kernel, rows, heads, cols)
    return kernel_call(kernel, out_shape, [qkv, rms, cos, sin, mask, w_out, cot], [vm] * 7, scratch, cid,
                       "attend")


def tail_kernel(rows, heads, per, d_attn, w_out, queries, kv, probs, rms, cos, sin, act_t, w_qkv, ffn, x_low,
                attn, gain, gain_grad, mixed_all, d_tok, out, grad_query, grad_out, kv_sum, gain_tiles, *refs):
    here = Place()
    width = HD
    counts = heads // 2
    part = rows // 2
    refs = list(refs)
    line_counts = 8 * per
    cols = d_attn.shape[1]
    extra = cols // (rows // per)

    def take(count):
        taken_refs = refs[:count]
        del refs[:count]
        return taken_refs

    total_refs = take(11)
    spread = Spread(here, 1, take(7))
    d_mixed, tiny_own, tiny_all, d_kv, give, taken, give_sems, tiny_send, tiny_recv = take(9)
    grad, grad_mixed, gain_sum, tile, tile_send, tile_recv, put_sems, local_sems, mixed_two, mixed_sems = take(10)

    def far(at):
        return turned(at // per)

    def near(at):
        at = jnp.minimum(at, line_counts - 1)
        x_stream, y_stream = spread.streams(at // 4)
        second = at // 2 % 2
        across = x_stream[0] + second * (y_stream[0] - x_stream[0])
        half_at = x_stream[1] + second * (y_stream[1] - x_stream[1])
        return across, at % 2, half_at

    def place_ffn(at):
        return here.shard(*far(at)) * per + at % per

    def place_tok(at):
        across, other, half_at = near(at)
        return jnp.where(at < line_counts, here.shard(across, other) * per + half_at, at)

    ffn_sum = take(1)[0]
    line = Line(here, line_counts, [ffn, ffn_sum] + take(8), place_ffn)
    contrib, summed = take(2)
    line_tok = Line(here, line_counts + extra, [contrib, summed] + take(8), place_tok)
    tiny = Tiny(here, tiny_own, tiny_all, (tiny_send, tiny_recv), False)
    got, core = spread.got, here.core
    product = products(here, d_attn, w_out, True, rows, width, counts)
    total = Reduce(here, counts, product, total_refs)
    greet(here, tiny.peers, True)
    line.begin()
    grad_mixed[...] = jnp.zeros_like(grad_mixed)

    def mixed_copy(step):
        span = pl.ds(pl.multiple_of(step * rows, rows), rows)
        return pltpu.make_async_copy(mixed_all.at[span, :], mixed_two.at[step % 2], mixed_sems.at[step % 2])

    mixed_copy(0).start()

    def beside(step):
        line.step(step)

        @pl.when(step < 8)
        def _():
            span = pl.ds(pl.multiple_of(step * rows, rows), rows)
            mixed_copy(step).wait()

            @pl.when(step < 7)
            def _():
                mixed_copy(step + 1).start()

            grad_mixed[...] += dot_tn(mixed_two[step % 2], d_attn[span, :])

    done = total.run(beside)
    grad_out[...] = grad_mixed[...].astype(grad_out.dtype)

    def land(at, first, second):
        for half_at, value in enumerate((first, second)):
            d_mixed[:, pl.ds(pl.multiple_of((half_at * counts + at) * width, width), width)] = value.astype(
                d_mixed.dtype)

    total.end(land)
    half = HD // 2
    scale = 1.0 / math.sqrt(HD)
    depth = w_qkv.shape[0] * 8
    d_kv[...] = jnp.zeros_like(d_kv)

    def one_head(head, dots):
        span = pl.ds(pl.multiple_of(head * HD, HD), HD)
        query = queries[:, span]
        cot = d_mixed[:, span]
        prob = probs[head]
        d_prob = jnp.concatenate([dot_nt(cot, kv[0, :, HD:]), dot_nt(cot, kv[1, :, HD:])], axis=1)
        delta = jnp.sum(prob * d_prob, axis=-1, keepdims=True)
        d_score = (prob * (d_prob - delta)).astype(jnp.bfloat16)
        prob_low = prob.astype(jnp.bfloat16)
        d_query = (dot_nn(d_score[:, :rows], kv[0, :, :HD]) + dot_nn(d_score[:, rows:], kv[1, :, :HD])) * scale
        for side in range(2):
            keys = slice(side * rows, (side + 1) * rows)
            d_kv[side, :, :HD] += dot_tn(d_score[:, keys], query)
            d_kv[side, :, HD:] += dot_tn(prob_low[:, keys], cot)
        dots = dots + jnp.sum(d_query * query.astype(jnp.float32), axis=-1, keepdims=True)
        lead, trail = d_query[:, :half], d_query[:, half:]
        first = ((lead * cos[0] + trail * sin[0]) * rms[0]).astype(got.dtype)
        second = ((trail * cos[0] - lead * sin[0]) * rms[0]).astype(got.dtype)
        for rows_at in range(2):
            piece = slice(rows_at * part, (rows_at + 1) * part)
            got[0, core, rows_at, 0, :, pl.ds(pl.multiple_of(head * HD, HD), half)] = first[piece, :]
            got[0, core, rows_at, 0, :, pl.ds(pl.multiple_of(head * HD + half, half), half)] = second[piece, :]

        line.step(done + head)
        return dots

    dots = lax.fori_loop(0, heads, one_head, jnp.zeros((rows, 1), jnp.float32))
    done += heads
    eye = diagonal()
    tiny_own[...] = jnp.zeros_like(tiny_own)
    for side in (1, 0):
        d_key, d_value = d_kv[side, :, :HD], d_kv[side, :, HD:]
        own = jnp.sum(d_key * kv[side, :, :HD].astype(jnp.float32) +
                      d_value * kv[side, :, HD:].astype(jnp.float32), axis=-1, keepdims=True)
        if side == 0:
            own = own + dots * (1.0 / scale)
        own = own * (rms[side] * rms[side] * (1.0 / depth))
        to_tile(tiny_own, side * (rows // LANES), own, eye)
        lead, trail = d_key[:, :half], d_key[:, half:]
        parts = [(lead * cos[side] + trail * sin[side]) * rms[side],
                 (trail * cos[side] - lead * sin[side]) * rms[side],
                 d_value[:, :half] * rms[side], d_value[:, half:] * rms[side]]
        for at, value in enumerate(parts):
            if side == 1:
                give[:, at * half : (at + 1) * half] = value.astype(give.dtype)
            else:
                d_kv[0, :, at * half : (at + 1) * half] = value
    given = remote(give, taken, give_sems.at[0], give_sems.at[1], spread.ydev)
    given.start()
    grad[...] = jnp.zeros_like(grad)
    given.wait()
    for rows_at in range(2):
        piece = slice(rows_at * part, (rows_at + 1) * part)
        value = d_kv[0, piece, :] + taken[piece, :].astype(jnp.float32)
        got[0, core, rows_at, 0, :, heads * HD :] = value.astype(got.dtype)
    tiny.begin()
    for hop in range(2):
        spread.x_copy(hop, 0).start()
        spread.y_copy(hop, 0).start()
    for stream in range(2):
        spread.sib_copy(0, stream, 0).start()
    gain_sum[...] = jnp.zeros_like(gain_sum)
    line.steps(done, line_counts + 2)
    tiny.end()

    def block_of(at):
        across, other, half_at = near(at)
        shard, partner = here.shard(across, other), here.shard((across + 2) % 4, other)
        block = got[across, (core + other) % 2, half_at, 0]
        first = pl.multiple_of(shard * rows + half_at * part, part)
        for tile_at in range(part // LANES):
            row = pl.ds(pl.multiple_of(first + tile_at * LANES, LANES), LANES)
            low_at = half_at * (part // LANES) + tile_at
            kept = rows // LANES + low_at
            dot = from_tile(tiny_all[shard, pl.ds(low_at, 1), :] + tiny_all[partner, pl.ds(kept, 1), :], eye)
            value = dot_nt(block[tile_at * LANES : (tile_at + 1) * LANES, :], w_qkv[...])
            x_rows = x_low[row, :].astype(jnp.float32)
            contrib[row, :] = (value * gain[...] - x_rows * dot).astype(contrib.dtype)
            gain_sum[...] += jnp.sum(value * x_rows, axis=0, keepdims=True)
        line_tok.launch(at, 1)
        rows_t = act_t[:, pl.ds(first, part)]
        for at_col in range((heads + 2) * HD // 512):
            span = slice(at_col * 512, (at_col + 1) * 512)
            grad[:, span] += dot_nn(rows_t, block[:, span])

    def stage_step(step, _):
        stage = step // 4

        @pl.when(jnp.logical_and(step % 4 == 0, jnp.logical_and(stage > 0, stage < 4)))
        def _():
            spread.x_copy(stage - 1, 0).wait_recv()
            spread.sib_copy(stage, 0, 0).start()
            spread.y_copy(stage - 1, 0).wait_recv()
            spread.sib_copy(stage, 1, 0).start()

        @pl.when(step == 4)
        def _():
            spread.x_copy(2, 0).start()
            spread.y_copy(2, 0).start()

        @pl.when(step < line_counts)
        def _():
            for stream in range(2):
                @pl.when(step % 4 == 2 * stream)
                def _(stream=stream):
                    spread.sib_copy(stage, stream, 0).wait_recv()

            block_of(step)

        @pl.when(step >= 4)
        def _():
            line_tok.step(step - 4)
        return 0

    lax.fori_loop(0, line_counts, stage_step, 0)
    for half_at in range(cols // (rows // per)):
        span = pl.ds(line_counts * (rows // per) + half_at * (rows // per), rows // per)
        source = slice(half_at * (rows // per), (half_at + 1) * (rows // per))
        contrib[span, :] = grad[source, heads * HD :].astype(contrib.dtype)
    line_tok.launch(line_counts, extra)
    grad_query[...] = grad[:, : heads * HD].astype(grad_query.dtype)
    for at in range(cols // LANES):
        tile[at : at + 1, :] = gain_sum[:, at * LANES : (at + 1) * LANES]
        spot = cols // LANES + at
        tile[spot : spot + 1, :] = gain_grad[:, at * LANES : (at + 1) * LANES]

    def tile_copy(step):
        return remote(tile, gain_tiles.at[here.z], tile_send.at[step], tile_recv.at[step],
                      (here.dp, here.seq, (here.z + step + 1) % 4))

    line.settle()
    me = here.shard(0, 0)
    columns = pl.ds(pl.multiple_of(me * cols, cols), cols)
    chunk = line.chunk

    def landing(which, at):
        sub = at % per if which == 0 else near(at)[2]
        return (out, d_tok)[which].at[pl.ds(pl.multiple_of(sub * chunk, chunk), chunk), columns]

    def put(which, at):
        kind = (line, line_tok)[which]
        goal = here.device(*(far(at) if which == 0 else near(at)[:2]))
        return remote(kind.from_end.at[at], landing(which, at), put_sems.at[which, 0, at], put_sems.at[which, 1, at],
                      goal)

    def keep(which, at):
        spot = at % per if which == 0 else near(at)[2]
        return pltpu.make_async_copy((line, line_tok)[which].from_end.at[at], landing(which, at),
                                     local_sems.at[which, spot])

    def emit(which, at):
        kind = (line, line_tok)[which]
        row = kind.rows(at)
        base = (attn, d_attn)[which][row, :].astype(jnp.float32)
        if which == 0:
            base = base + x_low[row, :].astype(jnp.float32)
        kind.from_end[at] = (base + kind.out[row, :].astype(jnp.float32)).astype(out.dtype)

    def is_own(which, at):
        return at >= 7 * per if which == 0 else jnp.logical_and(at < 4, at % 2 == 0)

    def send(which, at):
        own = is_own(which, at)

        @pl.when(own)
        def _():
            keep(which, at).start()

        @pl.when(jnp.logical_not(own))
        def _():
            put(which, at).start()

    for step in range(3):
        tile_copy(step).start()
    gain_tiles[here.z] = tile[...]

    @pl.when(line.inner == 1)
    def _():
        start = line_counts - 4

        def both(at, _):
            line_tok.step(at)
            spot = at - start

            @pl.when(jnp.logical_and(spot > 0, spot <= line_counts // 2))
            def _():
                for which in range(2):
                    for last in range(2):
                        send(which, 2 * spot - 2 + last)

            @pl.when(spot < line_counts // 2)
            def _():
                for which in range(2):
                    for last in range(2):
                        emit(which, 2 * spot + last)
            return 0

        lax.fori_loop(start, line_counts + extra + 2, both, 0)

        def drain(at, _):
            line_tok.down(at).wait_send()
            return 0

        lax.fori_loop(0, line_counts + extra, drain, 0)

    @pl.when(line.inner == 0)
    def _():
        def arrive(at, _):
            line_tok.up(at).wait_send()
            line_tok.down(at).wait_recv()

            @pl.when(jnp.logical_and(at > 0, at <= line_counts))
            def _():
                send(0, at - 1)
                send(1, at - 1)

            @pl.when(at < line_counts)
            def _():
                emit(0, at)
                emit(1, at)
            return 0

        lax.fori_loop(0, line_counts + extra, arrive, 0)

    for half_at in range(extra):
        span = pl.ds((line_counts + half_at) * chunk, chunk)
        kv_sum[half_at * chunk : (half_at + 1) * chunk, :] = summed[span, :]
    for hop in range(3):
        spread.x_copy(hop, 0).wait_send()
        spread.y_copy(hop, 0).wait_send()
    for stage in range(4):
        spread.sib_copy(stage, 0, 0).wait_send()
        spread.sib_copy(stage, 1, 0).wait_send()

    def finish(at, _):
        for which in range(2):
            own = is_own(which, at)

            @pl.when(own)
            def _():
                keep(which, at).wait()

            @pl.when(jnp.logical_not(own))
            def _():
                put(which, at).wait()
        return 0

    lax.fori_loop(0, line_counts, finish, 0)
    for step in range(3):
        tile_copy(step).wait()


def tail(d_attn, w_out, queries, kv, probs, rms, cos, sin, act_t, w_qkv, ffn, x_low, attn, gain, gain_grad,
         mixed_all, cid,
 per=2):
    total, cols = d_attn.shape
    rows = total // 8
    wide = w_out.shape[0]
    heads = wide // HD
    low, f32 = jnp.bfloat16, jnp.float32
    dma = pltpu.SemaphoreType.DMA
    vm = pl.BlockSpec(memory_space=pltpu.VMEM)
    counts = 8 * per
    chunk = rows // per
    extra = cols // chunk
    long = (total + cols, cols)
    out_shape = [
        jax.ShapeDtypeStruct((rows, 8 * cols), low),
        jax.ShapeDtypeStruct((rows, 8 * cols), low),
        jax.ShapeDtypeStruct((cols, wide), low),
        jax.ShapeDtypeStruct(w_out.shape, low),
        jax.ShapeDtypeStruct((cols, 2 * HD), low),
        jax.ShapeDtypeStruct((4, 8, LANES), f32),
    ]
    scratch = reduce_scratch(heads // 2, rows, HD, 2) + spread_scratch(1, rows // 2, wide + 2 * HD)
    scratch += [
        pltpu.VMEM((rows, wide), low),
        pltpu.VMEM((8, LANES), f32),
        pltpu.VMEM((8, 8, LANES), f32),
        pltpu.VMEM((2, rows, 2 * HD), f32),
        pltpu.VMEM((rows, 2 * HD), low),
        pltpu.VMEM((rows, 2 * HD), low),
        dma((2,)), dma((7,)), dma((7,)),
        pltpu.VMEM(w_qkv.shape, f32),
        pltpu.VMEM(w_out.shape, f32),
        pltpu.VMEM((1, cols), f32),
        pltpu.VMEM((8, LANES), f32),
        dma((3,)), dma((3,)), dma((2, 2, counts)), dma((2, per)),
        pltpu.VMEM((2, rows, wide), low), dma((2,)),
        pltpu.VMEM((total, cols), low),
    ] + line_scratch(counts, (total, cols), low)
    scratch += [pltpu.VMEM(long, low), pltpu.VMEM(long, low)] + line_scratch(counts + extra, long, low)
    operands = [d_attn, w_out, queries, kv, probs, rms, cos, sin, act_t, w_qkv, ffn, x_low, attn, gain,
                gain_grad, mixed_all]
    kernel = functools.partial(tail_kernel, rows, heads, per)
    specs = [vm] * (len(operands) - 1) + [pl.BlockSpec(memory_space=pl.ANY)]
    return kernel_call(kernel, out_shape, operands, specs, scratch, cid, "tail")


LANES = 128


def acts_move(
    tokens, seg_ids, gain_attn, w_query, kv_weight, w_out, gain_ffn, w_gate, w_up, w_down, d_out
):
    rows = tokens.shape[0]
    segs = seg_ids.astype(jnp.float32).reshape(2 * rows // LANES, LANES)
    segs = jnp.pad(segs, ((0, 8 - 2 * rows // LANES), (0, 0)))
    gain_one = gain_attn.astype(jnp.float32)[None, :]
    gain_two = gain_ffn.astype(jnp.float32)[None, :]
    wider = jnp.float32

    qkv, x_low, act_one_t, w_qkv, rms, cos, sin, mask = opening(
        tokens, gain_one, w_query, kv_weight, segs, 1
    )
    attn_part, mixed_all, g_low, kv, probs, queries, pair_rms = attend(
        qkv, rms, cos, sin, mask, w_out, d_out, 2
    )
    d_hidden, attn = scatter_product(g_low, w_down, 512, 3, attn_part)
    hidden, d_gate, d_up, act_two_t, dots = ffn_scatter(x_low, attn, gain_two, w_gate, w_up, d_hidden, 4)
    contrib, grad_gain_two, grad_gate, grad_up = back_gather(
        act_two_t, w_gate, w_up, d_gate, d_up, dots, x_low, attn, gain_two, 5
    )
    ffn, d_attn, grad_down = down_gather(g_low, w_down, hidden, contrib, 6)
    d_tokens, out, grad_query, grad_out, grad_kv, gain_tiles = tail(
        d_attn,
        w_out,
        queries,
        kv,
        probs,
        pair_rms,
        cos,
        sin,
        act_one_t,
        w_qkv,
        ffn,
        x_low,
        attn,
        gain_one,
        grad_gain_two,
        mixed_all,
        7,
    )
    gains = jnp.sum(gain_tiles, axis=0).reshape(2, -1)
    return (
        out,
        d_tokens.astype(wider),
        gains[0],
        grad_query.astype(wider),
        grad_kv.astype(wider),
        grad_out.astype(wider),
        gains[1],
        grad_gate.astype(wider),
        grad_up.astype(wider),
        grad_down.astype(wider),
    )


def solution(mesh):
    in_specs = (
        P(("dp", "seq"), None),
        P("dp"),
        P(("dp", "seq")),
        P(("dp", "seq"), "tensor"),
        P(("dp", "seq"), None),
        P("tensor", ("dp", "seq")),
        P(("dp", "seq")),
        P(("dp", "seq"), "tensor"),
        P(("dp", "seq"), "tensor"),
        P("tensor", ("dp", "seq")),
        P(("dp", "seq"), None),
    )
    out_specs = (
        P(("dp", "seq"), None),
        P(("dp", "seq"), None),
        P(("dp", "seq")),
        P(("dp", "seq"), "tensor"),
        P(("dp", "seq"), None),
        P("tensor", ("dp", "seq")),
        P(("dp", "seq")),
        P(("dp", "seq"), "tensor"),
        P(("dp", "seq"), "tensor"),
        P("tensor", ("dp", "seq")),
    )

    def shards(*arrays):
        tokens = arrays[0]
        sizes = tuple(mesh.shape[name] for name in ("dp", "seq", "tensor"))
        count = tokens.shape[0] * sizes[0] * sizes[1]
        plan = acts_move if sizes == (4, 2, 4) and count <= tokens.shape[1] else weights_move
        return plan(*arrays)

    return jax.shard_map(shards, mesh=mesh, in_specs=in_specs, out_specs=out_specs, check_vma=False)
```

```python
import functools
import math

import jax
import jax.numpy as jnp
from jax import lax
from jax.experimental import pallas as pl
from jax.experimental.pallas import tpu as pltpu
from jax.sharding import PartitionSpec as P

HD = 256


EPS = 1e-06
NEG = -1e30


def place_tables(segs):
    length = segs.shape[0]
    index = jnp.arange(length, dtype=jnp.int32)
    flags = jnp.concatenate([jnp.ones((1,), dtype=bool), segs[1:] != segs[:-1]])
    starts = lax.cummax(jnp.where(flags, index, jnp.zeros_like(index)), axis=0)
    places = index - starts
    half_size = HD // 2
    freqs = jnp.exp(jnp.arange(half_size, dtype=jnp.float32) * (-math.log(10000.0) / half_size))
    angles = places.astype(jnp.float32)[:, None] * freqs[None, :]
    return (places, jnp.cos(angles), jnp.sin(angles))


def rotate(vector, cos_table, sin_table):
    half_size = vector.shape[-1] // 2
    leading = vector[..., :half_size]
    trailing = vector[..., half_size:]
    return jnp.concatenate(
        [leading * cos_table - trailing * sin_table, trailing * cos_table + leading * sin_table],
        axis=-1,
    )


def rotate_back(vector, cos_table, sin_table):
    half_size = vector.shape[-1] // 2
    leading = vector[..., :half_size]
    trailing = vector[..., half_size:]
    return jnp.concatenate(
        [leading * cos_table + trailing * sin_table, trailing * cos_table - leading * sin_table],
        axis=-1,
    )


def matmul(left, right):
    return jnp.dot(left, right, preferred_element_type=jnp.float32)


def matmul_nt(left, right):
    return lax.dot_general(
        left, right, (((1,), (1,)), ((), ())), preferred_element_type=jnp.float32
    )


def matmul_tn(left, right):
    return lax.dot_general(
        left, right, (((0,), (0,)), ((), ())), preferred_element_type=jnp.float32
    )


def gelu_tanh(values):
    return jax.nn.gelu(values, approximate=True)


def norm_back(d_act, normed, rms_val, gain_val):
    scaled = d_act * gain_val
    return rms_val * (scaled - normed * jnp.mean(scaled * normed, axis=-1, keepdims=True))


def weights_move(
    tokens, seg_ids, gain_attn, w_query, kv_weight, w_out, gain_ffn, w_gate, w_up, w_down, d_out
):
    rows = tokens.shape[0]
    scale_factor = 1.0 / math.sqrt(HD)
    offset = lax.axis_index("seq") * rows
    places, cos_table, sin_table = place_tables(seg_ids)
    own_places = lax.dynamic_slice_in_dim(places, offset, rows, 0)
    own_segs = lax.dynamic_slice_in_dim(seg_ids, offset, rows, 0)
    own_cos = lax.dynamic_slice_in_dim(cos_table, offset, rows, 0)
    own_sin = lax.dynamic_slice_in_dim(sin_table, offset, rows, 0)
    allowed = (own_segs[:, None] == seg_ids[None, :]) & (own_places[:, None] >= places[None, :])
    full_query, full_out, full_kv, full_gain_one = (
        lax.all_gather(w_query, ("dp", "seq"), axis=0, tiled=True),
        lax.all_gather(w_out, ("dp", "seq"), axis=1, tiled=True),
        lax.all_gather(kv_weight, ("dp", "seq"), axis=0, tiled=True),
        lax.all_gather(gain_attn, ("dp", "seq"), axis=0, tiled=True),
    )
    gain_one = full_gain_one.astype(jnp.float32)
    inputs = tokens.astype(jnp.float32)
    rms_one = lax.rsqrt(jnp.mean(inputs * inputs, axis=-1, keepdims=True) + EPS)
    norm_one = inputs * rms_one
    act_one = (norm_one * gain_one).astype(jnp.bfloat16)
    query_pre = matmul(act_one, full_query)
    heads = query_pre.shape[1] // HD
    kv_pre = matmul(act_one, full_kv)
    queries = (
        rotate(query_pre.reshape(rows, heads, HD), own_cos[:, None, :], own_sin[:, None, :])
        * scale_factor
    ).astype(jnp.bfloat16)
    own_kv = jnp.concatenate(
        [rotate(kv_pre[:, :HD], own_cos, own_sin), kv_pre[:, HD:]], axis=1
    ).astype(jnp.bfloat16)
    all_kv = lax.all_gather(own_kv, "seq", axis=0, tiled=True)
    keys = all_kv[:, :HD]
    values_all = all_kv[:, HD:]
    scores = jnp.einsum("rhd,kd->hrk", queries, keys, preferred_element_type=jnp.float32)
    scores = jnp.where(allowed[None], scores, NEG)
    top_score = jnp.max(scores, axis=-1, keepdims=True)
    expd = jnp.exp(scores - top_score)
    total = jnp.sum(expd, axis=-1, keepdims=True)
    log_total = top_score + jnp.log(total)
    probs_low = (expd / total).astype(jnp.bfloat16)
    mixed = (
        jnp.einsum("hrk,kd->rhd", probs_low, values_all, preferred_element_type=jnp.float32)
        .reshape(rows, heads * HD)
        .astype(jnp.bfloat16)
    )
    attn = lax.psum(matmul(mixed, full_out), "tensor")
    resid = inputs + attn
    full_gate, full_up, full_down, full_gain_two = (
        lax.all_gather(w_gate, ("dp", "seq"), axis=0, tiled=True),
        lax.all_gather(w_up, ("dp", "seq"), axis=0, tiled=True),
        lax.all_gather(w_down, ("dp", "seq"), axis=1, tiled=True),
        lax.all_gather(gain_ffn, ("dp", "seq"), axis=0, tiled=True),
    )
    gain_two = full_gain_two.astype(jnp.float32)
    rms_two = lax.rsqrt(jnp.mean(resid * resid, axis=-1, keepdims=True) + EPS)
    norm_two = resid * rms_two
    act_two = (norm_two * gain_two).astype(jnp.bfloat16)
    gate = matmul(act_two, full_gate)
    up_val = matmul(act_two, full_up)
    gelu_val, gelu_pull = jax.vjp(gelu_tanh, gate)
    hidden = (gelu_val * up_val).astype(jnp.bfloat16)
    ffn = lax.psum(matmul(hidden, full_down).astype(jnp.bfloat16), "tensor").astype(jnp.float32)
    out = (resid + ffn).astype(jnp.bfloat16)
    back_gate, back_up, back_down = (
        lax.all_gather(w_gate, ("dp", "seq"), axis=0, tiled=True),
        lax.all_gather(w_up, ("dp", "seq"), axis=0, tiled=True),
        lax.all_gather(w_down, ("dp", "seq"), axis=1, tiled=True),
    )
    d_hidden = matmul_nt(d_out, back_down)
    grad_down = matmul_tn(hidden, d_out)
    d_gate = gelu_pull(d_hidden * up_val)[0].astype(jnp.bfloat16)
    d_up = (d_hidden * gelu_val).astype(jnp.bfloat16)
    grad_gate = matmul_tn(act_two, d_gate)
    grad_up = matmul_tn(act_two, d_up)
    d_act_two = lax.psum(matmul_nt(d_gate, back_gate) + matmul_nt(d_up, back_up), "tensor")
    grad_gain_two = jnp.sum(d_act_two * norm_two, axis=0)
    d_resid = d_out.astype(jnp.float32) + norm_back(d_act_two, norm_two, rms_two, gain_two)
    ffn_grads = (
        lax.psum_scatter(
            grad_gate.astype(jnp.bfloat16), ("dp", "seq"), scatter_dimension=0, tiled=True
        ).astype(jnp.float32),
        lax.psum_scatter(
            grad_up.astype(jnp.bfloat16), ("dp", "seq"), scatter_dimension=0, tiled=True
        ).astype(jnp.float32),
        lax.psum_scatter(
            grad_down.astype(jnp.bfloat16), ("dp", "seq"), scatter_dimension=1, tiled=True
        ).astype(jnp.float32),
        lax.psum_scatter(
            grad_gain_two.astype(jnp.bfloat16), ("dp", "seq"), scatter_dimension=0, tiled=True
        ).astype(jnp.float32),
    )
    back_query, back_out, back_kv = (
        lax.all_gather(w_query, ("dp", "seq"), axis=0, tiled=True),
        lax.all_gather(w_out, ("dp", "seq"), axis=1, tiled=True),
        lax.all_gather(kv_weight, ("dp", "seq"), axis=0, tiled=True),
    )
    d_attn = d_resid.astype(jnp.bfloat16)
    grad_out = matmul_tn(mixed, d_attn)
    d_mixed = matmul_nt(d_attn, back_out).astype(jnp.bfloat16).reshape(rows, heads, HD)
    scores_again = jnp.einsum("rhd,kd->hrk", queries, keys, preferred_element_type=jnp.float32)
    probs = jnp.where(allowed[None], jnp.exp(scores_again - log_total), 0.0)
    d_probs = jnp.einsum("rhd,kd->hrk", d_mixed, values_all, preferred_element_type=jnp.float32)
    delta = jnp.sum(probs * d_probs, axis=-1, keepdims=True)
    d_scores = (probs * (d_probs - delta)).astype(jnp.bfloat16)
    d_queries = (
        jnp.einsum("hrk,kd->rhd", d_scores, keys, preferred_element_type=jnp.float32) * scale_factor
    )
    d_query_pre = (
        rotate_back(d_queries, own_cos[:, None, :], own_sin[:, None, :])
        .reshape(rows, heads * HD)
        .astype(jnp.bfloat16)
    )
    d_keys_part = jnp.einsum("hrk,rhd->kd", d_scores, queries, preferred_element_type=jnp.float32)
    d_values_part = jnp.einsum(
        "hrk,rhd->kd", probs.astype(jnp.bfloat16), d_mixed, preferred_element_type=jnp.float32
    )
    own_kv_grad = lax.psum_scatter(
        jnp.concatenate([d_keys_part, d_values_part], axis=1).astype(jnp.bfloat16),
        "seq",
        scatter_dimension=0,
        tiled=True,
    )
    d_act_query = matmul_nt(d_query_pre, back_query)
    d_act_sum, kv_grad = (
        lax.psum(d_act_query.astype(jnp.bfloat16), "tensor").astype(jnp.float32),
        lax.psum(own_kv_grad, "tensor").astype(jnp.float32),
    )
    d_kv_pre = jnp.concatenate(
        [rotate_back(kv_grad[:, :HD], own_cos, own_sin), kv_grad[:, HD:]], axis=1
    ).astype(jnp.bfloat16)
    d_act_one = d_act_sum + matmul_nt(d_kv_pre, back_kv)
    grad_query = matmul_tn(act_one, d_query_pre)
    grad_kv = matmul_tn(act_one, d_kv_pre)
    grad_gain_one = jnp.sum(d_act_one * norm_one, axis=0)
    d_tokens = d_resid + norm_back(d_act_one, norm_one, rms_one, gain_one)
    attn_grads = (
        lax.psum_scatter(
            grad_query.astype(jnp.bfloat16), ("dp", "seq"), scatter_dimension=0, tiled=True
        ).astype(jnp.float32),
        lax.psum_scatter(
            grad_out.astype(jnp.bfloat16), ("dp", "seq"), scatter_dimension=1, tiled=True
        ).astype(jnp.float32),
        lax.psum_scatter(
            grad_kv.astype(jnp.bfloat16), ("dp", "seq"), scatter_dimension=0, tiled=True
        ).astype(jnp.float32),
        lax.psum_scatter(
            grad_gain_one.astype(jnp.bfloat16), ("dp", "seq"), scatter_dimension=0, tiled=True
        ).astype(jnp.float32),
    )
    return (
        out,
        d_tokens,
        attn_grads[3],
        attn_grads[0],
        attn_grads[2],
        attn_grads[1],
        ffn_grads[3],
        ffn_grads[0],
        ffn_grads[1],
        ffn_grads[2],
    )


MESH = pl.DeviceIdType.MESH
VMEM_LIMIT = 66000 * 1024


class Place:
    def __init__(self):
        self.dp = lax.axis_index("dp")
        self.seq = lax.axis_index("seq")
        self.z = lax.axis_index("tensor")
        self.core = lax.rem(self.dp, 2)
        self.chip = lax.div(self.dp, 2)

    def device(self, across, other):
        chip = (self.chip + across) % 2
        seq = (self.seq + across // 2) % 2
        core = (self.core + other) % 2
        return chip * 2 + core, seq, self.z

    def shard(self, across, other):
        dp, seq, _ = self.device(across, other)
        return dp * 2 + seq


def greet(here, peers, line=False):
    barrier = pltpu.get_barrier_semaphore()
    peers = list(peers)
    if line:
        peers += [(here.dp, here.seq, (here.z + step) % 4) for step in range(1, 4)]
    for peer in peers:
        pl.semaphore_signal(barrier, inc=1, device_id=peer, device_id_type=MESH)
    pl.semaphore_wait(barrier, len(peers))


def remote(src, dst, send, recv, peer):
    return pltpu.make_async_remote_copy(
        src_ref=src, dst_ref=dst, send_sem=send, recv_sem=recv, device_id=peer, device_id_type=MESH
    )


class Line:
    def __init__(self, here, counts, refs, place=None):
        self.own, self.out, self.from_end, self.from_mid = refs[:4]
        self.sems = refs[4:10]
        self.counts = counts
        self.chunk = self.own.shape[0] // counts
        self.place = place
        z = here.z
        self.inner = ((z + 1) // 2) % 2
        self.mate = (here.dp, here.seq, z + 1 - 2 * (z % 2))
        self.other = (here.dp, here.seq, 3 - z)

    def rows(self, at):
        at = at if self.place is None else self.place(at)
        return pl.ds(pl.multiple_of(at * self.chunk, self.chunk), self.chunk)

    def up(self, at):
        return remote(self.own.at[self.rows(at), :], self.from_end.at[at], self.sems[0].at[at],
                      self.sems[1].at[at], self.mate)

    def over(self, at):
        return remote(self.out.at[self.rows(at), :], self.from_mid.at[at], self.sems[2].at[at],
                      self.sems[3].at[at], self.other)

    def down(self, at):
        rows = self.rows(at)
        return remote(self.out.at[rows, :], self.out.at[rows, :], self.sems[4].at[at],
                      self.sems[5].at[at], self.mate)

    def launch(self, first, count):
        @pl.when(self.inner == 0)
        def _():
            def send(at, _):
                self.up(first + at).start()
                return 0

            lax.fori_loop(0, count, send, 0)

    def begin(self):
        self.launch(0, self.counts)

    def first(self, at):
        rows = self.rows(at)
        self.up(at).wait_recv()
        total = self.own[rows, :].astype(jnp.float32) + self.from_end[at].astype(jnp.float32)
        self.out[rows, :] = total.astype(self.out.dtype)
        self.over(at).start()

    def second(self, at):
        rows = self.rows(at)
        self.over(at).wait()
        total = self.out[rows, :].astype(jnp.float32) + self.from_mid[at].astype(jnp.float32)
        self.out[rows, :] = total.astype(self.out.dtype)
        self.down(at).start()

    def step(self, at, start=0, count=None):
        count = self.counts if count is None else count

        @pl.when(jnp.logical_and(self.inner == 1, at < count))
        def _():
            self.first(start + at)

        @pl.when(jnp.logical_and(self.inner == 1, jnp.logical_and(at > 1, at < count + 2)))
        def _():
            self.second(start + at - 2)

    def steps(self, first, last, start=0, count=None):
        def rest(at, _):
            self.step(at, start, count)
            return 0

        lax.fori_loop(first, last, rest, 0)

    def settle(self):
        @pl.when(self.inner == 0)
        def _():
            def take(at, _):
                self.up(at).wait_send()
                self.down(at).wait_recv()
                return 0

            lax.fori_loop(0, self.counts, take, 0)

        self.drain()

    def drain(self):
        @pl.when(self.inner == 1)
        def _():
            def drain(at, _):
                self.down(at).wait_send()
                return 0

            lax.fori_loop(0, self.counts, drain, 0)

    def end(self, done=0):
        self.steps(min(done, self.counts + 2), self.counts + 2)
        self.settle()


def line_scratch(counts, shape, low):
    buf = pltpu.VMEM((counts, shape[0] // counts, shape[1]), low)
    return [buf, buf] + [pltpu.SemaphoreType.DMA((counts,))] * 6


def turned(at):
    return 3 - at // 2, 1 - at % 2


def slice_peers(here):
    return [here.device(*turned(at)) for at in range(7)]


def kernel_call(kernel, out_shape, operands, specs, scratch, cid, name, out_specs=None):
    vm = pl.BlockSpec(memory_space=pltpu.VMEM)
    return pl.pallas_call(
        kernel,
        out_shape=out_shape,
        in_specs=specs,
        out_specs=out_specs or [vm] * len(out_shape),
        scratch_shapes=scratch,
        compiler_params=pltpu.CompilerParams(
            collective_id=cid, has_side_effects=True, vmem_limit_bytes=VMEM_LIMIT
        ),
        name=f"{name}_{cid}",
    )(*operands)


class Tiny:
    def __init__(self, here, src, dst, sems, spread):
        self.here, self.src, self.dst, self.sems, self.spread = here, src, dst, sems, spread
        self.peers = slice_peers(here)
        self.me = here.shard(0, 0)

    def tile(self, shard):
        return self.src.at[shard] if self.spread else self.src

    def copy(self, at):
        return remote(self.tile(self.here.shard(*turned(at))), self.dst.at[self.me], self.sems[0].at[at],
                      self.sems[1].at[at], self.peers[at])

    def begin(self):
        for at in range(7):
            self.copy(at).start()
        self.dst[self.me] = self.tile(self.me)[...]

    def end(self):
        for at in range(7):
            self.copy(at).wait()


class Reduce:
    def __init__(self, here, counts, product, refs, before=None):
        self.counts, self.product, self.before = counts, product, before
        self.held, self.sib_out, self.sib_in, self.from_x, self.from_y = refs[:5]
        self.sib_sems, self.x_sems, self.y_sems = refs[5:7], refs[7:9], refs[9:11]
        self.sib, self.xdev, self.ydev = here.device(0, 1), here.device(1, 0), here.device(2, 0)
        self.steps = 4 * counts
        self.ring = self.sib_out.shape[0]

    def streams(self, stage):
        far = stage // 3
        x_chip = jnp.where(stage == 0, 3, jnp.where(stage == 2, 0, 1))
        y_chip = jnp.where(stage == 0, 3, jnp.where(stage == 2, 0, 2))
        return (x_chip, far), (y_chip, 1 - far)

    def to_sib(self, step, stream):
        stage, at = step // self.counts, step % self.counts
        return remote(self.sib_out.at[step % self.ring, stream], self.sib_in.at[stage, stream, at],
                      self.sib_sems[0].at[stage, stream, at], self.sib_sems[1].at[stage, stream, at], self.sib)

    def to_x(self, hop, at, stage=0):
        return remote(self.held.at[stage, 0, at], self.from_x.at[hop, at], self.x_sems[0].at[hop, at],
                      self.x_sems[1].at[hop, at], self.xdev)

    def to_y(self, hop, at, stage=0):
        return remote(self.held.at[stage, 1, at], self.from_y.at[hop, at], self.y_sems[0].at[hop, at],
                      self.y_sems[1].at[hop, at], self.ydev)

    def compute(self, step):
        stage, at = step // self.counts, step % self.counts
        if self.before:
            for stop in range(3):
                @pl.when(step == stop * self.counts)
                def _():
                    self.before(stop)

        @pl.when(step >= self.ring)
        def _():
            for stream in range(2):
                self.to_sib(step - self.ring, stream).wait_send()

        for stream, (across, half) in enumerate(self.streams(stage)):
            self.sib_out[step % self.ring, stream] = self.product(across, 1, half, at).astype(jnp.bfloat16)
            self.held[stage, stream, at] = self.product(across, 0, half, at).astype(jnp.bfloat16)
        for stream in range(2):
            self.to_sib(step, stream).start()

    def finish(self, step):
        stage, at = step // self.counts, step % self.counts
        for stream in range(2):
            self.to_sib(step, stream).wait_recv()

        def total(stream):
            return self.held[stage, stream, at].astype(jnp.float32) + self.sib_in[stage, stream, at].astype(
                jnp.float32)

        @pl.when(stage < 3)
        def _():
            for stream in range(2):
                self.held[stage, stream, at] = total(stream).astype(jnp.bfloat16)

        @pl.when(stage == 3)
        def _():
            self.to_y(0, at).wait_recv()
            self.held[3, 0, at] = (total(0) + self.from_y[0, at].astype(jnp.float32)).astype(jnp.bfloat16)
            self.to_x(0, at).wait_recv()
            self.held[3, 1, at] = (total(1) + self.from_x[0, at].astype(jnp.float32)).astype(jnp.bfloat16)

        @pl.when(stage != 2)
        def _():
            hop = stage - stage // 3
            self.to_x(hop, at, stage).start()
            self.to_y(hop, at, stage).start()

    def run(self, hook=None):
        def body(step, _):
            @pl.when(step < self.steps)
            def _():
                self.compute(step)

            @pl.when(step > 0)
            def _():
                self.finish(step - 1)

            if hook:
                hook(step)
            return 0

        lax.fori_loop(0, self.steps + 1, body, 0)
        return self.steps + 1

    def end(self, emit):
        def last(at, _):
            values = []
            for half in range(2):
                xs, ys = (1, 2) if half == 0 else (2, 1)
                self.to_x(xs, at).wait_recv()
                self.to_y(ys, at).wait_recv()
                values.append(self.held[2, half, at].astype(jnp.float32) + self.from_x[xs, at].astype(jnp.float32)
                              + self.from_y[ys, at].astype(jnp.float32))
            emit(at, *values)
            for hop in range(3):
                self.to_x(hop, at).wait_send()
                self.to_y(hop, at).wait_send()
            return 0

        lax.fori_loop(0, self.counts, last, 0)

        def drain(at, _):
            for stream in range(2):
                self.to_sib(self.steps - self.ring + at, stream).wait_send()
            return 0

        lax.fori_loop(0, self.ring, drain, 0)


def reduce_scratch(counts, rows, width, ring=4):
    low, dma = jnp.bfloat16, pltpu.SemaphoreType.DMA
    block = pltpu.VMEM((4, 2, counts, rows, width), low)
    landed = pltpu.VMEM((3, counts, rows, width), low)
    sent = pltpu.VMEM((ring, 2, rows, width), low)
    return [block, sent, block, landed, landed] + [dma((4, 2, counts))] * 2 + [dma((3, counts))] * 4


class Spread:
    def __init__(self, here, counts, refs):
        self.counts = counts
        self.got = refs[0]
        self.x_sems, self.y_sems, self.sib_sems = refs[1:3], refs[3:5], refs[5:7]
        self.core = here.core
        self.sib, self.xdev, self.ydev = here.device(0, 1), here.device(1, 0), here.device(2, 0)

    def slot(self, across, half, at):
        return self.got.at[across, self.core, half, at]

    def x_copy(self, hop, at):
        half = jnp.minimum(hop, 1)
        src = self.slot(2 * (hop // 2), half, at)
        dst = self.slot(1 + 2 * (hop // 2), half, at)
        return remote(src, dst, self.x_sems[0].at[hop, at], self.x_sems[1].at[hop, at], self.xdev)

    def y_copy(self, hop, at):
        half = 1 - jnp.minimum(hop, 1)
        src = self.slot(hop // 2, half, at)
        dst = self.slot(2 + hop // 2, half, at)
        return remote(src, dst, self.y_sems[0].at[hop, at], self.y_sems[1].at[hop, at], self.ydev)

    def streams(self, stage):
        some, last, late = jnp.minimum(stage, 1), stage // 3, stage // 2
        return (some + 2 * last, late), (2 * some + last, 1 - late)

    def sib_copy(self, stage, stream, at):
        across, half = self.streams(stage)[stream]
        slot = self.slot(across, half, at)
        spot = (stage, stream, at)
        return remote(slot, slot, self.sib_sems[0].at[spot], self.sib_sems[1].at[spot], self.sib)

    def begin(self):
        def first(at, _):
            self.x_copy(0, at).start()
            self.y_copy(0, at).start()
            return 0

        def own(at, _):
            self.sib_copy(0, 0, at).start()
            self.sib_copy(0, 1, at).start()
            return 0

        lax.fori_loop(0, self.counts, first, 0)
        lax.fori_loop(0, self.counts, own, 0)

    def run(self, blocks, hook=None, done=None):
        counts = self.counts

        def body(step, _):
            stage, at = step // counts, step % counts

            @pl.when(jnp.logical_and(stage > 0, stage < 4))
            def _():
                self.x_copy(stage - 1, at).wait_recv()
                self.sib_copy(stage, 0, at).start()
                self.y_copy(stage - 1, at).wait_recv()
                self.sib_copy(stage, 1, at).start()

            @pl.when(jnp.logical_and(stage > 0, stage < 3))
            def _():
                self.x_copy(stage, at).start()
                self.y_copy(stage, at).start()

            @pl.when(step > 0)
            def _():
                old, spot = (step - 1) // counts, (step - 1) % counts
                for stream, (across, half) in enumerate(self.streams(old)):
                    self.sib_copy(old, stream, spot).wait_recv()
                    blocks(across, half, spot)
                if done:
                    done(old, spot)

            if hook:
                hook(step)
            return 0

        lax.fori_loop(0, 4 * counts + 1, body, 0)
        return 4 * counts + 1

    def end(self):
        def drain(at, _):
            for hop in range(3):
                self.x_copy(hop, at).wait_send()
                self.y_copy(hop, at).wait_send()
            for stage in range(4):
                self.sib_copy(stage, 0, at).wait_send()
                self.sib_copy(stage, 1, at).wait_send()
            return 0

        lax.fori_loop(0, self.counts, drain, 0)


def spread_scratch(counts, rows, width):
    dma = pltpu.SemaphoreType.DMA
    return [pltpu.VMEM((4, 2, 2, counts, rows, width), jnp.bfloat16)] + [dma((3, counts))] * 4 + [
        dma((4, 2, counts))] * 2


def row_span(here, across, other, rows):
    return pl.ds(pl.multiple_of(here.shard(across, other) * rows, rows), rows)


def dot_nt(left, right):
    return lax.dot_general(left, right, (((1,), (1,)), ((), ())), preferred_element_type=jnp.float32)


def dot_tn(left, right):
    return lax.dot_general(left, right, (((0,), (0,)), ((), ())), preferred_element_type=jnp.float32)


def dot_nn(left, right):
    return jnp.dot(left, right, preferred_element_type=jnp.float32)


def products(here, act, weight, nt, rows, width, counts):
    def product(across, other, half, at):
        cols = pl.ds(pl.multiple_of((half * counts + at) * width, width), width)
        block = act[row_span(here, across, other, rows), :]
        return dot_nt(block, weight[cols, :]) if nt else dot_nn(block, weight[:, cols])

    return product


def diagonal():
    return (lax.broadcasted_iota(jnp.int32, (LANES, LANES), 0) ==
            lax.broadcasted_iota(jnp.int32, (LANES, LANES), 1)).astype(jnp.float32)


def to_tile(tile, first, column, eye):
    for at in range(column.shape[0] // LANES):
        spread = column[at * LANES : (at + 1) * LANES, :] * eye
        tile[first + at : first + at + 1, :] = jnp.sum(spread, axis=0, keepdims=True)


def from_tile(row, eye):
    return jnp.sum(eye * row, axis=1, keepdims=True)


def make_tables(here, rows, segs, cos, sin, mask):
    eye = diagonal()
    tiles = rows // LANES
    freqs = jnp.exp(lax.broadcasted_iota(jnp.int32, (1, LANES), 1).astype(jnp.float32) * (-math.log(10000.0) / LANES))
    lane = lax.broadcasted_iota(jnp.int32, (1, LANES), 1)
    line = lax.broadcasted_iota(jnp.int32, (LANES, 1), 0)

    def row_of(side, at):
        return ((here.seq + side) % 2) * tiles + at

    for side in range(2):
        for at in range(tiles):
            row = row_of(side, at)
            ids = from_tile(segs[pl.ds(row, 1), :], eye)
            before = jnp.zeros((LANES, 1), jnp.float32)
            for other in range(2 * tiles):
                smaller = segs[other : other + 1, :] < ids
                before += jnp.sum(smaller.astype(jnp.float32), axis=-1, keepdims=True)
            index = row * LANES + line
            angles = (index.astype(jnp.float32) - before) * freqs
            span = slice(at * LANES, (at + 1) * LANES)
            cos[side, span, :] = jnp.cos(angles)
            sin[side, span, :] = jnp.sin(angles)
            if side == 0:
                for key_side in range(2):
                    for key_at in range(tiles):
                        key_row = row_of(key_side, key_at)
                        same = segs[pl.ds(key_row, 1), :] == ids
                        allowed = jnp.logical_and(same, key_row * LANES + lane <= index)
                        first = key_side * rows + key_at * LANES
                        mask[span, first : first + LANES] = allowed.astype(jnp.float32)


def open_kernel(rows, width, counts, tokens, gain, w_query, kv_weight, segs, qkv, x_low, act_t, w_qkv, rms, cos, sin,
                mask, *refs):
    here = Place()
    cols = gain.shape[1]
    act, turn_send, turn_recv, local_sems = refs[:4]
    me = here.shard(0, 0)
    own_rows = pl.ds(pl.multiple_of(me * rows, rows), rows)

    def turn_copy(at):
        across, other = turned(at)
        first = pl.multiple_of(here.shard(across, other) * cols, cols)
        return remote(tokens.at[:, pl.ds(first, cols)], x_low.at[own_rows, :], turn_send.at[at], turn_recv.at[at],
                      here.device(across, other))

    wide = w_query.shape[1]
    local = [
        pltpu.make_async_copy(w_query, w_qkv.at[:, :wide], local_sems.at[0]),
        pltpu.make_async_copy(kv_weight, w_qkv.at[:, wide:], local_sems.at[1]),
        pltpu.make_async_copy(tokens.at[:, pl.ds(pl.multiple_of(me * cols, cols), cols)], x_low.at[own_rows, :],
                              local_sems.at[2]),
    ]
    for copy in local:
        copy.start()
    greet(here, slice_peers(here))
    for at in range(7):
        turn_copy(at).start()
    for copy in local:
        copy.wait()

    def squares(at, total):
        values = tokens[:, pl.ds(pl.multiple_of(at * cols, cols), cols)].astype(jnp.float32)
        return total + jnp.sum(values * values, axis=-1, keepdims=True)

    total = lax.fori_loop(0, 8, squares, jnp.zeros((rows, 1), jnp.float32))
    rms[...] = jnp.broadcast_to(lax.rsqrt(total / (8 * cols) + EPS), rms.shape)
    make_tables(here, rows, segs, cos, sin, mask)

    def prepare(first, count):
        def one(step, _):
            at = first + step
            span = row_span(here, *turned(at), rows)
            value = (x_low[span, :].astype(jnp.float32) * gain[...]).astype(act.dtype)
            act[span, :] = value
            return 0

        lax.fori_loop(0, count, one, 0)

    def before(stop):
        first, count = ((0, 2), (2, 4), (6, 2))[stop]
        for at in range(first, min(first + count, 7)):
            turn_copy(at).wait_recv()
        prepare(first, count)

    def flip():
        def one(shard, _):
            span = pl.ds(pl.multiple_of(shard * rows, rows), rows)
            act_t[:, span] = act[span, :].T
            return 0

        lax.fori_loop(0, 8, one, 0)

    product = products(here, act, w_qkv, False, rows, width, counts)
    total = Reduce(here, counts, product, refs[4:15], before)
    total.run()
    flip()

    def emit(at, first, second):
        for half, value in enumerate((first, second)):
            qkv[:, pl.ds(pl.multiple_of((half * counts + at) * width, width), width)] = value

    total.end(emit)
    for at in range(7):
        turn_copy(at).wait_send()


def opening(tokens, gain, w_query, kv_weight, segs, cid, width=256):
    rows = tokens.shape[0]
    cols, wide = w_query.shape
    every = wide + kv_weight.shape[1]
    counts = every // (2 * width)
    low, f32 = jnp.bfloat16, jnp.float32
    dma = pltpu.SemaphoreType.DMA
    vm = pl.BlockSpec(memory_space=pltpu.VMEM)
    hbm = pl.BlockSpec(memory_space=pl.ANY)
    out_shape = [
        jax.ShapeDtypeStruct((rows, every), f32),
        jax.ShapeDtypeStruct((8 * rows, cols), low),
        jax.ShapeDtypeStruct((cols, 8 * rows), low),
        jax.ShapeDtypeStruct((cols, every), low),
        jax.ShapeDtypeStruct((rows, LANES), f32),
        jax.ShapeDtypeStruct((2, rows, LANES), f32),
        jax.ShapeDtypeStruct((2, rows, LANES), f32),
        jax.ShapeDtypeStruct((rows, 2 * rows), f32),
    ]
    scratch = [pltpu.VMEM((8 * rows, cols), low), dma((7,)), dma((7,)), dma((3,))]
    scratch += reduce_scratch(counts, rows, width)
    kernel = functools.partial(open_kernel, rows, width, counts)
    return kernel_call(kernel, out_shape, [tokens, gain, w_query, kv_weight, segs],
                       [vm, vm, hbm, hbm, vm], scratch, cid, "open")


def scatter_kernel(rows, width, counts, line_counts, act, weight, line_own, out, line_out, *refs):
    here = Place()
    line = Line(here, line_counts, [line_own, line_out] + list(refs[11:]))
    product = products(here, act, weight, True, rows, width, counts)
    total = Reduce(here, counts, product, refs[:11])
    greet(here, slice_peers(here), True)
    line.begin()
    done = total.run(line.step)
    line.end(done)

    def emit(at, first, second):
        for half, value in enumerate((first, second)):
            out[:, pl.ds(pl.multiple_of((half * counts + at) * width, width), width)] = value

    total.end(emit)


def scatter_product(act, weight, width, cid, line, line_counts=16):
    rows = act.shape[0] // 8
    every = weight.shape[0]
    counts = every // (2 * width)
    vm = pl.BlockSpec(memory_space=pltpu.VMEM)
    out_shape = [
        jax.ShapeDtypeStruct((rows, every), jnp.float32),
        jax.ShapeDtypeStruct(line.shape, line.dtype),
    ]
    scratch = reduce_scratch(counts, rows, width) + line_scratch(line_counts, line.shape, line.dtype)
    kernel = functools.partial(scatter_kernel, rows, width, counts, line_counts)
    return kernel_call(kernel, out_shape, [act, weight, line], [vm] * 3, scratch, cid, "scatter_product")


def ffn_kernel(rows, width, counts, x_low, attn, gain, w_gate, w_up, d_hidden, hidden, d_gate, d_up, act_t, tile_out,
               *refs):
    here = Place()
    cols = gain.shape[1]
    act, weight, tiny_own, tiny_all, tiny_send, tiny_recv, dots, local_sems = refs[:8]
    tiny = Tiny(here, tiny_own, tiny_all, (tiny_send, tiny_recv), True)
    half_cols = counts * width
    local = [
        pltpu.make_async_copy(w_gate, weight.at[:, :half_cols], local_sems.at[0]),
        pltpu.make_async_copy(w_up, weight.at[:, half_cols:], local_sems.at[1]),
    ]
    for copy in local:
        copy.start()
    eye = diagonal()
    tiny_own[...] = jnp.zeros_like(tiny_own)

    def prepare(shard, _):
        for at in range(rows // LANES):
            span = pl.ds(pl.multiple_of(shard * rows + at * LANES, LANES), LANES)
            resid = x_low[span, :].astype(jnp.float32) + attn[span, :].astype(jnp.float32)
            act[span, :] = (resid * gain[...]).astype(act.dtype)
            square = jnp.sum(resid * resid, axis=-1, keepdims=True)
            tiny_own[shard, at : at + 1, :] = jnp.sum(square * eye, axis=0, keepdims=True)
        return 0

    lax.fori_loop(0, 8, prepare, 0)
    greet(here, slice_peers(here))
    tiny.begin()
    for copy in local:
        copy.wait()
    product = products(here, act, weight, False, rows, width, counts)
    total = Reduce(here, counts, product, refs[8:19])
    total.run()

    def flip(shard, _):
        span = pl.ds(pl.multiple_of(shard * rows, rows), rows)
        act_t[:, span] = act[span, :].T
        return 0

    lax.fori_loop(0, 8, flip, 0)
    tiny.end()
    tiles = rows // LANES
    mean = [from_tile(jnp.sum(tiny_all[:, at, :], axis=0, keepdims=True), eye) for at in range(tiles)]
    scale = lax.rsqrt(jnp.concatenate(mean, axis=0) / (8 * cols) + EPS)
    dots[...] = jnp.zeros_like(dots)
    coeff = math.sqrt(2.0 / math.pi)

    def emit(at, first, second):
        span = pl.ds(pl.multiple_of(at * width, width), width)
        gate, up = first * scale, second * scale
        inner = jnp.tanh(coeff * (gate + 0.044715 * (gate * gate * gate)))
        gelu = 0.5 * gate * (1.0 + inner)
        slope = 0.5 * (1.0 + inner) + 0.5 * gate * (1.0 - inner * inner) * (
            coeff * (1.0 + 3.0 * 0.044715 * gate * gate))
        cot = d_hidden[:, span]
        hidden[:, span] = (gelu * up).astype(hidden.dtype)
        back_gate, back_up = cot * up * slope, cot * gelu
        d_gate[:, span] = (back_gate * scale).astype(d_gate.dtype)
        d_up[:, span] = (back_up * scale).astype(d_up.dtype)
        dots[...] += jnp.sum(back_gate * gate + back_up * up, axis=-1, keepdims=True)

    total.end(emit)
    tile_out[...] = jnp.zeros_like(tile_out)
    to_tile(tile_out, 0, dots[...] * (scale * scale * (1.0 / (8 * cols))), eye)


def ffn_scatter(x_low, attn, gain, w_gate, w_up, d_hidden, cid, width=512):
    rows, half = d_hidden.shape
    cols = gain.shape[1]
    counts = half // width
    low, f32 = jnp.bfloat16, jnp.float32
    dma = pltpu.SemaphoreType.DMA
    vm = pl.BlockSpec(memory_space=pltpu.VMEM)
    hbm = pl.BlockSpec(memory_space=pl.ANY)
    out_shape = [jax.ShapeDtypeStruct((rows, half), low)] * 3 + [
        jax.ShapeDtypeStruct((cols, 8 * rows), low),
        jax.ShapeDtypeStruct((8, LANES), f32),
    ]
    scratch = [
        pltpu.VMEM((8 * rows, cols), low),
        pltpu.VMEM((cols, 2 * half), low),
        pltpu.VMEM((8, 8, LANES), f32),
        pltpu.VMEM((8, 8, LANES), f32),
        dma((7,)), dma((7,)),
        pltpu.VMEM((rows, 1), f32),
        dma((2,)),
    ] + reduce_scratch(counts, rows, width)
    kernel = functools.partial(ffn_kernel, rows, width, counts)
    return kernel_call(kernel, out_shape, [x_low, attn, gain, w_gate, w_up, d_hidden], [vm, vm, vm, hbm, hbm, vm],
                       scratch, cid, "ffn")


def load_own(spread, payload, width, counts, sems):
    copies = []
    for half in range(2):
        for at in range(counts):
            first = at * width + (half * counts * width if len(payload) == 1 else 0)
            src = payload[half % len(payload)].at[:, first : first + width]
            copies.append(pltpu.make_async_copy(src, spread.slot(0, half, at), sems.at[half, at]))
    return copies


def back_kernel(rows, width, counts, act_t, w_gate, w_up, d_gate, d_up, dots, x_low, attn, gain, contrib, gain_grad,
                grad_gate, grad_up, *refs):
    here = Place()
    spread = Spread(here, counts, refs[:7])
    tiny_all, tiny_send, tiny_recv, own_sems, weight, sums, grads, staged, local_sems, out_sems = refs[7:17]
    tiny = Tiny(here, dots, tiny_all, (tiny_send, tiny_recv), False)
    half_cols = counts * width
    local = [
        pltpu.make_async_copy(w_gate, weight.at[:, :half_cols], local_sems.at[0]),
        pltpu.make_async_copy(w_up, weight.at[:, half_cols:], local_sems.at[1]),
    ]
    own = load_own(spread, (d_gate, d_up), width, counts, own_sems)
    for copy in own + local:
        copy.start()
    greet(here, tiny.peers)
    for copy in own:
        copy.wait()
    spread.begin()
    tiny.begin()
    sums[...] = jnp.zeros_like(sums)
    for copy in local:
        copy.wait()

    def columns(half, at):
        return pl.ds(pl.multiple_of((half * counts + at) * width, width), width)

    def clear(at, _):
        grads[:, columns(0, at)] = jnp.zeros((grads.shape[0], width), jnp.float32)
        return 0

    lax.fori_loop(0, 2 * counts, clear, 0)

    def blocks(across, half, at):
        cols = columns(half, at)
        gained = grads[:, cols]
        for other in range(2):
            row = row_span(here, across, other, rows)
            block = spread.got[across, (spread.core + other) % 2, half, at]
            sums[row, :] += dot_nt(block, weight[:, cols])
            gained = gained + dot_nn(act_t[:, row], block)
        grads[:, cols] = gained

    def leave(half, at):
        spot = pl.ds(pl.multiple_of(at * width, width), width)
        return pltpu.make_async_copy(staged.at[at % 2, half], (grad_gate, grad_up)[half].at[:, spot],
                                     out_sems.at[half, at])

    def done(stage, at):
        @pl.when(jnp.logical_and(stage == 3, at > 1))
        def _():
            leave(0, at - 2).wait()
            leave(1, at - 2).wait()

        @pl.when(stage == 3)
        def _():
            for half in range(2):
                staged[at % 2, half] = grads[:, columns(half, at)].astype(staged.dtype)
            leave(0, at).start()
            leave(1, at).start()

    spread.run(blocks, done=done)
    tiny.end()
    eye = diagonal()
    gain_grad[...] = jnp.zeros_like(gain_grad)

    def close_shard(shard, _):
        for at in range(rows // LANES):
            span = pl.ds(pl.multiple_of(shard * rows + at * LANES, LANES), LANES)
            dot = from_tile(tiny_all[shard, at : at + 1, :], eye)
            resid = x_low[span, :].astype(jnp.float32) + attn[span, :].astype(jnp.float32)
            value = sums[span, :]
            contrib[span, :] = (value * gain[...] - resid * dot).astype(contrib.dtype)
            gain_grad[...] += jnp.sum(value * resid, axis=0, keepdims=True)
        return 0

    lax.fori_loop(0, 8, close_shard, 0)
    spread.end()

    def drain(at, _):
        leave(0, at).wait()
        leave(1, at).wait()
        return 0

    lax.fori_loop(counts - 2, counts, drain, 0)


def back_gather(act_t, w_gate, w_up, d_gate, d_up, dots, x_low, attn, gain, cid, width=512):
    cols, total = act_t.shape
    rows, half = d_gate.shape
    counts = half // width
    low, f32 = jnp.bfloat16, jnp.float32
    dma = pltpu.SemaphoreType.DMA
    vm = pl.BlockSpec(memory_space=pltpu.VMEM)
    hbm = pl.BlockSpec(memory_space=pl.ANY)
    out_shape = [
        jax.ShapeDtypeStruct((total, cols), low),
        jax.ShapeDtypeStruct((1, cols), f32),
        jax.ShapeDtypeStruct((cols, half), low),
        jax.ShapeDtypeStruct((cols, half), low),
    ]
    scratch = spread_scratch(counts, rows, width) + [
        pltpu.VMEM((8, 8, LANES), f32), dma((7,)), dma((7,)), dma((2, counts)),
        pltpu.VMEM((cols, 2 * half), low),
        pltpu.VMEM((total, cols), f32),
        pltpu.VMEM((cols, 2 * half), f32),
        pltpu.VMEM((2, 2, cols, width), low),
        dma((2,)), dma((2, counts)),
    ]
    operands = [act_t, w_gate, w_up, d_gate, d_up, dots, x_low, attn, gain]
    kernel = functools.partial(back_kernel, rows, width, counts)
    return kernel_call(kernel, out_shape, operands, [vm] + [hbm] * 4 + [vm] * 4, scratch, cid, "back",
                       [vm, vm, hbm, hbm])


def down_kernel(rows, width, counts, line_counts, cot, weight, hidden, line_own, ffn, d_attn, grad, *refs):
    here = Place()
    spread = Spread(here, counts, refs[:7])
    own_sems, sums, grads, staged, out_sems, line_out = refs[7:13]
    line = Line(here, line_counts, [line_own, line_out] + list(refs[13:]))
    own = load_own(spread, (hidden,), width, counts, own_sems)
    for copy in own:
        copy.start()
    greet(here, slice_peers(here), True)
    line.begin()
    for copy in own:
        copy.wait()
    spread.begin()
    sums[...] = jnp.zeros_like(sums)
    grads[...] = jnp.zeros_like(grads)

    def columns(half, at):
        return pl.ds(pl.multiple_of((half * counts + at) * width, width), width)

    def blocks(across, half, at):
        cols = columns(half, at)
        gained = grads[cols, :]
        for other in range(2):
            row = row_span(here, across, other, rows)
            block = spread.got[across, (spread.core + other) % 2, half, at]
            sums[row, :] += dot_nn(block, weight[cols, :])
            gained = gained + dot_tn(block, cot[row, :])
        grads[cols, :] = gained

    def leave(half, at):
        return pltpu.make_async_copy(staged.at[at % 2, half], grad.at[columns(half, at), :], out_sems.at[half, at])

    def done(stage, at):
        @pl.when(jnp.logical_and(stage == 3, at > 1))
        def _():
            leave(0, at - 2).wait()
            leave(1, at - 2).wait()

        @pl.when(stage == 3)
        def _():
            for half in range(2):
                staged[at % 2, half] = grads[columns(half, at), :].astype(staged.dtype)
            leave(0, at).start()
            leave(1, at).start()

    steps = spread.run(blocks, line.step, done)
    line.end(steps)

    def close_shard(shard, _):
        span = pl.ds(pl.multiple_of(shard * rows, rows), rows)
        ffn[span, :] = sums[span, :].astype(ffn.dtype)
        d_attn[span, :] = (cot[span, :].astype(jnp.float32) + line_out[span, :].astype(jnp.float32)).astype(
            d_attn.dtype)
        return 0

    lax.fori_loop(0, 8, close_shard, 0)
    spread.end()

    def drain(at, _):
        leave(0, at).wait()
        leave(1, at).wait()
        return 0

    lax.fori_loop(counts - 2, counts, drain, 0)


def down_gather(cot, weight, hidden, line, cid, width=256, line_counts=16):
    total, cols = cot.shape
    rows, every = hidden.shape
    counts = every // (2 * width)
    low, f32 = jnp.bfloat16, jnp.float32
    dma = pltpu.SemaphoreType.DMA
    vm = pl.BlockSpec(memory_space=pltpu.VMEM)
    hbm = pl.BlockSpec(memory_space=pl.ANY)
    out_shape = [
        jax.ShapeDtypeStruct((total, cols), low),
        jax.ShapeDtypeStruct((total, cols), low),
        jax.ShapeDtypeStruct(weight.shape, low),
    ]
    scratch = spread_scratch(counts, rows, width) + [
        dma((2, counts)),
        pltpu.VMEM((total, cols), f32),
        pltpu.VMEM(weight.shape, f32),
        pltpu.VMEM((2, 2, width, cols), low),
        dma((2, counts)),
        pltpu.VMEM((total, cols), low),
    ] + line_scratch(line_counts, line.shape, low)
    kernel = functools.partial(down_kernel, rows, width, counts, line_counts)
    return kernel_call(kernel, out_shape, [cot, weight, hidden, line], [vm, vm, hbm, vm], scratch, cid, "down",
                       [vm, vm, hbm])


def attend_kernel(rows, heads, cols, qkv, rms, cos, sin, mask, w_out, cot, part, mixed_all, g_col, kv, probs, queries,
                  pair_rms, *refs):
    here = Place()
    spread = Spread(here, heads // 2, refs[:7])
    sums, pair_sems, turn_send, turn_recv, local_sem, tiny_own, tiny_pair = refs[7:14]
    got, core = spread.got, here.core
    greet(here, slice_peers(here))
    me = here.shard(0, 0)

    def turn_copy(at):
        across, other = turned(at)
        first = pl.multiple_of(here.shard(across, other) * cols, cols)
        return remote(cot.at[:, pl.ds(first, cols)], g_col.at[pl.ds(pl.multiple_of(me * rows, rows), rows), :],
                      turn_send.at[at], turn_recv.at[at], here.device(across, other))

    own_turn = pltpu.make_async_copy(cot.at[:, pl.ds(pl.multiple_of(me * cols, cols), cols)],
                                     g_col.at[pl.ds(pl.multiple_of(me * rows, rows), rows), :], local_sem)
    own_turn.start()
    half = HD // 2
    scale = 1.0 / math.sqrt(HD)
    wide = heads * HD

    def rotated(first):
        lead = qkv[:, first : first + half] * rms[...]
        trail = qkv[:, first + half : first + HD] * rms[...]
        return lead * cos[0] - trail * sin[0], trail * cos[0] + lead * sin[0]

    low_k, high_k = rotated(wide)
    kv[0, :, :half] = low_k.astype(kv.dtype)
    kv[0, :, half:HD] = high_k.astype(kv.dtype)
    for at in range(2):
        first = HD + at * half
        kv[0, :, first : first + half] = (qkv[:, wide + first : wide + first + half] * rms[...]).astype(kv.dtype)
    eye = diagonal()
    tiny_own[...] = jnp.zeros_like(tiny_own)
    to_tile(tiny_own, 0, rms[:, :1], eye)
    pair_rms[0] = rms[...]
    pair = remote(kv.at[0], kv.at[1], pair_sems.at[0], pair_sems.at[1], spread.ydev)
    tiny = remote(tiny_own, tiny_pair, pair_sems.at[2], pair_sems.at[3], spread.ydev)
    for head in range(heads):
        if head == 1:
            pair.start()
            tiny.start()
            turn_copy(2 * (3 - 1)).start()
            turn_copy(2 * (3 - 1) + 1).start()
        lead, trail = rotated(head * HD)
        queries[:, head * HD : head * HD + half] = (lead * scale).astype(queries.dtype)
        queries[:, head * HD + half : (head + 1) * HD] = (trail * scale).astype(queries.dtype)
    pair.wait()
    for at in range(7):
        if at // 2 != 2:
            turn_copy(at).start()

    def one_head(head, _):
        query = queries[:, pl.ds(pl.multiple_of(head * HD, HD), HD)]
        scores = jnp.concatenate([dot_nt(query, kv[0, :, :HD]), dot_nt(query, kv[1, :, :HD])], axis=1)
        scores = jnp.where(mask[...] > 0, scores, NEG)
        expd = jnp.exp(scores - jnp.max(scores, axis=-1, keepdims=True))
        prob = expd / jnp.sum(expd, axis=-1, keepdims=True)
        probs[head] = prob
        prob_low = prob.astype(jnp.bfloat16)
        mixed = dot_nn(prob_low[:, :rows], kv[0, :, HD:]) + dot_nn(prob_low[:, rows:], kv[1, :, HD:])
        got[0, core, head // (heads // 2), head % (heads // 2)] = mixed.astype(got.dtype)
        return 0

    lax.fori_loop(0, heads, one_head, 0)
    sums[...] = jnp.zeros_like(sums)
    spread.begin()

    def blocks(across, half_at, at):
        span = pl.ds(pl.multiple_of((half_at * (heads // 2) + at) * HD, HD), HD)
        for other in range(2):
            row = row_span(here, across, other, rows)
            block = got[across, (core + other) % 2, half_at, at]
            mixed_all[row, span] = block
            sums[row, :] += dot_nn(block, w_out[span, :])

    spread.run(blocks)
    part[...] = sums[...].astype(part.dtype)
    spread.end()
    tiny.wait()
    for at in range(rows // LANES):
        values = jnp.broadcast_to(from_tile(tiny_pair[at : at + 1, :], eye), (LANES, LANES))
        pair_rms[1, at * LANES : (at + 1) * LANES, :] = values
    own_turn.wait()
    for at in range(7):
        turn_copy(at).wait()


def attend(qkv, rms, cos, sin, mask, w_out, cot, cid):
    rows = qkv.shape[0]
    wide, cols = w_out.shape
    heads = wide // HD
    low, f32 = jnp.bfloat16, jnp.float32
    dma = pltpu.SemaphoreType.DMA
    vm = pl.BlockSpec(memory_space=pltpu.VMEM)
    out_shape = [
        jax.ShapeDtypeStruct((8 * rows, cols), low),
        jax.ShapeDtypeStruct((8 * rows, wide), low),
        jax.ShapeDtypeStruct((8 * rows, cols), low),
        jax.ShapeDtypeStruct((2, rows, 2 * HD), low),
        jax.ShapeDtypeStruct((heads, rows, 2 * rows), f32),
        jax.ShapeDtypeStruct((rows, wide), low),
        jax.ShapeDtypeStruct((2,) + rms.shape, f32),
    ]
    scratch = spread_scratch(heads // 2, rows, HD) + [
        pltpu.VMEM((8 * rows, cols), f32), dma((4,)), dma((7,)), dma((7,)), dma(()),
        pltpu.VMEM((8, LANES), f32), pltpu.VMEM((8, LANES), f32)]
    kernel = functools.partial(attend_kernel, rows, heads, cols)
    return kernel_call(kernel, out_shape, [qkv, rms, cos, sin, mask, w_out, cot], [vm] * 7, scratch, cid,
                       "attend")


def tail_kernel(rows, heads, per, d_attn, w_out, queries, kv, probs, rms, cos, sin, act_t, w_qkv, ffn, x_low,
                attn, gain, gain_grad, mixed_all, d_tok, out, grad_query, grad_out, kv_sum, gain_tiles, *refs):
    here = Place()
    width = HD
    counts = heads // 2
    part = rows // 2
    refs = list(refs)
    line_counts = 8 * per
    cols = d_attn.shape[1]
    extra = cols // (rows // per)

    def take(count):
        taken_refs = refs[:count]
        del refs[:count]
        return taken_refs

    total_refs = take(11)
    spread = Spread(here, 1, take(7))
    d_mixed, tiny_own, tiny_all, d_kv, give, taken, give_sems, tiny_send, tiny_recv = take(9)
    grad, grad_mixed, gain_sum, tile, tile_send, tile_recv, put_sems, local_sems, mixed_two, mixed_sems = take(10)

    def far(at):
        return turned(at // per)

    def near(at):
        at = jnp.minimum(at, line_counts - 1)
        x_stream, y_stream = spread.streams(at // 4)
        second = at // 2 % 2
        across = x_stream[0] + second * (y_stream[0] - x_stream[0])
        half_at = x_stream[1] + second * (y_stream[1] - x_stream[1])
        return across, at % 2, half_at

    def place_ffn(at):
        return here.shard(*far(at)) * per + at % per

    def place_tok(at):
        across, other, half_at = near(at)
        return jnp.where(at < line_counts, here.shard(across, other) * per + half_at, at)

    ffn_sum = take(1)[0]
    line = Line(here, line_counts, [ffn, ffn_sum] + take(8), place_ffn)
    contrib, summed = take(2)
    line_tok = Line(here, line_counts + extra, [contrib, summed] + take(8), place_tok)
    tiny = Tiny(here, tiny_own, tiny_all, (tiny_send, tiny_recv), False)
    got, core = spread.got, here.core
    product = products(here, d_attn, w_out, True, rows, width, counts)
    total = Reduce(here, counts, product, total_refs)
    greet(here, tiny.peers, True)
    line.begin()
    grad_mixed[...] = jnp.zeros_like(grad_mixed)

    def mixed_copy(step):
        span = pl.ds(pl.multiple_of(step * rows, rows), rows)
        return pltpu.make_async_copy(mixed_all.at[span, :], mixed_two.at[step % 2], mixed_sems.at[step % 2])

    mixed_copy(0).start()

    def beside(step):
        line.step(step)

        @pl.when(step < 8)
        def _():
            span = pl.ds(pl.multiple_of(step * rows, rows), rows)
            mixed_copy(step).wait()

            @pl.when(step < 7)
            def _():
                mixed_copy(step + 1).start()

            grad_mixed[...] += dot_tn(mixed_two[step % 2], d_attn[span, :])

    done = total.run(beside)
    grad_out[...] = grad_mixed[...].astype(grad_out.dtype)

    def land(at, first, second):
        for half_at, value in enumerate((first, second)):
            d_mixed[:, pl.ds(pl.multiple_of((half_at * counts + at) * width, width), width)] = value.astype(
                d_mixed.dtype)

    total.end(land)
    half = HD // 2
    scale = 1.0 / math.sqrt(HD)
    depth = w_qkv.shape[0] * 8
    d_kv[...] = jnp.zeros_like(d_kv)

    def one_head(head, dots):
        span = pl.ds(pl.multiple_of(head * HD, HD), HD)
        query = queries[:, span]
        cot = d_mixed[:, span]
        prob = probs[head]
        d_prob = jnp.concatenate([dot_nt(cot, kv[0, :, HD:]), dot_nt(cot, kv[1, :, HD:])], axis=1)
        delta = jnp.sum(prob * d_prob, axis=-1, keepdims=True)
        d_score = (prob * (d_prob - delta)).astype(jnp.bfloat16)
        prob_low = prob.astype(jnp.bfloat16)
        d_query = (dot_nn(d_score[:, :rows], kv[0, :, :HD]) + dot_nn(d_score[:, rows:], kv[1, :, :HD])) * scale
        for side in range(2):
            keys = slice(side * rows, (side + 1) * rows)
            d_kv[side, :, :HD] += dot_tn(d_score[:, keys], query)
            d_kv[side, :, HD:] += dot_tn(prob_low[:, keys], cot)
        dots = dots + jnp.sum(d_query * query.astype(jnp.float32), axis=-1, keepdims=True)
        lead, trail = d_query[:, :half], d_query[:, half:]
        first = ((lead * cos[0] + trail * sin[0]) * rms[0]).astype(got.dtype)
        second = ((trail * cos[0] - lead * sin[0]) * rms[0]).astype(got.dtype)
        for rows_at in range(2):
            piece = slice(rows_at * part, (rows_at + 1) * part)
            got[0, core, rows_at, 0, :, pl.ds(pl.multiple_of(head * HD, HD), half)] = first[piece, :]
            got[0, core, rows_at, 0, :, pl.ds(pl.multiple_of(head * HD + half, half), half)] = second[piece, :]

        line.step(done + head)
        return dots

    dots = lax.fori_loop(0, heads, one_head, jnp.zeros((rows, 1), jnp.float32))
    done += heads
    eye = diagonal()
    tiny_own[...] = jnp.zeros_like(tiny_own)
    for side in (1, 0):
        d_key, d_value = d_kv[side, :, :HD], d_kv[side, :, HD:]
        own = jnp.sum(d_key * kv[side, :, :HD].astype(jnp.float32) +
                      d_value * kv[side, :, HD:].astype(jnp.float32), axis=-1, keepdims=True)
        if side == 0:
            own = own + dots * (1.0 / scale)
        own = own * (rms[side] * rms[side] * (1.0 / depth))
        to_tile(tiny_own, side * (rows // LANES), own, eye)
        lead, trail = d_key[:, :half], d_key[:, half:]
        parts = [(lead * cos[side] + trail * sin[side]) * rms[side],
                 (trail * cos[side] - lead * sin[side]) * rms[side],
                 d_value[:, :half] * rms[side], d_value[:, half:] * rms[side]]
        for at, value in enumerate(parts):
            if side == 1:
                give[:, at * half : (at + 1) * half] = value.astype(give.dtype)
            else:
                d_kv[0, :, at * half : (at + 1) * half] = value
    given = remote(give, taken, give_sems.at[0], give_sems.at[1], spread.ydev)
    given.start()
    grad[...] = jnp.zeros_like(grad)
    given.wait()
    for rows_at in range(2):
        piece = slice(rows_at * part, (rows_at + 1) * part)
        value = d_kv[0, piece, :] + taken[piece, :].astype(jnp.float32)
        got[0, core, rows_at, 0, :, heads * HD :] = value.astype(got.dtype)
    tiny.begin()
    for hop in range(2):
        spread.x_copy(hop, 0).start()
        spread.y_copy(hop, 0).start()
    for stream in range(2):
        spread.sib_copy(0, stream, 0).start()
    gain_sum[...] = jnp.zeros_like(gain_sum)
    line.steps(done, line_counts + 2)
    tiny.end()

    def block_of(at):
        across, other, half_at = near(at)
        shard, partner = here.shard(across, other), here.shard((across + 2) % 4, other)
        block = got[across, (core + other) % 2, half_at, 0]
        first = pl.multiple_of(shard * rows + half_at * part, part)
        for tile_at in range(part // LANES):
            row = pl.ds(pl.multiple_of(first + tile_at * LANES, LANES), LANES)
            low_at = half_at * (part // LANES) + tile_at
            kept = rows // LANES + low_at
            dot = from_tile(tiny_all[shard, pl.ds(low_at, 1), :] + tiny_all[partner, pl.ds(kept, 1), :], eye)
            value = dot_nt(block[tile_at * LANES : (tile_at + 1) * LANES, :], w_qkv[...])
            x_rows = x_low[row, :].astype(jnp.float32)
            contrib[row, :] = (value * gain[...] - x_rows * dot).astype(contrib.dtype)
            gain_sum[...] += jnp.sum(value * x_rows, axis=0, keepdims=True)
        line_tok.launch(at, 1)
        rows_t = act_t[:, pl.ds(first, part)]
        for at_col in range((heads + 2) * HD // 512):
            span = slice(at_col * 512, (at_col + 1) * 512)
            grad[:, span] += dot_nn(rows_t, block[:, span])

    me = here.shard(0, 0)
    columns = pl.ds(pl.multiple_of(me * cols, cols), cols)
    chunk = line.chunk

    def landing(which, at):
        sub = at % per if which == 0 else near(at)[2]
        return (out, d_tok)[which].at[pl.ds(pl.multiple_of(sub * chunk, chunk), chunk), columns]

    def put(which, at):
        kind = (line, line_tok)[which]
        goal = here.device(*(far(at) if which == 0 else near(at)[:2]))
        return remote(kind.from_end.at[at], landing(which, at), put_sems.at[which, 0, at], put_sems.at[which, 1, at],
                      goal)

    def keep(which, at):
        spot = at % per if which == 0 else near(at)[2]
        return pltpu.make_async_copy((line, line_tok)[which].from_end.at[at], landing(which, at),
                                     local_sems.at[which, spot])

    def emit(which, at):
        kind = (line, line_tok)[which]
        row = kind.rows(at)
        base = (attn, d_attn)[which][row, :].astype(jnp.float32)
        if which == 0:
            base = base + x_low[row, :].astype(jnp.float32)
        kind.from_end[at] = (base + kind.out[row, :].astype(jnp.float32)).astype(out.dtype)

    def is_own(which, at):
        return at >= 7 * per if which == 0 else jnp.logical_and(at < 4, at % 2 == 0)

    def send(which, at):
        own = is_own(which, at)

        @pl.when(own)
        def _():
            keep(which, at).start()

        @pl.when(jnp.logical_not(own))
        def _():
            put(which, at).start()

    def stage_step(step, _):
        stage = step // 4

        @pl.when(jnp.logical_and(step % 4 == 0, jnp.logical_and(stage > 0, stage < 4)))
        def _():
            spread.x_copy(stage - 1, 0).wait_recv()
            spread.sib_copy(stage, 0, 0).start()
            spread.y_copy(stage - 1, 0).wait_recv()
            spread.sib_copy(stage, 1, 0).start()

        @pl.when(step == 4)
        def _():
            spread.x_copy(2, 0).start()
            spread.y_copy(2, 0).start()

        @pl.when(step < line_counts)
        def _():
            for stream in range(2):
                @pl.when(step % 4 == 2 * stream)
                def _(stream=stream):
                    spread.sib_copy(stage, stream, 0).wait_recv()

            block_of(step)

        @pl.when(step >= 4)
        def _():
            line_tok.step(step - 4)

        @pl.when(step > 0)
        def _():
            send(0, step - 1)

        @pl.when(line.inner == 0)
        def _():
            line.up(step).wait_send()
            line.down(step).wait_recv()

        emit(0, step)

        @pl.when(jnp.logical_and(line.inner == 1, step > 7))
        def _():
            send(1, step - 8)

        @pl.when(jnp.logical_and(line.inner == 1, step > 6))
        def _():
            emit(1, step - 7)
        return 0

    lax.fori_loop(0, line_counts, stage_step, 0)
    for half_at in range(cols // (rows // per)):
        span = pl.ds(line_counts * (rows // per) + half_at * (rows // per), rows // per)
        source = slice(half_at * (rows // per), (half_at + 1) * (rows // per))
        contrib[span, :] = grad[source, heads * HD :].astype(contrib.dtype)
    line_tok.launch(line_counts, extra)
    grad_query[...] = grad[:, : heads * HD].astype(grad_query.dtype)
    for at in range(cols // LANES):
        tile[at : at + 1, :] = gain_sum[:, at * LANES : (at + 1) * LANES]
        spot = cols // LANES + at
        tile[spot : spot + 1, :] = gain_grad[:, at * LANES : (at + 1) * LANES]

    def tile_copy(step):
        return remote(tile, gain_tiles.at[here.z], tile_send.at[step], tile_recv.at[step],
                      (here.dp, here.seq, (here.z + step + 1) % 4))

    send(0, line_counts - 1)
    line.drain()
    for step in range(3):
        tile_copy(step).start()
    gain_tiles[here.z] = tile[...]

    @pl.when(line.inner == 1)
    def _():
        start = line_counts - 4

        def both(at, _):
            line_tok.step(at)

            @pl.when(at < line_counts + 4)
            def _():
                send(1, at - 4)

            @pl.when(at < line_counts + 3)
            def _():
                emit(1, at - 3)
            return 0

        lax.fori_loop(start, line_counts + extra + 2, both, 0)

        def drain(at, _):
            line_tok.down(at).wait_send()
            return 0

        lax.fori_loop(0, line_counts + extra, drain, 0)

    @pl.when(line.inner == 0)
    def _():
        def arrive(at, _):
            line_tok.up(at).wait_send()
            line_tok.down(at).wait_recv()

            @pl.when(jnp.logical_and(at > 0, at <= line_counts))
            def _():
                send(1, at - 1)

            @pl.when(at < line_counts)
            def _():
                emit(1, at)
            return 0

        lax.fori_loop(0, line_counts + extra, arrive, 0)

    for half_at in range(extra):
        span = pl.ds((line_counts + half_at) * chunk, chunk)
        kv_sum[half_at * chunk : (half_at + 1) * chunk, :] = summed[span, :]
    for hop in range(3):
        spread.x_copy(hop, 0).wait_send()
        spread.y_copy(hop, 0).wait_send()
    for stage in range(4):
        spread.sib_copy(stage, 0, 0).wait_send()
        spread.sib_copy(stage, 1, 0).wait_send()

    def finish(at, _):
        for which in range(2):
            own = is_own(which, at)

            @pl.when(own)
            def _():
                keep(which, at).wait()

            @pl.when(jnp.logical_not(own))
            def _():
                put(which, at).wait()
        return 0

    lax.fori_loop(0, line_counts, finish, 0)
    for step in range(3):
        tile_copy(step).wait()


def tail(d_attn, w_out, queries, kv, probs, rms, cos, sin, act_t, w_qkv, ffn, x_low, attn, gain, gain_grad,
         mixed_all, cid,
 per=2):
    total, cols = d_attn.shape
    rows = total // 8
    wide = w_out.shape[0]
    heads = wide // HD
    low, f32 = jnp.bfloat16, jnp.float32
    dma = pltpu.SemaphoreType.DMA
    vm = pl.BlockSpec(memory_space=pltpu.VMEM)
    counts = 8 * per
    chunk = rows // per
    extra = cols // chunk
    long = (total + cols, cols)
    out_shape = [
        jax.ShapeDtypeStruct((rows, 8 * cols), low),
        jax.ShapeDtypeStruct((rows, 8 * cols), low),
        jax.ShapeDtypeStruct((cols, wide), low),
        jax.ShapeDtypeStruct(w_out.shape, low),
        jax.ShapeDtypeStruct((cols, 2 * HD), low),
        jax.ShapeDtypeStruct((4, 8, LANES), f32),
    ]
    scratch = reduce_scratch(heads // 2, rows, HD, 2) + spread_scratch(1, rows // 2, wide + 2 * HD)
    scratch += [
        pltpu.VMEM((rows, wide), low),
        pltpu.VMEM((8, LANES), f32),
        pltpu.VMEM((8, 8, LANES), f32),
        pltpu.VMEM((2, rows, 2 * HD), f32),
        pltpu.VMEM((rows, 2 * HD), low),
        pltpu.VMEM((rows, 2 * HD), low),
        dma((2,)), dma((7,)), dma((7,)),
        pltpu.VMEM(w_qkv.shape, f32),
        pltpu.VMEM(w_out.shape, f32),
        pltpu.VMEM((1, cols), f32),
        pltpu.VMEM((8, LANES), f32),
        dma((3,)), dma((3,)), dma((2, 2, counts)), dma((2, per)),
        pltpu.VMEM((2, rows, wide), low), dma((2,)),
        pltpu.VMEM((total, cols), low),
    ] + line_scratch(counts, (total, cols), low)
    scratch += [pltpu.VMEM(long, low), pltpu.VMEM(long, low)] + line_scratch(counts + extra, long, low)
    operands = [d_attn, w_out, queries, kv, probs, rms, cos, sin, act_t, w_qkv, ffn, x_low, attn, gain,
                gain_grad, mixed_all]
    kernel = functools.partial(tail_kernel, rows, heads, per)
    specs = [vm] * (len(operands) - 1) + [pl.BlockSpec(memory_space=pl.ANY)]
    return kernel_call(kernel, out_shape, operands, specs, scratch, cid, "tail")


LANES = 128


def acts_move(
    tokens, seg_ids, gain_attn, w_query, kv_weight, w_out, gain_ffn, w_gate, w_up, w_down, d_out
):
    rows = tokens.shape[0]
    segs = seg_ids.astype(jnp.float32).reshape(2 * rows // LANES, LANES)
    segs = jnp.pad(segs, ((0, 8 - 2 * rows // LANES), (0, 0)))
    gain_one = gain_attn.astype(jnp.float32)[None, :]
    gain_two = gain_ffn.astype(jnp.float32)[None, :]
    wider = jnp.float32

    qkv, x_low, act_one_t, w_qkv, rms, cos, sin, mask = opening(
        tokens, gain_one, w_query, kv_weight, segs, 1
    )
    attn_part, mixed_all, g_low, kv, probs, queries, pair_rms = attend(
        qkv, rms, cos, sin, mask, w_out, d_out, 2
    )
    d_hidden, attn = scatter_product(g_low, w_down, 512, 3, attn_part)
    hidden, d_gate, d_up, act_two_t, dots = ffn_scatter(x_low, attn, gain_two, w_gate, w_up, d_hidden, 4)
    contrib, grad_gain_two, grad_gate, grad_up = back_gather(
        act_two_t, w_gate, w_up, d_gate, d_up, dots, x_low, attn, gain_two, 5
    )
    ffn, d_attn, grad_down = down_gather(g_low, w_down, hidden, contrib, 6)
    d_tokens, out, grad_query, grad_out, grad_kv, gain_tiles = tail(
        d_attn,
        w_out,
        queries,
        kv,
        probs,
        pair_rms,
        cos,
        sin,
        act_one_t,
        w_qkv,
        ffn,
        x_low,
        attn,
        gain_one,
        grad_gain_two,
        mixed_all,
        7,
    )
    gains = jnp.sum(gain_tiles, axis=0).reshape(2, -1)
    return (
        out,
        d_tokens.astype(wider),
        gains[0],
        grad_query.astype(wider),
        grad_kv.astype(wider),
        grad_out.astype(wider),
        gains[1],
        grad_gate.astype(wider),
        grad_up.astype(wider),
        grad_down.astype(wider),
    )


def solution(mesh):
    in_specs = (
        P(("dp", "seq"), None),
        P("dp"),
        P(("dp", "seq")),
        P(("dp", "seq"), "tensor"),
        P(("dp", "seq"), None),
        P("tensor", ("dp", "seq")),
        P(("dp", "seq")),
        P(("dp", "seq"), "tensor"),
        P(("dp", "seq"), "tensor"),
        P("tensor", ("dp", "seq")),
        P(("dp", "seq"), None),
    )
    out_specs = (
        P(("dp", "seq"), None),
        P(("dp", "seq"), None),
        P(("dp", "seq")),
        P(("dp", "seq"), "tensor"),
        P(("dp", "seq"), None),
        P("tensor", ("dp", "seq")),
        P(("dp", "seq")),
        P(("dp", "seq"), "tensor"),
        P(("dp", "seq"), "tensor"),
        P("tensor", ("dp", "seq")),
    )

    def shards(*arrays):
        tokens = arrays[0]
        sizes = tuple(mesh.shape[name] for name in ("dp", "seq", "tensor"))
        count = tokens.shape[0] * sizes[0] * sizes[1]
        plan = acts_move if sizes == (4, 2, 4) and count <= tokens.shape[1] else weights_move
        return plan(*arrays)

    return jax.shard_map(shards, mesh=mesh, in_specs=in_specs, out_specs=out_specs, check_vma=False)
```

```python
import functools
import math

import jax
import jax.numpy as jnp
from jax import lax
from jax.experimental import pallas as pl
from jax.experimental.pallas import tpu as pltpu
from jax.sharding import PartitionSpec as P

HD = 256


EPS = 1e-06
NEG = -1e30


def place_tables(segs):
    length = segs.shape[0]
    index = jnp.arange(length, dtype=jnp.int32)
    flags = jnp.concatenate([jnp.ones((1,), dtype=bool), segs[1:] != segs[:-1]])
    starts = lax.cummax(jnp.where(flags, index, jnp.zeros_like(index)), axis=0)
    places = index - starts
    half_size = HD // 2
    freqs = jnp.exp(jnp.arange(half_size, dtype=jnp.float32) * (-math.log(10000.0) / half_size))
    angles = places.astype(jnp.float32)[:, None] * freqs[None, :]
    return (places, jnp.cos(angles), jnp.sin(angles))


def rotate(vector, cos_table, sin_table):
    half_size = vector.shape[-1] // 2
    leading = vector[..., :half_size]
    trailing = vector[..., half_size:]
    return jnp.concatenate(
        [leading * cos_table - trailing * sin_table, trailing * cos_table + leading * sin_table],
        axis=-1,
    )


def rotate_back(vector, cos_table, sin_table):
    half_size = vector.shape[-1] // 2
    leading = vector[..., :half_size]
    trailing = vector[..., half_size:]
    return jnp.concatenate(
        [leading * cos_table + trailing * sin_table, trailing * cos_table - leading * sin_table],
        axis=-1,
    )


def matmul(left, right):
    return jnp.dot(left, right, preferred_element_type=jnp.float32)


def matmul_nt(left, right):
    return lax.dot_general(
        left, right, (((1,), (1,)), ((), ())), preferred_element_type=jnp.float32
    )


def matmul_tn(left, right):
    return lax.dot_general(
        left, right, (((0,), (0,)), ((), ())), preferred_element_type=jnp.float32
    )


def gelu_tanh(values):
    return jax.nn.gelu(values, approximate=True)


def norm_back(d_act, normed, rms_val, gain_val):
    scaled = d_act * gain_val
    return rms_val * (scaled - normed * jnp.mean(scaled * normed, axis=-1, keepdims=True))


def weights_move(
    tokens, seg_ids, gain_attn, w_query, kv_weight, w_out, gain_ffn, w_gate, w_up, w_down, d_out
):
    rows = tokens.shape[0]
    scale_factor = 1.0 / math.sqrt(HD)
    offset = lax.axis_index("seq") * rows
    places, cos_table, sin_table = place_tables(seg_ids)
    own_places = lax.dynamic_slice_in_dim(places, offset, rows, 0)
    own_segs = lax.dynamic_slice_in_dim(seg_ids, offset, rows, 0)
    own_cos = lax.dynamic_slice_in_dim(cos_table, offset, rows, 0)
    own_sin = lax.dynamic_slice_in_dim(sin_table, offset, rows, 0)
    allowed = (own_segs[:, None] == seg_ids[None, :]) & (own_places[:, None] >= places[None, :])
    full_query, full_out, full_kv, full_gain_one = (
        lax.all_gather(w_query, ("dp", "seq"), axis=0, tiled=True),
        lax.all_gather(w_out, ("dp", "seq"), axis=1, tiled=True),
        lax.all_gather(kv_weight, ("dp", "seq"), axis=0, tiled=True),
        lax.all_gather(gain_attn, ("dp", "seq"), axis=0, tiled=True),
    )
    gain_one = full_gain_one.astype(jnp.float32)
    inputs = tokens.astype(jnp.float32)
    rms_one = lax.rsqrt(jnp.mean(inputs * inputs, axis=-1, keepdims=True) + EPS)
    norm_one = inputs * rms_one
    act_one = (norm_one * gain_one).astype(jnp.bfloat16)
    query_pre = matmul(act_one, full_query)
    heads = query_pre.shape[1] // HD
    kv_pre = matmul(act_one, full_kv)
    queries = (
        rotate(query_pre.reshape(rows, heads, HD), own_cos[:, None, :], own_sin[:, None, :])
        * scale_factor
    ).astype(jnp.bfloat16)
    own_kv = jnp.concatenate(
        [rotate(kv_pre[:, :HD], own_cos, own_sin), kv_pre[:, HD:]], axis=1
    ).astype(jnp.bfloat16)
    all_kv = lax.all_gather(own_kv, "seq", axis=0, tiled=True)
    keys = all_kv[:, :HD]
    values_all = all_kv[:, HD:]
    scores = jnp.einsum("rhd,kd->hrk", queries, keys, preferred_element_type=jnp.float32)
    scores = jnp.where(allowed[None], scores, NEG)
    top_score = jnp.max(scores, axis=-1, keepdims=True)
    expd = jnp.exp(scores - top_score)
    total = jnp.sum(expd, axis=-1, keepdims=True)
    log_total = top_score + jnp.log(total)
    probs_low = (expd / total).astype(jnp.bfloat16)
    mixed = (
        jnp.einsum("hrk,kd->rhd", probs_low, values_all, preferred_element_type=jnp.float32)
        .reshape(rows, heads * HD)
        .astype(jnp.bfloat16)
    )
    attn = lax.psum(matmul(mixed, full_out), "tensor")
    resid = inputs + attn
    full_gate, full_up, full_down, full_gain_two = (
        lax.all_gather(w_gate, ("dp", "seq"), axis=0, tiled=True),
        lax.all_gather(w_up, ("dp", "seq"), axis=0, tiled=True),
        lax.all_gather(w_down, ("dp", "seq"), axis=1, tiled=True),
        lax.all_gather(gain_ffn, ("dp", "seq"), axis=0, tiled=True),
    )
    gain_two = full_gain_two.astype(jnp.float32)
    rms_two = lax.rsqrt(jnp.mean(resid * resid, axis=-1, keepdims=True) + EPS)
    norm_two = resid * rms_two
    act_two = (norm_two * gain_two).astype(jnp.bfloat16)
    gate = matmul(act_two, full_gate)
    up_val = matmul(act_two, full_up)
    gelu_val, gelu_pull = jax.vjp(gelu_tanh, gate)
    hidden = (gelu_val * up_val).astype(jnp.bfloat16)
    ffn = lax.psum(matmul(hidden, full_down).astype(jnp.bfloat16), "tensor").astype(jnp.float32)
    out = (resid + ffn).astype(jnp.bfloat16)
    back_gate, back_up, back_down = (
        lax.all_gather(w_gate, ("dp", "seq"), axis=0, tiled=True),
        lax.all_gather(w_up, ("dp", "seq"), axis=0, tiled=True),
        lax.all_gather(w_down, ("dp", "seq"), axis=1, tiled=True),
    )
    d_hidden = matmul_nt(d_out, back_down)
    grad_down = matmul_tn(hidden, d_out)
    d_gate = gelu_pull(d_hidden * up_val)[0].astype(jnp.bfloat16)
    d_up = (d_hidden * gelu_val).astype(jnp.bfloat16)
    grad_gate = matmul_tn(act_two, d_gate)
    grad_up = matmul_tn(act_two, d_up)
    d_act_two = lax.psum(matmul_nt(d_gate, back_gate) + matmul_nt(d_up, back_up), "tensor")
    grad_gain_two = jnp.sum(d_act_two * norm_two, axis=0)
    d_resid = d_out.astype(jnp.float32) + norm_back(d_act_two, norm_two, rms_two, gain_two)
    ffn_grads = (
        lax.psum_scatter(
            grad_gate.astype(jnp.bfloat16), ("dp", "seq"), scatter_dimension=0, tiled=True
        ).astype(jnp.float32),
        lax.psum_scatter(
            grad_up.astype(jnp.bfloat16), ("dp", "seq"), scatter_dimension=0, tiled=True
        ).astype(jnp.float32),
        lax.psum_scatter(
            grad_down.astype(jnp.bfloat16), ("dp", "seq"), scatter_dimension=1, tiled=True
        ).astype(jnp.float32),
        lax.psum_scatter(
            grad_gain_two.astype(jnp.bfloat16), ("dp", "seq"), scatter_dimension=0, tiled=True
        ).astype(jnp.float32),
    )
    back_query, back_out, back_kv = (
        lax.all_gather(w_query, ("dp", "seq"), axis=0, tiled=True),
        lax.all_gather(w_out, ("dp", "seq"), axis=1, tiled=True),
        lax.all_gather(kv_weight, ("dp", "seq"), axis=0, tiled=True),
    )
    d_attn = d_resid.astype(jnp.bfloat16)
    grad_out = matmul_tn(mixed, d_attn)
    d_mixed = matmul_nt(d_attn, back_out).astype(jnp.bfloat16).reshape(rows, heads, HD)
    scores_again = jnp.einsum("rhd,kd->hrk", queries, keys, preferred_element_type=jnp.float32)
    probs = jnp.where(allowed[None], jnp.exp(scores_again - log_total), 0.0)
    d_probs = jnp.einsum("rhd,kd->hrk", d_mixed, values_all, preferred_element_type=jnp.float32)
    delta = jnp.sum(probs * d_probs, axis=-1, keepdims=True)
    d_scores = (probs * (d_probs - delta)).astype(jnp.bfloat16)
    d_queries = (
        jnp.einsum("hrk,kd->rhd", d_scores, keys, preferred_element_type=jnp.float32) * scale_factor
    )
    d_query_pre = (
        rotate_back(d_queries, own_cos[:, None, :], own_sin[:, None, :])
        .reshape(rows, heads * HD)
        .astype(jnp.bfloat16)
    )
    d_keys_part = jnp.einsum("hrk,rhd->kd", d_scores, queries, preferred_element_type=jnp.float32)
    d_values_part = jnp.einsum(
        "hrk,rhd->kd", probs.astype(jnp.bfloat16), d_mixed, preferred_element_type=jnp.float32
    )
    own_kv_grad = lax.psum_scatter(
        jnp.concatenate([d_keys_part, d_values_part], axis=1).astype(jnp.bfloat16),
        "seq",
        scatter_dimension=0,
        tiled=True,
    )
    d_act_query = matmul_nt(d_query_pre, back_query)
    d_act_sum, kv_grad = (
        lax.psum(d_act_query.astype(jnp.bfloat16), "tensor").astype(jnp.float32),
        lax.psum(own_kv_grad, "tensor").astype(jnp.float32),
    )
    d_kv_pre = jnp.concatenate(
        [rotate_back(kv_grad[:, :HD], own_cos, own_sin), kv_grad[:, HD:]], axis=1
    ).astype(jnp.bfloat16)
    d_act_one = d_act_sum + matmul_nt(d_kv_pre, back_kv)
    grad_query = matmul_tn(act_one, d_query_pre)
    grad_kv = matmul_tn(act_one, d_kv_pre)
    grad_gain_one = jnp.sum(d_act_one * norm_one, axis=0)
    d_tokens = d_resid + norm_back(d_act_one, norm_one, rms_one, gain_one)
    attn_grads = (
        lax.psum_scatter(
            grad_query.astype(jnp.bfloat16), ("dp", "seq"), scatter_dimension=0, tiled=True
        ).astype(jnp.float32),
        lax.psum_scatter(
            grad_out.astype(jnp.bfloat16), ("dp", "seq"), scatter_dimension=1, tiled=True
        ).astype(jnp.float32),
        lax.psum_scatter(
            grad_kv.astype(jnp.bfloat16), ("dp", "seq"), scatter_dimension=0, tiled=True
        ).astype(jnp.float32),
        lax.psum_scatter(
            grad_gain_one.astype(jnp.bfloat16), ("dp", "seq"), scatter_dimension=0, tiled=True
        ).astype(jnp.float32),
    )
    return (
        out,
        d_tokens,
        attn_grads[3],
        attn_grads[0],
        attn_grads[2],
        attn_grads[1],
        ffn_grads[3],
        ffn_grads[0],
        ffn_grads[1],
        ffn_grads[2],
    )


MESH = pl.DeviceIdType.MESH
VMEM_LIMIT = 66000 * 1024


class Place:
    def __init__(self):
        self.dp = lax.axis_index("dp")
        self.seq = lax.axis_index("seq")
        self.z = lax.axis_index("tensor")
        self.core = lax.rem(self.dp, 2)
        self.chip = lax.div(self.dp, 2)

    def device(self, across, other):
        chip = (self.chip + across) % 2
        seq = (self.seq + across // 2) % 2
        core = (self.core + other) % 2
        return chip * 2 + core, seq, self.z

    def shard(self, across, other):
        dp, seq, _ = self.device(across, other)
        return dp * 2 + seq


def greet(here, peers, line=False):
    barrier = pltpu.get_barrier_semaphore()
    peers = list(peers)
    if line:
        peers += [(here.dp, here.seq, (here.z + step) % 4) for step in range(1, 4)]
    for peer in peers:
        pl.semaphore_signal(barrier, inc=1, device_id=peer, device_id_type=MESH)
    pl.semaphore_wait(barrier, len(peers))


def remote(src, dst, send, recv, peer):
    return pltpu.make_async_remote_copy(
        src_ref=src, dst_ref=dst, send_sem=send, recv_sem=recv, device_id=peer, device_id_type=MESH
    )


class Line:
    def __init__(self, here, counts, refs, place=None):
        self.own, self.out, self.from_end, self.from_mid = refs[:4]
        self.sems = refs[4:10]
        self.counts = counts
        self.chunk = self.from_end.shape[1]
        self.place = place
        z = here.z
        self.inner = ((z + 1) // 2) % 2
        self.mate = (here.dp, here.seq, z + 1 - 2 * (z % 2))
        self.other = (here.dp, here.seq, 3 - z)

    def rows(self, at):
        at = at if self.place is None else self.place(at)
        return pl.ds(pl.multiple_of(at * self.chunk, self.chunk), self.chunk)

    def up(self, at):
        return remote(self.own.at[self.rows(at), :], self.from_end.at[at], self.sems[0].at[at],
                      self.sems[1].at[at], self.mate)

    def over(self, at):
        return remote(self.out.at[self.rows(at), :], self.from_mid.at[at], self.sems[2].at[at],
                      self.sems[3].at[at], self.other)

    def down(self, at):
        rows = self.rows(at)
        return remote(self.out.at[rows, :], self.out.at[rows, :], self.sems[4].at[at],
                      self.sems[5].at[at], self.mate)

    def launch(self, first, count):
        @pl.when(self.inner == 0)
        def _():
            def send(at, _):
                self.up(first + at).start()
                return 0

            lax.fori_loop(0, count, send, 0)

    def begin(self):
        self.launch(0, self.counts)

    def first(self, at):
        rows = self.rows(at)
        self.up(at).wait_recv()
        total = self.own[rows, :].astype(jnp.float32) + self.from_end[at].astype(jnp.float32)
        self.out[rows, :] = total.astype(self.out.dtype)
        self.over(at).start()

    def second(self, at):
        rows = self.rows(at)
        self.over(at).wait()
        total = self.out[rows, :].astype(jnp.float32) + self.from_mid[at].astype(jnp.float32)
        self.out[rows, :] = total.astype(self.out.dtype)
        self.down(at).start()

    def step(self, at, start=0, count=None):
        count = self.counts if count is None else count

        @pl.when(jnp.logical_and(self.inner == 1, at < count))
        def _():
            self.first(start + at)

        @pl.when(jnp.logical_and(self.inner == 1, jnp.logical_and(at > 1, at < count + 2)))
        def _():
            self.second(start + at - 2)

    def steps(self, first, last, start=0, count=None):
        def rest(at, _):
            self.step(at, start, count)
            return 0

        lax.fori_loop(first, last, rest, 0)

    def settle(self):
        @pl.when(self.inner == 0)
        def _():
            def take(at, _):
                self.up(at).wait_send()
                self.down(at).wait_recv()
                return 0

            lax.fori_loop(0, self.counts, take, 0)

        self.drain()

    def drain(self):
        @pl.when(self.inner == 1)
        def _():
            def drain(at, _):
                self.down(at).wait_send()
                return 0

            lax.fori_loop(0, self.counts, drain, 0)

    def end(self, done=0):
        self.steps(min(done, self.counts + 2), self.counts + 2)
        self.settle()


def line_scratch(counts, shape, low):
    buf = pltpu.VMEM((counts, shape[0] // counts, shape[1]), low)
    return [buf, buf] + [pltpu.SemaphoreType.DMA((counts,))] * 6


def turned(at):
    return 3 - at // 2, 1 - at % 2


def slice_peers(here):
    return [here.device(*turned(at)) for at in range(7)]


def kernel_call(kernel, out_shape, operands, specs, scratch, cid, name, out_specs=None):
    vm = pl.BlockSpec(memory_space=pltpu.VMEM)
    return pl.pallas_call(
        kernel,
        out_shape=out_shape,
        in_specs=specs,
        out_specs=out_specs or [vm] * len(out_shape),
        scratch_shapes=scratch,
        compiler_params=pltpu.CompilerParams(
            collective_id=cid, has_side_effects=True, vmem_limit_bytes=VMEM_LIMIT
        ),
        name=f"{name}_{cid}",
    )(*operands)


class Tiny:
    def __init__(self, here, src, dst, sems, spread):
        self.here, self.src, self.dst, self.sems, self.spread = here, src, dst, sems, spread
        self.peers = slice_peers(here)
        self.me = here.shard(0, 0)

    def tile(self, shard):
        return self.src.at[shard] if self.spread else self.src

    def copy(self, at):
        return remote(self.tile(self.here.shard(*turned(at))), self.dst.at[self.me], self.sems[0].at[at],
                      self.sems[1].at[at], self.peers[at])

    def begin(self):
        for at in range(7):
            self.copy(at).start()
        self.dst[self.me] = self.tile(self.me)[...]

    def end(self):
        for at in range(7):
            self.copy(at).wait()


class Reduce:
    def __init__(self, here, counts, product, refs, before=None):
        self.counts, self.product, self.before = counts, product, before
        self.held, self.sib_out, self.sib_in, self.from_x, self.from_y = refs[:5]
        self.sib_sems, self.x_sems, self.y_sems = refs[5:7], refs[7:9], refs[9:11]
        self.sib, self.xdev, self.ydev = here.device(0, 1), here.device(1, 0), here.device(2, 0)
        self.steps = 4 * counts
        self.ring = self.sib_out.shape[0]

    def streams(self, stage):
        far = stage // 3
        x_chip = jnp.where(stage == 0, 3, jnp.where(stage == 2, 0, 1))
        y_chip = jnp.where(stage == 0, 3, jnp.where(stage == 2, 0, 2))
        return (x_chip, far), (y_chip, 1 - far)

    def to_sib(self, step, stream):
        stage, at = step // self.counts, step % self.counts
        return remote(self.sib_out.at[step % self.ring, stream], self.sib_in.at[stage, stream, at],
                      self.sib_sems[0].at[stage, stream, at], self.sib_sems[1].at[stage, stream, at], self.sib)

    def to_x(self, hop, at, stage=0):
        return remote(self.held.at[stage, 0, at], self.from_x.at[hop, at], self.x_sems[0].at[hop, at],
                      self.x_sems[1].at[hop, at], self.xdev)

    def to_y(self, hop, at, stage=0):
        return remote(self.held.at[stage, 1, at], self.from_y.at[hop, at], self.y_sems[0].at[hop, at],
                      self.y_sems[1].at[hop, at], self.ydev)

    def compute(self, step):
        stage, at = step // self.counts, step % self.counts
        if self.before:
            for stop in range(3):
                @pl.when(step == stop * self.counts)
                def _():
                    self.before(stop)

        @pl.when(step >= self.ring)
        def _():
            for stream in range(2):
                self.to_sib(step - self.ring, stream).wait_send()

        for stream, (across, half) in enumerate(self.streams(stage)):
            self.sib_out[step % self.ring, stream] = self.product(across, 1, half, at).astype(jnp.bfloat16)
            self.held[stage, stream, at] = self.product(across, 0, half, at).astype(jnp.bfloat16)
        for stream in range(2):
            self.to_sib(step, stream).start()

    def finish(self, step):
        stage, at = step // self.counts, step % self.counts
        for stream in range(2):
            self.to_sib(step, stream).wait_recv()

        def total(stream):
            return self.held[stage, stream, at].astype(jnp.float32) + self.sib_in[stage, stream, at].astype(
                jnp.float32)

        @pl.when(stage < 3)
        def _():
            for stream in range(2):
                self.held[stage, stream, at] = total(stream).astype(jnp.bfloat16)

        @pl.when(stage == 3)
        def _():
            self.to_y(0, at).wait_recv()
            self.held[3, 0, at] = (total(0) + self.from_y[0, at].astype(jnp.float32)).astype(jnp.bfloat16)
            self.to_x(0, at).wait_recv()
            self.held[3, 1, at] = (total(1) + self.from_x[0, at].astype(jnp.float32)).astype(jnp.bfloat16)

        @pl.when(stage != 2)
        def _():
            hop = stage - stage // 3
            self.to_x(hop, at, stage).start()
            self.to_y(hop, at, stage).start()

    def run(self, hook=None):
        def body(step, _):
            @pl.when(step < self.steps)
            def _():
                self.compute(step)

            @pl.when(step > 0)
            def _():
                self.finish(step - 1)

            if hook:
                hook(step)
            return 0

        lax.fori_loop(0, self.steps + 1, body, 0)
        return self.steps + 1

    def end(self, emit):
        def last(at, _):
            values = []
            for half in range(2):
                xs, ys = (1, 2) if half == 0 else (2, 1)
                self.to_x(xs, at).wait_recv()
                self.to_y(ys, at).wait_recv()
                values.append(self.held[2, half, at].astype(jnp.float32) + self.from_x[xs, at].astype(jnp.float32)
                              + self.from_y[ys, at].astype(jnp.float32))
            emit(at, *values)
            for hop in range(3):
                self.to_x(hop, at).wait_send()
                self.to_y(hop, at).wait_send()
            return 0

        lax.fori_loop(0, self.counts, last, 0)

        def drain(at, _):
            for stream in range(2):
                self.to_sib(self.steps - self.ring + at, stream).wait_send()
            return 0

        lax.fori_loop(0, self.ring, drain, 0)


def reduce_scratch(counts, rows, width, ring=4):
    low, dma = jnp.bfloat16, pltpu.SemaphoreType.DMA
    block = pltpu.VMEM((4, 2, counts, rows, width), low)
    landed = pltpu.VMEM((3, counts, rows, width), low)
    sent = pltpu.VMEM((ring, 2, rows, width), low)
    return [block, sent, block, landed, landed] + [dma((4, 2, counts))] * 2 + [dma((3, counts))] * 4


class Spread:
    def __init__(self, here, counts, refs):
        self.counts = counts
        self.got = refs[0]
        self.x_sems, self.y_sems, self.sib_sems = refs[1:3], refs[3:5], refs[5:7]
        self.core = here.core
        self.sib, self.xdev, self.ydev = here.device(0, 1), here.device(1, 0), here.device(2, 0)

    def slot(self, across, half, at):
        return self.got.at[across, self.core, half, at]

    def x_copy(self, hop, at):
        half = jnp.minimum(hop, 1)
        src = self.slot(2 * (hop // 2), half, at)
        dst = self.slot(1 + 2 * (hop // 2), half, at)
        return remote(src, dst, self.x_sems[0].at[hop, at], self.x_sems[1].at[hop, at], self.xdev)

    def y_copy(self, hop, at):
        half = 1 - jnp.minimum(hop, 1)
        src = self.slot(hop // 2, half, at)
        dst = self.slot(2 + hop // 2, half, at)
        return remote(src, dst, self.y_sems[0].at[hop, at], self.y_sems[1].at[hop, at], self.ydev)

    def streams(self, stage):
        some, last, late = jnp.minimum(stage, 1), stage // 3, stage // 2
        return (some + 2 * last, late), (2 * some + last, 1 - late)

    def sib_copy(self, stage, stream, at):
        across, half = self.streams(stage)[stream]
        slot = self.slot(across, half, at)
        spot = (stage, stream, at)
        return remote(slot, slot, self.sib_sems[0].at[spot], self.sib_sems[1].at[spot], self.sib)

    def begin(self):
        def first(at, _):
            self.x_copy(0, at).start()
            self.y_copy(0, at).start()
            return 0

        def own(at, _):
            self.sib_copy(0, 0, at).start()
            self.sib_copy(0, 1, at).start()
            return 0

        lax.fori_loop(0, self.counts, first, 0)
        lax.fori_loop(0, self.counts, own, 0)

    def run(self, blocks, hook=None, done=None):
        counts = self.counts

        def body(step, _):
            stage, at = step // counts, step % counts

            @pl.when(jnp.logical_and(stage > 0, stage < 4))
            def _():
                self.x_copy(stage - 1, at).wait_recv()
                self.sib_copy(stage, 0, at).start()
                self.y_copy(stage - 1, at).wait_recv()
                self.sib_copy(stage, 1, at).start()

            @pl.when(jnp.logical_and(stage > 0, stage < 3))
            def _():
                self.x_copy(stage, at).start()
                self.y_copy(stage, at).start()

            @pl.when(step > 0)
            def _():
                old, spot = (step - 1) // counts, (step - 1) % counts
                for stream, (across, half) in enumerate(self.streams(old)):
                    self.sib_copy(old, stream, spot).wait_recv()
                    blocks(across, half, spot)
                if done:
                    done(old, spot)

            if hook:
                hook(step)
            return 0

        lax.fori_loop(0, 4 * counts + 1, body, 0)
        return 4 * counts + 1

    def end(self):
        def drain(at, _):
            for hop in range(3):
                self.x_copy(hop, at).wait_send()
                self.y_copy(hop, at).wait_send()
            for stage in range(4):
                self.sib_copy(stage, 0, at).wait_send()
                self.sib_copy(stage, 1, at).wait_send()
            return 0

        lax.fori_loop(0, self.counts, drain, 0)


def spread_scratch(counts, rows, width):
    dma = pltpu.SemaphoreType.DMA
    return [pltpu.VMEM((4, 2, 2, counts, rows, width), jnp.bfloat16)] + [dma((3, counts))] * 4 + [
        dma((4, 2, counts))] * 2


def row_span(here, across, other, rows):
    return pl.ds(pl.multiple_of(here.shard(across, other) * rows, rows), rows)


def dot_nt(left, right):
    return lax.dot_general(left, right, (((1,), (1,)), ((), ())), preferred_element_type=jnp.float32)


def dot_tn(left, right):
    return lax.dot_general(left, right, (((0,), (0,)), ((), ())), preferred_element_type=jnp.float32)


def dot_nn(left, right):
    return jnp.dot(left, right, preferred_element_type=jnp.float32)


def products(here, act, weight, nt, rows, width, counts):
    def product(across, other, half, at):
        cols = pl.ds(pl.multiple_of((half * counts + at) * width, width), width)
        block = act[row_span(here, across, other, rows), :]
        return dot_nt(block, weight[cols, :]) if nt else dot_nn(block, weight[:, cols])

    return product


def diagonal():
    return (lax.broadcasted_iota(jnp.int32, (LANES, LANES), 0) ==
            lax.broadcasted_iota(jnp.int32, (LANES, LANES), 1)).astype(jnp.float32)


def to_tile(tile, first, column, eye):
    for at in range(column.shape[0] // LANES):
        spread = column[at * LANES : (at + 1) * LANES, :] * eye
        tile[first + at : first + at + 1, :] = jnp.sum(spread, axis=0, keepdims=True)


def from_tile(row, eye):
    return jnp.sum(eye * row, axis=1, keepdims=True)


def make_tables(here, rows, segs, cos, sin, mask):
    eye = diagonal()
    tiles = rows // LANES
    freqs = jnp.exp(lax.broadcasted_iota(jnp.int32, (1, LANES), 1).astype(jnp.float32) * (-math.log(10000.0) / LANES))
    lane = lax.broadcasted_iota(jnp.int32, (1, LANES), 1)
    line = lax.broadcasted_iota(jnp.int32, (LANES, 1), 0)

    def row_of(side, at):
        return ((here.seq + side) % 2) * tiles + at

    for side in range(2):
        for at in range(tiles):
            row = row_of(side, at)
            ids = from_tile(segs[pl.ds(row, 1), :], eye)
            before = jnp.zeros((LANES, 1), jnp.float32)
            for other in range(2 * tiles):
                smaller = segs[other : other + 1, :] < ids
                before += jnp.sum(smaller.astype(jnp.float32), axis=-1, keepdims=True)
            index = row * LANES + line
            angles = (index.astype(jnp.float32) - before) * freqs
            span = slice(at * LANES, (at + 1) * LANES)
            cos[side, span, :] = jnp.cos(angles)
            sin[side, span, :] = jnp.sin(angles)
            if side == 0:
                for key_side in range(2):
                    for key_at in range(tiles):
                        key_row = row_of(key_side, key_at)
                        same = segs[pl.ds(key_row, 1), :] == ids
                        allowed = jnp.logical_and(same, key_row * LANES + lane <= index)
                        first = key_side * rows + key_at * LANES
                        mask[span, first : first + LANES] = allowed.astype(jnp.float32)


def open_kernel(rows, width, counts, tokens, gain, w_query, kv_weight, segs, qkv, x_low, act_t, w_qkv, rms, cos, sin,
                mask, *refs):
    here = Place()
    cols = gain.shape[1]
    act, turn_send, turn_recv, local_sems = refs[:4]
    me = here.shard(0, 0)
    own_rows = pl.ds(pl.multiple_of(me * rows, rows), rows)

    def turn_copy(at):
        across, other = turned(at)
        first = pl.multiple_of(here.shard(across, other) * cols, cols)
        return remote(tokens.at[:, pl.ds(first, cols)], x_low.at[own_rows, :], turn_send.at[at], turn_recv.at[at],
                      here.device(across, other))

    wide = w_query.shape[1]
    local = [
        pltpu.make_async_copy(w_query, w_qkv.at[:, :wide], local_sems.at[0]),
        pltpu.make_async_copy(kv_weight, w_qkv.at[:, wide:], local_sems.at[1]),
        pltpu.make_async_copy(tokens.at[:, pl.ds(pl.multiple_of(me * cols, cols), cols)], x_low.at[own_rows, :],
                              local_sems.at[2]),
    ]
    for copy in local:
        copy.start()
    greet(here, slice_peers(here))
    for at in range(7):
        turn_copy(at).start()
    for copy in local:
        copy.wait()

    def squares(at, total):
        values = tokens[:, pl.ds(pl.multiple_of(at * cols, cols), cols)].astype(jnp.float32)
        return total + jnp.sum(values * values, axis=-1, keepdims=True)

    total = lax.fori_loop(0, 8, squares, jnp.zeros((rows, 1), jnp.float32))
    rms[...] = jnp.broadcast_to(lax.rsqrt(total / (8 * cols) + EPS), rms.shape)
    make_tables(here, rows, segs, cos, sin, mask)

    def prepare(first, count):
        def one(step, _):
            at = first + step
            span = row_span(here, *turned(at), rows)
            value = (x_low[span, :].astype(jnp.float32) * gain[...]).astype(act.dtype)
            act[span, :] = value
            return 0

        lax.fori_loop(0, count, one, 0)

    def before(stop):
        first, count = ((0, 2), (2, 4), (6, 2))[stop]
        for at in range(first, min(first + count, 7)):
            turn_copy(at).wait_recv()
        prepare(first, count)

    def flip():
        def one(shard, _):
            span = pl.ds(pl.multiple_of(shard * rows, rows), rows)
            act_t[:, span] = act[span, :].T
            return 0

        lax.fori_loop(0, 8, one, 0)

    product = products(here, act, w_qkv, False, rows, width, counts)
    total = Reduce(here, counts, product, refs[4:15], before)
    total.run()
    flip()

    def emit(at, first, second):
        for half, value in enumerate((first, second)):
            qkv[:, pl.ds(pl.multiple_of((half * counts + at) * width, width), width)] = value

    total.end(emit)
    for at in range(7):
        turn_copy(at).wait_send()


def opening(tokens, gain, w_query, kv_weight, segs, cid, width=256):
    rows = tokens.shape[0]
    cols, wide = w_query.shape
    every = wide + kv_weight.shape[1]
    counts = every // (2 * width)
    low, f32 = jnp.bfloat16, jnp.float32
    dma = pltpu.SemaphoreType.DMA
    vm = pl.BlockSpec(memory_space=pltpu.VMEM)
    hbm = pl.BlockSpec(memory_space=pl.ANY)
    out_shape = [
        jax.ShapeDtypeStruct((rows, every), f32),
        jax.ShapeDtypeStruct((8 * rows, cols), low),
        jax.ShapeDtypeStruct((cols, 8 * rows), low),
        jax.ShapeDtypeStruct((cols, every), low),
        jax.ShapeDtypeStruct((rows, LANES), f32),
        jax.ShapeDtypeStruct((2, rows, LANES), f32),
        jax.ShapeDtypeStruct((2, rows, LANES), f32),
        jax.ShapeDtypeStruct((rows, 2 * rows), f32),
    ]
    scratch = [pltpu.VMEM((8 * rows, cols), low), dma((7,)), dma((7,)), dma((3,))]
    scratch += reduce_scratch(counts, rows, width)
    kernel = functools.partial(open_kernel, rows, width, counts)
    return kernel_call(kernel, out_shape, [tokens, gain, w_query, kv_weight, segs],
                       [vm, vm, hbm, hbm, vm], scratch, cid, "open")


def scatter_kernel(rows, width, counts, line_counts, act, weight, line_own, out, line_out, *refs):
    here = Place()
    line = Line(here, line_counts, [line_own, line_out] + list(refs[11:]))
    product = products(here, act, weight, True, rows, width, counts)
    total = Reduce(here, counts, product, refs[:11])
    greet(here, slice_peers(here), True)
    line.begin()
    done = total.run(line.step)
    line.end(done)

    def emit(at, first, second):
        for half, value in enumerate((first, second)):
            out[:, pl.ds(pl.multiple_of((half * counts + at) * width, width), width)] = value

    total.end(emit)


def scatter_product(act, weight, width, cid, line, line_counts=16):
    rows = act.shape[0] // 8
    every = weight.shape[0]
    counts = every // (2 * width)
    vm = pl.BlockSpec(memory_space=pltpu.VMEM)
    out_shape = [
        jax.ShapeDtypeStruct((rows, every), jnp.float32),
        jax.ShapeDtypeStruct(line.shape, line.dtype),
    ]
    scratch = reduce_scratch(counts, rows, width) + line_scratch(line_counts, line.shape, line.dtype)
    kernel = functools.partial(scatter_kernel, rows, width, counts, line_counts)
    return kernel_call(kernel, out_shape, [act, weight, line], [vm] * 3, scratch, cid, "scatter_product")


def ffn_kernel(rows, width, counts, x_low, attn, gain, w_gate, w_up, d_hidden, hidden, d_gate, d_up, act_t, tile_out,
               *refs):
    here = Place()
    cols = gain.shape[1]
    act, weight, tiny_own, tiny_all, tiny_send, tiny_recv, dots, local_sems = refs[:8]
    tiny = Tiny(here, tiny_own, tiny_all, (tiny_send, tiny_recv), True)
    half_cols = counts * width
    local = [
        pltpu.make_async_copy(w_gate, weight.at[:, :half_cols], local_sems.at[0]),
        pltpu.make_async_copy(w_up, weight.at[:, half_cols:], local_sems.at[1]),
    ]
    for copy in local:
        copy.start()
    eye = diagonal()
    tiny_own[...] = jnp.zeros_like(tiny_own)

    def prepare(shard, _):
        for at in range(rows // LANES):
            span = pl.ds(pl.multiple_of(shard * rows + at * LANES, LANES), LANES)
            resid = x_low[span, :].astype(jnp.float32) + attn[span, :].astype(jnp.float32)
            act[span, :] = (resid * gain[...]).astype(act.dtype)
            square = jnp.sum(resid * resid, axis=-1, keepdims=True)
            tiny_own[shard, at : at + 1, :] = jnp.sum(square * eye, axis=0, keepdims=True)
        return 0

    lax.fori_loop(0, 8, prepare, 0)
    greet(here, slice_peers(here))
    tiny.begin()
    for copy in local:
        copy.wait()
    product = products(here, act, weight, False, rows, width, counts)
    total = Reduce(here, counts, product, refs[8:19])
    total.run()

    def flip(shard, _):
        span = pl.ds(pl.multiple_of(shard * rows, rows), rows)
        act_t[:, span] = act[span, :].T
        return 0

    lax.fori_loop(0, 8, flip, 0)
    tiny.end()
    tiles = rows // LANES
    mean = [from_tile(jnp.sum(tiny_all[:, at, :], axis=0, keepdims=True), eye) for at in range(tiles)]
    scale = lax.rsqrt(jnp.concatenate(mean, axis=0) / (8 * cols) + EPS)
    dots[...] = jnp.zeros_like(dots)
    coeff = math.sqrt(2.0 / math.pi)

    def emit(at, first, second):
        span = pl.ds(pl.multiple_of(at * width, width), width)
        gate, up = first * scale, second * scale
        inner = jnp.tanh(coeff * (gate + 0.044715 * (gate * gate * gate)))
        gelu = 0.5 * gate * (1.0 + inner)
        slope = 0.5 * (1.0 + inner) + 0.5 * gate * (1.0 - inner * inner) * (
            coeff * (1.0 + 3.0 * 0.044715 * gate * gate))
        cot = d_hidden[:, span]
        hidden[:, span] = (gelu * up).astype(hidden.dtype)
        back_gate, back_up = cot * up * slope, cot * gelu
        d_gate[:, span] = (back_gate * scale).astype(d_gate.dtype)
        d_up[:, span] = (back_up * scale).astype(d_up.dtype)
        dots[...] += jnp.sum(back_gate * gate + back_up * up, axis=-1, keepdims=True)

    total.end(emit)
    tile_out[...] = jnp.zeros_like(tile_out)
    to_tile(tile_out, 0, dots[...] * (scale * scale * (1.0 / (8 * cols))), eye)


def ffn_scatter(x_low, attn, gain, w_gate, w_up, d_hidden, cid, width=512):
    rows, half = d_hidden.shape
    cols = gain.shape[1]
    counts = half // width
    low, f32 = jnp.bfloat16, jnp.float32
    dma = pltpu.SemaphoreType.DMA
    vm = pl.BlockSpec(memory_space=pltpu.VMEM)
    hbm = pl.BlockSpec(memory_space=pl.ANY)
    out_shape = [jax.ShapeDtypeStruct((rows, half), low)] * 3 + [
        jax.ShapeDtypeStruct((cols, 8 * rows), low),
        jax.ShapeDtypeStruct((8, LANES), f32),
    ]
    scratch = [
        pltpu.VMEM((8 * rows, cols), low),
        pltpu.VMEM((cols, 2 * half), low),
        pltpu.VMEM((8, 8, LANES), f32),
        pltpu.VMEM((8, 8, LANES), f32),
        dma((7,)), dma((7,)),
        pltpu.VMEM((rows, 1), f32),
        dma((2,)),
    ] + reduce_scratch(counts, rows, width)
    kernel = functools.partial(ffn_kernel, rows, width, counts)
    return kernel_call(kernel, out_shape, [x_low, attn, gain, w_gate, w_up, d_hidden], [vm, vm, vm, hbm, hbm, vm],
                       scratch, cid, "ffn")


def load_own(spread, payload, width, counts, sems):
    copies = []
    for half in range(2):
        for at in range(counts):
            first = at * width + (half * counts * width if len(payload) == 1 else 0)
            src = payload[half % len(payload)].at[:, first : first + width]
            copies.append(pltpu.make_async_copy(src, spread.slot(0, half, at), sems.at[half, at]))
    return copies


def chip_place(here, per):
    def place(at):
        return here.shard(at // (2 * per), at // per % 2) * per + at % per

    return place


def chip_steps(line, counts):
    def hook(step):
        @pl.when(jnp.logical_and(step >= counts, step < 2 * counts))
        def _():
            line.step(step - counts, 0, 4)

        @pl.when(step >= 3 * counts)
        def _():
            line.step(step - 3 * counts, 4, 8)

    return hook


def back_kernel(rows, width, counts, act_t, w_gate, w_up, d_gate, d_up, dots, x_low, attn, gain, d_norm, gain_grad,
                grad_gate, grad_up, *refs):
    here = Place()
    spread = Spread(here, counts, refs[:7])
    tiny_all, tiny_send, tiny_recv, own_sems, weight, sums, grads, staged, local_sems, out_sems = refs[7:17]
    contrib, rest, rest_sems = refs[17:20]
    line = Line(here, 12, [contrib, d_norm] + list(refs[20:]), chip_place(here, 2))
    tiny = Tiny(here, dots, tiny_all, (tiny_send, tiny_recv), False)
    half_cols = counts * width
    local = [
        pltpu.make_async_copy(w_gate, weight.at[:, :half_cols], local_sems.at[0]),
        pltpu.make_async_copy(w_up, weight.at[:, half_cols:], local_sems.at[1]),
    ]
    own = load_own(spread, (d_gate, d_up), width, counts, own_sems)
    for copy in own + local:
        copy.start()
    greet(here, tiny.peers, True)
    for copy in own:
        copy.wait()
    tiny.begin()
    spread.begin()
    sums[...] = jnp.zeros_like(sums)
    for copy in local:
        copy.wait()

    def columns(half, at):
        return pl.ds(pl.multiple_of((half * counts + at) * width, width), width)

    def clear(at, _):
        grads[:, columns(0, at)] = jnp.zeros((grads.shape[0], width), jnp.float32)
        return 0

    lax.fori_loop(0, 2 * counts, clear, 0)

    def blocks(across, half, at):
        cols = columns(half, at)
        gained = grads[:, cols]
        for other in range(2):
            row = row_span(here, across, other, rows)
            block = spread.got[across, (spread.core + other) % 2, half, at]
            sums[row, :] += dot_nt(block, weight[:, cols])
            gained = gained + dot_nn(act_t[:, row], block)
        grads[:, cols] = gained

    def leave(half, at):
        spot = pl.ds(pl.multiple_of(at * width, width), width)
        return pltpu.make_async_copy(staged.at[half], (grad_gate, grad_up)[half].at[:, spot],
                                     out_sems.at[half, at])

    eye = diagonal()
    gain_grad[...] = jnp.zeros_like(gain_grad)

    def close_chip(chip, target):
        def close_shard(other, _):
            shard = here.shard(chip, other)
            span = pl.ds(pl.multiple_of(shard * rows, rows), rows)
            loads = [pltpu.make_async_copy(src.at[span, :], rest.at[at], rest_sems.at[at])
                     for at, src in enumerate((x_low, attn))]
            for copy in loads:
                copy.start()
            for copy in loads:
                copy.wait()
            for at in range(rows // LANES):
                span = pl.ds(pl.multiple_of(shard * rows + at * LANES, LANES), LANES)
                piece = slice(at * LANES, (at + 1) * LANES)
                dot = from_tile(tiny_all[shard, at : at + 1, :], eye)
                resid = rest[0, piece, :].astype(jnp.float32) + rest[1, piece, :].astype(jnp.float32)
                value = sums[span, :]
                target[span, :] = (value * gain[...] - resid * dot).astype(target.dtype)
                gain_grad[...] += jnp.sum(value * resid, axis=0, keepdims=True)
            return 0

        lax.fori_loop(0, 2, close_shard, 0)

    def done(stage, at):
        @pl.when(jnp.logical_and(stage == 3, at > 0))
        def _():
            leave(0, at - 1).wait()
            leave(1, at - 1).wait()

        @pl.when(stage == 3)
        def _():
            for half in range(2):
                staged[half] = grads[:, columns(half, at)].astype(staged.dtype)
            leave(0, at).start()
            leave(1, at).start()

        @pl.when(jnp.logical_and(at == counts - 1, stage % 2 == 0))
        def _():
            def close(chip, _):
                close_chip(chip, contrib)
                line.launch(4 * chip, 4)
                return 0

            lax.fori_loop(stage // 2, stage // 2 * 2 + 1, close, 0)

    tiny.end()
    spread.run(blocks, chip_steps(line, counts), done)
    close_chip(3, d_norm)
    line.steps(counts + 1, 10, 4, 8)
    line.settle()
    spread.end()

    def drain(at, _):
        leave(0, at).wait()
        leave(1, at).wait()
        return 0

    lax.fori_loop(counts - 1, counts, drain, 0)


def back_gather(act_t, w_gate, w_up, d_gate, d_up, dots, x_low, attn, gain, cid, width=512):
    cols, total = act_t.shape
    rows, half = d_gate.shape
    counts = half // width
    low, f32 = jnp.bfloat16, jnp.float32
    dma = pltpu.SemaphoreType.DMA
    vm = pl.BlockSpec(memory_space=pltpu.VMEM)
    hbm = pl.BlockSpec(memory_space=pl.ANY)
    out_shape = [
        jax.ShapeDtypeStruct((total, cols), low),
        jax.ShapeDtypeStruct((1, cols), f32),
        jax.ShapeDtypeStruct((cols, half), low),
        jax.ShapeDtypeStruct((cols, half), low),
    ]
    scratch = spread_scratch(counts, rows, width) + [
        pltpu.VMEM((8, 8, LANES), f32), dma((7,)), dma((7,)), dma((2, counts)),
        pltpu.VMEM((cols, 2 * half), low),
        pltpu.VMEM((total, cols), f32),
        pltpu.VMEM((cols, 2 * half), f32),
        pltpu.VMEM((2, cols, width), low),
        dma((2,)), dma((2, counts)),
        pltpu.VMEM((total, cols), low),
        pltpu.VMEM((2, rows, cols), low),
        dma((2,)),
    ] + line_scratch(12, (12 * rows // 2, cols), low)
    operands = [act_t, w_gate, w_up, d_gate, d_up, dots, x_low, attn, gain]
    kernel = functools.partial(back_kernel, rows, width, counts)
    return kernel_call(kernel, out_shape, operands, [vm] + [hbm] * 4 + [vm, hbm, hbm, vm], scratch, cid, "back",
                       [vm, vm, hbm, hbm])


def down_kernel(rows, width, counts, cot, weight, hidden, d_norm, ffn, d_attn, grad, *refs):
    here = Place()
    spread = Spread(here, counts, refs[:7])
    own_sems, sums, grads, staged, out_sems, norm_out, part = refs[7:14]
    place = chip_place(here, 2)
    norm_line = Line(here, 4, [d_norm, norm_out] + list(refs[14:22]), lambda at: place(at + 12))
    line = Line(here, 12, [part, ffn] + list(refs[22:]), place)
    own = load_own(spread, (hidden,), width, counts, own_sems)
    for copy in own:
        copy.start()
    greet(here, slice_peers(here), True)
    norm_line.begin()
    for copy in own:
        copy.wait()
    spread.begin()
    sums[...] = jnp.zeros_like(sums)
    grads[...] = jnp.zeros_like(grads)

    def columns(half, at):
        return pl.ds(pl.multiple_of((half * counts + at) * width, width), width)

    def blocks(across, half, at):
        cols = columns(half, at)
        gained = grads[cols, :]
        for other in range(2):
            row = row_span(here, across, other, rows)
            block = spread.got[across, (spread.core + other) % 2, half, at]
            sums[row, :] += dot_nn(block, weight[cols, :])
            gained = gained + dot_tn(block, cot[row, :])
        grads[cols, :] = gained

    def leave(half, at):
        return pltpu.make_async_copy(staged.at[at % 2, half], grad.at[columns(half, at), :], out_sems.at[half, at])

    def done(stage, at):
        @pl.when(jnp.logical_and(stage == 3, at > 1))
        def _():
            leave(0, at - 2).wait()
            leave(1, at - 2).wait()

        @pl.when(stage == 3)
        def _():
            for half in range(2):
                staged[at % 2, half] = grads[columns(half, at), :].astype(staged.dtype)
            leave(0, at).start()
            leave(1, at).start()

        @pl.when(jnp.logical_and(at == counts - 1, stage % 2 == 0))
        def _():
            def close(chip, _):
                close_chip(chip, part)
                line.launch(4 * chip, 4)
                return 0

            lax.fori_loop(stage // 2, stage // 2 * 2 + 1, close, 0)

    def close_chip(chip, target):
        def close_shard(other, _):
            span = row_span(here, chip, other, rows)
            target[span, :] = sums[span, :].astype(target.dtype)
            return 0

        lax.fori_loop(0, 2, close_shard, 0)

    steps = chip_steps(line, counts)

    def hook(step):
        steps(step)

        @pl.when(step < counts)
        def _():
            norm_line.step(step)

    spread.run(blocks, hook, done)
    close_chip(3, ffn)
    line.steps(counts + 1, 10, 4, 8)
    norm_line.settle()

    def add_norm(at, _):
        def add(source):
            span = row_span(here, at // 2, at % 2, rows)
            d_attn[span, :] = (cot[span, :].astype(jnp.float32) + source[span, :].astype(jnp.float32)).astype(
                d_attn.dtype)

        @pl.when(at < 6)
        def _():
            add(d_norm)

        @pl.when(at >= 6)
        def _():
            add(norm_out)
        return 0

    lax.fori_loop(0, 8, add_norm, 0)
    line.settle()
    spread.end()

    def drain(at, _):
        leave(0, at).wait()
        leave(1, at).wait()
        return 0

    lax.fori_loop(counts - 2, counts, drain, 0)


def down_gather(cot, weight, hidden, d_norm, cid, width=256):
    total, cols = cot.shape
    rows, every = hidden.shape
    counts = every // (2 * width)
    low, f32 = jnp.bfloat16, jnp.float32
    dma = pltpu.SemaphoreType.DMA
    vm = pl.BlockSpec(memory_space=pltpu.VMEM)
    hbm = pl.BlockSpec(memory_space=pl.ANY)
    out_shape = [
        jax.ShapeDtypeStruct((total, cols), low),
        jax.ShapeDtypeStruct((total, cols), low),
        jax.ShapeDtypeStruct(weight.shape, low),
    ]
    scratch = spread_scratch(counts, rows, width) + [
        dma((2, counts)),
        pltpu.VMEM((total, cols), f32),
        pltpu.VMEM(weight.shape, f32),
        pltpu.VMEM((2, 2, width, cols), low),
        dma((2, counts)),
        pltpu.VMEM((total, cols), low),
        pltpu.VMEM((total, cols), low),
    ] + line_scratch(4, (4 * rows // 2, cols), low) + line_scratch(12, (12 * rows // 2, cols), low)
    kernel = functools.partial(down_kernel, rows, width, counts)
    return kernel_call(kernel, out_shape, [cot, weight, hidden, d_norm], [vm, vm, hbm, vm], scratch, cid, "down",
                       [vm, vm, hbm])


def attend_kernel(rows, heads, cols, qkv, rms, cos, sin, mask, w_out, cot, part, mixed_all, g_col, kv, probs, queries,
                  pair_rms, *refs):
    here = Place()
    spread = Spread(here, heads // 2, refs[:7])
    sums, pair_sems, turn_send, turn_recv, local_sem, tiny_own, tiny_pair = refs[7:14]
    got, core = spread.got, here.core
    greet(here, slice_peers(here))
    me = here.shard(0, 0)

    def turn_copy(at):
        across, other = turned(at)
        first = pl.multiple_of(here.shard(across, other) * cols, cols)
        return remote(cot.at[:, pl.ds(first, cols)], g_col.at[pl.ds(pl.multiple_of(me * rows, rows), rows), :],
                      turn_send.at[at], turn_recv.at[at], here.device(across, other))

    own_turn = pltpu.make_async_copy(cot.at[:, pl.ds(pl.multiple_of(me * cols, cols), cols)],
                                     g_col.at[pl.ds(pl.multiple_of(me * rows, rows), rows), :], local_sem)
    own_turn.start()
    half = HD // 2
    scale = 1.0 / math.sqrt(HD)
    wide = heads * HD

    def rotated(first):
        lead = qkv[:, first : first + half] * rms[...]
        trail = qkv[:, first + half : first + HD] * rms[...]
        return lead * cos[0] - trail * sin[0], trail * cos[0] + lead * sin[0]

    low_k, high_k = rotated(wide)
    kv[0, :, :half] = low_k.astype(kv.dtype)
    kv[0, :, half:HD] = high_k.astype(kv.dtype)
    for at in range(2):
        first = HD + at * half
        kv[0, :, first : first + half] = (qkv[:, wide + first : wide + first + half] * rms[...]).astype(kv.dtype)
    eye = diagonal()
    tiny_own[...] = jnp.zeros_like(tiny_own)
    to_tile(tiny_own, 0, rms[:, :1], eye)
    pair_rms[0] = rms[...]
    pair = remote(kv.at[0], kv.at[1], pair_sems.at[0], pair_sems.at[1], spread.ydev)
    tiny = remote(tiny_own, tiny_pair, pair_sems.at[2], pair_sems.at[3], spread.ydev)
    for head in range(heads):
        if head == 1:
            pair.start()
            tiny.start()
            turn_copy(2 * (3 - 1)).start()
            turn_copy(2 * (3 - 1) + 1).start()
        lead, trail = rotated(head * HD)
        queries[:, head * HD : head * HD + half] = (lead * scale).astype(queries.dtype)
        queries[:, head * HD + half : (head + 1) * HD] = (trail * scale).astype(queries.dtype)
    pair.wait()
    for at in range(7):
        if at // 2 != 2:
            turn_copy(at).start()

    def one_head(head, _):
        query = queries[:, pl.ds(pl.multiple_of(head * HD, HD), HD)]
        scores = jnp.concatenate([dot_nt(query, kv[0, :, :HD]), dot_nt(query, kv[1, :, :HD])], axis=1)
        scores = jnp.where(mask[...] > 0, scores, NEG)
        expd = jnp.exp(scores - jnp.max(scores, axis=-1, keepdims=True))
        prob = expd / jnp.sum(expd, axis=-1, keepdims=True)
        probs[head] = prob
        prob_low = prob.astype(jnp.bfloat16)
        mixed = dot_nn(prob_low[:, :rows], kv[0, :, HD:]) + dot_nn(prob_low[:, rows:], kv[1, :, HD:])
        got[0, core, head // (heads // 2), head % (heads // 2)] = mixed.astype(got.dtype)
        return 0

    lax.fori_loop(0, heads, one_head, 0)
    sums[...] = jnp.zeros_like(sums)
    spread.begin()

    def blocks(across, half_at, at):
        span = pl.ds(pl.multiple_of((half_at * (heads // 2) + at) * HD, HD), HD)
        for other in range(2):
            row = row_span(here, across, other, rows)
            block = got[across, (core + other) % 2, half_at, at]
            mixed_all[row, span] = block
            sums[row, :] += dot_nn(block, w_out[span, :])

    spread.run(blocks)
    part[...] = sums[...].astype(part.dtype)
    spread.end()
    tiny.wait()
    for at in range(rows // LANES):
        values = jnp.broadcast_to(from_tile(tiny_pair[at : at + 1, :], eye), (LANES, LANES))
        pair_rms[1, at * LANES : (at + 1) * LANES, :] = values
    own_turn.wait()
    for at in range(7):
        turn_copy(at).wait()


def attend(qkv, rms, cos, sin, mask, w_out, cot, cid):
    rows = qkv.shape[0]
    wide, cols = w_out.shape
    heads = wide // HD
    low, f32 = jnp.bfloat16, jnp.float32
    dma = pltpu.SemaphoreType.DMA
    vm = pl.BlockSpec(memory_space=pltpu.VMEM)
    out_shape = [
        jax.ShapeDtypeStruct((8 * rows, cols), low),
        jax.ShapeDtypeStruct((8 * rows, wide), low),
        jax.ShapeDtypeStruct((8 * rows, cols), low),
        jax.ShapeDtypeStruct((2, rows, 2 * HD), low),
        jax.ShapeDtypeStruct((heads, rows, 2 * rows), f32),
        jax.ShapeDtypeStruct((rows, wide), low),
        jax.ShapeDtypeStruct((2,) + rms.shape, f32),
    ]
    scratch = spread_scratch(heads // 2, rows, HD) + [
        pltpu.VMEM((8 * rows, cols), f32), dma((4,)), dma((7,)), dma((7,)), dma(()),
        pltpu.VMEM((8, LANES), f32), pltpu.VMEM((8, LANES), f32)]
    kernel = functools.partial(attend_kernel, rows, heads, cols)
    return kernel_call(kernel, out_shape, [qkv, rms, cos, sin, mask, w_out, cot], [vm] * 7, scratch, cid,
                       "attend")


def tail_kernel(rows, heads, per, d_attn, w_out, queries, kv, probs, rms, cos, sin, act_t, w_qkv, ffn, x_low,
                attn, gain, gain_grad, mixed_all, d_tok, out, grad_query, grad_out, kv_sum, gain_tiles, *refs):
    here = Place()
    width = HD
    counts = heads // 2
    part = rows // 2
    refs = list(refs)
    line_counts = 8 * per
    cols = d_attn.shape[1]
    extra = cols // (rows // per)

    def take(count):
        taken_refs = refs[:count]
        del refs[:count]
        return taken_refs

    total_refs = take(11)
    spread = Spread(here, 1, take(7))
    d_mixed, tiny_own, tiny_all, d_kv, give, taken, give_sems, tiny_send, tiny_recv = take(9)
    grad, grad_mixed, gain_sum, tile, tile_send, tile_recv, put_sems, local_sems, mixed_two, mixed_sems = take(10)

    def far(at):
        return turned(at // per)

    def near(at):
        at = jnp.minimum(at, line_counts - 1)
        x_stream, y_stream = spread.streams(at // 4)
        second = at // 2 % 2
        across = x_stream[0] + second * (y_stream[0] - x_stream[0])
        half_at = x_stream[1] + second * (y_stream[1] - x_stream[1])
        return across, at % 2, half_at

    def place_ffn(at):
        return here.shard(*far(at)) * per + at % per

    def place_tok(at):
        across, other, half_at = near(at)
        return jnp.where(at < line_counts, here.shard(across, other) * per + half_at, at)

    ffn_sum, leaving = take(2)
    by_chip = chip_place(here, per)
    line = Line(here, 2 * per, [ffn, ffn_sum] + take(8), lambda at: by_chip(at + 6 * per))
    contrib, summed = take(2)
    line_tok = Line(here, line_counts + extra, [contrib, summed] + take(8), place_tok)
    tiny = Tiny(here, tiny_own, tiny_all, (tiny_send, tiny_recv), False)
    got, core = spread.got, here.core
    product = products(here, d_attn, w_out, True, rows, width, counts)
    total = Reduce(here, counts, product, total_refs)
    greet(here, tiny.peers, True)
    line.begin()
    grad_mixed[...] = jnp.zeros_like(grad_mixed)

    def mixed_copy(step):
        span = pl.ds(pl.multiple_of(step * rows, rows), rows)
        return pltpu.make_async_copy(mixed_all.at[span, :], mixed_two.at[step % 2], mixed_sems.at[step % 2])

    mixed_copy(0).start()

    def beside(step):
        line.step(step)

        @pl.when(step < 8)
        def _():
            span = pl.ds(pl.multiple_of(step * rows, rows), rows)
            mixed_copy(step).wait()

            @pl.when(step < 7)
            def _():
                mixed_copy(step + 1).start()

            grad_mixed[...] += dot_tn(mixed_two[step % 2], d_attn[span, :])

    line.end(total.run(beside))
    grad_out[...] = grad_mixed[...].astype(grad_out.dtype)

    def land(at, first, second):
        for half_at, value in enumerate((first, second)):
            d_mixed[:, pl.ds(pl.multiple_of((half_at * counts + at) * width, width), width)] = value.astype(
                d_mixed.dtype)

    total.end(land)
    half = HD // 2
    scale = 1.0 / math.sqrt(HD)
    depth = w_qkv.shape[0] * 8
    d_kv[...] = jnp.zeros_like(d_kv)

    def one_head(head, dots):
        span = pl.ds(pl.multiple_of(head * HD, HD), HD)
        query = queries[:, span]
        cot = d_mixed[:, span]
        prob = probs[head]
        d_prob = jnp.concatenate([dot_nt(cot, kv[0, :, HD:]), dot_nt(cot, kv[1, :, HD:])], axis=1)
        delta = jnp.sum(prob * d_prob, axis=-1, keepdims=True)
        d_score = (prob * (d_prob - delta)).astype(jnp.bfloat16)
        prob_low = prob.astype(jnp.bfloat16)
        d_query = (dot_nn(d_score[:, :rows], kv[0, :, :HD]) + dot_nn(d_score[:, rows:], kv[1, :, :HD])) * scale
        for side in range(2):
            keys = slice(side * rows, (side + 1) * rows)
            d_kv[side, :, :HD] += dot_tn(d_score[:, keys], query)
            d_kv[side, :, HD:] += dot_tn(prob_low[:, keys], cot)
        dots = dots + jnp.sum(d_query * query.astype(jnp.float32), axis=-1, keepdims=True)
        lead, trail = d_query[:, :half], d_query[:, half:]
        first = ((lead * cos[0] + trail * sin[0]) * rms[0]).astype(got.dtype)
        second = ((trail * cos[0] - lead * sin[0]) * rms[0]).astype(got.dtype)
        for rows_at in range(2):
            piece = slice(rows_at * part, (rows_at + 1) * part)
            got[0, core, rows_at, 0, :, pl.ds(pl.multiple_of(head * HD, HD), half)] = first[piece, :]
            got[0, core, rows_at, 0, :, pl.ds(pl.multiple_of(head * HD + half, half), half)] = second[piece, :]

        return dots

    dots = lax.fori_loop(0, heads, one_head, jnp.zeros((rows, 1), jnp.float32))
    eye = diagonal()
    tiny_own[...] = jnp.zeros_like(tiny_own)
    for side in (1, 0):
        d_key, d_value = d_kv[side, :, :HD], d_kv[side, :, HD:]
        own = jnp.sum(d_key * kv[side, :, :HD].astype(jnp.float32) +
                      d_value * kv[side, :, HD:].astype(jnp.float32), axis=-1, keepdims=True)
        if side == 0:
            own = own + dots * (1.0 / scale)
        own = own * (rms[side] * rms[side] * (1.0 / depth))
        to_tile(tiny_own, side * (rows // LANES), own, eye)
        lead, trail = d_key[:, :half], d_key[:, half:]
        parts = [(lead * cos[side] + trail * sin[side]) * rms[side],
                 (trail * cos[side] - lead * sin[side]) * rms[side],
                 d_value[:, :half] * rms[side], d_value[:, half:] * rms[side]]
        for at, value in enumerate(parts):
            if side == 1:
                give[:, at * half : (at + 1) * half] = value.astype(give.dtype)
            else:
                d_kv[0, :, at * half : (at + 1) * half] = value
    given = remote(give, taken, give_sems.at[0], give_sems.at[1], spread.ydev)
    given.start()
    grad[...] = jnp.zeros_like(grad)
    given.wait()
    for rows_at in range(2):
        piece = slice(rows_at * part, (rows_at + 1) * part)
        value = d_kv[0, piece, :] + taken[piece, :].astype(jnp.float32)
        got[0, core, rows_at, 0, :, heads * HD :] = value.astype(got.dtype)
    tiny.begin()
    for hop in range(2):
        spread.x_copy(hop, 0).start()
        spread.y_copy(hop, 0).start()
    for stream in range(2):
        spread.sib_copy(0, stream, 0).start()
    gain_sum[...] = jnp.zeros_like(gain_sum)
    tiny.end()

    def block_of(at):
        across, other, half_at = near(at)
        shard, partner = here.shard(across, other), here.shard((across + 2) % 4, other)
        block = got[across, (core + other) % 2, half_at, 0]
        first = pl.multiple_of(shard * rows + half_at * part, part)
        for tile_at in range(part // LANES):
            row = pl.ds(pl.multiple_of(first + tile_at * LANES, LANES), LANES)
            low_at = half_at * (part // LANES) + tile_at
            kept = rows // LANES + low_at
            dot = from_tile(tiny_all[shard, pl.ds(low_at, 1), :] + tiny_all[partner, pl.ds(kept, 1), :], eye)
            value = dot_nt(block[tile_at * LANES : (tile_at + 1) * LANES, :], w_qkv[...])
            x_rows = x_low[row, :].astype(jnp.float32)
            contrib[row, :] = (value * gain[...] - x_rows * dot).astype(contrib.dtype)
            gain_sum[...] += jnp.sum(value * x_rows, axis=0, keepdims=True)
        line_tok.launch(at, 1)
        rows_t = act_t[:, pl.ds(first, part)]
        for at_col in range((heads + 2) * HD // 512):
            span = slice(at_col * 512, (at_col + 1) * 512)
            grad[:, span] += dot_nn(rows_t, block[:, span])

    me = here.shard(0, 0)
    columns = pl.ds(pl.multiple_of(me * cols, cols), cols)
    chunk = line.chunk

    def landing(which, at):
        sub = at % per if which == 0 else near(at)[2]
        return (out, d_tok)[which].at[pl.ds(pl.multiple_of(sub * chunk, chunk), chunk), columns]

    def leaver(which, at):
        return (leaving, line_tok.from_end)[which].at[at]

    def put(which, at):
        goal = here.device(*(far(at) if which == 0 else near(at)[:2]))
        return remote(leaver(which, at), landing(which, at), put_sems.at[which, 0, at], put_sems.at[which, 1, at],
                      goal)

    def keep(which, at):
        spot = at % per if which == 0 else near(at)[2]
        return pltpu.make_async_copy(leaver(which, at), landing(which, at), local_sems.at[which, spot])

    def emit(which, at):
        if which == 1:
            row = line_tok.rows(at)
            value = d_attn[row, :].astype(jnp.float32) + summed[row, :].astype(jnp.float32)
            line_tok.from_end[at] = value.astype(out.dtype)
            return
        row = pl.ds(pl.multiple_of(place_ffn(at) * chunk, chunk), chunk)

        def leave(source):
            value = x_low[row, :].astype(jnp.float32) + attn[row, :].astype(jnp.float32)
            leaving[at] = (value + source[row, :].astype(jnp.float32)).astype(out.dtype)

        @pl.when(at < 2 * per)
        def _():
            leave(ffn_sum)

        @pl.when(at >= 2 * per)
        def _():
            leave(ffn)

    def is_own(which, at):
        return at >= 7 * per if which == 0 else jnp.logical_and(at < 4, at % 2 == 0)

    def send(which, at):
        own = is_own(which, at)

        @pl.when(own)
        def _():
            keep(which, at).start()

        @pl.when(jnp.logical_not(own))
        def _():
            put(which, at).start()

    def stage_step(step, _):
        stage = step // 4

        @pl.when(jnp.logical_and(step % 4 == 0, jnp.logical_and(stage > 0, stage < 4)))
        def _():
            spread.x_copy(stage - 1, 0).wait_recv()
            spread.sib_copy(stage, 0, 0).start()
            spread.y_copy(stage - 1, 0).wait_recv()
            spread.sib_copy(stage, 1, 0).start()

        @pl.when(step == 4)
        def _():
            spread.x_copy(2, 0).start()
            spread.y_copy(2, 0).start()

        @pl.when(step < line_counts)
        def _():
            for stream in range(2):
                @pl.when(step % 4 == 2 * stream)
                def _(stream=stream):
                    spread.sib_copy(stage, stream, 0).wait_recv()

            block_of(step)

        @pl.when(step >= 4)
        def _():
            line_tok.step(step - 4)

        @pl.when(step > 0)
        def _():
            send(0, step - 1)

        emit(0, step)

        @pl.when(jnp.logical_and(line.inner == 1, step > 7))
        def _():
            send(1, step - 8)

        @pl.when(jnp.logical_and(line.inner == 1, step > 6))
        def _():
            emit(1, step - 7)
        return 0

    lax.fori_loop(0, line_counts, stage_step, 0)
    for half_at in range(cols // (rows // per)):
        span = pl.ds(line_counts * (rows // per) + half_at * (rows // per), rows // per)
        source = slice(half_at * (rows // per), (half_at + 1) * (rows // per))
        contrib[span, :] = grad[source, heads * HD :].astype(contrib.dtype)
    line_tok.launch(line_counts, extra)
    grad_query[...] = grad[:, : heads * HD].astype(grad_query.dtype)
    for at in range(cols // LANES):
        tile[at : at + 1, :] = gain_sum[:, at * LANES : (at + 1) * LANES]
        spot = cols // LANES + at
        tile[spot : spot + 1, :] = gain_grad[:, at * LANES : (at + 1) * LANES]

    def tile_copy(step):
        return remote(tile, gain_tiles.at[here.z], tile_send.at[step], tile_recv.at[step],
                      (here.dp, here.seq, (here.z + step + 1) % 4))

    send(0, line_counts - 1)
    for step in range(3):
        tile_copy(step).start()
    gain_tiles[here.z] = tile[...]

    @pl.when(line.inner == 1)
    def _():
        start = line_counts - 4

        def both(at, _):
            line_tok.step(at)

            @pl.when(at < line_counts + 4)
            def _():
                send(1, at - 4)

            @pl.when(at < line_counts + 3)
            def _():
                emit(1, at - 3)
            return 0

        lax.fori_loop(start, line_counts + extra + 2, both, 0)

        def drain(at, _):
            line_tok.down(at).wait_send()
            return 0

        lax.fori_loop(0, line_counts + extra, drain, 0)

    @pl.when(line.inner == 0)
    def _():
        def arrive(at, _):
            line_tok.up(at).wait_send()
            line_tok.down(at).wait_recv()

            @pl.when(jnp.logical_and(at > 0, at <= line_counts))
            def _():
                send(1, at - 1)

            @pl.when(at < line_counts)
            def _():
                emit(1, at)
            return 0

        lax.fori_loop(0, line_counts + extra, arrive, 0)

    for half_at in range(extra):
        span = pl.ds((line_counts + half_at) * chunk, chunk)
        kv_sum[half_at * chunk : (half_at + 1) * chunk, :] = summed[span, :]
    for hop in range(3):
        spread.x_copy(hop, 0).wait_send()
        spread.y_copy(hop, 0).wait_send()
    for stage in range(4):
        spread.sib_copy(stage, 0, 0).wait_send()
        spread.sib_copy(stage, 1, 0).wait_send()

    def finish(at, _):
        for which in range(2):
            own = is_own(which, at)

            @pl.when(own)
            def _():
                keep(which, at).wait()

            @pl.when(jnp.logical_not(own))
            def _():
                put(which, at).wait()
        return 0

    lax.fori_loop(0, line_counts, finish, 0)
    for step in range(3):
        tile_copy(step).wait()


def tail(d_attn, w_out, queries, kv, probs, rms, cos, sin, act_t, w_qkv, ffn, x_low, attn, gain, gain_grad,
         mixed_all, cid,
 per=2):
    total, cols = d_attn.shape
    rows = total // 8
    wide = w_out.shape[0]
    heads = wide // HD
    low, f32 = jnp.bfloat16, jnp.float32
    dma = pltpu.SemaphoreType.DMA
    vm = pl.BlockSpec(memory_space=pltpu.VMEM)
    counts = 8 * per
    chunk = rows // per
    extra = cols // chunk
    long = (total + cols, cols)
    out_shape = [
        jax.ShapeDtypeStruct((rows, 8 * cols), low),
        jax.ShapeDtypeStruct((rows, 8 * cols), low),
        jax.ShapeDtypeStruct((cols, wide), low),
        jax.ShapeDtypeStruct(w_out.shape, low),
        jax.ShapeDtypeStruct((cols, 2 * HD), low),
        jax.ShapeDtypeStruct((4, 8, LANES), f32),
    ]
    scratch = reduce_scratch(heads // 2, rows, HD, 2) + spread_scratch(1, rows // 2, wide + 2 * HD)
    scratch += [
        pltpu.VMEM((rows, wide), low),
        pltpu.VMEM((8, LANES), f32),
        pltpu.VMEM((8, 8, LANES), f32),
        pltpu.VMEM((2, rows, 2 * HD), f32),
        pltpu.VMEM((rows, 2 * HD), low),
        pltpu.VMEM((rows, 2 * HD), low),
        dma((2,)), dma((7,)), dma((7,)),
        pltpu.VMEM(w_qkv.shape, f32),
        pltpu.VMEM(w_out.shape, f32),
        pltpu.VMEM((1, cols), f32),
        pltpu.VMEM((8, LANES), f32),
        dma((3,)), dma((3,)), dma((2, 2, counts)), dma((2, per)),
        pltpu.VMEM((2, rows, wide), low), dma((2,)),
        pltpu.VMEM((total, cols), low),
        pltpu.VMEM((counts, chunk, cols), low),
    ] + line_scratch(2 * per, (2 * per * chunk, cols), low)
    scratch += [pltpu.VMEM(long, low), pltpu.VMEM(long, low)] + line_scratch(counts + extra, long, low)
    operands = [d_attn, w_out, queries, kv, probs, rms, cos, sin, act_t, w_qkv, ffn, x_low, attn, gain,
                gain_grad, mixed_all]
    kernel = functools.partial(tail_kernel, rows, heads, per)
    specs = [vm] * (len(operands) - 1) + [pl.BlockSpec(memory_space=pl.ANY)]
    return kernel_call(kernel, out_shape, operands, specs, scratch, cid, "tail")


LANES = 128


def acts_move(
    tokens, seg_ids, gain_attn, w_query, kv_weight, w_out, gain_ffn, w_gate, w_up, w_down, d_out
):
    rows = tokens.shape[0]
    segs = seg_ids.astype(jnp.float32).reshape(2 * rows // LANES, LANES)
    segs = jnp.pad(segs, ((0, 8 - 2 * rows // LANES), (0, 0)))
    gain_one = gain_attn.astype(jnp.float32)[None, :]
    gain_two = gain_ffn.astype(jnp.float32)[None, :]
    wider = jnp.float32

    qkv, x_low, act_one_t, w_qkv, rms, cos, sin, mask = opening(
        tokens, gain_one, w_query, kv_weight, segs, 1
    )
    attn_part, mixed_all, g_low, kv, probs, queries, pair_rms = attend(
        qkv, rms, cos, sin, mask, w_out, d_out, 2
    )
    d_hidden, attn = scatter_product(g_low, w_down, 512, 3, attn_part)
    hidden, d_gate, d_up, act_two_t, dots = ffn_scatter(x_low, attn, gain_two, w_gate, w_up, d_hidden, 4)
    d_norm, grad_gain_two, grad_gate, grad_up = back_gather(
        act_two_t, w_gate, w_up, d_gate, d_up, dots, x_low, attn, gain_two, 5
    )
    ffn, d_attn, grad_down = down_gather(g_low, w_down, hidden, d_norm, 6)
    d_tokens, out, grad_query, grad_out, grad_kv, gain_tiles = tail(
        d_attn,
        w_out,
        queries,
        kv,
        probs,
        pair_rms,
        cos,
        sin,
        act_one_t,
        w_qkv,
        ffn,
        x_low,
        attn,
        gain_one,
        grad_gain_two,
        mixed_all,
        7,
    )
    gains = jnp.sum(gain_tiles, axis=0).reshape(2, -1)
    return (
        out,
        d_tokens.astype(wider),
        gains[0],
        grad_query.astype(wider),
        grad_kv.astype(wider),
        grad_out.astype(wider),
        gains[1],
        grad_gate.astype(wider),
        grad_up.astype(wider),
        grad_down.astype(wider),
    )


def solution(mesh):
    in_specs = (
        P(("dp", "seq"), None),
        P("dp"),
        P(("dp", "seq")),
        P(("dp", "seq"), "tensor"),
        P(("dp", "seq"), None),
        P("tensor", ("dp", "seq")),
        P(("dp", "seq")),
        P(("dp", "seq"), "tensor"),
        P(("dp", "seq"), "tensor"),
        P("tensor", ("dp", "seq")),
        P(("dp", "seq"), None),
    )
    out_specs = (
        P(("dp", "seq"), None),
        P(("dp", "seq"), None),
        P(("dp", "seq")),
        P(("dp", "seq"), "tensor"),
        P(("dp", "seq"), None),
        P("tensor", ("dp", "seq")),
        P(("dp", "seq")),
        P(("dp", "seq"), "tensor"),
        P(("dp", "seq"), "tensor"),
        P("tensor", ("dp", "seq")),
    )

    def shards(*arrays):
        tokens = arrays[0]
        sizes = tuple(mesh.shape[name] for name in ("dp", "seq", "tensor"))
        count = tokens.shape[0] * sizes[0] * sizes[1]
        plan = acts_move if sizes == (4, 2, 4) and count <= tokens.shape[1] else weights_move
        return plan(*arrays)

    return jax.shard_map(shards, mesh=mesh, in_specs=in_specs, out_specs=out_specs, check_vma=False)
```

```python
import functools
import math

import jax
import jax.numpy as jnp
from jax import lax
from jax.experimental import pallas as pl
from jax.experimental.pallas import tpu as pltpu
from jax.sharding import PartitionSpec as P

HD = 256


EPS = 1e-06
NEG = -1e30


def place_tables(segs):
    length = segs.shape[0]
    index = jnp.arange(length, dtype=jnp.int32)
    flags = jnp.concatenate([jnp.ones((1,), dtype=bool), segs[1:] != segs[:-1]])
    starts = lax.cummax(jnp.where(flags, index, jnp.zeros_like(index)), axis=0)
    places = index - starts
    half_size = HD // 2
    freqs = jnp.exp(jnp.arange(half_size, dtype=jnp.float32) * (-math.log(10000.0) / half_size))
    angles = places.astype(jnp.float32)[:, None] * freqs[None, :]
    return (places, jnp.cos(angles), jnp.sin(angles))


def rotate(vector, cos_table, sin_table):
    half_size = vector.shape[-1] // 2
    leading = vector[..., :half_size]
    trailing = vector[..., half_size:]
    return jnp.concatenate(
        [leading * cos_table - trailing * sin_table, trailing * cos_table + leading * sin_table],
        axis=-1,
    )


def rotate_back(vector, cos_table, sin_table):
    half_size = vector.shape[-1] // 2
    leading = vector[..., :half_size]
    trailing = vector[..., half_size:]
    return jnp.concatenate(
        [leading * cos_table + trailing * sin_table, trailing * cos_table - leading * sin_table],
        axis=-1,
    )


def matmul(left, right):
    return jnp.dot(left, right, preferred_element_type=jnp.float32)


def matmul_nt(left, right):
    return lax.dot_general(
        left, right, (((1,), (1,)), ((), ())), preferred_element_type=jnp.float32
    )


def matmul_tn(left, right):
    return lax.dot_general(
        left, right, (((0,), (0,)), ((), ())), preferred_element_type=jnp.float32
    )


def gelu_tanh(values):
    return jax.nn.gelu(values, approximate=True)


def norm_back(d_act, normed, rms_val, gain_val):
    scaled = d_act * gain_val
    return rms_val * (scaled - normed * jnp.mean(scaled * normed, axis=-1, keepdims=True))


def weights_move(
    tokens, seg_ids, gain_attn, w_query, kv_weight, w_out, gain_ffn, w_gate, w_up, w_down, d_out
):
    rows = tokens.shape[0]
    scale_factor = 1.0 / math.sqrt(HD)
    offset = lax.axis_index("seq") * rows
    places, cos_table, sin_table = place_tables(seg_ids)
    own_places = lax.dynamic_slice_in_dim(places, offset, rows, 0)
    own_segs = lax.dynamic_slice_in_dim(seg_ids, offset, rows, 0)
    own_cos = lax.dynamic_slice_in_dim(cos_table, offset, rows, 0)
    own_sin = lax.dynamic_slice_in_dim(sin_table, offset, rows, 0)
    allowed = (own_segs[:, None] == seg_ids[None, :]) & (own_places[:, None] >= places[None, :])
    full_query, full_out, full_kv, full_gain_one = (
        lax.all_gather(w_query, ("dp", "seq"), axis=0, tiled=True),
        lax.all_gather(w_out, ("dp", "seq"), axis=1, tiled=True),
        lax.all_gather(kv_weight, ("dp", "seq"), axis=0, tiled=True),
        lax.all_gather(gain_attn, ("dp", "seq"), axis=0, tiled=True),
    )
    gain_one = full_gain_one.astype(jnp.float32)
    inputs = tokens.astype(jnp.float32)
    rms_one = lax.rsqrt(jnp.mean(inputs * inputs, axis=-1, keepdims=True) + EPS)
    norm_one = inputs * rms_one
    act_one = (norm_one * gain_one).astype(jnp.bfloat16)
    query_pre = matmul(act_one, full_query)
    heads = query_pre.shape[1] // HD
    kv_pre = matmul(act_one, full_kv)
    queries = (
        rotate(query_pre.reshape(rows, heads, HD), own_cos[:, None, :], own_sin[:, None, :])
        * scale_factor
    ).astype(jnp.bfloat16)
    own_kv = jnp.concatenate(
        [rotate(kv_pre[:, :HD], own_cos, own_sin), kv_pre[:, HD:]], axis=1
    ).astype(jnp.bfloat16)
    all_kv = lax.all_gather(own_kv, "seq", axis=0, tiled=True)
    keys = all_kv[:, :HD]
    values_all = all_kv[:, HD:]
    scores = jnp.einsum("rhd,kd->hrk", queries, keys, preferred_element_type=jnp.float32)
    scores = jnp.where(allowed[None], scores, NEG)
    top_score = jnp.max(scores, axis=-1, keepdims=True)
    expd = jnp.exp(scores - top_score)
    total = jnp.sum(expd, axis=-1, keepdims=True)
    log_total = top_score + jnp.log(total)
    probs_low = (expd / total).astype(jnp.bfloat16)
    mixed = (
        jnp.einsum("hrk,kd->rhd", probs_low, values_all, preferred_element_type=jnp.float32)
        .reshape(rows, heads * HD)
        .astype(jnp.bfloat16)
    )
    attn = lax.psum(matmul(mixed, full_out), "tensor")
    resid = inputs + attn
    full_gate, full_up, full_down, full_gain_two = (
        lax.all_gather(w_gate, ("dp", "seq"), axis=0, tiled=True),
        lax.all_gather(w_up, ("dp", "seq"), axis=0, tiled=True),
        lax.all_gather(w_down, ("dp", "seq"), axis=1, tiled=True),
        lax.all_gather(gain_ffn, ("dp", "seq"), axis=0, tiled=True),
    )
    gain_two = full_gain_two.astype(jnp.float32)
    rms_two = lax.rsqrt(jnp.mean(resid * resid, axis=-1, keepdims=True) + EPS)
    norm_two = resid * rms_two
    act_two = (norm_two * gain_two).astype(jnp.bfloat16)
    gate = matmul(act_two, full_gate)
    up_val = matmul(act_two, full_up)
    gelu_val, gelu_pull = jax.vjp(gelu_tanh, gate)
    hidden = (gelu_val * up_val).astype(jnp.bfloat16)
    ffn = lax.psum(matmul(hidden, full_down).astype(jnp.bfloat16), "tensor").astype(jnp.float32)
    out = (resid + ffn).astype(jnp.bfloat16)
    back_gate, back_up, back_down = (
        lax.all_gather(w_gate, ("dp", "seq"), axis=0, tiled=True),
        lax.all_gather(w_up, ("dp", "seq"), axis=0, tiled=True),
        lax.all_gather(w_down, ("dp", "seq"), axis=1, tiled=True),
    )
    d_hidden = matmul_nt(d_out, back_down)
    grad_down = matmul_tn(hidden, d_out)
    d_gate = gelu_pull(d_hidden * up_val)[0].astype(jnp.bfloat16)
    d_up = (d_hidden * gelu_val).astype(jnp.bfloat16)
    grad_gate = matmul_tn(act_two, d_gate)
    grad_up = matmul_tn(act_two, d_up)
    d_act_two = lax.psum(matmul_nt(d_gate, back_gate) + matmul_nt(d_up, back_up), "tensor")
    grad_gain_two = jnp.sum(d_act_two * norm_two, axis=0)
    d_resid = d_out.astype(jnp.float32) + norm_back(d_act_two, norm_two, rms_two, gain_two)
    ffn_grads = (
        lax.psum_scatter(
            grad_gate.astype(jnp.bfloat16), ("dp", "seq"), scatter_dimension=0, tiled=True
        ).astype(jnp.float32),
        lax.psum_scatter(
            grad_up.astype(jnp.bfloat16), ("dp", "seq"), scatter_dimension=0, tiled=True
        ).astype(jnp.float32),
        lax.psum_scatter(
            grad_down.astype(jnp.bfloat16), ("dp", "seq"), scatter_dimension=1, tiled=True
        ).astype(jnp.float32),
        lax.psum_scatter(
            grad_gain_two.astype(jnp.bfloat16), ("dp", "seq"), scatter_dimension=0, tiled=True
        ).astype(jnp.float32),
    )
    back_query, back_out, back_kv = (
        lax.all_gather(w_query, ("dp", "seq"), axis=0, tiled=True),
        lax.all_gather(w_out, ("dp", "seq"), axis=1, tiled=True),
        lax.all_gather(kv_weight, ("dp", "seq"), axis=0, tiled=True),
    )
    d_attn = d_resid.astype(jnp.bfloat16)
    grad_out = matmul_tn(mixed, d_attn)
    d_mixed = matmul_nt(d_attn, back_out).astype(jnp.bfloat16).reshape(rows, heads, HD)
    scores_again = jnp.einsum("rhd,kd->hrk", queries, keys, preferred_element_type=jnp.float32)
    probs = jnp.where(allowed[None], jnp.exp(scores_again - log_total), 0.0)
    d_probs = jnp.einsum("rhd,kd->hrk", d_mixed, values_all, preferred_element_type=jnp.float32)
    delta = jnp.sum(probs * d_probs, axis=-1, keepdims=True)
    d_scores = (probs * (d_probs - delta)).astype(jnp.bfloat16)
    d_queries = (
        jnp.einsum("hrk,kd->rhd", d_scores, keys, preferred_element_type=jnp.float32) * scale_factor
    )
    d_query_pre = (
        rotate_back(d_queries, own_cos[:, None, :], own_sin[:, None, :])
        .reshape(rows, heads * HD)
        .astype(jnp.bfloat16)
    )
    d_keys_part = jnp.einsum("hrk,rhd->kd", d_scores, queries, preferred_element_type=jnp.float32)
    d_values_part = jnp.einsum(
        "hrk,rhd->kd", probs.astype(jnp.bfloat16), d_mixed, preferred_element_type=jnp.float32
    )
    own_kv_grad = lax.psum_scatter(
        jnp.concatenate([d_keys_part, d_values_part], axis=1).astype(jnp.bfloat16),
        "seq",
        scatter_dimension=0,
        tiled=True,
    )
    d_act_query = matmul_nt(d_query_pre, back_query)
    d_act_sum, kv_grad = (
        lax.psum(d_act_query.astype(jnp.bfloat16), "tensor").astype(jnp.float32),
        lax.psum(own_kv_grad, "tensor").astype(jnp.float32),
    )
    d_kv_pre = jnp.concatenate(
        [rotate_back(kv_grad[:, :HD], own_cos, own_sin), kv_grad[:, HD:]], axis=1
    ).astype(jnp.bfloat16)
    d_act_one = d_act_sum + matmul_nt(d_kv_pre, back_kv)
    grad_query = matmul_tn(act_one, d_query_pre)
    grad_kv = matmul_tn(act_one, d_kv_pre)
    grad_gain_one = jnp.sum(d_act_one * norm_one, axis=0)
    d_tokens = d_resid + norm_back(d_act_one, norm_one, rms_one, gain_one)
    attn_grads = (
        lax.psum_scatter(
            grad_query.astype(jnp.bfloat16), ("dp", "seq"), scatter_dimension=0, tiled=True
        ).astype(jnp.float32),
        lax.psum_scatter(
            grad_out.astype(jnp.bfloat16), ("dp", "seq"), scatter_dimension=1, tiled=True
        ).astype(jnp.float32),
        lax.psum_scatter(
            grad_kv.astype(jnp.bfloat16), ("dp", "seq"), scatter_dimension=0, tiled=True
        ).astype(jnp.float32),
        lax.psum_scatter(
            grad_gain_one.astype(jnp.bfloat16), ("dp", "seq"), scatter_dimension=0, tiled=True
        ).astype(jnp.float32),
    )
    return (
        out,
        d_tokens,
        attn_grads[3],
        attn_grads[0],
        attn_grads[2],
        attn_grads[1],
        ffn_grads[3],
        ffn_grads[0],
        ffn_grads[1],
        ffn_grads[2],
    )


MESH = pl.DeviceIdType.MESH
VMEM_LIMIT = 66000 * 1024


class Place:
    def __init__(self):
        self.dp = lax.axis_index("dp")
        self.seq = lax.axis_index("seq")
        self.z = lax.axis_index("tensor")
        self.core = lax.rem(self.dp, 2)
        self.chip = lax.div(self.dp, 2)

    def device(self, across, other):
        chip = (self.chip + across) % 2
        seq = (self.seq + across // 2) % 2
        core = (self.core + other) % 2
        return chip * 2 + core, seq, self.z

    def shard(self, across, other):
        dp, seq, _ = self.device(across, other)
        return dp * 2 + seq


def greet(here, peers, line=False):
    barrier = pltpu.get_barrier_semaphore()
    peers = list(peers)
    if line:
        peers += [(here.dp, here.seq, (here.z + step) % 4) for step in range(1, 4)]
    for peer in peers:
        pl.semaphore_signal(barrier, inc=1, device_id=peer, device_id_type=MESH)
    pl.semaphore_wait(barrier, len(peers))


def remote(src, dst, send, recv, peer):
    return pltpu.make_async_remote_copy(
        src_ref=src, dst_ref=dst, send_sem=send, recv_sem=recv, device_id=peer, device_id_type=MESH
    )


class Line:
    def __init__(self, here, counts, refs, place=None):
        self.own, self.out, self.from_end, self.from_mid = refs[:4]
        self.sems = refs[4:10]
        self.counts = counts
        self.chunk = self.from_end.shape[1]
        self.place = place
        z = here.z
        self.inner = ((z + 1) // 2) % 2
        self.mate = (here.dp, here.seq, z + 1 - 2 * (z % 2))
        self.other = (here.dp, here.seq, 3 - z)

    def rows(self, at):
        at = at if self.place is None else self.place(at)
        return pl.ds(pl.multiple_of(at * self.chunk, self.chunk), self.chunk)

    def up(self, at):
        return remote(self.own.at[self.rows(at), :], self.from_end.at[at], self.sems[0].at[at],
                      self.sems[1].at[at], self.mate)

    def over(self, at):
        return remote(self.out.at[self.rows(at), :], self.from_mid.at[at], self.sems[2].at[at],
                      self.sems[3].at[at], self.other)

    def down(self, at):
        rows = self.rows(at)
        return remote(self.out.at[rows, :], self.out.at[rows, :], self.sems[4].at[at],
                      self.sems[5].at[at], self.mate)

    def launch(self, first, count):
        @pl.when(self.inner == 0)
        def _():
            def send(at, _):
                self.up(first + at).start()
                return 0

            lax.fori_loop(0, count, send, 0)

    def begin(self):
        self.launch(0, self.counts)

    def first(self, at):
        rows = self.rows(at)
        self.up(at).wait_recv()
        total = self.own[rows, :].astype(jnp.float32) + self.from_end[at].astype(jnp.float32)
        self.out[rows, :] = total.astype(self.out.dtype)
        self.over(at).start()

    def second(self, at):
        rows = self.rows(at)
        self.over(at).wait()
        total = self.out[rows, :].astype(jnp.float32) + self.from_mid[at].astype(jnp.float32)
        self.out[rows, :] = total.astype(self.out.dtype)
        self.down(at).start()

    def step(self, at, start=0, count=None):
        count = self.counts if count is None else count

        @pl.when(jnp.logical_and(self.inner == 1, at < count))
        def _():
            self.first(start + at)

        @pl.when(jnp.logical_and(self.inner == 1, jnp.logical_and(at > 1, at < count + 2)))
        def _():
            self.second(start + at - 2)

    def steps(self, first, last, start=0, count=None):
        def rest(at, _):
            self.step(at, start, count)
            return 0

        lax.fori_loop(first, last, rest, 0)

    def settle(self):
        @pl.when(self.inner == 0)
        def _():
            def take(at, _):
                self.up(at).wait_send()
                self.down(at).wait_recv()
                return 0

            lax.fori_loop(0, self.counts, take, 0)

        self.drain()

    def drain(self):
        @pl.when(self.inner == 1)
        def _():
            def drain(at, _):
                self.down(at).wait_send()
                return 0

            lax.fori_loop(0, self.counts, drain, 0)

    def end(self, done=0):
        self.steps(min(done, self.counts + 2), self.counts + 2)
        self.settle()


def line_scratch(counts, shape, low):
    buf = pltpu.VMEM((counts, shape[0] // counts, shape[1]), low)
    return [buf, buf] + [pltpu.SemaphoreType.DMA((counts,))] * 6


def turned(at):
    return 3 - at // 2, 1 - at % 2


def slice_peers(here):
    return [here.device(*turned(at)) for at in range(7)]


def kernel_call(kernel, out_shape, operands, specs, scratch, cid, name, out_specs=None):
    vm = pl.BlockSpec(memory_space=pltpu.VMEM)
    return pl.pallas_call(
        kernel,
        out_shape=out_shape,
        in_specs=specs,
        out_specs=out_specs or [vm] * len(out_shape),
        scratch_shapes=scratch,
        compiler_params=pltpu.CompilerParams(
            collective_id=cid, has_side_effects=True, vmem_limit_bytes=VMEM_LIMIT
        ),
        name=f"{name}_{cid}",
    )(*operands)


class Tiny:
    def __init__(self, here, src, dst, sems, spread):
        self.here, self.src, self.dst, self.sems, self.spread = here, src, dst, sems, spread
        self.peers = slice_peers(here)
        self.me = here.shard(0, 0)

    def tile(self, shard):
        return self.src.at[shard] if self.spread else self.src

    def copy(self, at):
        return remote(self.tile(self.here.shard(*turned(at))), self.dst.at[self.me], self.sems[0].at[at],
                      self.sems[1].at[at], self.peers[at])

    def begin(self):
        for at in range(7):
            self.copy(at).start()
        self.dst[self.me] = self.tile(self.me)[...]

    def end(self):
        for at in range(7):
            self.copy(at).wait()


class Reduce:
    def __init__(self, here, counts, product, refs, before=None):
        self.counts, self.product, self.before = counts, product, before
        self.held, self.sib_out, self.sib_in, self.from_x, self.from_y = refs[:5]
        self.sib_sems, self.x_sems, self.y_sems = refs[5:7], refs[7:9], refs[9:11]
        self.sib, self.xdev, self.ydev = here.device(0, 1), here.device(1, 0), here.device(2, 0)
        self.steps = 4 * counts
        self.ring = self.sib_out.shape[0]

    def streams(self, stage):
        far = stage // 3
        x_chip = jnp.where(stage == 0, 3, jnp.where(stage == 2, 0, 1))
        y_chip = jnp.where(stage == 0, 3, jnp.where(stage == 2, 0, 2))
        return (x_chip, far), (y_chip, 1 - far)

    def to_sib(self, step, stream):
        stage, at = step // self.counts, step % self.counts
        return remote(self.sib_out.at[step % self.ring, stream], self.sib_in.at[stage, stream, at],
                      self.sib_sems[0].at[stage, stream, at], self.sib_sems[1].at[stage, stream, at], self.sib)

    def to_x(self, hop, at, stage=0):
        return remote(self.held.at[stage, 0, at], self.from_x.at[hop, at], self.x_sems[0].at[hop, at],
                      self.x_sems[1].at[hop, at], self.xdev)

    def to_y(self, hop, at, stage=0):
        return remote(self.held.at[stage, 1, at], self.from_y.at[hop, at], self.y_sems[0].at[hop, at],
                      self.y_sems[1].at[hop, at], self.ydev)

    def compute(self, step):
        stage, at = step // self.counts, step % self.counts
        if self.before:
            for stop in range(3):
                @pl.when(step == stop * self.counts)
                def _():
                    self.before(stop)

        @pl.when(step >= self.ring)
        def _():
            for stream in range(2):
                self.to_sib(step - self.ring, stream).wait_send()

        for stream, (across, half) in enumerate(self.streams(stage)):
            self.sib_out[step % self.ring, stream] = self.product(across, 1, half, at).astype(jnp.bfloat16)
            self.held[stage, stream, at] = self.product(across, 0, half, at).astype(jnp.bfloat16)
        for stream in range(2):
            self.to_sib(step, stream).start()

    def finish(self, step):
        stage, at = step // self.counts, step % self.counts
        for stream in range(2):
            self.to_sib(step, stream).wait_recv()

        def total(stream):
            return self.held[stage, stream, at].astype(jnp.float32) + self.sib_in[stage, stream, at].astype(
                jnp.float32)

        @pl.when(stage < 3)
        def _():
            for stream in range(2):
                self.held[stage, stream, at] = total(stream).astype(jnp.bfloat16)

        @pl.when(stage == 3)
        def _():
            self.to_y(0, at).wait_recv()
            self.held[3, 0, at] = (total(0) + self.from_y[0, at].astype(jnp.float32)).astype(jnp.bfloat16)
            self.to_x(0, at).wait_recv()
            self.held[3, 1, at] = (total(1) + self.from_x[0, at].astype(jnp.float32)).astype(jnp.bfloat16)

        @pl.when(stage != 2)
        def _():
            hop = stage - stage // 3
            self.to_x(hop, at, stage).start()
            self.to_y(hop, at, stage).start()

    def run(self, hook=None):
        def body(step, _):
            @pl.when(step < self.steps)
            def _():
                self.compute(step)

            @pl.when(step > 0)
            def _():
                self.finish(step - 1)

            if hook:
                hook(step)
            return 0

        lax.fori_loop(0, self.steps + 1, body, 0)
        return self.steps + 1

    def end(self, emit):
        def last(at, _):
            values = []
            for half in range(2):
                xs, ys = (1, 2) if half == 0 else (2, 1)
                self.to_x(xs, at).wait_recv()
                self.to_y(ys, at).wait_recv()
                values.append(self.held[2, half, at].astype(jnp.float32) + self.from_x[xs, at].astype(jnp.float32)
                              + self.from_y[ys, at].astype(jnp.float32))
            emit(at, *values)
            for hop in range(3):
                self.to_x(hop, at).wait_send()
                self.to_y(hop, at).wait_send()
            return 0

        lax.fori_loop(0, self.counts, last, 0)

        def drain(at, _):
            for stream in range(2):
                self.to_sib(self.steps - self.ring + at, stream).wait_send()
            return 0

        lax.fori_loop(0, self.ring, drain, 0)


def reduce_scratch(counts, rows, width, ring=4):
    low, dma = jnp.bfloat16, pltpu.SemaphoreType.DMA
    block = pltpu.VMEM((4, 2, counts, rows, width), low)
    landed = pltpu.VMEM((3, counts, rows, width), low)
    sent = pltpu.VMEM((ring, 2, rows, width), low)
    return [block, sent, block, landed, landed] + [dma((4, 2, counts))] * 2 + [dma((3, counts))] * 4


class Spread:
    def __init__(self, here, counts, refs):
        self.counts = counts
        self.got = refs[0]
        self.x_sems, self.y_sems, self.sib_sems = refs[1:3], refs[3:5], refs[5:7]
        self.core = here.core
        self.sib, self.xdev, self.ydev = here.device(0, 1), here.device(1, 0), here.device(2, 0)

    def slot(self, across, half, at):
        return self.got.at[across, self.core, half, at]

    def x_copy(self, hop, at):
        half = jnp.minimum(hop, 1)
        src = self.slot(2 * (hop // 2), half, at)
        dst = self.slot(1 + 2 * (hop // 2), half, at)
        return remote(src, dst, self.x_sems[0].at[hop, at], self.x_sems[1].at[hop, at], self.xdev)

    def y_copy(self, hop, at):
        half = 1 - jnp.minimum(hop, 1)
        src = self.slot(hop // 2, half, at)
        dst = self.slot(2 + hop // 2, half, at)
        return remote(src, dst, self.y_sems[0].at[hop, at], self.y_sems[1].at[hop, at], self.ydev)

    def streams(self, stage):
        some, last, late = jnp.minimum(stage, 1), stage // 3, stage // 2
        return (some + 2 * last, late), (2 * some + last, 1 - late)

    def sib_copy(self, stage, stream, at):
        across, half = self.streams(stage)[stream]
        slot = self.slot(across, half, at)
        spot = (stage, stream, at)
        return remote(slot, slot, self.sib_sems[0].at[spot], self.sib_sems[1].at[spot], self.sib)

    def begin(self):
        def first(at, _):
            self.x_copy(0, at).start()
            self.y_copy(0, at).start()
            return 0

        def own(at, _):
            self.sib_copy(0, 0, at).start()
            self.sib_copy(0, 1, at).start()
            return 0

        lax.fori_loop(0, self.counts, first, 0)
        lax.fori_loop(0, self.counts, own, 0)

    def run(self, blocks, hook=None, done=None):
        counts = self.counts

        def body(step, _):
            stage, at = step // counts, step % counts

            @pl.when(jnp.logical_and(stage > 0, stage < 4))
            def _():
                self.x_copy(stage - 1, at).wait_recv()
                self.sib_copy(stage, 0, at).start()
                self.y_copy(stage - 1, at).wait_recv()
                self.sib_copy(stage, 1, at).start()

            @pl.when(jnp.logical_and(stage > 0, stage < 3))
            def _():
                self.x_copy(stage, at).start()
                self.y_copy(stage, at).start()

            @pl.when(step > 0)
            def _():
                old, spot = (step - 1) // counts, (step - 1) % counts
                for stream, (across, half) in enumerate(self.streams(old)):
                    self.sib_copy(old, stream, spot).wait_recv()
                    blocks(across, half, spot)
                if done:
                    done(old, spot)

            if hook:
                hook(step)
            return 0

        lax.fori_loop(0, 4 * counts + 1, body, 0)
        return 4 * counts + 1

    def end(self):
        def drain(at, _):
            for hop in range(3):
                self.x_copy(hop, at).wait_send()
                self.y_copy(hop, at).wait_send()
            for stage in range(4):
                self.sib_copy(stage, 0, at).wait_send()
                self.sib_copy(stage, 1, at).wait_send()
            return 0

        lax.fori_loop(0, self.counts, drain, 0)


def spread_scratch(counts, rows, width):
    dma = pltpu.SemaphoreType.DMA
    return [pltpu.VMEM((4, 2, 2, counts, rows, width), jnp.bfloat16)] + [dma((3, counts))] * 4 + [
        dma((4, 2, counts))] * 2


def row_span(here, across, other, rows):
    return pl.ds(pl.multiple_of(here.shard(across, other) * rows, rows), rows)


def dot_nt(left, right):
    return lax.dot_general(left, right, (((1,), (1,)), ((), ())), preferred_element_type=jnp.float32)


def dot_tn(left, right):
    return lax.dot_general(left, right, (((0,), (0,)), ((), ())), preferred_element_type=jnp.float32)


def dot_nn(left, right):
    return jnp.dot(left, right, preferred_element_type=jnp.float32)


def products(here, act, weight, nt, rows, width, counts):
    def product(across, other, half, at):
        cols = pl.ds(pl.multiple_of((half * counts + at) * width, width), width)
        block = act[row_span(here, across, other, rows), :]
        return dot_nt(block, weight[cols, :]) if nt else dot_nn(block, weight[:, cols])

    return product


def diagonal():
    return (lax.broadcasted_iota(jnp.int32, (LANES, LANES), 0) ==
            lax.broadcasted_iota(jnp.int32, (LANES, LANES), 1)).astype(jnp.float32)


def to_tile(tile, first, column, eye):
    for at in range(column.shape[0] // LANES):
        spread = column[at * LANES : (at + 1) * LANES, :] * eye
        tile[first + at : first + at + 1, :] = jnp.sum(spread, axis=0, keepdims=True)


def from_tile(row, eye):
    return jnp.sum(eye * row, axis=1, keepdims=True)


def make_tables(here, rows, segs, cos, sin, mask):
    eye = diagonal()
    tiles = rows // LANES
    freqs = jnp.exp(lax.broadcasted_iota(jnp.int32, (1, LANES), 1).astype(jnp.float32) * (-math.log(10000.0) / LANES))
    lane = lax.broadcasted_iota(jnp.int32, (1, LANES), 1)
    line = lax.broadcasted_iota(jnp.int32, (LANES, 1), 0)

    def row_of(side, at):
        return ((here.seq + side) % 2) * tiles + at

    for side in range(2):
        for at in range(tiles):
            row = row_of(side, at)
            ids = from_tile(segs[pl.ds(row, 1), :], eye)
            before = jnp.zeros((LANES, 1), jnp.float32)
            for other in range(2 * tiles):
                smaller = segs[other : other + 1, :] < ids
                before += jnp.sum(smaller.astype(jnp.float32), axis=-1, keepdims=True)
            index = row * LANES + line
            angles = (index.astype(jnp.float32) - before) * freqs
            span = slice(at * LANES, (at + 1) * LANES)
            cos[side, span, :] = jnp.cos(angles)
            sin[side, span, :] = jnp.sin(angles)
            if side == 0:
                for key_side in range(2):
                    for key_at in range(tiles):
                        key_row = row_of(key_side, key_at)
                        same = segs[pl.ds(key_row, 1), :] == ids
                        allowed = jnp.logical_and(same, key_row * LANES + lane <= index)
                        first = key_side * rows + key_at * LANES
                        mask[span, first : first + LANES] = allowed.astype(jnp.float32)


def open_kernel(rows, width, counts, tokens, gain, w_query, kv_weight, segs, qkv, x_low, act_t, w_qkv, rms, cos, sin,
                mask, *refs):
    here = Place()
    cols = gain.shape[1]
    act, turn_send, turn_recv, local_sems = refs[:4]
    me = here.shard(0, 0)
    own_rows = pl.ds(pl.multiple_of(me * rows, rows), rows)

    def turn_copy(at):
        across, other = turned(at)
        first = pl.multiple_of(here.shard(across, other) * cols, cols)
        return remote(tokens.at[:, pl.ds(first, cols)], x_low.at[own_rows, :], turn_send.at[at], turn_recv.at[at],
                      here.device(across, other))

    wide = w_query.shape[1]
    local = [
        pltpu.make_async_copy(w_query, w_qkv.at[:, :wide], local_sems.at[0]),
        pltpu.make_async_copy(kv_weight, w_qkv.at[:, wide:], local_sems.at[1]),
        pltpu.make_async_copy(tokens.at[:, pl.ds(pl.multiple_of(me * cols, cols), cols)], x_low.at[own_rows, :],
                              local_sems.at[2]),
    ]
    for copy in local:
        copy.start()
    greet(here, slice_peers(here))
    for at in range(7):
        turn_copy(at).start()
    for copy in local:
        copy.wait()

    def squares(at, total):
        values = tokens[:, pl.ds(pl.multiple_of(at * cols, cols), cols)].astype(jnp.float32)
        return total + jnp.sum(values * values, axis=-1, keepdims=True)

    total = lax.fori_loop(0, 8, squares, jnp.zeros((rows, 1), jnp.float32))
    rms[...] = jnp.broadcast_to(lax.rsqrt(total / (8 * cols) + EPS), rms.shape)
    make_tables(here, rows, segs, cos, sin, mask)

    def prepare(first, count):
        def one(step, _):
            at = first + step
            span = row_span(here, *turned(at), rows)
            value = (x_low[span, :].astype(jnp.float32) * gain[...]).astype(act.dtype)
            act[span, :] = value
            return 0

        lax.fori_loop(0, count, one, 0)

    def before(stop):
        first, count = ((0, 2), (2, 4), (6, 2))[stop]
        for at in range(first, min(first + count, 7)):
            turn_copy(at).wait_recv()
        prepare(first, count)

    def flip():
        def one(shard, _):
            span = pl.ds(pl.multiple_of(shard * rows, rows), rows)
            act_t[:, span] = act[span, :].T
            return 0

        lax.fori_loop(0, 8, one, 0)

    product = products(here, act, w_qkv, False, rows, width, counts)
    total = Reduce(here, counts, product, refs[4:15], before)
    total.run()
    flip()

    def emit(at, first, second):
        for half, value in enumerate((first, second)):
            qkv[:, pl.ds(pl.multiple_of((half * counts + at) * width, width), width)] = value

    total.end(emit)
    for at in range(7):
        turn_copy(at).wait_send()


def opening(tokens, gain, w_query, kv_weight, segs, cid, width=256):
    rows = tokens.shape[0]
    cols, wide = w_query.shape
    every = wide + kv_weight.shape[1]
    counts = every // (2 * width)
    low, f32 = jnp.bfloat16, jnp.float32
    dma = pltpu.SemaphoreType.DMA
    vm = pl.BlockSpec(memory_space=pltpu.VMEM)
    hbm = pl.BlockSpec(memory_space=pl.ANY)
    out_shape = [
        jax.ShapeDtypeStruct((rows, every), f32),
        jax.ShapeDtypeStruct((8 * rows, cols), low),
        jax.ShapeDtypeStruct((cols, 8 * rows), low),
        jax.ShapeDtypeStruct((cols, every), low),
        jax.ShapeDtypeStruct((rows, LANES), f32),
        jax.ShapeDtypeStruct((2, rows, LANES), f32),
        jax.ShapeDtypeStruct((2, rows, LANES), f32),
        jax.ShapeDtypeStruct((rows, 2 * rows), f32),
    ]
    scratch = [pltpu.VMEM((8 * rows, cols), low), dma((7,)), dma((7,)), dma((3,))]
    scratch += reduce_scratch(counts, rows, width)
    kernel = functools.partial(open_kernel, rows, width, counts)
    return kernel_call(kernel, out_shape, [tokens, gain, w_query, kv_weight, segs],
                       [vm, vm, hbm, hbm, vm], scratch, cid, "open")


def scatter_kernel(rows, width, counts, line_counts, act, weight, line_own, out, line_out, *refs):
    here = Place()
    line = Line(here, line_counts, [line_own, line_out] + list(refs[11:]))
    product = products(here, act, weight, True, rows, width, counts)
    total = Reduce(here, counts, product, refs[:11])
    greet(here, slice_peers(here), True)
    line.begin()
    done = total.run(line.step)
    line.end(done)

    def emit(at, first, second):
        for half, value in enumerate((first, second)):
            out[:, pl.ds(pl.multiple_of((half * counts + at) * width, width), width)] = value

    total.end(emit)


def scatter_product(act, weight, width, cid, line, line_counts=16):
    rows = act.shape[0] // 8
    every = weight.shape[0]
    counts = every // (2 * width)
    vm = pl.BlockSpec(memory_space=pltpu.VMEM)
    out_shape = [
        jax.ShapeDtypeStruct((rows, every), jnp.float32),
        jax.ShapeDtypeStruct(line.shape, line.dtype),
    ]
    scratch = reduce_scratch(counts, rows, width) + line_scratch(line_counts, line.shape, line.dtype)
    kernel = functools.partial(scatter_kernel, rows, width, counts, line_counts)
    return kernel_call(kernel, out_shape, [act, weight, line], [vm] * 3, scratch, cid, "scatter_product")


def ffn_kernel(rows, width, counts, x_low, attn, gain, w_gate, w_up, d_hidden, hidden, d_gate, d_up, act_t, tile_out,
               *refs):
    here = Place()
    cols = gain.shape[1]
    act, weight, tiny_own, tiny_all, tiny_send, tiny_recv, dots, local_sems = refs[:8]
    tiny = Tiny(here, tiny_own, tiny_all, (tiny_send, tiny_recv), True)
    half_cols = counts * width
    local = [
        pltpu.make_async_copy(w_gate, weight.at[:, :half_cols], local_sems.at[0]),
        pltpu.make_async_copy(w_up, weight.at[:, half_cols:], local_sems.at[1]),
    ]
    for copy in local:
        copy.start()
    eye = diagonal()
    tiny_own[...] = jnp.zeros_like(tiny_own)

    def prepare(shard, _):
        for at in range(rows // LANES):
            span = pl.ds(pl.multiple_of(shard * rows + at * LANES, LANES), LANES)
            resid = x_low[span, :].astype(jnp.float32) + attn[span, :].astype(jnp.float32)
            act[span, :] = (resid * gain[...]).astype(act.dtype)
            square = jnp.sum(resid * resid, axis=-1, keepdims=True)
            tiny_own[shard, at : at + 1, :] = jnp.sum(square * eye, axis=0, keepdims=True)
        return 0

    lax.fori_loop(0, 8, prepare, 0)
    greet(here, slice_peers(here))
    tiny.begin()
    for copy in local:
        copy.wait()
    product = products(here, act, weight, False, rows, width, counts)
    total = Reduce(here, counts, product, refs[8:19])
    total.run()

    def flip(shard, _):
        span = pl.ds(pl.multiple_of(shard * rows, rows), rows)
        act_t[:, span] = act[span, :].T
        return 0

    lax.fori_loop(0, 8, flip, 0)
    tiny.end()
    tiles = rows // LANES
    mean = [from_tile(jnp.sum(tiny_all[:, at, :], axis=0, keepdims=True), eye) for at in range(tiles)]
    scale = lax.rsqrt(jnp.concatenate(mean, axis=0) / (8 * cols) + EPS)
    dots[...] = jnp.zeros_like(dots)
    coeff = math.sqrt(2.0 / math.pi)

    def emit(at, first, second):
        span = pl.ds(pl.multiple_of(at * width, width), width)
        gate, up = first * scale, second * scale
        inner = jnp.tanh(coeff * (gate + 0.044715 * (gate * gate * gate)))
        gelu = 0.5 * gate * (1.0 + inner)
        slope = 0.5 * (1.0 + inner) + 0.5 * gate * (1.0 - inner * inner) * (
            coeff * (1.0 + 3.0 * 0.044715 * gate * gate))
        cot = d_hidden[:, span]
        hidden[:, span] = (gelu * up).astype(hidden.dtype)
        back_gate, back_up = cot * up * slope, cot * gelu
        d_gate[:, span] = (back_gate * scale).astype(d_gate.dtype)
        d_up[:, span] = (back_up * scale).astype(d_up.dtype)
        dots[...] += jnp.sum(back_gate * gate + back_up * up, axis=-1, keepdims=True)

    total.end(emit)
    tile_out[...] = jnp.zeros_like(tile_out)
    to_tile(tile_out, 0, dots[...] * (scale * scale * (1.0 / (8 * cols))), eye)


def ffn_scatter(x_low, attn, gain, w_gate, w_up, d_hidden, cid, width=512):
    rows, half = d_hidden.shape
    cols = gain.shape[1]
    counts = half // width
    low, f32 = jnp.bfloat16, jnp.float32
    dma = pltpu.SemaphoreType.DMA
    vm = pl.BlockSpec(memory_space=pltpu.VMEM)
    hbm = pl.BlockSpec(memory_space=pl.ANY)
    out_shape = [jax.ShapeDtypeStruct((rows, half), low)] * 3 + [
        jax.ShapeDtypeStruct((cols, 8 * rows), low),
        jax.ShapeDtypeStruct((8, LANES), f32),
    ]
    scratch = [
        pltpu.VMEM((8 * rows, cols), low),
        pltpu.VMEM((cols, 2 * half), low),
        pltpu.VMEM((8, 8, LANES), f32),
        pltpu.VMEM((8, 8, LANES), f32),
        dma((7,)), dma((7,)),
        pltpu.VMEM((rows, 1), f32),
        dma((2,)),
    ] + reduce_scratch(counts, rows, width)
    kernel = functools.partial(ffn_kernel, rows, width, counts)
    return kernel_call(kernel, out_shape, [x_low, attn, gain, w_gate, w_up, d_hidden], [vm, vm, vm, hbm, hbm, vm],
                       scratch, cid, "ffn")


def load_own(spread, payload, width, counts, sems):
    copies = []
    for half in range(2):
        for at in range(counts):
            first = at * width + (half * counts * width if len(payload) == 1 else 0)
            src = payload[half % len(payload)].at[:, first : first + width]
            copies.append(pltpu.make_async_copy(src, spread.slot(0, half, at), sems.at[half, at]))
    return copies


def chip_place(here, per):
    def place(at):
        return here.shard(at // (2 * per), at // per % 2) * per + at % per

    return place


def back_kernel(rows, width, counts, act_t, w_gate, w_up, d_gate, d_up, dots, x_low, attn, gain, d_norm, gain_grad,
                grad_gate, grad_up, *refs):
    here = Place()
    spread = Spread(here, counts, refs[:7])
    tiny_all, tiny_send, tiny_recv, own_sems, weight, sums, grads, staged, local_sems, out_sems = refs[7:17]
    contrib, rest, rest_sems = refs[17:20]
    line = Line(here, 4, [contrib, d_norm] + list(refs[20:]), chip_place(here, 2))
    tiny = Tiny(here, dots, tiny_all, (tiny_send, tiny_recv), False)
    half_cols = counts * width
    local = [
        pltpu.make_async_copy(w_gate, weight.at[:, :half_cols], local_sems.at[0]),
        pltpu.make_async_copy(w_up, weight.at[:, half_cols:], local_sems.at[1]),
    ]
    own = load_own(spread, (d_gate, d_up), width, counts, own_sems)
    for copy in own + local:
        copy.start()
    greet(here, tiny.peers, True)
    for copy in own:
        copy.wait()
    tiny.begin()
    spread.begin()
    sums[...] = jnp.zeros_like(sums)
    for copy in local:
        copy.wait()

    def columns(half, at):
        return pl.ds(pl.multiple_of((half * counts + at) * width, width), width)

    def clear(at, _):
        grads[:, columns(0, at)] = jnp.zeros((grads.shape[0], width), jnp.float32)
        return 0

    lax.fori_loop(0, 2 * counts, clear, 0)

    def blocks(across, half, at):
        cols = columns(half, at)
        gained = grads[:, cols]
        for other in range(2):
            row = row_span(here, across, other, rows)
            block = spread.got[across, (spread.core + other) % 2, half, at]
            sums[row, :] += dot_nt(block, weight[:, cols])
            gained = gained + dot_nn(act_t[:, row], block)
        grads[:, cols] = gained

    def leave(half, at):
        spot = pl.ds(pl.multiple_of(at * width, width), width)
        return pltpu.make_async_copy(staged.at[half], (grad_gate, grad_up)[half].at[:, spot],
                                     out_sems.at[half, at])

    eye = diagonal()
    gain_grad[...] = jnp.zeros_like(gain_grad)

    def close_chip(chip, target):
        def close_shard(other, _):
            shard = here.shard(chip, other)
            span = pl.ds(pl.multiple_of(shard * rows, rows), rows)
            loads = [pltpu.make_async_copy(src.at[span, :], rest.at[at], rest_sems.at[at])
                     for at, src in enumerate((x_low, attn))]
            for copy in loads:
                copy.start()
            for copy in loads:
                copy.wait()
            for at in range(rows // LANES):
                span = pl.ds(pl.multiple_of(shard * rows + at * LANES, LANES), LANES)
                piece = slice(at * LANES, (at + 1) * LANES)
                dot = from_tile(tiny_all[shard, at : at + 1, :], eye)
                resid = rest[0, piece, :].astype(jnp.float32) + rest[1, piece, :].astype(jnp.float32)
                value = sums[span, :]
                target[span, :] = (value * gain[...] - resid * dot).astype(target.dtype)
                gain_grad[...] += jnp.sum(value * resid, axis=0, keepdims=True)
            return 0

        lax.fori_loop(0, 2, close_shard, 0)

    def done(stage, at):
        @pl.when(jnp.logical_and(stage == 3, at > 0))
        def _():
            leave(0, at - 1).wait()
            leave(1, at - 1).wait()

        @pl.when(stage == 3)
        def _():
            for half in range(2):
                staged[half] = grads[:, columns(half, at)].astype(staged.dtype)
            leave(0, at).start()
            leave(1, at).start()

        @pl.when(jnp.logical_and(at == counts - 1, stage == 0))
        def _():
            close_chip(0, contrib)
            line.launch(0, 4)

        @pl.when(jnp.logical_and(at == counts - 1, stage == 2))
        def _():
            lax.fori_loop(1, 3, lambda chip, _: (close_chip(chip, d_norm), 0)[1], 0)

    def hook(step):
        @pl.when(jnp.logical_and(step >= counts, step < counts + 6))
        def _():
            line.step(step - counts)

    tiny.end()
    spread.run(blocks, hook, done)
    close_chip(3, d_norm)
    line.settle()
    spread.end()

    def drain(at, _):
        leave(0, at).wait()
        leave(1, at).wait()
        return 0

    lax.fori_loop(counts - 1, counts, drain, 0)


def back_gather(act_t, w_gate, w_up, d_gate, d_up, dots, x_low, attn, gain, cid, width=512):
    cols, total = act_t.shape
    rows, half = d_gate.shape
    counts = half // width
    low, f32 = jnp.bfloat16, jnp.float32
    dma = pltpu.SemaphoreType.DMA
    vm = pl.BlockSpec(memory_space=pltpu.VMEM)
    hbm = pl.BlockSpec(memory_space=pl.ANY)
    out_shape = [
        jax.ShapeDtypeStruct((total, cols), low),
        jax.ShapeDtypeStruct((1, cols), f32),
        jax.ShapeDtypeStruct((cols, half), low),
        jax.ShapeDtypeStruct((cols, half), low),
    ]
    scratch = spread_scratch(counts, rows, width) + [
        pltpu.VMEM((8, 8, LANES), f32), dma((7,)), dma((7,)), dma((2, counts)),
        pltpu.VMEM((cols, 2 * half), low),
        pltpu.VMEM((total, cols), f32),
        pltpu.VMEM((cols, 2 * half), f32),
        pltpu.VMEM((2, cols, width), low),
        dma((2,)), dma((2, counts)),
        pltpu.VMEM((total, cols), low),
        pltpu.VMEM((2, rows, cols), low),
        dma((2,)),
    ] + line_scratch(4, (4 * rows // 2, cols), low)
    operands = [act_t, w_gate, w_up, d_gate, d_up, dots, x_low, attn, gain]
    kernel = functools.partial(back_kernel, rows, width, counts)
    return kernel_call(kernel, out_shape, operands, [vm] + [hbm] * 4 + [vm, hbm, hbm, vm], scratch, cid, "back",
                       [vm, vm, hbm, hbm])


def down_kernel(rows, width, counts, cot, weight, hidden, d_norm, ffn, d_attn, grad, *refs):
    here = Place()
    spread = Spread(here, counts, refs[:7])
    own_sems, sums, grads, staged, out_sems, norm_out, part = refs[7:14]
    place = chip_place(here, 2)
    norm_line = Line(here, 12, [d_norm, norm_out] + list(refs[14:22]), lambda at: place(at + 4))
    line = Line(here, 4, [part, ffn] + list(refs[22:]), place)
    own = load_own(spread, (hidden,), width, counts, own_sems)
    for copy in own:
        copy.start()
    greet(here, slice_peers(here), True)
    norm_line.begin()
    for copy in own:
        copy.wait()
    spread.begin()
    sums[...] = jnp.zeros_like(sums)
    grads[...] = jnp.zeros_like(grads)

    def columns(half, at):
        return pl.ds(pl.multiple_of((half * counts + at) * width, width), width)

    def blocks(across, half, at):
        cols = columns(half, at)
        gained = grads[cols, :]
        for other in range(2):
            row = row_span(here, across, other, rows)
            block = spread.got[across, (spread.core + other) % 2, half, at]
            sums[row, :] += dot_nn(block, weight[cols, :])
            gained = gained + dot_tn(block, cot[row, :])
        grads[cols, :] = gained

    def leave(half, at):
        return pltpu.make_async_copy(staged.at[at % 2, half], grad.at[columns(half, at), :], out_sems.at[half, at])

    def done(stage, at):
        @pl.when(jnp.logical_and(stage == 3, at > 1))
        def _():
            leave(0, at - 2).wait()
            leave(1, at - 2).wait()

        @pl.when(stage == 3)
        def _():
            for half in range(2):
                staged[at % 2, half] = grads[columns(half, at), :].astype(staged.dtype)
            leave(0, at).start()
            leave(1, at).start()

        @pl.when(jnp.logical_and(at == counts - 1, stage == 0))
        def _():
            close_chip(0, part)
            line.launch(0, 4)

    def close_chip(chip, target):
        def close_shard(other, _):
            span = row_span(here, chip, other, rows)
            target[span, :] = sums[span, :].astype(target.dtype)
            return 0

        lax.fori_loop(0, 2, close_shard, 0)

    last_steps = 4 * counts - 5

    def hook(step):
        @pl.when(jnp.logical_and(step % 3 < 2, step <= last_steps))
        def _():
            norm_line.step(step // 3 * 2 + step % 3)

        @pl.when(step >= last_steps)
        def _():
            line.step(step - last_steps)

    spread.run(blocks, hook, done)
    lax.fori_loop(1, 4, lambda chip, _: (close_chip(chip, ffn), 0)[1], 0)
    norm_line.settle()

    def add_norm(at, _):
        def add(source):
            span = row_span(here, at // 2, at % 2, rows)
            d_attn[span, :] = (cot[span, :].astype(jnp.float32) + source[span, :].astype(jnp.float32)).astype(
                d_attn.dtype)

        @pl.when(at < 2)
        def _():
            add(d_norm)

        @pl.when(at >= 2)
        def _():
            add(norm_out)
        return 0

    lax.fori_loop(0, 8, add_norm, 0)
    line.settle()
    spread.end()

    def drain(at, _):
        leave(0, at).wait()
        leave(1, at).wait()
        return 0

    lax.fori_loop(counts - 2, counts, drain, 0)


def down_gather(cot, weight, hidden, d_norm, cid, width=256):
    total, cols = cot.shape
    rows, every = hidden.shape
    counts = every // (2 * width)
    low, f32 = jnp.bfloat16, jnp.float32
    dma = pltpu.SemaphoreType.DMA
    vm = pl.BlockSpec(memory_space=pltpu.VMEM)
    hbm = pl.BlockSpec(memory_space=pl.ANY)
    out_shape = [
        jax.ShapeDtypeStruct((total, cols), low),
        jax.ShapeDtypeStruct((total, cols), low),
        jax.ShapeDtypeStruct(weight.shape, low),
    ]
    scratch = spread_scratch(counts, rows, width) + [
        dma((2, counts)),
        pltpu.VMEM((total, cols), f32),
        pltpu.VMEM(weight.shape, f32),
        pltpu.VMEM((2, 2, width, cols), low),
        dma((2, counts)),
        pltpu.VMEM((total, cols), low),
        pltpu.VMEM((total, cols), low),
    ] + line_scratch(12, (12 * rows // 2, cols), low) + line_scratch(
        4, (4 * rows // 2, cols), low)
    kernel = functools.partial(down_kernel, rows, width, counts)
    return kernel_call(kernel, out_shape, [cot, weight, hidden, d_norm], [vm, vm, hbm, vm], scratch, cid, "down",
                       [vm, vm, hbm])


def attend_kernel(rows, heads, cols, qkv, rms, cos, sin, mask, w_out, cot, part, mixed_all, g_col, kv, probs, queries,
                  pair_rms, *refs):
    here = Place()
    spread = Spread(here, heads // 2, refs[:7])
    sums, pair_sems, turn_send, turn_recv, local_sem, tiny_own, tiny_pair = refs[7:14]
    got, core = spread.got, here.core
    greet(here, slice_peers(here))
    me = here.shard(0, 0)

    def turn_copy(at):
        across, other = turned(at)
        first = pl.multiple_of(here.shard(across, other) * cols, cols)
        return remote(cot.at[:, pl.ds(first, cols)], g_col.at[pl.ds(pl.multiple_of(me * rows, rows), rows), :],
                      turn_send.at[at], turn_recv.at[at], here.device(across, other))

    own_turn = pltpu.make_async_copy(cot.at[:, pl.ds(pl.multiple_of(me * cols, cols), cols)],
                                     g_col.at[pl.ds(pl.multiple_of(me * rows, rows), rows), :], local_sem)
    own_turn.start()
    half = HD // 2
    scale = 1.0 / math.sqrt(HD)
    wide = heads * HD

    def rotated(first):
        lead = qkv[:, first : first + half] * rms[...]
        trail = qkv[:, first + half : first + HD] * rms[...]
        return lead * cos[0] - trail * sin[0], trail * cos[0] + lead * sin[0]

    low_k, high_k = rotated(wide)
    kv[0, :, :half] = low_k.astype(kv.dtype)
    kv[0, :, half:HD] = high_k.astype(kv.dtype)
    for at in range(2):
        first = HD + at * half
        kv[0, :, first : first + half] = (qkv[:, wide + first : wide + first + half] * rms[...]).astype(kv.dtype)
    eye = diagonal()
    tiny_own[...] = jnp.zeros_like(tiny_own)
    to_tile(tiny_own, 0, rms[:, :1], eye)
    pair_rms[0] = rms[...]
    pair = remote(kv.at[0], kv.at[1], pair_sems.at[0], pair_sems.at[1], spread.ydev)
    tiny = remote(tiny_own, tiny_pair, pair_sems.at[2], pair_sems.at[3], spread.ydev)
    for head in range(heads):
        if head == 1:
            pair.start()
            tiny.start()
            turn_copy(2 * (3 - 1)).start()
            turn_copy(2 * (3 - 1) + 1).start()
        lead, trail = rotated(head * HD)
        queries[:, head * HD : head * HD + half] = (lead * scale).astype(queries.dtype)
        queries[:, head * HD + half : (head + 1) * HD] = (trail * scale).astype(queries.dtype)
    pair.wait()
    for at in range(7):
        if at // 2 != 2:
            turn_copy(at).start()

    def one_head(head, _):
        query = queries[:, pl.ds(pl.multiple_of(head * HD, HD), HD)]
        scores = jnp.concatenate([dot_nt(query, kv[0, :, :HD]), dot_nt(query, kv[1, :, :HD])], axis=1)
        scores = jnp.where(mask[...] > 0, scores, NEG)
        expd = jnp.exp(scores - jnp.max(scores, axis=-1, keepdims=True))
        prob = expd / jnp.sum(expd, axis=-1, keepdims=True)
        probs[head] = prob
        prob_low = prob.astype(jnp.bfloat16)
        mixed = dot_nn(prob_low[:, :rows], kv[0, :, HD:]) + dot_nn(prob_low[:, rows:], kv[1, :, HD:])
        got[0, core, head // (heads // 2), head % (heads // 2)] = mixed.astype(got.dtype)
        return 0

    lax.fori_loop(0, heads, one_head, 0)
    sums[...] = jnp.zeros_like(sums)
    spread.begin()

    def blocks(across, half_at, at):
        span = pl.ds(pl.multiple_of((half_at * (heads // 2) + at) * HD, HD), HD)
        for other in range(2):
            row = row_span(here, across, other, rows)
            block = got[across, (core + other) % 2, half_at, at]
            mixed_all[row, span] = block
            sums[row, :] += dot_nn(block, w_out[span, :])

    spread.run(blocks)
    part[...] = sums[...].astype(part.dtype)
    spread.end()
    tiny.wait()
    for at in range(rows // LANES):
        values = jnp.broadcast_to(from_tile(tiny_pair[at : at + 1, :], eye), (LANES, LANES))
        pair_rms[1, at * LANES : (at + 1) * LANES, :] = values
    own_turn.wait()
    for at in range(7):
        turn_copy(at).wait()


def attend(qkv, rms, cos, sin, mask, w_out, cot, cid):
    rows = qkv.shape[0]
    wide, cols = w_out.shape
    heads = wide // HD
    low, f32 = jnp.bfloat16, jnp.float32
    dma = pltpu.SemaphoreType.DMA
    vm = pl.BlockSpec(memory_space=pltpu.VMEM)
    out_shape = [
        jax.ShapeDtypeStruct((8 * rows, cols), low),
        jax.ShapeDtypeStruct((8 * rows, wide), low),
        jax.ShapeDtypeStruct((8 * rows, cols), low),
        jax.ShapeDtypeStruct((2, rows, 2 * HD), low),
        jax.ShapeDtypeStruct((heads, rows, 2 * rows), f32),
        jax.ShapeDtypeStruct((rows, wide), low),
        jax.ShapeDtypeStruct((2,) + rms.shape, f32),
    ]
    scratch = spread_scratch(heads // 2, rows, HD) + [
        pltpu.VMEM((8 * rows, cols), f32), dma((4,)), dma((7,)), dma((7,)), dma(()),
        pltpu.VMEM((8, LANES), f32), pltpu.VMEM((8, LANES), f32)]
    kernel = functools.partial(attend_kernel, rows, heads, cols)
    return kernel_call(kernel, out_shape, [qkv, rms, cos, sin, mask, w_out, cot], [vm] * 7, scratch, cid,
                       "attend")


def tail_kernel(rows, heads, per, d_attn, w_out, queries, kv, probs, rms, cos, sin, act_t, w_qkv, ffn, x_low,
                attn, gain, gain_grad, mixed_all, d_tok, out, grad_query, grad_out, kv_sum, gain_tiles, *refs):
    here = Place()
    width = HD
    counts = heads // 2
    part = rows // 2
    refs = list(refs)
    line_counts = 8 * per
    cols = d_attn.shape[1]
    extra = cols // (rows // per)

    def take(count):
        taken_refs = refs[:count]
        del refs[:count]
        return taken_refs

    total_refs = take(11)
    spread = Spread(here, 1, take(7))
    d_mixed, tiny_own, tiny_all, d_kv, give, taken, give_sems, tiny_send, tiny_recv = take(9)
    grad, grad_mixed, gain_sum, tile, tile_send, tile_recv, put_sems, local_sems, mixed_two, mixed_sems = take(10)

    def far(at):
        return turned(at // per)

    def near(at):
        at = jnp.minimum(at, line_counts - 1)
        x_stream, y_stream = spread.streams(at // 4)
        second = at // 2 % 2
        across = x_stream[0] + second * (y_stream[0] - x_stream[0])
        half_at = x_stream[1] + second * (y_stream[1] - x_stream[1])
        return across, at % 2, half_at

    def place_ffn(at):
        return here.shard(*far(at)) * per + at % per

    def place_tok(at):
        across, other, half_at = near(at)
        return jnp.where(at < line_counts, here.shard(across, other) * per + half_at, at)

    ffn_sum, leaving = take(2)
    by_chip = chip_place(here, per)
    line = Line(here, 6 * per, [ffn, ffn_sum] + take(8), lambda at: by_chip(at + 2 * per))
    contrib, summed = take(2)
    line_tok = Line(here, line_counts + extra, [contrib, summed] + take(8), place_tok)
    tiny = Tiny(here, tiny_own, tiny_all, (tiny_send, tiny_recv), False)
    got, core = spread.got, here.core
    product = products(here, d_attn, w_out, True, rows, width, counts)
    total = Reduce(here, counts, product, total_refs)
    greet(here, tiny.peers, True)
    line.begin()
    grad_mixed[...] = jnp.zeros_like(grad_mixed)

    def mixed_copy(step):
        span = pl.ds(pl.multiple_of(step * rows, rows), rows)
        return pltpu.make_async_copy(mixed_all.at[span, :], mixed_two.at[step % 2], mixed_sems.at[step % 2])

    mixed_copy(0).start()

    def beside(step):
        line.step(step)

        @pl.when(step < 8)
        def _():
            span = pl.ds(pl.multiple_of(step * rows, rows), rows)
            mixed_copy(step).wait()

            @pl.when(step < 7)
            def _():
                mixed_copy(step + 1).start()

            grad_mixed[...] += dot_tn(mixed_two[step % 2], d_attn[span, :])

    done = total.run(beside)
    grad_out[...] = grad_mixed[...].astype(grad_out.dtype)

    def land(at, first, second):
        for half_at, value in enumerate((first, second)):
            d_mixed[:, pl.ds(pl.multiple_of((half_at * counts + at) * width, width), width)] = value.astype(
                d_mixed.dtype)

    total.end(land)
    half = HD // 2
    scale = 1.0 / math.sqrt(HD)
    depth = w_qkv.shape[0] * 8
    d_kv[...] = jnp.zeros_like(d_kv)

    def one_head(head, dots):
        span = pl.ds(pl.multiple_of(head * HD, HD), HD)
        query = queries[:, span]
        cot = d_mixed[:, span]
        prob = probs[head]
        d_prob = jnp.concatenate([dot_nt(cot, kv[0, :, HD:]), dot_nt(cot, kv[1, :, HD:])], axis=1)
        delta = jnp.sum(prob * d_prob, axis=-1, keepdims=True)
        d_score = (prob * (d_prob - delta)).astype(jnp.bfloat16)
        prob_low = prob.astype(jnp.bfloat16)
        d_query = (dot_nn(d_score[:, :rows], kv[0, :, :HD]) + dot_nn(d_score[:, rows:], kv[1, :, :HD])) * scale
        for side in range(2):
            keys = slice(side * rows, (side + 1) * rows)
            d_kv[side, :, :HD] += dot_tn(d_score[:, keys], query)
            d_kv[side, :, HD:] += dot_tn(prob_low[:, keys], cot)
        dots = dots + jnp.sum(d_query * query.astype(jnp.float32), axis=-1, keepdims=True)
        lead, trail = d_query[:, :half], d_query[:, half:]
        first = ((lead * cos[0] + trail * sin[0]) * rms[0]).astype(got.dtype)
        second = ((trail * cos[0] - lead * sin[0]) * rms[0]).astype(got.dtype)
        line.step(done + head)
        for rows_at in range(2):
            piece = slice(rows_at * part, (rows_at + 1) * part)
            got[0, core, rows_at, 0, :, pl.ds(pl.multiple_of(head * HD, HD), half)] = first[piece, :]
            got[0, core, rows_at, 0, :, pl.ds(pl.multiple_of(head * HD + half, half), half)] = second[piece, :]

        return dots

    dots = lax.fori_loop(0, heads, one_head, jnp.zeros((rows, 1), jnp.float32))
    eye = diagonal()
    tiny_own[...] = jnp.zeros_like(tiny_own)
    for side in (1, 0):
        d_key, d_value = d_kv[side, :, :HD], d_kv[side, :, HD:]
        own = jnp.sum(d_key * kv[side, :, :HD].astype(jnp.float32) +
                      d_value * kv[side, :, HD:].astype(jnp.float32), axis=-1, keepdims=True)
        if side == 0:
            own = own + dots * (1.0 / scale)
        own = own * (rms[side] * rms[side] * (1.0 / depth))
        to_tile(tiny_own, side * (rows // LANES), own, eye)
        lead, trail = d_key[:, :half], d_key[:, half:]
        parts = [(lead * cos[side] + trail * sin[side]) * rms[side],
                 (trail * cos[side] - lead * sin[side]) * rms[side],
                 d_value[:, :half] * rms[side], d_value[:, half:] * rms[side]]
        for at, value in enumerate(parts):
            if side == 1:
                give[:, at * half : (at + 1) * half] = value.astype(give.dtype)
            else:
                d_kv[0, :, at * half : (at + 1) * half] = value
    given = remote(give, taken, give_sems.at[0], give_sems.at[1], spread.ydev)
    given.start()
    grad[...] = jnp.zeros_like(grad)
    given.wait()
    for rows_at in range(2):
        piece = slice(rows_at * part, (rows_at + 1) * part)
        value = d_kv[0, piece, :] + taken[piece, :].astype(jnp.float32)
        got[0, core, rows_at, 0, :, heads * HD :] = value.astype(got.dtype)
    tiny.begin()
    for hop in range(2):
        spread.x_copy(hop, 0).start()
        spread.y_copy(hop, 0).start()
    for stream in range(2):
        spread.sib_copy(0, stream, 0).start()
    gain_sum[...] = jnp.zeros_like(gain_sum)
    line.end(done + heads)
    tiny.end()

    def block_of(at):
        across, other, half_at = near(at)
        shard, partner = here.shard(across, other), here.shard((across + 2) % 4, other)
        block = got[across, (core + other) % 2, half_at, 0]
        first = pl.multiple_of(shard * rows + half_at * part, part)
        for tile_at in range(part // LANES):
            row = pl.ds(pl.multiple_of(first + tile_at * LANES, LANES), LANES)
            low_at = half_at * (part // LANES) + tile_at
            kept = rows // LANES + low_at
            dot = from_tile(tiny_all[shard, pl.ds(low_at, 1), :] + tiny_all[partner, pl.ds(kept, 1), :], eye)
            value = dot_nt(block[tile_at * LANES : (tile_at + 1) * LANES, :], w_qkv[...])
            x_rows = x_low[row, :].astype(jnp.float32)
            contrib[row, :] = (value * gain[...] - x_rows * dot).astype(contrib.dtype)
            gain_sum[...] += jnp.sum(value * x_rows, axis=0, keepdims=True)
        line_tok.launch(at, 1)
        rows_t = act_t[:, pl.ds(first, part)]
        for at_col in range((heads + 2) * HD // 512):
            span = slice(at_col * 512, (at_col + 1) * 512)
            grad[:, span] += dot_nn(rows_t, block[:, span])

    me = here.shard(0, 0)
    columns = pl.ds(pl.multiple_of(me * cols, cols), cols)
    chunk = line.chunk

    def landing(which, at):
        sub = at % per if which == 0 else near(at)[2]
        return (out, d_tok)[which].at[pl.ds(pl.multiple_of(sub * chunk, chunk), chunk), columns]

    def leaver(which, at):
        return (leaving, line_tok.from_end)[which].at[at]

    def put(which, at):
        goal = here.device(*(far(at) if which == 0 else near(at)[:2]))
        return remote(leaver(which, at), landing(which, at), put_sems.at[which, 0, at], put_sems.at[which, 1, at],
                      goal)

    def keep(which, at):
        spot = at % per if which == 0 else near(at)[2]
        return pltpu.make_async_copy(leaver(which, at), landing(which, at), local_sems.at[which, spot])

    def emit(which, at):
        if which == 1:
            row = line_tok.rows(at)
            value = d_attn[row, :].astype(jnp.float32) + summed[row, :].astype(jnp.float32)
            line_tok.from_end[at] = value.astype(out.dtype)
            return
        row = pl.ds(pl.multiple_of(place_ffn(at) * chunk, chunk), chunk)

        def leave(source):
            value = x_low[row, :].astype(jnp.float32) + attn[row, :].astype(jnp.float32)
            leaving[at] = (value + source[row, :].astype(jnp.float32)).astype(out.dtype)

        @pl.when(at < 6 * per)
        def _():
            leave(ffn_sum)

        @pl.when(at >= 6 * per)
        def _():
            leave(ffn)

    def is_own(which, at):
        return at >= 7 * per if which == 0 else jnp.logical_and(at < 4, at % 2 == 0)

    def send(which, at):
        own = is_own(which, at)

        @pl.when(own)
        def _():
            keep(which, at).start()

        @pl.when(jnp.logical_not(own))
        def _():
            put(which, at).start()

    def stage_step(step, _):
        stage = step // 4

        @pl.when(jnp.logical_and(step % 4 == 0, jnp.logical_and(stage > 0, stage < 4)))
        def _():
            spread.x_copy(stage - 1, 0).wait_recv()
            spread.sib_copy(stage, 0, 0).start()
            spread.y_copy(stage - 1, 0).wait_recv()
            spread.sib_copy(stage, 1, 0).start()

        @pl.when(step == 4)
        def _():
            spread.x_copy(2, 0).start()
            spread.y_copy(2, 0).start()

        @pl.when(step < line_counts)
        def _():
            for stream in range(2):
                @pl.when(step % 4 == 2 * stream)
                def _(stream=stream):
                    spread.sib_copy(stage, stream, 0).wait_recv()

            block_of(step)

        @pl.when(step >= 4)
        def _():
            line_tok.step(step - 4)

        @pl.when(step > 0)
        def _():
            send(0, step - 1)

        emit(0, step)

        @pl.when(jnp.logical_and(line.inner == 1, step > 7))
        def _():
            send(1, step - 8)

        @pl.when(jnp.logical_and(line.inner == 1, step > 6))
        def _():
            emit(1, step - 7)
        return 0

    lax.fori_loop(0, line_counts, stage_step, 0)
    for half_at in range(cols // (rows // per)):
        span = pl.ds(line_counts * (rows // per) + half_at * (rows // per), rows // per)
        source = slice(half_at * (rows // per), (half_at + 1) * (rows // per))
        contrib[span, :] = grad[source, heads * HD :].astype(contrib.dtype)
    line_tok.launch(line_counts, extra)
    grad_query[...] = grad[:, : heads * HD].astype(grad_query.dtype)
    for at in range(cols // LANES):
        tile[at : at + 1, :] = gain_sum[:, at * LANES : (at + 1) * LANES]
        spot = cols // LANES + at
        tile[spot : spot + 1, :] = gain_grad[:, at * LANES : (at + 1) * LANES]

    def tile_copy(step):
        return remote(tile, gain_tiles.at[here.z], tile_send.at[step], tile_recv.at[step],
                      (here.dp, here.seq, (here.z + step + 1) % 4))

    send(0, line_counts - 1)
    for step in range(3):
        tile_copy(step).start()
    gain_tiles[here.z] = tile[...]

    @pl.when(line.inner == 1)
    def _():
        start = line_counts - 4

        def both(at, _):
            line_tok.step(at)

            @pl.when(at < line_counts + 4)
            def _():
                send(1, at - 4)

            @pl.when(at < line_counts + 3)
            def _():
                emit(1, at - 3)
            return 0

        lax.fori_loop(start, line_counts + extra + 2, both, 0)

        def drain(at, _):
            line_tok.down(at).wait_send()
            return 0

        lax.fori_loop(0, line_counts + extra, drain, 0)

    @pl.when(line.inner == 0)
    def _():
        def arrive(at, _):
            line_tok.up(at).wait_send()
            line_tok.down(at).wait_recv()

            @pl.when(jnp.logical_and(at > 0, at <= line_counts))
            def _():
                send(1, at - 1)

            @pl.when(at < line_counts)
            def _():
                emit(1, at)
            return 0

        lax.fori_loop(0, line_counts + extra, arrive, 0)

    for half_at in range(extra):
        span = pl.ds((line_counts + half_at) * chunk, chunk)
        kv_sum[half_at * chunk : (half_at + 1) * chunk, :] = summed[span, :]
    for hop in range(3):
        spread.x_copy(hop, 0).wait_send()
        spread.y_copy(hop, 0).wait_send()
    for stage in range(4):
        spread.sib_copy(stage, 0, 0).wait_send()
        spread.sib_copy(stage, 1, 0).wait_send()

    def finish(at, _):
        for which in range(2):
            own = is_own(which, at)

            @pl.when(own)
            def _():
                keep(which, at).wait()

            @pl.when(jnp.logical_not(own))
            def _():
                put(which, at).wait()
        return 0

    lax.fori_loop(0, line_counts, finish, 0)
    for step in range(3):
        tile_copy(step).wait()


def tail(d_attn, w_out, queries, kv, probs, rms, cos, sin, act_t, w_qkv, ffn, x_low, attn, gain, gain_grad,
         mixed_all, cid,
 per=2):
    total, cols = d_attn.shape
    rows = total // 8
    wide = w_out.shape[0]
    heads = wide // HD
    low, f32 = jnp.bfloat16, jnp.float32
    dma = pltpu.SemaphoreType.DMA
    vm = pl.BlockSpec(memory_space=pltpu.VMEM)
    counts = 8 * per
    chunk = rows // per
    extra = cols // chunk
    long = (total + cols, cols)
    out_shape = [
        jax.ShapeDtypeStruct((rows, 8 * cols), low),
        jax.ShapeDtypeStruct((rows, 8 * cols), low),
        jax.ShapeDtypeStruct((cols, wide), low),
        jax.ShapeDtypeStruct(w_out.shape, low),
        jax.ShapeDtypeStruct((cols, 2 * HD), low),
        jax.ShapeDtypeStruct((4, 8, LANES), f32),
    ]
    scratch = reduce_scratch(heads // 2, rows, HD, 2) + spread_scratch(1, rows // 2, wide + 2 * HD)
    scratch += [
        pltpu.VMEM((rows, wide), low),
        pltpu.VMEM((8, LANES), f32),
        pltpu.VMEM((8, 8, LANES), f32),
        pltpu.VMEM((2, rows, 2 * HD), f32),
        pltpu.VMEM((rows, 2 * HD), low),
        pltpu.VMEM((rows, 2 * HD), low),
        dma((2,)), dma((7,)), dma((7,)),
        pltpu.VMEM(w_qkv.shape, f32),
        pltpu.VMEM(w_out.shape, f32),
        pltpu.VMEM((1, cols), f32),
        pltpu.VMEM((8, LANES), f32),
        dma((3,)), dma((3,)), dma((2, 2, counts)), dma((2, per)),
        pltpu.VMEM((2, rows, wide), low), dma((2,)),
        pltpu.VMEM((total, cols), low),
        pltpu.VMEM((counts, chunk, cols), low),
    ] + line_scratch(6 * per, (6 * per * chunk, cols), low)
    scratch += [pltpu.VMEM(long, low), pltpu.VMEM(long, low)] + line_scratch(counts + extra, long, low)
    operands = [d_attn, w_out, queries, kv, probs, rms, cos, sin, act_t, w_qkv, ffn, x_low, attn, gain,
                gain_grad, mixed_all]
    kernel = functools.partial(tail_kernel, rows, heads, per)
    specs = [vm] * (len(operands) - 1) + [pl.BlockSpec(memory_space=pl.ANY)]
    return kernel_call(kernel, out_shape, operands, specs, scratch, cid, "tail")


LANES = 128


def acts_move(
    tokens, seg_ids, gain_attn, w_query, kv_weight, w_out, gain_ffn, w_gate, w_up, w_down, d_out
):
    rows = tokens.shape[0]
    segs = seg_ids.astype(jnp.float32).reshape(2 * rows // LANES, LANES)
    segs = jnp.pad(segs, ((0, 8 - 2 * rows // LANES), (0, 0)))
    gain_one = gain_attn.astype(jnp.float32)[None, :]
    gain_two = gain_ffn.astype(jnp.float32)[None, :]
    wider = jnp.float32

    qkv, x_low, act_one_t, w_qkv, rms, cos, sin, mask = opening(
        tokens, gain_one, w_query, kv_weight, segs, 1
    )
    attn_part, mixed_all, g_low, kv, probs, queries, pair_rms = attend(
        qkv, rms, cos, sin, mask, w_out, d_out, 2
    )
    d_hidden, attn = scatter_product(g_low, w_down, 512, 3, attn_part)
    hidden, d_gate, d_up, act_two_t, dots = ffn_scatter(x_low, attn, gain_two, w_gate, w_up, d_hidden, 4)
    d_norm, grad_gain_two, grad_gate, grad_up = back_gather(
        act_two_t, w_gate, w_up, d_gate, d_up, dots, x_low, attn, gain_two, 5
    )
    ffn, d_attn, grad_down = down_gather(g_low, w_down, hidden, d_norm, 6)
    d_tokens, out, grad_query, grad_out, grad_kv, gain_tiles = tail(
        d_attn,
        w_out,
        queries,
        kv,
        probs,
        pair_rms,
        cos,
        sin,
        act_one_t,
        w_qkv,
        ffn,
        x_low,
        attn,
        gain_one,
        grad_gain_two,
        mixed_all,
        7,
    )
    gains = jnp.sum(gain_tiles, axis=0).reshape(2, -1)
    return (
        out,
        d_tokens.astype(wider),
        gains[0],
        grad_query.astype(wider),
        grad_kv.astype(wider),
        grad_out.astype(wider),
        gains[1],
        grad_gate.astype(wider),
        grad_up.astype(wider),
        grad_down.astype(wider),
    )


def solution(mesh):
    in_specs = (
        P(("dp", "seq"), None),
        P("dp"),
        P(("dp", "seq")),
        P(("dp", "seq"), "tensor"),
        P(("dp", "seq"), None),
        P("tensor", ("dp", "seq")),
        P(("dp", "seq")),
        P(("dp", "seq"), "tensor"),
        P(("dp", "seq"), "tensor"),
        P("tensor", ("dp", "seq")),
        P(("dp", "seq"), None),
    )
    out_specs = (
        P(("dp", "seq"), None),
        P(("dp", "seq"), None),
        P(("dp", "seq")),
        P(("dp", "seq"), "tensor"),
        P(("dp", "seq"), None),
        P("tensor", ("dp", "seq")),
        P(("dp", "seq")),
        P(("dp", "seq"), "tensor"),
        P(("dp", "seq"), "tensor"),
        P("tensor", ("dp", "seq")),
    )

    def shards(*arrays):
        tokens = arrays[0]
        sizes = tuple(mesh.shape[name] for name in ("dp", "seq", "tensor"))
        count = tokens.shape[0] * sizes[0] * sizes[1]
        plan = acts_move if sizes == (4, 2, 4) and count <= tokens.shape[1] else weights_move
        return plan(*arrays)

    return jax.shard_map(shards, mesh=mesh, in_specs=in_specs, out_specs=out_specs, check_vma=False)
```

```python
import functools
import math

import jax
import jax.numpy as jnp
from jax import lax
from jax.experimental import pallas as pl
from jax.experimental.pallas import tpu as pltpu
from jax.sharding import PartitionSpec as P

HD = 256


EPS = 1e-06
NEG = -1e30


def place_tables(segs):
    length = segs.shape[0]
    index = jnp.arange(length, dtype=jnp.int32)
    flags = jnp.concatenate([jnp.ones((1,), dtype=bool), segs[1:] != segs[:-1]])
    starts = lax.cummax(jnp.where(flags, index, jnp.zeros_like(index)), axis=0)
    places = index - starts
    half_size = HD // 2
    freqs = jnp.exp(jnp.arange(half_size, dtype=jnp.float32) * (-math.log(10000.0) / half_size))
    angles = places.astype(jnp.float32)[:, None] * freqs[None, :]
    return (places, jnp.cos(angles), jnp.sin(angles))


def rotate(vector, cos_table, sin_table):
    half_size = vector.shape[-1] // 2
    leading = vector[..., :half_size]
    trailing = vector[..., half_size:]
    return jnp.concatenate(
        [leading * cos_table - trailing * sin_table, trailing * cos_table + leading * sin_table],
        axis=-1,
    )


def rotate_back(vector, cos_table, sin_table):
    half_size = vector.shape[-1] // 2
    leading = vector[..., :half_size]
    trailing = vector[..., half_size:]
    return jnp.concatenate(
        [leading * cos_table + trailing * sin_table, trailing * cos_table - leading * sin_table],
        axis=-1,
    )


def matmul(left, right):
    return jnp.dot(left, right, preferred_element_type=jnp.float32)


def matmul_nt(left, right):
    return lax.dot_general(
        left, right, (((1,), (1,)), ((), ())), preferred_element_type=jnp.float32
    )


def matmul_tn(left, right):
    return lax.dot_general(
        left, right, (((0,), (0,)), ((), ())), preferred_element_type=jnp.float32
    )


def gelu_tanh(values):
    return jax.nn.gelu(values, approximate=True)


def norm_back(d_act, normed, rms_val, gain_val):
    scaled = d_act * gain_val
    return rms_val * (scaled - normed * jnp.mean(scaled * normed, axis=-1, keepdims=True))


def weights_move(
    tokens, seg_ids, gain_attn, w_query, kv_weight, w_out, gain_ffn, w_gate, w_up, w_down, d_out
):
    rows = tokens.shape[0]
    scale_factor = 1.0 / math.sqrt(HD)
    offset = lax.axis_index("seq") * rows
    places, cos_table, sin_table = place_tables(seg_ids)
    own_places = lax.dynamic_slice_in_dim(places, offset, rows, 0)
    own_segs = lax.dynamic_slice_in_dim(seg_ids, offset, rows, 0)
    own_cos = lax.dynamic_slice_in_dim(cos_table, offset, rows, 0)
    own_sin = lax.dynamic_slice_in_dim(sin_table, offset, rows, 0)
    allowed = (own_segs[:, None] == seg_ids[None, :]) & (own_places[:, None] >= places[None, :])
    full_query, full_out, full_kv, full_gain_one = (
        lax.all_gather(w_query, ("dp", "seq"), axis=0, tiled=True),
        lax.all_gather(w_out, ("dp", "seq"), axis=1, tiled=True),
        lax.all_gather(kv_weight, ("dp", "seq"), axis=0, tiled=True),
        lax.all_gather(gain_attn, ("dp", "seq"), axis=0, tiled=True),
    )
    gain_one = full_gain_one.astype(jnp.float32)
    inputs = tokens.astype(jnp.float32)
    rms_one = lax.rsqrt(jnp.mean(inputs * inputs, axis=-1, keepdims=True) + EPS)
    norm_one = inputs * rms_one
    act_one = (norm_one * gain_one).astype(jnp.bfloat16)
    query_pre = matmul(act_one, full_query)
    heads = query_pre.shape[1] // HD
    kv_pre = matmul(act_one, full_kv)
    queries = (
        rotate(query_pre.reshape(rows, heads, HD), own_cos[:, None, :], own_sin[:, None, :])
        * scale_factor
    ).astype(jnp.bfloat16)
    own_kv = jnp.concatenate(
        [rotate(kv_pre[:, :HD], own_cos, own_sin), kv_pre[:, HD:]], axis=1
    ).astype(jnp.bfloat16)
    all_kv = lax.all_gather(own_kv, "seq", axis=0, tiled=True)
    keys = all_kv[:, :HD]
    values_all = all_kv[:, HD:]
    scores = jnp.einsum("rhd,kd->hrk", queries, keys, preferred_element_type=jnp.float32)
    scores = jnp.where(allowed[None], scores, NEG)
    top_score = jnp.max(scores, axis=-1, keepdims=True)
    expd = jnp.exp(scores - top_score)
    total = jnp.sum(expd, axis=-1, keepdims=True)
    log_total = top_score + jnp.log(total)
    probs_low = (expd / total).astype(jnp.bfloat16)
    mixed = (
        jnp.einsum("hrk,kd->rhd", probs_low, values_all, preferred_element_type=jnp.float32)
        .reshape(rows, heads * HD)
        .astype(jnp.bfloat16)
    )
    attn = lax.psum(matmul(mixed, full_out), "tensor")
    resid = inputs + attn
    full_gate, full_up, full_down, full_gain_two = (
        lax.all_gather(w_gate, ("dp", "seq"), axis=0, tiled=True),
        lax.all_gather(w_up, ("dp", "seq"), axis=0, tiled=True),
        lax.all_gather(w_down, ("dp", "seq"), axis=1, tiled=True),
        lax.all_gather(gain_ffn, ("dp", "seq"), axis=0, tiled=True),
    )
    gain_two = full_gain_two.astype(jnp.float32)
    rms_two = lax.rsqrt(jnp.mean(resid * resid, axis=-1, keepdims=True) + EPS)
    norm_two = resid * rms_two
    act_two = (norm_two * gain_two).astype(jnp.bfloat16)
    gate = matmul(act_two, full_gate)
    up_val = matmul(act_two, full_up)
    gelu_val, gelu_pull = jax.vjp(gelu_tanh, gate)
    hidden = (gelu_val * up_val).astype(jnp.bfloat16)
    ffn = lax.psum(matmul(hidden, full_down).astype(jnp.bfloat16), "tensor").astype(jnp.float32)
    out = (resid + ffn).astype(jnp.bfloat16)
    back_gate, back_up, back_down = (
        lax.all_gather(w_gate, ("dp", "seq"), axis=0, tiled=True),
        lax.all_gather(w_up, ("dp", "seq"), axis=0, tiled=True),
        lax.all_gather(w_down, ("dp", "seq"), axis=1, tiled=True),
    )
    d_hidden = matmul_nt(d_out, back_down)
    grad_down = matmul_tn(hidden, d_out)
    d_gate = gelu_pull(d_hidden * up_val)[0].astype(jnp.bfloat16)
    d_up = (d_hidden * gelu_val).astype(jnp.bfloat16)
    grad_gate = matmul_tn(act_two, d_gate)
    grad_up = matmul_tn(act_two, d_up)
    d_act_two = lax.psum(matmul_nt(d_gate, back_gate) + matmul_nt(d_up, back_up), "tensor")
    grad_gain_two = jnp.sum(d_act_two * norm_two, axis=0)
    d_resid = d_out.astype(jnp.float32) + norm_back(d_act_two, norm_two, rms_two, gain_two)
    ffn_grads = (
        lax.psum_scatter(
            grad_gate.astype(jnp.bfloat16), ("dp", "seq"), scatter_dimension=0, tiled=True
        ).astype(jnp.float32),
        lax.psum_scatter(
            grad_up.astype(jnp.bfloat16), ("dp", "seq"), scatter_dimension=0, tiled=True
        ).astype(jnp.float32),
        lax.psum_scatter(
            grad_down.astype(jnp.bfloat16), ("dp", "seq"), scatter_dimension=1, tiled=True
        ).astype(jnp.float32),
        lax.psum_scatter(
            grad_gain_two.astype(jnp.bfloat16), ("dp", "seq"), scatter_dimension=0, tiled=True
        ).astype(jnp.float32),
    )
    back_query, back_out, back_kv = (
        lax.all_gather(w_query, ("dp", "seq"), axis=0, tiled=True),
        lax.all_gather(w_out, ("dp", "seq"), axis=1, tiled=True),
        lax.all_gather(kv_weight, ("dp", "seq"), axis=0, tiled=True),
    )
    d_attn = d_resid.astype(jnp.bfloat16)
    grad_out = matmul_tn(mixed, d_attn)
    d_mixed = matmul_nt(d_attn, back_out).astype(jnp.bfloat16).reshape(rows, heads, HD)
    scores_again = jnp.einsum("rhd,kd->hrk", queries, keys, preferred_element_type=jnp.float32)
    probs = jnp.where(allowed[None], jnp.exp(scores_again - log_total), 0.0)
    d_probs = jnp.einsum("rhd,kd->hrk", d_mixed, values_all, preferred_element_type=jnp.float32)
    delta = jnp.sum(probs * d_probs, axis=-1, keepdims=True)
    d_scores = (probs * (d_probs - delta)).astype(jnp.bfloat16)
    d_queries = (
        jnp.einsum("hrk,kd->rhd", d_scores, keys, preferred_element_type=jnp.float32) * scale_factor
    )
    d_query_pre = (
        rotate_back(d_queries, own_cos[:, None, :], own_sin[:, None, :])
        .reshape(rows, heads * HD)
        .astype(jnp.bfloat16)
    )
    d_keys_part = jnp.einsum("hrk,rhd->kd", d_scores, queries, preferred_element_type=jnp.float32)
    d_values_part = jnp.einsum(
        "hrk,rhd->kd", probs.astype(jnp.bfloat16), d_mixed, preferred_element_type=jnp.float32
    )
    own_kv_grad = lax.psum_scatter(
        jnp.concatenate([d_keys_part, d_values_part], axis=1).astype(jnp.bfloat16),
        "seq",
        scatter_dimension=0,
        tiled=True,
    )
    d_act_query = matmul_nt(d_query_pre, back_query)
    d_act_sum, kv_grad = (
        lax.psum(d_act_query.astype(jnp.bfloat16), "tensor").astype(jnp.float32),
        lax.psum(own_kv_grad, "tensor").astype(jnp.float32),
    )
    d_kv_pre = jnp.concatenate(
        [rotate_back(kv_grad[:, :HD], own_cos, own_sin), kv_grad[:, HD:]], axis=1
    ).astype(jnp.bfloat16)
    d_act_one = d_act_sum + matmul_nt(d_kv_pre, back_kv)
    grad_query = matmul_tn(act_one, d_query_pre)
    grad_kv = matmul_tn(act_one, d_kv_pre)
    grad_gain_one = jnp.sum(d_act_one * norm_one, axis=0)
    d_tokens = d_resid + norm_back(d_act_one, norm_one, rms_one, gain_one)
    attn_grads = (
        lax.psum_scatter(
            grad_query.astype(jnp.bfloat16), ("dp", "seq"), scatter_dimension=0, tiled=True
        ).astype(jnp.float32),
        lax.psum_scatter(
            grad_out.astype(jnp.bfloat16), ("dp", "seq"), scatter_dimension=1, tiled=True
        ).astype(jnp.float32),
        lax.psum_scatter(
            grad_kv.astype(jnp.bfloat16), ("dp", "seq"), scatter_dimension=0, tiled=True
        ).astype(jnp.float32),
        lax.psum_scatter(
            grad_gain_one.astype(jnp.bfloat16), ("dp", "seq"), scatter_dimension=0, tiled=True
        ).astype(jnp.float32),
    )
    return (
        out,
        d_tokens,
        attn_grads[3],
        attn_grads[0],
        attn_grads[2],
        attn_grads[1],
        ffn_grads[3],
        ffn_grads[0],
        ffn_grads[1],
        ffn_grads[2],
    )


MESH = pl.DeviceIdType.MESH
VMEM_LIMIT = 66000 * 1024


class Place:
    def __init__(self):
        self.dp = lax.axis_index("dp")
        self.seq = lax.axis_index("seq")
        self.z = lax.axis_index("tensor")
        self.core = lax.rem(self.dp, 2)
        self.chip = lax.div(self.dp, 2)

    def device(self, across, other):
        chip = (self.chip + across) % 2
        seq = (self.seq + across // 2) % 2
        core = (self.core + other) % 2
        return chip * 2 + core, seq, self.z

    def shard(self, across, other):
        dp, seq, _ = self.device(across, other)
        return dp * 2 + seq


def greet(here, peers, line=False):
    barrier = pltpu.get_barrier_semaphore()
    peers = list(peers)
    if line:
        peers += [(here.dp, here.seq, (here.z + step) % 4) for step in range(1, 4)]
    for peer in peers:
        pl.semaphore_signal(barrier, inc=1, device_id=peer, device_id_type=MESH)
    pl.semaphore_wait(barrier, len(peers))


def remote(src, dst, send, recv, peer):
    return pltpu.make_async_remote_copy(
        src_ref=src, dst_ref=dst, send_sem=send, recv_sem=recv, device_id=peer, device_id_type=MESH
    )


class Line:
    def __init__(self, here, counts, refs, place=None):
        self.own, self.out, self.from_end, self.from_mid = refs[:4]
        self.sems = refs[4:10]
        self.counts = counts
        self.chunk = self.from_end.shape[1]
        self.place = place
        z = here.z
        self.inner = ((z + 1) // 2) % 2
        self.mate = (here.dp, here.seq, z + 1 - 2 * (z % 2))
        self.other = (here.dp, here.seq, 3 - z)

    def rows(self, at):
        at = at if self.place is None else self.place(at)
        return pl.ds(pl.multiple_of(at * self.chunk, self.chunk), self.chunk)

    def up(self, at):
        return remote(self.own.at[self.rows(at), :], self.from_end.at[at], self.sems[0].at[at],
                      self.sems[1].at[at], self.mate)

    def over(self, at):
        return remote(self.out.at[self.rows(at), :], self.from_mid.at[at], self.sems[2].at[at],
                      self.sems[3].at[at], self.other)

    def down(self, at):
        rows = self.rows(at)
        return remote(self.out.at[rows, :], self.out.at[rows, :], self.sems[4].at[at],
                      self.sems[5].at[at], self.mate)

    def launch(self, first, count):
        @pl.when(self.inner == 0)
        def _():
            def send(at, _):
                self.up(first + at).start()
                return 0

            lax.fori_loop(0, count, send, 0)

    def begin(self):
        self.launch(0, self.counts)

    def first(self, at):
        rows = self.rows(at)
        self.up(at).wait_recv()
        total = self.own[rows, :].astype(jnp.float32) + self.from_end[at].astype(jnp.float32)
        self.out[rows, :] = total.astype(self.out.dtype)
        self.over(at).start()

    def second(self, at):
        rows = self.rows(at)
        self.over(at).wait()
        total = self.out[rows, :].astype(jnp.float32) + self.from_mid[at].astype(jnp.float32)
        self.out[rows, :] = total.astype(self.out.dtype)
        self.down(at).start()

    def step(self, at, start=0, count=None):
        count = self.counts if count is None else count

        @pl.when(jnp.logical_and(self.inner == 1, at < count))
        def _():
            self.first(start + at)

        @pl.when(jnp.logical_and(self.inner == 1, jnp.logical_and(at > 1, at < count + 2)))
        def _():
            self.second(start + at - 2)

    def steps(self, first, last, start=0, count=None):
        def rest(at, _):
            self.step(at, start, count)
            return 0

        lax.fori_loop(first, last, rest, 0)

    def settle(self):
        @pl.when(self.inner == 0)
        def _():
            def take(at, _):
                self.up(at).wait_send()
                self.down(at).wait_recv()
                return 0

            lax.fori_loop(0, self.counts, take, 0)

        self.drain()

    def drain(self):
        @pl.when(self.inner == 1)
        def _():
            def drain(at, _):
                self.down(at).wait_send()
                return 0

            lax.fori_loop(0, self.counts, drain, 0)

    def end(self, done=0):
        self.steps(min(done, self.counts + 2), self.counts + 2)
        self.settle()


def line_scratch(counts, shape, low):
    buf = pltpu.VMEM((counts, shape[0] // counts, shape[1]), low)
    return [buf, buf] + [pltpu.SemaphoreType.DMA((counts,))] * 6


def turned(at):
    return 3 - at // 2, 1 - at % 2


def slice_peers(here):
    return [here.device(*turned(at)) for at in range(7)]


def kernel_call(kernel, out_shape, operands, specs, scratch, cid, name, out_specs=None, late=()):
    vm = pl.BlockSpec(memory_space=pltpu.VMEM)
    specs = [pl.BlockSpec(memory_space=pl.ANY) if at in late else spec for at, spec in enumerate(specs)]
    inside = [pltpu.VMEM(operands[at].shape, operands[at].dtype) for at in late]
    if late:
        inside.append(pltpu.SemaphoreType.DMA((len(late),)))

    def body(*refs):
        if not late:
            kernel(*refs)
            return
        ins, rest, own = list(refs[: len(operands)]), refs[len(operands) : -len(inside)], refs[-len(inside) :]
        copies = []
        for spot, at in enumerate(late):
            copy = pltpu.make_async_copy(ins[at], own[spot], own[-1].at[spot])
            copy.start()
            copies.append(copy)
            ins[at] = own[spot]
        kernel(*ins, *rest, late=copies)

    return pl.pallas_call(
        body,
        out_shape=out_shape,
        in_specs=specs,
        out_specs=out_specs or [vm] * len(out_shape),
        scratch_shapes=scratch + inside,
        compiler_params=pltpu.CompilerParams(
            collective_id=cid, has_side_effects=True, vmem_limit_bytes=VMEM_LIMIT
        ),
        name=f"{name}_{cid}",
    )(*operands)


class Tiny:
    def __init__(self, here, src, dst, sems, spread):
        self.here, self.src, self.dst, self.sems, self.spread = here, src, dst, sems, spread
        self.peers = slice_peers(here)
        self.me = here.shard(0, 0)

    def tile(self, shard):
        return self.src.at[shard] if self.spread else self.src

    def copy(self, at):
        return remote(self.tile(self.here.shard(*turned(at))), self.dst.at[self.me], self.sems[0].at[at],
                      self.sems[1].at[at], self.peers[at])

    def begin(self):
        for at in range(7):
            self.copy(at).start()
        self.dst[self.me] = self.tile(self.me)[...]

    def end(self):
        for at in range(7):
            self.copy(at).wait()


class Reduce:
    def __init__(self, here, counts, product, refs, before=None):
        self.counts, self.product, self.before = counts, product, before
        self.held, self.sib_out, self.sib_in, self.from_x, self.from_y = refs[:5]
        self.sib_sems, self.x_sems, self.y_sems = refs[5:7], refs[7:9], refs[9:11]
        self.sib, self.xdev, self.ydev = here.device(0, 1), here.device(1, 0), here.device(2, 0)
        self.steps = 4 * counts
        self.ring = self.sib_out.shape[0]

    def streams(self, stage):
        far = stage // 3
        x_chip = jnp.where(stage == 0, 3, jnp.where(stage == 2, 0, 1))
        y_chip = jnp.where(stage == 0, 3, jnp.where(stage == 2, 0, 2))
        return (x_chip, far), (y_chip, 1 - far)

    def to_sib(self, step, stream):
        stage, at = step // self.counts, step % self.counts
        return remote(self.sib_out.at[step % self.ring, stream], self.sib_in.at[stage, stream, at],
                      self.sib_sems[0].at[stage, stream, at], self.sib_sems[1].at[stage, stream, at], self.sib)

    def to_x(self, hop, at, stage=0):
        return remote(self.held.at[stage, 0, at], self.from_x.at[hop, at], self.x_sems[0].at[hop, at],
                      self.x_sems[1].at[hop, at], self.xdev)

    def to_y(self, hop, at, stage=0):
        return remote(self.held.at[stage, 1, at], self.from_y.at[hop, at], self.y_sems[0].at[hop, at],
                      self.y_sems[1].at[hop, at], self.ydev)

    def compute(self, step):
        stage, at = step // self.counts, step % self.counts
        if self.before:
            for stop in range(3):
                @pl.when(step == stop * self.counts)
                def _():
                    self.before(stop)

        @pl.when(step >= self.ring)
        def _():
            for stream in range(2):
                self.to_sib(step - self.ring, stream).wait_send()

        for stream, (across, half) in enumerate(self.streams(stage)):
            self.sib_out[step % self.ring, stream] = self.product(across, 1, half, at).astype(jnp.bfloat16)
            self.held[stage, stream, at] = self.product(across, 0, half, at).astype(jnp.bfloat16)
        for stream in range(2):
            self.to_sib(step, stream).start()

    def finish(self, step):
        stage, at = step // self.counts, step % self.counts
        for stream in range(2):
            self.to_sib(step, stream).wait_recv()

        def total(stream):
            return self.held[stage, stream, at].astype(jnp.float32) + self.sib_in[stage, stream, at].astype(
                jnp.float32)

        @pl.when(stage < 3)
        def _():
            for stream in range(2):
                self.held[stage, stream, at] = total(stream).astype(jnp.bfloat16)

        @pl.when(stage == 3)
        def _():
            self.to_y(0, at).wait_recv()
            self.held[3, 0, at] = (total(0) + self.from_y[0, at].astype(jnp.float32)).astype(jnp.bfloat16)
            self.to_x(0, at).wait_recv()
            self.held[3, 1, at] = (total(1) + self.from_x[0, at].astype(jnp.float32)).astype(jnp.bfloat16)

        @pl.when(stage != 2)
        def _():
            hop = stage - stage // 3
            self.to_x(hop, at, stage).start()
            self.to_y(hop, at, stage).start()

    def run(self, hook=None):
        def body(step, _):
            @pl.when(step < self.steps)
            def _():
                self.compute(step)

            @pl.when(step > 0)
            def _():
                self.finish(step - 1)

            if hook:
                hook(step)
            return 0

        lax.fori_loop(0, self.steps + 1, body, 0)
        return self.steps + 1

    def end(self, emit):
        def last(at, _):
            values = []
            for half in range(2):
                xs, ys = (1, 2) if half == 0 else (2, 1)
                self.to_x(xs, at).wait_recv()
                self.to_y(ys, at).wait_recv()
                values.append(self.held[2, half, at].astype(jnp.float32) + self.from_x[xs, at].astype(jnp.float32)
                              + self.from_y[ys, at].astype(jnp.float32))
            emit(at, *values)
            for hop in range(3):
                self.to_x(hop, at).wait_send()
                self.to_y(hop, at).wait_send()
            return 0

        lax.fori_loop(0, self.counts, last, 0)

        def drain(at, _):
            for stream in range(2):
                self.to_sib(self.steps - self.ring + at, stream).wait_send()
            return 0

        lax.fori_loop(0, self.ring, drain, 0)


def reduce_scratch(counts, rows, width, ring=4):
    low, dma = jnp.bfloat16, pltpu.SemaphoreType.DMA
    block = pltpu.VMEM((4, 2, counts, rows, width), low)
    landed = pltpu.VMEM((3, counts, rows, width), low)
    sent = pltpu.VMEM((ring, 2, rows, width), low)
    return [block, sent, block, landed, landed] + [dma((4, 2, counts))] * 2 + [dma((3, counts))] * 4


class Spread:
    def __init__(self, here, counts, refs):
        self.counts = counts
        self.got = refs[0]
        self.x_sems, self.y_sems, self.sib_sems = refs[1:3], refs[3:5], refs[5:7]
        self.core = here.core
        self.sib, self.xdev, self.ydev = here.device(0, 1), here.device(1, 0), here.device(2, 0)

    def slot(self, across, half, at):
        return self.got.at[across, self.core, half, at]

    def x_copy(self, hop, at):
        half = jnp.minimum(hop, 1)
        src = self.slot(2 * (hop // 2), half, at)
        dst = self.slot(1 + 2 * (hop // 2), half, at)
        return remote(src, dst, self.x_sems[0].at[hop, at], self.x_sems[1].at[hop, at], self.xdev)

    def y_copy(self, hop, at):
        half = 1 - jnp.minimum(hop, 1)
        src = self.slot(hop // 2, half, at)
        dst = self.slot(2 + hop // 2, half, at)
        return remote(src, dst, self.y_sems[0].at[hop, at], self.y_sems[1].at[hop, at], self.ydev)

    def streams(self, stage):
        some, last, late = jnp.minimum(stage, 1), stage // 3, stage // 2
        return (some + 2 * last, late), (2 * some + last, 1 - late)

    def sib_copy(self, stage, stream, at):
        across, half = self.streams(stage)[stream]
        slot = self.slot(across, half, at)
        spot = (stage, stream, at)
        return remote(slot, slot, self.sib_sems[0].at[spot], self.sib_sems[1].at[spot], self.sib)

    def begin(self):
        def first(at, _):
            self.x_copy(0, at).start()
            self.y_copy(0, at).start()
            return 0

        def own(at, _):
            self.sib_copy(0, 0, at).start()
            self.sib_copy(0, 1, at).start()
            return 0

        lax.fori_loop(0, self.counts, first, 0)
        lax.fori_loop(0, self.counts, own, 0)

    def run(self, blocks, hook=None, done=None):
        counts = self.counts

        def body(step, _):
            stage, at = step // counts, step % counts

            @pl.when(jnp.logical_and(stage > 0, stage < 4))
            def _():
                self.x_copy(stage - 1, at).wait_recv()
                self.sib_copy(stage, 0, at).start()
                self.y_copy(stage - 1, at).wait_recv()
                self.sib_copy(stage, 1, at).start()

            @pl.when(jnp.logical_and(stage > 0, stage < 3))
            def _():
                self.x_copy(stage, at).start()
                self.y_copy(stage, at).start()

            @pl.when(step > 0)
            def _():
                old, spot = (step - 1) // counts, (step - 1) % counts
                for stream, (across, half) in enumerate(self.streams(old)):
                    self.sib_copy(old, stream, spot).wait_recv()
                    blocks(across, half, spot)
                if done:
                    done(old, spot)

            if hook:
                hook(step)
            return 0

        lax.fori_loop(0, 4 * counts + 1, body, 0)
        return 4 * counts + 1

    def end(self):
        def drain(at, _):
            for hop in range(3):
                self.x_copy(hop, at).wait_send()
                self.y_copy(hop, at).wait_send()
            for stage in range(4):
                self.sib_copy(stage, 0, at).wait_send()
                self.sib_copy(stage, 1, at).wait_send()
            return 0

        lax.fori_loop(0, self.counts, drain, 0)


def spread_scratch(counts, rows, width):
    dma = pltpu.SemaphoreType.DMA
    return [pltpu.VMEM((4, 2, 2, counts, rows, width), jnp.bfloat16)] + [dma((3, counts))] * 4 + [
        dma((4, 2, counts))] * 2


def row_span(here, across, other, rows):
    return pl.ds(pl.multiple_of(here.shard(across, other) * rows, rows), rows)


def dot_nt(left, right):
    return lax.dot_general(left, right, (((1,), (1,)), ((), ())), preferred_element_type=jnp.float32)


def dot_tn(left, right):
    return lax.dot_general(left, right, (((0,), (0,)), ((), ())), preferred_element_type=jnp.float32)


def dot_nn(left, right):
    return jnp.dot(left, right, preferred_element_type=jnp.float32)


def products(here, act, weight, nt, rows, width, counts):
    def product(across, other, half, at):
        cols = pl.ds(pl.multiple_of((half * counts + at) * width, width), width)
        block = act[row_span(here, across, other, rows), :]
        return dot_nt(block, weight[cols, :]) if nt else dot_nn(block, weight[:, cols])

    return product


def diagonal():
    return (lax.broadcasted_iota(jnp.int32, (LANES, LANES), 0) ==
            lax.broadcasted_iota(jnp.int32, (LANES, LANES), 1)).astype(jnp.float32)


def to_tile(tile, first, column, eye):
    for at in range(column.shape[0] // LANES):
        spread = column[at * LANES : (at + 1) * LANES, :] * eye
        tile[first + at : first + at + 1, :] = jnp.sum(spread, axis=0, keepdims=True)


def from_tile(row, eye):
    return jnp.sum(eye * row, axis=1, keepdims=True)


def make_tables(here, rows, segs, cos, sin, mask):
    eye = diagonal()
    tiles = rows // LANES
    freqs = jnp.exp(lax.broadcasted_iota(jnp.int32, (1, LANES), 1).astype(jnp.float32) * (-math.log(10000.0) / LANES))
    lane = lax.broadcasted_iota(jnp.int32, (1, LANES), 1)
    line = lax.broadcasted_iota(jnp.int32, (LANES, 1), 0)

    def row_of(side, at):
        return ((here.seq + side) % 2) * tiles + at

    for side in range(2):
        for at in range(tiles):
            row = row_of(side, at)
            ids = from_tile(segs[pl.ds(row, 1), :], eye)
            before = jnp.zeros((LANES, 1), jnp.float32)
            for other in range(2 * tiles):
                smaller = segs[other : other + 1, :] < ids
                before += jnp.sum(smaller.astype(jnp.float32), axis=-1, keepdims=True)
            index = row * LANES + line
            angles = (index.astype(jnp.float32) - before) * freqs
            span = slice(at * LANES, (at + 1) * LANES)
            cos[side, span, :] = jnp.cos(angles)
            sin[side, span, :] = jnp.sin(angles)
            if side == 0:
                for key_side in range(2):
                    for key_at in range(tiles):
                        key_row = row_of(key_side, key_at)
                        same = segs[pl.ds(key_row, 1), :] == ids
                        allowed = jnp.logical_and(same, key_row * LANES + lane <= index)
                        first = key_side * rows + key_at * LANES
                        mask[span, first : first + LANES] = allowed.astype(jnp.float32)


def open_kernel(rows, width, counts, tokens, gain, w_query, kv_weight, segs, qkv, x_low, act_t, w_qkv, rms, cos, sin,
                mask, *refs):
    here = Place()
    cols = gain.shape[1]
    act, turn_send, turn_recv, local_sems = refs[:4]
    me = here.shard(0, 0)
    own_rows = pl.ds(pl.multiple_of(me * rows, rows), rows)

    def turn_copy(at):
        across, other = turned(at)
        first = pl.multiple_of(here.shard(across, other) * cols, cols)
        return remote(tokens.at[:, pl.ds(first, cols)], x_low.at[own_rows, :], turn_send.at[at], turn_recv.at[at],
                      here.device(across, other))

    wide = w_query.shape[1]
    local = [
        pltpu.make_async_copy(w_query, w_qkv.at[:, :wide], local_sems.at[0]),
        pltpu.make_async_copy(kv_weight, w_qkv.at[:, wide:], local_sems.at[1]),
        pltpu.make_async_copy(tokens.at[:, pl.ds(pl.multiple_of(me * cols, cols), cols)], x_low.at[own_rows, :],
                              local_sems.at[2]),
    ]
    for copy in local:
        copy.start()
    greet(here, slice_peers(here))
    for at in range(7):
        turn_copy(at).start()
    for copy in local:
        copy.wait()

    def squares(at, total):
        values = tokens[:, pl.ds(pl.multiple_of(at * cols, cols), cols)].astype(jnp.float32)
        return total + jnp.sum(values * values, axis=-1, keepdims=True)

    total = lax.fori_loop(0, 8, squares, jnp.zeros((rows, 1), jnp.float32))
    rms[...] = jnp.broadcast_to(lax.rsqrt(total / (8 * cols) + EPS), rms.shape)
    make_tables(here, rows, segs, cos, sin, mask)

    def prepare(first, count):
        def one(step, _):
            at = first + step
            span = row_span(here, *turned(at), rows)
            value = (x_low[span, :].astype(jnp.float32) * gain[0:1, :]).astype(act.dtype)
            act[span, :] = value
            return 0

        lax.fori_loop(0, count, one, 0)

    def before(stop):
        first, count = ((0, 2), (2, 4), (6, 2))[stop]
        for at in range(first, min(first + count, 7)):
            turn_copy(at).wait_recv()
        prepare(first, count)

    def flip():
        def one(shard, _):
            span = pl.ds(pl.multiple_of(shard * rows, rows), rows)
            act_t[:, span] = act[span, :].T
            return 0

        lax.fori_loop(0, 8, one, 0)

    product = products(here, act, w_qkv, False, rows, width, counts)
    total = Reduce(here, counts, product, refs[4:15], before)
    total.run()
    flip()

    def emit(at, first, second):
        for half, value in enumerate((first, second)):
            qkv[:, pl.ds(pl.multiple_of((half * counts + at) * width, width), width)] = value

    total.end(emit)
    for at in range(7):
        turn_copy(at).wait_send()


def opening(tokens, gain, w_query, kv_weight, segs, cid, width=256):
    rows = tokens.shape[0]
    cols, wide = w_query.shape
    every = wide + kv_weight.shape[1]
    counts = every // (2 * width)
    low, f32 = jnp.bfloat16, jnp.float32
    dma = pltpu.SemaphoreType.DMA
    vm = pl.BlockSpec(memory_space=pltpu.VMEM)
    hbm = pl.BlockSpec(memory_space=pl.ANY)
    out_shape = [
        jax.ShapeDtypeStruct((rows, every), f32),
        jax.ShapeDtypeStruct((8 * rows, cols), low),
        jax.ShapeDtypeStruct((cols, 8 * rows), low),
        jax.ShapeDtypeStruct((cols, every), low),
        jax.ShapeDtypeStruct((rows, LANES), f32),
        jax.ShapeDtypeStruct((2, rows, LANES), f32),
        jax.ShapeDtypeStruct((2, rows, LANES), f32),
        jax.ShapeDtypeStruct((rows, 2 * rows), f32),
    ]
    scratch = [pltpu.VMEM((8 * rows, cols), low), dma((7,)), dma((7,)), dma((3,))]
    scratch += reduce_scratch(counts, rows, width)
    kernel = functools.partial(open_kernel, rows, width, counts)
    return kernel_call(kernel, out_shape, [tokens, gain, w_query, kv_weight, segs],
                       [vm, vm, hbm, hbm, vm], scratch, cid, "open")


def scatter_kernel(rows, width, counts, line_counts, act, weight, line_own, out, line_out, *refs):
    here = Place()
    line = Line(here, line_counts, [line_own, line_out] + list(refs[11:]))
    product = products(here, act, weight, True, rows, width, counts)
    total = Reduce(here, counts, product, refs[:11])
    greet(here, slice_peers(here), True)
    line.begin()
    def beside(step):
        line.step(2 * step)
        line.step(2 * step + 1)

    line.end(2 * total.run(beside))

    def emit(at, first, second):
        for half, value in enumerate((first, second)):
            out[:, pl.ds(pl.multiple_of((half * counts + at) * width, width), width)] = value

    total.end(emit)


def scatter_product(act, weight, width, cid, line, line_counts=32):
    rows = act.shape[0] // 8
    every = weight.shape[0]
    counts = every // (2 * width)
    vm = pl.BlockSpec(memory_space=pltpu.VMEM)
    out_shape = [
        jax.ShapeDtypeStruct((rows, every), jnp.float32),
        jax.ShapeDtypeStruct(line.shape, line.dtype),
    ]
    scratch = reduce_scratch(counts, rows, width) + line_scratch(line_counts, line.shape, line.dtype)
    kernel = functools.partial(scatter_kernel, rows, width, counts, line_counts)
    return kernel_call(kernel, out_shape, [act, weight, line], [vm] * 3, scratch, cid, "scatter_product")


def ffn_kernel(rows, width, counts, x_low, attn, gain, w_gate, w_up, d_hidden, hidden, d_gate, d_up, act_t, tile_out,
               *refs, late):
    here = Place()
    cols = gain.shape[1]
    act, weight, tiny_own, tiny_all, tiny_send, tiny_recv, dots, local_sems = refs[:8]
    tiny = Tiny(here, tiny_own, tiny_all, (tiny_send, tiny_recv), True)
    half_cols = counts * width
    local = [
        pltpu.make_async_copy(w_gate, weight.at[:, :half_cols], local_sems.at[0]),
        pltpu.make_async_copy(w_up, weight.at[:, half_cols:], local_sems.at[1]),
    ]
    for copy in local:
        copy.start()
    eye = diagonal()
    tiny_own[...] = jnp.zeros_like(tiny_own)

    def prepare(shard, _):
        for at in range(rows // LANES):
            span = pl.ds(pl.multiple_of(shard * rows + at * LANES, LANES), LANES)
            resid = x_low[span, :].astype(jnp.float32) + attn[span, :].astype(jnp.float32)
            act[span, :] = (resid * gain[0:1, :]).astype(act.dtype)
            square = jnp.sum(resid * resid, axis=-1, keepdims=True)
            tiny_own[shard, at : at + 1, :] = jnp.sum(square * eye, axis=0, keepdims=True)
        return 0

    lax.fori_loop(0, 8, prepare, 0)
    greet(here, slice_peers(here))
    tiny.begin()
    for copy in local:
        copy.wait()
    product = products(here, act, weight, False, rows, width, counts)
    total = Reduce(here, counts, product, refs[8:19])
    total.run()

    def flip(shard, _):
        span = pl.ds(pl.multiple_of(shard * rows, rows), rows)
        act_t[:, span] = act[span, :].T
        return 0

    lax.fori_loop(0, 8, flip, 0)
    tiny.end()
    tiles = rows // LANES
    mean = [from_tile(jnp.sum(tiny_all[:, at, :], axis=0, keepdims=True), eye) for at in range(tiles)]
    scale = lax.rsqrt(jnp.concatenate(mean, axis=0) / (8 * cols) + EPS)
    dots[...] = jnp.zeros_like(dots)
    late[0].wait()
    coeff = math.sqrt(2.0 / math.pi)

    def emit(at, first, second):
        span = pl.ds(pl.multiple_of(at * width, width), width)
        gate, up = first * scale, second * scale
        inner = jnp.tanh(coeff * (gate + 0.044715 * (gate * gate * gate)))
        gelu = 0.5 * gate * (1.0 + inner)
        slope = 0.5 * (1.0 + inner) + 0.5 * gate * (1.0 - inner * inner) * (
            coeff * (1.0 + 3.0 * 0.044715 * gate * gate))
        cot = d_hidden[:, span]
        hidden[:, span] = (gelu * up).astype(hidden.dtype)
        back_gate, back_up = cot * up * slope, cot * gelu
        d_gate[:, span] = (back_gate * scale).astype(d_gate.dtype)
        d_up[:, span] = (back_up * scale).astype(d_up.dtype)
        dots[...] += jnp.sum(back_gate * gate + back_up * up, axis=-1, keepdims=True)

    total.end(emit)
    tile_out[...] = jnp.zeros_like(tile_out)
    to_tile(tile_out, 0, dots[...] * (scale * scale * (1.0 / (8 * cols))), eye)


def ffn_scatter(x_low, attn, gain, w_gate, w_up, d_hidden, cid, width=512):
    rows, half = d_hidden.shape
    cols = gain.shape[1]
    counts = half // width
    low, f32 = jnp.bfloat16, jnp.float32
    dma = pltpu.SemaphoreType.DMA
    vm = pl.BlockSpec(memory_space=pltpu.VMEM)
    hbm = pl.BlockSpec(memory_space=pl.ANY)
    out_shape = [jax.ShapeDtypeStruct((rows, half), low)] * 3 + [
        jax.ShapeDtypeStruct((cols, 8 * rows), low),
        jax.ShapeDtypeStruct((8, LANES), f32),
    ]
    scratch = [
        pltpu.VMEM((8 * rows, cols), low),
        pltpu.VMEM((cols, 2 * half), low),
        pltpu.VMEM((8, 8, LANES), f32),
        pltpu.VMEM((8, 8, LANES), f32),
        dma((7,)), dma((7,)),
        pltpu.VMEM((rows, 1), f32),
        dma((2,)),
    ] + reduce_scratch(counts, rows, width)
    kernel = functools.partial(ffn_kernel, rows, width, counts)
    return kernel_call(kernel, out_shape, [x_low, attn, gain, w_gate, w_up, d_hidden], [vm, vm, vm, hbm, hbm, vm],
                       scratch, cid, "ffn", late=(5,))


def load_own(spread, payload, width, counts, sems):
    copies = []
    for half in range(2):
        for at in range(counts):
            first = at * width + (half * counts * width if len(payload) == 1 else 0)
            src = payload[half % len(payload)].at[:, first : first + width]
            copies.append(pltpu.make_async_copy(src, spread.slot(0, half, at), sems.at[half, at]))
    return copies


def chip_place(here, per):
    def place(at):
        return here.shard(at // (2 * per), at // per % 2) * per + at % per

    return place


def back_kernel(rows, width, counts, act_t, w_gate, w_up, d_gate, d_up, dots, x_low, attn, gain, d_norm, gain_grad,
                grad_gate, grad_up, *refs, late):
    here = Place()
    spread = Spread(here, counts, refs[:7])
    tiny_all, tiny_send, tiny_recv, own_sems, weight, sums, grads, staged, local_sems, out_sems = refs[7:17]
    contrib, rest, rest_sems = refs[17:20]
    line = Line(here, 4, [contrib, d_norm] + list(refs[20:]), chip_place(here, 2))
    tiny = Tiny(here, dots, tiny_all, (tiny_send, tiny_recv), False)
    half_cols = counts * width
    local = [
        pltpu.make_async_copy(w_gate, weight.at[:, :half_cols], local_sems.at[0]),
        pltpu.make_async_copy(w_up, weight.at[:, half_cols:], local_sems.at[1]),
    ]
    own = load_own(spread, (d_gate, d_up), width, counts, own_sems)
    for copy in own + local:
        copy.start()
    greet(here, tiny.peers, True)
    for copy in own:
        copy.wait()
    tiny.begin()
    spread.begin()
    sums[...] = jnp.zeros_like(sums)
    for copy in local + late:
        copy.wait()

    def columns(half, at):
        return pl.ds(pl.multiple_of((half * counts + at) * width, width), width)

    def clear(at, _):
        grads[:, columns(0, at)] = jnp.zeros((grads.shape[0], width), jnp.float32)
        return 0

    lax.fori_loop(0, 2 * counts, clear, 0)

    def blocks(across, half, at):
        cols = columns(half, at)
        gained = grads[:, cols]
        for other in range(2):
            row = row_span(here, across, other, rows)
            block = spread.got[across, (spread.core + other) % 2, half, at]
            sums[row, :] += dot_nt(block, weight[:, cols])
            gained = gained + dot_nn(act_t[:, row], block)
        grads[:, cols] = gained

    def leave(half, at):
        spot = pl.ds(pl.multiple_of(at * width, width), width)
        return pltpu.make_async_copy(staged.at[half], (grad_gate, grad_up)[half].at[:, spot],
                                     out_sems.at[half, at])

    eye = diagonal()
    gain_grad[...] = jnp.zeros_like(gain_grad)

    def close_chip(chip, target):
        def close_shard(other, _):
            shard = here.shard(chip, other)
            span = pl.ds(pl.multiple_of(shard * rows, rows), rows)
            loads = [pltpu.make_async_copy(src.at[span, :], rest.at[at], rest_sems.at[at])
                     for at, src in enumerate((x_low, attn))]
            for copy in loads:
                copy.start()
            for copy in loads:
                copy.wait()
            for at in range(rows // LANES):
                span = pl.ds(pl.multiple_of(shard * rows + at * LANES, LANES), LANES)
                piece = slice(at * LANES, (at + 1) * LANES)
                dot = from_tile(tiny_all[shard, at : at + 1, :], eye)
                resid = rest[0, piece, :].astype(jnp.float32) + rest[1, piece, :].astype(jnp.float32)
                value = sums[span, :]
                target[span, :] = (value * gain[0:1, :] - resid * dot).astype(target.dtype)
                gain_grad[...] += jnp.sum(value * resid, axis=0, keepdims=True)
            return 0

        lax.fori_loop(0, 2, close_shard, 0)

    def done(stage, at):
        @pl.when(jnp.logical_and(stage == 3, at > 0))
        def _():
            leave(0, at - 1).wait()
            leave(1, at - 1).wait()

        @pl.when(stage == 3)
        def _():
            for half in range(2):
                staged[half] = grads[:, columns(half, at)].astype(staged.dtype)
            leave(0, at).start()
            leave(1, at).start()

        @pl.when(jnp.logical_and(at == counts - 1, stage == 0))
        def _():
            close_chip(0, contrib)
            line.launch(0, 4)

        @pl.when(jnp.logical_and(at == counts - 1, stage == 2))
        def _():
            lax.fori_loop(1, 3, lambda chip, _: (close_chip(chip, d_norm), 0)[1], 0)

    def hook(step):
        @pl.when(jnp.logical_and(step >= counts, step < counts + 6))
        def _():
            line.step(step - counts)

    tiny.end()
    spread.run(blocks, hook, done)
    close_chip(3, d_norm)
    line.settle()
    spread.end()

    def drain(at, _):
        leave(0, at).wait()
        leave(1, at).wait()
        return 0

    lax.fori_loop(counts - 1, counts, drain, 0)


def back_gather(act_t, w_gate, w_up, d_gate, d_up, dots, x_low, attn, gain, cid, width=512):
    cols, total = act_t.shape
    rows, half = d_gate.shape
    counts = half // width
    low, f32 = jnp.bfloat16, jnp.float32
    dma = pltpu.SemaphoreType.DMA
    vm = pl.BlockSpec(memory_space=pltpu.VMEM)
    hbm = pl.BlockSpec(memory_space=pl.ANY)
    out_shape = [
        jax.ShapeDtypeStruct((total, cols), low),
        jax.ShapeDtypeStruct((1, cols), f32),
        jax.ShapeDtypeStruct((cols, half), low),
        jax.ShapeDtypeStruct((cols, half), low),
    ]
    scratch = spread_scratch(counts, rows, width) + [
        pltpu.VMEM((8, 8, LANES), f32), dma((7,)), dma((7,)), dma((2, counts)),
        pltpu.VMEM((cols, 2 * half), low),
        pltpu.VMEM((total, cols), f32),
        pltpu.VMEM((cols, 2 * half), f32),
        pltpu.VMEM((2, cols, width), low),
        dma((2,)), dma((2, counts)),
        pltpu.VMEM((total, cols), low),
        pltpu.VMEM((2, rows, cols), low),
        dma((2,)),
    ] + line_scratch(4, (4 * rows // 2, cols), low)
    operands = [act_t, w_gate, w_up, d_gate, d_up, dots, x_low, attn, gain]
    kernel = functools.partial(back_kernel, rows, width, counts)
    return kernel_call(kernel, out_shape, operands, [vm] + [hbm] * 4 + [vm, hbm, hbm, vm], scratch, cid, "back",
                       [vm, vm, hbm, hbm], (0,))


def down_kernel(rows, width, counts, cot, weight, hidden, d_norm, ffn, d_attn, grad, *refs, late):
    here = Place()
    spread = Spread(here, counts, refs[:7])
    own_sems, sums, grads, staged, out_sems, norm_out = refs[7:13]
    place = chip_place(here, 4)
    norm_line = Line(here, 24, [d_norm, norm_out] + list(refs[13:]), lambda at: place(at + 8))
    own = load_own(spread, (hidden,), width, counts, own_sems)
    for copy in own:
        copy.start()
    greet(here, slice_peers(here), True)
    norm_line.begin()
    for copy in own:
        copy.wait()
    spread.begin()
    sums[...] = jnp.zeros_like(sums)
    grads[...] = jnp.zeros_like(grads)
    for copy in late:
        copy.wait()

    def columns(half, at):
        return pl.ds(pl.multiple_of((half * counts + at) * width, width), width)

    def blocks(across, half, at):
        cols = columns(half, at)
        gained = grads[cols, :]
        for other in range(2):
            row = row_span(here, across, other, rows)
            block = spread.got[across, (spread.core + other) % 2, half, at]
            sums[row, :] += dot_nn(block, weight[cols, :])
            gained = gained + dot_tn(block, cot[row, :])
        grads[cols, :] = gained

    def leave(half, at):
        return pltpu.make_async_copy(staged.at[at % 2, half], grad.at[columns(half, at), :], out_sems.at[half, at])

    def done(stage, at):
        @pl.when(jnp.logical_and(stage == 3, at > 1))
        def _():
            leave(0, at - 2).wait()
            leave(1, at - 2).wait()

        @pl.when(stage == 3)
        def _():
            for half in range(2):
                staged[at % 2, half] = grads[columns(half, at), :].astype(staged.dtype)
            leave(0, at).start()
            leave(1, at).start()

    norm_line.steps(spread.run(blocks, norm_line.step, done), 26)
    ffn[...] = sums[...].astype(ffn.dtype)
    norm_line.settle()

    def add_norm(at, _):
        def add(source):
            span = row_span(here, at // 2, at % 2, rows)
            d_attn[span, :] = (cot[span, :].astype(jnp.float32) + source[span, :].astype(jnp.float32)).astype(
                d_attn.dtype)

        @pl.when(at < 2)
        def _():
            add(d_norm)

        @pl.when(at >= 2)
        def _():
            add(norm_out)
        return 0

    lax.fori_loop(0, 8, add_norm, 0)
    spread.end()

    def drain(at, _):
        leave(0, at).wait()
        leave(1, at).wait()
        return 0

    lax.fori_loop(counts - 2, counts, drain, 0)


def down_gather(cot, weight, hidden, d_norm, cid, width=256):
    total, cols = cot.shape
    rows, every = hidden.shape
    counts = every // (2 * width)
    low, f32 = jnp.bfloat16, jnp.float32
    dma = pltpu.SemaphoreType.DMA
    vm = pl.BlockSpec(memory_space=pltpu.VMEM)
    hbm = pl.BlockSpec(memory_space=pl.ANY)
    out_shape = [
        jax.ShapeDtypeStruct((total, cols), low),
        jax.ShapeDtypeStruct((total, cols), low),
        jax.ShapeDtypeStruct(weight.shape, low),
    ]
    scratch = spread_scratch(counts, rows, width) + [
        dma((2, counts)),
        pltpu.VMEM((total, cols), f32),
        pltpu.VMEM(weight.shape, f32),
        pltpu.VMEM((2, 2, width, cols), low),
        dma((2, counts)),
        pltpu.VMEM((total, cols), low),
    ] + line_scratch(24, (24 * rows // 4, cols), low)
    kernel = functools.partial(down_kernel, rows, width, counts)
    return kernel_call(kernel, out_shape, [cot, weight, hidden, d_norm], [vm, vm, hbm, vm], scratch, cid, "down",
                       [vm, vm, hbm], (0, 1))


def attend_kernel(rows, heads, cols, qkv, rms, cos, sin, mask, w_out, cot, part, mixed_all, g_col, kv, probs, queries,
                  pair_rms, *refs, late):
    here = Place()
    spread = Spread(here, heads // 2, refs[:7])
    sums, pair_sems, turn_send, turn_recv, local_sem, tiny_own, tiny_pair = refs[7:14]
    got, core = spread.got, here.core
    greet(here, slice_peers(here))
    me = here.shard(0, 0)

    def turn_copy(at):
        across, other = turned(at)
        first = pl.multiple_of(here.shard(across, other) * cols, cols)
        return remote(cot.at[:, pl.ds(first, cols)], g_col.at[pl.ds(pl.multiple_of(me * rows, rows), rows), :],
                      turn_send.at[at], turn_recv.at[at], here.device(across, other))

    own_turn = pltpu.make_async_copy(cot.at[:, pl.ds(pl.multiple_of(me * cols, cols), cols)],
                                     g_col.at[pl.ds(pl.multiple_of(me * rows, rows), rows), :], local_sem)
    own_turn.start()
    half = HD // 2
    scale = 1.0 / math.sqrt(HD)
    wide = heads * HD

    def rotated(first):
        lead = qkv[:, first : first + half] * rms[...]
        trail = qkv[:, first + half : first + HD] * rms[...]
        return lead * cos[0] - trail * sin[0], trail * cos[0] + lead * sin[0]

    low_k, high_k = rotated(wide)
    kv[0, :, :half] = low_k.astype(kv.dtype)
    kv[0, :, half:HD] = high_k.astype(kv.dtype)
    for at in range(2):
        first = HD + at * half
        kv[0, :, first : first + half] = (qkv[:, wide + first : wide + first + half] * rms[...]).astype(kv.dtype)
    eye = diagonal()
    tiny_own[...] = jnp.zeros_like(tiny_own)
    to_tile(tiny_own, 0, rms[:, :1], eye)
    pair_rms[0] = rms[...]
    pair = remote(kv.at[0], kv.at[1], pair_sems.at[0], pair_sems.at[1], spread.ydev)
    tiny = remote(tiny_own, tiny_pair, pair_sems.at[2], pair_sems.at[3], spread.ydev)
    for head in range(heads):
        if head == 1:
            pair.start()
            tiny.start()
            turn_copy(2 * (3 - 1)).start()
            turn_copy(2 * (3 - 1) + 1).start()
        lead, trail = rotated(head * HD)
        queries[:, head * HD : head * HD + half] = (lead * scale).astype(queries.dtype)
        queries[:, head * HD + half : (head + 1) * HD] = (trail * scale).astype(queries.dtype)
    pair.wait()
    for copy in late:
        copy.wait()
    for at in range(7):
        if at // 2 != 2:
            turn_copy(at).start()

    def one_head(head, _):
        query = queries[:, pl.ds(pl.multiple_of(head * HD, HD), HD)]
        scores = jnp.concatenate([dot_nt(query, kv[0, :, :HD]), dot_nt(query, kv[1, :, :HD])], axis=1)
        scores = jnp.where(mask[...] > 0, scores, NEG)
        expd = jnp.exp(scores - jnp.max(scores, axis=-1, keepdims=True))
        prob = expd / jnp.sum(expd, axis=-1, keepdims=True)
        probs[head] = prob
        prob_low = prob.astype(jnp.bfloat16)
        mixed = dot_nn(prob_low[:, :rows], kv[0, :, HD:]) + dot_nn(prob_low[:, rows:], kv[1, :, HD:])
        got[0, core, head // (heads // 2), head % (heads // 2)] = mixed.astype(got.dtype)
        return 0

    lax.fori_loop(0, heads, one_head, 0)
    sums[...] = jnp.zeros_like(sums)
    spread.begin()

    def blocks(across, half_at, at):
        span = pl.ds(pl.multiple_of((half_at * (heads // 2) + at) * HD, HD), HD)
        for other in range(2):
            row = row_span(here, across, other, rows)
            block = got[across, (core + other) % 2, half_at, at]
            mixed_all[row, span] = block
            sums[row, :] += dot_nn(block, w_out[span, :])

    spread.run(blocks)
    part[...] = sums[...].astype(part.dtype)
    spread.end()
    tiny.wait()
    for at in range(rows // LANES):
        values = jnp.broadcast_to(from_tile(tiny_pair[at : at + 1, :], eye), (LANES, LANES))
        pair_rms[1, at * LANES : (at + 1) * LANES, :] = values
    own_turn.wait()
    for at in range(7):
        turn_copy(at).wait()


def attend(qkv, rms, cos, sin, mask, w_out, cot, cid):
    rows = qkv.shape[0]
    wide, cols = w_out.shape
    heads = wide // HD
    low, f32 = jnp.bfloat16, jnp.float32
    dma = pltpu.SemaphoreType.DMA
    vm = pl.BlockSpec(memory_space=pltpu.VMEM)
    out_shape = [
        jax.ShapeDtypeStruct((8 * rows, cols), low),
        jax.ShapeDtypeStruct((8 * rows, wide), low),
        jax.ShapeDtypeStruct((8 * rows, cols), low),
        jax.ShapeDtypeStruct((2, rows, 2 * HD), low),
        jax.ShapeDtypeStruct((heads, rows, 2 * rows), f32),
        jax.ShapeDtypeStruct((rows, wide), low),
        jax.ShapeDtypeStruct((2,) + rms.shape, f32),
    ]
    scratch = spread_scratch(heads // 2, rows, HD) + [
        pltpu.VMEM((8 * rows, cols), f32), dma((4,)), dma((7,)), dma((7,)), dma(()),
        pltpu.VMEM((8, LANES), f32), pltpu.VMEM((8, LANES), f32)]
    kernel = functools.partial(attend_kernel, rows, heads, cols)
    return kernel_call(kernel, out_shape, [qkv, rms, cos, sin, mask, w_out, cot], [vm] * 7, scratch, cid,
                       "attend", late=(4, 5))


def tail_kernel(rows, heads, per, d_attn, w_out, queries, kv, probs, rms, cos, sin, act_t, w_qkv, ffn, x_low,
                attn, gain, gain_grad, mixed_all, d_tok, out, grad_query, grad_out, kv_sum, gain_tiles, *refs, late):
    here = Place()
    width = HD
    counts = heads // 2
    part = rows // 2
    refs = list(refs)
    line_counts = 8 * per
    cols = d_attn.shape[1]
    extra = cols // (rows // per)

    def take(count):
        taken_refs = refs[:count]
        del refs[:count]
        return taken_refs

    total_refs = take(11)
    spread = Spread(here, 1, take(7))
    d_mixed, tiny_own, tiny_all, d_kv, give, taken, give_sems, tiny_send, tiny_recv = take(9)
    grad, grad_mixed, gain_sum, tile, tile_send, tile_recv, put_sems, local_sems, mixed_two, mixed_sems = take(10)

    def far(at):
        return turned(at // per)

    def near(at):
        at = jnp.minimum(at, line_counts - 1)
        x_stream, y_stream = spread.streams(at // 4)
        second = at // 2 % 2
        across = x_stream[0] + second * (y_stream[0] - x_stream[0])
        half_at = x_stream[1] + second * (y_stream[1] - x_stream[1])
        return across, at % 2, half_at

    def place_ffn(at):
        return here.shard(*far(at)) * per + at % per

    def place_tok(at):
        across, other, half_at = near(at)
        return jnp.where(at < line_counts, here.shard(across, other) * per + half_at, at)

    ffn_sum, leaving = take(2)
    by_chip = chip_place(here, per)
    line = Line(here, line_counts, [ffn, ffn_sum] + take(8), by_chip)
    contrib, summed = take(2)
    line_tok = Line(here, line_counts + extra, [contrib, summed] + take(8), place_tok)
    tiny = Tiny(here, tiny_own, tiny_all, (tiny_send, tiny_recv), False)
    got, core = spread.got, here.core
    product = products(here, d_attn, w_out, True, rows, width, counts)
    total = Reduce(here, counts, product, total_refs)
    greet(here, tiny.peers, True)
    line.begin()
    grad_mixed[...] = jnp.zeros_like(grad_mixed)

    def mixed_copy(step):
        span = pl.ds(pl.multiple_of(step * rows, rows), rows)
        return pltpu.make_async_copy(mixed_all.at[span, :], mixed_two.at[step % 2], mixed_sems.at[step % 2])

    mixed_copy(0).start()

    def beside(step):
        line.step(step)

        @pl.when(step < 8)
        def _():
            span = pl.ds(pl.multiple_of(step * rows, rows), rows)
            mixed_copy(step).wait()

            @pl.when(step < 7)
            def _():
                mixed_copy(step + 1).start()

            grad_mixed[...] += dot_tn(mixed_two[step % 2], d_attn[span, :])

    done = total.run(beside)
    grad_out[...] = grad_mixed[...].astype(grad_out.dtype)

    def land(at, first, second):
        for half_at, value in enumerate((first, second)):
            d_mixed[:, pl.ds(pl.multiple_of((half_at * counts + at) * width, width), width)] = value.astype(
                d_mixed.dtype)

    total.end(land)
    half = HD // 2
    scale = 1.0 / math.sqrt(HD)
    depth = w_qkv.shape[0] * 8
    d_kv[...] = jnp.zeros_like(d_kv)
    for copy in late:
        copy.wait()

    def one_head(head, dots):
        span = pl.ds(pl.multiple_of(head * HD, HD), HD)
        query = queries[:, span]
        cot = d_mixed[:, span]
        prob = probs[head]
        d_prob = jnp.concatenate([dot_nt(cot, kv[0, :, HD:]), dot_nt(cot, kv[1, :, HD:])], axis=1)
        delta = jnp.sum(prob * d_prob, axis=-1, keepdims=True)
        d_score = (prob * (d_prob - delta)).astype(jnp.bfloat16)
        prob_low = prob.astype(jnp.bfloat16)
        d_query = (dot_nn(d_score[:, :rows], kv[0, :, :HD]) + dot_nn(d_score[:, rows:], kv[1, :, :HD])) * scale
        for side in range(2):
            keys = slice(side * rows, (side + 1) * rows)
            d_kv[side, :, :HD] += dot_tn(d_score[:, keys], query)
            d_kv[side, :, HD:] += dot_tn(prob_low[:, keys], cot)
        dots = dots + jnp.sum(d_query * query.astype(jnp.float32), axis=-1, keepdims=True)
        lead, trail = d_query[:, :half], d_query[:, half:]
        first = ((lead * cos[0] + trail * sin[0]) * rms[0]).astype(got.dtype)
        second = ((trail * cos[0] - lead * sin[0]) * rms[0]).astype(got.dtype)
        line.step(done + head)
        for rows_at in range(2):
            piece = slice(rows_at * part, (rows_at + 1) * part)
            got[0, core, rows_at, 0, :, pl.ds(pl.multiple_of(head * HD, HD), half)] = first[piece, :]
            got[0, core, rows_at, 0, :, pl.ds(pl.multiple_of(head * HD + half, half), half)] = second[piece, :]

        return dots

    dots = lax.fori_loop(0, heads, one_head, jnp.zeros((rows, 1), jnp.float32))
    eye = diagonal()
    tiny_own[...] = jnp.zeros_like(tiny_own)
    for side in (1, 0):
        d_key, d_value = d_kv[side, :, :HD], d_kv[side, :, HD:]
        own = jnp.sum(d_key * kv[side, :, :HD].astype(jnp.float32) +
                      d_value * kv[side, :, HD:].astype(jnp.float32), axis=-1, keepdims=True)
        if side == 0:
            own = own + dots * (1.0 / scale)
        own = own * (rms[side] * rms[side] * (1.0 / depth))
        to_tile(tiny_own, side * (rows // LANES), own, eye)
        lead, trail = d_key[:, :half], d_key[:, half:]
        parts = [(lead * cos[side] + trail * sin[side]) * rms[side],
                 (trail * cos[side] - lead * sin[side]) * rms[side],
                 d_value[:, :half] * rms[side], d_value[:, half:] * rms[side]]
        for at, value in enumerate(parts):
            if side == 1:
                give[:, at * half : (at + 1) * half] = value.astype(give.dtype)
            else:
                d_kv[0, :, at * half : (at + 1) * half] = value
    given = remote(give, taken, give_sems.at[0], give_sems.at[1], spread.ydev)
    given.start()
    grad[...] = jnp.zeros_like(grad)
    given.wait()
    for rows_at in range(2):
        piece = slice(rows_at * part, (rows_at + 1) * part)
        value = d_kv[0, piece, :] + taken[piece, :].astype(jnp.float32)
        got[0, core, rows_at, 0, :, heads * HD :] = value.astype(got.dtype)
    tiny.begin()
    for hop in range(2):
        spread.x_copy(hop, 0).start()
        spread.y_copy(hop, 0).start()
    for stream in range(2):
        spread.sib_copy(0, stream, 0).start()
    gain_sum[...] = jnp.zeros_like(gain_sum)
    line.end(done + heads)
    tiny.end()

    def block_of(at):
        across, other, half_at = near(at)
        shard, partner = here.shard(across, other), here.shard((across + 2) % 4, other)
        block = got[across, (core + other) % 2, half_at, 0]
        first = pl.multiple_of(shard * rows + half_at * part, part)
        for tile_at in range(part // LANES):
            row = pl.ds(pl.multiple_of(first + tile_at * LANES, LANES), LANES)
            low_at = half_at * (part // LANES) + tile_at
            kept = rows // LANES + low_at
            dot = from_tile(tiny_all[shard, pl.ds(low_at, 1), :] + tiny_all[partner, pl.ds(kept, 1), :], eye)
            value = dot_nt(block[tile_at * LANES : (tile_at + 1) * LANES, :], w_qkv[...])
            x_rows = x_low[row, :].astype(jnp.float32)
            contrib[row, :] = (value * gain[0:1, :] - x_rows * dot).astype(contrib.dtype)
            gain_sum[...] += jnp.sum(value * x_rows, axis=0, keepdims=True)
        line_tok.launch(at, 1)
        rows_t = act_t[:, pl.ds(first, part)]
        for at_col in range((heads + 2) * HD // 512):
            span = slice(at_col * 512, (at_col + 1) * 512)
            grad[:, span] += dot_nn(rows_t, block[:, span])

    me = here.shard(0, 0)
    columns = pl.ds(pl.multiple_of(me * cols, cols), cols)
    chunk = line.chunk

    def landing(which, at):
        sub = at % per if which == 0 else near(at)[2]
        return (out, d_tok)[which].at[pl.ds(pl.multiple_of(sub * chunk, chunk), chunk), columns]

    def leaver(which, at):
        return (leaving, line_tok.from_end)[which].at[at]

    def put(which, at):
        goal = here.device(*(far(at) if which == 0 else near(at)[:2]))
        return remote(leaver(which, at), landing(which, at), put_sems.at[which, 0, at], put_sems.at[which, 1, at],
                      goal)

    def keep(which, at):
        spot = at % per if which == 0 else near(at)[2]
        return pltpu.make_async_copy(leaver(which, at), landing(which, at), local_sems.at[which, spot])

    def emit(which, at):
        if which == 1:
            row = line_tok.rows(at)
            value = d_attn[row, :].astype(jnp.float32) + summed[row, :].astype(jnp.float32)
            line_tok.from_end[at] = value.astype(out.dtype)
            return
        row = pl.ds(pl.multiple_of(place_ffn(at) * chunk, chunk), chunk)

        def leave(source):
            value = x_low[row, :].astype(jnp.float32) + attn[row, :].astype(jnp.float32)
            leaving[at] = (value + source[row, :].astype(jnp.float32)).astype(out.dtype)

        leave(ffn_sum)

    def is_own(which, at):
        return at >= 7 * per if which == 0 else jnp.logical_and(at < 4, at % 2 == 0)

    def send(which, at):
        own = is_own(which, at)

        @pl.when(own)
        def _():
            keep(which, at).start()

        @pl.when(jnp.logical_not(own))
        def _():
            put(which, at).start()

    def stage_step(step, _):
        stage = step // 4

        @pl.when(jnp.logical_and(step % 4 == 0, jnp.logical_and(stage > 0, stage < 4)))
        def _():
            spread.x_copy(stage - 1, 0).wait_recv()
            spread.sib_copy(stage, 0, 0).start()
            spread.y_copy(stage - 1, 0).wait_recv()
            spread.sib_copy(stage, 1, 0).start()

        @pl.when(step == 4)
        def _():
            spread.x_copy(2, 0).start()
            spread.y_copy(2, 0).start()

        @pl.when(step < line_counts)
        def _():
            for stream in range(2):
                @pl.when(step % 4 == 2 * stream)
                def _(stream=stream):
                    spread.sib_copy(stage, stream, 0).wait_recv()

            block_of(step)

        @pl.when(step >= 4)
        def _():
            line_tok.step(step - 4)

        @pl.when(step > 0)
        def _():
            send(0, step - 1)

        emit(0, step)

        @pl.when(jnp.logical_and(line.inner == 1, step > 7))
        def _():
            send(1, step - 8)

        @pl.when(jnp.logical_and(line.inner == 1, step > 6))
        def _():
            emit(1, step - 7)
        return 0

    lax.fori_loop(0, line_counts, stage_step, 0)
    for half_at in range(cols // (rows // per)):
        span = pl.ds(line_counts * (rows // per) + half_at * (rows // per), rows // per)
        source = slice(half_at * (rows // per), (half_at + 1) * (rows // per))
        contrib[span, :] = grad[source, heads * HD :].astype(contrib.dtype)
    line_tok.launch(line_counts, extra)
    grad_query[...] = grad[:, : heads * HD].astype(grad_query.dtype)
    for at in range(cols // LANES):
        tile[at : at + 1, :] = gain_sum[:, at * LANES : (at + 1) * LANES]
        spot = cols // LANES + at
        tile[spot : spot + 1, :] = gain_grad[:, at * LANES : (at + 1) * LANES]

    def tile_copy(step):
        return remote(tile, gain_tiles.at[here.z], tile_send.at[step], tile_recv.at[step],
                      (here.dp, here.seq, (here.z + step + 1) % 4))

    send(0, line_counts - 1)
    for step in range(3):
        tile_copy(step).start()
    gain_tiles[here.z] = tile[...]

    @pl.when(line.inner == 1)
    def _():
        start = line_counts - 4

        def both(at, _):
            line_tok.step(at)

            @pl.when(at < line_counts + 4)
            def _():
                send(1, at - 4)

            @pl.when(at < line_counts + 3)
            def _():
                emit(1, at - 3)
            return 0

        lax.fori_loop(start, line_counts + extra + 2, both, 0)

        def drain(at, _):
            line_tok.down(at).wait_send()
            return 0

        lax.fori_loop(0, line_counts + extra, drain, 0)

    @pl.when(line.inner == 0)
    def _():
        def arrive(at, _):
            line_tok.up(at).wait_send()
            line_tok.down(at).wait_recv()

            @pl.when(jnp.logical_and(at > 0, at <= line_counts))
            def _():
                send(1, at - 1)

            @pl.when(at < line_counts)
            def _():
                emit(1, at)
            return 0

        lax.fori_loop(0, line_counts + extra, arrive, 0)

    for half_at in range(extra):
        span = pl.ds((line_counts + half_at) * chunk, chunk)
        kv_sum[half_at * chunk : (half_at + 1) * chunk, :] = summed[span, :]
    for hop in range(3):
        spread.x_copy(hop, 0).wait_send()
        spread.y_copy(hop, 0).wait_send()
    for stage in range(4):
        spread.sib_copy(stage, 0, 0).wait_send()
        spread.sib_copy(stage, 1, 0).wait_send()

    def finish(at, _):
        for which in range(2):
            own = is_own(which, at)

            @pl.when(own)
            def _():
                keep(which, at).wait()

            @pl.when(jnp.logical_not(own))
            def _():
                put(which, at).wait()
        return 0

    lax.fori_loop(0, line_counts, finish, 0)
    for step in range(3):
        tile_copy(step).wait()


def tail(d_attn, w_out, queries, kv, probs, rms, cos, sin, act_t, w_qkv, ffn, x_low, attn, gain, gain_grad,
         mixed_all, cid,
 per=2):
    total, cols = d_attn.shape
    rows = total // 8
    wide = w_out.shape[0]
    heads = wide // HD
    low, f32 = jnp.bfloat16, jnp.float32
    dma = pltpu.SemaphoreType.DMA
    vm = pl.BlockSpec(memory_space=pltpu.VMEM)
    counts = 8 * per
    chunk = rows // per
    extra = cols // chunk
    long = (total + cols, cols)
    out_shape = [
        jax.ShapeDtypeStruct((rows, 8 * cols), low),
        jax.ShapeDtypeStruct((rows, 8 * cols), low),
        jax.ShapeDtypeStruct((cols, wide), low),
        jax.ShapeDtypeStruct(w_out.shape, low),
        jax.ShapeDtypeStruct((cols, 2 * HD), low),
        jax.ShapeDtypeStruct((4, 8, LANES), f32),
    ]
    scratch = reduce_scratch(heads // 2, rows, HD, 2) + spread_scratch(1, rows // 2, wide + 2 * HD)
    scratch += [
        pltpu.VMEM((rows, wide), low),
        pltpu.VMEM((8, LANES), f32),
        pltpu.VMEM((8, 8, LANES), f32),
        pltpu.VMEM((2, rows, 2 * HD), f32),
        pltpu.VMEM((rows, 2 * HD), low),
        pltpu.VMEM((rows, 2 * HD), low),
        dma((2,)), dma((7,)), dma((7,)),
        pltpu.VMEM(w_qkv.shape, f32),
        pltpu.VMEM(w_out.shape, f32),
        pltpu.VMEM((1, cols), f32),
        pltpu.VMEM((8, LANES), f32),
        dma((3,)), dma((3,)), dma((2, 2, counts)), dma((2, per)),
        pltpu.VMEM((2, rows, wide), low), dma((2,)),
        pltpu.VMEM((total, cols), low),
        pltpu.VMEM((counts, chunk, cols), low),
    ] + line_scratch(counts, (total, cols), low)
    scratch += [pltpu.VMEM(long, low), pltpu.VMEM(long, low)] + line_scratch(counts + extra, long, low)
    operands = [d_attn, w_out, queries, kv, probs, rms, cos, sin, act_t, w_qkv, ffn, x_low, attn, gain,
                gain_grad, mixed_all]
    kernel = functools.partial(tail_kernel, rows, heads, per)
    specs = [vm] * (len(operands) - 1) + [pl.BlockSpec(memory_space=pl.ANY)]
    return kernel_call(kernel, out_shape, operands, specs, scratch, cid, "tail",
                       late=(2, 3, 4, 8, 9, 11, 12))


LANES = 128


def acts_move(
    tokens, seg_ids, gain_attn, w_query, kv_weight, w_out, gain_ffn, w_gate, w_up, w_down, d_out
):
    rows = tokens.shape[0]
    segs = seg_ids.astype(jnp.float32).reshape(2 * rows // LANES, LANES)
    segs = jnp.pad(segs, ((0, 8 - 2 * rows // LANES), (0, 0)))
    both = jnp.stack([gain_attn, gain_ffn, gain_ffn, gain_attn]).astype(jnp.float32)
    gain_one, gain_two = both[:2], both[2:]
    wider = jnp.float32

    qkv, x_low, act_one_t, w_qkv, rms, cos, sin, mask = opening(
        tokens, gain_one, w_query, kv_weight, segs, 1
    )
    attn_part, mixed_all, g_low, kv, probs, queries, pair_rms = attend(
        qkv, rms, cos, sin, mask, w_out, d_out, 2
    )
    d_hidden, attn = scatter_product(g_low, w_down, 512, 3, attn_part)
    hidden, d_gate, d_up, act_two_t, dots = ffn_scatter(x_low, attn, gain_two, w_gate, w_up, d_hidden, 4)
    d_norm, grad_gain_two, grad_gate, grad_up = back_gather(
        act_two_t, w_gate, w_up, d_gate, d_up, dots, x_low, attn, gain_two, 5
    )
    ffn, d_attn, grad_down = down_gather(g_low, w_down, hidden, d_norm, 6)
    d_tokens, out, grad_query, grad_out, grad_kv, gain_tiles = tail(
        d_attn,
        w_out,
        queries,
        kv,
        probs,
        pair_rms,
        cos,
        sin,
        act_one_t,
        w_qkv,
        ffn,
        x_low,
        attn,
        gain_one,
        grad_gain_two,
        mixed_all,
        7,
    )
    gains = jnp.sum(gain_tiles, axis=0).reshape(2, -1)
    return (
        out,
        d_tokens.astype(wider),
        gains[0],
        grad_query.astype(wider),
        grad_kv.astype(wider),
        grad_out.astype(wider),
        gains[1],
        grad_gate.astype(wider),
        grad_up.astype(wider),
        grad_down.astype(wider),
    )


def solution(mesh):
    in_specs = (
        P(("dp", "seq"), None),
        P("dp"),
        P(("dp", "seq")),
        P(("dp", "seq"), "tensor"),
        P(("dp", "seq"), None),
        P("tensor", ("dp", "seq")),
        P(("dp", "seq")),
        P(("dp", "seq"), "tensor"),
        P(("dp", "seq"), "tensor"),
        P("tensor", ("dp", "seq")),
        P(("dp", "seq"), None),
    )
    out_specs = (
        P(("dp", "seq"), None),
        P(("dp", "seq"), None),
        P(("dp", "seq")),
        P(("dp", "seq"), "tensor"),
        P(("dp", "seq"), None),
        P("tensor", ("dp", "seq")),
        P(("dp", "seq")),
        P(("dp", "seq"), "tensor"),
        P(("dp", "seq"), "tensor"),
        P("tensor", ("dp", "seq")),
    )

    def shards(*arrays):
        tokens = arrays[0]
        sizes = tuple(mesh.shape[name] for name in ("dp", "seq", "tensor"))
        count = tokens.shape[0] * sizes[0] * sizes[1]
        plan = acts_move if sizes == (4, 2, 4) and count <= tokens.shape[1] else weights_move
        return plan(*arrays)

    return jax.shard_map(shards, mesh=mesh, in_specs=in_specs, out_specs=out_specs, check_vma=False)
```

```python
import functools
import math

import jax
import jax.numpy as jnp
from jax import lax
from jax.experimental import pallas as pl
from jax.experimental.pallas import tpu as pltpu
from jax.sharding import PartitionSpec as P

HD = 256


EPS = 1e-06
NEG = -1e30


def place_tables(segs):
    length = segs.shape[0]
    index = jnp.arange(length, dtype=jnp.int32)
    flags = jnp.concatenate([jnp.ones((1,), dtype=bool), segs[1:] != segs[:-1]])
    starts = lax.cummax(jnp.where(flags, index, jnp.zeros_like(index)), axis=0)
    places = index - starts
    half_size = HD // 2
    freqs = jnp.exp(jnp.arange(half_size, dtype=jnp.float32) * (-math.log(10000.0) / half_size))
    angles = places.astype(jnp.float32)[:, None] * freqs[None, :]
    return (places, jnp.cos(angles), jnp.sin(angles))


def rotate(vector, cos_table, sin_table):
    half_size = vector.shape[-1] // 2
    leading = vector[..., :half_size]
    trailing = vector[..., half_size:]
    return jnp.concatenate(
        [leading * cos_table - trailing * sin_table, trailing * cos_table + leading * sin_table],
        axis=-1,
    )


def rotate_back(vector, cos_table, sin_table):
    half_size = vector.shape[-1] // 2
    leading = vector[..., :half_size]
    trailing = vector[..., half_size:]
    return jnp.concatenate(
        [leading * cos_table + trailing * sin_table, trailing * cos_table - leading * sin_table],
        axis=-1,
    )


def matmul(left, right):
    return jnp.dot(left, right, preferred_element_type=jnp.float32)


def matmul_nt(left, right):
    return lax.dot_general(
        left, right, (((1,), (1,)), ((), ())), preferred_element_type=jnp.float32
    )


def matmul_tn(left, right):
    return lax.dot_general(
        left, right, (((0,), (0,)), ((), ())), preferred_element_type=jnp.float32
    )


def gelu_tanh(values):
    return jax.nn.gelu(values, approximate=True)


def norm_back(d_act, normed, rms_val, gain_val):
    scaled = d_act * gain_val
    return rms_val * (scaled - normed * jnp.mean(scaled * normed, axis=-1, keepdims=True))


def weights_move(
    tokens, seg_ids, gain_attn, w_query, kv_weight, w_out, gain_ffn, w_gate, w_up, w_down, d_out
):
    rows = tokens.shape[0]
    scale_factor = 1.0 / math.sqrt(HD)
    offset = lax.axis_index("seq") * rows
    places, cos_table, sin_table = place_tables(seg_ids)
    own_places = lax.dynamic_slice_in_dim(places, offset, rows, 0)
    own_segs = lax.dynamic_slice_in_dim(seg_ids, offset, rows, 0)
    own_cos = lax.dynamic_slice_in_dim(cos_table, offset, rows, 0)
    own_sin = lax.dynamic_slice_in_dim(sin_table, offset, rows, 0)
    allowed = (own_segs[:, None] == seg_ids[None, :]) & (own_places[:, None] >= places[None, :])
    full_query, full_out, full_kv, full_gain_one = (
        lax.all_gather(w_query, ("dp", "seq"), axis=0, tiled=True),
        lax.all_gather(w_out, ("dp", "seq"), axis=1, tiled=True),
        lax.all_gather(kv_weight, ("dp", "seq"), axis=0, tiled=True),
        lax.all_gather(gain_attn, ("dp", "seq"), axis=0, tiled=True),
    )
    gain_one = full_gain_one.astype(jnp.float32)
    inputs = tokens.astype(jnp.float32)
    rms_one = lax.rsqrt(jnp.mean(inputs * inputs, axis=-1, keepdims=True) + EPS)
    norm_one = inputs * rms_one
    act_one = (norm_one * gain_one).astype(jnp.bfloat16)
    query_pre = matmul(act_one, full_query)
    heads = query_pre.shape[1] // HD
    kv_pre = matmul(act_one, full_kv)
    queries = (
        rotate(query_pre.reshape(rows, heads, HD), own_cos[:, None, :], own_sin[:, None, :])
        * scale_factor
    ).astype(jnp.bfloat16)
    own_kv = jnp.concatenate(
        [rotate(kv_pre[:, :HD], own_cos, own_sin), kv_pre[:, HD:]], axis=1
    ).astype(jnp.bfloat16)
    all_kv = lax.all_gather(own_kv, "seq", axis=0, tiled=True)
    keys = all_kv[:, :HD]
    values_all = all_kv[:, HD:]
    scores = jnp.einsum("rhd,kd->hrk", queries, keys, preferred_element_type=jnp.float32)
    scores = jnp.where(allowed[None], scores, NEG)
    top_score = jnp.max(scores, axis=-1, keepdims=True)
    expd = jnp.exp(scores - top_score)
    total = jnp.sum(expd, axis=-1, keepdims=True)
    log_total = top_score + jnp.log(total)
    probs_low = (expd / total).astype(jnp.bfloat16)
    mixed = (
        jnp.einsum("hrk,kd->rhd", probs_low, values_all, preferred_element_type=jnp.float32)
        .reshape(rows, heads * HD)
        .astype(jnp.bfloat16)
    )
    attn = lax.psum(matmul(mixed, full_out), "tensor")
    resid = inputs + attn
    full_gate, full_up, full_down, full_gain_two = (
        lax.all_gather(w_gate, ("dp", "seq"), axis=0, tiled=True),
        lax.all_gather(w_up, ("dp", "seq"), axis=0, tiled=True),
        lax.all_gather(w_down, ("dp", "seq"), axis=1, tiled=True),
        lax.all_gather(gain_ffn, ("dp", "seq"), axis=0, tiled=True),
    )
    gain_two = full_gain_two.astype(jnp.float32)
    rms_two = lax.rsqrt(jnp.mean(resid * resid, axis=-1, keepdims=True) + EPS)
    norm_two = resid * rms_two
    act_two = (norm_two * gain_two).astype(jnp.bfloat16)
    gate = matmul(act_two, full_gate)
    up_val = matmul(act_two, full_up)
    gelu_val, gelu_pull = jax.vjp(gelu_tanh, gate)
    hidden = (gelu_val * up_val).astype(jnp.bfloat16)
    ffn = lax.psum(matmul(hidden, full_down).astype(jnp.bfloat16), "tensor").astype(jnp.float32)
    out = (resid + ffn).astype(jnp.bfloat16)
    back_gate, back_up, back_down = (
        lax.all_gather(w_gate, ("dp", "seq"), axis=0, tiled=True),
        lax.all_gather(w_up, ("dp", "seq"), axis=0, tiled=True),
        lax.all_gather(w_down, ("dp", "seq"), axis=1, tiled=True),
    )
    d_hidden = matmul_nt(d_out, back_down)
    grad_down = matmul_tn(hidden, d_out)
    d_gate = gelu_pull(d_hidden * up_val)[0].astype(jnp.bfloat16)
    d_up = (d_hidden * gelu_val).astype(jnp.bfloat16)
    grad_gate = matmul_tn(act_two, d_gate)
    grad_up = matmul_tn(act_two, d_up)
    d_act_two = lax.psum(matmul_nt(d_gate, back_gate) + matmul_nt(d_up, back_up), "tensor")
    grad_gain_two = jnp.sum(d_act_two * norm_two, axis=0)
    d_resid = d_out.astype(jnp.float32) + norm_back(d_act_two, norm_two, rms_two, gain_two)
    ffn_grads = (
        lax.psum_scatter(
            grad_gate.astype(jnp.bfloat16), ("dp", "seq"), scatter_dimension=0, tiled=True
        ).astype(jnp.float32),
        lax.psum_scatter(
            grad_up.astype(jnp.bfloat16), ("dp", "seq"), scatter_dimension=0, tiled=True
        ).astype(jnp.float32),
        lax.psum_scatter(
            grad_down.astype(jnp.bfloat16), ("dp", "seq"), scatter_dimension=1, tiled=True
        ).astype(jnp.float32),
        lax.psum_scatter(
            grad_gain_two.astype(jnp.bfloat16), ("dp", "seq"), scatter_dimension=0, tiled=True
        ).astype(jnp.float32),
    )
    back_query, back_out, back_kv = (
        lax.all_gather(w_query, ("dp", "seq"), axis=0, tiled=True),
        lax.all_gather(w_out, ("dp", "seq"), axis=1, tiled=True),
        lax.all_gather(kv_weight, ("dp", "seq"), axis=0, tiled=True),
    )
    d_attn = d_resid.astype(jnp.bfloat16)
    grad_out = matmul_tn(mixed, d_attn)
    d_mixed = matmul_nt(d_attn, back_out).astype(jnp.bfloat16).reshape(rows, heads, HD)
    scores_again = jnp.einsum("rhd,kd->hrk", queries, keys, preferred_element_type=jnp.float32)
    probs = jnp.where(allowed[None], jnp.exp(scores_again - log_total), 0.0)
    d_probs = jnp.einsum("rhd,kd->hrk", d_mixed, values_all, preferred_element_type=jnp.float32)
    delta = jnp.sum(probs * d_probs, axis=-1, keepdims=True)
    d_scores = (probs * (d_probs - delta)).astype(jnp.bfloat16)
    d_queries = (
        jnp.einsum("hrk,kd->rhd", d_scores, keys, preferred_element_type=jnp.float32) * scale_factor
    )
    d_query_pre = (
        rotate_back(d_queries, own_cos[:, None, :], own_sin[:, None, :])
        .reshape(rows, heads * HD)
        .astype(jnp.bfloat16)
    )
    d_keys_part = jnp.einsum("hrk,rhd->kd", d_scores, queries, preferred_element_type=jnp.float32)
    d_values_part = jnp.einsum(
        "hrk,rhd->kd", probs.astype(jnp.bfloat16), d_mixed, preferred_element_type=jnp.float32
    )
    own_kv_grad = lax.psum_scatter(
        jnp.concatenate([d_keys_part, d_values_part], axis=1).astype(jnp.bfloat16),
        "seq",
        scatter_dimension=0,
        tiled=True,
    )
    d_act_query = matmul_nt(d_query_pre, back_query)
    d_act_sum, kv_grad = (
        lax.psum(d_act_query.astype(jnp.bfloat16), "tensor").astype(jnp.float32),
        lax.psum(own_kv_grad, "tensor").astype(jnp.float32),
    )
    d_kv_pre = jnp.concatenate(
        [rotate_back(kv_grad[:, :HD], own_cos, own_sin), kv_grad[:, HD:]], axis=1
    ).astype(jnp.bfloat16)
    d_act_one = d_act_sum + matmul_nt(d_kv_pre, back_kv)
    grad_query = matmul_tn(act_one, d_query_pre)
    grad_kv = matmul_tn(act_one, d_kv_pre)
    grad_gain_one = jnp.sum(d_act_one * norm_one, axis=0)
    d_tokens = d_resid + norm_back(d_act_one, norm_one, rms_one, gain_one)
    attn_grads = (
        lax.psum_scatter(
            grad_query.astype(jnp.bfloat16), ("dp", "seq"), scatter_dimension=0, tiled=True
        ).astype(jnp.float32),
        lax.psum_scatter(
            grad_out.astype(jnp.bfloat16), ("dp", "seq"), scatter_dimension=1, tiled=True
        ).astype(jnp.float32),
        lax.psum_scatter(
            grad_kv.astype(jnp.bfloat16), ("dp", "seq"), scatter_dimension=0, tiled=True
        ).astype(jnp.float32),
        lax.psum_scatter(
            grad_gain_one.astype(jnp.bfloat16), ("dp", "seq"), scatter_dimension=0, tiled=True
        ).astype(jnp.float32),
    )
    return (
        out,
        d_tokens,
        attn_grads[3],
        attn_grads[0],
        attn_grads[2],
        attn_grads[1],
        ffn_grads[3],
        ffn_grads[0],
        ffn_grads[1],
        ffn_grads[2],
    )


MESH = pl.DeviceIdType.MESH
VMEM_LIMIT = 66000 * 1024


class Place:
    def __init__(self):
        self.dp = lax.axis_index("dp")
        self.seq = lax.axis_index("seq")
        self.z = lax.axis_index("tensor")
        self.core = lax.rem(self.dp, 2)
        self.chip = lax.div(self.dp, 2)

    def device(self, across, other):
        chip = (self.chip + across) % 2
        seq = (self.seq + across // 2) % 2
        core = (self.core + other) % 2
        return chip * 2 + core, seq, self.z

    def shard(self, across, other):
        dp, seq, _ = self.device(across, other)
        return dp * 2 + seq


def greet(here, peers, line=False):
    barrier = pltpu.get_barrier_semaphore()
    peers = list(peers)
    if line:
        peers += [(here.dp, here.seq, (here.z + step) % 4) for step in range(1, 4)]
    for peer in peers:
        pl.semaphore_signal(barrier, inc=1, device_id=peer, device_id_type=MESH)
    pl.semaphore_wait(barrier, len(peers))


def remote(src, dst, send, recv, peer):
    return pltpu.make_async_remote_copy(
        src_ref=src, dst_ref=dst, send_sem=send, recv_sem=recv, device_id=peer, device_id_type=MESH
    )


class Line:
    def __init__(self, here, counts, refs, place=None):
        self.own, self.out, self.from_end, self.from_mid = refs[:4]
        self.sems = refs[4:10]
        self.counts = counts
        self.chunk = self.from_end.shape[1]
        self.place = place
        z = here.z
        self.inner = ((z + 1) // 2) % 2
        self.mate = (here.dp, here.seq, z + 1 - 2 * (z % 2))
        self.other = (here.dp, here.seq, 3 - z)

    def rows(self, at):
        at = at if self.place is None else self.place(at)
        return pl.ds(pl.multiple_of(at * self.chunk, self.chunk), self.chunk)

    def up(self, at):
        return remote(self.own.at[self.rows(at), :], self.from_end.at[at], self.sems[0].at[at],
                      self.sems[1].at[at], self.mate)

    def over(self, at):
        return remote(self.out.at[self.rows(at), :], self.from_mid.at[at], self.sems[2].at[at],
                      self.sems[3].at[at], self.other)

    def down(self, at):
        rows = self.rows(at)
        return remote(self.out.at[rows, :], self.out.at[rows, :], self.sems[4].at[at],
                      self.sems[5].at[at], self.mate)

    def launch(self, first, count):
        @pl.when(self.inner == 0)
        def _():
            def send(at, _):
                self.up(first + at).start()
                return 0

            lax.fori_loop(0, count, send, 0)

    def begin(self):
        self.launch(0, self.counts)

    def first(self, at):
        rows = self.rows(at)
        self.up(at).wait_recv()
        total = self.own[rows, :].astype(jnp.float32) + self.from_end[at].astype(jnp.float32)
        self.out[rows, :] = total.astype(self.out.dtype)
        self.over(at).start()

    def second(self, at):
        rows = self.rows(at)
        self.over(at).wait()
        total = self.out[rows, :].astype(jnp.float32) + self.from_mid[at].astype(jnp.float32)
        self.out[rows, :] = total.astype(self.out.dtype)
        self.down(at).start()

    def step(self, at, start=0, count=None):
        count = self.counts if count is None else count

        @pl.when(jnp.logical_and(self.inner == 1, at < count))
        def _():
            self.first(start + at)

        @pl.when(jnp.logical_and(self.inner == 1, jnp.logical_and(at > 1, at < count + 2)))
        def _():
            self.second(start + at - 2)

    def steps(self, first, last, start=0, count=None):
        def rest(at, _):
            self.step(at, start, count)
            return 0

        lax.fori_loop(first, last, rest, 0)

    def settle(self):
        @pl.when(self.inner == 0)
        def _():
            def take(at, _):
                self.up(at).wait_send()
                self.down(at).wait_recv()
                return 0

            lax.fori_loop(0, self.counts, take, 0)

        self.drain()

    def drain(self):
        @pl.when(self.inner == 1)
        def _():
            def drain(at, _):
                self.down(at).wait_send()
                return 0

            lax.fori_loop(0, self.counts, drain, 0)

    def end(self, done=0):
        self.steps(min(done, self.counts + 2), self.counts + 2)
        self.settle()


def line_scratch(counts, shape, low):
    buf = pltpu.VMEM((counts, shape[0] // counts, shape[1]), low)
    return [buf, buf] + [pltpu.SemaphoreType.DMA((counts,))] * 6


def turned(at):
    return 3 - at // 2, 1 - at % 2


def slice_peers(here):
    return [here.device(*turned(at)) for at in range(7)]


def kernel_call(kernel, out_shape, operands, specs, scratch, cid, name, out_specs=None, late=()):
    vm = pl.BlockSpec(memory_space=pltpu.VMEM)
    specs = [pl.BlockSpec(memory_space=pl.ANY) if at in late else spec for at, spec in enumerate(specs)]
    inside = [pltpu.VMEM(operands[at].shape, operands[at].dtype) for at in late]
    if late:
        inside.append(pltpu.SemaphoreType.DMA((len(late),)))

    def body(*refs):
        if not late:
            kernel(*refs)
            return
        ins, rest, own = list(refs[: len(operands)]), refs[len(operands) : -len(inside)], refs[-len(inside) :]
        copies = []
        for spot, at in enumerate(late):
            copy = pltpu.make_async_copy(ins[at], own[spot], own[-1].at[spot])
            copy.start()
            copies.append(copy)
            ins[at] = own[spot]
        kernel(*ins, *rest, late=copies)

    return pl.pallas_call(
        body,
        out_shape=out_shape,
        in_specs=specs,
        out_specs=out_specs or [vm] * len(out_shape),
        scratch_shapes=scratch + inside,
        compiler_params=pltpu.CompilerParams(
            collective_id=cid, has_side_effects=True, vmem_limit_bytes=VMEM_LIMIT
        ),
        name=f"{name}_{cid}",
    )(*operands)


class Tiny:
    def __init__(self, here, src, dst, sems, spread):
        self.here, self.src, self.dst, self.sems, self.spread = here, src, dst, sems, spread
        self.peers = slice_peers(here)
        self.me = here.shard(0, 0)

    def tile(self, shard):
        return self.src.at[shard] if self.spread else self.src

    def copy(self, at):
        return remote(self.tile(self.here.shard(*turned(at))), self.dst.at[self.me], self.sems[0].at[at],
                      self.sems[1].at[at], self.peers[at])

    def begin(self):
        for at in range(7):
            self.copy(at).start()
        self.dst[self.me] = self.tile(self.me)[...]

    def end(self):
        for at in range(7):
            self.copy(at).wait()


class Reduce:
    def __init__(self, here, counts, product, refs, before=None):
        self.counts, self.product, self.before = counts, product, before
        self.held, self.sib_out, self.sib_in, self.from_x, self.from_y = refs[:5]
        self.sib_sems, self.x_sems, self.y_sems = refs[5:7], refs[7:9], refs[9:11]
        self.sib, self.xdev, self.ydev = here.device(0, 1), here.device(1, 0), here.device(2, 0)
        self.steps = 4 * counts
        self.ring = self.sib_out.shape[0]

    def streams(self, stage):
        far = stage // 3
        x_chip = jnp.where(stage == 0, 3, jnp.where(stage == 2, 0, 1))
        y_chip = jnp.where(stage == 0, 3, jnp.where(stage == 2, 0, 2))
        return (x_chip, far), (y_chip, 1 - far)

    def to_sib(self, step, stream):
        stage, at = step // self.counts, step % self.counts
        return remote(self.sib_out.at[step % self.ring, stream], self.sib_in.at[stage, stream, at],
                      self.sib_sems[0].at[stage, stream, at], self.sib_sems[1].at[stage, stream, at], self.sib)

    def to_x(self, hop, at, stage=0):
        return remote(self.held.at[stage, 0, at], self.from_x.at[hop, at], self.x_sems[0].at[hop, at],
                      self.x_sems[1].at[hop, at], self.xdev)

    def to_y(self, hop, at, stage=0):
        return remote(self.held.at[stage, 1, at], self.from_y.at[hop, at], self.y_sems[0].at[hop, at],
                      self.y_sems[1].at[hop, at], self.ydev)

    def compute(self, step):
        stage, at = step // self.counts, step % self.counts
        if self.before:
            for stop in range(3):
                @pl.when(step == stop * self.counts)
                def _():
                    self.before(stop)

        @pl.when(step >= self.ring)
        def _():
            for stream in range(2):
                self.to_sib(step - self.ring, stream).wait_send()

        for stream, (across, half) in enumerate(self.streams(stage)):
            self.sib_out[step % self.ring, stream] = self.product(across, 1, half, at).astype(jnp.bfloat16)
            self.held[stage, stream, at] = self.product(across, 0, half, at).astype(jnp.bfloat16)
        for stream in range(2):
            self.to_sib(step, stream).start()

    def finish(self, step):
        stage, at = step // self.counts, step % self.counts
        for stream in range(2):
            self.to_sib(step, stream).wait_recv()

        def total(stream):
            return self.held[stage, stream, at].astype(jnp.float32) + self.sib_in[stage, stream, at].astype(
                jnp.float32)

        @pl.when(stage < 3)
        def _():
            for stream in range(2):
                self.held[stage, stream, at] = total(stream).astype(jnp.bfloat16)

        @pl.when(stage == 3)
        def _():
            self.to_y(0, at).wait_recv()
            self.held[3, 0, at] = (total(0) + self.from_y[0, at].astype(jnp.float32)).astype(jnp.bfloat16)
            self.to_x(0, at).wait_recv()
            self.held[3, 1, at] = (total(1) + self.from_x[0, at].astype(jnp.float32)).astype(jnp.bfloat16)

        @pl.when(stage != 2)
        def _():
            hop = stage - stage // 3
            self.to_x(hop, at, stage).start()
            self.to_y(hop, at, stage).start()

    def advance(self, step):
        @pl.when(step < self.steps)
        def _():
            self.compute(step)

        @pl.when(jnp.logical_and(step > 0, step <= self.steps))
        def _():
            self.finish(step - 1)

    def run(self, hook=None):
        def body(step, _):
            self.advance(step)

            if hook:
                hook(step)
            return 0

        lax.fori_loop(0, self.steps + 1, body, 0)
        return self.steps + 1

    def end(self, emit):
        def last(at, _):
            values = []
            for half in range(2):
                xs, ys = (1, 2) if half == 0 else (2, 1)
                self.to_x(xs, at).wait_recv()
                self.to_y(ys, at).wait_recv()
                values.append(self.held[2, half, at].astype(jnp.float32) + self.from_x[xs, at].astype(jnp.float32)
                              + self.from_y[ys, at].astype(jnp.float32))
            emit(at, *values)
            for hop in range(3):
                self.to_x(hop, at).wait_send()
                self.to_y(hop, at).wait_send()
            return 0

        lax.fori_loop(0, self.counts, last, 0)

        def drain(at, _):
            for stream in range(2):
                self.to_sib(self.steps - self.ring + at, stream).wait_send()
            return 0

        lax.fori_loop(0, self.ring, drain, 0)


def reduce_scratch(counts, rows, width, ring=4):
    low, dma = jnp.bfloat16, pltpu.SemaphoreType.DMA
    block = pltpu.VMEM((4, 2, counts, rows, width), low)
    landed = pltpu.VMEM((3, counts, rows, width), low)
    sent = pltpu.VMEM((ring, 2, rows, width), low)
    return [block, sent, block, landed, landed] + [dma((4, 2, counts))] * 2 + [dma((3, counts))] * 4


class Spread:
    def __init__(self, here, counts, refs):
        self.counts = counts
        self.got = refs[0]
        self.x_sems, self.y_sems, self.sib_sems = refs[1:3], refs[3:5], refs[5:7]
        self.core = here.core
        self.sib, self.xdev, self.ydev = here.device(0, 1), here.device(1, 0), here.device(2, 0)

    def slot(self, across, half, at):
        return self.got.at[across, self.core, half, at]

    def x_copy(self, hop, at):
        half = jnp.minimum(hop, 1)
        src = self.slot(2 * (hop // 2), half, at)
        dst = self.slot(1 + 2 * (hop // 2), half, at)
        return remote(src, dst, self.x_sems[0].at[hop, at], self.x_sems[1].at[hop, at], self.xdev)

    def y_copy(self, hop, at):
        half = 1 - jnp.minimum(hop, 1)
        src = self.slot(hop // 2, half, at)
        dst = self.slot(2 + hop // 2, half, at)
        return remote(src, dst, self.y_sems[0].at[hop, at], self.y_sems[1].at[hop, at], self.ydev)

    def streams(self, stage):
        some, last, late = jnp.minimum(stage, 1), stage // 3, stage // 2
        return (some + 2 * last, late), (2 * some + last, 1 - late)

    def block(self, at):
        x_stream, y_stream = self.streams(at // 4)
        second = at // 2 % 2
        across = x_stream[0] + second * (y_stream[0] - x_stream[0])
        half = x_stream[1] + second * (y_stream[1] - x_stream[1])
        return across, at % 2, half

    def begin_rows(self):
        for hop in range(2):
            self.x_copy(hop, 0).start()
            self.y_copy(hop, 0).start()
        for stream in range(2):
            self.sib_copy(0, stream, 0).start()

    def receive_rows(self, step):
        stage = step // 4

        @pl.when(jnp.logical_and(step % 4 == 0, jnp.logical_and(stage > 0, stage < 4)))
        def _():
            self.x_copy(stage - 1, 0).wait_recv()
            self.sib_copy(stage, 0, 0).start()
            self.y_copy(stage - 1, 0).wait_recv()
            self.sib_copy(stage, 1, 0).start()

        @pl.when(step == 4)
        def _():
            self.x_copy(2, 0).start()
            self.y_copy(2, 0).start()

        for stream in range(2):
            @pl.when(jnp.logical_and(step % 4 == 2 * stream, step < 16))
            def _(stream=stream):
                self.sib_copy(stage, stream, 0).wait_recv()

    def sib_copy(self, stage, stream, at):
        across, half = self.streams(stage)[stream]
        slot = self.slot(across, half, at)
        spot = (stage, stream, at)
        return remote(slot, slot, self.sib_sems[0].at[spot], self.sib_sems[1].at[spot], self.sib)

    def begin(self):
        def first(at, _):
            self.x_copy(0, at).start()
            self.y_copy(0, at).start()
            return 0

        def own(at, _):
            self.sib_copy(0, 0, at).start()
            self.sib_copy(0, 1, at).start()
            return 0

        lax.fori_loop(0, self.counts, first, 0)
        lax.fori_loop(0, self.counts, own, 0)

    def run(self, blocks, hook=None, done=None):
        counts = self.counts

        def body(step, _):
            stage, at = step // counts, step % counts

            @pl.when(jnp.logical_and(stage > 0, stage < 4))
            def _():
                self.x_copy(stage - 1, at).wait_recv()
                self.sib_copy(stage, 0, at).start()
                self.y_copy(stage - 1, at).wait_recv()
                self.sib_copy(stage, 1, at).start()

            @pl.when(jnp.logical_and(stage > 0, stage < 3))
            def _():
                self.x_copy(stage, at).start()
                self.y_copy(stage, at).start()

            @pl.when(step > 0)
            def _():
                old, spot = (step - 1) // counts, (step - 1) % counts
                for stream, (across, half) in enumerate(self.streams(old)):
                    self.sib_copy(old, stream, spot).wait_recv()
                    blocks(across, half, spot)
                if done:
                    done(old, spot)

            if hook:
                hook(step)
            return 0

        lax.fori_loop(0, 4 * counts + 1, body, 0)
        return 4 * counts + 1

    def end(self):
        def drain(at, _):
            for hop in range(3):
                self.x_copy(hop, at).wait_send()
                self.y_copy(hop, at).wait_send()
            for stage in range(4):
                self.sib_copy(stage, 0, at).wait_send()
                self.sib_copy(stage, 1, at).wait_send()
            return 0

        lax.fori_loop(0, self.counts, drain, 0)


def spread_scratch(counts, rows, width):
    dma = pltpu.SemaphoreType.DMA
    return [pltpu.VMEM((4, 2, 2, counts, rows, width), jnp.bfloat16)] + [dma((3, counts))] * 4 + [
        dma((4, 2, counts))] * 2


def row_span(here, across, other, rows):
    return pl.ds(pl.multiple_of(here.shard(across, other) * rows, rows), rows)


def dot_nt(left, right):
    return lax.dot_general(left, right, (((1,), (1,)), ((), ())), preferred_element_type=jnp.float32)


def dot_tn(left, right):
    return lax.dot_general(left, right, (((0,), (0,)), ((), ())), preferred_element_type=jnp.float32)


def dot_nn(left, right):
    return jnp.dot(left, right, preferred_element_type=jnp.float32)


def products(here, act, weight, nt, rows, width, counts):
    def product(across, other, half, at):
        cols = pl.ds(pl.multiple_of((half * counts + at) * width, width), width)
        block = act[row_span(here, across, other, rows), :]
        return dot_nt(block, weight[cols, :]) if nt else dot_nn(block, weight[:, cols])

    return product


def diagonal():
    return (lax.broadcasted_iota(jnp.int32, (LANES, LANES), 0) ==
            lax.broadcasted_iota(jnp.int32, (LANES, LANES), 1)).astype(jnp.float32)


def to_tile(tile, first, column, eye):
    for at in range(column.shape[0] // LANES):
        spread = column[at * LANES : (at + 1) * LANES, :] * eye
        tile[first + at : first + at + 1, :] = jnp.sum(spread, axis=0, keepdims=True)


def from_tile(row, eye):
    return jnp.sum(eye * row, axis=1, keepdims=True)


def make_tables(here, rows, segs, cos, sin, mask):
    eye = diagonal()
    tiles = rows // LANES
    freqs = jnp.exp(lax.broadcasted_iota(jnp.int32, (1, LANES), 1).astype(jnp.float32) * (-math.log(10000.0) / LANES))
    lane = lax.broadcasted_iota(jnp.int32, (1, LANES), 1)
    line = lax.broadcasted_iota(jnp.int32, (LANES, 1), 0)

    def row_of(side, at):
        return ((here.seq + side) % 2) * tiles + at

    for side in range(2):
        for at in range(tiles):
            row = row_of(side, at)
            ids = from_tile(segs[pl.ds(row, 1), :], eye)
            before = jnp.zeros((LANES, 1), jnp.float32)
            for other in range(2 * tiles):
                smaller = segs[other : other + 1, :] < ids
                before += jnp.sum(smaller.astype(jnp.float32), axis=-1, keepdims=True)
            index = row * LANES + line
            angles = (index.astype(jnp.float32) - before) * freqs
            span = slice(at * LANES, (at + 1) * LANES)
            cos[side, span, :] = jnp.cos(angles)
            sin[side, span, :] = jnp.sin(angles)
            if side == 0:
                for key_side in range(2):
                    for key_at in range(tiles):
                        key_row = row_of(key_side, key_at)
                        same = segs[pl.ds(key_row, 1), :] == ids
                        allowed = jnp.logical_and(same, key_row * LANES + lane <= index)
                        first = key_side * rows + key_at * LANES
                        mask[span, first : first + LANES] = allowed.astype(jnp.float32)


def open_kernel(rows, width, counts, tokens, gain, w_query, kv_weight, segs, qkv, x_low, act_t, w_qkv, rms, cos, sin,
                mask, *refs):
    here = Place()
    cols = gain.shape[1]
    act, turn_send, turn_recv, local_sems = refs[:4]
    me = here.shard(0, 0)
    own_rows = pl.ds(pl.multiple_of(me * rows, rows), rows)

    def turn_copy(at):
        across, other = turned(at)
        first = pl.multiple_of(here.shard(across, other) * cols, cols)
        return remote(tokens.at[:, pl.ds(first, cols)], x_low.at[own_rows, :], turn_send.at[at], turn_recv.at[at],
                      here.device(across, other))

    wide = w_query.shape[1]
    local = [
        pltpu.make_async_copy(w_query, w_qkv.at[:, :wide], local_sems.at[0]),
        pltpu.make_async_copy(kv_weight, w_qkv.at[:, wide:], local_sems.at[1]),
        pltpu.make_async_copy(tokens.at[:, pl.ds(pl.multiple_of(me * cols, cols), cols)], x_low.at[own_rows, :],
                              local_sems.at[2]),
    ]
    for copy in local:
        copy.start()
    greet(here, slice_peers(here))
    for at in range(7):
        turn_copy(at).start()
    for copy in local:
        copy.wait()

    def squares(at, total):
        values = tokens[:, pl.ds(pl.multiple_of(at * cols, cols), cols)].astype(jnp.float32)
        return total + jnp.sum(values * values, axis=-1, keepdims=True)

    total = lax.fori_loop(0, 8, squares, jnp.zeros((rows, 1), jnp.float32))
    rms[...] = jnp.broadcast_to(lax.rsqrt(total / (8 * cols) + EPS), rms.shape)
    make_tables(here, rows, segs, cos, sin, mask)

    def prepare(first, count):
        def one(step, _):
            at = first + step
            span = row_span(here, *turned(at), rows)
            value = (x_low[span, :].astype(jnp.float32) * gain[0:1, :]).astype(act.dtype)
            act[span, :] = value
            return 0

        lax.fori_loop(0, count, one, 0)

    def before(stop):
        first, count = ((0, 2), (2, 4), (6, 2))[stop]
        for at in range(first, min(first + count, 7)):
            turn_copy(at).wait_recv()
        prepare(first, count)

    def flip():
        def one(shard, _):
            span = pl.ds(pl.multiple_of(shard * rows, rows), rows)
            act_t[:, span] = act[span, :].T
            return 0

        lax.fori_loop(0, 8, one, 0)

    product = products(here, act, w_qkv, False, rows, width, counts)
    total = Reduce(here, counts, product, refs[4:15], before)
    total.run()
    flip()

    def emit(at, first, second):
        for half, value in enumerate((first, second)):
            qkv[:, pl.ds(pl.multiple_of((half * counts + at) * width, width), width)] = value

    total.end(emit)
    for at in range(7):
        turn_copy(at).wait_send()


def opening(tokens, gain, w_query, kv_weight, segs, cid, width=256):
    rows = tokens.shape[0]
    cols, wide = w_query.shape
    every = wide + kv_weight.shape[1]
    counts = every // (2 * width)
    low, f32 = jnp.bfloat16, jnp.float32
    dma = pltpu.SemaphoreType.DMA
    vm = pl.BlockSpec(memory_space=pltpu.VMEM)
    hbm = pl.BlockSpec(memory_space=pl.ANY)
    out_shape = [
        jax.ShapeDtypeStruct((rows, every), f32),
        jax.ShapeDtypeStruct((8 * rows, cols), low),
        jax.ShapeDtypeStruct((cols, 8 * rows), low),
        jax.ShapeDtypeStruct((cols, every), low),
        jax.ShapeDtypeStruct((rows, LANES), f32),
        jax.ShapeDtypeStruct((2, rows, LANES), f32),
        jax.ShapeDtypeStruct((2, rows, LANES), f32),
        jax.ShapeDtypeStruct((rows, 2 * rows), f32),
    ]
    scratch = [pltpu.VMEM((8 * rows, cols), low), dma((7,)), dma((7,)), dma((3,))]
    scratch += reduce_scratch(counts, rows, width)
    kernel = functools.partial(open_kernel, rows, width, counts)
    return kernel_call(kernel, out_shape, [tokens, gain, w_query, kv_weight, segs],
                       [vm, vm, hbm, hbm, vm], scratch, cid, "open")


def ffn_kernel(rows, width, counts, x_low, attn, gain, w_gate, w_up, d_hidden, hidden, d_gate, d_up, act_t, tile_out,
               *refs, late):
    here = Place()
    cols = gain.shape[1]
    act, weight, tiny_own, tiny_all, tiny_send, tiny_recv, dots, local_sems = refs[:8]
    tiny = Tiny(here, tiny_own, tiny_all, (tiny_send, tiny_recv), True)
    half_cols = counts * width
    local = [
        pltpu.make_async_copy(w_gate, weight.at[:, :half_cols], local_sems.at[0]),
        pltpu.make_async_copy(w_up, weight.at[:, half_cols:], local_sems.at[1]),
    ]
    for copy in local:
        copy.start()
    eye = diagonal()
    tiny_own[...] = jnp.zeros_like(tiny_own)

    def prepare(shard, _):
        for at in range(rows // LANES):
            span = pl.ds(pl.multiple_of(shard * rows + at * LANES, LANES), LANES)
            resid = x_low[span, :].astype(jnp.float32) + attn[span, :].astype(jnp.float32)
            act[span, :] = (resid * gain[0:1, :]).astype(act.dtype)
            square = jnp.sum(resid * resid, axis=-1, keepdims=True)
            tiny_own[shard, at : at + 1, :] = jnp.sum(square * eye, axis=0, keepdims=True)
        return 0

    lax.fori_loop(0, 8, prepare, 0)
    greet(here, slice_peers(here))
    tiny.begin()
    for copy in local:
        copy.wait()
    product = products(here, act, weight, False, rows, width, counts)
    total = Reduce(here, counts, product, refs[8:19])
    total.run()

    def flip(shard, _):
        span = pl.ds(pl.multiple_of(shard * rows, rows), rows)
        act_t[:, span] = act[span, :].T
        return 0

    lax.fori_loop(0, 8, flip, 0)
    tiny.end()
    tiles = rows // LANES
    mean = [from_tile(jnp.sum(tiny_all[:, at, :], axis=0, keepdims=True), eye) for at in range(tiles)]
    scale = lax.rsqrt(jnp.concatenate(mean, axis=0) / (8 * cols) + EPS)
    dots[...] = jnp.zeros_like(dots)
    late[0].wait()
    coeff = math.sqrt(2.0 / math.pi)

    def emit(at, first, second):
        span = pl.ds(pl.multiple_of(at * width, width), width)
        gate, up = first * scale, second * scale
        inner = jnp.tanh(coeff * (gate + 0.044715 * (gate * gate * gate)))
        gelu = 0.5 * gate * (1.0 + inner)
        slope = 0.5 * (1.0 + inner) + 0.5 * gate * (1.0 - inner * inner) * (
            coeff * (1.0 + 3.0 * 0.044715 * gate * gate))
        cot = d_hidden[:, span]
        hidden[:, span] = (gelu * up).astype(hidden.dtype)
        back_gate, back_up = cot * up * slope, cot * gelu
        d_gate[:, span] = (back_gate * scale).astype(d_gate.dtype)
        d_up[:, span] = (back_up * scale).astype(d_up.dtype)
        dots[...] += jnp.sum(back_gate * gate + back_up * up, axis=-1, keepdims=True)

    total.end(emit)
    tile_out[...] = jnp.zeros_like(tile_out)
    to_tile(tile_out, 0, dots[...] * (scale * scale * (1.0 / (8 * cols))), eye)


def ffn_scatter(x_low, attn, gain, w_gate, w_up, d_hidden, cid, width=512):
    rows, half = d_hidden.shape
    cols = gain.shape[1]
    counts = half // width
    low, f32 = jnp.bfloat16, jnp.float32
    dma = pltpu.SemaphoreType.DMA
    vm = pl.BlockSpec(memory_space=pltpu.VMEM)
    hbm = pl.BlockSpec(memory_space=pl.ANY)
    out_shape = [jax.ShapeDtypeStruct((rows, half), low)] * 3 + [
        jax.ShapeDtypeStruct((cols, 8 * rows), low),
        jax.ShapeDtypeStruct((8, LANES), f32),
    ]
    scratch = [
        pltpu.VMEM((8 * rows, cols), low),
        pltpu.VMEM((cols, 2 * half), low),
        pltpu.VMEM((8, 8, LANES), f32),
        pltpu.VMEM((8, 8, LANES), f32),
        dma((7,)), dma((7,)),
        pltpu.VMEM((rows, 1), f32),
        dma((2,)),
    ] + reduce_scratch(counts, rows, width)
    kernel = functools.partial(ffn_kernel, rows, width, counts)
    return kernel_call(kernel, out_shape, [x_low, attn, gain, w_gate, w_up, d_hidden], [vm, vm, vm, hbm, hbm, vm],
                       scratch, cid, "ffn", late=(5,))


def load_own(spread, payload, width, counts, sems):
    copies = []
    for half in range(2):
        for at in range(counts):
            first = at * width + (half * counts * width if len(payload) == 1 else 0)
            src = payload[half % len(payload)].at[:, first : first + width]
            copies.append(pltpu.make_async_copy(src, spread.slot(0, half, at), sems.at[half, at]))
    return copies


def chip_place(here, per):
    def place(at):
        return here.shard(at // (2 * per), at // per % 2) * per + at % per

    return place


def back_kernel(rows, width, counts, act_t, w_gate, w_up, d_gate, d_up, dots, x_low, attn, gain, d_norm, gain_grad,
                grad_gate, grad_up, *refs, late):
    here = Place()
    spread = Spread(here, counts, refs[:7])
    tiny_all, tiny_send, tiny_recv, own_sems, weight, sums, grads, staged, local_sems, out_sems = refs[7:17]
    contrib, rest, rest_sems = refs[17:20]
    line = Line(here, 4, [contrib, d_norm] + list(refs[20:]), chip_place(here, 2))
    tiny = Tiny(here, dots, tiny_all, (tiny_send, tiny_recv), False)
    half_cols = counts * width
    local = [
        pltpu.make_async_copy(w_gate, weight.at[:, :half_cols], local_sems.at[0]),
        pltpu.make_async_copy(w_up, weight.at[:, half_cols:], local_sems.at[1]),
    ]
    own = load_own(spread, (d_gate, d_up), width, counts, own_sems)
    for copy in own + local:
        copy.start()
    greet(here, tiny.peers, True)
    for copy in own:
        copy.wait()
    tiny.begin()
    spread.begin()
    sums[...] = jnp.zeros_like(sums)
    for copy in local + late:
        copy.wait()

    def columns(half, at):
        return pl.ds(pl.multiple_of((half * counts + at) * width, width), width)

    def clear(at, _):
        grads[:, columns(0, at)] = jnp.zeros((grads.shape[0], width), jnp.float32)
        return 0

    lax.fori_loop(0, 2 * counts, clear, 0)

    def blocks(across, half, at):
        cols = columns(half, at)
        gained = grads[:, cols]
        for other in range(2):
            row = row_span(here, across, other, rows)
            block = spread.got[across, (spread.core + other) % 2, half, at]
            sums[row, :] += dot_nt(block, weight[:, cols])
            gained = gained + dot_nn(act_t[:, row], block)
        grads[:, cols] = gained

    def leave(half, at):
        spot = pl.ds(pl.multiple_of(at * width, width), width)
        return pltpu.make_async_copy(staged.at[half], (grad_gate, grad_up)[half].at[:, spot],
                                     out_sems.at[half, at])

    eye = diagonal()
    gain_grad[...] = jnp.zeros_like(gain_grad)

    def close_chip(chip, target):
        def close_shard(other, _):
            shard = here.shard(chip, other)
            span = pl.ds(pl.multiple_of(shard * rows, rows), rows)
            loads = [pltpu.make_async_copy(src.at[span, :], rest.at[at], rest_sems.at[at])
                     for at, src in enumerate((x_low, attn))]
            for copy in loads:
                copy.start()
            for copy in loads:
                copy.wait()
            for at in range(rows // LANES):
                span = pl.ds(pl.multiple_of(shard * rows + at * LANES, LANES), LANES)
                piece = slice(at * LANES, (at + 1) * LANES)
                dot = from_tile(tiny_all[shard, at : at + 1, :], eye)
                resid = rest[0, piece, :].astype(jnp.float32) + rest[1, piece, :].astype(jnp.float32)
                value = sums[span, :]
                target[span, :] = (value * gain[0:1, :] - resid * dot).astype(target.dtype)
                gain_grad[...] += jnp.sum(value * resid, axis=0, keepdims=True)
            return 0

        lax.fori_loop(0, 2, close_shard, 0)

    def done(stage, at):
        @pl.when(jnp.logical_and(stage == 3, at > 0))
        def _():
            leave(0, at - 1).wait()
            leave(1, at - 1).wait()

        @pl.when(stage == 3)
        def _():
            for half in range(2):
                staged[half] = grads[:, columns(half, at)].astype(staged.dtype)
            leave(0, at).start()
            leave(1, at).start()

        @pl.when(jnp.logical_and(at == counts - 1, stage == 0))
        def _():
            close_chip(0, contrib)
            line.launch(0, 4)

        @pl.when(jnp.logical_and(at == counts - 1, stage == 2))
        def _():
            lax.fori_loop(1, 3, lambda chip, _: (close_chip(chip, d_norm), 0)[1], 0)

    def hook(step):
        @pl.when(jnp.logical_and(step >= counts, step < counts + 6))
        def _():
            line.step(step - counts)

    tiny.end()
    spread.run(blocks, hook, done)
    close_chip(3, d_norm)
    line.settle()
    spread.end()

    def drain(at, _):
        leave(0, at).wait()
        leave(1, at).wait()
        return 0

    lax.fori_loop(counts - 1, counts, drain, 0)


def back_gather(act_t, w_gate, w_up, d_gate, d_up, dots, x_low, attn, gain, cid, width=512):
    cols, total = act_t.shape
    rows, half = d_gate.shape
    counts = half // width
    low, f32 = jnp.bfloat16, jnp.float32
    dma = pltpu.SemaphoreType.DMA
    vm = pl.BlockSpec(memory_space=pltpu.VMEM)
    hbm = pl.BlockSpec(memory_space=pl.ANY)
    out_shape = [
        jax.ShapeDtypeStruct((total, cols), low),
        jax.ShapeDtypeStruct((1, cols), f32),
        jax.ShapeDtypeStruct((cols, half), low),
        jax.ShapeDtypeStruct((cols, half), low),
    ]
    scratch = spread_scratch(counts, rows, width) + [
        pltpu.VMEM((8, 8, LANES), f32), dma((7,)), dma((7,)), dma((2, counts)),
        pltpu.VMEM((cols, 2 * half), low),
        pltpu.VMEM((total, cols), f32),
        pltpu.VMEM((cols, 2 * half), f32),
        pltpu.VMEM((2, cols, width), low),
        dma((2,)), dma((2, counts)),
        pltpu.VMEM((total, cols), low),
        pltpu.VMEM((2, rows, cols), low),
        dma((2,)),
    ] + line_scratch(4, (4 * rows // 2, cols), low)
    operands = [act_t, w_gate, w_up, d_gate, d_up, dots, x_low, attn, gain]
    kernel = functools.partial(back_kernel, rows, width, counts)
    return kernel_call(kernel, out_shape, operands, [vm] + [hbm] * 4 + [vm, hbm, hbm, vm], scratch, cid, "back",
                       [vm, vm, hbm, hbm], (0,))


def down_kernel(rows, width, counts, cot, weight, hidden, d_norm, ffn, d_attn, grad, *refs, late):
    here = Place()
    spread = Spread(here, counts, refs[:7])
    own_sems, sums, grads, staged, out_sems, norm_out = refs[7:13]
    place = chip_place(here, 4)
    norm_line = Line(here, 24, [d_norm, norm_out] + list(refs[13:]), lambda at: place(at + 8))
    own = load_own(spread, (hidden,), width, counts, own_sems)
    for copy in own:
        copy.start()
    greet(here, slice_peers(here), True)
    norm_line.begin()
    for copy in own:
        copy.wait()
    spread.begin()
    sums[...] = jnp.zeros_like(sums)
    grads[...] = jnp.zeros_like(grads)
    for copy in late:
        copy.wait()

    def columns(half, at):
        return pl.ds(pl.multiple_of((half * counts + at) * width, width), width)

    def blocks(across, half, at):
        cols = columns(half, at)
        gained = grads[cols, :]
        for other in range(2):
            row = row_span(here, across, other, rows)
            block = spread.got[across, (spread.core + other) % 2, half, at]
            sums[row, :] += dot_nn(block, weight[cols, :])
            gained = gained + dot_tn(block, cot[row, :])
        grads[cols, :] = gained

    def leave(half, at):
        return pltpu.make_async_copy(staged.at[at % 2, half], grad.at[columns(half, at), :], out_sems.at[half, at])

    def done(stage, at):
        @pl.when(jnp.logical_and(stage == 3, at > 1))
        def _():
            leave(0, at - 2).wait()
            leave(1, at - 2).wait()

        @pl.when(stage == 3)
        def _():
            for half in range(2):
                staged[at % 2, half] = grads[columns(half, at), :].astype(staged.dtype)
            leave(0, at).start()
            leave(1, at).start()

    norm_line.steps(spread.run(blocks, norm_line.step, done), 26)
    ffn[...] = sums[...].astype(ffn.dtype)
    norm_line.settle()

    def add_norm(at, _):
        def add(source):
            span = row_span(here, at // 2, at % 2, rows)
            d_attn[span, :] = (cot[span, :].astype(jnp.float32) + source[span, :].astype(jnp.float32)).astype(
                d_attn.dtype)

        @pl.when(at < 2)
        def _():
            add(d_norm)

        @pl.when(at >= 2)
        def _():
            add(norm_out)
        return 0

    lax.fori_loop(0, 8, add_norm, 0)
    spread.end()

    def drain(at, _):
        leave(0, at).wait()
        leave(1, at).wait()
        return 0

    lax.fori_loop(counts - 2, counts, drain, 0)


def down_gather(cot, weight, hidden, d_norm, cid, width=256):
    total, cols = cot.shape
    rows, every = hidden.shape
    counts = every // (2 * width)
    low, f32 = jnp.bfloat16, jnp.float32
    dma = pltpu.SemaphoreType.DMA
    vm = pl.BlockSpec(memory_space=pltpu.VMEM)
    hbm = pl.BlockSpec(memory_space=pl.ANY)
    out_shape = [
        jax.ShapeDtypeStruct((total, cols), low),
        jax.ShapeDtypeStruct((total, cols), low),
        jax.ShapeDtypeStruct(weight.shape, low),
    ]
    scratch = spread_scratch(counts, rows, width) + [
        dma((2, counts)),
        pltpu.VMEM((total, cols), f32),
        pltpu.VMEM(weight.shape, f32),
        pltpu.VMEM((2, 2, width, cols), low),
        dma((2, counts)),
        pltpu.VMEM((total, cols), low),
    ] + line_scratch(24, (24 * rows // 4, cols), low)
    kernel = functools.partial(down_kernel, rows, width, counts)
    return kernel_call(kernel, out_shape, [cot, weight, hidden, d_norm], [vm, vm, hbm, vm], scratch, cid, "down",
                       [vm, vm, hbm], (0, 1))


def attend_kernel(rows, heads, cols, width, counts, qkv, rms, cos, sin, mask, w_out, cot, w_down, attn, mixed_all, g_col,
                  kv, probs, queries, pair_rms, d_hidden, *refs, late):
    here = Place()
    spread = Spread(here, 1, refs[:7])
    part, pair_sems, turn_send, turn_recv, local_sem, tiny_own, tiny_pair, mixed_sems = refs[7:15]
    product = products(here, g_col, w_down, True, rows, width, counts)
    total = Reduce(here, counts, product, refs[15:26])
    piece = rows // 2

    def place(at):
        across, other, half_at = spread.block(at)
        return here.shard(across, other) * 2 + half_at

    line = Line(here, 16, [part, attn] + list(refs[26:]), place)
    got, core = spread.got, here.core
    greet(here, slice_peers(here), True)
    me = here.shard(0, 0)

    def turn_copy(at):
        across, other = turned(at)
        first = pl.multiple_of(here.shard(across, other) * cols, cols)
        return remote(cot.at[:, pl.ds(first, cols)], g_col.at[pl.ds(pl.multiple_of(me * rows, rows), rows), :],
                      turn_send.at[at], turn_recv.at[at], here.device(across, other))

    own_turn = pltpu.make_async_copy(cot.at[:, pl.ds(pl.multiple_of(me * cols, cols), cols)],
                                     g_col.at[pl.ds(pl.multiple_of(me * rows, rows), rows), :], local_sem)
    own_turn.start()
    half = HD // 2
    scale = 1.0 / math.sqrt(HD)
    wide = heads * HD

    def rotated(first):
        lead = qkv[:, first : first + half] * rms[...]
        trail = qkv[:, first + half : first + HD] * rms[...]
        return lead * cos[0] - trail * sin[0], trail * cos[0] + lead * sin[0]

    low_k, high_k = rotated(wide)
    kv[0, :, :half] = low_k.astype(kv.dtype)
    kv[0, :, half:HD] = high_k.astype(kv.dtype)
    for at in range(2):
        first = HD + at * half
        kv[0, :, first : first + half] = (qkv[:, wide + first : wide + first + half] * rms[...]).astype(kv.dtype)
    eye = diagonal()
    tiny_own[...] = jnp.zeros_like(tiny_own)
    to_tile(tiny_own, 0, rms[:, :1], eye)
    pair_rms[0] = rms[...]
    pair = remote(kv.at[0], kv.at[1], pair_sems.at[0], pair_sems.at[1], spread.ydev)
    tiny = remote(tiny_own, tiny_pair, pair_sems.at[2], pair_sems.at[3], spread.ydev)
    for head in range(heads):
        if head == 1:
            pair.start()
            tiny.start()
            turn_copy(2 * (3 - 1)).start()
            turn_copy(2 * (3 - 1) + 1).start()
        lead, trail = rotated(head * HD)
        queries[:, head * HD : head * HD + half] = (lead * scale).astype(queries.dtype)
        queries[:, head * HD + half : (head + 1) * HD] = (trail * scale).astype(queries.dtype)
    pair.wait()
    for copy in late:
        copy.wait()
    for at in range(7):
        if at // 2 != 2:
            turn_copy(at).start()

    def one_head(head, _):
        query = queries[:, pl.ds(pl.multiple_of(head * HD, HD), HD)]
        scores = jnp.concatenate([dot_nt(query, kv[0, :, :HD]), dot_nt(query, kv[1, :, :HD])], axis=1)
        scores = jnp.where(mask[...] > 0, scores, NEG)
        expd = jnp.exp(scores - jnp.max(scores, axis=-1, keepdims=True))
        prob = expd / jnp.sum(expd, axis=-1, keepdims=True)
        probs[head] = prob
        prob_low = prob.astype(jnp.bfloat16)
        mixed = dot_nn(prob_low[:, :rows], kv[0, :, HD:]) + dot_nn(prob_low[:, rows:], kv[1, :, HD:])
        span = pl.ds(pl.multiple_of(head * HD, HD), HD)
        for half_at in range(2):
            low_mixed = mixed[half_at * piece : (half_at + 1) * piece, :].astype(got.dtype)
            got[0, core, half_at, 0, :, span] = low_mixed
        return 0

    lax.fori_loop(0, heads, one_head, 0)
    spread.begin_rows()

    def mixed_copy(at):
        across, other, half_at = spread.block(at)
        span = pl.ds(pl.multiple_of(place(at) * piece, piece), piece)
        return pltpu.make_async_copy(got.at[across, (core + other) % 2, half_at, 0], mixed_all.at[span, :],
                                     mixed_sems.at[at])

    def one_step(step, _):
        spread.receive_rows(step)

        @pl.when(step < 16)
        def _():
            across, other, half_at = spread.block(step)
            value = dot_nn(got[across, (core + other) % 2, half_at, 0], w_out[...])
            part[pl.ds(pl.multiple_of(place(step) * piece, piece), piece), :] = value.astype(part.dtype)
            mixed_copy(step).start()
            line.launch(step, 1)

        @pl.when(step == 4)
        def _():
            own_turn.wait()
            for at in range(7):
                turn_copy(at).wait_recv()

        @pl.when(step >= 4)
        def _():
            total.advance(step - 4)
            line.step(step - 4)
        return 0

    lax.fori_loop(0, 4 + max(16, total.steps + 1), one_step, 0)
    line.end(max(16, total.steps + 1))

    def emit(at, first, second):
        for half_at, value in enumerate((first, second)):
            d_hidden[:, pl.ds(pl.multiple_of((half_at * counts + at) * width, width), width)] = value

    total.end(emit)
    for hop in range(3):
        spread.x_copy(hop, 0).wait_send()
        spread.y_copy(hop, 0).wait_send()
    for stage in range(4):
        for stream in range(2):
            spread.sib_copy(stage, stream, 0).wait_send()
    for at in range(16):
        mixed_copy(at).wait()
    tiny.wait()
    for at in range(rows // LANES):
        values = jnp.broadcast_to(from_tile(tiny_pair[at : at + 1, :], eye), (LANES, LANES))
        pair_rms[1, at * LANES : (at + 1) * LANES, :] = values
    for at in range(7):
        turn_copy(at).wait_send()


def attend(qkv, rms, cos, sin, mask, w_out, cot, w_down, cid, width=512):
    rows = qkv.shape[0]
    wide, cols = w_out.shape
    heads = wide // HD
    counts = w_down.shape[0] // (2 * width)
    low, f32 = jnp.bfloat16, jnp.float32
    dma = pltpu.SemaphoreType.DMA
    vm = pl.BlockSpec(memory_space=pltpu.VMEM)
    out_shape = [
        jax.ShapeDtypeStruct((8 * rows, cols), low),
        jax.ShapeDtypeStruct((8 * rows, wide), low),
        jax.ShapeDtypeStruct((8 * rows, cols), low),
        jax.ShapeDtypeStruct((2, rows, 2 * HD), low),
        jax.ShapeDtypeStruct((heads, rows, 2 * rows), f32),
        jax.ShapeDtypeStruct((rows, wide), low),
        jax.ShapeDtypeStruct((2,) + rms.shape, f32),
        jax.ShapeDtypeStruct((rows, w_down.shape[0]), f32),
    ]
    scratch = spread_scratch(1, rows // 2, wide) + [
        pltpu.VMEM((8 * rows, cols), low), dma((4,)), dma((7,)), dma((7,)), dma(()),
        pltpu.VMEM((8, LANES), f32), pltpu.VMEM((8, LANES), f32), dma((16,)),
    ] + reduce_scratch(counts, rows, width) + line_scratch(16, (8 * rows, cols), low)
    kernel = functools.partial(attend_kernel, rows, heads, cols, width, counts)
    operands = [qkv, rms, cos, sin, mask, w_out, cot, w_down]
    out_specs = [vm, pl.BlockSpec(memory_space=pl.ANY)] + [vm] * 6
    return kernel_call(kernel, out_shape, operands, [vm] * 8, scratch, cid, "attend", out_specs, (4, 5, 7))


def tail_kernel(rows, heads, per, d_attn, w_out, queries, kv, probs, rms, cos, sin, act_t, w_qkv, ffn, x_low,
                attn, gain, gain_grad, mixed_all, d_tok, out, grad_query, grad_out, kv_sum, gain_tiles, *refs, late):
    here = Place()
    width = HD
    counts = heads // 2
    part = rows // 2
    refs = list(refs)
    line_counts = 8 * per
    cols = d_attn.shape[1]
    extra = cols // (rows // per)

    def take(count):
        taken_refs = refs[:count]
        del refs[:count]
        return taken_refs

    total_refs = take(11)
    spread = Spread(here, 1, take(7))
    d_mixed, tiny_own, tiny_all, d_kv, give, taken, give_sems, tiny_send, tiny_recv = take(9)
    grad, grad_mixed, gain_sum, tile, tile_send, tile_recv, put_sems, local_sems, mixed_two, mixed_sems = take(10)

    def far(at):
        return at // (2 * per), at // per % 2

    def near(at):
        return spread.block(jnp.minimum(at, line_counts - 1))

    def place_ffn(at):
        return here.shard(*far(at)) * per + at % per

    def place_tok(at):
        across, other, half_at = near(at)
        return jnp.where(at < line_counts, here.shard(across, other) * per + half_at, at)

    ffn_sum, leaving = take(2)
    by_chip = chip_place(here, per)
    line = Line(here, line_counts, [ffn, ffn_sum] + take(8), by_chip)
    contrib, summed = take(2)
    line_tok = Line(here, line_counts + extra, [contrib, summed] + take(8), place_tok)
    tiny = Tiny(here, tiny_own, tiny_all, (tiny_send, tiny_recv), False)
    got, core = spread.got, here.core
    product = products(here, d_attn, w_out, True, rows, width, counts)
    total = Reduce(here, counts, product, total_refs)
    greet(here, tiny.peers, True)
    line.begin()
    grad_mixed[...] = jnp.zeros_like(grad_mixed)

    def mixed_copy(step):
        span = pl.ds(pl.multiple_of(step * rows, rows), rows)
        return pltpu.make_async_copy(mixed_all.at[span, :], mixed_two.at[step % 2], mixed_sems.at[step % 2])

    mixed_copy(0).start()

    def beside(step):
        line.step(step)

        @pl.when(step < 8)
        def _():
            span = pl.ds(pl.multiple_of(step * rows, rows), rows)
            mixed_copy(step).wait()

            @pl.when(step < 7)
            def _():
                mixed_copy(step + 1).start()

            grad_mixed[...] += dot_tn(mixed_two[step % 2], d_attn[span, :])

    done = total.run(beside)
    grad_out[...] = grad_mixed[...].astype(grad_out.dtype)

    def land(at, first, second):
        for half_at, value in enumerate((first, second)):
            d_mixed[:, pl.ds(pl.multiple_of((half_at * counts + at) * width, width), width)] = value.astype(
                d_mixed.dtype)

    total.end(land)
    half = HD // 2
    scale = 1.0 / math.sqrt(HD)
    depth = w_qkv.shape[0] * 8
    d_kv[...] = jnp.zeros_like(d_kv)
    for copy in late:
        copy.wait()

    def one_head(head, dots):
        span = pl.ds(pl.multiple_of(head * HD, HD), HD)
        query = queries[:, span]
        cot = d_mixed[:, span]
        prob = probs[head]
        d_prob = jnp.concatenate([dot_nt(cot, kv[0, :, HD:]), dot_nt(cot, kv[1, :, HD:])], axis=1)
        delta = jnp.sum(prob * d_prob, axis=-1, keepdims=True)
        d_score = (prob * (d_prob - delta)).astype(jnp.bfloat16)
        prob_low = prob.astype(jnp.bfloat16)
        d_query = (dot_nn(d_score[:, :rows], kv[0, :, :HD]) + dot_nn(d_score[:, rows:], kv[1, :, :HD])) * scale
        for side in range(2):
            keys = slice(side * rows, (side + 1) * rows)
            d_kv[side, :, :HD] += dot_tn(d_score[:, keys], query)
            d_kv[side, :, HD:] += dot_tn(prob_low[:, keys], cot)
        dots = dots + jnp.sum(d_query * query.astype(jnp.float32), axis=-1, keepdims=True)
        lead, trail = d_query[:, :half], d_query[:, half:]
        first = ((lead * cos[0] + trail * sin[0]) * rms[0]).astype(got.dtype)
        second = ((trail * cos[0] - lead * sin[0]) * rms[0]).astype(got.dtype)
        line.step(done + head)
        for rows_at in range(2):
            piece = slice(rows_at * part, (rows_at + 1) * part)
            got[0, core, rows_at, 0, :, pl.ds(pl.multiple_of(head * HD, HD), half)] = first[piece, :]
            got[0, core, rows_at, 0, :, pl.ds(pl.multiple_of(head * HD + half, half), half)] = second[piece, :]

        return dots

    dots = lax.fori_loop(0, heads, one_head, jnp.zeros((rows, 1), jnp.float32))
    eye = diagonal()
    tiny_own[...] = jnp.zeros_like(tiny_own)
    for side in (1, 0):
        d_key, d_value = d_kv[side, :, :HD], d_kv[side, :, HD:]
        own = jnp.sum(d_key * kv[side, :, :HD].astype(jnp.float32) +
                      d_value * kv[side, :, HD:].astype(jnp.float32), axis=-1, keepdims=True)
        if side == 0:
            own = own + dots * (1.0 / scale)
        own = own * (rms[side] * rms[side] * (1.0 / depth))
        to_tile(tiny_own, side * (rows // LANES), own, eye)
        lead, trail = d_key[:, :half], d_key[:, half:]
        parts = [(lead * cos[side] + trail * sin[side]) * rms[side],
                 (trail * cos[side] - lead * sin[side]) * rms[side],
                 d_value[:, :half] * rms[side], d_value[:, half:] * rms[side]]
        for at, value in enumerate(parts):
            if side == 1:
                give[:, at * half : (at + 1) * half] = value.astype(give.dtype)
            else:
                d_kv[0, :, at * half : (at + 1) * half] = value
    given = remote(give, taken, give_sems.at[0], give_sems.at[1], spread.ydev)
    given.start()
    grad[...] = jnp.zeros_like(grad)
    given.wait()
    for rows_at in range(2):
        piece = slice(rows_at * part, (rows_at + 1) * part)
        value = d_kv[0, piece, :] + taken[piece, :].astype(jnp.float32)
        got[0, core, rows_at, 0, :, heads * HD :] = value.astype(got.dtype)
    tiny.begin()
    spread.begin_rows()
    gain_sum[...] = jnp.zeros_like(gain_sum)
    tiny.end()

    def block_of(at):
        across, other, half_at = near(at)
        shard, partner = here.shard(across, other), here.shard((across + 2) % 4, other)
        block = got[across, (core + other) % 2, half_at, 0]
        first = pl.multiple_of(shard * rows + half_at * part, part)
        for tile_at in range(part // LANES):
            row = pl.ds(pl.multiple_of(first + tile_at * LANES, LANES), LANES)
            low_at = half_at * (part // LANES) + tile_at
            kept = rows // LANES + low_at
            dot = from_tile(tiny_all[shard, pl.ds(low_at, 1), :] + tiny_all[partner, pl.ds(kept, 1), :], eye)
            value = dot_nt(block[tile_at * LANES : (tile_at + 1) * LANES, :], w_qkv[...])
            x_rows = x_low[row, :].astype(jnp.float32)
            contrib[row, :] = (value * gain[0:1, :] - x_rows * dot).astype(contrib.dtype)
            gain_sum[...] += jnp.sum(value * x_rows, axis=0, keepdims=True)
        line_tok.launch(at, 1)
        rows_t = act_t[:, pl.ds(first, part)]
        for at_col in range((heads + 2) * HD // 512):
            span = slice(at_col * 512, (at_col + 1) * 512)
            grad[:, span] += dot_nn(rows_t, block[:, span])

    me = here.shard(0, 0)
    columns = pl.ds(pl.multiple_of(me * cols, cols), cols)
    chunk = line.chunk

    def landing(which, at):
        sub = at % per if which == 0 else near(at)[2]
        return (out, d_tok)[which].at[pl.ds(pl.multiple_of(sub * chunk, chunk), chunk), columns]

    def leaver(which, at):
        return (leaving, line_tok.from_end)[which].at[at]

    def put(which, at):
        goal = here.device(*(far(at) if which == 0 else near(at)[:2]))
        return remote(leaver(which, at), landing(which, at), put_sems.at[which, 0, at], put_sems.at[which, 1, at],
                      goal)

    def keep(which, at):
        spot = at % per if which == 0 else near(at)[2]
        return pltpu.make_async_copy(leaver(which, at), landing(which, at), local_sems.at[which, spot])

    def emit(which, at):
        if which == 1:
            row = line_tok.rows(at)
            value = d_attn[row, :].astype(jnp.float32) + summed[row, :].astype(jnp.float32)
            line_tok.from_end[at] = value.astype(out.dtype)
            return
        row = pl.ds(pl.multiple_of(place_ffn(at) * chunk, chunk), chunk)

        def leave(source):
            value = x_low[row, :].astype(jnp.float32) + attn[row, :].astype(jnp.float32)
            leaving[at] = (value + source[row, :].astype(jnp.float32)).astype(out.dtype)

        leave(ffn_sum)

    def is_own(which, at):
        return at < per if which == 0 else jnp.logical_and(at < 4, at % 2 == 0)

    def send(which, at):
        own = is_own(which, at)

        @pl.when(own)
        def _():
            keep(which, at).start()

        @pl.when(jnp.logical_not(own))
        def _():
            put(which, at).start()

    def stage_step(step, _):
        spread.receive_rows(step)

        @pl.when(step < line_counts)
        def _():
            block_of(step)

        @pl.when(step < 5)
        def _():
            line.step(done + heads + step)

        @pl.when(step >= 4)
        def _():
            line_tok.step(step - 4)

        @pl.when(step > 0)
        def _():
            send(0, step - 1)

        @pl.when(line.inner == 0)
        def _():
            line.up(step).wait_send()
            line.down(step).wait_recv()

        emit(0, step)

        @pl.when(jnp.logical_and(line.inner == 1, step > 7))
        def _():
            send(1, step - 8)

        @pl.when(jnp.logical_and(line.inner == 1, step > 6))
        def _():
            emit(1, step - 7)
        return 0

    lax.fori_loop(0, line_counts, stage_step, 0)
    for half_at in range(cols // (rows // per)):
        span = pl.ds(line_counts * (rows // per) + half_at * (rows // per), rows // per)
        source = slice(half_at * (rows // per), (half_at + 1) * (rows // per))
        contrib[span, :] = grad[source, heads * HD :].astype(contrib.dtype)
    line_tok.launch(line_counts, extra)
    grad_query[...] = grad[:, : heads * HD].astype(grad_query.dtype)
    for at in range(cols // LANES):
        tile[at : at + 1, :] = gain_sum[:, at * LANES : (at + 1) * LANES]
        spot = cols // LANES + at
        tile[spot : spot + 1, :] = gain_grad[:, at * LANES : (at + 1) * LANES]

    def tile_copy(step):
        return remote(tile, gain_tiles.at[here.z], tile_send.at[step], tile_recv.at[step],
                      (here.dp, here.seq, (here.z + step + 1) % 4))

    send(0, line_counts - 1)
    line.drain()
    for step in range(3):
        tile_copy(step).start()
    gain_tiles[here.z] = tile[...]

    @pl.when(line.inner == 1)
    def _():
        start = line_counts - 4

        def both(at, _):
            line_tok.step(at)

            @pl.when(at < line_counts + 4)
            def _():
                send(1, at - 4)

            @pl.when(at < line_counts + 3)
            def _():
                emit(1, at - 3)
            return 0

        lax.fori_loop(start, line_counts + extra + 2, both, 0)

        def drain(at, _):
            line_tok.down(at).wait_send()
            return 0

        lax.fori_loop(0, line_counts + extra, drain, 0)

    @pl.when(line.inner == 0)
    def _():
        def arrive(at, _):
            line_tok.up(at).wait_send()
            line_tok.down(at).wait_recv()

            @pl.when(jnp.logical_and(at > 0, at <= line_counts))
            def _():
                send(1, at - 1)

            @pl.when(at < line_counts)
            def _():
                emit(1, at)
            return 0

        lax.fori_loop(0, line_counts + extra, arrive, 0)

    for half_at in range(extra):
        span = pl.ds((line_counts + half_at) * chunk, chunk)
        kv_sum[half_at * chunk : (half_at + 1) * chunk, :] = summed[span, :]
    for hop in range(3):
        spread.x_copy(hop, 0).wait_send()
        spread.y_copy(hop, 0).wait_send()
    for stage in range(4):
        spread.sib_copy(stage, 0, 0).wait_send()
        spread.sib_copy(stage, 1, 0).wait_send()

    def finish(at, _):
        for which in range(2):
            own = is_own(which, at)

            @pl.when(own)
            def _():
                keep(which, at).wait()

            @pl.when(jnp.logical_not(own))
            def _():
                put(which, at).wait()
        return 0

    lax.fori_loop(0, line_counts, finish, 0)
    for step in range(3):
        tile_copy(step).wait()


def tail(d_attn, w_out, queries, kv, probs, rms, cos, sin, act_t, w_qkv, ffn, x_low, attn, gain, gain_grad,
         mixed_all, cid,
 per=2):
    total, cols = d_attn.shape
    rows = total // 8
    wide = w_out.shape[0]
    heads = wide // HD
    low, f32 = jnp.bfloat16, jnp.float32
    dma = pltpu.SemaphoreType.DMA
    vm = pl.BlockSpec(memory_space=pltpu.VMEM)
    counts = 8 * per
    chunk = rows // per
    extra = cols // chunk
    long = (total + cols, cols)
    out_shape = [
        jax.ShapeDtypeStruct((rows, 8 * cols), low),
        jax.ShapeDtypeStruct((rows, 8 * cols), low),
        jax.ShapeDtypeStruct((cols, wide), low),
        jax.ShapeDtypeStruct(w_out.shape, low),
        jax.ShapeDtypeStruct((cols, 2 * HD), low),
        jax.ShapeDtypeStruct((4, 8, LANES), f32),
    ]
    scratch = reduce_scratch(heads // 2, rows, HD, 2) + spread_scratch(1, rows // 2, wide + 2 * HD)
    scratch += [
        pltpu.VMEM((rows, wide), low),
        pltpu.VMEM((8, LANES), f32),
        pltpu.VMEM((8, 8, LANES), f32),
        pltpu.VMEM((2, rows, 2 * HD), f32),
        pltpu.VMEM((rows, 2 * HD), low),
        pltpu.VMEM((rows, 2 * HD), low),
        dma((2,)), dma((7,)), dma((7,)),
        pltpu.VMEM(w_qkv.shape, f32),
        pltpu.VMEM(w_out.shape, f32),
        pltpu.VMEM((1, cols), f32),
        pltpu.VMEM((8, LANES), f32),
        dma((3,)), dma((3,)), dma((2, 2, counts)), dma((2, per)),
        pltpu.VMEM((2, rows, wide), low), dma((2,)),
        pltpu.VMEM((total, cols), low),
        pltpu.VMEM((counts, chunk, cols), low),
    ] + line_scratch(counts, (total, cols), low)
    scratch += [pltpu.VMEM(long, low), pltpu.VMEM(long, low)] + line_scratch(counts + extra, long, low)
    operands = [d_attn, w_out, queries, kv, probs, rms, cos, sin, act_t, w_qkv, ffn, x_low, attn, gain,
                gain_grad, mixed_all]
    kernel = functools.partial(tail_kernel, rows, heads, per)
    specs = [vm] * (len(operands) - 1) + [pl.BlockSpec(memory_space=pl.ANY)]
    return kernel_call(kernel, out_shape, operands, specs, scratch, cid, "tail",
                       late=(2, 3, 4, 8, 9, 11, 12))


LANES = 128


def acts_move(
    tokens, seg_ids, gain_attn, w_query, kv_weight, w_out, gain_ffn, w_gate, w_up, w_down, d_out
):
    rows = tokens.shape[0]
    segs = seg_ids.astype(jnp.float32).reshape(2 * rows // LANES, LANES)
    segs = jnp.pad(segs, ((0, 8 - 2 * rows // LANES), (0, 0)))
    both = jnp.stack([gain_attn, gain_ffn, gain_ffn, gain_attn]).astype(jnp.float32)
    gain_one, gain_two = both[:2], both[2:]
    wider = jnp.float32

    qkv, x_low, act_one_t, w_qkv, rms, cos, sin, mask = opening(
        tokens, gain_one, w_query, kv_weight, segs, 1
    )
    attn, mixed_all, g_low, kv, probs, queries, pair_rms, d_hidden = attend(
        qkv, rms, cos, sin, mask, w_out, d_out, w_down, 2
    )
    hidden, d_gate, d_up, act_two_t, dots = ffn_scatter(x_low, attn, gain_two, w_gate, w_up, d_hidden, 4)
    d_norm, grad_gain_two, grad_gate, grad_up = back_gather(
        act_two_t, w_gate, w_up, d_gate, d_up, dots, x_low, attn, gain_two, 5
    )
    ffn, d_attn, grad_down = down_gather(g_low, w_down, hidden, d_norm, 6)
    d_tokens, out, grad_query, grad_out, grad_kv, gain_tiles = tail(
        d_attn,
        w_out,
        queries,
        kv,
        probs,
        pair_rms,
        cos,
        sin,
        act_one_t,
        w_qkv,
        ffn,
        x_low,
        attn,
        gain_one,
        grad_gain_two,
        mixed_all,
        7,
    )
    gains = jnp.sum(gain_tiles, axis=0).reshape(2, -1)
    return (
        out,
        d_tokens.astype(wider),
        gains[0],
        grad_query.astype(wider),
        grad_kv.astype(wider),
        grad_out.astype(wider),
        gains[1],
        grad_gate.astype(wider),
        grad_up.astype(wider),
        grad_down.astype(wider),
    )


def solution(mesh):
    in_specs = (
        P(("dp", "seq"), None),
        P("dp"),
        P(("dp", "seq")),
        P(("dp", "seq"), "tensor"),
        P(("dp", "seq"), None),
        P("tensor", ("dp", "seq")),
        P(("dp", "seq")),
        P(("dp", "seq"), "tensor"),
        P(("dp", "seq"), "tensor"),
        P("tensor", ("dp", "seq")),
        P(("dp", "seq"), None),
    )
    out_specs = (
        P(("dp", "seq"), None),
        P(("dp", "seq"), None),
        P(("dp", "seq")),
        P(("dp", "seq"), "tensor"),
        P(("dp", "seq"), None),
        P("tensor", ("dp", "seq")),
        P(("dp", "seq")),
        P(("dp", "seq"), "tensor"),
        P(("dp", "seq"), "tensor"),
        P("tensor", ("dp", "seq")),
    )

    def shards(*arrays):
        tokens = arrays[0]
        sizes = tuple(mesh.shape[name] for name in ("dp", "seq", "tensor"))
        count = tokens.shape[0] * sizes[0] * sizes[1]
        plan = acts_move if sizes == (4, 2, 4) and count <= tokens.shape[1] else weights_move
        return plan(*arrays)

    return jax.shard_map(shards, mesh=mesh, in_specs=in_specs, out_specs=out_specs, check_vma=False)
```

```python
import functools
import math

import jax
import jax.numpy as jnp
from jax import lax
from jax.experimental import pallas as pl
from jax.experimental.pallas import tpu as pltpu
from jax.sharding import PartitionSpec as P

HD = 256


EPS = 1e-06
NEG = -1e30


def place_tables(segs):
    length = segs.shape[0]
    index = jnp.arange(length, dtype=jnp.int32)
    flags = jnp.concatenate([jnp.ones((1,), dtype=bool), segs[1:] != segs[:-1]])
    starts = lax.cummax(jnp.where(flags, index, jnp.zeros_like(index)), axis=0)
    places = index - starts
    half_size = HD // 2
    freqs = jnp.exp(jnp.arange(half_size, dtype=jnp.float32) * (-math.log(10000.0) / half_size))
    angles = places.astype(jnp.float32)[:, None] * freqs[None, :]
    return (places, jnp.cos(angles), jnp.sin(angles))


def rotate(vector, cos_table, sin_table):
    half_size = vector.shape[-1] // 2
    leading = vector[..., :half_size]
    trailing = vector[..., half_size:]
    return jnp.concatenate(
        [leading * cos_table - trailing * sin_table, trailing * cos_table + leading * sin_table],
        axis=-1,
    )


def rotate_back(vector, cos_table, sin_table):
    half_size = vector.shape[-1] // 2
    leading = vector[..., :half_size]
    trailing = vector[..., half_size:]
    return jnp.concatenate(
        [leading * cos_table + trailing * sin_table, trailing * cos_table - leading * sin_table],
        axis=-1,
    )


def matmul(left, right):
    return jnp.dot(left, right, preferred_element_type=jnp.float32)


def matmul_nt(left, right):
    return lax.dot_general(
        left, right, (((1,), (1,)), ((), ())), preferred_element_type=jnp.float32
    )


def matmul_tn(left, right):
    return lax.dot_general(
        left, right, (((0,), (0,)), ((), ())), preferred_element_type=jnp.float32
    )


def gelu_tanh(values):
    return jax.nn.gelu(values, approximate=True)


def norm_back(d_act, normed, rms_val, gain_val):
    scaled = d_act * gain_val
    return rms_val * (scaled - normed * jnp.mean(scaled * normed, axis=-1, keepdims=True))


def weights_move(
    tokens, seg_ids, gain_attn, w_query, kv_weight, w_out, gain_ffn, w_gate, w_up, w_down, d_out
):
    rows = tokens.shape[0]
    scale_factor = 1.0 / math.sqrt(HD)
    offset = lax.axis_index("seq") * rows
    places, cos_table, sin_table = place_tables(seg_ids)
    own_places = lax.dynamic_slice_in_dim(places, offset, rows, 0)
    own_segs = lax.dynamic_slice_in_dim(seg_ids, offset, rows, 0)
    own_cos = lax.dynamic_slice_in_dim(cos_table, offset, rows, 0)
    own_sin = lax.dynamic_slice_in_dim(sin_table, offset, rows, 0)
    allowed = (own_segs[:, None] == seg_ids[None, :]) & (own_places[:, None] >= places[None, :])
    full_query, full_out, full_kv, full_gain_one = (
        lax.all_gather(w_query, ("dp", "seq"), axis=0, tiled=True),
        lax.all_gather(w_out, ("dp", "seq"), axis=1, tiled=True),
        lax.all_gather(kv_weight, ("dp", "seq"), axis=0, tiled=True),
        lax.all_gather(gain_attn, ("dp", "seq"), axis=0, tiled=True),
    )
    gain_one = full_gain_one.astype(jnp.float32)
    inputs = tokens.astype(jnp.float32)
    rms_one = lax.rsqrt(jnp.mean(inputs * inputs, axis=-1, keepdims=True) + EPS)
    norm_one = inputs * rms_one
    act_one = (norm_one * gain_one).astype(jnp.bfloat16)
    query_pre = matmul(act_one, full_query)
    heads = query_pre.shape[1] // HD
    kv_pre = matmul(act_one, full_kv)
    queries = (
        rotate(query_pre.reshape(rows, heads, HD), own_cos[:, None, :], own_sin[:, None, :])
        * scale_factor
    ).astype(jnp.bfloat16)
    own_kv = jnp.concatenate(
        [rotate(kv_pre[:, :HD], own_cos, own_sin), kv_pre[:, HD:]], axis=1
    ).astype(jnp.bfloat16)
    all_kv = lax.all_gather(own_kv, "seq", axis=0, tiled=True)
    keys = all_kv[:, :HD]
    values_all = all_kv[:, HD:]
    scores = jnp.einsum("rhd,kd->hrk", queries, keys, preferred_element_type=jnp.float32)
    scores = jnp.where(allowed[None], scores, NEG)
    top_score = jnp.max(scores, axis=-1, keepdims=True)
    expd = jnp.exp(scores - top_score)
    total = jnp.sum(expd, axis=-1, keepdims=True)
    log_total = top_score + jnp.log(total)
    probs_low = (expd / total).astype(jnp.bfloat16)
    mixed = (
        jnp.einsum("hrk,kd->rhd", probs_low, values_all, preferred_element_type=jnp.float32)
        .reshape(rows, heads * HD)
        .astype(jnp.bfloat16)
    )
    attn = lax.psum(matmul(mixed, full_out), "tensor")
    resid = inputs + attn
    full_gate, full_up, full_down, full_gain_two = (
        lax.all_gather(w_gate, ("dp", "seq"), axis=0, tiled=True),
        lax.all_gather(w_up, ("dp", "seq"), axis=0, tiled=True),
        lax.all_gather(w_down, ("dp", "seq"), axis=1, tiled=True),
        lax.all_gather(gain_ffn, ("dp", "seq"), axis=0, tiled=True),
    )
    gain_two = full_gain_two.astype(jnp.float32)
    rms_two = lax.rsqrt(jnp.mean(resid * resid, axis=-1, keepdims=True) + EPS)
    norm_two = resid * rms_two
    act_two = (norm_two * gain_two).astype(jnp.bfloat16)
    gate = matmul(act_two, full_gate)
    up_val = matmul(act_two, full_up)
    gelu_val, gelu_pull = jax.vjp(gelu_tanh, gate)
    hidden = (gelu_val * up_val).astype(jnp.bfloat16)
    ffn = lax.psum(matmul(hidden, full_down).astype(jnp.bfloat16), "tensor").astype(jnp.float32)
    out = (resid + ffn).astype(jnp.bfloat16)
    back_gate, back_up, back_down = (
        lax.all_gather(w_gate, ("dp", "seq"), axis=0, tiled=True),
        lax.all_gather(w_up, ("dp", "seq"), axis=0, tiled=True),
        lax.all_gather(w_down, ("dp", "seq"), axis=1, tiled=True),
    )
    d_hidden = matmul_nt(d_out, back_down)
    grad_down = matmul_tn(hidden, d_out)
    d_gate = gelu_pull(d_hidden * up_val)[0].astype(jnp.bfloat16)
    d_up = (d_hidden * gelu_val).astype(jnp.bfloat16)
    grad_gate = matmul_tn(act_two, d_gate)
    grad_up = matmul_tn(act_two, d_up)
    d_act_two = lax.psum(matmul_nt(d_gate, back_gate) + matmul_nt(d_up, back_up), "tensor")
    grad_gain_two = jnp.sum(d_act_two * norm_two, axis=0)
    d_resid = d_out.astype(jnp.float32) + norm_back(d_act_two, norm_two, rms_two, gain_two)
    ffn_grads = (
        lax.psum_scatter(
            grad_gate.astype(jnp.bfloat16), ("dp", "seq"), scatter_dimension=0, tiled=True
        ).astype(jnp.float32),
        lax.psum_scatter(
            grad_up.astype(jnp.bfloat16), ("dp", "seq"), scatter_dimension=0, tiled=True
        ).astype(jnp.float32),
        lax.psum_scatter(
            grad_down.astype(jnp.bfloat16), ("dp", "seq"), scatter_dimension=1, tiled=True
        ).astype(jnp.float32),
        lax.psum_scatter(
            grad_gain_two.astype(jnp.bfloat16), ("dp", "seq"), scatter_dimension=0, tiled=True
        ).astype(jnp.float32),
    )
    back_query, back_out, back_kv = (
        lax.all_gather(w_query, ("dp", "seq"), axis=0, tiled=True),
        lax.all_gather(w_out, ("dp", "seq"), axis=1, tiled=True),
        lax.all_gather(kv_weight, ("dp", "seq"), axis=0, tiled=True),
    )
    d_attn = d_resid.astype(jnp.bfloat16)
    grad_out = matmul_tn(mixed, d_attn)
    d_mixed = matmul_nt(d_attn, back_out).astype(jnp.bfloat16).reshape(rows, heads, HD)
    scores_again = jnp.einsum("rhd,kd->hrk", queries, keys, preferred_element_type=jnp.float32)
    probs = jnp.where(allowed[None], jnp.exp(scores_again - log_total), 0.0)
    d_probs = jnp.einsum("rhd,kd->hrk", d_mixed, values_all, preferred_element_type=jnp.float32)
    delta = jnp.sum(probs * d_probs, axis=-1, keepdims=True)
    d_scores = (probs * (d_probs - delta)).astype(jnp.bfloat16)
    d_queries = (
        jnp.einsum("hrk,kd->rhd", d_scores, keys, preferred_element_type=jnp.float32) * scale_factor
    )
    d_query_pre = (
        rotate_back(d_queries, own_cos[:, None, :], own_sin[:, None, :])
        .reshape(rows, heads * HD)
        .astype(jnp.bfloat16)
    )
    d_keys_part = jnp.einsum("hrk,rhd->kd", d_scores, queries, preferred_element_type=jnp.float32)
    d_values_part = jnp.einsum(
        "hrk,rhd->kd", probs.astype(jnp.bfloat16), d_mixed, preferred_element_type=jnp.float32
    )
    own_kv_grad = lax.psum_scatter(
        jnp.concatenate([d_keys_part, d_values_part], axis=1).astype(jnp.bfloat16),
        "seq",
        scatter_dimension=0,
        tiled=True,
    )
    d_act_query = matmul_nt(d_query_pre, back_query)
    d_act_sum, kv_grad = (
        lax.psum(d_act_query.astype(jnp.bfloat16), "tensor").astype(jnp.float32),
        lax.psum(own_kv_grad, "tensor").astype(jnp.float32),
    )
    d_kv_pre = jnp.concatenate(
        [rotate_back(kv_grad[:, :HD], own_cos, own_sin), kv_grad[:, HD:]], axis=1
    ).astype(jnp.bfloat16)
    d_act_one = d_act_sum + matmul_nt(d_kv_pre, back_kv)
    grad_query = matmul_tn(act_one, d_query_pre)
    grad_kv = matmul_tn(act_one, d_kv_pre)
    grad_gain_one = jnp.sum(d_act_one * norm_one, axis=0)
    d_tokens = d_resid + norm_back(d_act_one, norm_one, rms_one, gain_one)
    attn_grads = (
        lax.psum_scatter(
            grad_query.astype(jnp.bfloat16), ("dp", "seq"), scatter_dimension=0, tiled=True
        ).astype(jnp.float32),
        lax.psum_scatter(
            grad_out.astype(jnp.bfloat16), ("dp", "seq"), scatter_dimension=1, tiled=True
        ).astype(jnp.float32),
        lax.psum_scatter(
            grad_kv.astype(jnp.bfloat16), ("dp", "seq"), scatter_dimension=0, tiled=True
        ).astype(jnp.float32),
        lax.psum_scatter(
            grad_gain_one.astype(jnp.bfloat16), ("dp", "seq"), scatter_dimension=0, tiled=True
        ).astype(jnp.float32),
    )
    return (
        out,
        d_tokens,
        attn_grads[3],
        attn_grads[0],
        attn_grads[2],
        attn_grads[1],
        ffn_grads[3],
        ffn_grads[0],
        ffn_grads[1],
        ffn_grads[2],
    )


MESH = pl.DeviceIdType.MESH
VMEM_LIMIT = 66000 * 1024


class Place:
    def __init__(self):
        self.dp = lax.axis_index("dp")
        self.seq = lax.axis_index("seq")
        self.z = lax.axis_index("tensor")
        self.core = lax.rem(self.dp, 2)
        self.chip = lax.div(self.dp, 2)

    def device(self, across, other):
        chip = (self.chip + across) % 2
        seq = (self.seq + across // 2) % 2
        core = (self.core + other) % 2
        return chip * 2 + core, seq, self.z

    def shard(self, across, other):
        dp, seq, _ = self.device(across, other)
        return dp * 2 + seq


def greet(here, peers, line=False):
    barrier = pltpu.get_barrier_semaphore()
    peers = list(peers)
    if line:
        peers += [(here.dp, here.seq, (here.z + step) % 4) for step in range(1, 4)]
    for peer in peers:
        pl.semaphore_signal(barrier, inc=1, device_id=peer, device_id_type=MESH)
    pl.semaphore_wait(barrier, len(peers))


def remote(src, dst, send, recv, peer):
    return pltpu.make_async_remote_copy(
        src_ref=src, dst_ref=dst, send_sem=send, recv_sem=recv, device_id=peer, device_id_type=MESH
    )


class Line:
    def __init__(self, here, counts, refs, place=None):
        self.own, self.out, self.from_end, self.from_mid = refs[:4]
        self.sems = refs[4:10]
        self.counts = counts
        self.chunk = self.from_end.shape[1]
        self.place = place
        z = here.z
        self.inner = ((z + 1) // 2) % 2
        self.mate = (here.dp, here.seq, z + 1 - 2 * (z % 2))
        self.other = (here.dp, here.seq, 3 - z)

    def rows(self, at):
        at = at if self.place is None else self.place(at)
        return pl.ds(pl.multiple_of(at * self.chunk, self.chunk), self.chunk)

    def up(self, at):
        return remote(self.own.at[self.rows(at), :], self.from_end.at[at], self.sems[0].at[at],
                      self.sems[1].at[at], self.mate)

    def over(self, at):
        return remote(self.out.at[self.rows(at), :], self.from_mid.at[at], self.sems[2].at[at],
                      self.sems[3].at[at], self.other)

    def down(self, at):
        rows = self.rows(at)
        return remote(self.out.at[rows, :], self.out.at[rows, :], self.sems[4].at[at],
                      self.sems[5].at[at], self.mate)

    def launch(self, first, count):
        @pl.when(self.inner == 0)
        def _():
            def send(at, _):
                self.up(first + at).start()
                return 0

            lax.fori_loop(0, count, send, 0)

    def begin(self):
        self.launch(0, self.counts)

    def first(self, at):
        rows = self.rows(at)
        self.up(at).wait_recv()
        total = self.own[rows, :].astype(jnp.float32) + self.from_end[at].astype(jnp.float32)
        self.out[rows, :] = total.astype(self.out.dtype)
        self.over(at).start()

    def second(self, at):
        rows = self.rows(at)
        self.over(at).wait()
        total = self.out[rows, :].astype(jnp.float32) + self.from_mid[at].astype(jnp.float32)
        self.out[rows, :] = total.astype(self.out.dtype)
        self.down(at).start()

    def step(self, at, start=0, count=None):
        count = self.counts if count is None else count

        @pl.when(jnp.logical_and(self.inner == 1, at < count))
        def _():
            self.first(start + at)

        @pl.when(jnp.logical_and(self.inner == 1, jnp.logical_and(at > 1, at < count + 2)))
        def _():
            self.second(start + at - 2)

    def steps(self, first, last, start=0, count=None):
        def rest(at, _):
            self.step(at, start, count)
            return 0

        lax.fori_loop(first, last, rest, 0)

    def settle(self):
        @pl.when(self.inner == 0)
        def _():
            def take(at, _):
                self.up(at).wait_send()
                self.down(at).wait_recv()
                return 0

            lax.fori_loop(0, self.counts, take, 0)

        self.drain()

    def drain(self):
        @pl.when(self.inner == 1)
        def _():
            def drain(at, _):
                self.down(at).wait_send()
                return 0

            lax.fori_loop(0, self.counts, drain, 0)

    def end(self, done=0):
        self.steps(min(done, self.counts + 2), self.counts + 2)
        self.settle()


def line_scratch(counts, shape, low):
    buf = pltpu.VMEM((counts, shape[0] // counts, shape[1]), low)
    return [buf, buf] + [pltpu.SemaphoreType.DMA((counts,))] * 6


def turned(at):
    return 3 - at // 2, 1 - at % 2


def slice_peers(here):
    return [here.device(*turned(at)) for at in range(7)]


def kernel_call(kernel, out_shape, operands, specs, scratch, cid, name, out_specs=None, late=()):
    vm = pl.BlockSpec(memory_space=pltpu.VMEM)
    specs = [pl.BlockSpec(memory_space=pl.ANY) if at in late else spec for at, spec in enumerate(specs)]
    inside = [pltpu.VMEM(operands[at].shape, operands[at].dtype) for at in late]
    if late:
        inside.append(pltpu.SemaphoreType.DMA((len(late),)))

    def body(*refs):
        if not late:
            kernel(*refs)
            return
        ins, rest, own = list(refs[: len(operands)]), refs[len(operands) : -len(inside)], refs[-len(inside) :]
        copies = []
        for spot, at in enumerate(late):
            copy = pltpu.make_async_copy(ins[at], own[spot], own[-1].at[spot])
            copy.start()
            copies.append(copy)
            ins[at] = own[spot]
        kernel(*ins, *rest, late=copies)

    return pl.pallas_call(
        body,
        out_shape=out_shape,
        in_specs=specs,
        out_specs=out_specs or [vm] * len(out_shape),
        scratch_shapes=scratch + inside,
        compiler_params=pltpu.CompilerParams(
            collective_id=cid, has_side_effects=True, vmem_limit_bytes=VMEM_LIMIT
        ),
        name=f"{name}_{cid}",
    )(*operands)


class Tiny:
    def __init__(self, here, src, dst, sems, spread):
        self.here, self.src, self.dst, self.sems, self.spread = here, src, dst, sems, spread
        self.peers = slice_peers(here)
        self.me = here.shard(0, 0)

    def tile(self, shard):
        return self.src.at[shard] if self.spread else self.src

    def copy(self, at):
        return remote(self.tile(self.here.shard(*turned(at))), self.dst.at[self.me], self.sems[0].at[at],
                      self.sems[1].at[at], self.peers[at])

    def begin(self):
        for at in range(7):
            self.copy(at).start()
        self.dst[self.me] = self.tile(self.me)[...]

    def end(self):
        for at in range(7):
            self.copy(at).wait()


class Reduce:
    def __init__(self, here, counts, product, refs, before=None):
        self.counts, self.product, self.before = counts, product, before
        self.held, self.sib_out, self.sib_in, self.from_x, self.from_y = refs[:5]
        self.sib_sems, self.x_sems, self.y_sems = refs[5:7], refs[7:9], refs[9:11]
        self.sib, self.xdev, self.ydev = here.device(0, 1), here.device(1, 0), here.device(2, 0)
        self.steps = 4 * counts
        self.ring = self.sib_out.shape[0]

    def streams(self, stage):
        far = stage // 3
        x_chip = jnp.where(stage == 0, 3, jnp.where(stage == 2, 0, 1))
        y_chip = jnp.where(stage == 0, 3, jnp.where(stage == 2, 0, 2))
        return (x_chip, far), (y_chip, 1 - far)

    def to_sib(self, step, stream):
        stage, at = step // self.counts, step % self.counts
        return remote(self.sib_out.at[step % self.ring, stream], self.sib_in.at[stage, stream, at],
                      self.sib_sems[0].at[stage, stream, at], self.sib_sems[1].at[stage, stream, at], self.sib)

    def to_x(self, hop, at, stage=0):
        return remote(self.held.at[stage, 0, at], self.from_x.at[hop, at], self.x_sems[0].at[hop, at],
                      self.x_sems[1].at[hop, at], self.xdev)

    def to_y(self, hop, at, stage=0):
        return remote(self.held.at[stage, 1, at], self.from_y.at[hop, at], self.y_sems[0].at[hop, at],
                      self.y_sems[1].at[hop, at], self.ydev)

    def compute(self, step):
        stage, at = step // self.counts, step % self.counts
        if self.before:
            for stop in range(3):
                @pl.when(step == stop * self.counts)
                def _():
                    self.before(stop)

        @pl.when(step >= self.ring)
        def _():
            for stream in range(2):
                self.to_sib(step - self.ring, stream).wait_send()

        for stream, (across, half) in enumerate(self.streams(stage)):
            self.sib_out[step % self.ring, stream] = self.product(across, 1, half, at).astype(jnp.bfloat16)
            self.held[stage, stream, at] = self.product(across, 0, half, at).astype(jnp.bfloat16)
        for stream in range(2):
            self.to_sib(step, stream).start()

    def finish(self, step):
        stage, at = step // self.counts, step % self.counts
        for stream in range(2):
            self.to_sib(step, stream).wait_recv()

        def total(stream):
            return self.held[stage, stream, at].astype(jnp.float32) + self.sib_in[stage, stream, at].astype(
                jnp.float32)

        @pl.when(stage < 3)
        def _():
            for stream in range(2):
                self.held[stage, stream, at] = total(stream).astype(jnp.bfloat16)

        @pl.when(stage == 3)
        def _():
            self.to_y(0, at).wait_recv()
            self.held[3, 0, at] = (total(0) + self.from_y[0, at].astype(jnp.float32)).astype(jnp.bfloat16)
            self.to_x(0, at).wait_recv()
            self.held[3, 1, at] = (total(1) + self.from_x[0, at].astype(jnp.float32)).astype(jnp.bfloat16)

        @pl.when(stage != 2)
        def _():
            hop = stage - stage // 3
            self.to_x(hop, at, stage).start()
            self.to_y(hop, at, stage).start()

    def advance(self, step):
        @pl.when(step < self.steps)
        def _():
            self.compute(step)

        @pl.when(jnp.logical_and(step > 0, step <= self.steps))
        def _():
            self.finish(step - 1)

    def run(self, hook=None):
        def body(step, _):
            self.advance(step)

            if hook:
                hook(step)
            return 0

        lax.fori_loop(0, self.steps + 1, body, 0)
        return self.steps + 1

    def end(self, emit):
        def last(at, _):
            values = []
            for half in range(2):
                xs, ys = (1, 2) if half == 0 else (2, 1)
                self.to_x(xs, at).wait_recv()
                self.to_y(ys, at).wait_recv()
                values.append(self.held[2, half, at].astype(jnp.float32) + self.from_x[xs, at].astype(jnp.float32)
                              + self.from_y[ys, at].astype(jnp.float32))
            emit(at, *values)
            for hop in range(3):
                self.to_x(hop, at).wait_send()
                self.to_y(hop, at).wait_send()
            return 0

        lax.fori_loop(0, self.counts, last, 0)

        def drain(at, _):
            for stream in range(2):
                self.to_sib(self.steps - self.ring + at, stream).wait_send()
            return 0

        lax.fori_loop(0, self.ring, drain, 0)


def reduce_scratch(counts, rows, width, ring=4):
    low, dma = jnp.bfloat16, pltpu.SemaphoreType.DMA
    block = pltpu.VMEM((4, 2, counts, rows, width), low)
    landed = pltpu.VMEM((3, counts, rows, width), low)
    sent = pltpu.VMEM((ring, 2, rows, width), low)
    return [block, sent, block, landed, landed] + [dma((4, 2, counts))] * 2 + [dma((3, counts))] * 4


class Spread:
    def __init__(self, here, counts, refs):
        self.counts = counts
        self.got = refs[0]
        self.x_sems, self.y_sems, self.sib_sems = refs[1:3], refs[3:5], refs[5:7]
        self.core = here.core
        self.sib, self.xdev, self.ydev = here.device(0, 1), here.device(1, 0), here.device(2, 0)

    def slot(self, across, half, at):
        return self.got.at[across, self.core, half, at]

    def x_copy(self, hop, at):
        half = jnp.minimum(hop, 1)
        src = self.slot(2 * (hop // 2), half, at)
        dst = self.slot(1 + 2 * (hop // 2), half, at)
        return remote(src, dst, self.x_sems[0].at[hop, at], self.x_sems[1].at[hop, at], self.xdev)

    def y_copy(self, hop, at):
        half = 1 - jnp.minimum(hop, 1)
        src = self.slot(hop // 2, half, at)
        dst = self.slot(2 + hop // 2, half, at)
        return remote(src, dst, self.y_sems[0].at[hop, at], self.y_sems[1].at[hop, at], self.ydev)

    def streams(self, stage):
        some, last, late = jnp.minimum(stage, 1), stage // 3, stage // 2
        return (some + 2 * last, late), (2 * some + last, 1 - late)

    def block(self, at):
        x_stream, y_stream = self.streams(at // 4)
        second = at // 2 % 2
        across = x_stream[0] + second * (y_stream[0] - x_stream[0])
        half = x_stream[1] + second * (y_stream[1] - x_stream[1])
        return across, at % 2, half

    def begin_rows(self):
        for hop in range(2):
            self.x_copy(hop, 0).start()
            self.y_copy(hop, 0).start()
        for stream in range(2):
            self.sib_copy(0, stream, 0).start()

    def receive_rows(self, step):
        stage = step // 4

        @pl.when(jnp.logical_and(step % 4 == 0, jnp.logical_and(stage > 0, stage < 4)))
        def _():
            self.x_copy(stage - 1, 0).wait_recv()
            self.sib_copy(stage, 0, 0).start()
            self.y_copy(stage - 1, 0).wait_recv()
            self.sib_copy(stage, 1, 0).start()

        @pl.when(step == 4)
        def _():
            self.x_copy(2, 0).start()
            self.y_copy(2, 0).start()

        for stream in range(2):
            @pl.when(jnp.logical_and(step % 4 == 2 * stream, step < 16))
            def _(stream=stream):
                self.sib_copy(stage, stream, 0).wait_recv()

    def sib_copy(self, stage, stream, at):
        across, half = self.streams(stage)[stream]
        slot = self.slot(across, half, at)
        spot = (stage, stream, at)
        return remote(slot, slot, self.sib_sems[0].at[spot], self.sib_sems[1].at[spot], self.sib)

    def begin(self):
        def first(at, _):
            self.x_copy(0, at).start()
            self.y_copy(0, at).start()
            return 0

        def own(at, _):
            self.sib_copy(0, 0, at).start()
            self.sib_copy(0, 1, at).start()
            return 0

        lax.fori_loop(0, self.counts, first, 0)
        lax.fori_loop(0, self.counts, own, 0)

    def run(self, blocks, hook=None, done=None):
        counts = self.counts

        def body(step, _):
            stage, at = step // counts, step % counts

            @pl.when(jnp.logical_and(stage > 0, stage < 4))
            def _():
                self.x_copy(stage - 1, at).wait_recv()
                self.sib_copy(stage, 0, at).start()
                self.y_copy(stage - 1, at).wait_recv()
                self.sib_copy(stage, 1, at).start()

            @pl.when(jnp.logical_and(stage > 0, stage < 3))
            def _():
                self.x_copy(stage, at).start()
                self.y_copy(stage, at).start()

            @pl.when(step > 0)
            def _():
                old, spot = (step - 1) // counts, (step - 1) % counts
                for stream, (across, half) in enumerate(self.streams(old)):
                    self.sib_copy(old, stream, spot).wait_recv()
                    blocks(across, half, spot)
                if done:
                    done(old, spot)

            if hook:
                hook(step)
            return 0

        lax.fori_loop(0, 4 * counts + 1, body, 0)
        return 4 * counts + 1

    def end(self):
        def drain(at, _):
            for hop in range(3):
                self.x_copy(hop, at).wait_send()
                self.y_copy(hop, at).wait_send()
            for stage in range(4):
                self.sib_copy(stage, 0, at).wait_send()
                self.sib_copy(stage, 1, at).wait_send()
            return 0

        lax.fori_loop(0, self.counts, drain, 0)


def spread_scratch(counts, rows, width):
    dma = pltpu.SemaphoreType.DMA
    return [pltpu.VMEM((4, 2, 2, counts, rows, width), jnp.bfloat16)] + [dma((3, counts))] * 4 + [
        dma((4, 2, counts))] * 2


def row_span(here, across, other, rows):
    return pl.ds(pl.multiple_of(here.shard(across, other) * rows, rows), rows)


def dot_nt(left, right):
    return lax.dot_general(left, right, (((1,), (1,)), ((), ())), preferred_element_type=jnp.float32)


def dot_tn(left, right):
    return lax.dot_general(left, right, (((0,), (0,)), ((), ())), preferred_element_type=jnp.float32)


def dot_nn(left, right):
    return jnp.dot(left, right, preferred_element_type=jnp.float32)


def products(here, act, weight, nt, rows, width, counts):
    def product(across, other, half, at):
        cols = pl.ds(pl.multiple_of((half * counts + at) * width, width), width)
        block = act[row_span(here, across, other, rows), :]
        return dot_nt(block, weight[cols, :]) if nt else dot_nn(block, weight[:, cols])

    return product


def diagonal():
    return (lax.broadcasted_iota(jnp.int32, (LANES, LANES), 0) ==
            lax.broadcasted_iota(jnp.int32, (LANES, LANES), 1)).astype(jnp.float32)


def to_tile(tile, first, column, eye):
    for at in range(column.shape[0] // LANES):
        spread = column[at * LANES : (at + 1) * LANES, :] * eye
        tile[first + at : first + at + 1, :] = jnp.sum(spread, axis=0, keepdims=True)


def from_tile(row, eye):
    return jnp.sum(eye * row, axis=1, keepdims=True)


def make_tables(here, rows, segs, cos, sin, mask):
    eye = diagonal()
    tiles = rows // LANES
    freqs = jnp.exp(lax.broadcasted_iota(jnp.int32, (1, LANES), 1).astype(jnp.float32) * (-math.log(10000.0) / LANES))
    lane = lax.broadcasted_iota(jnp.int32, (1, LANES), 1)
    line = lax.broadcasted_iota(jnp.int32, (LANES, 1), 0)

    def row_of(side, at):
        return ((here.seq + side) % 2) * tiles + at

    for side in range(2):
        for at in range(tiles):
            row = row_of(side, at)
            ids = from_tile(segs[pl.ds(row, 1), :], eye)
            before = jnp.zeros((LANES, 1), jnp.float32)
            for other in range(2 * tiles):
                smaller = segs[other : other + 1, :] < ids
                before += jnp.sum(smaller.astype(jnp.float32), axis=-1, keepdims=True)
            index = row * LANES + line
            angles = (index.astype(jnp.float32) - before) * freqs
            span = slice(at * LANES, (at + 1) * LANES)
            cos[side, span, :] = jnp.cos(angles)
            sin[side, span, :] = jnp.sin(angles)
            if side == 0:
                for key_side in range(2):
                    for key_at in range(tiles):
                        key_row = row_of(key_side, key_at)
                        same = segs[pl.ds(key_row, 1), :] == ids
                        allowed = jnp.logical_and(same, key_row * LANES + lane <= index)
                        first = key_side * rows + key_at * LANES
                        mask[span, first : first + LANES] = allowed.astype(jnp.float32)


def open_kernel(rows, width, counts, tokens, gain, w_query, kv_weight, segs, cot, qkv, x_low, act_t, w_qkv, rms, cos, sin,
                mask, g_col, *refs):
    here = Place()
    cols = gain.shape[1]
    act, turn_send, turn_recv, local_sems, cot_part, g_send, g_recv, z_send, z_recv = refs[:9]
    share = rows // 4
    me = here.shard(0, 0)
    own_rows = pl.ds(pl.multiple_of(me * rows, rows), rows)

    def turn_copy(at):
        across, other = turned(at)
        first = pl.multiple_of(here.shard(across, other) * cols, cols)
        return remote(tokens.at[:, pl.ds(first, cols)], x_low.at[own_rows, :], turn_send.at[at], turn_recv.at[at],
                      here.device(across, other))

    wide = w_query.shape[1]
    local = [
        pltpu.make_async_copy(w_query, w_qkv.at[:, :wide], local_sems.at[0]),
        pltpu.make_async_copy(kv_weight, w_qkv.at[:, wide:], local_sems.at[1]),
        pltpu.make_async_copy(tokens.at[:, pl.ds(pl.multiple_of(me * cols, cols), cols)], x_low.at[own_rows, :],
                              local_sems.at[2]),
    ]
    load = pltpu.make_async_copy(cot.at[pl.ds(pl.multiple_of(here.z * share, share), share), :], cot_part,
                                 local_sems.at[3])
    load.start()
    for copy in local:
        copy.start()

    def g_copy(at):
        across, other = turned(at)
        first = pl.multiple_of(here.shard(across, other) * cols, cols)
        return remote(cot_part.at[:, pl.ds(first, cols)], g_col.at[me, here.z], g_send.at[at], g_recv.at[at],
                      here.device(across, other))

    def own_part():
        return pltpu.make_async_copy(cot_part.at[:, pl.ds(pl.multiple_of(me * cols, cols), cols)],
                                     g_col.at[me, here.z], local_sems.at[4])

    def quarter(way, at, step, peer):
        spot = g_col.at[:, at]
        return remote(spot, spot, z_send.at[way, step], z_recv.at[way, step], (here.dp, here.seq, here.z + peer))

    def pass_on(step):
        @pl.when(jnp.logical_and(here.z < 3, here.z >= step))
        def _():
            quarter(0, here.z - step, step, 1).start()

        @pl.when(jnp.logical_and(here.z > 0, here.z <= 3 - step))
        def _():
            quarter(1, here.z + step, step, -1).start()

    def take_quarters(step):
        @pl.when(here.z > step)
        def _():
            quarter(0, here.z - 1 - step, step, -1).wait_recv()

        @pl.when(here.z < 3 - step)
        def _():
            quarter(1, here.z + 1 + step, step, 1).wait_recv()

    greet(here, slice_peers(here), True)
    load.wait()
    own_part().start()
    for at in range(7):
        g_copy(at).start()
    for at in range(7):
        turn_copy(at).start()
    for copy in local:
        copy.wait()

    def squares(at, total):
        values = tokens[:, pl.ds(pl.multiple_of(at * cols, cols), cols)].astype(jnp.float32)
        return total + jnp.sum(values * values, axis=-1, keepdims=True)

    total = lax.fori_loop(0, 8, squares, jnp.zeros((rows, 1), jnp.float32))
    rms[...] = jnp.broadcast_to(lax.rsqrt(total / (8 * cols) + EPS), rms.shape)
    make_tables(here, rows, segs, cos, sin, mask)

    def prepare(first, count):
        def one(step, _):
            at = first + step
            span = row_span(here, *turned(at), rows)
            value = (x_low[span, :].astype(jnp.float32) * gain[0:1, :]).astype(act.dtype)
            act[span, :] = value
            return 0

        lax.fori_loop(0, count, one, 0)

    def before(stop):
        first, count = ((0, 2), (2, 4), (6, 2))[stop]
        if stop == 0:
            own_part().wait()
            for at in range(7):
                g_copy(at).wait_recv()
        else:
            take_quarters(stop - 1)
        pass_on(stop)
        for at in range(first, min(first + count, 7)):
            turn_copy(at).wait_recv()
        prepare(first, count)

    def flip():
        def one(shard, _):
            span = pl.ds(pl.multiple_of(shard * rows, rows), rows)
            act_t[:, span] = act[span, :].T
            return 0

        lax.fori_loop(0, 8, one, 0)

    product = products(here, act, w_qkv, False, rows, width, counts)
    total = Reduce(here, counts, product, refs[9:20], before)
    total.run()
    flip()

    def emit(at, first, second):
        for half, value in enumerate((first, second)):
            qkv[:, pl.ds(pl.multiple_of((half * counts + at) * width, width), width)] = value

    total.end(emit)
    take_quarters(2)
    for at in range(7):
        turn_copy(at).wait_send()
        g_copy(at).wait_send()
    for step in range(3):
        @pl.when(jnp.logical_and(here.z < 3, here.z >= step))
        def _(step=step):
            quarter(0, here.z - step, step, 1).wait_send()

        @pl.when(jnp.logical_and(here.z > 0, here.z <= 3 - step))
        def _(step=step):
            quarter(1, here.z + step, step, -1).wait_send()


def opening(tokens, gain, w_query, kv_weight, segs, cot, cid, width=256):
    rows = tokens.shape[0]
    cols, wide = w_query.shape
    every = wide + kv_weight.shape[1]
    counts = every // (2 * width)
    low, f32 = jnp.bfloat16, jnp.float32
    dma = pltpu.SemaphoreType.DMA
    vm = pl.BlockSpec(memory_space=pltpu.VMEM)
    hbm = pl.BlockSpec(memory_space=pl.ANY)
    out_shape = [
        jax.ShapeDtypeStruct((rows, every), f32),
        jax.ShapeDtypeStruct((8 * rows, cols), low),
        jax.ShapeDtypeStruct((cols, 8 * rows), low),
        jax.ShapeDtypeStruct((cols, every), low),
        jax.ShapeDtypeStruct((rows, LANES), f32),
        jax.ShapeDtypeStruct((2, rows, LANES), f32),
        jax.ShapeDtypeStruct((2, rows, LANES), f32),
        jax.ShapeDtypeStruct((rows, 2 * rows), f32),
        jax.ShapeDtypeStruct((8, 4, rows // 4, cols), low),
    ]
    scratch = [
        pltpu.VMEM((8 * rows, cols), low), dma((7,)), dma((7,)), dma((5,)),
        pltpu.VMEM((rows // 4, 8 * cols), low), dma((7,)), dma((7,)), dma((2, 3)), dma((2, 3)),
    ]
    scratch += reduce_scratch(counts, rows, width)
    kernel = functools.partial(open_kernel, rows, width, counts)
    return kernel_call(kernel, out_shape, [tokens, gain, w_query, kv_weight, segs, cot],
                       [vm, vm, hbm, hbm, vm, hbm], scratch, cid, "open")


def ffn_kernel(rows, width, counts, x_low, attn, gain, w_gate, w_up, d_hidden, hidden, d_gate, d_up, act_t, tile_out,
               *refs, late):
    here = Place()
    cols = gain.shape[1]
    act, weight, tiny_own, tiny_all, tiny_send, tiny_recv, dots, local_sems = refs[:8]
    tiny = Tiny(here, tiny_own, tiny_all, (tiny_send, tiny_recv), True)
    half_cols = counts * width
    local = [
        pltpu.make_async_copy(w_gate, weight.at[:, :half_cols], local_sems.at[0]),
        pltpu.make_async_copy(w_up, weight.at[:, half_cols:], local_sems.at[1]),
    ]
    for copy in local:
        copy.start()
    eye = diagonal()
    tiny_own[...] = jnp.zeros_like(tiny_own)

    def prepare(shard, _):
        for at in range(rows // LANES):
            span = pl.ds(pl.multiple_of(shard * rows + at * LANES, LANES), LANES)
            resid = x_low[span, :].astype(jnp.float32) + attn[span, :].astype(jnp.float32)
            act[span, :] = (resid * gain[0:1, :]).astype(act.dtype)
            square = jnp.sum(resid * resid, axis=-1, keepdims=True)
            tiny_own[shard, at : at + 1, :] = jnp.sum(square * eye, axis=0, keepdims=True)
        return 0

    lax.fori_loop(0, 8, prepare, 0)
    greet(here, slice_peers(here))
    tiny.begin()
    for copy in local:
        copy.wait()
    product = products(here, act, weight, False, rows, width, counts)
    total = Reduce(here, counts, product, refs[8:19])
    total.run()

    def flip(shard, _):
        span = pl.ds(pl.multiple_of(shard * rows, rows), rows)
        act_t[:, span] = act[span, :].T
        return 0

    lax.fori_loop(0, 8, flip, 0)
    tiny.end()
    tiles = rows // LANES
    mean = [from_tile(jnp.sum(tiny_all[:, at, :], axis=0, keepdims=True), eye) for at in range(tiles)]
    scale = lax.rsqrt(jnp.concatenate(mean, axis=0) / (8 * cols) + EPS)
    dots[...] = jnp.zeros_like(dots)
    late[0].wait()
    coeff = math.sqrt(2.0 / math.pi)

    def emit(at, first, second):
        span = pl.ds(pl.multiple_of(at * width, width), width)
        gate, up = first * scale, second * scale
        inner = jnp.tanh(coeff * (gate + 0.044715 * (gate * gate * gate)))
        gelu = 0.5 * gate * (1.0 + inner)
        slope = 0.5 * (1.0 + inner) + 0.5 * gate * (1.0 - inner * inner) * (
            coeff * (1.0 + 3.0 * 0.044715 * gate * gate))
        cot = d_hidden[:, span]
        hidden[:, span] = (gelu * up).astype(hidden.dtype)
        back_gate, back_up = cot * up * slope, cot * gelu
        d_gate[:, span] = (back_gate * scale).astype(d_gate.dtype)
        d_up[:, span] = (back_up * scale).astype(d_up.dtype)
        dots[...] += jnp.sum(back_gate * gate + back_up * up, axis=-1, keepdims=True)

    total.end(emit)
    tile_out[...] = jnp.zeros_like(tile_out)
    to_tile(tile_out, 0, dots[...] * (scale * scale * (1.0 / (8 * cols))), eye)


def ffn_scatter(x_low, attn, gain, w_gate, w_up, d_hidden, cid, width=512):
    rows, half = d_hidden.shape
    cols = gain.shape[1]
    counts = half // width
    low, f32 = jnp.bfloat16, jnp.float32
    dma = pltpu.SemaphoreType.DMA
    vm = pl.BlockSpec(memory_space=pltpu.VMEM)
    hbm = pl.BlockSpec(memory_space=pl.ANY)
    out_shape = [jax.ShapeDtypeStruct((rows, half), low)] * 3 + [
        jax.ShapeDtypeStruct((cols, 8 * rows), low),
        jax.ShapeDtypeStruct((8, LANES), f32),
    ]
    scratch = [
        pltpu.VMEM((8 * rows, cols), low),
        pltpu.VMEM((cols, 2 * half), low),
        pltpu.VMEM((8, 8, LANES), f32),
        pltpu.VMEM((8, 8, LANES), f32),
        dma((7,)), dma((7,)),
        pltpu.VMEM((rows, 1), f32),
        dma((2,)),
    ] + reduce_scratch(counts, rows, width)
    kernel = functools.partial(ffn_kernel, rows, width, counts)
    return kernel_call(kernel, out_shape, [x_low, attn, gain, w_gate, w_up, d_hidden], [vm, vm, vm, hbm, hbm, vm],
                       scratch, cid, "ffn", late=(5,))


def load_own(spread, payload, width, counts, sems):
    copies = []
    for half in range(2):
        for at in range(counts):
            first = at * width + (half * counts * width if len(payload) == 1 else 0)
            src = payload[half % len(payload)].at[:, first : first + width]
            copies.append(pltpu.make_async_copy(src, spread.slot(0, half, at), sems.at[half, at]))
    return copies


def chip_place(here, per):
    def place(at):
        return here.shard(at // (2 * per), at // per % 2) * per + at % per

    return place


def back_kernel(rows, width, counts, act_t, w_gate, w_up, d_gate, d_up, dots, x_low, attn, gain, d_norm, gain_grad,
                grad_gate, grad_up, *refs, late):
    here = Place()
    spread = Spread(here, counts, refs[:7])
    tiny_all, tiny_send, tiny_recv, own_sems, weight, sums, grads, staged, local_sems, out_sems = refs[7:17]
    contrib, rest, rest_sems = refs[17:20]
    line = Line(here, 4, [contrib, d_norm] + list(refs[20:]), chip_place(here, 2))
    tiny = Tiny(here, dots, tiny_all, (tiny_send, tiny_recv), False)
    half_cols = counts * width
    local = [
        pltpu.make_async_copy(w_gate, weight.at[:, :half_cols], local_sems.at[0]),
        pltpu.make_async_copy(w_up, weight.at[:, half_cols:], local_sems.at[1]),
    ]
    own = load_own(spread, (d_gate, d_up), width, counts, own_sems)
    for copy in own + local:
        copy.start()
    greet(here, tiny.peers, True)
    for copy in own:
        copy.wait()
    tiny.begin()
    spread.begin()
    sums[...] = jnp.zeros_like(sums)
    for copy in local + late:
        copy.wait()

    def columns(half, at):
        return pl.ds(pl.multiple_of((half * counts + at) * width, width), width)

    def clear(at, _):
        grads[:, columns(0, at)] = jnp.zeros((grads.shape[0], width), jnp.float32)
        return 0

    lax.fori_loop(0, 2 * counts, clear, 0)

    def blocks(across, half, at):
        cols = columns(half, at)
        gained = grads[:, cols]
        for other in range(2):
            row = row_span(here, across, other, rows)
            block = spread.got[across, (spread.core + other) % 2, half, at]
            sums[row, :] += dot_nt(block, weight[:, cols])
            gained = gained + dot_nn(act_t[:, row], block)
        grads[:, cols] = gained

    def leave(half, at):
        spot = pl.ds(pl.multiple_of(at * width, width), width)
        return pltpu.make_async_copy(staged.at[half], (grad_gate, grad_up)[half].at[:, spot],
                                     out_sems.at[half, at])

    eye = diagonal()
    gain_grad[...] = jnp.zeros_like(gain_grad)

    def close_chip(chip, target):
        def close_shard(other, _):
            shard = here.shard(chip, other)
            span = pl.ds(pl.multiple_of(shard * rows, rows), rows)
            loads = [pltpu.make_async_copy(src.at[span, :], rest.at[at], rest_sems.at[at])
                     for at, src in enumerate((x_low, attn))]
            for copy in loads:
                copy.start()
            for copy in loads:
                copy.wait()
            for at in range(rows // LANES):
                span = pl.ds(pl.multiple_of(shard * rows + at * LANES, LANES), LANES)
                piece = slice(at * LANES, (at + 1) * LANES)
                dot = from_tile(tiny_all[shard, at : at + 1, :], eye)
                resid = rest[0, piece, :].astype(jnp.float32) + rest[1, piece, :].astype(jnp.float32)
                value = sums[span, :]
                target[span, :] = (value * gain[0:1, :] - resid * dot).astype(target.dtype)
                gain_grad[...] += jnp.sum(value * resid, axis=0, keepdims=True)
            return 0

        lax.fori_loop(0, 2, close_shard, 0)

    def done(stage, at):
        @pl.when(jnp.logical_and(stage == 3, at > 0))
        def _():
            leave(0, at - 1).wait()
            leave(1, at - 1).wait()

        @pl.when(stage == 3)
        def _():
            for half in range(2):
                staged[half] = grads[:, columns(half, at)].astype(staged.dtype)
            leave(0, at).start()
            leave(1, at).start()

        @pl.when(jnp.logical_and(at == counts - 1, stage == 0))
        def _():
            close_chip(0, contrib)
            line.launch(0, 4)

        @pl.when(jnp.logical_and(at == counts - 1, stage == 2))
        def _():
            lax.fori_loop(1, 3, lambda chip, _: (close_chip(chip, d_norm), 0)[1], 0)

    def hook(step):
        @pl.when(jnp.logical_and(step >= counts, step < counts + 6))
        def _():
            line.step(step - counts)

    tiny.end()
    spread.run(blocks, hook, done)
    close_chip(3, d_norm)
    line.settle()
    spread.end()

    def drain(at, _):
        leave(0, at).wait()
        leave(1, at).wait()
        return 0

    lax.fori_loop(counts - 1, counts, drain, 0)


def back_gather(act_t, w_gate, w_up, d_gate, d_up, dots, x_low, attn, gain, cid, width=512):
    cols, total = act_t.shape
    rows, half = d_gate.shape
    counts = half // width
    low, f32 = jnp.bfloat16, jnp.float32
    dma = pltpu.SemaphoreType.DMA
    vm = pl.BlockSpec(memory_space=pltpu.VMEM)
    hbm = pl.BlockSpec(memory_space=pl.ANY)
    out_shape = [
        jax.ShapeDtypeStruct((total, cols), low),
        jax.ShapeDtypeStruct((1, cols), f32),
        jax.ShapeDtypeStruct((cols, half), low),
        jax.ShapeDtypeStruct((cols, half), low),
    ]
    scratch = spread_scratch(counts, rows, width) + [
        pltpu.VMEM((8, 8, LANES), f32), dma((7,)), dma((7,)), dma((2, counts)),
        pltpu.VMEM((cols, 2 * half), low),
        pltpu.VMEM((total, cols), f32),
        pltpu.VMEM((cols, 2 * half), f32),
        pltpu.VMEM((2, cols, width), low),
        dma((2,)), dma((2, counts)),
        pltpu.VMEM((total, cols), low),
        pltpu.VMEM((2, rows, cols), low),
        dma((2,)),
    ] + line_scratch(4, (4 * rows // 2, cols), low)
    operands = [act_t, w_gate, w_up, d_gate, d_up, dots, x_low, attn, gain]
    kernel = functools.partial(back_kernel, rows, width, counts)
    return kernel_call(kernel, out_shape, operands, [vm] + [hbm] * 4 + [vm, hbm, hbm, vm], scratch, cid, "back",
                       [vm, vm, hbm, hbm], (0,))


def down_kernel(rows, width, counts, cot, weight, hidden, d_norm, ffn, d_attn, grad, *refs, late):
    here = Place()
    spread = Spread(here, counts, refs[:7])
    own_sems, sums, grads, staged, out_sems, norm_out, part = refs[7:14]
    place = chip_place(here, 4)
    norm_line = Line(here, 24, [d_norm, norm_out] + list(refs[14:22]), lambda at: place(at + 8))
    line = Line(here, 4, [part, ffn] + list(refs[22:]), chip_place(here, 2))
    own = load_own(spread, (hidden,), width, counts, own_sems)
    for copy in own:
        copy.start()
    greet(here, slice_peers(here), True)
    norm_line.begin()
    for copy in own:
        copy.wait()
    spread.begin()
    sums[...] = jnp.zeros_like(sums)
    grads[...] = jnp.zeros_like(grads)
    for copy in late:
        copy.wait()

    def columns(half, at):
        return pl.ds(pl.multiple_of((half * counts + at) * width, width), width)

    def blocks(across, half, at):
        cols = columns(half, at)
        gained = grads[cols, :]
        for other in range(2):
            row = row_span(here, across, other, rows)
            block = spread.got[across, (spread.core + other) % 2, half, at]
            sums[row, :] += dot_nn(block, weight[cols, :])
            gained = gained + dot_tn(block, cot[row, :])
        grads[cols, :] = gained

    def leave(half, at):
        return pltpu.make_async_copy(staged.at[at % 2, half], grad.at[columns(half, at), :], out_sems.at[half, at])

    def done(stage, at):
        @pl.when(jnp.logical_and(stage == 3, at > 1))
        def _():
            leave(0, at - 2).wait()
            leave(1, at - 2).wait()

        @pl.when(stage == 3)
        def _():
            for half in range(2):
                staged[at % 2, half] = grads[columns(half, at), :].astype(staged.dtype)
            leave(0, at).start()
            leave(1, at).start()

        @pl.when(jnp.logical_and(at == counts - 1, stage == 0))
        def _():
            close_chip(0, part)
            line.launch(0, 4)

    def close_chip(chip, target):
        def close_shard(other, _):
            span = row_span(here, chip, other, rows)
            target[span, :] = sums[span, :].astype(target.dtype)
            return 0

        lax.fori_loop(0, 2, close_shard, 0)

    def hook(step):
        norm_line.step(step)

        @pl.when(step >= 4 * counts - 5)
        def _():
            line.step(step - (4 * counts - 5))

    norm_line.steps(spread.run(blocks, hook, done), 26)
    lax.fori_loop(1, 4, lambda chip, _: (close_chip(chip, ffn), 0)[1], 0)
    norm_line.settle()

    def add_norm(at, _):
        def add(source):
            span = row_span(here, at // 2, at % 2, rows)
            d_attn[span, :] = (cot[span, :].astype(jnp.float32) + source[span, :].astype(jnp.float32)).astype(
                d_attn.dtype)

        @pl.when(at < 2)
        def _():
            add(d_norm)

        @pl.when(at >= 2)
        def _():
            add(norm_out)
        return 0

    lax.fori_loop(0, 8, add_norm, 0)
    line.settle()
    spread.end()

    def drain(at, _):
        leave(0, at).wait()
        leave(1, at).wait()
        return 0

    lax.fori_loop(counts - 2, counts, drain, 0)


def down_gather(cot, weight, hidden, d_norm, cid, width=256):
    total, cols = cot.shape
    rows, every = hidden.shape
    counts = every // (2 * width)
    low, f32 = jnp.bfloat16, jnp.float32
    dma = pltpu.SemaphoreType.DMA
    vm = pl.BlockSpec(memory_space=pltpu.VMEM)
    hbm = pl.BlockSpec(memory_space=pl.ANY)
    out_shape = [
        jax.ShapeDtypeStruct((total, cols), low),
        jax.ShapeDtypeStruct((total, cols), low),
        jax.ShapeDtypeStruct(weight.shape, low),
    ]
    scratch = spread_scratch(counts, rows, width) + [
        dma((2, counts)),
        pltpu.VMEM((total, cols), f32),
        pltpu.VMEM(weight.shape, f32),
        pltpu.VMEM((2, 2, width, cols), low),
        dma((2, counts)),
        pltpu.VMEM((total, cols), low),
        pltpu.VMEM((total, cols), low),
    ] + line_scratch(24, (24 * rows // 4, cols), low) + line_scratch(4, (4 * rows // 2, cols), low)
    kernel = functools.partial(down_kernel, rows, width, counts)
    return kernel_call(kernel, out_shape, [cot, weight, hidden, d_norm], [vm, vm, hbm, vm], scratch, cid, "down",
                       [vm, vm, hbm], (0, 1))


def attend_kernel(rows, heads, cols, width, counts, qkv, rms, cos, sin, mask, w_out, g_col, w_down, attn, mixed_all,
                  kv, probs, queries, pair_rms, d_hidden, *refs, late):
    here = Place()
    spread = Spread(here, 1, refs[:7])
    part, pair_sems, tiny_own, tiny_pair, mixed_sems = refs[7:12]
    product = products(here, g_col, w_down, True, rows, width, counts)
    total = Reduce(here, counts, product, refs[12:23])
    piece = rows // 2

    def place(at):
        across, other, half_at = spread.block(at)
        return here.shard(across, other) * 2 + half_at

    line = Line(here, 16, [part, attn] + list(refs[23:]), place)
    got, core = spread.got, here.core
    greet(here, slice_peers(here), True)
    half = HD // 2
    scale = 1.0 / math.sqrt(HD)
    wide = heads * HD

    def rotated(first):
        lead = qkv[:, first : first + half] * rms[...]
        trail = qkv[:, first + half : first + HD] * rms[...]
        return lead * cos[0] - trail * sin[0], trail * cos[0] + lead * sin[0]

    low_k, high_k = rotated(wide)
    kv[0, :, :half] = low_k.astype(kv.dtype)
    kv[0, :, half:HD] = high_k.astype(kv.dtype)
    for at in range(2):
        first = HD + at * half
        kv[0, :, first : first + half] = (qkv[:, wide + first : wide + first + half] * rms[...]).astype(kv.dtype)
    eye = diagonal()
    tiny_own[...] = jnp.zeros_like(tiny_own)
    to_tile(tiny_own, 0, rms[:, :1], eye)
    pair_rms[0] = rms[...]
    pair = remote(kv.at[0], kv.at[1], pair_sems.at[0], pair_sems.at[1], spread.ydev)
    tiny = remote(tiny_own, tiny_pair, pair_sems.at[2], pair_sems.at[3], spread.ydev)
    for head in range(heads):
        if head == 1:
            pair.start()
            tiny.start()
        lead, trail = rotated(head * HD)
        queries[:, head * HD : head * HD + half] = (lead * scale).astype(queries.dtype)
        queries[:, head * HD + half : (head + 1) * HD] = (trail * scale).astype(queries.dtype)
    pair.wait()
    for copy in late:
        copy.wait()

    def one_head(head, _):
        query = queries[:, pl.ds(pl.multiple_of(head * HD, HD), HD)]
        scores = jnp.concatenate([dot_nt(query, kv[0, :, :HD]), dot_nt(query, kv[1, :, :HD])], axis=1)
        scores = jnp.where(mask[...] > 0, scores, NEG)
        expd = jnp.exp(scores - jnp.max(scores, axis=-1, keepdims=True))
        prob = expd / jnp.sum(expd, axis=-1, keepdims=True)
        probs[head] = prob
        prob_low = prob.astype(jnp.bfloat16)
        mixed = dot_nn(prob_low[:, :rows], kv[0, :, HD:]) + dot_nn(prob_low[:, rows:], kv[1, :, HD:])
        span = pl.ds(pl.multiple_of(head * HD, HD), HD)
        for half_at in range(2):
            low_mixed = mixed[half_at * piece : (half_at + 1) * piece, :].astype(got.dtype)
            got[0, core, half_at, 0, :, span] = low_mixed
        return 0

    lax.fori_loop(0, heads, one_head, 0)
    spread.begin_rows()

    def mixed_copy(at):
        across, other, half_at = spread.block(at)
        span = pl.ds(pl.multiple_of(place(at) * piece, piece), piece)
        return pltpu.make_async_copy(got.at[across, (core + other) % 2, half_at, 0], mixed_all.at[span, :],
                                     mixed_sems.at[at])

    def one_step(step, _):
        spread.receive_rows(step)

        @pl.when(step < 16)
        def _():
            across, other, half_at = spread.block(step)
            value = dot_nn(got[across, (core + other) % 2, half_at, 0], w_out[...])
            part[pl.ds(pl.multiple_of(place(step) * piece, piece), piece), :] = value.astype(part.dtype)
            mixed_copy(step).start()
            line.launch(step, 1)

        @pl.when(step >= 2)
        def _():
            total.advance(step - 2)

        @pl.when(step >= 4)
        def _():
            line.step(step - 4)
        return 0

    lax.fori_loop(0, 4 + max(16, total.steps + 1), one_step, 0)
    line.end(max(16, total.steps + 1))

    def emit(at, first, second):
        for half_at, value in enumerate((first, second)):
            d_hidden[:, pl.ds(pl.multiple_of((half_at * counts + at) * width, width), width)] = value

    total.end(emit)
    for hop in range(3):
        spread.x_copy(hop, 0).wait_send()
        spread.y_copy(hop, 0).wait_send()
    for stage in range(4):
        for stream in range(2):
            spread.sib_copy(stage, stream, 0).wait_send()
    for at in range(16):
        mixed_copy(at).wait()
    tiny.wait()
    for at in range(rows // LANES):
        values = jnp.broadcast_to(from_tile(tiny_pair[at : at + 1, :], eye), (LANES, LANES))
        pair_rms[1, at * LANES : (at + 1) * LANES, :] = values


def attend(qkv, rms, cos, sin, mask, w_out, g_col, w_down, cid, width=512):
    rows = qkv.shape[0]
    wide, cols = w_out.shape
    heads = wide // HD
    counts = w_down.shape[0] // (2 * width)
    low, f32 = jnp.bfloat16, jnp.float32
    dma = pltpu.SemaphoreType.DMA
    vm = pl.BlockSpec(memory_space=pltpu.VMEM)
    out_shape = [
        jax.ShapeDtypeStruct((8 * rows, cols), low),
        jax.ShapeDtypeStruct((8 * rows, wide), low),
        jax.ShapeDtypeStruct((2, rows, 2 * HD), low),
        jax.ShapeDtypeStruct((heads, rows, 2 * rows), f32),
        jax.ShapeDtypeStruct((rows, wide), low),
        jax.ShapeDtypeStruct((2,) + rms.shape, f32),
        jax.ShapeDtypeStruct((rows, w_down.shape[0]), f32),
    ]
    scratch = spread_scratch(1, rows // 2, wide) + [
        pltpu.VMEM((8 * rows, cols), low), dma((4,)),
        pltpu.VMEM((8, LANES), f32), pltpu.VMEM((8, LANES), f32), dma((16,)),
    ] + reduce_scratch(counts, rows, width) + line_scratch(16, (8 * rows, cols), low)
    kernel = functools.partial(attend_kernel, rows, heads, cols, width, counts)
    operands = [qkv, rms, cos, sin, mask, w_out, g_col, w_down]
    out_specs = [vm, pl.BlockSpec(memory_space=pl.ANY)] + [vm] * 5
    return kernel_call(kernel, out_shape, operands, [vm] * 8, scratch, cid, "attend", out_specs, (4, 5, 6, 7))


def tail_kernel(rows, heads, per, d_attn, w_out, queries, kv, probs, rms, cos, sin, act_t, w_qkv, ffn, x_low,
                attn, gain, gain_grad, mixed_all, d_tok, out, grad_query, grad_out, kv_sum, gain_tiles, *refs, late):
    here = Place()
    width = HD
    counts = heads // 2
    part = rows // 2
    refs = list(refs)
    line_counts = 8 * per
    cols = d_attn.shape[1]
    extra = cols // (rows // per)

    def take(count):
        taken_refs = refs[:count]
        del refs[:count]
        return taken_refs

    total_refs = take(11)
    spread = Spread(here, 1, take(7))
    d_mixed, tiny_own, tiny_all, d_kv, give, taken, give_sems, tiny_send, tiny_recv = take(9)
    grad, grad_mixed, gain_sum, tile, tile_send, tile_recv, put_sems, local_sems, mixed_two, mixed_sems = take(10)

    def far(at):
        return at // (2 * per), at // per % 2

    def near(at):
        return spread.block(jnp.minimum(at, line_counts - 1))

    def place_ffn(at):
        return here.shard(*far(at)) * per + at % per

    def place_tok(at):
        across, other, half_at = near(at)
        return jnp.where(at < line_counts, here.shard(across, other) * per + half_at, at)

    ffn_sum, leaving = take(2)
    by_chip = chip_place(here, per)
    line = Line(here, 6 * per, [ffn, ffn_sum] + take(8), lambda at: by_chip(at + 2 * per))
    contrib, summed = take(2)
    line_tok = Line(here, line_counts + extra, [contrib, summed] + take(8), place_tok)
    tiny = Tiny(here, tiny_own, tiny_all, (tiny_send, tiny_recv), False)
    got, core = spread.got, here.core
    product = products(here, d_attn, w_out, True, rows, width, counts)
    total = Reduce(here, counts, product, total_refs)
    greet(here, tiny.peers, True)
    line.begin()
    grad_mixed[...] = jnp.zeros_like(grad_mixed)

    def mixed_copy(step):
        span = pl.ds(pl.multiple_of(step * rows, rows), rows)
        return pltpu.make_async_copy(mixed_all.at[span, :], mixed_two.at[step % 2], mixed_sems.at[step % 2])

    mixed_copy(0).start()

    def beside(step):
        line.step(step)

        @pl.when(step < 8)
        def _():
            span = pl.ds(pl.multiple_of(step * rows, rows), rows)
            mixed_copy(step).wait()

            @pl.when(step < 7)
            def _():
                mixed_copy(step + 1).start()

            grad_mixed[...] += dot_tn(mixed_two[step % 2], d_attn[span, :])

    done = total.run(beside)
    grad_out[...] = grad_mixed[...].astype(grad_out.dtype)

    def land(at, first, second):
        for half_at, value in enumerate((first, second)):
            d_mixed[:, pl.ds(pl.multiple_of((half_at * counts + at) * width, width), width)] = value.astype(
                d_mixed.dtype)

    total.end(land)
    half = HD // 2
    scale = 1.0 / math.sqrt(HD)
    depth = w_qkv.shape[0] * 8
    d_kv[...] = jnp.zeros_like(d_kv)
    for copy in late:
        copy.wait()

    def one_head(head, dots):
        span = pl.ds(pl.multiple_of(head * HD, HD), HD)
        query = queries[:, span]
        cot = d_mixed[:, span]
        prob = probs[head]
        d_prob = jnp.concatenate([dot_nt(cot, kv[0, :, HD:]), dot_nt(cot, kv[1, :, HD:])], axis=1)
        delta = jnp.sum(prob * d_prob, axis=-1, keepdims=True)
        d_score = (prob * (d_prob - delta)).astype(jnp.bfloat16)
        prob_low = prob.astype(jnp.bfloat16)
        d_query = (dot_nn(d_score[:, :rows], kv[0, :, :HD]) + dot_nn(d_score[:, rows:], kv[1, :, :HD])) * scale
        for side in range(2):
            keys = slice(side * rows, (side + 1) * rows)
            d_kv[side, :, :HD] += dot_tn(d_score[:, keys], query)
            d_kv[side, :, HD:] += dot_tn(prob_low[:, keys], cot)
        dots = dots + jnp.sum(d_query * query.astype(jnp.float32), axis=-1, keepdims=True)
        lead, trail = d_query[:, :half], d_query[:, half:]
        first = ((lead * cos[0] + trail * sin[0]) * rms[0]).astype(got.dtype)
        second = ((trail * cos[0] - lead * sin[0]) * rms[0]).astype(got.dtype)
        line.step(done + head)
        for rows_at in range(2):
            piece = slice(rows_at * part, (rows_at + 1) * part)
            got[0, core, rows_at, 0, :, pl.ds(pl.multiple_of(head * HD, HD), half)] = first[piece, :]
            got[0, core, rows_at, 0, :, pl.ds(pl.multiple_of(head * HD + half, half), half)] = second[piece, :]

        return dots

    dots = lax.fori_loop(0, heads, one_head, jnp.zeros((rows, 1), jnp.float32))
    eye = diagonal()
    tiny_own[...] = jnp.zeros_like(tiny_own)
    for side in (1, 0):
        d_key, d_value = d_kv[side, :, :HD], d_kv[side, :, HD:]
        own = jnp.sum(d_key * kv[side, :, :HD].astype(jnp.float32) +
                      d_value * kv[side, :, HD:].astype(jnp.float32), axis=-1, keepdims=True)
        if side == 0:
            own = own + dots * (1.0 / scale)
        own = own * (rms[side] * rms[side] * (1.0 / depth))
        to_tile(tiny_own, side * (rows // LANES), own, eye)
        lead, trail = d_key[:, :half], d_key[:, half:]
        parts = [(lead * cos[side] + trail * sin[side]) * rms[side],
                 (trail * cos[side] - lead * sin[side]) * rms[side],
                 d_value[:, :half] * rms[side], d_value[:, half:] * rms[side]]
        for at, value in enumerate(parts):
            if side == 1:
                give[:, at * half : (at + 1) * half] = value.astype(give.dtype)
            else:
                d_kv[0, :, at * half : (at + 1) * half] = value
    given = remote(give, taken, give_sems.at[0], give_sems.at[1], spread.ydev)
    given.start()
    grad[...] = jnp.zeros_like(grad)
    given.wait()
    for rows_at in range(2):
        piece = slice(rows_at * part, (rows_at + 1) * part)
        value = d_kv[0, piece, :] + taken[piece, :].astype(jnp.float32)
        got[0, core, rows_at, 0, :, heads * HD :] = value.astype(got.dtype)
    tiny.begin()
    spread.begin_rows()
    gain_sum[...] = jnp.zeros_like(gain_sum)
    tiny.end()

    def block_of(at):
        across, other, half_at = near(at)
        shard, partner = here.shard(across, other), here.shard((across + 2) % 4, other)
        block = got[across, (core + other) % 2, half_at, 0]
        first = pl.multiple_of(shard * rows + half_at * part, part)
        for tile_at in range(part // LANES):
            row = pl.ds(pl.multiple_of(first + tile_at * LANES, LANES), LANES)
            low_at = half_at * (part // LANES) + tile_at
            kept = rows // LANES + low_at
            dot = from_tile(tiny_all[shard, pl.ds(low_at, 1), :] + tiny_all[partner, pl.ds(kept, 1), :], eye)
            value = dot_nt(block[tile_at * LANES : (tile_at + 1) * LANES, :], w_qkv[...])
            x_rows = x_low[row, :].astype(jnp.float32)
            contrib[row, :] = (value * gain[0:1, :] - x_rows * dot).astype(contrib.dtype)
            gain_sum[...] += jnp.sum(value * x_rows, axis=0, keepdims=True)
        line_tok.launch(at, 1)
        rows_t = act_t[:, pl.ds(first, part)]
        for at_col in range((heads + 2) * HD // 512):
            span = slice(at_col * 512, (at_col + 1) * 512)
            grad[:, span] += dot_nn(rows_t, block[:, span])

    me = here.shard(0, 0)
    columns = pl.ds(pl.multiple_of(me * cols, cols), cols)
    chunk = line.chunk

    def landing(which, at):
        sub = at % per if which == 0 else near(at)[2]
        return (out, d_tok)[which].at[pl.ds(pl.multiple_of(sub * chunk, chunk), chunk), columns]

    def leaver(which, at):
        return (leaving, line_tok.from_end)[which].at[at]

    def put(which, at):
        goal = here.device(*(far(at) if which == 0 else near(at)[:2]))
        return remote(leaver(which, at), landing(which, at), put_sems.at[which, 0, at], put_sems.at[which, 1, at],
                      goal)

    def keep(which, at):
        spot = at % per if which == 0 else near(at)[2]
        return pltpu.make_async_copy(leaver(which, at), landing(which, at), local_sems.at[which, spot])

    def emit(which, at):
        if which == 1:
            row = line_tok.rows(at)
            value = d_attn[row, :].astype(jnp.float32) + summed[row, :].astype(jnp.float32)
            line_tok.from_end[at] = value.astype(out.dtype)
            return
        row = pl.ds(pl.multiple_of(place_ffn(at) * chunk, chunk), chunk)

        def leave(source):
            value = x_low[row, :].astype(jnp.float32) + attn[row, :].astype(jnp.float32)
            leaving[at] = (value + source[row, :].astype(jnp.float32)).astype(out.dtype)

        @pl.when(at < 2 * per)
        def _():
            leave(ffn)

        @pl.when(at >= 2 * per)
        def _():
            leave(ffn_sum)

    def is_own(which, at):
        return at < per if which == 0 else jnp.logical_and(at < 4, at % 2 == 0)

    def send(which, at):
        own = is_own(which, at)

        @pl.when(own)
        def _():
            keep(which, at).start()

        @pl.when(jnp.logical_not(own))
        def _():
            put(which, at).start()

    def stage_step(step, _):
        spread.receive_rows(step)

        @pl.when(step < line_counts)
        def _():
            block_of(step)

        @pl.when(step < 5)
        def _():
            line.step(done + heads + step)

        @pl.when(step >= 4)
        def _():
            line_tok.step(step - 4)

        @pl.when(step > 0)
        def _():
            send(0, step - 1)

        @pl.when(jnp.logical_and(line.inner == 0, step >= 2 * per))
        def _():
            line.up(step - 2 * per).wait_send()
            line.down(step - 2 * per).wait_recv()

        emit(0, step)

        @pl.when(jnp.logical_and(line.inner == 1, step > 7))
        def _():
            send(1, step - 8)

        @pl.when(jnp.logical_and(line.inner == 1, step > 6))
        def _():
            emit(1, step - 7)
        return 0

    lax.fori_loop(0, line_counts, stage_step, 0)
    for half_at in range(cols // (rows // per)):
        span = pl.ds(line_counts * (rows // per) + half_at * (rows // per), rows // per)
        source = slice(half_at * (rows // per), (half_at + 1) * (rows // per))
        contrib[span, :] = grad[source, heads * HD :].astype(contrib.dtype)
    line_tok.launch(line_counts, extra)
    grad_query[...] = grad[:, : heads * HD].astype(grad_query.dtype)
    for at in range(cols // LANES):
        tile[at : at + 1, :] = gain_sum[:, at * LANES : (at + 1) * LANES]
        spot = cols // LANES + at
        tile[spot : spot + 1, :] = gain_grad[:, at * LANES : (at + 1) * LANES]

    def tile_copy(step):
        return remote(tile, gain_tiles.at[here.z], tile_send.at[step], tile_recv.at[step],
                      (here.dp, here.seq, (here.z + step + 1) % 4))

    send(0, line_counts - 1)
    line.drain()
    for step in range(3):
        tile_copy(step).start()
    gain_tiles[here.z] = tile[...]

    @pl.when(line.inner == 1)
    def _():
        start = line_counts - 4

        def both(at, _):
            line_tok.step(at)

            @pl.when(at < line_counts + 4)
            def _():
                send(1, at - 4)

            @pl.when(at < line_counts + 3)
            def _():
                emit(1, at - 3)
            return 0

        lax.fori_loop(start, line_counts + extra + 2, both, 0)

        def drain(at, _):
            line_tok.down(at).wait_send()
            return 0

        lax.fori_loop(0, line_counts + extra, drain, 0)

    @pl.when(line.inner == 0)
    def _():
        def arrive(at, _):
            line_tok.up(at).wait_send()
            line_tok.down(at).wait_recv()

            @pl.when(jnp.logical_and(at > 0, at <= line_counts))
            def _():
                send(1, at - 1)

            @pl.when(at < line_counts)
            def _():
                emit(1, at)
            return 0

        lax.fori_loop(0, line_counts + extra, arrive, 0)

    for half_at in range(extra):
        span = pl.ds((line_counts + half_at) * chunk, chunk)
        kv_sum[half_at * chunk : (half_at + 1) * chunk, :] = summed[span, :]
    for hop in range(3):
        spread.x_copy(hop, 0).wait_send()
        spread.y_copy(hop, 0).wait_send()
    for stage in range(4):
        spread.sib_copy(stage, 0, 0).wait_send()
        spread.sib_copy(stage, 1, 0).wait_send()

    def finish(at, _):
        for which in range(2):
            own = is_own(which, at)

            @pl.when(own)
            def _():
                keep(which, at).wait()

            @pl.when(jnp.logical_not(own))
            def _():
                put(which, at).wait()
        return 0

    lax.fori_loop(0, line_counts, finish, 0)
    for step in range(3):
        tile_copy(step).wait()


def tail(d_attn, w_out, queries, kv, probs, rms, cos, sin, act_t, w_qkv, ffn, x_low, attn, gain, gain_grad,
         mixed_all, cid,
 per=2):
    total, cols = d_attn.shape
    rows = total // 8
    wide = w_out.shape[0]
    heads = wide // HD
    low, f32 = jnp.bfloat16, jnp.float32
    dma = pltpu.SemaphoreType.DMA
    vm = pl.BlockSpec(memory_space=pltpu.VMEM)
    counts = 8 * per
    chunk = rows // per
    extra = cols // chunk
    long = (total + cols, cols)
    out_shape = [
        jax.ShapeDtypeStruct((rows, 8 * cols), low),
        jax.ShapeDtypeStruct((rows, 8 * cols), low),
        jax.ShapeDtypeStruct((cols, wide), low),
        jax.ShapeDtypeStruct(w_out.shape, low),
        jax.ShapeDtypeStruct((cols, 2 * HD), low),
        jax.ShapeDtypeStruct((4, 8, LANES), f32),
    ]
    scratch = reduce_scratch(heads // 2, rows, HD, 2) + spread_scratch(1, rows // 2, wide + 2 * HD)
    scratch += [
        pltpu.VMEM((rows, wide), low),
        pltpu.VMEM((8, LANES), f32),
        pltpu.VMEM((8, 8, LANES), f32),
        pltpu.VMEM((2, rows, 2 * HD), f32),
        pltpu.VMEM((rows, 2 * HD), low),
        pltpu.VMEM((rows, 2 * HD), low),
        dma((2,)), dma((7,)), dma((7,)),
        pltpu.VMEM(w_qkv.shape, f32),
        pltpu.VMEM(w_out.shape, f32),
        pltpu.VMEM((1, cols), f32),
        pltpu.VMEM((8, LANES), f32),
        dma((3,)), dma((3,)), dma((2, 2, counts)), dma((2, per)),
        pltpu.VMEM((2, rows, wide), low), dma((2,)),
        pltpu.VMEM((total, cols), low),
        pltpu.VMEM((counts, chunk, cols), low),
    ] + line_scratch(6 * per, (6 * per * chunk, cols), low)
    scratch += [pltpu.VMEM(long, low), pltpu.VMEM(long, low)] + line_scratch(counts + extra, long, low)
    operands = [d_attn, w_out, queries, kv, probs, rms, cos, sin, act_t, w_qkv, ffn, x_low, attn, gain,
                gain_grad, mixed_all]
    kernel = functools.partial(tail_kernel, rows, heads, per)
    specs = [vm] * (len(operands) - 1) + [pl.BlockSpec(memory_space=pl.ANY)]
    return kernel_call(kernel, out_shape, operands, specs, scratch, cid, "tail",
                       late=(2, 3, 4, 8, 9, 11, 12))


LANES = 128


def acts_move(
    tokens, seg_ids, gain_attn, w_query, kv_weight, w_out, gain_ffn, w_gate, w_up, w_down, d_out
):
    rows = tokens.shape[0]
    segs = seg_ids.astype(jnp.float32).reshape(2 * rows // LANES, LANES)
    segs = jnp.pad(segs, ((0, 8 - 2 * rows // LANES), (0, 0)))
    both = jnp.stack([gain_attn, gain_ffn, gain_ffn, gain_attn]).astype(jnp.float32)
    gain_one, gain_two = both[:2], both[2:]
    wider = jnp.float32

    qkv, x_low, act_one_t, w_qkv, rms, cos, sin, mask, g_parts = opening(
        tokens, gain_one, w_query, kv_weight, segs, d_out, 1
    )
    g_low = g_parts.reshape(x_low.shape)
    attn, mixed_all, kv, probs, queries, pair_rms, d_hidden = attend(
        qkv, rms, cos, sin, mask, w_out, g_low, w_down, 2
    )
    hidden, d_gate, d_up, act_two_t, dots = ffn_scatter(x_low, attn, gain_two, w_gate, w_up, d_hidden, 4)
    d_norm, grad_gain_two, grad_gate, grad_up = back_gather(
        act_two_t, w_gate, w_up, d_gate, d_up, dots, x_low, attn, gain_two, 5
    )
    ffn, d_attn, grad_down = down_gather(g_low, w_down, hidden, d_norm, 6)
    d_tokens, out, grad_query, grad_out, grad_kv, gain_tiles = tail(
        d_attn,
        w_out,
        queries,
        kv,
        probs,
        pair_rms,
        cos,
        sin,
        act_one_t,
        w_qkv,
        ffn,
        x_low,
        attn,
        gain_one,
        grad_gain_two,
        mixed_all,
        7,
    )
    gains = jnp.sum(gain_tiles, axis=0).reshape(2, -1)
    return (
        out,
        d_tokens.astype(wider),
        gains[0],
        grad_query.astype(wider),
        grad_kv.astype(wider),
        grad_out.astype(wider),
        gains[1],
        grad_gate.astype(wider),
        grad_up.astype(wider),
        grad_down.astype(wider),
    )


def solution(mesh):
    in_specs = (
        P(("dp", "seq"), None),
        P("dp"),
        P(("dp", "seq")),
        P(("dp", "seq"), "tensor"),
        P(("dp", "seq"), None),
        P("tensor", ("dp", "seq")),
        P(("dp", "seq")),
        P(("dp", "seq"), "tensor"),
        P(("dp", "seq"), "tensor"),
        P("tensor", ("dp", "seq")),
        P(("dp", "seq"), None),
    )
    out_specs = (
        P(("dp", "seq"), None),
        P(("dp", "seq"), None),
        P(("dp", "seq")),
        P(("dp", "seq"), "tensor"),
        P(("dp", "seq"), None),
        P("tensor", ("dp", "seq")),
        P(("dp", "seq")),
        P(("dp", "seq"), "tensor"),
        P(("dp", "seq"), "tensor"),
        P("tensor", ("dp", "seq")),
    )

    def shards(*arrays):
        tokens = arrays[0]
        sizes = tuple(mesh.shape[name] for name in ("dp", "seq", "tensor"))
        count = tokens.shape[0] * sizes[0] * sizes[1]
        plan = acts_move if sizes == (4, 2, 4) and count <= tokens.shape[1] else weights_move
        return plan(*arrays)

    return jax.shard_map(shards, mesh=mesh, in_specs=in_specs, out_specs=out_specs, check_vma=False)
```

```python
import functools
import math

import jax
import jax.numpy as jnp
from jax import lax
from jax.experimental import pallas as pl
from jax.experimental.pallas import tpu as pltpu
from jax.sharding import PartitionSpec as P

HD = 256


EPS = 1e-06
NEG = -1e30


def place_tables(segs):
    length = segs.shape[0]
    index = jnp.arange(length, dtype=jnp.int32)
    flags = jnp.concatenate([jnp.ones((1,), dtype=bool), segs[1:] != segs[:-1]])
    starts = lax.cummax(jnp.where(flags, index, jnp.zeros_like(index)), axis=0)
    places = index - starts
    half_size = HD // 2
    freqs = jnp.exp(jnp.arange(half_size, dtype=jnp.float32) * (-math.log(10000.0) / half_size))
    angles = places.astype(jnp.float32)[:, None] * freqs[None, :]
    return (places, jnp.cos(angles), jnp.sin(angles))


def rotate(vector, cos_table, sin_table):
    half_size = vector.shape[-1] // 2
    leading = vector[..., :half_size]
    trailing = vector[..., half_size:]
    return jnp.concatenate(
        [leading * cos_table - trailing * sin_table, trailing * cos_table + leading * sin_table],
        axis=-1,
    )


def rotate_back(vector, cos_table, sin_table):
    half_size = vector.shape[-1] // 2
    leading = vector[..., :half_size]
    trailing = vector[..., half_size:]
    return jnp.concatenate(
        [leading * cos_table + trailing * sin_table, trailing * cos_table - leading * sin_table],
        axis=-1,
    )


def matmul(left, right):
    return jnp.dot(left, right, preferred_element_type=jnp.float32)


def matmul_nt(left, right):
    return lax.dot_general(
        left, right, (((1,), (1,)), ((), ())), preferred_element_type=jnp.float32
    )


def matmul_tn(left, right):
    return lax.dot_general(
        left, right, (((0,), (0,)), ((), ())), preferred_element_type=jnp.float32
    )


def gelu_tanh(values):
    return jax.nn.gelu(values, approximate=True)


def norm_back(d_act, normed, rms_val, gain_val):
    scaled = d_act * gain_val
    return rms_val * (scaled - normed * jnp.mean(scaled * normed, axis=-1, keepdims=True))


def weights_move(
    tokens, seg_ids, gain_attn, w_query, kv_weight, w_out, gain_ffn, w_gate, w_up, w_down, d_out
):
    rows = tokens.shape[0]
    scale_factor = 1.0 / math.sqrt(HD)
    offset = lax.axis_index("seq") * rows
    places, cos_table, sin_table = place_tables(seg_ids)
    own_places = lax.dynamic_slice_in_dim(places, offset, rows, 0)
    own_segs = lax.dynamic_slice_in_dim(seg_ids, offset, rows, 0)
    own_cos = lax.dynamic_slice_in_dim(cos_table, offset, rows, 0)
    own_sin = lax.dynamic_slice_in_dim(sin_table, offset, rows, 0)
    allowed = (own_segs[:, None] == seg_ids[None, :]) & (own_places[:, None] >= places[None, :])
    full_query, full_out, full_kv, full_gain_one = (
        lax.all_gather(w_query, ("dp", "seq"), axis=0, tiled=True),
        lax.all_gather(w_out, ("dp", "seq"), axis=1, tiled=True),
        lax.all_gather(kv_weight, ("dp", "seq"), axis=0, tiled=True),
        lax.all_gather(gain_attn, ("dp", "seq"), axis=0, tiled=True),
    )
    gain_one = full_gain_one.astype(jnp.float32)
    inputs = tokens.astype(jnp.float32)
    rms_one = lax.rsqrt(jnp.mean(inputs * inputs, axis=-1, keepdims=True) + EPS)
    norm_one = inputs * rms_one
    act_one = (norm_one * gain_one).astype(jnp.bfloat16)
    query_pre = matmul(act_one, full_query)
    heads = query_pre.shape[1] // HD
    kv_pre = matmul(act_one, full_kv)
    queries = (
        rotate(query_pre.reshape(rows, heads, HD), own_cos[:, None, :], own_sin[:, None, :])
        * scale_factor
    ).astype(jnp.bfloat16)
    own_kv = jnp.concatenate(
        [rotate(kv_pre[:, :HD], own_cos, own_sin), kv_pre[:, HD:]], axis=1
    ).astype(jnp.bfloat16)
    all_kv = lax.all_gather(own_kv, "seq", axis=0, tiled=True)
    keys = all_kv[:, :HD]
    values_all = all_kv[:, HD:]
    scores = jnp.einsum("rhd,kd->hrk", queries, keys, preferred_element_type=jnp.float32)
    scores = jnp.where(allowed[None], scores, NEG)
    top_score = jnp.max(scores, axis=-1, keepdims=True)
    expd = jnp.exp(scores - top_score)
    total = jnp.sum(expd, axis=-1, keepdims=True)
    log_total = top_score + jnp.log(total)
    probs_low = (expd / total).astype(jnp.bfloat16)
    mixed = (
        jnp.einsum("hrk,kd->rhd", probs_low, values_all, preferred_element_type=jnp.float32)
        .reshape(rows, heads * HD)
        .astype(jnp.bfloat16)
    )
    attn = lax.psum(matmul(mixed, full_out), "tensor")
    resid = inputs + attn
    full_gate, full_up, full_down, full_gain_two = (
        lax.all_gather(w_gate, ("dp", "seq"), axis=0, tiled=True),
        lax.all_gather(w_up, ("dp", "seq"), axis=0, tiled=True),
        lax.all_gather(w_down, ("dp", "seq"), axis=1, tiled=True),
        lax.all_gather(gain_ffn, ("dp", "seq"), axis=0, tiled=True),
    )
    gain_two = full_gain_two.astype(jnp.float32)
    rms_two = lax.rsqrt(jnp.mean(resid * resid, axis=-1, keepdims=True) + EPS)
    norm_two = resid * rms_two
    act_two = (norm_two * gain_two).astype(jnp.bfloat16)
    gate = matmul(act_two, full_gate)
    up_val = matmul(act_two, full_up)
    gelu_val, gelu_pull = jax.vjp(gelu_tanh, gate)
    hidden = (gelu_val * up_val).astype(jnp.bfloat16)
    ffn = lax.psum(matmul(hidden, full_down).astype(jnp.bfloat16), "tensor").astype(jnp.float32)
    out = (resid + ffn).astype(jnp.bfloat16)
    back_gate, back_up, back_down = (
        lax.all_gather(w_gate, ("dp", "seq"), axis=0, tiled=True),
        lax.all_gather(w_up, ("dp", "seq"), axis=0, tiled=True),
        lax.all_gather(w_down, ("dp", "seq"), axis=1, tiled=True),
    )
    d_hidden = matmul_nt(d_out, back_down)
    grad_down = matmul_tn(hidden, d_out)
    d_gate = gelu_pull(d_hidden * up_val)[0].astype(jnp.bfloat16)
    d_up = (d_hidden * gelu_val).astype(jnp.bfloat16)
    grad_gate = matmul_tn(act_two, d_gate)
    grad_up = matmul_tn(act_two, d_up)
    d_act_two = lax.psum(matmul_nt(d_gate, back_gate) + matmul_nt(d_up, back_up), "tensor")
    grad_gain_two = jnp.sum(d_act_two * norm_two, axis=0)
    d_resid = d_out.astype(jnp.float32) + norm_back(d_act_two, norm_two, rms_two, gain_two)
    ffn_grads = (
        lax.psum_scatter(
            grad_gate.astype(jnp.bfloat16), ("dp", "seq"), scatter_dimension=0, tiled=True
        ).astype(jnp.float32),
        lax.psum_scatter(
            grad_up.astype(jnp.bfloat16), ("dp", "seq"), scatter_dimension=0, tiled=True
        ).astype(jnp.float32),
        lax.psum_scatter(
            grad_down.astype(jnp.bfloat16), ("dp", "seq"), scatter_dimension=1, tiled=True
        ).astype(jnp.float32),
        lax.psum_scatter(
            grad_gain_two.astype(jnp.bfloat16), ("dp", "seq"), scatter_dimension=0, tiled=True
        ).astype(jnp.float32),
    )
    back_query, back_out, back_kv = (
        lax.all_gather(w_query, ("dp", "seq"), axis=0, tiled=True),
        lax.all_gather(w_out, ("dp", "seq"), axis=1, tiled=True),
        lax.all_gather(kv_weight, ("dp", "seq"), axis=0, tiled=True),
    )
    d_attn = d_resid.astype(jnp.bfloat16)
    grad_out = matmul_tn(mixed, d_attn)
    d_mixed = matmul_nt(d_attn, back_out).astype(jnp.bfloat16).reshape(rows, heads, HD)
    scores_again = jnp.einsum("rhd,kd->hrk", queries, keys, preferred_element_type=jnp.float32)
    probs = jnp.where(allowed[None], jnp.exp(scores_again - log_total), 0.0)
    d_probs = jnp.einsum("rhd,kd->hrk", d_mixed, values_all, preferred_element_type=jnp.float32)
    delta = jnp.sum(probs * d_probs, axis=-1, keepdims=True)
    d_scores = (probs * (d_probs - delta)).astype(jnp.bfloat16)
    d_queries = (
        jnp.einsum("hrk,kd->rhd", d_scores, keys, preferred_element_type=jnp.float32) * scale_factor
    )
    d_query_pre = (
        rotate_back(d_queries, own_cos[:, None, :], own_sin[:, None, :])
        .reshape(rows, heads * HD)
        .astype(jnp.bfloat16)
    )
    d_keys_part = jnp.einsum("hrk,rhd->kd", d_scores, queries, preferred_element_type=jnp.float32)
    d_values_part = jnp.einsum(
        "hrk,rhd->kd", probs.astype(jnp.bfloat16), d_mixed, preferred_element_type=jnp.float32
    )
    own_kv_grad = lax.psum_scatter(
        jnp.concatenate([d_keys_part, d_values_part], axis=1).astype(jnp.bfloat16),
        "seq",
        scatter_dimension=0,
        tiled=True,
    )
    d_act_query = matmul_nt(d_query_pre, back_query)
    d_act_sum, kv_grad = (
        lax.psum(d_act_query.astype(jnp.bfloat16), "tensor").astype(jnp.float32),
        lax.psum(own_kv_grad, "tensor").astype(jnp.float32),
    )
    d_kv_pre = jnp.concatenate(
        [rotate_back(kv_grad[:, :HD], own_cos, own_sin), kv_grad[:, HD:]], axis=1
    ).astype(jnp.bfloat16)
    d_act_one = d_act_sum + matmul_nt(d_kv_pre, back_kv)
    grad_query = matmul_tn(act_one, d_query_pre)
    grad_kv = matmul_tn(act_one, d_kv_pre)
    grad_gain_one = jnp.sum(d_act_one * norm_one, axis=0)
    d_tokens = d_resid + norm_back(d_act_one, norm_one, rms_one, gain_one)
    attn_grads = (
        lax.psum_scatter(
            grad_query.astype(jnp.bfloat16), ("dp", "seq"), scatter_dimension=0, tiled=True
        ).astype(jnp.float32),
        lax.psum_scatter(
            grad_out.astype(jnp.bfloat16), ("dp", "seq"), scatter_dimension=1, tiled=True
        ).astype(jnp.float32),
        lax.psum_scatter(
            grad_kv.astype(jnp.bfloat16), ("dp", "seq"), scatter_dimension=0, tiled=True
        ).astype(jnp.float32),
        lax.psum_scatter(
            grad_gain_one.astype(jnp.bfloat16), ("dp", "seq"), scatter_dimension=0, tiled=True
        ).astype(jnp.float32),
    )
    return (
        out,
        d_tokens,
        attn_grads[3],
        attn_grads[0],
        attn_grads[2],
        attn_grads[1],
        ffn_grads[3],
        ffn_grads[0],
        ffn_grads[1],
        ffn_grads[2],
    )


MESH = pl.DeviceIdType.MESH
VMEM_LIMIT = 66000 * 1024


class Place:
    def __init__(self):
        self.dp = lax.axis_index("dp")
        self.seq = lax.axis_index("seq")
        self.z = lax.axis_index("tensor")
        self.core = lax.rem(self.dp, 2)
        self.chip = lax.div(self.dp, 2)

    def device(self, across, other):
        chip = (self.chip + across) % 2
        seq = (self.seq + across // 2) % 2
        core = (self.core + other) % 2
        return chip * 2 + core, seq, self.z

    def shard(self, across, other):
        dp, seq, _ = self.device(across, other)
        return dp * 2 + seq


def greet(here, peers, line=False):
    barrier = pltpu.get_barrier_semaphore()
    peers = list(peers)
    if line:
        peers += [(here.dp, here.seq, (here.z + step) % 4) for step in range(1, 4)]
    for peer in peers:
        pl.semaphore_signal(barrier, inc=1, device_id=peer, device_id_type=MESH)
    pl.semaphore_wait(barrier, len(peers))


def remote(src, dst, send, recv, peer):
    return pltpu.make_async_remote_copy(
        src_ref=src, dst_ref=dst, send_sem=send, recv_sem=recv, device_id=peer, device_id_type=MESH
    )


class Line:
    def __init__(self, here, counts, refs, place=None):
        self.own, self.out, self.from_end, self.from_mid = refs[:4]
        self.sems = refs[4:10]
        self.counts = counts
        self.chunk = self.from_end.shape[1]
        self.place = place
        z = here.z
        self.inner = ((z + 1) // 2) % 2
        self.mate = (here.dp, here.seq, z + 1 - 2 * (z % 2))
        self.other = (here.dp, here.seq, 3 - z)

    def rows(self, at):
        at = at if self.place is None else self.place(at)
        return pl.ds(pl.multiple_of(at * self.chunk, self.chunk), self.chunk)

    def up(self, at):
        return remote(self.own.at[self.rows(at), :], self.from_end.at[at], self.sems[0].at[at],
                      self.sems[1].at[at], self.mate)

    def over(self, at):
        return remote(self.out.at[self.rows(at), :], self.from_mid.at[at], self.sems[2].at[at],
                      self.sems[3].at[at], self.other)

    def down(self, at):
        rows = self.rows(at)
        return remote(self.out.at[rows, :], self.out.at[rows, :], self.sems[4].at[at],
                      self.sems[5].at[at], self.mate)

    def launch(self, first, count):
        @pl.when(self.inner == 0)
        def _():
            def send(at, _):
                self.up(first + at).start()
                return 0

            lax.fori_loop(0, count, send, 0)

    def begin(self):
        self.launch(0, self.counts)

    def first(self, at):
        rows = self.rows(at)
        self.up(at).wait_recv()
        total = self.own[rows, :].astype(jnp.float32) + self.from_end[at].astype(jnp.float32)
        self.out[rows, :] = total.astype(self.out.dtype)
        self.over(at).start()

    def second(self, at):
        rows = self.rows(at)
        self.over(at).wait()
        total = self.out[rows, :].astype(jnp.float32) + self.from_mid[at].astype(jnp.float32)
        self.out[rows, :] = total.astype(self.out.dtype)
        self.down(at).start()

    def step(self, at, start=0, count=None):
        count = self.counts if count is None else count

        @pl.when(jnp.logical_and(self.inner == 1, at < count))
        def _():
            self.first(start + at)

        @pl.when(jnp.logical_and(self.inner == 1, jnp.logical_and(at > 1, at < count + 2)))
        def _():
            self.second(start + at - 2)

    def steps(self, first, last, start=0, count=None):
        def rest(at, _):
            self.step(at, start, count)
            return 0

        lax.fori_loop(first, last, rest, 0)

    def settle(self):
        @pl.when(self.inner == 0)
        def _():
            def take(at, _):
                self.up(at).wait_send()
                self.down(at).wait_recv()
                return 0

            lax.fori_loop(0, self.counts, take, 0)

        self.drain()

    def drain(self):
        @pl.when(self.inner == 1)
        def _():
            def drain(at, _):
                self.down(at).wait_send()
                return 0

            lax.fori_loop(0, self.counts, drain, 0)

    def end(self, done=0):
        self.steps(min(done, self.counts + 2), self.counts + 2)
        self.settle()


def line_scratch(counts, shape, low):
    buf = pltpu.VMEM((counts, shape[0] // counts, shape[1]), low)
    return [buf, buf] + [pltpu.SemaphoreType.DMA((counts,))] * 6


def turned(at):
    return 3 - at // 2, 1 - at % 2


def slice_peers(here):
    return [here.device(*turned(at)) for at in range(7)]


def kernel_call(kernel, out_shape, operands, specs, scratch, cid, name, out_specs=None, late=()):
    vm = pl.BlockSpec(memory_space=pltpu.VMEM)
    specs = [pl.BlockSpec(memory_space=pl.ANY) if at in late else spec for at, spec in enumerate(specs)]
    inside = [pltpu.VMEM(operands[at].shape, operands[at].dtype) for at in late]
    if late:
        inside.append(pltpu.SemaphoreType.DMA((len(late),)))

    def body(*refs):
        if not late:
            kernel(*refs)
            return
        ins, rest, own = list(refs[: len(operands)]), refs[len(operands) : -len(inside)], refs[-len(inside) :]
        copies = []
        for spot, at in enumerate(late):
            copy = pltpu.make_async_copy(ins[at], own[spot], own[-1].at[spot])
            copy.start()
            copies.append(copy)
            ins[at] = own[spot]
        kernel(*ins, *rest, late=copies)

    return pl.pallas_call(
        body,
        out_shape=out_shape,
        in_specs=specs,
        out_specs=out_specs or [vm] * len(out_shape),
        scratch_shapes=scratch + inside,
        compiler_params=pltpu.CompilerParams(
            collective_id=cid, has_side_effects=True, vmem_limit_bytes=VMEM_LIMIT
        ),
        name=f"{name}_{cid}",
    )(*operands)


class Tiny:
    def __init__(self, here, src, dst, sems, spread):
        self.here, self.src, self.dst, self.sems, self.spread = here, src, dst, sems, spread
        self.peers = slice_peers(here)
        self.me = here.shard(0, 0)

    def tile(self, shard):
        return self.src.at[shard] if self.spread else self.src

    def copy(self, at):
        return remote(self.tile(self.here.shard(*turned(at))), self.dst.at[self.me], self.sems[0].at[at],
                      self.sems[1].at[at], self.peers[at])

    def begin(self):
        for at in range(7):
            self.copy(at).start()
        self.dst[self.me] = self.tile(self.me)[...]

    def end(self):
        for at in range(7):
            self.copy(at).wait()


class Reduce:
    def __init__(self, here, counts, product, refs, before=None):
        self.counts, self.product, self.before = counts, product, before
        self.held, self.sib_out, self.sib_in, self.from_x, self.from_y = refs[:5]
        self.sib_sems, self.x_sems, self.y_sems = refs[5:7], refs[7:9], refs[9:11]
        self.sib, self.xdev, self.ydev = here.device(0, 1), here.device(1, 0), here.device(2, 0)
        self.steps = 4 * counts
        self.ring = self.sib_out.shape[0]

    def streams(self, stage):
        far = stage // 3
        x_chip = jnp.where(stage == 0, 3, jnp.where(stage == 2, 0, 1))
        y_chip = jnp.where(stage == 0, 3, jnp.where(stage == 2, 0, 2))
        return (x_chip, far), (y_chip, 1 - far)

    def to_sib(self, step, stream):
        stage, at = step // self.counts, step % self.counts
        return remote(self.sib_out.at[step % self.ring, stream], self.sib_in.at[stage, stream, at],
                      self.sib_sems[0].at[stage, stream, at], self.sib_sems[1].at[stage, stream, at], self.sib)

    def to_x(self, hop, at, stage=0):
        return remote(self.held.at[stage, 0, at], self.from_x.at[hop, at], self.x_sems[0].at[hop, at],
                      self.x_sems[1].at[hop, at], self.xdev)

    def to_y(self, hop, at, stage=0):
        return remote(self.held.at[stage, 1, at], self.from_y.at[hop, at], self.y_sems[0].at[hop, at],
                      self.y_sems[1].at[hop, at], self.ydev)

    def compute(self, step):
        stage, at = step // self.counts, step % self.counts
        if self.before:
            for stop in range(3):
                @pl.when(step == stop * self.counts)
                def _():
                    self.before(stop)

        @pl.when(step >= self.ring)
        def _():
            for stream in range(2):
                self.to_sib(step - self.ring, stream).wait_send()

        for stream, (across, half) in enumerate(self.streams(stage)):
            self.sib_out[step % self.ring, stream] = self.product(across, 1, half, at).astype(jnp.bfloat16)
            self.held[stage, stream, at] = self.product(across, 0, half, at).astype(jnp.bfloat16)
        for stream in range(2):
            self.to_sib(step, stream).start()

    def finish(self, step):
        stage, at = step // self.counts, step % self.counts
        for stream in range(2):
            self.to_sib(step, stream).wait_recv()

        def total(stream):
            return self.held[stage, stream, at].astype(jnp.float32) + self.sib_in[stage, stream, at].astype(
                jnp.float32)

        @pl.when(stage < 3)
        def _():
            for stream in range(2):
                self.held[stage, stream, at] = total(stream).astype(jnp.bfloat16)

        @pl.when(stage == 3)
        def _():
            self.to_y(0, at).wait_recv()
            self.held[3, 0, at] = (total(0) + self.from_y[0, at].astype(jnp.float32)).astype(jnp.bfloat16)
            self.to_x(0, at).wait_recv()
            self.held[3, 1, at] = (total(1) + self.from_x[0, at].astype(jnp.float32)).astype(jnp.bfloat16)

        @pl.when(stage != 2)
        def _():
            hop = stage - stage // 3
            self.to_x(hop, at, stage).start()
            self.to_y(hop, at, stage).start()

    def advance(self, step):
        @pl.when(step < self.steps)
        def _():
            self.compute(step)

        @pl.when(jnp.logical_and(step > 0, step <= self.steps))
        def _():
            self.finish(step - 1)

    def run(self, hook=None):
        def body(step, _):
            self.advance(step)

            if hook:
                hook(step)
            return 0

        lax.fori_loop(0, self.steps + 1, body, 0)
        return self.steps + 1

    def end(self, emit):
        def last(at, _):
            values = []
            for half in range(2):
                xs, ys = (1, 2) if half == 0 else (2, 1)
                self.to_x(xs, at).wait_recv()
                self.to_y(ys, at).wait_recv()
                values.append(self.held[2, half, at].astype(jnp.float32) + self.from_x[xs, at].astype(jnp.float32)
                              + self.from_y[ys, at].astype(jnp.float32))
            emit(at, *values)
            for hop in range(3):
                self.to_x(hop, at).wait_send()
                self.to_y(hop, at).wait_send()
            return 0

        lax.fori_loop(0, self.counts, last, 0)

        def drain(at, _):
            for stream in range(2):
                self.to_sib(self.steps - self.ring + at, stream).wait_send()
            return 0

        lax.fori_loop(0, self.ring, drain, 0)


def reduce_scratch(counts, rows, width, ring=4):
    low, dma = jnp.bfloat16, pltpu.SemaphoreType.DMA
    block = pltpu.VMEM((4, 2, counts, rows, width), low)
    landed = pltpu.VMEM((3, counts, rows, width), low)
    sent = pltpu.VMEM((ring, 2, rows, width), low)
    return [block, sent, block, landed, landed] + [dma((4, 2, counts))] * 2 + [dma((3, counts))] * 4


class Spread:
    def __init__(self, here, counts, refs):
        self.counts = counts
        self.got = refs[0]
        self.x_sems, self.y_sems, self.sib_sems = refs[1:3], refs[3:5], refs[5:7]
        self.core = here.core
        self.sib, self.xdev, self.ydev = here.device(0, 1), here.device(1, 0), here.device(2, 0)

    def slot(self, across, half, at):
        return self.got.at[across, self.core, half, at]

    def x_copy(self, hop, at):
        half = jnp.minimum(hop, 1)
        src = self.slot(2 * (hop // 2), half, at)
        dst = self.slot(1 + 2 * (hop // 2), half, at)
        return remote(src, dst, self.x_sems[0].at[hop, at], self.x_sems[1].at[hop, at], self.xdev)

    def y_copy(self, hop, at):
        half = 1 - jnp.minimum(hop, 1)
        src = self.slot(hop // 2, half, at)
        dst = self.slot(2 + hop // 2, half, at)
        return remote(src, dst, self.y_sems[0].at[hop, at], self.y_sems[1].at[hop, at], self.ydev)

    def streams(self, stage):
        some, last, late = jnp.minimum(stage, 1), stage // 3, stage // 2
        return (some + 2 * last, late), (2 * some + last, 1 - late)

    def block(self, at):
        x_stream, y_stream = self.streams(at // 4)
        second = at // 2 % 2
        across = x_stream[0] + second * (y_stream[0] - x_stream[0])
        half = x_stream[1] + second * (y_stream[1] - x_stream[1])
        return across, at % 2, half

    def begin_rows(self):
        for hop in range(2):
            self.x_copy(hop, 0).start()
            self.y_copy(hop, 0).start()
        for stream in range(2):
            self.sib_copy(0, stream, 0).start()

    def receive_rows(self, step):
        stage = step // 4

        @pl.when(jnp.logical_and(step % 4 == 0, jnp.logical_and(stage > 0, stage < 4)))
        def _():
            self.x_copy(stage - 1, 0).wait_recv()
            self.sib_copy(stage, 0, 0).start()
            self.y_copy(stage - 1, 0).wait_recv()
            self.sib_copy(stage, 1, 0).start()

        @pl.when(step == 4)
        def _():
            self.x_copy(2, 0).start()
            self.y_copy(2, 0).start()

        for stream in range(2):
            @pl.when(jnp.logical_and(step % 4 == 2 * stream, step < 16))
            def _(stream=stream):
                self.sib_copy(stage, stream, 0).wait_recv()

    def sib_copy(self, stage, stream, at):
        across, half = self.streams(stage)[stream]
        slot = self.slot(across, half, at)
        spot = (stage, stream, at)
        return remote(slot, slot, self.sib_sems[0].at[spot], self.sib_sems[1].at[spot], self.sib)

    def begin(self):
        def first(at, _):
            self.x_copy(0, at).start()
            self.y_copy(0, at).start()
            return 0

        def own(at, _):
            self.sib_copy(0, 0, at).start()
            self.sib_copy(0, 1, at).start()
            return 0

        lax.fori_loop(0, self.counts, first, 0)
        lax.fori_loop(0, self.counts, own, 0)

    def run(self, blocks, hook=None, done=None):
        counts = self.counts

        def body(step, _):
            stage, at = step // counts, step % counts

            @pl.when(jnp.logical_and(stage > 0, stage < 4))
            def _():
                self.x_copy(stage - 1, at).wait_recv()
                self.sib_copy(stage, 0, at).start()
                self.y_copy(stage - 1, at).wait_recv()
                self.sib_copy(stage, 1, at).start()

            @pl.when(jnp.logical_and(stage > 0, stage < 3))
            def _():
                self.x_copy(stage, at).start()
                self.y_copy(stage, at).start()

            @pl.when(step > 0)
            def _():
                old, spot = (step - 1) // counts, (step - 1) % counts
                for stream, (across, half) in enumerate(self.streams(old)):
                    self.sib_copy(old, stream, spot).wait_recv()
                    blocks(across, half, spot)
                if done:
                    done(old, spot)

            if hook:
                hook(step)
            return 0

        lax.fori_loop(0, 4 * counts + 1, body, 0)
        return 4 * counts + 1

    def end(self):
        def drain(at, _):
            for hop in range(3):
                self.x_copy(hop, at).wait_send()
                self.y_copy(hop, at).wait_send()
            for stage in range(4):
                self.sib_copy(stage, 0, at).wait_send()
                self.sib_copy(stage, 1, at).wait_send()
            return 0

        lax.fori_loop(0, self.counts, drain, 0)


def spread_scratch(counts, rows, width):
    dma = pltpu.SemaphoreType.DMA
    return [pltpu.VMEM((4, 2, 2, counts, rows, width), jnp.bfloat16)] + [dma((3, counts))] * 4 + [
        dma((4, 2, counts))] * 2


def row_span(here, across, other, rows):
    return pl.ds(pl.multiple_of(here.shard(across, other) * rows, rows), rows)


def dot_nt(left, right):
    return lax.dot_general(left, right, (((1,), (1,)), ((), ())), preferred_element_type=jnp.float32)


def dot_tn(left, right):
    return lax.dot_general(left, right, (((0,), (0,)), ((), ())), preferred_element_type=jnp.float32)


def dot_nn(left, right):
    return jnp.dot(left, right, preferred_element_type=jnp.float32)


def products(here, act, weight, nt, rows, width, counts):
    def product(across, other, half, at):
        cols = pl.ds(pl.multiple_of((half * counts + at) * width, width), width)
        block = act[row_span(here, across, other, rows), :]
        return dot_nt(block, weight[cols, :]) if nt else dot_nn(block, weight[:, cols])

    return product


def diagonal():
    return (lax.broadcasted_iota(jnp.int32, (LANES, LANES), 0) ==
            lax.broadcasted_iota(jnp.int32, (LANES, LANES), 1)).astype(jnp.float32)


def to_tile(tile, first, column, eye):
    for at in range(column.shape[0] // LANES):
        spread = column[at * LANES : (at + 1) * LANES, :] * eye
        tile[first + at : first + at + 1, :] = jnp.sum(spread, axis=0, keepdims=True)


def from_tile(row, eye):
    return jnp.sum(eye * row, axis=1, keepdims=True)


def make_tables(here, rows, segs, cos, sin, mask):
    eye = diagonal()
    tiles = rows // LANES
    freqs = jnp.exp(lax.broadcasted_iota(jnp.int32, (1, LANES), 1).astype(jnp.float32) * (-math.log(10000.0) / LANES))
    lane = lax.broadcasted_iota(jnp.int32, (1, LANES), 1)
    line = lax.broadcasted_iota(jnp.int32, (LANES, 1), 0)

    def ids_of(row):
        return segs[2:3, pl.ds(pl.multiple_of(row * LANES, LANES), LANES)]

    def row_of(side, at):
        return ((here.seq + side) % 2) * tiles + at

    for side in range(2):
        for at in range(tiles):
            row = row_of(side, at)
            ids = from_tile(ids_of(row), eye)
            before = jnp.zeros((LANES, 1), jnp.float32)
            for other in range(2 * tiles):
                smaller = ids_of(other) < ids
                before += jnp.sum(smaller.astype(jnp.float32), axis=-1, keepdims=True)
            index = row * LANES + line
            angles = (index.astype(jnp.float32) - before) * freqs
            span = slice(at * LANES, (at + 1) * LANES)
            cos[side, span, :] = jnp.cos(angles)
            sin[side, span, :] = jnp.sin(angles)
            if side == 0:
                for key_side in range(2):
                    for key_at in range(tiles):
                        key_row = row_of(key_side, key_at)
                        same = ids_of(key_row) == ids
                        allowed = jnp.logical_and(same, key_row * LANES + lane <= index)
                        first = key_side * rows + key_at * LANES
                        mask[span, first : first + LANES] = allowed.astype(jnp.float32)


def open_kernel(rows, width, counts, tokens, gain, w_query, kv_weight, cot, qkv, x_low, act_t, w_qkv, rms, cos, sin,
                mask, g_col, *refs):
    here = Place()
    cols, segs = gain.shape[1], gain
    act, turn_send, turn_recv, local_sems, cot_part, g_send, g_recv, z_send, z_recv = refs[:9]
    share = rows // 4
    me = here.shard(0, 0)
    own_rows = pl.ds(pl.multiple_of(me * rows, rows), rows)

    def turn_copy(at):
        across, other = turned(at)
        first = pl.multiple_of(here.shard(across, other) * cols, cols)
        return remote(tokens.at[:, pl.ds(first, cols)], x_low.at[own_rows, :], turn_send.at[at], turn_recv.at[at],
                      here.device(across, other))

    wide = w_query.shape[1]
    local = [
        pltpu.make_async_copy(w_query, w_qkv.at[:, :wide], local_sems.at[0]),
        pltpu.make_async_copy(kv_weight, w_qkv.at[:, wide:], local_sems.at[1]),
        pltpu.make_async_copy(tokens.at[:, pl.ds(pl.multiple_of(me * cols, cols), cols)], x_low.at[own_rows, :],
                              local_sems.at[2]),
    ]
    load = pltpu.make_async_copy(cot.at[pl.ds(pl.multiple_of(here.z * share, share), share), :], cot_part,
                                 local_sems.at[3])
    load.start()
    for copy in local:
        copy.start()

    def g_copy(at):
        across, other = turned(at)
        first = pl.multiple_of(here.shard(across, other) * cols, cols)
        return remote(cot_part.at[:, pl.ds(first, cols)], g_col.at[me, here.z], g_send.at[at], g_recv.at[at],
                      here.device(across, other))

    def own_part():
        return pltpu.make_async_copy(cot_part.at[:, pl.ds(pl.multiple_of(me * cols, cols), cols)],
                                     g_col.at[me, here.z], local_sems.at[4])

    def quarter(way, at, step, peer):
        spot = g_col.at[:, at]
        return remote(spot, spot, z_send.at[way, step], z_recv.at[way, step], (here.dp, here.seq, here.z + peer))

    def pass_on(step):
        @pl.when(jnp.logical_and(here.z < 3, here.z >= step))
        def _():
            quarter(0, here.z - step, step, 1).start()

        @pl.when(jnp.logical_and(here.z > 0, here.z <= 3 - step))
        def _():
            quarter(1, here.z + step, step, -1).start()

    def take_quarters(step):
        @pl.when(here.z > step)
        def _():
            quarter(0, here.z - 1 - step, step, -1).wait_recv()

        @pl.when(here.z < 3 - step)
        def _():
            quarter(1, here.z + 1 + step, step, 1).wait_recv()

    greet(here, slice_peers(here), True)
    load.wait()
    own_part().start()
    for at in range(7):
        g_copy(at).start()
    for at in range(7):
        turn_copy(at).start()
    for copy in local:
        copy.wait()

    def squares(at, total):
        values = tokens[:, pl.ds(pl.multiple_of(at * cols, cols), cols)].astype(jnp.float32)
        return total + jnp.sum(values * values, axis=-1, keepdims=True)

    total = lax.fori_loop(0, 8, squares, jnp.zeros((rows, 1), jnp.float32))
    rms[...] = jnp.broadcast_to(lax.rsqrt(total / (8 * cols) + EPS), rms.shape)
    make_tables(here, rows, segs, cos, sin, mask)

    def prepare(first, count):
        def one(step, _):
            at = first + step
            span = row_span(here, *turned(at), rows)
            value = (x_low[span, :].astype(jnp.float32) * gain[0:1, :]).astype(act.dtype)
            act[span, :] = value
            return 0

        lax.fori_loop(0, count, one, 0)

    def before(stop):
        first, count = ((0, 2), (2, 4), (6, 2))[stop]
        if stop == 0:
            own_part().wait()
            for at in range(7):
                g_copy(at).wait_recv()
        else:
            take_quarters(stop - 1)
        pass_on(stop)
        for at in range(first, min(first + count, 7)):
            turn_copy(at).wait_recv()
        prepare(first, count)

    def flip():
        def one(shard, _):
            span = pl.ds(pl.multiple_of(shard * rows, rows), rows)
            act_t[:, span] = act[span, :].T
            return 0

        lax.fori_loop(0, 8, one, 0)

    product = products(here, act, w_qkv, False, rows, width, counts)
    total = Reduce(here, counts, product, refs[9:20], before)
    total.run()
    flip()

    def emit(at, first, second):
        for half, value in enumerate((first, second)):
            qkv[:, pl.ds(pl.multiple_of((half * counts + at) * width, width), width)] = value

    total.end(emit)
    take_quarters(2)
    for at in range(7):
        turn_copy(at).wait_send()
        g_copy(at).wait_send()
    for step in range(3):
        @pl.when(jnp.logical_and(here.z < 3, here.z >= step))
        def _(step=step):
            quarter(0, here.z - step, step, 1).wait_send()

        @pl.when(jnp.logical_and(here.z > 0, here.z <= 3 - step))
        def _(step=step):
            quarter(1, here.z + step, step, -1).wait_send()


def opening(tokens, gain, w_query, kv_weight, cot, cid, width=256):
    rows = tokens.shape[0]
    cols, wide = w_query.shape
    every = wide + kv_weight.shape[1]
    counts = every // (2 * width)
    low, f32 = jnp.bfloat16, jnp.float32
    dma = pltpu.SemaphoreType.DMA
    vm = pl.BlockSpec(memory_space=pltpu.VMEM)
    hbm = pl.BlockSpec(memory_space=pl.ANY)
    out_shape = [
        jax.ShapeDtypeStruct((rows, every), f32),
        jax.ShapeDtypeStruct((8 * rows, cols), low),
        jax.ShapeDtypeStruct((cols, 8 * rows), low),
        jax.ShapeDtypeStruct((cols, every), low),
        jax.ShapeDtypeStruct((rows, LANES), f32),
        jax.ShapeDtypeStruct((2, rows, LANES), f32),
        jax.ShapeDtypeStruct((2, rows, LANES), f32),
        jax.ShapeDtypeStruct((rows, 2 * rows), f32),
        jax.ShapeDtypeStruct((8, 4, rows // 4, cols), low),
    ]
    scratch = [
        pltpu.VMEM((8 * rows, cols), low), dma((7,)), dma((7,)), dma((5,)),
        pltpu.VMEM((rows // 4, 8 * cols), low), dma((7,)), dma((7,)), dma((2, 3)), dma((2, 3)),
    ]
    scratch += reduce_scratch(counts, rows, width)
    kernel = functools.partial(open_kernel, rows, width, counts)
    return kernel_call(kernel, out_shape, [tokens, gain, w_query, kv_weight, cot],
                       [vm, vm, hbm, hbm, hbm], scratch, cid, "open")


def ffn_kernel(rows, width, counts, x_low, attn, gain, w_gate, w_up, d_hidden, hidden, d_gate, d_up, act_t, tile_out,
               *refs, late):
    here = Place()
    cols = gain.shape[1]
    act, weight, tiny_own, tiny_all, tiny_send, tiny_recv, dots, local_sems = refs[:8]
    tiny = Tiny(here, tiny_own, tiny_all, (tiny_send, tiny_recv), True)
    half_cols = counts * width
    local = [
        pltpu.make_async_copy(w_gate, weight.at[:, :half_cols], local_sems.at[0]),
        pltpu.make_async_copy(w_up, weight.at[:, half_cols:], local_sems.at[1]),
    ]
    for copy in local:
        copy.start()
    eye = diagonal()
    tiny_own[...] = jnp.zeros_like(tiny_own)

    def prepare(shard, _):
        for at in range(rows // LANES):
            span = pl.ds(pl.multiple_of(shard * rows + at * LANES, LANES), LANES)
            resid = x_low[span, :].astype(jnp.float32) + attn[span, :].astype(jnp.float32)
            act[span, :] = (resid * gain[1:2, :]).astype(act.dtype)
            square = jnp.sum(resid * resid, axis=-1, keepdims=True)
            tiny_own[shard, at : at + 1, :] = jnp.sum(square * eye, axis=0, keepdims=True)
        return 0

    lax.fori_loop(0, 8, prepare, 0)
    greet(here, slice_peers(here))
    tiny.begin()
    for copy in local:
        copy.wait()
    product = products(here, act, weight, False, rows, width, counts)
    total = Reduce(here, counts, product, refs[8:19])
    total.run()

    def flip(shard, _):
        span = pl.ds(pl.multiple_of(shard * rows, rows), rows)
        act_t[:, span] = act[span, :].T
        return 0

    lax.fori_loop(0, 8, flip, 0)
    tiny.end()
    tiles = rows // LANES
    mean = [from_tile(jnp.sum(tiny_all[:, at, :], axis=0, keepdims=True), eye) for at in range(tiles)]
    scale = lax.rsqrt(jnp.concatenate(mean, axis=0) / (8 * cols) + EPS)
    dots[...] = jnp.zeros_like(dots)
    late[0].wait()
    coeff = math.sqrt(2.0 / math.pi)

    def emit(at, first, second):
        span = pl.ds(pl.multiple_of(at * width, width), width)
        gate, up = first * scale, second * scale
        inner = jnp.tanh(coeff * (gate + 0.044715 * (gate * gate * gate)))
        gelu = 0.5 * gate * (1.0 + inner)
        slope = 0.5 * (1.0 + inner) + 0.5 * gate * (1.0 - inner * inner) * (
            coeff * (1.0 + 3.0 * 0.044715 * gate * gate))
        cot = d_hidden[:, span]
        hidden[:, span] = (gelu * up).astype(hidden.dtype)
        back_gate, back_up = cot * up * slope, cot * gelu
        d_gate[:, span] = (back_gate * scale).astype(d_gate.dtype)
        d_up[:, span] = (back_up * scale).astype(d_up.dtype)
        dots[...] += jnp.sum(back_gate * gate + back_up * up, axis=-1, keepdims=True)

    total.end(emit)
    tile_out[...] = jnp.zeros_like(tile_out)
    to_tile(tile_out, 0, dots[...] * (scale * scale * (1.0 / (8 * cols))), eye)


def ffn_scatter(x_low, attn, gain, w_gate, w_up, d_hidden, cid, width=512):
    rows, half = d_hidden.shape
    cols = gain.shape[1]
    counts = half // width
    low, f32 = jnp.bfloat16, jnp.float32
    dma = pltpu.SemaphoreType.DMA
    vm = pl.BlockSpec(memory_space=pltpu.VMEM)
    hbm = pl.BlockSpec(memory_space=pl.ANY)
    out_shape = [jax.ShapeDtypeStruct((rows, half), low)] * 3 + [
        jax.ShapeDtypeStruct((cols, 8 * rows), low),
        jax.ShapeDtypeStruct((8, LANES), f32),
    ]
    scratch = [
        pltpu.VMEM((8 * rows, cols), low),
        pltpu.VMEM((cols, 2 * half), low),
        pltpu.VMEM((8, 8, LANES), f32),
        pltpu.VMEM((8, 8, LANES), f32),
        dma((7,)), dma((7,)),
        pltpu.VMEM((rows, 1), f32),
        dma((2,)),
    ] + reduce_scratch(counts, rows, width)
    kernel = functools.partial(ffn_kernel, rows, width, counts)
    return kernel_call(kernel, out_shape, [x_low, attn, gain, w_gate, w_up, d_hidden], [vm, vm, vm, hbm, hbm, vm],
                       scratch, cid, "ffn", late=(5,))


def load_own(spread, payload, width, counts, sems):
    copies = []
    for half in range(2):
        for at in range(counts):
            first = at * width + (half * counts * width if len(payload) == 1 else 0)
            src = payload[half % len(payload)].at[:, first : first + width]
            copies.append(pltpu.make_async_copy(src, spread.slot(0, half, at), sems.at[half, at]))
    return copies


def chip_place(here, per):
    def place(at):
        return here.shard(at // (2 * per), at // per % 2) * per + at % per

    return place


def back_kernel(rows, width, counts, act_t, w_gate, w_up, d_gate, d_up, dots, x_low, attn, gain, d_norm, gain_grad,
                grad_gate, grad_up, *refs, late):
    here = Place()
    spread = Spread(here, counts, refs[:7])
    tiny_all, tiny_send, tiny_recv, own_sems, weight, sums, grads, staged, local_sems, out_sems = refs[7:17]
    contrib, rest, rest_sems = refs[17:20]
    line = Line(here, 4, [contrib, d_norm] + list(refs[20:]), chip_place(here, 2))
    tiny = Tiny(here, dots, tiny_all, (tiny_send, tiny_recv), False)
    half_cols = counts * width
    local = [
        pltpu.make_async_copy(w_gate, weight.at[:, :half_cols], local_sems.at[0]),
        pltpu.make_async_copy(w_up, weight.at[:, half_cols:], local_sems.at[1]),
    ]
    own = load_own(spread, (d_gate, d_up), width, counts, own_sems)
    for copy in own + local:
        copy.start()
    greet(here, tiny.peers, True)
    for copy in own:
        copy.wait()
    tiny.begin()
    spread.begin()
    sums[...] = jnp.zeros_like(sums)
    for copy in local + late:
        copy.wait()

    def columns(half, at):
        return pl.ds(pl.multiple_of((half * counts + at) * width, width), width)

    def clear(at, _):
        grads[:, columns(0, at)] = jnp.zeros((grads.shape[0], width), jnp.float32)
        return 0

    lax.fori_loop(0, 2 * counts, clear, 0)

    def blocks(across, half, at):
        cols = columns(half, at)
        gained = grads[:, cols]
        for other in range(2):
            row = row_span(here, across, other, rows)
            block = spread.got[across, (spread.core + other) % 2, half, at]
            sums[row, :] += dot_nt(block, weight[:, cols])
            gained = gained + dot_nn(act_t[:, row], block)
        grads[:, cols] = gained

    def leave(half, at):
        spot = pl.ds(pl.multiple_of(at * width, width), width)
        return pltpu.make_async_copy(staged.at[half], (grad_gate, grad_up)[half].at[:, spot],
                                     out_sems.at[half, at])

    eye = diagonal()
    gain_grad[...] = jnp.zeros_like(gain_grad)

    def close_chip(chip, target):
        def close_shard(other, _):
            shard = here.shard(chip, other)
            span = pl.ds(pl.multiple_of(shard * rows, rows), rows)
            loads = [pltpu.make_async_copy(src.at[span, :], rest.at[at], rest_sems.at[at])
                     for at, src in enumerate((x_low, attn))]
            for copy in loads:
                copy.start()
            for copy in loads:
                copy.wait()
            for at in range(rows // LANES):
                span = pl.ds(pl.multiple_of(shard * rows + at * LANES, LANES), LANES)
                piece = slice(at * LANES, (at + 1) * LANES)
                dot = from_tile(tiny_all[shard, at : at + 1, :], eye)
                resid = rest[0, piece, :].astype(jnp.float32) + rest[1, piece, :].astype(jnp.float32)
                value = sums[span, :]
                target[span, :] = (value * gain[1:2, :] - resid * dot).astype(target.dtype)
                gain_grad[...] += jnp.sum(value * resid, axis=0, keepdims=True)
            return 0

        lax.fori_loop(0, 2, close_shard, 0)

    def done(stage, at):
        @pl.when(jnp.logical_and(stage == 3, at > 0))
        def _():
            leave(0, at - 1).wait()
            leave(1, at - 1).wait()

        @pl.when(stage == 3)
        def _():
            for half in range(2):
                staged[half] = grads[:, columns(half, at)].astype(staged.dtype)
            leave(0, at).start()
            leave(1, at).start()

        @pl.when(jnp.logical_and(at == counts - 1, stage == 0))
        def _():
            close_chip(0, contrib)
            line.launch(0, 4)

        @pl.when(jnp.logical_and(at == counts - 1, stage == 2))
        def _():
            lax.fori_loop(1, 3, lambda chip, _: (close_chip(chip, d_norm), 0)[1], 0)

    def hook(step):
        @pl.when(jnp.logical_and(step >= counts, step < counts + 6))
        def _():
            line.step(step - counts)

    tiny.end()
    spread.run(blocks, hook, done)
    close_chip(3, d_norm)
    line.settle()
    spread.end()

    def drain(at, _):
        leave(0, at).wait()
        leave(1, at).wait()
        return 0

    lax.fori_loop(counts - 1, counts, drain, 0)


def back_gather(act_t, w_gate, w_up, d_gate, d_up, dots, x_low, attn, gain, cid, width=512):
    cols, total = act_t.shape
    rows, half = d_gate.shape
    counts = half // width
    low, f32 = jnp.bfloat16, jnp.float32
    dma = pltpu.SemaphoreType.DMA
    vm = pl.BlockSpec(memory_space=pltpu.VMEM)
    hbm = pl.BlockSpec(memory_space=pl.ANY)
    out_shape = [
        jax.ShapeDtypeStruct((total, cols), low),
        jax.ShapeDtypeStruct((1, cols), f32),
        jax.ShapeDtypeStruct((cols, half), low),
        jax.ShapeDtypeStruct((cols, half), low),
    ]
    scratch = spread_scratch(counts, rows, width) + [
        pltpu.VMEM((8, 8, LANES), f32), dma((7,)), dma((7,)), dma((2, counts)),
        pltpu.VMEM((cols, 2 * half), low),
        pltpu.VMEM((total, cols), f32),
        pltpu.VMEM((cols, 2 * half), f32),
        pltpu.VMEM((2, cols, width), low),
        dma((2,)), dma((2, counts)),
        pltpu.VMEM((total, cols), low),
        pltpu.VMEM((2, rows, cols), low),
        dma((2,)),
    ] + line_scratch(4, (4 * rows // 2, cols), low)
    operands = [act_t, w_gate, w_up, d_gate, d_up, dots, x_low, attn, gain]
    kernel = functools.partial(back_kernel, rows, width, counts)
    return kernel_call(kernel, out_shape, operands, [vm] + [hbm] * 4 + [vm, hbm, hbm, vm], scratch, cid, "back",
                       [vm, vm, hbm, hbm], (0,))


def down_kernel(rows, width, counts, cot, weight, hidden, d_norm, ffn, d_attn, grad, *refs, late):
    here = Place()
    spread = Spread(here, counts, refs[:7])
    own_sems, sums, grads, staged, out_sems, norm_out = refs[7:13]
    place = chip_place(here, 4)
    norm_line = Line(here, 24, [d_norm, norm_out] + list(refs[13:]), lambda at: place(at + 8))
    own = load_own(spread, (hidden,), width, counts, own_sems)
    for copy in own:
        copy.start()
    greet(here, slice_peers(here), True)
    norm_line.begin()
    for copy in own:
        copy.wait()
    spread.begin()
    sums[...] = jnp.zeros_like(sums)
    grads[...] = jnp.zeros_like(grads)
    for copy in late:
        copy.wait()

    def columns(half, at):
        return pl.ds(pl.multiple_of((half * counts + at) * width, width), width)

    def blocks(across, half, at):
        cols = columns(half, at)
        gained = grads[cols, :]
        for other in range(2):
            row = row_span(here, across, other, rows)
            block = spread.got[across, (spread.core + other) % 2, half, at]
            sums[row, :] += dot_nn(block, weight[cols, :])
            gained = gained + dot_tn(block, cot[row, :])
        grads[cols, :] = gained

    def leave(half, at):
        return pltpu.make_async_copy(staged.at[at % 2, half], grad.at[columns(half, at), :], out_sems.at[half, at])

    def done(stage, at):
        @pl.when(jnp.logical_and(stage == 3, at > 1))
        def _():
            leave(0, at - 2).wait()
            leave(1, at - 2).wait()

        @pl.when(stage == 3)
        def _():
            for half in range(2):
                staged[at % 2, half] = grads[columns(half, at), :].astype(staged.dtype)
            leave(0, at).start()
            leave(1, at).start()

    norm_line.steps(spread.run(blocks, norm_line.step, done), 26)
    ffn[...] = sums[...].astype(ffn.dtype)
    norm_line.settle()

    def add_norm(at, _):
        def add(source):
            span = row_span(here, at // 2, at % 2, rows)
            d_attn[span, :] = (cot[span, :].astype(jnp.float32) + source[span, :].astype(jnp.float32)).astype(
                d_attn.dtype)

        @pl.when(at < 2)
        def _():
            add(d_norm)

        @pl.when(at >= 2)
        def _():
            add(norm_out)
        return 0

    lax.fori_loop(0, 8, add_norm, 0)
    spread.end()

    def drain(at, _):
        leave(0, at).wait()
        leave(1, at).wait()
        return 0

    lax.fori_loop(counts - 2, counts, drain, 0)


def down_gather(cot, weight, hidden, d_norm, cid, width=256):
    total, cols = cot.shape
    rows, every = hidden.shape
    counts = every // (2 * width)
    low, f32 = jnp.bfloat16, jnp.float32
    dma = pltpu.SemaphoreType.DMA
    vm = pl.BlockSpec(memory_space=pltpu.VMEM)
    hbm = pl.BlockSpec(memory_space=pl.ANY)
    out_shape = [
        jax.ShapeDtypeStruct((total, cols), low),
        jax.ShapeDtypeStruct((total, cols), low),
        jax.ShapeDtypeStruct(weight.shape, low),
    ]
    scratch = spread_scratch(counts, rows, width) + [
        dma((2, counts)),
        pltpu.VMEM((total, cols), f32),
        pltpu.VMEM(weight.shape, f32),
        pltpu.VMEM((2, 2, width, cols), low),
        dma((2, counts)),
        pltpu.VMEM((total, cols), low),
    ] + line_scratch(24, (24 * rows // 4, cols), low)
    kernel = functools.partial(down_kernel, rows, width, counts)
    return kernel_call(kernel, out_shape, [cot, weight, hidden, d_norm], [vm, vm, hbm, vm], scratch, cid, "down",
                       [vm, vm, hbm], (0, 1))


def attend_kernel(rows, heads, cols, width, counts, qkv, rms, cos, sin, mask, w_out, g_col, w_down, attn, mixed_all,
                  kv, probs, queries, pair_rms, d_hidden, *refs, late):
    here = Place()
    spread = Spread(here, 1, refs[:7])
    part, pair_sems, tiny_own, tiny_pair, mixed_sems = refs[7:12]
    product = products(here, g_col, w_down, True, rows, width, counts)
    total = Reduce(here, counts, product, refs[12:23])
    piece = rows // 2

    def place(at):
        across, other, half_at = spread.block(at)
        return here.shard(across, other) * 2 + half_at

    line = Line(here, 32, [part, attn] + list(refs[23:]), lambda at: place(at // 2) * 2 + at % 2)
    got, core = spread.got, here.core
    greet(here, slice_peers(here), True)
    half = HD // 2
    scale = 1.0 / math.sqrt(HD)
    wide = heads * HD

    def rotated(first):
        lead = qkv[:, first : first + half] * rms[...]
        trail = qkv[:, first + half : first + HD] * rms[...]
        return lead * cos[0] - trail * sin[0], trail * cos[0] + lead * sin[0]

    low_k, high_k = rotated(wide)
    kv[0, :, :half] = low_k.astype(kv.dtype)
    kv[0, :, half:HD] = high_k.astype(kv.dtype)
    for at in range(2):
        first = HD + at * half
        kv[0, :, first : first + half] = (qkv[:, wide + first : wide + first + half] * rms[...]).astype(kv.dtype)
    eye = diagonal()
    tiny_own[...] = jnp.zeros_like(tiny_own)
    to_tile(tiny_own, 0, rms[:, :1], eye)
    pair_rms[0] = rms[...]
    pair = remote(kv.at[0], kv.at[1], pair_sems.at[0], pair_sems.at[1], spread.ydev)
    tiny = remote(tiny_own, tiny_pair, pair_sems.at[2], pair_sems.at[3], spread.ydev)
    for head in range(heads):
        if head == 1:
            pair.start()
            tiny.start()
        lead, trail = rotated(head * HD)
        queries[:, head * HD : head * HD + half] = (lead * scale).astype(queries.dtype)
        queries[:, head * HD + half : (head + 1) * HD] = (trail * scale).astype(queries.dtype)
    pair.wait()
    for copy in late:
        copy.wait()

    def one_head(head, _):
        query = queries[:, pl.ds(pl.multiple_of(head * HD, HD), HD)]
        scores = jnp.concatenate([dot_nt(query, kv[0, :, :HD]), dot_nt(query, kv[1, :, :HD])], axis=1)
        scores = jnp.where(mask[...] > 0, scores, NEG)
        expd = jnp.exp(scores - jnp.max(scores, axis=-1, keepdims=True))
        prob = expd / jnp.sum(expd, axis=-1, keepdims=True)
        probs[head] = prob
        prob_low = prob.astype(jnp.bfloat16)
        mixed = dot_nn(prob_low[:, :rows], kv[0, :, HD:]) + dot_nn(prob_low[:, rows:], kv[1, :, HD:])
        span = pl.ds(pl.multiple_of(head * HD, HD), HD)
        for half_at in range(2):
            low_mixed = mixed[half_at * piece : (half_at + 1) * piece, :].astype(got.dtype)
            got[0, core, half_at, 0, :, span] = low_mixed
        return 0

    lax.fori_loop(0, heads, one_head, 0)
    spread.begin_rows()

    def mixed_copy(at):
        across, other, half_at = spread.block(at)
        span = pl.ds(pl.multiple_of(place(at) * piece, piece), piece)
        return pltpu.make_async_copy(got.at[across, (core + other) % 2, half_at, 0], mixed_all.at[span, :],
                                     mixed_sems.at[at])

    def one_step(step, _):
        spread.receive_rows(step)

        @pl.when(step < 16)
        def _():
            across, other, half_at = spread.block(step)
            value = dot_nn(got[across, (core + other) % 2, half_at, 0], w_out[...])
            part[pl.ds(pl.multiple_of(place(step) * piece, piece), piece), :] = value.astype(part.dtype)
            mixed_copy(step).start()
            line.launch(2 * step, 2)

        @pl.when(step >= 2)
        def _():
            total.advance(step - 2)

        @pl.when(step >= 4)
        def _():
            line.step(2 * step - 8)
            line.step(2 * step - 7)
        return 0

    lax.fori_loop(0, 20, one_step, 0)
    line.end(32)

    def emit(at, first, second):
        for half_at, value in enumerate((first, second)):
            d_hidden[:, pl.ds(pl.multiple_of((half_at * counts + at) * width, width), width)] = value

    total.end(emit)
    for hop in range(3):
        spread.x_copy(hop, 0).wait_send()
        spread.y_copy(hop, 0).wait_send()
    for stage in range(4):
        for stream in range(2):
            spread.sib_copy(stage, stream, 0).wait_send()
    for at in range(16):
        mixed_copy(at).wait()
    tiny.wait()
    for at in range(rows // LANES):
        values = jnp.broadcast_to(from_tile(tiny_pair[at : at + 1, :], eye), (LANES, LANES))
        pair_rms[1, at * LANES : (at + 1) * LANES, :] = values


def attend(qkv, rms, cos, sin, mask, w_out, g_col, w_down, cid, width=512):
    rows = qkv.shape[0]
    wide, cols = w_out.shape
    heads = wide // HD
    counts = w_down.shape[0] // (2 * width)
    low, f32 = jnp.bfloat16, jnp.float32
    dma = pltpu.SemaphoreType.DMA
    vm = pl.BlockSpec(memory_space=pltpu.VMEM)
    out_shape = [
        jax.ShapeDtypeStruct((8 * rows, cols), low),
        jax.ShapeDtypeStruct((8 * rows, wide), low),
        jax.ShapeDtypeStruct((2, rows, 2 * HD), low),
        jax.ShapeDtypeStruct((heads, rows, 2 * rows), f32),
        jax.ShapeDtypeStruct((rows, wide), low),
        jax.ShapeDtypeStruct((2,) + rms.shape, f32),
        jax.ShapeDtypeStruct((rows, w_down.shape[0]), f32),
    ]
    scratch = spread_scratch(1, rows // 2, wide) + [
        pltpu.VMEM((8 * rows, cols), low), dma((4,)),
        pltpu.VMEM((8, LANES), f32), pltpu.VMEM((8, LANES), f32), dma((16,)),
    ] + reduce_scratch(counts, rows, width) + line_scratch(32, (8 * rows, cols), low)
    kernel = functools.partial(attend_kernel, rows, heads, cols, width, counts)
    operands = [qkv, rms, cos, sin, mask, w_out, g_col, w_down]
    out_specs = [vm, pl.BlockSpec(memory_space=pl.ANY)] + [vm] * 5
    return kernel_call(kernel, out_shape, operands, [vm] * 8, scratch, cid, "attend", out_specs, (4, 5, 6, 7))


def tail_kernel(rows, heads, per, d_attn, w_out, queries, kv, probs, rms, cos, sin, act_t, w_qkv, ffn, x_low,
                attn, gain, gain_grad, mixed_all, d_tok, out, grad_query, grad_out, kv_sum, gain_tiles, *refs, late):
    here = Place()
    width = HD
    counts = heads // 2
    part = rows // 2
    refs = list(refs)
    line_counts = 8 * per
    cols = d_attn.shape[1]
    extra = cols // (rows // per)

    def take(count):
        taken_refs = refs[:count]
        del refs[:count]
        return taken_refs

    total_refs = take(11)
    spread = Spread(here, 1, take(7))
    d_mixed, tiny_own, tiny_all, d_kv, give, taken, give_sems, tiny_send, tiny_recv = take(9)
    grad, grad_mixed, gain_sum, tile, tile_send, tile_recv, put_sems, local_sems, mixed_two, mixed_sems = take(10)

    def far(at):
        return at // (2 * per), at // per % 2

    def near(at):
        return spread.block(jnp.minimum(at, line_counts - 1))

    def place_ffn(at):
        return here.shard(*far(at)) * per + at % per

    def place_tok(at):
        across, other, half_at = near(at)
        return jnp.where(at < line_counts, here.shard(across, other) * per + half_at, at)

    ffn_sum, leaving = take(2)
    by_chip = chip_place(here, per)
    line = Line(here, line_counts, [ffn, ffn_sum] + take(8), by_chip)
    contrib, summed = take(2)
    line_tok = Line(here, line_counts + extra, [contrib, summed] + take(8), place_tok)
    tiny = Tiny(here, tiny_own, tiny_all, (tiny_send, tiny_recv), False)
    got, core = spread.got, here.core
    product = products(here, d_attn, w_out, True, rows, width, counts)
    total = Reduce(here, counts, product, total_refs)
    greet(here, tiny.peers, True)
    line.begin()
    grad_mixed[...] = jnp.zeros_like(grad_mixed)

    def mixed_copy(step):
        span = pl.ds(pl.multiple_of(step * rows, rows), rows)
        return pltpu.make_async_copy(mixed_all.at[span, :], mixed_two.at[step % 2], mixed_sems.at[step % 2])

    mixed_copy(0).start()

    def beside(step):
        line.step(step)

        @pl.when(step < 8)
        def _():
            span = pl.ds(pl.multiple_of(step * rows, rows), rows)
            mixed_copy(step).wait()

            @pl.when(step < 7)
            def _():
                mixed_copy(step + 1).start()

            grad_mixed[...] += dot_tn(mixed_two[step % 2], d_attn[span, :])

    done = total.run(beside)
    grad_out[...] = grad_mixed[...].astype(grad_out.dtype)

    def land(at, first, second):
        for half_at, value in enumerate((first, second)):
            d_mixed[:, pl.ds(pl.multiple_of((half_at * counts + at) * width, width), width)] = value.astype(
                d_mixed.dtype)

    total.end(land)
    half = HD // 2
    scale = 1.0 / math.sqrt(HD)
    depth = w_qkv.shape[0] * 8
    d_kv[...] = jnp.zeros_like(d_kv)
    for copy in late:
        copy.wait()

    def one_head(head, dots):
        span = pl.ds(pl.multiple_of(head * HD, HD), HD)
        query = queries[:, span]
        cot = d_mixed[:, span]
        prob = probs[head]
        d_prob = jnp.concatenate([dot_nt(cot, kv[0, :, HD:]), dot_nt(cot, kv[1, :, HD:])], axis=1)
        delta = jnp.sum(prob * d_prob, axis=-1, keepdims=True)
        d_score = (prob * (d_prob - delta)).astype(jnp.bfloat16)
        prob_low = prob.astype(jnp.bfloat16)
        d_query = (dot_nn(d_score[:, :rows], kv[0, :, :HD]) + dot_nn(d_score[:, rows:], kv[1, :, :HD])) * scale
        for side in range(2):
            keys = slice(side * rows, (side + 1) * rows)
            d_kv[side, :, :HD] += dot_tn(d_score[:, keys], query)
            d_kv[side, :, HD:] += dot_tn(prob_low[:, keys], cot)
        dots = dots + jnp.sum(d_query * query.astype(jnp.float32), axis=-1, keepdims=True)
        lead, trail = d_query[:, :half], d_query[:, half:]
        first = ((lead * cos[0] + trail * sin[0]) * rms[0]).astype(got.dtype)
        second = ((trail * cos[0] - lead * sin[0]) * rms[0]).astype(got.dtype)
        line.step(done + head)
        for rows_at in range(2):
            piece = slice(rows_at * part, (rows_at + 1) * part)
            got[0, core, rows_at, 0, :, pl.ds(pl.multiple_of(head * HD, HD), half)] = first[piece, :]
            got[0, core, rows_at, 0, :, pl.ds(pl.multiple_of(head * HD + half, half), half)] = second[piece, :]

        return dots

    dots = lax.fori_loop(0, heads, one_head, jnp.zeros((rows, 1), jnp.float32))
    eye = diagonal()
    tiny_own[...] = jnp.zeros_like(tiny_own)
    for side in (1, 0):
        d_key, d_value = d_kv[side, :, :HD], d_kv[side, :, HD:]
        own = jnp.sum(d_key * kv[side, :, :HD].astype(jnp.float32) +
                      d_value * kv[side, :, HD:].astype(jnp.float32), axis=-1, keepdims=True)
        if side == 0:
            own = own + dots * (1.0 / scale)
        own = own * (rms[side] * rms[side] * (1.0 / depth))
        to_tile(tiny_own, side * (rows // LANES), own, eye)
        lead, trail = d_key[:, :half], d_key[:, half:]
        parts = [(lead * cos[side] + trail * sin[side]) * rms[side],
                 (trail * cos[side] - lead * sin[side]) * rms[side],
                 d_value[:, :half] * rms[side], d_value[:, half:] * rms[side]]
        for at, value in enumerate(parts):
            if side == 1:
                give[:, at * half : (at + 1) * half] = value.astype(give.dtype)
            else:
                d_kv[0, :, at * half : (at + 1) * half] = value
    given = remote(give, taken, give_sems.at[0], give_sems.at[1], spread.ydev)
    given.start()
    grad[...] = jnp.zeros_like(grad)
    given.wait()
    for rows_at in range(2):
        piece = slice(rows_at * part, (rows_at + 1) * part)
        value = d_kv[0, piece, :] + taken[piece, :].astype(jnp.float32)
        got[0, core, rows_at, 0, :, heads * HD :] = value.astype(got.dtype)
    tiny.begin()
    spread.begin_rows()
    gain_sum[...] = jnp.zeros_like(gain_sum)
    tiny.end()

    def block_of(at):
        across, other, half_at = near(at)
        shard, partner = here.shard(across, other), here.shard((across + 2) % 4, other)
        block = got[across, (core + other) % 2, half_at, 0]
        first = pl.multiple_of(shard * rows + half_at * part, part)
        for tile_at in range(part // LANES):
            row = pl.ds(pl.multiple_of(first + tile_at * LANES, LANES), LANES)
            low_at = half_at * (part // LANES) + tile_at
            kept = rows // LANES + low_at
            dot = from_tile(tiny_all[shard, pl.ds(low_at, 1), :] + tiny_all[partner, pl.ds(kept, 1), :], eye)
            value = dot_nt(block[tile_at * LANES : (tile_at + 1) * LANES, :], w_qkv[...])
            x_rows = x_low[row, :].astype(jnp.float32)
            contrib[row, :] = (value * gain[0:1, :] - x_rows * dot).astype(contrib.dtype)
            gain_sum[...] += jnp.sum(value * x_rows, axis=0, keepdims=True)
        line_tok.launch(at, 1)
        rows_t = act_t[:, pl.ds(first, part)]
        for at_col in range((heads + 2) * HD // 512):
            span = slice(at_col * 512, (at_col + 1) * 512)
            grad[:, span] += dot_nn(rows_t, block[:, span])

    me = here.shard(0, 0)
    columns = pl.ds(pl.multiple_of(me * cols, cols), cols)
    chunk = line.chunk

    def landing(which, at):
        sub = at % per if which == 0 else near(at)[2]
        return (out, d_tok)[which].at[pl.ds(pl.multiple_of(sub * chunk, chunk), chunk), columns]

    def leaver(which, at):
        return (leaving, line_tok.from_end)[which].at[at]

    def put(which, at):
        goal = here.device(*(far(at) if which == 0 else near(at)[:2]))
        return remote(leaver(which, at), landing(which, at), put_sems.at[which, 0, at], put_sems.at[which, 1, at],
                      goal)

    def keep(which, at):
        spot = at % per if which == 0 else near(at)[2]
        return pltpu.make_async_copy(leaver(which, at), landing(which, at), local_sems.at[which, spot])

    def emit(which, at):
        if which == 1:
            row = line_tok.rows(at)
            value = d_attn[row, :].astype(jnp.float32) + summed[row, :].astype(jnp.float32)
            line_tok.from_end[at] = value.astype(out.dtype)
            return
        row = pl.ds(pl.multiple_of(place_ffn(at) * chunk, chunk), chunk)

        def leave(source):
            value = x_low[row, :].astype(jnp.float32) + attn[row, :].astype(jnp.float32)
            leaving[at] = (value + source[row, :].astype(jnp.float32)).astype(out.dtype)

        leave(ffn_sum)

    def is_own(which, at):
        return at < per if which == 0 else jnp.logical_and(at < 4, at % 2 == 0)

    def send(which, at):
        own = is_own(which, at)

        @pl.when(own)
        def _():
            keep(which, at).start()

        @pl.when(jnp.logical_not(own))
        def _():
            put(which, at).start()

    def stage_step(step, _):
        spread.receive_rows(step)

        @pl.when(step < line_counts)
        def _():
            block_of(step)

        @pl.when(step < 5)
        def _():
            line.step(done + heads + step)

        @pl.when(step >= 4)
        def _():
            line_tok.step(step - 4)

        @pl.when(step > 0)
        def _():
            send(0, step - 1)

        @pl.when(line.inner == 0)
        def _():
            line.up(step).wait_send()
            line.down(step).wait_recv()

        emit(0, step)

        @pl.when(jnp.logical_and(line.inner == 1, step > 7))
        def _():
            send(1, step - 8)

        @pl.when(jnp.logical_and(line.inner == 1, step > 6))
        def _():
            emit(1, step - 7)
        return 0

    lax.fori_loop(0, line_counts, stage_step, 0)
    for half_at in range(cols // (rows // per)):
        span = pl.ds(line_counts * (rows // per) + half_at * (rows // per), rows // per)
        source = slice(half_at * (rows // per), (half_at + 1) * (rows // per))
        contrib[span, :] = grad[source, heads * HD :].astype(contrib.dtype)
    line_tok.launch(line_counts, extra)
    grad_query[...] = grad[:, : heads * HD].astype(grad_query.dtype)
    for at in range(cols // LANES):
        tile[at : at + 1, :] = gain_sum[:, at * LANES : (at + 1) * LANES]
        spot = cols // LANES + at
        tile[spot : spot + 1, :] = gain_grad[:, at * LANES : (at + 1) * LANES]

    def tile_copy(step):
        return remote(tile, gain_tiles.at[here.z], tile_send.at[step], tile_recv.at[step],
                      (here.dp, here.seq, (here.z + step + 1) % 4))

    send(0, line_counts - 1)
    line.drain()
    for step in range(3):
        tile_copy(step).start()
    gain_tiles[here.z] = tile[...]

    @pl.when(line.inner == 1)
    def _():
        start = line_counts - 4

        def both(at, _):
            line_tok.step(at)

            @pl.when(at < line_counts + 4)
            def _():
                send(1, at - 4)

            @pl.when(at < line_counts + 3)
            def _():
                emit(1, at - 3)
            return 0

        lax.fori_loop(start, line_counts + extra + 2, both, 0)

        def drain(at, _):
            line_tok.down(at).wait_send()
            return 0

        lax.fori_loop(0, line_counts + extra, drain, 0)

    @pl.when(line.inner == 0)
    def _():
        def arrive(at, _):
            line_tok.up(at).wait_send()
            line_tok.down(at).wait_recv()

            @pl.when(jnp.logical_and(at > 0, at <= line_counts))
            def _():
                send(1, at - 1)

            @pl.when(at < line_counts)
            def _():
                emit(1, at)
            return 0

        lax.fori_loop(0, line_counts + extra, arrive, 0)

    for half_at in range(extra):
        span = pl.ds((line_counts + half_at) * chunk, chunk)
        kv_sum[half_at * chunk : (half_at + 1) * chunk, :] = summed[span, :]
    for hop in range(3):
        spread.x_copy(hop, 0).wait_send()
        spread.y_copy(hop, 0).wait_send()
    for stage in range(4):
        spread.sib_copy(stage, 0, 0).wait_send()
        spread.sib_copy(stage, 1, 0).wait_send()

    def finish(at, _):
        for which in range(2):
            own = is_own(which, at)

            @pl.when(own)
            def _():
                keep(which, at).wait()

            @pl.when(jnp.logical_not(own))
            def _():
                put(which, at).wait()
        return 0

    lax.fori_loop(0, line_counts, finish, 0)
    for step in range(3):
        tile_copy(step).wait()


def tail(d_attn, w_out, queries, kv, probs, rms, cos, sin, act_t, w_qkv, ffn, x_low, attn, gain, gain_grad,
         mixed_all, cid,
 per=2):
    total, cols = d_attn.shape
    rows = total // 8
    wide = w_out.shape[0]
    heads = wide // HD
    low, f32 = jnp.bfloat16, jnp.float32
    dma = pltpu.SemaphoreType.DMA
    vm = pl.BlockSpec(memory_space=pltpu.VMEM)
    counts = 8 * per
    chunk = rows // per
    extra = cols // chunk
    long = (total + cols, cols)
    out_shape = [
        jax.ShapeDtypeStruct((rows, 8 * cols), low),
        jax.ShapeDtypeStruct((rows, 8 * cols), low),
        jax.ShapeDtypeStruct((cols, wide), low),
        jax.ShapeDtypeStruct(w_out.shape, low),
        jax.ShapeDtypeStruct((cols, 2 * HD), low),
        jax.ShapeDtypeStruct((4, 8, LANES), f32),
    ]
    scratch = reduce_scratch(heads // 2, rows, HD, 2) + spread_scratch(1, rows // 2, wide + 2 * HD)
    scratch += [
        pltpu.VMEM((rows, wide), low),
        pltpu.VMEM((8, LANES), f32),
        pltpu.VMEM((8, 8, LANES), f32),
        pltpu.VMEM((2, rows, 2 * HD), f32),
        pltpu.VMEM((rows, 2 * HD), low),
        pltpu.VMEM((rows, 2 * HD), low),
        dma((2,)), dma((7,)), dma((7,)),
        pltpu.VMEM(w_qkv.shape, f32),
        pltpu.VMEM(w_out.shape, f32),
        pltpu.VMEM((1, cols), f32),
        pltpu.VMEM((8, LANES), f32),
        dma((3,)), dma((3,)), dma((2, 2, counts)), dma((2, per)),
        pltpu.VMEM((2, rows, wide), low), dma((2,)),
        pltpu.VMEM((total, cols), low),
        pltpu.VMEM((counts, chunk, cols), low),
    ] + line_scratch(counts, (total, cols), low)
    scratch += [pltpu.VMEM(long, low), pltpu.VMEM(long, low)] + line_scratch(counts + extra, long, low)
    operands = [d_attn, w_out, queries, kv, probs, rms, cos, sin, act_t, w_qkv, ffn, x_low, attn, gain,
                gain_grad, mixed_all]
    kernel = functools.partial(tail_kernel, rows, heads, per)
    specs = [vm] * (len(operands) - 1) + [pl.BlockSpec(memory_space=pl.ANY)]
    return kernel_call(kernel, out_shape, operands, specs, scratch, cid, "tail",
                       late=(2, 3, 4, 8, 9, 11, 12))


def widen_kernel(plan, *refs):
    count = len(plan)
    sources, results, scratch = refs[:count], refs[count : 2 * count], refs[2 * count :]

    def part(ref, at, step):
        span = plan[at][0]
        return ref.at[pl.ds(pl.multiple_of(step * span, span), span), :]

    def load(at, step):
        taken, sems = scratch[4 * at], scratch[4 * at + 2]
        return pltpu.make_async_copy(part(sources[at], at, step), taken.at[step % 3], sems.at[step % 3])

    def store(at, step):
        given, sems = scratch[4 * at + 1], scratch[4 * at + 3]
        return pltpu.make_async_copy(given.at[step % 3], part(results[at], at, step), sems.at[step % 3])

    for at, (_, steps) in enumerate(plan):
        for step in range(min(3, steps)):
            load(at, step).start()
    for at, (_, steps) in enumerate(plan):
        taken, given = scratch[4 * at], scratch[4 * at + 1]

        def one(step, _, at=at, steps=steps, taken=taken, given=given):
            load(at, step).wait()

            @pl.when(step >= 3)
            def _():
                store(at, step - 3).wait()

            given[step % 3] = taken[step % 3].astype(given.dtype)
            store(at, step).start()

            @pl.when(step + 3 < steps)
            def _():
                load(at, step + 3).start()
            return 0

        lax.fori_loop(0, steps, one, 0)
    for at, (_, steps) in enumerate(plan):
        for step in range(max(0, steps - 3), steps):
            store(at, step).wait()


def widen(arrays, block=2 ** 17):
    plan, scratch = [], []
    dma = pltpu.SemaphoreType.DMA
    for array in arrays:
        height, width = array.shape
        span = min(height, max(8, block // width))
        while height % span:
            span //= 2
        plan.append((span, height // span))
        scratch += [pltpu.VMEM((3, span, width), array.dtype), pltpu.VMEM((3, span, width), jnp.float32),
                    dma((3,)), dma((3,))]
    hbm = pl.BlockSpec(memory_space=pl.ANY)
    return pl.pallas_call(
        functools.partial(widen_kernel, tuple(plan)),
        out_shape=[jax.ShapeDtypeStruct(array.shape, jnp.float32) for array in arrays],
        in_specs=[hbm] * len(arrays),
        out_specs=[hbm] * len(arrays),
        scratch_shapes=scratch,
        compiler_params=pltpu.CompilerParams(vmem_limit_bytes=VMEM_LIMIT),
        name="widen",
    )(*arrays)


LANES = 128


def acts_move(
    tokens, seg_ids, gain_attn, w_query, kv_weight, w_out, gain_ffn, w_gate, w_up, w_down, d_out
):
    small = jnp.stack([gain_attn, gain_ffn, seg_ids.astype(gain_ffn.dtype), gain_attn]).astype(jnp.float32)

    qkv, x_low, act_one_t, w_qkv, rms, cos, sin, mask, g_parts = opening(
        tokens, small, w_query, kv_weight, d_out, 1
    )
    g_low = g_parts.reshape(x_low.shape)
    attn, mixed_all, kv, probs, queries, pair_rms, d_hidden = attend(
        qkv, rms, cos, sin, mask, w_out, g_low, w_down, 2
    )
    hidden, d_gate, d_up, act_two_t, dots = ffn_scatter(x_low, attn, small, w_gate, w_up, d_hidden, 4)
    d_norm, grad_gain_two, grad_gate, grad_up = back_gather(
        act_two_t, w_gate, w_up, d_gate, d_up, dots, x_low, attn, small, 5
    )
    ffn, d_attn, grad_down = down_gather(g_low, w_down, hidden, d_norm, 6)
    d_tokens, out, grad_query, grad_out, grad_kv, gain_tiles = tail(
        d_attn,
        w_out,
        queries,
        kv,
        probs,
        pair_rms,
        cos,
        sin,
        act_one_t,
        w_qkv,
        ffn,
        x_low,
        attn,
        small,
        grad_gain_two,
        mixed_all,
        7,
    )
    gains = jnp.sum(gain_tiles, axis=0).reshape(2, -1)
    d_tokens, grad_query, grad_kv, grad_out, grad_gate, grad_up, grad_down = widen(
        [d_tokens, grad_query, grad_kv, grad_out, grad_gate, grad_up, grad_down]
    )
    return (
        out,
        d_tokens,
        gains[0],
        grad_query,
        grad_kv,
        grad_out,
        gains[1],
        grad_gate,
        grad_up,
        grad_down,
    )


def solution(mesh):
    in_specs = (
        P(("dp", "seq"), None),
        P("dp"),
        P(("dp", "seq")),
        P(("dp", "seq"), "tensor"),
        P(("dp", "seq"), None),
        P("tensor", ("dp", "seq")),
        P(("dp", "seq")),
        P(("dp", "seq"), "tensor"),
        P(("dp", "seq"), "tensor"),
        P("tensor", ("dp", "seq")),
        P(("dp", "seq"), None),
    )
    out_specs = (
        P(("dp", "seq"), None),
        P(("dp", "seq"), None),
        P(("dp", "seq")),
        P(("dp", "seq"), "tensor"),
        P(("dp", "seq"), None),
        P("tensor", ("dp", "seq")),
        P(("dp", "seq")),
        P(("dp", "seq"), "tensor"),
        P(("dp", "seq"), "tensor"),
        P("tensor", ("dp", "seq")),
    )

    def shards(*arrays):
        tokens = arrays[0]
        sizes = tuple(mesh.shape[name] for name in ("dp", "seq", "tensor"))
        count = tokens.shape[0] * sizes[0] * sizes[1]
        plan = acts_move if sizes == (4, 2, 4) and count <= tokens.shape[1] else weights_move
        return plan(*arrays)

    return jax.shard_map(shards, mesh=mesh, in_specs=in_specs, out_specs=out_specs, check_vma=False)
```

```python
import functools
import math

import jax
import jax.numpy as jnp
from jax import lax
from jax.experimental import pallas as pl
from jax.experimental.pallas import tpu as pltpu
from jax.sharding import PartitionSpec as P

HD = 256


EPS = 1e-06
NEG = -1e30


def place_tables(segs):
    length = segs.shape[0]
    index = jnp.arange(length, dtype=jnp.int32)
    flags = jnp.concatenate([jnp.ones((1,), dtype=bool), segs[1:] != segs[:-1]])
    starts = lax.cummax(jnp.where(flags, index, jnp.zeros_like(index)), axis=0)
    places = index - starts
    half_size = HD // 2
    freqs = jnp.exp(jnp.arange(half_size, dtype=jnp.float32) * (-math.log(10000.0) / half_size))
    angles = places.astype(jnp.float32)[:, None] * freqs[None, :]
    return (places, jnp.cos(angles), jnp.sin(angles))


def rotate(vector, cos_table, sin_table):
    half_size = vector.shape[-1] // 2
    leading = vector[..., :half_size]
    trailing = vector[..., half_size:]
    return jnp.concatenate(
        [leading * cos_table - trailing * sin_table, trailing * cos_table + leading * sin_table],
        axis=-1,
    )


def rotate_back(vector, cos_table, sin_table):
    half_size = vector.shape[-1] // 2
    leading = vector[..., :half_size]
    trailing = vector[..., half_size:]
    return jnp.concatenate(
        [leading * cos_table + trailing * sin_table, trailing * cos_table - leading * sin_table],
        axis=-1,
    )


def matmul(left, right):
    return jnp.dot(left, right, preferred_element_type=jnp.float32)


def matmul_nt(left, right):
    return lax.dot_general(
        left, right, (((1,), (1,)), ((), ())), preferred_element_type=jnp.float32
    )


def matmul_tn(left, right):
    return lax.dot_general(
        left, right, (((0,), (0,)), ((), ())), preferred_element_type=jnp.float32
    )


def gelu_tanh(values):
    return jax.nn.gelu(values, approximate=True)


def norm_back(d_act, normed, rms_val, gain_val):
    scaled = d_act * gain_val
    return rms_val * (scaled - normed * jnp.mean(scaled * normed, axis=-1, keepdims=True))


def weights_move(
    tokens, seg_ids, gain_attn, w_query, kv_weight, w_out, gain_ffn, w_gate, w_up, w_down, d_out
):
    rows = tokens.shape[0]
    scale_factor = 1.0 / math.sqrt(HD)
    offset = lax.axis_index("seq") * rows
    places, cos_table, sin_table = place_tables(seg_ids)
    own_places = lax.dynamic_slice_in_dim(places, offset, rows, 0)
    own_segs = lax.dynamic_slice_in_dim(seg_ids, offset, rows, 0)
    own_cos = lax.dynamic_slice_in_dim(cos_table, offset, rows, 0)
    own_sin = lax.dynamic_slice_in_dim(sin_table, offset, rows, 0)
    allowed = (own_segs[:, None] == seg_ids[None, :]) & (own_places[:, None] >= places[None, :])
    full_query, full_out, full_kv, full_gain_one = (
        lax.all_gather(w_query, ("dp", "seq"), axis=0, tiled=True),
        lax.all_gather(w_out, ("dp", "seq"), axis=1, tiled=True),
        lax.all_gather(kv_weight, ("dp", "seq"), axis=0, tiled=True),
        lax.all_gather(gain_attn, ("dp", "seq"), axis=0, tiled=True),
    )
    gain_one = full_gain_one.astype(jnp.float32)
    inputs = tokens.astype(jnp.float32)
    rms_one = lax.rsqrt(jnp.mean(inputs * inputs, axis=-1, keepdims=True) + EPS)
    norm_one = inputs * rms_one
    act_one = (norm_one * gain_one).astype(jnp.bfloat16)
    query_pre = matmul(act_one, full_query)
    heads = query_pre.shape[1] // HD
    kv_pre = matmul(act_one, full_kv)
    queries = (
        rotate(query_pre.reshape(rows, heads, HD), own_cos[:, None, :], own_sin[:, None, :])
        * scale_factor
    ).astype(jnp.bfloat16)
    own_kv = jnp.concatenate(
        [rotate(kv_pre[:, :HD], own_cos, own_sin), kv_pre[:, HD:]], axis=1
    ).astype(jnp.bfloat16)
    all_kv = lax.all_gather(own_kv, "seq", axis=0, tiled=True)
    keys = all_kv[:, :HD]
    values_all = all_kv[:, HD:]
    scores = jnp.einsum("rhd,kd->hrk", queries, keys, preferred_element_type=jnp.float32)
    scores = jnp.where(allowed[None], scores, NEG)
    top_score = jnp.max(scores, axis=-1, keepdims=True)
    expd = jnp.exp(scores - top_score)
    total = jnp.sum(expd, axis=-1, keepdims=True)
    log_total = top_score + jnp.log(total)
    probs_low = (expd / total).astype(jnp.bfloat16)
    mixed = (
        jnp.einsum("hrk,kd->rhd", probs_low, values_all, preferred_element_type=jnp.float32)
        .reshape(rows, heads * HD)
        .astype(jnp.bfloat16)
    )
    attn = lax.psum(matmul(mixed, full_out), "tensor")
    resid = inputs + attn
    full_gate, full_up, full_down, full_gain_two = (
        lax.all_gather(w_gate, ("dp", "seq"), axis=0, tiled=True),
        lax.all_gather(w_up, ("dp", "seq"), axis=0, tiled=True),
        lax.all_gather(w_down, ("dp", "seq"), axis=1, tiled=True),
        lax.all_gather(gain_ffn, ("dp", "seq"), axis=0, tiled=True),
    )
    gain_two = full_gain_two.astype(jnp.float32)
    rms_two = lax.rsqrt(jnp.mean(resid * resid, axis=-1, keepdims=True) + EPS)
    norm_two = resid * rms_two
    act_two = (norm_two * gain_two).astype(jnp.bfloat16)
    gate = matmul(act_two, full_gate)
    up_val = matmul(act_two, full_up)
    gelu_val, gelu_pull = jax.vjp(gelu_tanh, gate)
    hidden = (gelu_val * up_val).astype(jnp.bfloat16)
    ffn = lax.psum(matmul(hidden, full_down).astype(jnp.bfloat16), "tensor").astype(jnp.float32)
    out = (resid + ffn).astype(jnp.bfloat16)
    back_gate, back_up, back_down = (
        lax.all_gather(w_gate, ("dp", "seq"), axis=0, tiled=True),
        lax.all_gather(w_up, ("dp", "seq"), axis=0, tiled=True),
        lax.all_gather(w_down, ("dp", "seq"), axis=1, tiled=True),
    )
    d_hidden = matmul_nt(d_out, back_down)
    grad_down = matmul_tn(hidden, d_out)
    d_gate = gelu_pull(d_hidden * up_val)[0].astype(jnp.bfloat16)
    d_up = (d_hidden * gelu_val).astype(jnp.bfloat16)
    grad_gate = matmul_tn(act_two, d_gate)
    grad_up = matmul_tn(act_two, d_up)
    d_act_two = lax.psum(matmul_nt(d_gate, back_gate) + matmul_nt(d_up, back_up), "tensor")
    grad_gain_two = jnp.sum(d_act_two * norm_two, axis=0)
    d_resid = d_out.astype(jnp.float32) + norm_back(d_act_two, norm_two, rms_two, gain_two)
    ffn_grads = (
        lax.psum_scatter(
            grad_gate.astype(jnp.bfloat16), ("dp", "seq"), scatter_dimension=0, tiled=True
        ).astype(jnp.float32),
        lax.psum_scatter(
            grad_up.astype(jnp.bfloat16), ("dp", "seq"), scatter_dimension=0, tiled=True
        ).astype(jnp.float32),
        lax.psum_scatter(
            grad_down.astype(jnp.bfloat16), ("dp", "seq"), scatter_dimension=1, tiled=True
        ).astype(jnp.float32),
        lax.psum_scatter(
            grad_gain_two.astype(jnp.bfloat16), ("dp", "seq"), scatter_dimension=0, tiled=True
        ).astype(jnp.float32),
    )
    back_query, back_out, back_kv = (
        lax.all_gather(w_query, ("dp", "seq"), axis=0, tiled=True),
        lax.all_gather(w_out, ("dp", "seq"), axis=1, tiled=True),
        lax.all_gather(kv_weight, ("dp", "seq"), axis=0, tiled=True),
    )
    d_attn = d_resid.astype(jnp.bfloat16)
    grad_out = matmul_tn(mixed, d_attn)
    d_mixed = matmul_nt(d_attn, back_out).astype(jnp.bfloat16).reshape(rows, heads, HD)
    scores_again = jnp.einsum("rhd,kd->hrk", queries, keys, preferred_element_type=jnp.float32)
    probs = jnp.where(allowed[None], jnp.exp(scores_again - log_total), 0.0)
    d_probs = jnp.einsum("rhd,kd->hrk", d_mixed, values_all, preferred_element_type=jnp.float32)
    delta = jnp.sum(probs * d_probs, axis=-1, keepdims=True)
    d_scores = (probs * (d_probs - delta)).astype(jnp.bfloat16)
    d_queries = (
        jnp.einsum("hrk,kd->rhd", d_scores, keys, preferred_element_type=jnp.float32) * scale_factor
    )
    d_query_pre = (
        rotate_back(d_queries, own_cos[:, None, :], own_sin[:, None, :])
        .reshape(rows, heads * HD)
        .astype(jnp.bfloat16)
    )
    d_keys_part = jnp.einsum("hrk,rhd->kd", d_scores, queries, preferred_element_type=jnp.float32)
    d_values_part = jnp.einsum(
        "hrk,rhd->kd", probs.astype(jnp.bfloat16), d_mixed, preferred_element_type=jnp.float32
    )
    own_kv_grad = lax.psum_scatter(
        jnp.concatenate([d_keys_part, d_values_part], axis=1).astype(jnp.bfloat16),
        "seq",
        scatter_dimension=0,
        tiled=True,
    )
    d_act_query = matmul_nt(d_query_pre, back_query)
    d_act_sum, kv_grad = (
        lax.psum(d_act_query.astype(jnp.bfloat16), "tensor").astype(jnp.float32),
        lax.psum(own_kv_grad, "tensor").astype(jnp.float32),
    )
    d_kv_pre = jnp.concatenate(
        [rotate_back(kv_grad[:, :HD], own_cos, own_sin), kv_grad[:, HD:]], axis=1
    ).astype(jnp.bfloat16)
    d_act_one = d_act_sum + matmul_nt(d_kv_pre, back_kv)
    grad_query = matmul_tn(act_one, d_query_pre)
    grad_kv = matmul_tn(act_one, d_kv_pre)
    grad_gain_one = jnp.sum(d_act_one * norm_one, axis=0)
    d_tokens = d_resid + norm_back(d_act_one, norm_one, rms_one, gain_one)
    attn_grads = (
        lax.psum_scatter(
            grad_query.astype(jnp.bfloat16), ("dp", "seq"), scatter_dimension=0, tiled=True
        ).astype(jnp.float32),
        lax.psum_scatter(
            grad_out.astype(jnp.bfloat16), ("dp", "seq"), scatter_dimension=1, tiled=True
        ).astype(jnp.float32),
        lax.psum_scatter(
            grad_kv.astype(jnp.bfloat16), ("dp", "seq"), scatter_dimension=0, tiled=True
        ).astype(jnp.float32),
        lax.psum_scatter(
            grad_gain_one.astype(jnp.bfloat16), ("dp", "seq"), scatter_dimension=0, tiled=True
        ).astype(jnp.float32),
    )
    return (
        out,
        d_tokens,
        attn_grads[3],
        attn_grads[0],
        attn_grads[2],
        attn_grads[1],
        ffn_grads[3],
        ffn_grads[0],
        ffn_grads[1],
        ffn_grads[2],
    )


MESH = pl.DeviceIdType.MESH
VMEM_LIMIT = 66000 * 1024


class Place:
    def __init__(self):
        self.dp = lax.axis_index("dp")
        self.seq = lax.axis_index("seq")
        self.z = lax.axis_index("tensor")
        self.core = lax.rem(self.dp, 2)
        self.chip = lax.div(self.dp, 2)

    def device(self, across, other):
        chip = (self.chip + across) % 2
        seq = (self.seq + across // 2) % 2
        core = (self.core + other) % 2
        return chip * 2 + core, seq, self.z

    def shard(self, across, other):
        dp, seq, _ = self.device(across, other)
        return dp * 2 + seq


def greet(here, peers, line=False):
    barrier = pltpu.get_barrier_semaphore()
    peers = list(peers)
    if line:
        peers += [(here.dp, here.seq, (here.z + step) % 4) for step in range(1, 4)]
    for peer in peers:
        pl.semaphore_signal(barrier, inc=1, device_id=peer, device_id_type=MESH)
    pl.semaphore_wait(barrier, len(peers))


def remote(src, dst, send, recv, peer):
    return pltpu.make_async_remote_copy(
        src_ref=src, dst_ref=dst, send_sem=send, recv_sem=recv, device_id=peer, device_id_type=MESH
    )


class Line:
    def __init__(self, here, counts, refs, place=None):
        self.own, self.out, self.from_end, self.from_mid = refs[:4]
        self.sems = refs[4:10]
        self.counts = counts
        self.chunk = self.from_mid.shape[1]
        self.fold = self.from_end.shape[1] // self.chunk
        self.place = place
        z = here.z
        self.inner = ((z + 1) // 2) % 2
        self.mate = (here.dp, here.seq, z + 1 - 2 * (z % 2))
        self.other = (here.dp, here.seq, 3 - z)

    def rows(self, at):
        at = at if self.place is None else self.place(at)
        return pl.ds(pl.multiple_of(at * self.chunk, self.chunk), self.chunk)

    def inbox(self, at):
        span = pl.ds(pl.multiple_of(at % self.fold * self.chunk, self.chunk), self.chunk)
        return self.from_end.at[at // self.fold, span, :]

    def up(self, at):
        return remote(self.own.at[self.rows(at), :], self.inbox(at), self.sems[0].at[at],
                      self.sems[1].at[at], self.mate)

    def over(self, at):
        return remote(self.out.at[self.rows(at), :], self.from_mid.at[at], self.sems[2].at[at],
                      self.sems[3].at[at], self.other)

    def down(self, at):
        rows = self.rows(at)
        return remote(self.out.at[rows, :], self.out.at[rows, :], self.sems[4].at[at],
                      self.sems[5].at[at], self.mate)

    def launch(self, first, count):
        @pl.when(self.inner == 0)
        def _():
            def send(at, _):
                self.up(first + at).start()
                return 0

            lax.fori_loop(0, count, send, 0)

    def begin(self):
        self.launch(0, self.counts)

    def first(self, at):
        rows = self.rows(at)
        self.up(at).wait_recv()
        total = self.own[rows, :].astype(jnp.float32) + self.inbox(at)[...].astype(jnp.float32)
        self.out[rows, :] = total.astype(self.out.dtype)
        self.over(at).start()

    def second(self, at):
        rows = self.rows(at)
        self.over(at).wait()
        total = self.out[rows, :].astype(jnp.float32) + self.from_mid[at].astype(jnp.float32)
        self.out[rows, :] = total.astype(self.out.dtype)
        self.down(at).start()

    def step(self, at, start=0, count=None):
        count = self.counts if count is None else count

        @pl.when(jnp.logical_and(self.inner == 1, at < count))
        def _():
            self.first(start + at)

        @pl.when(jnp.logical_and(self.inner == 1, jnp.logical_and(at > 1, at < count + 2)))
        def _():
            self.second(start + at - 2)

    def steps(self, first, last, start=0, count=None):
        def rest(at, _):
            self.step(at, start, count)
            return 0

        lax.fori_loop(first, last, rest, 0)

    def settle(self):
        @pl.when(self.inner == 0)
        def _():
            def take(at, _):
                self.up(at).wait_send()
                self.down(at).wait_recv()
                return 0

            lax.fori_loop(0, self.counts, take, 0)

        self.drain()

    def drain(self):
        @pl.when(self.inner == 1)
        def _():
            def drain(at, _):
                self.down(at).wait_send()
                return 0

            lax.fori_loop(0, self.counts, drain, 0)

    def end(self, done=0):
        self.steps(min(done, self.counts + 2), self.counts + 2)
        self.settle()


def line_scratch(counts, shape, low, fold=1):
    chunk = shape[0] // counts
    inbox = pltpu.VMEM((counts // fold, chunk * fold, shape[1]), low)
    return [inbox, pltpu.VMEM((counts, chunk, shape[1]), low)] + [pltpu.SemaphoreType.DMA((counts,))] * 6


def turned(at):
    return 3 - at // 2, 1 - at % 2


def slice_peers(here):
    return [here.device(*turned(at)) for at in range(7)]


def kernel_call(kernel, out_shape, operands, specs, scratch, cid, name, out_specs=None, late=()):
    vm = pl.BlockSpec(memory_space=pltpu.VMEM)
    specs = [pl.BlockSpec(memory_space=pl.ANY) if at in late else spec for at, spec in enumerate(specs)]
    inside = [pltpu.VMEM(operands[at].shape, operands[at].dtype) for at in late]
    if late:
        inside.append(pltpu.SemaphoreType.DMA((len(late),)))

    def body(*refs):
        if not late:
            kernel(*refs)
            return
        ins, rest, own = list(refs[: len(operands)]), refs[len(operands) : -len(inside)], refs[-len(inside) :]
        copies = []
        for spot, at in enumerate(late):
            copy = pltpu.make_async_copy(ins[at], own[spot], own[-1].at[spot])
            copy.start()
            copies.append(copy)
            ins[at] = own[spot]
        kernel(*ins, *rest, late=copies)

    return pl.pallas_call(
        body,
        out_shape=out_shape,
        in_specs=specs,
        out_specs=out_specs or [vm] * len(out_shape),
        scratch_shapes=scratch + inside,
        compiler_params=pltpu.CompilerParams(
            collective_id=cid, has_side_effects=True, vmem_limit_bytes=VMEM_LIMIT
        ),
        name=f"{name}_{cid}",
    )(*operands)


class Tiny:
    def __init__(self, here, src, dst, sems, spread):
        self.here, self.src, self.dst, self.sems, self.spread = here, src, dst, sems, spread
        self.peers = slice_peers(here)
        self.me = here.shard(0, 0)

    def tile(self, shard):
        return self.src.at[shard] if self.spread else self.src

    def copy(self, at):
        return remote(self.tile(self.here.shard(*turned(at))), self.dst.at[self.me], self.sems[0].at[at],
                      self.sems[1].at[at], self.peers[at])

    def begin(self):
        for at in range(7):
            self.copy(at).start()
        self.dst[self.me] = self.tile(self.me)[...]

    def end(self):
        for at in range(7):
            self.copy(at).wait()


class Reduce:
    def __init__(self, here, counts, product, refs, before=None):
        self.counts, self.product, self.before = counts, product, before
        self.held, self.sib_out, self.sib_in, self.from_x, self.from_y = refs[:5]
        self.sib_sems, self.x_sems, self.y_sems = refs[5:7], refs[7:9], refs[9:11]
        self.sib, self.xdev, self.ydev = here.device(0, 1), here.device(1, 0), here.device(2, 0)
        self.steps = 4 * counts
        self.ring = self.sib_out.shape[0]

    def streams(self, stage):
        far = stage // 3
        x_chip = jnp.where(stage == 0, 3, jnp.where(stage == 2, 0, 1))
        y_chip = jnp.where(stage == 0, 3, jnp.where(stage == 2, 0, 2))
        return (x_chip, far), (y_chip, 1 - far)

    def to_sib(self, step, stream):
        stage, at = step // self.counts, step % self.counts
        return remote(self.sib_out.at[step % self.ring, stream], self.sib_in.at[stage, stream, at],
                      self.sib_sems[0].at[stage, stream, at], self.sib_sems[1].at[stage, stream, at], self.sib)

    def to_x(self, hop, at, stage=0):
        return remote(self.held.at[stage, 0, at], self.from_x.at[hop, at], self.x_sems[0].at[hop, at],
                      self.x_sems[1].at[hop, at], self.xdev)

    def to_y(self, hop, at, stage=0):
        return remote(self.held.at[stage, 1, at], self.from_y.at[hop, at], self.y_sems[0].at[hop, at],
                      self.y_sems[1].at[hop, at], self.ydev)

    def compute(self, step):
        stage, at = step // self.counts, step % self.counts
        if self.before:
            for stop in range(3):
                @pl.when(step == stop * self.counts)
                def _():
                    self.before(stop)

        @pl.when(step >= self.ring)
        def _():
            for stream in range(2):
                self.to_sib(step - self.ring, stream).wait_send()

        for stream, (across, half) in enumerate(self.streams(stage)):
            self.sib_out[step % self.ring, stream] = self.product(across, 1, half, at).astype(jnp.bfloat16)
            self.held[stage, stream, at] = self.product(across, 0, half, at).astype(jnp.bfloat16)
        for stream in range(2):
            self.to_sib(step, stream).start()

    def finish(self, step):
        stage, at = step // self.counts, step % self.counts
        for stream in range(2):
            self.to_sib(step, stream).wait_recv()

        def total(stream):
            return self.held[stage, stream, at].astype(jnp.float32) + self.sib_in[stage, stream, at].astype(
                jnp.float32)

        @pl.when(stage < 3)
        def _():
            for stream in range(2):
                self.held[stage, stream, at] = total(stream).astype(jnp.bfloat16)

        @pl.when(stage == 3)
        def _():
            self.to_y(0, at).wait_recv()
            self.held[3, 0, at] = (total(0) + self.from_y[0, at].astype(jnp.float32)).astype(jnp.bfloat16)
            self.to_x(0, at).wait_recv()
            self.held[3, 1, at] = (total(1) + self.from_x[0, at].astype(jnp.float32)).astype(jnp.bfloat16)

        @pl.when(stage != 2)
        def _():
            hop = stage - stage // 3
            self.to_x(hop, at, stage).start()
            self.to_y(hop, at, stage).start()

    def advance(self, step):
        @pl.when(step < self.steps)
        def _():
            self.compute(step)

        @pl.when(jnp.logical_and(step > 0, step <= self.steps))
        def _():
            self.finish(step - 1)

    def run(self, hook=None):
        def body(step, _):
            self.advance(step)

            if hook:
                hook(step)
            return 0

        lax.fori_loop(0, self.steps + 1, body, 0)
        return self.steps + 1

    def end(self, emit):
        def last(at, _):
            values = []
            for half in range(2):
                xs, ys = (1, 2) if half == 0 else (2, 1)
                self.to_x(xs, at).wait_recv()
                self.to_y(ys, at).wait_recv()
                values.append(self.held[2, half, at].astype(jnp.float32) + self.from_x[xs, at].astype(jnp.float32)
                              + self.from_y[ys, at].astype(jnp.float32))
            emit(at, *values)
            for hop in range(3):
                self.to_x(hop, at).wait_send()
                self.to_y(hop, at).wait_send()
            return 0

        lax.fori_loop(0, self.counts, last, 0)

        def drain(at, _):
            for stream in range(2):
                self.to_sib(self.steps - self.ring + at, stream).wait_send()
            return 0

        lax.fori_loop(0, self.ring, drain, 0)


def reduce_scratch(counts, rows, width, ring=4):
    low, dma = jnp.bfloat16, pltpu.SemaphoreType.DMA
    block = pltpu.VMEM((4, 2, counts, rows, width), low)
    landed = pltpu.VMEM((3, counts, rows, width), low)
    sent = pltpu.VMEM((ring, 2, rows, width), low)
    return [block, sent, block, landed, landed] + [dma((4, 2, counts))] * 2 + [dma((3, counts))] * 4


class Spread:
    def __init__(self, here, counts, refs):
        self.counts = counts
        self.got = refs[0]
        self.x_sems, self.y_sems, self.sib_sems = refs[1:3], refs[3:5], refs[5:7]
        self.core = here.core
        self.sib, self.xdev, self.ydev = here.device(0, 1), here.device(1, 0), here.device(2, 0)

    def slot(self, across, half, at):
        return self.got.at[across, self.core, half, at]

    def x_copy(self, hop, at):
        half = jnp.minimum(hop, 1)
        src = self.slot(2 * (hop // 2), half, at)
        dst = self.slot(1 + 2 * (hop // 2), half, at)
        return remote(src, dst, self.x_sems[0].at[hop, at], self.x_sems[1].at[hop, at], self.xdev)

    def y_copy(self, hop, at):
        half = 1 - jnp.minimum(hop, 1)
        src = self.slot(hop // 2, half, at)
        dst = self.slot(2 + hop // 2, half, at)
        return remote(src, dst, self.y_sems[0].at[hop, at], self.y_sems[1].at[hop, at], self.ydev)

    def streams(self, stage):
        some, last, late = jnp.minimum(stage, 1), stage // 3, stage // 2
        return (some + 2 * last, late), (2 * some + last, 1 - late)

    def block(self, at):
        x_stream, y_stream = self.streams(at // 4)
        second = at // 2 % 2
        across = x_stream[0] + second * (y_stream[0] - x_stream[0])
        half = x_stream[1] + second * (y_stream[1] - x_stream[1])
        return across, at % 2, half

    def begin_rows(self):
        for hop in range(2):
            self.x_copy(hop, 0).start()
            self.y_copy(hop, 0).start()
        for stream in range(2):
            self.sib_copy(0, stream, 0).start()

    def receive_rows(self, step):
        stage = step // 4

        @pl.when(jnp.logical_and(step % 4 == 0, jnp.logical_and(stage > 0, stage < 4)))
        def _():
            self.x_copy(stage - 1, 0).wait_recv()
            self.sib_copy(stage, 0, 0).start()
            self.y_copy(stage - 1, 0).wait_recv()
            self.sib_copy(stage, 1, 0).start()

        @pl.when(step == 4)
        def _():
            self.x_copy(2, 0).start()
            self.y_copy(2, 0).start()

        for stream in range(2):
            @pl.when(jnp.logical_and(step % 4 == 2 * stream, step < 16))
            def _(stream=stream):
                self.sib_copy(stage, stream, 0).wait_recv()

    def sib_copy(self, stage, stream, at):
        across, half = self.streams(stage)[stream]
        slot = self.slot(across, half, at)
        spot = (stage, stream, at)
        return remote(slot, slot, self.sib_sems[0].at[spot], self.sib_sems[1].at[spot], self.sib)

    def begin(self):
        def first(at, _):
            self.x_copy(0, at).start()
            self.y_copy(0, at).start()
            return 0

        def own(at, _):
            self.sib_copy(0, 0, at).start()
            self.sib_copy(0, 1, at).start()
            return 0

        lax.fori_loop(0, self.counts, first, 0)
        lax.fori_loop(0, self.counts, own, 0)

    def run(self, blocks, hook=None, done=None):
        counts = self.counts

        def body(step, _):
            stage, at = step // counts, step % counts

            @pl.when(jnp.logical_and(stage > 0, stage < 4))
            def _():
                self.x_copy(stage - 1, at).wait_recv()
                self.sib_copy(stage, 0, at).start()
                self.y_copy(stage - 1, at).wait_recv()
                self.sib_copy(stage, 1, at).start()

            @pl.when(jnp.logical_and(stage > 0, stage < 3))
            def _():
                self.x_copy(stage, at).start()
                self.y_copy(stage, at).start()

            @pl.when(step > 0)
            def _():
                old, spot = (step - 1) // counts, (step - 1) % counts
                for stream, (across, half) in enumerate(self.streams(old)):
                    self.sib_copy(old, stream, spot).wait_recv()
                    blocks(across, half, spot)
                if done:
                    done(old, spot)

            if hook:
                hook(step)
            return 0

        lax.fori_loop(0, 4 * counts + 1, body, 0)
        return 4 * counts + 1

    def end(self):
        def drain(at, _):
            for hop in range(3):
                self.x_copy(hop, at).wait_send()
                self.y_copy(hop, at).wait_send()
            for stage in range(4):
                self.sib_copy(stage, 0, at).wait_send()
                self.sib_copy(stage, 1, at).wait_send()
            return 0

        lax.fori_loop(0, self.counts, drain, 0)


def spread_scratch(counts, rows, width):
    dma = pltpu.SemaphoreType.DMA
    return [pltpu.VMEM((4, 2, 2, counts, rows, width), jnp.bfloat16)] + [dma((3, counts))] * 4 + [
        dma((4, 2, counts))] * 2


def row_span(here, across, other, rows):
    return pl.ds(pl.multiple_of(here.shard(across, other) * rows, rows), rows)


def dot_nt(left, right):
    return lax.dot_general(left, right, (((1,), (1,)), ((), ())), preferred_element_type=jnp.float32)


def dot_tn(left, right):
    return lax.dot_general(left, right, (((0,), (0,)), ((), ())), preferred_element_type=jnp.float32)


def dot_nn(left, right):
    return jnp.dot(left, right, preferred_element_type=jnp.float32)


def products(here, act, weight, nt, rows, width, counts):
    def product(across, other, half, at):
        cols = pl.ds(pl.multiple_of((half * counts + at) * width, width), width)
        block = act[row_span(here, across, other, rows), :]
        return dot_nt(block, weight[cols, :]) if nt else dot_nn(block, weight[:, cols])

    return product


def diagonal():
    return (lax.broadcasted_iota(jnp.int32, (LANES, LANES), 0) ==
            lax.broadcasted_iota(jnp.int32, (LANES, LANES), 1)).astype(jnp.float32)


def to_tile(tile, first, column, eye):
    for at in range(column.shape[0] // LANES):
        spread = column[at * LANES : (at + 1) * LANES, :] * eye
        tile[first + at : first + at + 1, :] = jnp.sum(spread, axis=0, keepdims=True)


def from_tile(row, eye):
    return jnp.sum(eye * row, axis=1, keepdims=True)


def make_tables(here, rows, segs, cos, sin, mask):
    eye = diagonal()
    tiles = rows // LANES
    freqs = jnp.exp(lax.broadcasted_iota(jnp.int32, (1, LANES), 1).astype(jnp.float32) * (-math.log(10000.0) / LANES))
    lane = lax.broadcasted_iota(jnp.int32, (1, LANES), 1)
    line = lax.broadcasted_iota(jnp.int32, (LANES, 1), 0)

    def ids_of(row):
        return segs[2:3, pl.ds(pl.multiple_of(row * LANES, LANES), LANES)]

    def row_of(side, at):
        return ((here.seq + side) % 2) * tiles + at

    for side in range(2):
        for at in range(tiles):
            row = row_of(side, at)
            ids = from_tile(ids_of(row), eye)
            before = jnp.zeros((LANES, 1), jnp.float32)
            for other in range(2 * tiles):
                smaller = ids_of(other) < ids
                before += jnp.sum(smaller.astype(jnp.float32), axis=-1, keepdims=True)
            index = row * LANES + line
            angles = (index.astype(jnp.float32) - before) * freqs
            span = slice(at * LANES, (at + 1) * LANES)
            cos[side, span, :] = jnp.cos(angles)
            sin[side, span, :] = jnp.sin(angles)
            if side == 0:
                for key_side in range(2):
                    for key_at in range(tiles):
                        key_row = row_of(key_side, key_at)
                        same = ids_of(key_row) == ids
                        allowed = jnp.logical_and(same, key_row * LANES + lane <= index)
                        first = key_side * rows + key_at * LANES
                        mask[span, first : first + LANES] = allowed.astype(jnp.float32)


def open_kernel(rows, width, counts, tokens, gain, w_query, kv_weight, cot, qkv, x_low, act_t, w_qkv, rms, cos, sin,
                mask, g_col, *refs):
    here = Place()
    cols, segs = gain.shape[1], gain
    act, turn_send, turn_recv, local_sems, cot_part, g_send, g_recv, z_send, z_recv = refs[:9]
    share = rows // 4
    me = here.shard(0, 0)
    own_rows = pl.ds(pl.multiple_of(me * rows, rows), rows)

    def turn_copy(at):
        across, other = turned(at)
        first = pl.multiple_of(here.shard(across, other) * cols, cols)
        return remote(tokens.at[:, pl.ds(first, cols)], x_low.at[own_rows, :], turn_send.at[at], turn_recv.at[at],
                      here.device(across, other))

    wide = w_query.shape[1]
    local = [
        pltpu.make_async_copy(w_query, w_qkv.at[:, :wide], local_sems.at[0]),
        pltpu.make_async_copy(kv_weight, w_qkv.at[:, wide:], local_sems.at[1]),
        pltpu.make_async_copy(tokens.at[:, pl.ds(pl.multiple_of(me * cols, cols), cols)], x_low.at[own_rows, :],
                              local_sems.at[2]),
    ]
    load = pltpu.make_async_copy(cot.at[pl.ds(pl.multiple_of(here.z * share, share), share), :], cot_part,
                                 local_sems.at[3])
    load.start()
    for copy in local:
        copy.start()

    def g_copy(at):
        across, other = turned(at)
        first = pl.multiple_of(here.shard(across, other) * cols, cols)
        return remote(cot_part.at[:, pl.ds(first, cols)], g_col.at[me, here.z], g_send.at[at], g_recv.at[at],
                      here.device(across, other))

    def own_part():
        return pltpu.make_async_copy(cot_part.at[:, pl.ds(pl.multiple_of(me * cols, cols), cols)],
                                     g_col.at[me, here.z], local_sems.at[4])

    def quarter(way, at, step, peer):
        spot = g_col.at[:, at]
        return remote(spot, spot, z_send.at[way, step], z_recv.at[way, step], (here.dp, here.seq, here.z + peer))

    def pass_on(step):
        @pl.when(jnp.logical_and(here.z < 3, here.z >= step))
        def _():
            quarter(0, here.z - step, step, 1).start()

        @pl.when(jnp.logical_and(here.z > 0, here.z <= 3 - step))
        def _():
            quarter(1, here.z + step, step, -1).start()

    def take_quarters(step):
        @pl.when(here.z > step)
        def _():
            quarter(0, here.z - 1 - step, step, -1).wait_recv()

        @pl.when(here.z < 3 - step)
        def _():
            quarter(1, here.z + 1 + step, step, 1).wait_recv()

    greet(here, slice_peers(here), True)
    load.wait()
    own_part().start()
    for at in range(7):
        g_copy(at).start()
    for at in range(7):
        turn_copy(at).start()
    for copy in local:
        copy.wait()

    def squares(at, total):
        values = tokens[:, pl.ds(pl.multiple_of(at * cols, cols), cols)].astype(jnp.float32)
        return total + jnp.sum(values * values, axis=-1, keepdims=True)

    total = lax.fori_loop(0, 8, squares, jnp.zeros((rows, 1), jnp.float32))
    rms[...] = jnp.broadcast_to(lax.rsqrt(total / (8 * cols) + EPS), rms.shape)
    make_tables(here, rows, segs, cos, sin, mask)

    def prepare(first, count):
        def one(step, _):
            at = first + step
            span = row_span(here, *turned(at), rows)
            value = (x_low[span, :].astype(jnp.float32) * gain[0:1, :]).astype(act.dtype)
            act[span, :] = value
            return 0

        lax.fori_loop(0, count, one, 0)

    def before(stop):
        first, count = ((0, 2), (2, 4), (6, 2))[stop]
        if stop == 0:
            own_part().wait()
            for at in range(7):
                g_copy(at).wait_recv()
        else:
            take_quarters(stop - 1)
        pass_on(stop)
        for at in range(first, min(first + count, 7)):
            turn_copy(at).wait_recv()
        prepare(first, count)

    def flip():
        def one(shard, _):
            span = pl.ds(pl.multiple_of(shard * rows, rows), rows)
            act_t[:, span] = act[span, :].T
            return 0

        lax.fori_loop(0, 8, one, 0)

    product = products(here, act, w_qkv, False, rows, width, counts)
    total = Reduce(here, counts, product, refs[9:20], before)
    total.run()
    flip()

    def emit(at, first, second):
        for half, value in enumerate((first, second)):
            qkv[:, pl.ds(pl.multiple_of((half * counts + at) * width, width), width)] = value

    total.end(emit)
    take_quarters(2)
    for at in range(7):
        turn_copy(at).wait_send()
        g_copy(at).wait_send()
    for step in range(3):
        @pl.when(jnp.logical_and(here.z < 3, here.z >= step))
        def _(step=step):
            quarter(0, here.z - step, step, 1).wait_send()

        @pl.when(jnp.logical_and(here.z > 0, here.z <= 3 - step))
        def _(step=step):
            quarter(1, here.z + step, step, -1).wait_send()


def opening(tokens, gain, w_query, kv_weight, cot, cid, width=256):
    rows = tokens.shape[0]
    cols, wide = w_query.shape
    every = wide + kv_weight.shape[1]
    counts = every // (2 * width)
    low, f32 = jnp.bfloat16, jnp.float32
    dma = pltpu.SemaphoreType.DMA
    vm = pl.BlockSpec(memory_space=pltpu.VMEM)
    hbm = pl.BlockSpec(memory_space=pl.ANY)
    out_shape = [
        jax.ShapeDtypeStruct((rows, every), f32),
        jax.ShapeDtypeStruct((8 * rows, cols), low),
        jax.ShapeDtypeStruct((cols, 8 * rows), low),
        jax.ShapeDtypeStruct((cols, every), low),
        jax.ShapeDtypeStruct((rows, LANES), f32),
        jax.ShapeDtypeStruct((2, rows, LANES), f32),
        jax.ShapeDtypeStruct((2, rows, LANES), f32),
        jax.ShapeDtypeStruct((rows, 2 * rows), f32),
        jax.ShapeDtypeStruct((8, 4, rows // 4, cols), low),
    ]
    scratch = [
        pltpu.VMEM((8 * rows, cols), low), dma((7,)), dma((7,)), dma((5,)),
        pltpu.VMEM((rows // 4, 8 * cols), low), dma((7,)), dma((7,)), dma((2, 3)), dma((2, 3)),
    ]
    scratch += reduce_scratch(counts, rows, width)
    kernel = functools.partial(open_kernel, rows, width, counts)
    return kernel_call(kernel, out_shape, [tokens, gain, w_query, kv_weight, cot],
                       [vm, vm, hbm, hbm, hbm], scratch, cid, "open")


def ffn_kernel(rows, width, counts, x_low, attn, gain, w_gate, w_up, d_hidden, hidden, d_gate, d_up, act_t, tile_out,
               *refs, late):
    here = Place()
    cols = gain.shape[1]
    act, weight, tiny_own, tiny_all, tiny_send, tiny_recv, dots, local_sems = refs[:8]
    tiny = Tiny(here, tiny_own, tiny_all, (tiny_send, tiny_recv), True)
    half_cols = counts * width
    local = [
        pltpu.make_async_copy(w_gate, weight.at[:, :half_cols], local_sems.at[0]),
        pltpu.make_async_copy(w_up, weight.at[:, half_cols:], local_sems.at[1]),
    ]
    for copy in local:
        copy.start()
    eye = diagonal()
    tiny_own[...] = jnp.zeros_like(tiny_own)

    def prepare(number, _):
        shard = here.shard(*turned(number))
        for at in range(rows // LANES):
            span = pl.ds(pl.multiple_of(shard * rows + at * LANES, LANES), LANES)
            resid = x_low[span, :].astype(jnp.float32) + attn[span, :].astype(jnp.float32)
            act[span, :] = (resid * gain[1:2, :]).astype(act.dtype)
            square = jnp.sum(resid * resid, axis=-1, keepdims=True)
            tiny_own[shard, at : at + 1, :] = jnp.sum(square * eye, axis=0, keepdims=True)
        return 0

    def before(stop):
        if stop == 1:
            lax.fori_loop(2, 6, prepare, 0)
        if stop == 2:
            lax.fori_loop(6, 8, prepare, 0)
            tiny.begin()

    lax.fori_loop(0, 2, prepare, 0)
    greet(here, slice_peers(here))
    for copy in local:
        copy.wait()
    product = products(here, act, weight, False, rows, width, counts)
    total = Reduce(here, counts, product, refs[8:19], before)
    total.run()

    def flip(shard, _):
        span = pl.ds(pl.multiple_of(shard * rows, rows), rows)
        act_t[:, span] = act[span, :].T
        return 0

    lax.fori_loop(0, 8, flip, 0)
    tiny.end()
    tiles = rows // LANES
    mean = [from_tile(jnp.sum(tiny_all[:, at, :], axis=0, keepdims=True), eye) for at in range(tiles)]
    scale = lax.rsqrt(jnp.concatenate(mean, axis=0) / (8 * cols) + EPS)
    dots[...] = jnp.zeros_like(dots)
    late[0].wait()
    coeff = math.sqrt(2.0 / math.pi)

    def emit(at, first, second):
        span = pl.ds(pl.multiple_of(at * width, width), width)
        gate, up = first * scale, second * scale
        inner = jnp.tanh(coeff * (gate + 0.044715 * (gate * gate * gate)))
        gelu = 0.5 * gate * (1.0 + inner)
        slope = 0.5 * (1.0 + inner) + 0.5 * gate * (1.0 - inner * inner) * (
            coeff * (1.0 + 3.0 * 0.044715 * gate * gate))
        cot = d_hidden[:, span]
        hidden[:, span] = (gelu * up).astype(hidden.dtype)
        back_gate, back_up = cot * up * slope, cot * gelu
        d_gate[:, span] = (back_gate * scale).astype(d_gate.dtype)
        d_up[:, span] = (back_up * scale).astype(d_up.dtype)
        dots[...] += jnp.sum(back_gate * gate + back_up * up, axis=-1, keepdims=True)

    total.end(emit)
    tile_out[...] = jnp.zeros_like(tile_out)
    to_tile(tile_out, 0, dots[...] * (scale * scale * (1.0 / (8 * cols))), eye)


def ffn_scatter(x_low, attn, gain, w_gate, w_up, d_hidden, cid, width=512):
    rows, half = d_hidden.shape
    cols = gain.shape[1]
    counts = half // width
    low, f32 = jnp.bfloat16, jnp.float32
    dma = pltpu.SemaphoreType.DMA
    vm = pl.BlockSpec(memory_space=pltpu.VMEM)
    hbm = pl.BlockSpec(memory_space=pl.ANY)
    out_shape = [jax.ShapeDtypeStruct((rows, half), low)] * 3 + [
        jax.ShapeDtypeStruct((cols, 8 * rows), low),
        jax.ShapeDtypeStruct((8, LANES), f32),
    ]
    scratch = [
        pltpu.VMEM((8 * rows, cols), low),
        pltpu.VMEM((cols, 2 * half), low),
        pltpu.VMEM((8, 8, LANES), f32),
        pltpu.VMEM((8, 8, LANES), f32),
        dma((7,)), dma((7,)),
        pltpu.VMEM((rows, 1), f32),
        dma((2,)),
    ] + reduce_scratch(counts, rows, width)
    kernel = functools.partial(ffn_kernel, rows, width, counts)
    return kernel_call(kernel, out_shape, [x_low, attn, gain, w_gate, w_up, d_hidden], [vm, vm, vm, hbm, hbm, vm],
                       scratch, cid, "ffn", late=(5,))


def load_own(spread, payload, width, counts, sems):
    copies = []
    for half in range(2):
        for at in range(counts):
            first = at * width + (half * counts * width if len(payload) == 1 else 0)
            src = payload[half % len(payload)].at[:, first : first + width]
            copies.append(pltpu.make_async_copy(src, spread.slot(0, half, at), sems.at[half, at]))
    return copies


def chip_place(here, per):
    def place(at):
        return here.shard(at // (2 * per), at // per % 2) * per + at % per

    return place


def back_kernel(rows, width, counts, act_t, w_gate, w_up, d_gate, d_up, dots, x_low, attn, gain, d_norm, gain_grad,
                grad_gate, grad_up, *refs, late):
    here = Place()
    spread = Spread(here, counts, refs[:7])
    tiny_all, tiny_send, tiny_recv, own_sems, weight, sums, grads, staged, local_sems, out_sems = refs[7:17]
    contrib, rest, rest_sems = refs[17:20]
    line = Line(here, 4, [contrib, d_norm] + list(refs[20:]), chip_place(here, 2))
    tiny = Tiny(here, dots, tiny_all, (tiny_send, tiny_recv), False)
    half_cols = counts * width
    local = [
        pltpu.make_async_copy(w_gate, weight.at[:, :half_cols], local_sems.at[0]),
        pltpu.make_async_copy(w_up, weight.at[:, half_cols:], local_sems.at[1]),
    ]
    own = load_own(spread, (d_gate, d_up), width, counts, own_sems)
    for copy in own + local:
        copy.start()
    greet(here, tiny.peers, True)
    for copy in own:
        copy.wait()
    tiny.begin()
    spread.begin()
    sums[...] = jnp.zeros_like(sums)
    for copy in local + late:
        copy.wait()

    def columns(half, at):
        return pl.ds(pl.multiple_of((half * counts + at) * width, width), width)

    def clear(at, _):
        grads[:, columns(0, at)] = jnp.zeros((grads.shape[0], width), jnp.float32)
        return 0

    lax.fori_loop(0, 2 * counts, clear, 0)

    def blocks(across, half, at):
        cols = columns(half, at)
        gained = grads[:, cols]
        for other in range(2):
            row = row_span(here, across, other, rows)
            block = spread.got[across, (spread.core + other) % 2, half, at]
            sums[row, :] += dot_nt(block, weight[:, cols])
            gained = gained + dot_nn(act_t[:, row], block)
        grads[:, cols] = gained

    def leave(half, at):
        spot = pl.ds(pl.multiple_of(at * width, width), width)
        return pltpu.make_async_copy(staged.at[half], (grad_gate, grad_up)[half].at[:, spot],
                                     out_sems.at[half, at])

    eye = diagonal()
    gain_grad[...] = jnp.zeros_like(gain_grad)

    def close_chip(chip, target):
        def close_shard(other, _):
            shard = here.shard(chip, other)
            span = pl.ds(pl.multiple_of(shard * rows, rows), rows)
            loads = [pltpu.make_async_copy(src.at[span, :], rest.at[at], rest_sems.at[at])
                     for at, src in enumerate((x_low, attn))]
            for copy in loads:
                copy.start()
            for copy in loads:
                copy.wait()
            for at in range(rows // LANES):
                span = pl.ds(pl.multiple_of(shard * rows + at * LANES, LANES), LANES)
                piece = slice(at * LANES, (at + 1) * LANES)
                dot = from_tile(tiny_all[shard, at : at + 1, :], eye)
                resid = rest[0, piece, :].astype(jnp.float32) + rest[1, piece, :].astype(jnp.float32)
                value = sums[span, :]
                target[span, :] = (value * gain[1:2, :] - resid * dot).astype(target.dtype)
                gain_grad[...] += jnp.sum(value * resid, axis=0, keepdims=True)
            return 0

        lax.fori_loop(0, 2, close_shard, 0)

    def done(stage, at):
        @pl.when(jnp.logical_and(stage == 3, at > 0))
        def _():
            leave(0, at - 1).wait()
            leave(1, at - 1).wait()

        @pl.when(stage == 3)
        def _():
            for half in range(2):
                staged[half] = grads[:, columns(half, at)].astype(staged.dtype)
            leave(0, at).start()
            leave(1, at).start()

        @pl.when(jnp.logical_and(at == counts - 1, stage == 0))
        def _():
            close_chip(0, contrib)
            line.launch(0, 4)

        @pl.when(jnp.logical_and(at == counts - 1, stage == 2))
        def _():
            lax.fori_loop(1, 3, lambda chip, _: (close_chip(chip, d_norm), 0)[1], 0)

    def hook(step):
        @pl.when(jnp.logical_and(step >= counts, step < counts + 6))
        def _():
            line.step(step - counts)

    tiny.end()
    spread.run(blocks, hook, done)
    close_chip(3, d_norm)
    line.settle()
    spread.end()

    def drain(at, _):
        leave(0, at).wait()
        leave(1, at).wait()
        return 0

    lax.fori_loop(counts - 1, counts, drain, 0)


def back_gather(act_t, w_gate, w_up, d_gate, d_up, dots, x_low, attn, gain, cid, width=512):
    cols, total = act_t.shape
    rows, half = d_gate.shape
    counts = half // width
    low, f32 = jnp.bfloat16, jnp.float32
    dma = pltpu.SemaphoreType.DMA
    vm = pl.BlockSpec(memory_space=pltpu.VMEM)
    hbm = pl.BlockSpec(memory_space=pl.ANY)
    out_shape = [
        jax.ShapeDtypeStruct((total, cols), low),
        jax.ShapeDtypeStruct((1, cols), f32),
        jax.ShapeDtypeStruct((cols, half), low),
        jax.ShapeDtypeStruct((cols, half), low),
    ]
    scratch = spread_scratch(counts, rows, width) + [
        pltpu.VMEM((8, 8, LANES), f32), dma((7,)), dma((7,)), dma((2, counts)),
        pltpu.VMEM((cols, 2 * half), low),
        pltpu.VMEM((total, cols), f32),
        pltpu.VMEM((cols, 2 * half), f32),
        pltpu.VMEM((2, cols, width), low),
        dma((2,)), dma((2, counts)),
        pltpu.VMEM((total, cols), low),
        pltpu.VMEM((2, rows, cols), low),
        dma((2,)),
    ] + line_scratch(4, (4 * rows // 2, cols), low)
    operands = [act_t, w_gate, w_up, d_gate, d_up, dots, x_low, attn, gain]
    kernel = functools.partial(back_kernel, rows, width, counts)
    return kernel_call(kernel, out_shape, operands, [vm] + [hbm] * 4 + [vm, hbm, hbm, vm], scratch, cid, "back",
                       [vm, vm, hbm, hbm], (0,))


def down_kernel(rows, width, counts, cot, weight, hidden, d_norm, ffn, d_attn, grad, *refs, late):
    here = Place()
    spread = Spread(here, counts, refs[:7])
    own_sems, sums, grads, staged, out_sems, norm_out = refs[7:13]
    place = chip_place(here, 4)
    norm_line = Line(here, 24, [d_norm, norm_out] + list(refs[13:]), lambda at: place(at + 8))
    own = load_own(spread, (hidden,), width, counts, own_sems)
    for copy in own:
        copy.start()
    greet(here, slice_peers(here), True)
    norm_line.begin()
    for copy in own:
        copy.wait()
    spread.begin()
    sums[...] = jnp.zeros_like(sums)
    grads[...] = jnp.zeros_like(grads)
    for copy in late:
        copy.wait()

    def columns(half, at):
        return pl.ds(pl.multiple_of((half * counts + at) * width, width), width)

    def blocks(across, half, at):
        cols = columns(half, at)
        gained = grads[cols, :]
        for other in range(2):
            row = row_span(here, across, other, rows)
            block = spread.got[across, (spread.core + other) % 2, half, at]
            sums[row, :] += dot_nn(block, weight[cols, :])
            gained = gained + dot_tn(block, cot[row, :])
        grads[cols, :] = gained

    def leave(half, at):
        return pltpu.make_async_copy(staged.at[at % 2, half], grad.at[columns(half, at), :], out_sems.at[half, at])

    def done(stage, at):
        @pl.when(jnp.logical_and(stage == 3, at > 1))
        def _():
            leave(0, at - 2).wait()
            leave(1, at - 2).wait()

        @pl.when(stage == 3)
        def _():
            for half in range(2):
                staged[at % 2, half] = grads[columns(half, at), :].astype(staged.dtype)
            leave(0, at).start()
            leave(1, at).start()

    norm_line.steps(spread.run(blocks, norm_line.step, done), 26)
    ffn[...] = sums[...].astype(ffn.dtype)
    norm_line.settle()

    def add_norm(at, _):
        def add(source):
            span = row_span(here, at // 2, at % 2, rows)
            d_attn[span, :] = (cot[span, :].astype(jnp.float32) + source[span, :].astype(jnp.float32)).astype(
                d_attn.dtype)

        @pl.when(at < 2)
        def _():
            add(d_norm)

        @pl.when(at >= 2)
        def _():
            add(norm_out)
        return 0

    lax.fori_loop(0, 8, add_norm, 0)
    spread.end()

    def drain(at, _):
        leave(0, at).wait()
        leave(1, at).wait()
        return 0

    lax.fori_loop(counts - 2, counts, drain, 0)


def down_gather(cot, weight, hidden, d_norm, cid, width=256):
    total, cols = cot.shape
    rows, every = hidden.shape
    counts = every // (2 * width)
    low, f32 = jnp.bfloat16, jnp.float32
    dma = pltpu.SemaphoreType.DMA
    vm = pl.BlockSpec(memory_space=pltpu.VMEM)
    hbm = pl.BlockSpec(memory_space=pl.ANY)
    out_shape = [
        jax.ShapeDtypeStruct((total, cols), low),
        jax.ShapeDtypeStruct((total, cols), low),
        jax.ShapeDtypeStruct(weight.shape, low),
    ]
    scratch = spread_scratch(counts, rows, width) + [
        dma((2, counts)),
        pltpu.VMEM((total, cols), f32),
        pltpu.VMEM(weight.shape, f32),
        pltpu.VMEM((2, 2, width, cols), low),
        dma((2, counts)),
        pltpu.VMEM((total, cols), low),
    ] + line_scratch(24, (24 * rows // 4, cols), low)
    kernel = functools.partial(down_kernel, rows, width, counts)
    return kernel_call(kernel, out_shape, [cot, weight, hidden, d_norm], [vm, vm, hbm, vm], scratch, cid, "down",
                       [vm, vm, hbm], (0, 1))


def attend_kernel(rows, heads, cols, width, counts, qkv, rms, cos, sin, mask, w_out, g_col, w_down, attn, mixed_all,
                  kv, probs, queries, pair_rms, d_hidden, *refs, late):
    here = Place()
    spread = Spread(here, 1, refs[:7])
    part, pair_sems, tiny_own, tiny_pair, mixed_sems = refs[7:12]
    product = products(here, g_col, w_down, True, rows, width, counts)
    total = Reduce(here, counts, product, refs[12:23])
    piece = rows // 2

    def place(at):
        across, other, half_at = spread.block(at)
        return here.shard(across, other) * 2 + half_at

    line = Line(here, 32, [part, attn] + list(refs[23:]), lambda at: place(at // 2) * 2 + at % 2)
    got, core = spread.got, here.core
    greet(here, slice_peers(here), True)
    half = HD // 2
    scale = 1.0 / math.sqrt(HD)
    wide = heads * HD

    def rotated(first):
        lead = qkv[:, first : first + half] * rms[...]
        trail = qkv[:, first + half : first + HD] * rms[...]
        return lead * cos[0] - trail * sin[0], trail * cos[0] + lead * sin[0]

    low_k, high_k = rotated(wide)
    kv[0, :, :half] = low_k.astype(kv.dtype)
    kv[0, :, half:HD] = high_k.astype(kv.dtype)
    for at in range(2):
        first = HD + at * half
        kv[0, :, first : first + half] = (qkv[:, wide + first : wide + first + half] * rms[...]).astype(kv.dtype)
    eye = diagonal()
    tiny_own[...] = jnp.zeros_like(tiny_own)
    to_tile(tiny_own, 0, rms[:, :1], eye)
    pair_rms[0] = rms[...]
    pair = remote(kv.at[0], kv.at[1], pair_sems.at[0], pair_sems.at[1], spread.ydev)
    tiny = remote(tiny_own, tiny_pair, pair_sems.at[2], pair_sems.at[3], spread.ydev)
    for head in range(heads):
        if head == 1:
            pair.start()
            tiny.start()
        lead, trail = rotated(head * HD)
        queries[:, head * HD : head * HD + half] = (lead * scale).astype(queries.dtype)
        queries[:, head * HD + half : (head + 1) * HD] = (trail * scale).astype(queries.dtype)
    pair.wait()
    for copy in late:
        copy.wait()

    def one_head(head, _):
        query = queries[:, pl.ds(pl.multiple_of(head * HD, HD), HD)]
        scores = jnp.concatenate([dot_nt(query, kv[0, :, :HD]), dot_nt(query, kv[1, :, :HD])], axis=1)
        scores = jnp.where(mask[...] > 0, scores, NEG)
        expd = jnp.exp(scores - jnp.max(scores, axis=-1, keepdims=True))
        prob = expd / jnp.sum(expd, axis=-1, keepdims=True)
        probs[head] = prob
        prob_low = prob.astype(jnp.bfloat16)
        mixed = dot_nn(prob_low[:, :rows], kv[0, :, HD:]) + dot_nn(prob_low[:, rows:], kv[1, :, HD:])
        span = pl.ds(pl.multiple_of(head * HD, HD), HD)
        for half_at in range(2):
            low_mixed = mixed[half_at * piece : (half_at + 1) * piece, :].astype(got.dtype)
            got[0, core, half_at, 0, :, span] = low_mixed
        return 0

    lax.fori_loop(0, heads, one_head, 0)
    spread.begin_rows()

    def mixed_copy(at):
        across, other, half_at = spread.block(at)
        span = pl.ds(pl.multiple_of(place(at) * piece, piece), piece)
        return pltpu.make_async_copy(got.at[across, (core + other) % 2, half_at, 0], mixed_all.at[span, :],
                                     mixed_sems.at[at])

    def one_step(step, _):
        spread.receive_rows(step)

        @pl.when(step < 16)
        def _():
            across, other, half_at = spread.block(step)
            value = dot_nn(got[across, (core + other) % 2, half_at, 0], w_out[...])
            part[pl.ds(pl.multiple_of(place(step) * piece, piece), piece), :] = value.astype(part.dtype)
            mixed_copy(step).start()
            line.launch(2 * step, 2)

        @pl.when(step >= 2)
        def _():
            total.advance(step - 2)

        @pl.when(step >= 4)
        def _():
            line.step(2 * step - 8)
            line.step(2 * step - 7)
        return 0

    lax.fori_loop(0, 20, one_step, 0)
    line.end(32)

    def emit(at, first, second):
        for half_at, value in enumerate((first, second)):
            d_hidden[:, pl.ds(pl.multiple_of((half_at * counts + at) * width, width), width)] = value

    total.end(emit)
    for hop in range(3):
        spread.x_copy(hop, 0).wait_send()
        spread.y_copy(hop, 0).wait_send()
    for stage in range(4):
        for stream in range(2):
            spread.sib_copy(stage, stream, 0).wait_send()
    for at in range(16):
        mixed_copy(at).wait()
    tiny.wait()
    for at in range(rows // LANES):
        values = jnp.broadcast_to(from_tile(tiny_pair[at : at + 1, :], eye), (LANES, LANES))
        pair_rms[1, at * LANES : (at + 1) * LANES, :] = values


def attend(qkv, rms, cos, sin, mask, w_out, g_col, w_down, cid, width=512):
    rows = qkv.shape[0]
    wide, cols = w_out.shape
    heads = wide // HD
    counts = w_down.shape[0] // (2 * width)
    low, f32 = jnp.bfloat16, jnp.float32
    dma = pltpu.SemaphoreType.DMA
    vm = pl.BlockSpec(memory_space=pltpu.VMEM)
    out_shape = [
        jax.ShapeDtypeStruct((8 * rows, cols), low),
        jax.ShapeDtypeStruct((8 * rows, wide), low),
        jax.ShapeDtypeStruct((2, rows, 2 * HD), low),
        jax.ShapeDtypeStruct((heads, rows, 2 * rows), f32),
        jax.ShapeDtypeStruct((rows, wide), low),
        jax.ShapeDtypeStruct((2,) + rms.shape, f32),
        jax.ShapeDtypeStruct((rows, w_down.shape[0]), f32),
    ]
    scratch = spread_scratch(1, rows // 2, wide) + [
        pltpu.VMEM((8 * rows, cols), low), dma((4,)),
        pltpu.VMEM((8, LANES), f32), pltpu.VMEM((8, LANES), f32), dma((16,)),
    ] + reduce_scratch(counts, rows, width) + line_scratch(32, (8 * rows, cols), low)
    kernel = functools.partial(attend_kernel, rows, heads, cols, width, counts)
    operands = [qkv, rms, cos, sin, mask, w_out, g_col, w_down]
    out_specs = [vm, pl.BlockSpec(memory_space=pl.ANY)] + [vm] * 5
    return kernel_call(kernel, out_shape, operands, [vm] * 8, scratch, cid, "attend", out_specs, (4, 5, 6, 7))


def tail_kernel(rows, heads, per, d_attn, w_out, queries, kv, probs, rms, cos, sin, act_t, w_qkv, ffn, x_low,
                attn, gain, gain_grad, mixed_all, d_tok, out, grad_query, grad_out, kv_sum, gain_tiles, *refs, late):
    here = Place()
    width = HD
    counts = heads // 2
    part = rows // 2
    refs = list(refs)
    line_counts = 8 * per
    cols = d_attn.shape[1]
    extra = cols // (rows // per)

    def take(count):
        taken_refs = refs[:count]
        del refs[:count]
        return taken_refs

    total_refs = take(11)
    spread = Spread(here, 1, take(7))
    d_mixed, tiny_own, tiny_all, d_kv, give, taken, give_sems, tiny_send, tiny_recv = take(9)
    grad, grad_mixed, gain_sum, tile, tile_send, tile_recv, put_sems, local_sems, mixed_two, mixed_sems = take(10)

    def far(at):
        return at // (2 * per), at // per % 2

    def near(at):
        return spread.block(jnp.minimum(at, line_counts - 1))

    def place_ffn(at):
        return here.shard(*far(at)) * per + at % per

    def place_tok(at):
        across, other, half_at = near(at)
        return here.shard(across, other) * per + half_at

    def place_half(at):
        return jnp.where(at < 2 * line_counts, 2 * place_tok(at // 2) + at % 2, at)

    ffn_sum, leaving = take(2)
    line = Line(here, 2 * line_counts, [ffn, ffn_sum] + take(8), chip_place(here, 2 * per))
    contrib, summed = take(2)
    line_tok = Line(here, 2 * (line_counts + extra), [contrib, summed] + take(8), place_half)
    tiny = Tiny(here, tiny_own, tiny_all, (tiny_send, tiny_recv), False)
    got, core = spread.got, here.core
    product = products(here, d_attn, w_out, True, rows, width, counts)
    total = Reduce(here, counts, product, total_refs)
    greet(here, tiny.peers, True)
    line.begin()
    grad_mixed[...] = jnp.zeros_like(grad_mixed)

    def mixed_copy(step):
        span = pl.ds(pl.multiple_of(step * rows, rows), rows)
        return pltpu.make_async_copy(mixed_all.at[span, :], mixed_two.at[step % 2], mixed_sems.at[step % 2])

    mixed_copy(0).start()

    def both_steps(which, at):
        which.step(2 * at)
        which.step(2 * at + 1)

    def beside(step):
        both_steps(line, step)

        @pl.when(step < 8)
        def _():
            span = pl.ds(pl.multiple_of(step * rows, rows), rows)
            mixed_copy(step).wait()

            @pl.when(step < 7)
            def _():
                mixed_copy(step + 1).start()

            grad_mixed[...] += dot_tn(mixed_two[step % 2], d_attn[span, :])

    done = total.run(beside)
    grad_out[...] = grad_mixed[...].astype(grad_out.dtype)

    def land(at, first, second):
        for half_at, value in enumerate((first, second)):
            d_mixed[:, pl.ds(pl.multiple_of((half_at * counts + at) * width, width), width)] = value.astype(
                d_mixed.dtype)

    total.end(land)
    half = HD // 2
    scale = 1.0 / math.sqrt(HD)
    depth = w_qkv.shape[0] * 8
    d_kv[...] = jnp.zeros_like(d_kv)
    for copy in late:
        copy.wait()

    def one_head(head, dots):
        span = pl.ds(pl.multiple_of(head * HD, HD), HD)
        query = queries[:, span]
        cot = d_mixed[:, span]
        prob = probs[head]
        d_prob = jnp.concatenate([dot_nt(cot, kv[0, :, HD:]), dot_nt(cot, kv[1, :, HD:])], axis=1)
        delta = jnp.sum(prob * d_prob, axis=-1, keepdims=True)
        d_score = (prob * (d_prob - delta)).astype(jnp.bfloat16)
        prob_low = prob.astype(jnp.bfloat16)
        d_query = (dot_nn(d_score[:, :rows], kv[0, :, :HD]) + dot_nn(d_score[:, rows:], kv[1, :, :HD])) * scale
        for side in range(2):
            keys = slice(side * rows, (side + 1) * rows)
            d_kv[side, :, :HD] += dot_tn(d_score[:, keys], query)
            d_kv[side, :, HD:] += dot_tn(prob_low[:, keys], cot)
        dots = dots + jnp.sum(d_query * query.astype(jnp.float32), axis=-1, keepdims=True)
        lead, trail = d_query[:, :half], d_query[:, half:]
        first = ((lead * cos[0] + trail * sin[0]) * rms[0]).astype(got.dtype)
        second = ((trail * cos[0] - lead * sin[0]) * rms[0]).astype(got.dtype)
        both_steps(line, done + head)
        for rows_at in range(2):
            piece = slice(rows_at * part, (rows_at + 1) * part)
            got[0, core, rows_at, 0, :, pl.ds(pl.multiple_of(head * HD, HD), half)] = first[piece, :]
            got[0, core, rows_at, 0, :, pl.ds(pl.multiple_of(head * HD + half, half), half)] = second[piece, :]

        return dots

    dots = lax.fori_loop(0, heads, one_head, jnp.zeros((rows, 1), jnp.float32))
    eye = diagonal()
    tiny_own[...] = jnp.zeros_like(tiny_own)
    for side in (1, 0):
        d_key, d_value = d_kv[side, :, :HD], d_kv[side, :, HD:]
        own = jnp.sum(d_key * kv[side, :, :HD].astype(jnp.float32) +
                      d_value * kv[side, :, HD:].astype(jnp.float32), axis=-1, keepdims=True)
        if side == 0:
            own = own + dots * (1.0 / scale)
        own = own * (rms[side] * rms[side] * (1.0 / depth))
        to_tile(tiny_own, side * (rows // LANES), own, eye)
        lead, trail = d_key[:, :half], d_key[:, half:]
        parts = [(lead * cos[side] + trail * sin[side]) * rms[side],
                 (trail * cos[side] - lead * sin[side]) * rms[side],
                 d_value[:, :half] * rms[side], d_value[:, half:] * rms[side]]
        for at, value in enumerate(parts):
            if side == 1:
                give[:, at * half : (at + 1) * half] = value.astype(give.dtype)
            else:
                d_kv[0, :, at * half : (at + 1) * half] = value
    given = remote(give, taken, give_sems.at[0], give_sems.at[1], spread.ydev)
    given.start()
    grad[...] = jnp.zeros_like(grad)
    given.wait()
    for rows_at in range(2):
        piece = slice(rows_at * part, (rows_at + 1) * part)
        value = d_kv[0, piece, :] + taken[piece, :].astype(jnp.float32)
        got[0, core, rows_at, 0, :, heads * HD :] = value.astype(got.dtype)
    tiny.begin()
    spread.begin_rows()
    gain_sum[...] = jnp.zeros_like(gain_sum)
    tiny.end()

    def block_of(at):
        across, other, half_at = near(at)
        shard, partner = here.shard(across, other), here.shard((across + 2) % 4, other)
        block = got[across, (core + other) % 2, half_at, 0]
        first = pl.multiple_of(shard * rows + half_at * part, part)
        for tile_at in range(part // LANES):
            row = pl.ds(pl.multiple_of(first + tile_at * LANES, LANES), LANES)
            low_at = half_at * (part // LANES) + tile_at
            kept = rows // LANES + low_at
            dot = from_tile(tiny_all[shard, pl.ds(low_at, 1), :] + tiny_all[partner, pl.ds(kept, 1), :], eye)
            value = dot_nt(block[tile_at * LANES : (tile_at + 1) * LANES, :], w_qkv[...])
            x_rows = x_low[row, :].astype(jnp.float32)
            contrib[row, :] = (value * gain[0:1, :] - x_rows * dot).astype(contrib.dtype)
            gain_sum[...] += jnp.sum(value * x_rows, axis=0, keepdims=True)
        line_tok.launch(2 * at, 2)
        rows_t = act_t[:, pl.ds(first, part)]
        for at_col in range((heads + 2) * HD // 512):
            span = slice(at_col * 512, (at_col + 1) * 512)
            grad[:, span] += dot_nn(rows_t, block[:, span])

    me = here.shard(0, 0)
    columns = pl.ds(pl.multiple_of(me * cols, cols), cols)
    chunk = rows // per

    def landing(which, at):
        sub = at % per if which == 0 else near(at)[2]
        return (out, d_tok)[which].at[pl.ds(pl.multiple_of(sub * chunk, chunk), chunk), columns]

    def leaver(which, at):
        return (leaving, line_tok.from_end)[which].at[at]

    def put(which, at):
        goal = here.device(*(far(at) if which == 0 else near(at)[:2]))
        return remote(leaver(which, at), landing(which, at), put_sems.at[which, 0, at], put_sems.at[which, 1, at],
                      goal)

    def keep(which, at):
        spot = at % per if which == 0 else near(at)[2]
        return pltpu.make_async_copy(leaver(which, at), landing(which, at), local_sems.at[which, spot])

    def emit(which, at):
        if which == 1:
            row = pl.ds(pl.multiple_of(place_tok(at) * chunk, chunk), chunk)
            value = d_attn[row, :].astype(jnp.float32) + summed[row, :].astype(jnp.float32)
            line_tok.from_end[at] = value.astype(out.dtype)
            return
        row = pl.ds(pl.multiple_of(place_ffn(at) * chunk, chunk), chunk)

        def leave(source):
            value = x_low[row, :].astype(jnp.float32) + attn[row, :].astype(jnp.float32)
            leaving[at] = (value + source[row, :].astype(jnp.float32)).astype(out.dtype)

        leave(ffn_sum)

    def is_own(which, at):
        return at < per if which == 0 else jnp.logical_and(at < 4, at % 2 == 0)

    def send(which, at):
        own = is_own(which, at)

        @pl.when(own)
        def _():
            keep(which, at).start()

        @pl.when(jnp.logical_not(own))
        def _():
            put(which, at).start()

    def stage_step(step, _):
        spread.receive_rows(step)

        @pl.when(step < line_counts)
        def _():
            block_of(step)

        @pl.when(step < 5)
        def _():
            both_steps(line, done + heads + step)

        @pl.when(step >= 4)
        def _():
            both_steps(line_tok, step - 4)

        @pl.when(step > 0)
        def _():
            send(0, step - 1)

        @pl.when(line.inner == 0)
        def _():
            for last in range(2):
                line.up(2 * step + last).wait_send()
                line.down(2 * step + last).wait_recv()

        emit(0, step)

        @pl.when(jnp.logical_and(line.inner == 1, step > 7))
        def _():
            send(1, step - 8)

        @pl.when(jnp.logical_and(line.inner == 1, step > 6))
        def _():
            emit(1, step - 7)
        return 0

    lax.fori_loop(0, line_counts, stage_step, 0)
    for half_at in range(cols // (rows // per)):
        span = pl.ds(line_counts * (rows // per) + half_at * (rows // per), rows // per)
        source = slice(half_at * (rows // per), (half_at + 1) * (rows // per))
        contrib[span, :] = grad[source, heads * HD :].astype(contrib.dtype)
    line_tok.launch(2 * line_counts, 2 * extra)
    grad_query[...] = grad[:, : heads * HD].astype(grad_query.dtype)
    for at in range(cols // LANES):
        tile[at : at + 1, :] = gain_sum[:, at * LANES : (at + 1) * LANES]
        spot = cols // LANES + at
        tile[spot : spot + 1, :] = gain_grad[:, at * LANES : (at + 1) * LANES]

    def tile_copy(step):
        return remote(tile, gain_tiles.at[here.z], tile_send.at[step], tile_recv.at[step],
                      (here.dp, here.seq, (here.z + step + 1) % 4))

    send(0, line_counts - 1)
    line.drain()
    for step in range(3):
        tile_copy(step).start()
    gain_tiles[here.z] = tile[...]

    @pl.when(line.inner == 1)
    def _():
        start = line_counts - 4

        def both(at, _):
            both_steps(line_tok, at)

            @pl.when(at < line_counts + 4)
            def _():
                send(1, at - 4)

            @pl.when(at < line_counts + 3)
            def _():
                emit(1, at - 3)
            return 0

        lax.fori_loop(start, line_counts + extra + 2, both, 0)

        def drain(at, _):
            line_tok.down(at).wait_send()
            return 0

        lax.fori_loop(0, 2 * (line_counts + extra), drain, 0)

    @pl.when(line.inner == 0)
    def _():
        def arrive(at, _):
            for last in range(2):
                line_tok.up(2 * at + last).wait_send()
                line_tok.down(2 * at + last).wait_recv()

            @pl.when(jnp.logical_and(at > 0, at <= line_counts))
            def _():
                send(1, at - 1)

            @pl.when(at < line_counts)
            def _():
                emit(1, at)
            return 0

        lax.fori_loop(0, line_counts + extra, arrive, 0)

    for half_at in range(extra):
        span = pl.ds((line_counts + half_at) * chunk, chunk)
        kv_sum[half_at * chunk : (half_at + 1) * chunk, :] = summed[span, :]
    for hop in range(3):
        spread.x_copy(hop, 0).wait_send()
        spread.y_copy(hop, 0).wait_send()
    for stage in range(4):
        spread.sib_copy(stage, 0, 0).wait_send()
        spread.sib_copy(stage, 1, 0).wait_send()

    def finish(at, _):
        for which in range(2):
            own = is_own(which, at)

            @pl.when(own)
            def _():
                keep(which, at).wait()

            @pl.when(jnp.logical_not(own))
            def _():
                put(which, at).wait()
        return 0

    lax.fori_loop(0, line_counts, finish, 0)
    for step in range(3):
        tile_copy(step).wait()


def tail(d_attn, w_out, queries, kv, probs, rms, cos, sin, act_t, w_qkv, ffn, x_low, attn, gain, gain_grad,
         mixed_all, cid,
 per=2):
    total, cols = d_attn.shape
    rows = total // 8
    wide = w_out.shape[0]
    heads = wide // HD
    low, f32 = jnp.bfloat16, jnp.float32
    dma = pltpu.SemaphoreType.DMA
    vm = pl.BlockSpec(memory_space=pltpu.VMEM)
    counts = 8 * per
    chunk = rows // per
    extra = cols // chunk
    long = (total + cols, cols)
    out_shape = [
        jax.ShapeDtypeStruct((rows, 8 * cols), low),
        jax.ShapeDtypeStruct((rows, 8 * cols), low),
        jax.ShapeDtypeStruct((cols, wide), low),
        jax.ShapeDtypeStruct(w_out.shape, low),
        jax.ShapeDtypeStruct((cols, 2 * HD), low),
        jax.ShapeDtypeStruct((4, 8, LANES), f32),
    ]
    scratch = reduce_scratch(heads // 2, rows, HD, 2) + spread_scratch(1, rows // 2, wide + 2 * HD)
    scratch += [
        pltpu.VMEM((rows, wide), low),
        pltpu.VMEM((8, LANES), f32),
        pltpu.VMEM((8, 8, LANES), f32),
        pltpu.VMEM((2, rows, 2 * HD), f32),
        pltpu.VMEM((rows, 2 * HD), low),
        pltpu.VMEM((rows, 2 * HD), low),
        dma((2,)), dma((7,)), dma((7,)),
        pltpu.VMEM(w_qkv.shape, f32),
        pltpu.VMEM(w_out.shape, f32),
        pltpu.VMEM((1, cols), f32),
        pltpu.VMEM((8, LANES), f32),
        dma((3,)), dma((3,)), dma((2, 2, counts)), dma((2, per)),
        pltpu.VMEM((2, rows, wide), low), dma((2,)),
        pltpu.VMEM((total, cols), low),
        pltpu.VMEM((counts, chunk, cols), low),
    ] + line_scratch(2 * counts, (total, cols), low)
    scratch += [pltpu.VMEM(long, low), pltpu.VMEM(long, low)] + line_scratch(2 * (counts + extra), long, low, 2)
    operands = [d_attn, w_out, queries, kv, probs, rms, cos, sin, act_t, w_qkv, ffn, x_low, attn, gain,
                gain_grad, mixed_all]
    kernel = functools.partial(tail_kernel, rows, heads, per)
    specs = [vm] * (len(operands) - 1) + [pl.BlockSpec(memory_space=pl.ANY)]
    return kernel_call(kernel, out_shape, operands, specs, scratch, cid, "tail",
                       late=(2, 3, 4, 8, 9, 11, 12))


LANES = 128


def acts_move(
    tokens, seg_ids, gain_attn, w_query, kv_weight, w_out, gain_ffn, w_gate, w_up, w_down, d_out
):
    small = jnp.stack([gain_attn, gain_ffn, seg_ids.astype(gain_ffn.dtype), gain_attn]).astype(jnp.float32)

    qkv, x_low, act_one_t, w_qkv, rms, cos, sin, mask, g_parts = opening(
        tokens, small, w_query, kv_weight, d_out, 1
    )
    g_low = g_parts.reshape(x_low.shape)
    attn, mixed_all, kv, probs, queries, pair_rms, d_hidden = attend(
        qkv, rms, cos, sin, mask, w_out, g_low, w_down, 2
    )
    hidden, d_gate, d_up, act_two_t, dots = ffn_scatter(x_low, attn, small, w_gate, w_up, d_hidden, 4)
    d_norm, grad_gain_two, grad_gate, grad_up = back_gather(
        act_two_t, w_gate, w_up, d_gate, d_up, dots, x_low, attn, small, 5
    )
    ffn, d_attn, grad_down = down_gather(g_low, w_down, hidden, d_norm, 6)
    d_tokens, out, grad_query, grad_out, grad_kv, gain_tiles = tail(
        d_attn,
        w_out,
        queries,
        kv,
        probs,
        pair_rms,
        cos,
        sin,
        act_one_t,
        w_qkv,
        ffn,
        x_low,
        attn,
        small,
        grad_gain_two,
        mixed_all,
        7,
    )
    gains = jnp.sum(gain_tiles, axis=0).reshape(2, -1)
    wider = jnp.float32
    return (
        out,
        d_tokens.astype(wider),
        gains[0],
        grad_query.astype(wider),
        grad_kv.astype(wider),
        grad_out.astype(wider),
        gains[1],
        grad_gate.astype(wider),
        grad_up.astype(wider),
        grad_down.astype(wider),
    )


def solution(mesh):
    in_specs = (
        P(("dp", "seq"), None),
        P("dp"),
        P(("dp", "seq")),
        P(("dp", "seq"), "tensor"),
        P(("dp", "seq"), None),
        P("tensor", ("dp", "seq")),
        P(("dp", "seq")),
        P(("dp", "seq"), "tensor"),
        P(("dp", "seq"), "tensor"),
        P("tensor", ("dp", "seq")),
        P(("dp", "seq"), None),
    )
    out_specs = (
        P(("dp", "seq"), None),
        P(("dp", "seq"), None),
        P(("dp", "seq")),
        P(("dp", "seq"), "tensor"),
        P(("dp", "seq"), None),
        P("tensor", ("dp", "seq")),
        P(("dp", "seq")),
        P(("dp", "seq"), "tensor"),
        P(("dp", "seq"), "tensor"),
        P("tensor", ("dp", "seq")),
    )

    def shards(*arrays):
        tokens = arrays[0]
        sizes = tuple(mesh.shape[name] for name in ("dp", "seq", "tensor"))
        count = tokens.shape[0] * sizes[0] * sizes[1]
        plan = acts_move if sizes == (4, 2, 4) and count <= tokens.shape[1] else weights_move
        return plan(*arrays)

    return jax.shard_map(shards, mesh=mesh, in_specs=in_specs, out_specs=out_specs, check_vma=False)
```

```python
import functools
import math

import jax
import jax.numpy as jnp
from jax import lax
from jax.experimental import pallas as pl
from jax.experimental.pallas import tpu as pltpu
from jax.sharding import PartitionSpec as P

HD = 256


EPS = 1e-06
NEG = -1e30


def place_tables(segs):
    length = segs.shape[0]
    index = jnp.arange(length, dtype=jnp.int32)
    flags = jnp.concatenate([jnp.ones((1,), dtype=bool), segs[1:] != segs[:-1]])
    starts = lax.cummax(jnp.where(flags, index, jnp.zeros_like(index)), axis=0)
    places = index - starts
    half_size = HD // 2
    freqs = jnp.exp(jnp.arange(half_size, dtype=jnp.float32) * (-math.log(10000.0) / half_size))
    angles = places.astype(jnp.float32)[:, None] * freqs[None, :]
    return (places, jnp.cos(angles), jnp.sin(angles))


def rotate(vector, cos_table, sin_table):
    half_size = vector.shape[-1] // 2
    leading = vector[..., :half_size]
    trailing = vector[..., half_size:]
    return jnp.concatenate(
        [leading * cos_table - trailing * sin_table, trailing * cos_table + leading * sin_table],
        axis=-1,
    )


def rotate_back(vector, cos_table, sin_table):
    half_size = vector.shape[-1] // 2
    leading = vector[..., :half_size]
    trailing = vector[..., half_size:]
    return jnp.concatenate(
        [leading * cos_table + trailing * sin_table, trailing * cos_table - leading * sin_table],
        axis=-1,
    )


def matmul(left, right):
    return jnp.dot(left, right, preferred_element_type=jnp.float32)


def matmul_nt(left, right):
    return lax.dot_general(
        left, right, (((1,), (1,)), ((), ())), preferred_element_type=jnp.float32
    )


def matmul_tn(left, right):
    return lax.dot_general(
        left, right, (((0,), (0,)), ((), ())), preferred_element_type=jnp.float32
    )


def gelu_tanh(values):
    return jax.nn.gelu(values, approximate=True)


def norm_back(d_act, normed, rms_val, gain_val):
    scaled = d_act * gain_val
    return rms_val * (scaled - normed * jnp.mean(scaled * normed, axis=-1, keepdims=True))


def weights_move(
    tokens, seg_ids, gain_attn, w_query, kv_weight, w_out, gain_ffn, w_gate, w_up, w_down, d_out
):
    rows = tokens.shape[0]
    scale_factor = 1.0 / math.sqrt(HD)
    offset = lax.axis_index("seq") * rows
    places, cos_table, sin_table = place_tables(seg_ids)
    own_places = lax.dynamic_slice_in_dim(places, offset, rows, 0)
    own_segs = lax.dynamic_slice_in_dim(seg_ids, offset, rows, 0)
    own_cos = lax.dynamic_slice_in_dim(cos_table, offset, rows, 0)
    own_sin = lax.dynamic_slice_in_dim(sin_table, offset, rows, 0)
    allowed = (own_segs[:, None] == seg_ids[None, :]) & (own_places[:, None] >= places[None, :])
    full_query, full_out, full_kv, full_gain_one = (
        lax.all_gather(w_query, ("dp", "seq"), axis=0, tiled=True),
        lax.all_gather(w_out, ("dp", "seq"), axis=1, tiled=True),
        lax.all_gather(kv_weight, ("dp", "seq"), axis=0, tiled=True),
        lax.all_gather(gain_attn, ("dp", "seq"), axis=0, tiled=True),
    )
    gain_one = full_gain_one.astype(jnp.float32)
    inputs = tokens.astype(jnp.float32)
    rms_one = lax.rsqrt(jnp.mean(inputs * inputs, axis=-1, keepdims=True) + EPS)
    norm_one = inputs * rms_one
    act_one = (norm_one * gain_one).astype(jnp.bfloat16)
    query_pre = matmul(act_one, full_query)
    heads = query_pre.shape[1] // HD
    kv_pre = matmul(act_one, full_kv)
    queries = (
        rotate(query_pre.reshape(rows, heads, HD), own_cos[:, None, :], own_sin[:, None, :])
        * scale_factor
    ).astype(jnp.bfloat16)
    own_kv = jnp.concatenate(
        [rotate(kv_pre[:, :HD], own_cos, own_sin), kv_pre[:, HD:]], axis=1
    ).astype(jnp.bfloat16)
    all_kv = lax.all_gather(own_kv, "seq", axis=0, tiled=True)
    keys = all_kv[:, :HD]
    values_all = all_kv[:, HD:]
    scores = jnp.einsum("rhd,kd->hrk", queries, keys, preferred_element_type=jnp.float32)
    scores = jnp.where(allowed[None], scores, NEG)
    top_score = jnp.max(scores, axis=-1, keepdims=True)
    expd = jnp.exp(scores - top_score)
    total = jnp.sum(expd, axis=-1, keepdims=True)
    log_total = top_score + jnp.log(total)
    probs_low = (expd / total).astype(jnp.bfloat16)
    mixed = (
        jnp.einsum("hrk,kd->rhd", probs_low, values_all, preferred_element_type=jnp.float32)
        .reshape(rows, heads * HD)
        .astype(jnp.bfloat16)
    )
    attn = lax.psum(matmul(mixed, full_out), "tensor")
    resid = inputs + attn
    full_gate, full_up, full_down, full_gain_two = (
        lax.all_gather(w_gate, ("dp", "seq"), axis=0, tiled=True),
        lax.all_gather(w_up, ("dp", "seq"), axis=0, tiled=True),
        lax.all_gather(w_down, ("dp", "seq"), axis=1, tiled=True),
        lax.all_gather(gain_ffn, ("dp", "seq"), axis=0, tiled=True),
    )
    gain_two = full_gain_two.astype(jnp.float32)
    rms_two = lax.rsqrt(jnp.mean(resid * resid, axis=-1, keepdims=True) + EPS)
    norm_two = resid * rms_two
    act_two = (norm_two * gain_two).astype(jnp.bfloat16)
    gate = matmul(act_two, full_gate)
    up_val = matmul(act_two, full_up)
    gelu_val, gelu_pull = jax.vjp(gelu_tanh, gate)
    hidden = (gelu_val * up_val).astype(jnp.bfloat16)
    ffn = lax.psum(matmul(hidden, full_down).astype(jnp.bfloat16), "tensor").astype(jnp.float32)
    out = (resid + ffn).astype(jnp.bfloat16)
    back_gate, back_up, back_down = (
        lax.all_gather(w_gate, ("dp", "seq"), axis=0, tiled=True),
        lax.all_gather(w_up, ("dp", "seq"), axis=0, tiled=True),
        lax.all_gather(w_down, ("dp", "seq"), axis=1, tiled=True),
    )
    d_hidden = matmul_nt(d_out, back_down)
    grad_down = matmul_tn(hidden, d_out)
    d_gate = gelu_pull(d_hidden * up_val)[0].astype(jnp.bfloat16)
    d_up = (d_hidden * gelu_val).astype(jnp.bfloat16)
    grad_gate = matmul_tn(act_two, d_gate)
    grad_up = matmul_tn(act_two, d_up)
    d_act_two = lax.psum(matmul_nt(d_gate, back_gate) + matmul_nt(d_up, back_up), "tensor")
    grad_gain_two = jnp.sum(d_act_two * norm_two, axis=0)
    d_resid = d_out.astype(jnp.float32) + norm_back(d_act_two, norm_two, rms_two, gain_two)
    ffn_grads = (
        lax.psum_scatter(
            grad_gate.astype(jnp.bfloat16), ("dp", "seq"), scatter_dimension=0, tiled=True
        ).astype(jnp.float32),
        lax.psum_scatter(
            grad_up.astype(jnp.bfloat16), ("dp", "seq"), scatter_dimension=0, tiled=True
        ).astype(jnp.float32),
        lax.psum_scatter(
            grad_down.astype(jnp.bfloat16), ("dp", "seq"), scatter_dimension=1, tiled=True
        ).astype(jnp.float32),
        lax.psum_scatter(
            grad_gain_two.astype(jnp.bfloat16), ("dp", "seq"), scatter_dimension=0, tiled=True
        ).astype(jnp.float32),
    )
    back_query, back_out, back_kv = (
        lax.all_gather(w_query, ("dp", "seq"), axis=0, tiled=True),
        lax.all_gather(w_out, ("dp", "seq"), axis=1, tiled=True),
        lax.all_gather(kv_weight, ("dp", "seq"), axis=0, tiled=True),
    )
    d_attn = d_resid.astype(jnp.bfloat16)
    grad_out = matmul_tn(mixed, d_attn)
    d_mixed = matmul_nt(d_attn, back_out).astype(jnp.bfloat16).reshape(rows, heads, HD)
    scores_again = jnp.einsum("rhd,kd->hrk", queries, keys, preferred_element_type=jnp.float32)
    probs = jnp.where(allowed[None], jnp.exp(scores_again - log_total), 0.0)
    d_probs = jnp.einsum("rhd,kd->hrk", d_mixed, values_all, preferred_element_type=jnp.float32)
    delta = jnp.sum(probs * d_probs, axis=-1, keepdims=True)
    d_scores = (probs * (d_probs - delta)).astype(jnp.bfloat16)
    d_queries = (
        jnp.einsum("hrk,kd->rhd", d_scores, keys, preferred_element_type=jnp.float32) * scale_factor
    )
    d_query_pre = (
        rotate_back(d_queries, own_cos[:, None, :], own_sin[:, None, :])
        .reshape(rows, heads * HD)
        .astype(jnp.bfloat16)
    )
    d_keys_part = jnp.einsum("hrk,rhd->kd", d_scores, queries, preferred_element_type=jnp.float32)
    d_values_part = jnp.einsum(
        "hrk,rhd->kd", probs.astype(jnp.bfloat16), d_mixed, preferred_element_type=jnp.float32
    )
    own_kv_grad = lax.psum_scatter(
        jnp.concatenate([d_keys_part, d_values_part], axis=1).astype(jnp.bfloat16),
        "seq",
        scatter_dimension=0,
        tiled=True,
    )
    d_act_query = matmul_nt(d_query_pre, back_query)
    d_act_sum, kv_grad = (
        lax.psum(d_act_query.astype(jnp.bfloat16), "tensor").astype(jnp.float32),
        lax.psum(own_kv_grad, "tensor").astype(jnp.float32),
    )
    d_kv_pre = jnp.concatenate(
        [rotate_back(kv_grad[:, :HD], own_cos, own_sin), kv_grad[:, HD:]], axis=1
    ).astype(jnp.bfloat16)
    d_act_one = d_act_sum + matmul_nt(d_kv_pre, back_kv)
    grad_query = matmul_tn(act_one, d_query_pre)
    grad_kv = matmul_tn(act_one, d_kv_pre)
    grad_gain_one = jnp.sum(d_act_one * norm_one, axis=0)
    d_tokens = d_resid + norm_back(d_act_one, norm_one, rms_one, gain_one)
    attn_grads = (
        lax.psum_scatter(
            grad_query.astype(jnp.bfloat16), ("dp", "seq"), scatter_dimension=0, tiled=True
        ).astype(jnp.float32),
        lax.psum_scatter(
            grad_out.astype(jnp.bfloat16), ("dp", "seq"), scatter_dimension=1, tiled=True
        ).astype(jnp.float32),
        lax.psum_scatter(
            grad_kv.astype(jnp.bfloat16), ("dp", "seq"), scatter_dimension=0, tiled=True
        ).astype(jnp.float32),
        lax.psum_scatter(
            grad_gain_one.astype(jnp.bfloat16), ("dp", "seq"), scatter_dimension=0, tiled=True
        ).astype(jnp.float32),
    )
    return (
        out,
        d_tokens,
        attn_grads[3],
        attn_grads[0],
        attn_grads[2],
        attn_grads[1],
        ffn_grads[3],
        ffn_grads[0],
        ffn_grads[1],
        ffn_grads[2],
    )


MESH = pl.DeviceIdType.MESH
VMEM_LIMIT = 66000 * 1024


class Place:
    def __init__(self):
        self.dp = lax.axis_index("dp")
        self.seq = lax.axis_index("seq")
        self.z = lax.axis_index("tensor")
        self.core = lax.rem(self.dp, 2)
        self.chip = lax.div(self.dp, 2)

    def device(self, across, other):
        chip = (self.chip + across) % 2
        seq = (self.seq + across // 2) % 2
        core = (self.core + other) % 2
        return chip * 2 + core, seq, self.z

    def shard(self, across, other):
        dp, seq, _ = self.device(across, other)
        return dp * 2 + seq


def greet(here, peers, line=False):
    barrier = pltpu.get_barrier_semaphore()
    peers = list(peers)
    if line:
        peers += [(here.dp, here.seq, (here.z + step) % 4) for step in range(1, 4)]
    for peer in peers:
        pl.semaphore_signal(barrier, inc=1, device_id=peer, device_id_type=MESH)
    pl.semaphore_wait(barrier, len(peers))


def remote(src, dst, send, recv, peer):
    return pltpu.make_async_remote_copy(
        src_ref=src, dst_ref=dst, send_sem=send, recv_sem=recv, device_id=peer, device_id_type=MESH
    )


class Line:
    def __init__(self, here, counts, refs, place=None):
        self.own, self.out, self.from_end, self.from_mid = refs[:4]
        self.sems = refs[4:10]
        self.counts = counts
        self.chunk = self.from_mid.shape[1]
        self.fold = self.from_end.shape[1] // self.chunk
        self.place = place
        z = here.z
        self.inner = ((z + 1) // 2) % 2
        self.mate = (here.dp, here.seq, z + 1 - 2 * (z % 2))
        self.other = (here.dp, here.seq, 3 - z)

    def rows(self, at):
        at = at if self.place is None else self.place(at)
        return pl.ds(pl.multiple_of(at * self.chunk, self.chunk), self.chunk)

    def inbox(self, at):
        span = pl.ds(pl.multiple_of(at % self.fold * self.chunk, self.chunk), self.chunk)
        return self.from_end.at[at // self.fold, span, :]

    def up(self, at):
        return remote(self.own.at[self.rows(at), :], self.inbox(at), self.sems[0].at[at],
                      self.sems[1].at[at], self.mate)

    def over(self, at):
        return remote(self.out.at[self.rows(at), :], self.from_mid.at[at], self.sems[2].at[at],
                      self.sems[3].at[at], self.other)

    def down(self, at):
        rows = self.rows(at)
        return remote(self.out.at[rows, :], self.out.at[rows, :], self.sems[4].at[at],
                      self.sems[5].at[at], self.mate)

    def launch(self, first, count):
        @pl.when(self.inner == 0)
        def _():
            def send(at, _):
                self.up(first + at).start()
                return 0

            lax.fori_loop(0, count, send, 0)

    def begin(self):
        self.launch(0, self.counts)

    def first(self, at):
        rows = self.rows(at)
        self.up(at).wait_recv()
        total = self.own[rows, :].astype(jnp.float32) + self.inbox(at)[...].astype(jnp.float32)
        self.out[rows, :] = total.astype(self.out.dtype)
        self.over(at).start()

    def second(self, at):
        rows = self.rows(at)
        self.over(at).wait()
        total = self.out[rows, :].astype(jnp.float32) + self.from_mid[at].astype(jnp.float32)
        self.out[rows, :] = total.astype(self.out.dtype)
        self.down(at).start()

    def step(self, at, start=0, count=None):
        count = self.counts if count is None else count

        @pl.when(jnp.logical_and(self.inner == 1, at < count))
        def _():
            self.first(start + at)

        @pl.when(jnp.logical_and(self.inner == 1, jnp.logical_and(at > 1, at < count + 2)))
        def _():
            self.second(start + at - 2)

    def steps(self, first, last, start=0, count=None):
        def rest(at, _):
            self.step(at, start, count)
            return 0

        lax.fori_loop(first, last, rest, 0)

    def settle(self):
        @pl.when(self.inner == 0)
        def _():
            def take(at, _):
                self.up(at).wait_send()
                self.down(at).wait_recv()
                return 0

            lax.fori_loop(0, self.counts, take, 0)

        self.drain()

    def drain(self):
        @pl.when(self.inner == 1)
        def _():
            def drain(at, _):
                self.down(at).wait_send()
                return 0

            lax.fori_loop(0, self.counts, drain, 0)

    def end(self, done=0):
        self.steps(min(done, self.counts + 2), self.counts + 2)
        self.settle()


def line_scratch(counts, shape, low, fold=1):
    chunk = shape[0] // counts
    inbox = pltpu.VMEM((counts // fold, chunk * fold, shape[1]), low)
    return [inbox, pltpu.VMEM((counts, chunk, shape[1]), low)] + [pltpu.SemaphoreType.DMA((counts,))] * 6


def turned(at):
    return 3 - at // 2, 1 - at % 2


def slice_peers(here):
    return [here.device(*turned(at)) for at in range(7)]


def kernel_call(kernel, out_shape, operands, specs, scratch, cid, name, out_specs=None, late=()):
    vm = pl.BlockSpec(memory_space=pltpu.VMEM)
    specs = [pl.BlockSpec(memory_space=pl.ANY) if at in late else spec for at, spec in enumerate(specs)]
    inside = [pltpu.VMEM(operands[at].shape, operands[at].dtype) for at in late]
    if late:
        inside.append(pltpu.SemaphoreType.DMA((len(late),)))

    def body(*refs):
        if not late:
            kernel(*refs)
            return
        ins, rest, own = list(refs[: len(operands)]), refs[len(operands) : -len(inside)], refs[-len(inside) :]
        copies = []
        for spot, at in enumerate(late):
            copy = pltpu.make_async_copy(ins[at], own[spot], own[-1].at[spot])
            copy.start()
            copies.append(copy)
            ins[at] = own[spot]
        kernel(*ins, *rest, late=copies)

    return pl.pallas_call(
        body,
        out_shape=out_shape,
        in_specs=specs,
        out_specs=out_specs or [vm] * len(out_shape),
        scratch_shapes=scratch + inside,
        compiler_params=pltpu.CompilerParams(
            collective_id=cid, has_side_effects=True, vmem_limit_bytes=VMEM_LIMIT
        ),
        name=f"{name}_{cid}",
    )(*operands)


class Tiny:
    def __init__(self, here, src, dst, sems, spread):
        self.here, self.src, self.dst, self.sems, self.spread = here, src, dst, sems, spread
        self.peers = slice_peers(here)
        self.me = here.shard(0, 0)

    def tile(self, shard):
        return self.src.at[shard] if self.spread else self.src

    def copy(self, at):
        return remote(self.tile(self.here.shard(*turned(at))), self.dst.at[self.me], self.sems[0].at[at],
                      self.sems[1].at[at], self.peers[at])

    def begin(self):
        for at in range(7):
            self.copy(at).start()
        self.dst[self.me] = self.tile(self.me)[...]

    def end(self):
        for at in range(7):
            self.copy(at).wait()


class Reduce:
    def __init__(self, here, counts, product, refs, before=None):
        self.counts, self.product, self.before = counts, product, before
        self.held, self.sib_out, self.sib_in, self.from_x, self.from_y = refs[:5]
        self.sib_sems, self.x_sems, self.y_sems = refs[5:7], refs[7:9], refs[9:11]
        self.sib, self.xdev, self.ydev = here.device(0, 1), here.device(1, 0), here.device(2, 0)
        self.steps = 4 * counts
        self.ring = self.sib_out.shape[0]

    def streams(self, stage):
        far = stage // 3
        x_chip = jnp.where(stage == 0, 3, jnp.where(stage == 2, 0, 1))
        y_chip = jnp.where(stage == 0, 3, jnp.where(stage == 2, 0, 2))
        return (x_chip, far), (y_chip, 1 - far)

    def to_sib(self, step, stream):
        stage, at = step // self.counts, step % self.counts
        return remote(self.sib_out.at[step % self.ring, stream], self.sib_in.at[stage, stream, at],
                      self.sib_sems[0].at[stage, stream, at], self.sib_sems[1].at[stage, stream, at], self.sib)

    def to_x(self, hop, at, stage=0):
        return remote(self.held.at[stage, 0, at], self.from_x.at[hop, at], self.x_sems[0].at[hop, at],
                      self.x_sems[1].at[hop, at], self.xdev)

    def to_y(self, hop, at, stage=0):
        return remote(self.held.at[stage, 1, at], self.from_y.at[hop, at], self.y_sems[0].at[hop, at],
                      self.y_sems[1].at[hop, at], self.ydev)

    def compute(self, step):
        stage, at = step // self.counts, step % self.counts
        if self.before:
            for stop in range(3):
                @pl.when(step == stop * self.counts)
                def _():
                    self.before(stop)

        @pl.when(step >= self.ring)
        def _():
            for stream in range(2):
                self.to_sib(step - self.ring, stream).wait_send()

        for stream, (across, half) in enumerate(self.streams(stage)):
            self.sib_out[step % self.ring, stream] = self.product(across, 1, half, at).astype(jnp.bfloat16)
            self.held[stage, stream, at] = self.product(across, 0, half, at).astype(jnp.bfloat16)
        for stream in range(2):
            self.to_sib(step, stream).start()

    def finish(self, step):
        stage, at = step // self.counts, step % self.counts
        for stream in range(2):
            self.to_sib(step, stream).wait_recv()

        def total(stream):
            return self.held[stage, stream, at].astype(jnp.float32) + self.sib_in[stage, stream, at].astype(
                jnp.float32)

        @pl.when(stage < 3)
        def _():
            for stream in range(2):
                self.held[stage, stream, at] = total(stream).astype(jnp.bfloat16)

        @pl.when(stage == 3)
        def _():
            self.to_y(0, at).wait_recv()
            self.held[3, 0, at] = (total(0) + self.from_y[0, at].astype(jnp.float32)).astype(jnp.bfloat16)
            self.to_x(0, at).wait_recv()
            self.held[3, 1, at] = (total(1) + self.from_x[0, at].astype(jnp.float32)).astype(jnp.bfloat16)

        @pl.when(stage != 2)
        def _():
            hop = stage - stage // 3
            self.to_x(hop, at, stage).start()
            self.to_y(hop, at, stage).start()

    def advance(self, step):
        @pl.when(step < self.steps)
        def _():
            self.compute(step)

        @pl.when(jnp.logical_and(step > 0, step <= self.steps))
        def _():
            self.finish(step - 1)

    def run(self, hook=None):
        def body(step, _):
            self.advance(step)

            if hook:
                hook(step)
            return 0

        lax.fori_loop(0, self.steps + 1, body, 0)
        return self.steps + 1

    def end(self, emit):
        def last(at, _):
            values = []
            for half in range(2):
                xs, ys = (1, 2) if half == 0 else (2, 1)
                self.to_x(xs, at).wait_recv()
                self.to_y(ys, at).wait_recv()
                values.append(self.held[2, half, at].astype(jnp.float32) + self.from_x[xs, at].astype(jnp.float32)
                              + self.from_y[ys, at].astype(jnp.float32))
            emit(at, *values)
            for hop in range(3):
                self.to_x(hop, at).wait_send()
                self.to_y(hop, at).wait_send()
            return 0

        lax.fori_loop(0, self.counts, last, 0)

        def drain(at, _):
            for stream in range(2):
                self.to_sib(self.steps - self.ring + at, stream).wait_send()
            return 0

        lax.fori_loop(0, self.ring, drain, 0)


def reduce_scratch(counts, rows, width, ring=4):
    low, dma = jnp.bfloat16, pltpu.SemaphoreType.DMA
    block = pltpu.VMEM((4, 2, counts, rows, width), low)
    landed = pltpu.VMEM((3, counts, rows, width), low)
    sent = pltpu.VMEM((ring, 2, rows, width), low)
    return [block, sent, block, landed, landed] + [dma((4, 2, counts))] * 2 + [dma((3, counts))] * 4


class Spread:
    def __init__(self, here, counts, refs):
        self.counts = counts
        self.got = refs[0]
        self.x_sems, self.y_sems, self.sib_sems = refs[1:3], refs[3:5], refs[5:7]
        self.core = here.core
        self.sib, self.xdev, self.ydev = here.device(0, 1), here.device(1, 0), here.device(2, 0)

    def slot(self, across, half, at):
        return self.got.at[across, self.core, half, at]

    def x_copy(self, hop, at):
        half = jnp.minimum(hop, 1)
        src = self.slot(2 * (hop // 2), half, at)
        dst = self.slot(1 + 2 * (hop // 2), half, at)
        return remote(src, dst, self.x_sems[0].at[hop, at], self.x_sems[1].at[hop, at], self.xdev)

    def y_copy(self, hop, at):
        half = 1 - jnp.minimum(hop, 1)
        src = self.slot(hop // 2, half, at)
        dst = self.slot(2 + hop // 2, half, at)
        return remote(src, dst, self.y_sems[0].at[hop, at], self.y_sems[1].at[hop, at], self.ydev)

    def streams(self, stage):
        some, last, late = jnp.minimum(stage, 1), stage // 3, stage // 2
        return (some + 2 * last, late), (2 * some + last, 1 - late)

    def block(self, at):
        x_stream, y_stream = self.streams(at // 4)
        second = at // 2 % 2
        across = x_stream[0] + second * (y_stream[0] - x_stream[0])
        half = x_stream[1] + second * (y_stream[1] - x_stream[1])
        return across, at % 2, half

    def begin_rows(self):
        for hop in range(2):
            self.x_copy(hop, 0).start()
            self.y_copy(hop, 0).start()
        for stream in range(2):
            self.sib_copy(0, stream, 0).start()

    def receive_rows(self, step):
        stage = step // 4

        @pl.when(jnp.logical_and(step % 4 == 0, jnp.logical_and(stage > 0, stage < 4)))
        def _():
            self.x_copy(stage - 1, 0).wait_recv()
            self.sib_copy(stage, 0, 0).start()
            self.y_copy(stage - 1, 0).wait_recv()
            self.sib_copy(stage, 1, 0).start()

        @pl.when(step == 4)
        def _():
            self.x_copy(2, 0).start()
            self.y_copy(2, 0).start()

        for stream in range(2):
            @pl.when(jnp.logical_and(step % 4 == 2 * stream, step < 16))
            def _(stream=stream):
                self.sib_copy(stage, stream, 0).wait_recv()

    def sib_copy(self, stage, stream, at):
        across, half = self.streams(stage)[stream]
        slot = self.slot(across, half, at)
        spot = (stage, stream, at)
        return remote(slot, slot, self.sib_sems[0].at[spot], self.sib_sems[1].at[spot], self.sib)

    def begin(self):
        def first(at, _):
            self.x_copy(0, at).start()
            self.y_copy(0, at).start()
            return 0

        def own(at, _):
            self.sib_copy(0, 0, at).start()
            self.sib_copy(0, 1, at).start()
            return 0

        lax.fori_loop(0, self.counts, first, 0)
        lax.fori_loop(0, self.counts, own, 0)

    def run(self, blocks, hook=None, done=None):
        counts = self.counts

        def body(step, _):
            stage, at = step // counts, step % counts

            @pl.when(jnp.logical_and(stage > 0, stage < 4))
            def _():
                self.x_copy(stage - 1, at).wait_recv()
                self.sib_copy(stage, 0, at).start()
                self.y_copy(stage - 1, at).wait_recv()
                self.sib_copy(stage, 1, at).start()

            @pl.when(jnp.logical_and(stage > 0, stage < 3))
            def _():
                self.x_copy(stage, at).start()
                self.y_copy(stage, at).start()

            @pl.when(step > 0)
            def _():
                old, spot = (step - 1) // counts, (step - 1) % counts
                for stream, (across, half) in enumerate(self.streams(old)):
                    self.sib_copy(old, stream, spot).wait_recv()
                    blocks(across, half, spot)
                if done:
                    done(old, spot)

            if hook:
                hook(step)
            return 0

        lax.fori_loop(0, 4 * counts + 1, body, 0)
        return 4 * counts + 1

    def end(self):
        def drain(at, _):
            for hop in range(3):
                self.x_copy(hop, at).wait_send()
                self.y_copy(hop, at).wait_send()
            for stage in range(4):
                self.sib_copy(stage, 0, at).wait_send()
                self.sib_copy(stage, 1, at).wait_send()
            return 0

        lax.fori_loop(0, self.counts, drain, 0)


def spread_scratch(counts, rows, width):
    dma = pltpu.SemaphoreType.DMA
    return [pltpu.VMEM((4, 2, 2, counts, rows, width), jnp.bfloat16)] + [dma((3, counts))] * 4 + [
        dma((4, 2, counts))] * 2


def row_span(here, across, other, rows):
    return pl.ds(pl.multiple_of(here.shard(across, other) * rows, rows), rows)


def dot_nt(left, right):
    return lax.dot_general(left, right, (((1,), (1,)), ((), ())), preferred_element_type=jnp.float32)


def dot_tn(left, right):
    return lax.dot_general(left, right, (((0,), (0,)), ((), ())), preferred_element_type=jnp.float32)


def dot_nn(left, right):
    return jnp.dot(left, right, preferred_element_type=jnp.float32)


def products(here, act, weight, nt, rows, width, counts):
    def product(across, other, half, at):
        cols = pl.ds(pl.multiple_of((half * counts + at) * width, width), width)
        block = act[row_span(here, across, other, rows), :]
        return dot_nt(block, weight[cols, :]) if nt else dot_nn(block, weight[:, cols])

    return product


def diagonal():
    return (lax.broadcasted_iota(jnp.int32, (LANES, LANES), 0) ==
            lax.broadcasted_iota(jnp.int32, (LANES, LANES), 1)).astype(jnp.float32)


def to_tile(tile, first, column, eye):
    for at in range(column.shape[0] // LANES):
        spread = column[at * LANES : (at + 1) * LANES, :] * eye
        tile[first + at : first + at + 1, :] = jnp.sum(spread, axis=0, keepdims=True)


def from_tile(row, eye):
    return jnp.sum(eye * row, axis=1, keepdims=True)


def make_tables(here, rows, segs, cos, sin, mask):
    eye = diagonal()
    tiles = rows // LANES
    freqs = jnp.exp(lax.broadcasted_iota(jnp.int32, (1, LANES), 1).astype(jnp.float32) * (-math.log(10000.0) / LANES))
    lane = lax.broadcasted_iota(jnp.int32, (1, LANES), 1)
    line = lax.broadcasted_iota(jnp.int32, (LANES, 1), 0)

    def ids_of(row):
        return segs[2:3, pl.ds(pl.multiple_of(row * LANES, LANES), LANES)]

    def row_of(side, at):
        return ((here.seq + side) % 2) * tiles + at

    for side in range(2):
        for at in range(tiles):
            row = row_of(side, at)
            ids = from_tile(ids_of(row), eye)
            before = jnp.zeros((LANES, 1), jnp.float32)
            for other in range(2 * tiles):
                smaller = ids_of(other) < ids
                before += jnp.sum(smaller.astype(jnp.float32), axis=-1, keepdims=True)
            index = row * LANES + line
            angles = (index.astype(jnp.float32) - before) * freqs
            span = slice(at * LANES, (at + 1) * LANES)
            cos[side, span, :] = jnp.cos(angles)
            sin[side, span, :] = jnp.sin(angles)
            if side == 0:
                for key_side in range(2):
                    for key_at in range(tiles):
                        key_row = row_of(key_side, key_at)
                        same = ids_of(key_row) == ids
                        allowed = jnp.logical_and(same, key_row * LANES + lane <= index)
                        first = key_side * rows + key_at * LANES
                        mask[span, first : first + LANES] = allowed.astype(jnp.float32)


def open_kernel(rows, width, counts, tokens, gain, w_query, kv_weight, cot, qkv, x_low, act_t, w_qkv, rms, cos, sin,
                mask, g_col, *refs):
    here = Place()
    cols, segs = gain.shape[1], gain
    act, turn_send, turn_recv, local_sems, cot_part, g_send, g_recv, z_send, z_recv = refs[:9]
    share = rows // 4
    me = here.shard(0, 0)
    own_rows = pl.ds(pl.multiple_of(me * rows, rows), rows)

    def turn_copy(at):
        across, other = turned(at)
        first = pl.multiple_of(here.shard(across, other) * cols, cols)
        return remote(tokens.at[:, pl.ds(first, cols)], x_low.at[own_rows, :], turn_send.at[at], turn_recv.at[at],
                      here.device(across, other))

    wide = w_query.shape[1]
    local = [
        pltpu.make_async_copy(w_query, w_qkv.at[:, :wide], local_sems.at[0]),
        pltpu.make_async_copy(kv_weight, w_qkv.at[:, wide:], local_sems.at[1]),
        pltpu.make_async_copy(tokens.at[:, pl.ds(pl.multiple_of(me * cols, cols), cols)], x_low.at[own_rows, :],
                              local_sems.at[2]),
    ]
    load = pltpu.make_async_copy(cot.at[pl.ds(pl.multiple_of(here.z * share, share), share), :], cot_part,
                                 local_sems.at[3])
    load.start()
    for copy in local:
        copy.start()

    def g_copy(at):
        across, other = turned(at)
        first = pl.multiple_of(here.shard(across, other) * cols, cols)
        return remote(cot_part.at[:, pl.ds(first, cols)], g_col.at[me, here.z], g_send.at[at], g_recv.at[at],
                      here.device(across, other))

    def own_part():
        return pltpu.make_async_copy(cot_part.at[:, pl.ds(pl.multiple_of(me * cols, cols), cols)],
                                     g_col.at[me, here.z], local_sems.at[4])

    def quarter(way, at, step, peer):
        spot = g_col.at[:, at]
        return remote(spot, spot, z_send.at[way, step], z_recv.at[way, step], (here.dp, here.seq, here.z + peer))

    def pass_on(step):
        @pl.when(jnp.logical_and(here.z < 3, here.z >= step))
        def _():
            quarter(0, here.z - step, step, 1).start()

        @pl.when(jnp.logical_and(here.z > 0, here.z <= 3 - step))
        def _():
            quarter(1, here.z + step, step, -1).start()

    def take_quarters(step):
        @pl.when(here.z > step)
        def _():
            quarter(0, here.z - 1 - step, step, -1).wait_recv()

        @pl.when(here.z < 3 - step)
        def _():
            quarter(1, here.z + 1 + step, step, 1).wait_recv()

    greet(here, slice_peers(here), True)
    load.wait()
    own_part().start()
    for at in range(7):
        g_copy(at).start()
    for at in range(7):
        turn_copy(at).start()
    for copy in local:
        copy.wait()

    def squares(at, total):
        values = tokens[:, pl.ds(pl.multiple_of(at * cols, cols), cols)].astype(jnp.float32)
        return total + jnp.sum(values * values, axis=-1, keepdims=True)

    total = lax.fori_loop(0, 8, squares, jnp.zeros((rows, 1), jnp.float32))
    rms[...] = jnp.broadcast_to(lax.rsqrt(total / (8 * cols) + EPS), rms.shape)
    make_tables(here, rows, segs, cos, sin, mask)

    def prepare(first, count):
        def one(step, _):
            at = first + step
            span = row_span(here, *turned(at), rows)
            value = (x_low[span, :].astype(jnp.float32) * gain[0:1, :]).astype(act.dtype)
            act[span, :] = value
            return 0

        lax.fori_loop(0, count, one, 0)

    def before(stop):
        first, count = ((0, 2), (2, 4), (6, 2))[stop]
        if stop == 0:
            own_part().wait()
            for at in range(7):
                g_copy(at).wait_recv()
        else:
            take_quarters(stop - 1)
        pass_on(stop)
        for at in range(first, min(first + count, 7)):
            turn_copy(at).wait_recv()
        prepare(first, count)

    def flip():
        def one(shard, _):
            span = pl.ds(pl.multiple_of(shard * rows, rows), rows)
            act_t[:, span] = act[span, :].T
            return 0

        lax.fori_loop(0, 8, one, 0)

    product = products(here, act, w_qkv, False, rows, width, counts)
    total = Reduce(here, counts, product, refs[9:20], before)
    total.run()
    flip()

    def emit(at, first, second):
        for half, value in enumerate((first, second)):
            qkv[:, pl.ds(pl.multiple_of((half * counts + at) * width, width), width)] = value

    total.end(emit)
    take_quarters(2)
    for at in range(7):
        turn_copy(at).wait_send()
        g_copy(at).wait_send()
    for step in range(3):
        @pl.when(jnp.logical_and(here.z < 3, here.z >= step))
        def _(step=step):
            quarter(0, here.z - step, step, 1).wait_send()

        @pl.when(jnp.logical_and(here.z > 0, here.z <= 3 - step))
        def _(step=step):
            quarter(1, here.z + step, step, -1).wait_send()


def opening(tokens, gain, w_query, kv_weight, cot, cid, width=256):
    rows = tokens.shape[0]
    cols, wide = w_query.shape
    every = wide + kv_weight.shape[1]
    counts = every // (2 * width)
    low, f32 = jnp.bfloat16, jnp.float32
    dma = pltpu.SemaphoreType.DMA
    vm = pl.BlockSpec(memory_space=pltpu.VMEM)
    hbm = pl.BlockSpec(memory_space=pl.ANY)
    out_shape = [
        jax.ShapeDtypeStruct((rows, every), f32),
        jax.ShapeDtypeStruct((8 * rows, cols), low),
        jax.ShapeDtypeStruct((cols, 8 * rows), low),
        jax.ShapeDtypeStruct((cols, every), low),
        jax.ShapeDtypeStruct((rows, LANES), f32),
        jax.ShapeDtypeStruct((2, rows, LANES), f32),
        jax.ShapeDtypeStruct((2, rows, LANES), f32),
        jax.ShapeDtypeStruct((rows, 2 * rows), f32),
        jax.ShapeDtypeStruct((8, 4, rows // 4, cols), low),
    ]
    scratch = [
        pltpu.VMEM((8 * rows, cols), low), dma((7,)), dma((7,)), dma((5,)),
        pltpu.VMEM((rows // 4, 8 * cols), low), dma((7,)), dma((7,)), dma((2, 3)), dma((2, 3)),
    ]
    scratch += reduce_scratch(counts, rows, width)
    kernel = functools.partial(open_kernel, rows, width, counts)
    return kernel_call(kernel, out_shape, [tokens, gain, w_query, kv_weight, cot],
                       [vm, vm, hbm, hbm, hbm], scratch, cid, "open")


def ffn_kernel(rows, width, counts, x_low, attn, gain, w_gate, w_up, d_hidden, hidden, d_gate, d_up, act_t, tile_out,
               *refs, late):
    here = Place()
    cols = gain.shape[1]
    act, weight, tiny_own, tiny_all, tiny_send, tiny_recv, dots, local_sems = refs[:8]
    tiny = Tiny(here, tiny_own, tiny_all, (tiny_send, tiny_recv), True)
    half_cols = counts * width
    local = [
        pltpu.make_async_copy(w_gate, weight.at[:, :half_cols], local_sems.at[0]),
        pltpu.make_async_copy(w_up, weight.at[:, half_cols:], local_sems.at[1]),
    ]
    for copy in local:
        copy.start()
    eye = diagonal()
    tiny_own[...] = jnp.zeros_like(tiny_own)

    def prepare(number, _):
        shard = here.shard(*turned(number))
        for at in range(rows // LANES):
            span = pl.ds(pl.multiple_of(shard * rows + at * LANES, LANES), LANES)
            resid = x_low[span, :].astype(jnp.float32) + attn[span, :].astype(jnp.float32)
            act[span, :] = (resid * gain[1:2, :]).astype(act.dtype)
            square = jnp.sum(resid * resid, axis=-1, keepdims=True)
            tiny_own[shard, at : at + 1, :] = jnp.sum(square * eye, axis=0, keepdims=True)
        return 0

    def before(stop):
        if stop == 1:
            lax.fori_loop(2, 6, prepare, 0)
        if stop == 2:
            lax.fori_loop(6, 8, prepare, 0)
            tiny.begin()

    lax.fori_loop(0, 2, prepare, 0)
    greet(here, slice_peers(here))
    for copy in local:
        copy.wait()
    product = products(here, act, weight, False, rows, width, counts)
    total = Reduce(here, counts, product, refs[8:19], before)
    total.run()

    def flip(shard, _):
        span = pl.ds(pl.multiple_of(shard * rows, rows), rows)
        act_t[:, span] = act[span, :].T
        return 0

    lax.fori_loop(0, 8, flip, 0)
    tiny.end()
    tiles = rows // LANES
    mean = [from_tile(jnp.sum(tiny_all[:, at, :], axis=0, keepdims=True), eye) for at in range(tiles)]
    scale = lax.rsqrt(jnp.concatenate(mean, axis=0) / (8 * cols) + EPS)
    dots[...] = jnp.zeros_like(dots)
    late[0].wait()
    coeff = math.sqrt(2.0 / math.pi)

    def emit(at, first, second):
        span = pl.ds(pl.multiple_of(at * width, width), width)
        gate, up = first * scale, second * scale
        inner = jnp.tanh(coeff * (gate + 0.044715 * (gate * gate * gate)))
        gelu = 0.5 * gate * (1.0 + inner)
        slope = 0.5 * (1.0 + inner) + 0.5 * gate * (1.0 - inner * inner) * (
            coeff * (1.0 + 3.0 * 0.044715 * gate * gate))
        cot = d_hidden[:, span]
        hidden[:, span] = (gelu * up).astype(hidden.dtype)
        back_gate, back_up = cot * up * slope, cot * gelu
        d_gate[:, span] = (back_gate * scale).astype(d_gate.dtype)
        d_up[:, span] = (back_up * scale).astype(d_up.dtype)
        dots[...] += jnp.sum(back_gate * gate + back_up * up, axis=-1, keepdims=True)

    total.end(emit)
    tile_out[...] = jnp.zeros_like(tile_out)
    to_tile(tile_out, 0, dots[...] * (scale * scale * (1.0 / (8 * cols))), eye)


def ffn_scatter(x_low, attn, gain, w_gate, w_up, d_hidden, cid, width=512):
    rows, half = d_hidden.shape
    cols = gain.shape[1]
    counts = half // width
    low, f32 = jnp.bfloat16, jnp.float32
    dma = pltpu.SemaphoreType.DMA
    vm = pl.BlockSpec(memory_space=pltpu.VMEM)
    hbm = pl.BlockSpec(memory_space=pl.ANY)
    out_shape = [jax.ShapeDtypeStruct((rows, half), low)] * 3 + [
        jax.ShapeDtypeStruct((cols, 8 * rows), low),
        jax.ShapeDtypeStruct((8, LANES), f32),
    ]
    scratch = [
        pltpu.VMEM((8 * rows, cols), low),
        pltpu.VMEM((cols, 2 * half), low),
        pltpu.VMEM((8, 8, LANES), f32),
        pltpu.VMEM((8, 8, LANES), f32),
        dma((7,)), dma((7,)),
        pltpu.VMEM((rows, 1), f32),
        dma((2,)),
    ] + reduce_scratch(counts, rows, width)
    kernel = functools.partial(ffn_kernel, rows, width, counts)
    return kernel_call(kernel, out_shape, [x_low, attn, gain, w_gate, w_up, d_hidden], [vm, vm, vm, hbm, hbm, vm],
                       scratch, cid, "ffn", late=(5,))


def load_own(spread, payload, width, counts, sems):
    copies = []
    for half in range(2):
        for at in range(counts):
            first = at * width + (half * counts * width if len(payload) == 1 else 0)
            src = payload[half % len(payload)].at[:, first : first + width]
            copies.append(pltpu.make_async_copy(src, spread.slot(0, half, at), sems.at[half, at]))
    return copies


def chip_place(here, per):
    def place(at):
        return here.shard(at // (2 * per), at // per % 2) * per + at % per

    return place


def back_kernel(rows, width, counts, act_t, w_gate, w_up, d_gate, d_up, dots, x_low, attn, gain, d_norm, gain_grad,
                grad_gate, grad_up, *refs, late):
    here = Place()
    spread = Spread(here, counts, refs[:7])
    tiny_all, tiny_send, tiny_recv, own_sems, weight, sums, grads, staged, local_sems, out_sems = refs[7:17]
    contrib, rest, rest_sems = refs[17:20]
    line = Line(here, 4, [contrib, d_norm] + list(refs[20:]), chip_place(here, 2))
    tiny = Tiny(here, dots, tiny_all, (tiny_send, tiny_recv), False)
    half_cols = counts * width
    local = [
        pltpu.make_async_copy(w_gate, weight.at[:, :half_cols], local_sems.at[0]),
        pltpu.make_async_copy(w_up, weight.at[:, half_cols:], local_sems.at[1]),
    ]
    own = load_own(spread, (d_gate, d_up), width, counts, own_sems)
    for copy in own + local:
        copy.start()
    greet(here, tiny.peers, True)
    for copy in own:
        copy.wait()
    tiny.begin()
    spread.begin()
    sums[...] = jnp.zeros_like(sums)
    for copy in local + late:
        copy.wait()

    def columns(half, at):
        return pl.ds(pl.multiple_of((half * counts + at) * width, width), width)

    def clear(at, _):
        grads[:, columns(0, at)] = jnp.zeros((grads.shape[0], width), jnp.float32)
        return 0

    lax.fori_loop(0, 2 * counts, clear, 0)

    def blocks(across, half, at):
        cols = columns(half, at)
        gained = grads[:, cols]
        for other in range(2):
            row = row_span(here, across, other, rows)
            block = spread.got[across, (spread.core + other) % 2, half, at]
            sums[row, :] += dot_nt(block, weight[:, cols])
            gained = gained + dot_nn(act_t[:, row], block)
        grads[:, cols] = gained

    def leave(half, at):
        spot = pl.ds(pl.multiple_of(at * width, width), width)
        return pltpu.make_async_copy(staged.at[half], (grad_gate, grad_up)[half].at[:, spot],
                                     out_sems.at[half, at])

    eye = diagonal()
    gain_grad[...] = jnp.zeros_like(gain_grad)

    def close_chip(chip, target):
        def close_shard(other, _):
            shard = here.shard(chip, other)
            span = pl.ds(pl.multiple_of(shard * rows, rows), rows)
            loads = [pltpu.make_async_copy(src.at[span, :], rest.at[at], rest_sems.at[at])
                     for at, src in enumerate((x_low, attn))]
            for copy in loads:
                copy.start()
            for copy in loads:
                copy.wait()
            for at in range(rows // LANES):
                span = pl.ds(pl.multiple_of(shard * rows + at * LANES, LANES), LANES)
                piece = slice(at * LANES, (at + 1) * LANES)
                dot = from_tile(tiny_all[shard, at : at + 1, :], eye)
                resid = rest[0, piece, :].astype(jnp.float32) + rest[1, piece, :].astype(jnp.float32)
                value = sums[span, :]
                target[span, :] = (value * gain[1:2, :] - resid * dot).astype(target.dtype)
                gain_grad[...] += jnp.sum(value * resid, axis=0, keepdims=True)
            return 0

        lax.fori_loop(0, 2, close_shard, 0)

    def done(stage, at):
        @pl.when(jnp.logical_and(stage == 3, at > 0))
        def _():
            leave(0, at - 1).wait()
            leave(1, at - 1).wait()

        @pl.when(stage == 3)
        def _():
            for half in range(2):
                staged[half] = grads[:, columns(half, at)].astype(staged.dtype)
            leave(0, at).start()
            leave(1, at).start()

        @pl.when(jnp.logical_and(at == counts - 1, stage == 0))
        def _():
            close_chip(0, contrib)
            line.launch(0, 4)

        @pl.when(jnp.logical_and(at == counts - 1, stage == 2))
        def _():
            lax.fori_loop(1, 3, lambda chip, _: (close_chip(chip, d_norm), 0)[1], 0)

    def hook(step):
        @pl.when(jnp.logical_and(step >= counts, step < counts + 6))
        def _():
            line.step(step - counts)

    tiny.end()
    spread.run(blocks, hook, done)
    close_chip(3, d_norm)
    line.settle()
    spread.end()

    def drain(at, _):
        leave(0, at).wait()
        leave(1, at).wait()
        return 0

    lax.fori_loop(counts - 1, counts, drain, 0)


def back_gather(act_t, w_gate, w_up, d_gate, d_up, dots, x_low, attn, gain, cid, width=512):
    cols, total = act_t.shape
    rows, half = d_gate.shape
    counts = half // width
    low, f32 = jnp.bfloat16, jnp.float32
    dma = pltpu.SemaphoreType.DMA
    vm = pl.BlockSpec(memory_space=pltpu.VMEM)
    hbm = pl.BlockSpec(memory_space=pl.ANY)
    out_shape = [
        jax.ShapeDtypeStruct((total, cols), low),
        jax.ShapeDtypeStruct((1, cols), f32),
        jax.ShapeDtypeStruct((cols, half), low),
        jax.ShapeDtypeStruct((cols, half), low),
    ]
    scratch = spread_scratch(counts, rows, width) + [
        pltpu.VMEM((8, 8, LANES), f32), dma((7,)), dma((7,)), dma((2, counts)),
        pltpu.VMEM((cols, 2 * half), low),
        pltpu.VMEM((total, cols), f32),
        pltpu.VMEM((cols, 2 * half), f32),
        pltpu.VMEM((2, cols, width), low),
        dma((2,)), dma((2, counts)),
        pltpu.VMEM((total, cols), low),
        pltpu.VMEM((2, rows, cols), low),
        dma((2,)),
    ] + line_scratch(4, (4 * rows // 2, cols), low)
    operands = [act_t, w_gate, w_up, d_gate, d_up, dots, x_low, attn, gain]
    kernel = functools.partial(back_kernel, rows, width, counts)
    return kernel_call(kernel, out_shape, operands, [vm] + [hbm] * 4 + [vm, hbm, hbm, vm], scratch, cid, "back",
                       [vm, vm, hbm, hbm], (0,))


def down_kernel(rows, width, counts, cot, weight, hidden, d_norm, ffn, d_attn, grad, *refs, late):
    here = Place()
    spread = Spread(here, counts, refs[:7])
    own_sems, sums, grads, staged, out_sems, norm_out = refs[7:13]
    place = chip_place(here, 4)
    norm_line = Line(here, 24, [d_norm, norm_out] + list(refs[13:]), lambda at: place(at + 8))
    own = load_own(spread, (hidden,), width, counts, own_sems)
    for copy in own:
        copy.start()
    greet(here, slice_peers(here), True)
    norm_line.begin()
    for copy in own:
        copy.wait()
    spread.begin()
    sums[...] = jnp.zeros_like(sums)
    grads[...] = jnp.zeros_like(grads)
    for copy in late:
        copy.wait()

    def columns(half, at):
        return pl.ds(pl.multiple_of((half * counts + at) * width, width), width)

    def blocks(across, half, at):
        cols = columns(half, at)
        gained = grads[cols, :]
        for other in range(2):
            row = row_span(here, across, other, rows)
            block = spread.got[across, (spread.core + other) % 2, half, at]
            sums[row, :] += dot_nn(block, weight[cols, :])
            gained = gained + dot_tn(block, cot[row, :])
        grads[cols, :] = gained

    def leave(half, at):
        return pltpu.make_async_copy(staged.at[at % 2, half], grad.at[columns(half, at), :], out_sems.at[half, at])

    def done(stage, at):
        @pl.when(jnp.logical_and(stage == 3, at > 1))
        def _():
            leave(0, at - 2).wait()
            leave(1, at - 2).wait()

        @pl.when(stage == 3)
        def _():
            for half in range(2):
                staged[at % 2, half] = grads[columns(half, at), :].astype(staged.dtype)
            leave(0, at).start()
            leave(1, at).start()

    norm_line.steps(spread.run(blocks, norm_line.step, done), 26)
    ffn[...] = sums[...].astype(ffn.dtype)
    norm_line.settle()

    def add_norm(at, _):
        def add(source):
            span = row_span(here, at // 2, at % 2, rows)
            d_attn[span, :] = (cot[span, :].astype(jnp.float32) + source[span, :].astype(jnp.float32)).astype(
                d_attn.dtype)

        @pl.when(at < 2)
        def _():
            add(d_norm)

        @pl.when(at >= 2)
        def _():
            add(norm_out)
        return 0

    lax.fori_loop(0, 8, add_norm, 0)
    spread.end()

    def drain(at, _):
        leave(0, at).wait()
        leave(1, at).wait()
        return 0

    lax.fori_loop(counts - 2, counts, drain, 0)


def down_gather(cot, weight, hidden, d_norm, cid, width=256):
    total, cols = cot.shape
    rows, every = hidden.shape
    counts = every // (2 * width)
    low, f32 = jnp.bfloat16, jnp.float32
    dma = pltpu.SemaphoreType.DMA
    vm = pl.BlockSpec(memory_space=pltpu.VMEM)
    hbm = pl.BlockSpec(memory_space=pl.ANY)
    out_shape = [
        jax.ShapeDtypeStruct((total, cols), low),
        jax.ShapeDtypeStruct((total, cols), low),
        jax.ShapeDtypeStruct(weight.shape, low),
    ]
    scratch = spread_scratch(counts, rows, width) + [
        dma((2, counts)),
        pltpu.VMEM((total, cols), f32),
        pltpu.VMEM(weight.shape, f32),
        pltpu.VMEM((2, 2, width, cols), low),
        dma((2, counts)),
        pltpu.VMEM((total, cols), low),
    ] + line_scratch(24, (24 * rows // 4, cols), low)
    kernel = functools.partial(down_kernel, rows, width, counts)
    return kernel_call(kernel, out_shape, [cot, weight, hidden, d_norm], [vm, vm, hbm, vm], scratch, cid, "down",
                       [vm, vm, hbm], (0, 1))


def attend_kernel(rows, heads, cols, width, counts, qkv, rms, cos, sin, mask, w_out, g_col, w_down, attn, mixed_all,
                  kv, probs, queries, pair_rms, d_hidden, *refs, late):
    here = Place()
    spread = Spread(here, 1, refs[:7])
    part, pair_sems, tiny_own, tiny_pair, mixed_sems = refs[7:12]
    product = products(here, g_col, w_down, True, rows, width, counts)
    total = Reduce(here, counts, product, refs[12:23])
    piece = rows // 2

    def place(at):
        across, other, half_at = spread.block(at)
        return here.shard(across, other) * 2 + half_at

    line = Line(here, 32, [part, attn] + list(refs[23:]), lambda at: place(at // 2) * 2 + at % 2)
    got, core = spread.got, here.core
    greet(here, slice_peers(here), True)
    half = HD // 2
    scale = 1.0 / math.sqrt(HD)
    wide = heads * HD

    def rotated(first):
        lead = qkv[:, first : first + half] * rms[...]
        trail = qkv[:, first + half : first + HD] * rms[...]
        return lead * cos[0] - trail * sin[0], trail * cos[0] + lead * sin[0]

    low_k, high_k = rotated(wide)
    kv[0, :, :half] = low_k.astype(kv.dtype)
    kv[0, :, half:HD] = high_k.astype(kv.dtype)
    for at in range(2):
        first = HD + at * half
        kv[0, :, first : first + half] = (qkv[:, wide + first : wide + first + half] * rms[...]).astype(kv.dtype)
    eye = diagonal()
    tiny_own[...] = jnp.zeros_like(tiny_own)
    to_tile(tiny_own, 0, rms[:, :1], eye)
    pair_rms[0] = rms[...]
    pair = remote(kv.at[0], kv.at[1], pair_sems.at[0], pair_sems.at[1], spread.ydev)
    tiny = remote(tiny_own, tiny_pair, pair_sems.at[2], pair_sems.at[3], spread.ydev)
    for head in range(heads):
        if head == 1:
            pair.start()
            tiny.start()
        lead, trail = rotated(head * HD)
        queries[:, head * HD : head * HD + half] = (lead * scale).astype(queries.dtype)
        queries[:, head * HD + half : (head + 1) * HD] = (trail * scale).astype(queries.dtype)
    pair.wait()
    for copy in late:
        copy.wait()

    def one_head(head, _):
        query = queries[:, pl.ds(pl.multiple_of(head * HD, HD), HD)]
        scores = jnp.concatenate([dot_nt(query, kv[0, :, :HD]), dot_nt(query, kv[1, :, :HD])], axis=1)
        scores = jnp.where(mask[...] > 0, scores, NEG)
        expd = jnp.exp(scores - jnp.max(scores, axis=-1, keepdims=True))
        prob = expd / jnp.sum(expd, axis=-1, keepdims=True)
        probs[head] = prob
        prob_low = prob.astype(jnp.bfloat16)
        mixed = dot_nn(prob_low[:, :rows], kv[0, :, HD:]) + dot_nn(prob_low[:, rows:], kv[1, :, HD:])
        span = pl.ds(pl.multiple_of(head * HD, HD), HD)
        for half_at in range(2):
            low_mixed = mixed[half_at * piece : (half_at + 1) * piece, :].astype(got.dtype)
            got[0, core, half_at, 0, :, span] = low_mixed
        return 0

    lax.fori_loop(0, heads, one_head, 0)
    spread.begin_rows()

    def mixed_copy(at):
        across, other, half_at = spread.block(at)
        span = pl.ds(pl.multiple_of(place(at) * piece, piece), piece)
        return pltpu.make_async_copy(got.at[across, (core + other) % 2, half_at, 0], mixed_all.at[span, :],
                                     mixed_sems.at[at])

    def one_step(step, _):
        spread.receive_rows(step)

        @pl.when(step < 16)
        def _():
            across, other, half_at = spread.block(step)
            value = dot_nn(got[across, (core + other) % 2, half_at, 0], w_out[...])
            part[pl.ds(pl.multiple_of(place(step) * piece, piece), piece), :] = value.astype(part.dtype)
            mixed_copy(step).start()
            line.launch(2 * step, 2)

        @pl.when(step >= 2)
        def _():
            total.advance(step - 2)

        @pl.when(step >= 4)
        def _():
            line.step(2 * step - 8)
            line.step(2 * step - 7)
        return 0

    lax.fori_loop(0, 20, one_step, 0)
    line.end(32)

    def emit(at, first, second):
        for half_at, value in enumerate((first, second)):
            d_hidden[:, pl.ds(pl.multiple_of((half_at * counts + at) * width, width), width)] = value

    total.end(emit)
    for hop in range(3):
        spread.x_copy(hop, 0).wait_send()
        spread.y_copy(hop, 0).wait_send()
    for stage in range(4):
        for stream in range(2):
            spread.sib_copy(stage, stream, 0).wait_send()
    for at in range(16):
        mixed_copy(at).wait()
    tiny.wait()
    for at in range(rows // LANES):
        values = jnp.broadcast_to(from_tile(tiny_pair[at : at + 1, :], eye), (LANES, LANES))
        pair_rms[1, at * LANES : (at + 1) * LANES, :] = values


def attend(qkv, rms, cos, sin, mask, w_out, g_col, w_down, cid, width=512):
    rows = qkv.shape[0]
    wide, cols = w_out.shape
    heads = wide // HD
    counts = w_down.shape[0] // (2 * width)
    low, f32 = jnp.bfloat16, jnp.float32
    dma = pltpu.SemaphoreType.DMA
    vm = pl.BlockSpec(memory_space=pltpu.VMEM)
    out_shape = [
        jax.ShapeDtypeStruct((8 * rows, cols), low),
        jax.ShapeDtypeStruct((8 * rows, wide), low),
        jax.ShapeDtypeStruct((2, rows, 2 * HD), low),
        jax.ShapeDtypeStruct((heads, rows, 2 * rows), f32),
        jax.ShapeDtypeStruct((rows, wide), low),
        jax.ShapeDtypeStruct((2,) + rms.shape, f32),
        jax.ShapeDtypeStruct((rows, w_down.shape[0]), f32),
    ]
    scratch = spread_scratch(1, rows // 2, wide) + [
        pltpu.VMEM((8 * rows, cols), low), dma((4,)),
        pltpu.VMEM((8, LANES), f32), pltpu.VMEM((8, LANES), f32), dma((16,)),
    ] + reduce_scratch(counts, rows, width) + line_scratch(32, (8 * rows, cols), low)
    kernel = functools.partial(attend_kernel, rows, heads, cols, width, counts)
    operands = [qkv, rms, cos, sin, mask, w_out, g_col, w_down]
    out_specs = [vm, pl.BlockSpec(memory_space=pl.ANY)] + [vm] * 5
    return kernel_call(kernel, out_shape, operands, [vm] * 8, scratch, cid, "attend", out_specs, (4, 5, 6, 7))


def tail_kernel(rows, heads, per, d_attn, w_out, queries, kv, probs, rms, cos, sin, act_t, w_qkv, ffn, x_low,
                attn, gain, gain_grad, mixed_all, d_tok, out, grad_query, grad_out, kv_sum, gain_tiles, *refs, late):
    here = Place()
    width = HD
    counts = heads // 2
    part = rows // 2
    refs = list(refs)
    line_counts = 8 * per
    cols = d_attn.shape[1]
    extra = cols // (rows // per)

    def take(count):
        taken_refs = refs[:count]
        del refs[:count]
        return taken_refs

    total_refs = take(11)
    spread = Spread(here, 1, take(7))
    d_mixed, tiny_own, tiny_all, d_kv, give, taken, give_sems, tiny_send, tiny_recv = take(9)
    grad, grad_mixed, gain_sum, tile, tile_send, tile_recv, put_sems, local_sems, mixed_two, mixed_sems = take(10)

    def far(at):
        return at // (2 * per), at // per % 2

    def near(at):
        return spread.block(jnp.minimum(at, line_counts - 1))

    def place_ffn(at):
        return here.shard(*far(at)) * per + at % per

    def place_tok(at):
        across, other, half_at = near(at)
        return jnp.where(at < line_counts, here.shard(across, other) * per + half_at, at)

    ffn_sum, leaving = take(2)
    by_chip = chip_place(here, per)
    line = Line(here, line_counts, [ffn, ffn_sum] + take(8), by_chip)
    contrib, summed = take(2)
    line_tok = Line(here, line_counts + extra, [contrib, summed] + take(8), place_tok)
    tiny = Tiny(here, tiny_own, tiny_all, (tiny_send, tiny_recv), False)
    got, core = spread.got, here.core
    product = products(here, d_attn, w_out, True, rows, width, counts)
    total = Reduce(here, counts, product, total_refs)
    greet(here, tiny.peers, True)
    line.begin()
    grad_mixed[...] = jnp.zeros_like(grad_mixed)

    def mixed_copy(step):
        span = pl.ds(pl.multiple_of(step * rows, rows), rows)
        return pltpu.make_async_copy(mixed_all.at[span, :], mixed_two.at[step % 2], mixed_sems.at[step % 2])

    mixed_copy(0).start()

    def beside(step):
        line.step(step)

        @pl.when(step < 8)
        def _():
            span = pl.ds(pl.multiple_of(step * rows, rows), rows)
            mixed_copy(step).wait()

            @pl.when(step < 7)
            def _():
                mixed_copy(step + 1).start()

            grad_mixed[...] += dot_tn(mixed_two[step % 2], d_attn[span, :])

    done = total.run(beside)
    grad_out[...] = grad_mixed[...].astype(grad_out.dtype)

    def land(at, first, second):
        for half_at, value in enumerate((first, second)):
            d_mixed[:, pl.ds(pl.multiple_of((half_at * counts + at) * width, width), width)] = value.astype(
                d_mixed.dtype)

    total.end(land)
    half = HD // 2
    scale = 1.0 / math.sqrt(HD)
    depth = w_qkv.shape[0] * 8
    d_kv[...] = jnp.zeros_like(d_kv)
    for copy in late:
        copy.wait()

    def one_head(head, dots):
        span = pl.ds(pl.multiple_of(head * HD, HD), HD)
        query = queries[:, span]
        cot = d_mixed[:, span]
        prob = probs[head]
        d_prob = jnp.concatenate([dot_nt(cot, kv[0, :, HD:]), dot_nt(cot, kv[1, :, HD:])], axis=1)
        delta = jnp.sum(prob * d_prob, axis=-1, keepdims=True)
        d_score = (prob * (d_prob - delta)).astype(jnp.bfloat16)
        prob_low = prob.astype(jnp.bfloat16)
        d_query = (dot_nn(d_score[:, :rows], kv[0, :, :HD]) + dot_nn(d_score[:, rows:], kv[1, :, :HD])) * scale
        for side in range(2):
            keys = slice(side * rows, (side + 1) * rows)
            d_kv[side, :, :HD] += dot_tn(d_score[:, keys], query)
            d_kv[side, :, HD:] += dot_tn(prob_low[:, keys], cot)
        dots = dots + jnp.sum(d_query * query.astype(jnp.float32), axis=-1, keepdims=True)
        lead, trail = d_query[:, :half], d_query[:, half:]
        first = ((lead * cos[0] + trail * sin[0]) * rms[0]).astype(got.dtype)
        second = ((trail * cos[0] - lead * sin[0]) * rms[0]).astype(got.dtype)
        line.step(done + head)
        for rows_at in range(2):
            piece = slice(rows_at * part, (rows_at + 1) * part)
            got[0, core, rows_at, 0, :, pl.ds(pl.multiple_of(head * HD, HD), half)] = first[piece, :]
            got[0, core, rows_at, 0, :, pl.ds(pl.multiple_of(head * HD + half, half), half)] = second[piece, :]

        return dots

    dots = lax.fori_loop(0, heads, one_head, jnp.zeros((rows, 1), jnp.float32))
    eye = diagonal()
    tiny_own[...] = jnp.zeros_like(tiny_own)
    for side in (1, 0):
        d_key, d_value = d_kv[side, :, :HD], d_kv[side, :, HD:]
        own = jnp.sum(d_key * kv[side, :, :HD].astype(jnp.float32) +
                      d_value * kv[side, :, HD:].astype(jnp.float32), axis=-1, keepdims=True)
        if side == 0:
            own = own + dots * (1.0 / scale)
        own = own * (rms[side] * rms[side] * (1.0 / depth))
        to_tile(tiny_own, side * (rows // LANES), own, eye)
        lead, trail = d_key[:, :half], d_key[:, half:]
        parts = [(lead * cos[side] + trail * sin[side]) * rms[side],
                 (trail * cos[side] - lead * sin[side]) * rms[side],
                 d_value[:, :half] * rms[side], d_value[:, half:] * rms[side]]
        for at, value in enumerate(parts):
            if side == 1:
                give[:, at * half : (at + 1) * half] = value.astype(give.dtype)
            else:
                d_kv[0, :, at * half : (at + 1) * half] = value
    given = remote(give, taken, give_sems.at[0], give_sems.at[1], spread.ydev)
    given.start()
    grad[...] = jnp.zeros_like(grad)
    given.wait()
    for rows_at in range(2):
        piece = slice(rows_at * part, (rows_at + 1) * part)
        value = d_kv[0, piece, :] + taken[piece, :].astype(jnp.float32)
        got[0, core, rows_at, 0, :, heads * HD :] = value.astype(got.dtype)
    tiny.begin()
    spread.begin_rows()
    gain_sum[...] = jnp.zeros_like(gain_sum)
    tiny.end()

    def block_of(at):
        across, other, half_at = near(at)
        shard, partner = here.shard(across, other), here.shard((across + 2) % 4, other)
        block = got[across, (core + other) % 2, half_at, 0]
        first = pl.multiple_of(shard * rows + half_at * part, part)
        for tile_at in range(part // LANES):
            row = pl.ds(pl.multiple_of(first + tile_at * LANES, LANES), LANES)
            low_at = half_at * (part // LANES) + tile_at
            kept = rows // LANES + low_at
            dot = from_tile(tiny_all[shard, pl.ds(low_at, 1), :] + tiny_all[partner, pl.ds(kept, 1), :], eye)
            value = dot_nt(block[tile_at * LANES : (tile_at + 1) * LANES, :], w_qkv[...])
            x_rows = x_low[row, :].astype(jnp.float32)
            contrib[row, :] = (value * gain[0:1, :] - x_rows * dot).astype(contrib.dtype)
            gain_sum[...] += jnp.sum(value * x_rows, axis=0, keepdims=True)
        line_tok.launch(at, 1)

        @pl.when(other == 1)
        def _():
            twin = got[across, core, half_at, 0]
            twin_first = pl.multiple_of(here.shard(across, 0) * rows + half_at * part, part)
            rows_t, twin_t = act_t[:, pl.ds(first, part)], act_t[:, pl.ds(twin_first, part)]
            for at_col in range((heads + 2) * HD // 512):
                span = slice(at_col * 512, (at_col + 1) * 512)
                grad[:, span] += dot_nn(rows_t, block[:, span]) + dot_nn(twin_t, twin[:, span])

    me = here.shard(0, 0)
    columns = pl.ds(pl.multiple_of(me * cols, cols), cols)
    chunk = line.chunk

    def landing(which, at):
        sub = at % per if which == 0 else near(at)[2]
        return (out, d_tok)[which].at[pl.ds(pl.multiple_of(sub * chunk, chunk), chunk), columns]

    def leaver(which, at):
        return (leaving, line_tok.from_end)[which].at[at]

    def put(which, at):
        goal = here.device(*(far(at) if which == 0 else near(at)[:2]))
        return remote(leaver(which, at), landing(which, at), put_sems.at[which, 0, at], put_sems.at[which, 1, at],
                      goal)

    def keep(which, at):
        spot = at % per if which == 0 else near(at)[2]
        return pltpu.make_async_copy(leaver(which, at), landing(which, at), local_sems.at[which, spot])

    def emit(which, at):
        if which == 1:
            row = line_tok.rows(at)
            value = d_attn[row, :].astype(jnp.float32) + summed[row, :].astype(jnp.float32)
            line_tok.from_end[at] = value.astype(out.dtype)
            return
        row = pl.ds(pl.multiple_of(place_ffn(at) * chunk, chunk), chunk)

        def leave(source):
            value = x_low[row, :].astype(jnp.float32) + attn[row, :].astype(jnp.float32)
            leaving[at] = (value + source[row, :].astype(jnp.float32)).astype(out.dtype)

        leave(ffn_sum)

    def is_own(which, at):
        return at < per if which == 0 else jnp.logical_and(at < 4, at % 2 == 0)

    def send(which, at):
        own = is_own(which, at)

        @pl.when(own)
        def _():
            keep(which, at).start()

        @pl.when(jnp.logical_not(own))
        def _():
            put(which, at).start()

    def stage_step(step, _):
        spread.receive_rows(step)

        @pl.when(step < line_counts)
        def _():
            block_of(step)

        @pl.when(step < 5)
        def _():
            line.step(done + heads + step)

        @pl.when(step >= 4)
        def _():
            line_tok.step(step - 4)

        @pl.when(step > 0)
        def _():
            send(0, step - 1)

        @pl.when(line.inner == 0)
        def _():
            line.up(step).wait_send()
            line.down(step).wait_recv()

        emit(0, step)

        @pl.when(jnp.logical_and(line.inner == 1, step > 7))
        def _():
            send(1, step - 8)

        @pl.when(jnp.logical_and(line.inner == 1, step > 6))
        def _():
            emit(1, step - 7)
        return 0

    lax.fori_loop(0, line_counts, stage_step, 0)
    for half_at in range(cols // (rows // per)):
        span = pl.ds(line_counts * (rows // per) + half_at * (rows // per), rows // per)
        source = slice(half_at * (rows // per), (half_at + 1) * (rows // per))
        contrib[span, :] = grad[source, heads * HD :].astype(contrib.dtype)
    line_tok.launch(line_counts, extra)
    grad_query[...] = grad[:, : heads * HD].astype(grad_query.dtype)
    for at in range(cols // LANES):
        tile[at : at + 1, :] = gain_sum[:, at * LANES : (at + 1) * LANES]
        spot = cols // LANES + at
        tile[spot : spot + 1, :] = gain_grad[:, at * LANES : (at + 1) * LANES]

    def tile_copy(step):
        return remote(tile, gain_tiles.at[here.z], tile_send.at[step], tile_recv.at[step],
                      (here.dp, here.seq, (here.z + step + 1) % 4))

    send(0, line_counts - 1)
    line.drain()
    for step in range(3):
        tile_copy(step).start()
    gain_tiles[here.z] = tile[...]

    @pl.when(line.inner == 1)
    def _():
        start = line_counts - 4

        def both(at, _):
            line_tok.step(at)

            @pl.when(at < line_counts + 4)
            def _():
                send(1, at - 4)

            @pl.when(at < line_counts + 3)
            def _():
                emit(1, at - 3)
            return 0

        lax.fori_loop(start, line_counts + extra + 2, both, 0)

        def drain(at, _):
            line_tok.down(at).wait_send()
            return 0

        lax.fori_loop(0, line_counts + extra, drain, 0)

    @pl.when(line.inner == 0)
    def _():
        def arrive(at, _):
            line_tok.up(at).wait_send()
            line_tok.down(at).wait_recv()

            @pl.when(jnp.logical_and(at > 0, at <= line_counts))
            def _():
                send(1, at - 1)

            @pl.when(at < line_counts)
            def _():
                emit(1, at)
            return 0

        lax.fori_loop(0, line_counts + extra, arrive, 0)

    for half_at in range(extra):
        span = pl.ds((line_counts + half_at) * chunk, chunk)
        kv_sum[half_at * chunk : (half_at + 1) * chunk, :] = summed[span, :]
    for hop in range(3):
        spread.x_copy(hop, 0).wait_send()
        spread.y_copy(hop, 0).wait_send()
    for stage in range(4):
        spread.sib_copy(stage, 0, 0).wait_send()
        spread.sib_copy(stage, 1, 0).wait_send()

    def finish(at, _):
        for which in range(2):
            own = is_own(which, at)

            @pl.when(own)
            def _():
                keep(which, at).wait()

            @pl.when(jnp.logical_not(own))
            def _():
                put(which, at).wait()
        return 0

    lax.fori_loop(0, line_counts, finish, 0)
    for step in range(3):
        tile_copy(step).wait()


def tail(d_attn, w_out, queries, kv, probs, rms, cos, sin, act_t, w_qkv, ffn, x_low, attn, gain, gain_grad,
         mixed_all, cid,
 per=2):
    total, cols = d_attn.shape
    rows = total // 8
    wide = w_out.shape[0]
    heads = wide // HD
    low, f32 = jnp.bfloat16, jnp.float32
    dma = pltpu.SemaphoreType.DMA
    vm = pl.BlockSpec(memory_space=pltpu.VMEM)
    counts = 8 * per
    chunk = rows // per
    extra = cols // chunk
    long = (total + cols, cols)
    out_shape = [
        jax.ShapeDtypeStruct((rows, 8 * cols), low),
        jax.ShapeDtypeStruct((rows, 8 * cols), low),
        jax.ShapeDtypeStruct((cols, wide), low),
        jax.ShapeDtypeStruct(w_out.shape, low),
        jax.ShapeDtypeStruct((cols, 2 * HD), low),
        jax.ShapeDtypeStruct((4, 8, LANES), f32),
    ]
    scratch = reduce_scratch(heads // 2, rows, HD, 2) + spread_scratch(1, rows // 2, wide + 2 * HD)
    scratch += [
        pltpu.VMEM((rows, wide), low),
        pltpu.VMEM((8, LANES), f32),
        pltpu.VMEM((8, 8, LANES), f32),
        pltpu.VMEM((2, rows, 2 * HD), f32),
        pltpu.VMEM((rows, 2 * HD), low),
        pltpu.VMEM((rows, 2 * HD), low),
        dma((2,)), dma((7,)), dma((7,)),
        pltpu.VMEM(w_qkv.shape, f32),
        pltpu.VMEM(w_out.shape, f32),
        pltpu.VMEM((1, cols), f32),
        pltpu.VMEM((8, LANES), f32),
        dma((3,)), dma((3,)), dma((2, 2, counts)), dma((2, per)),
        pltpu.VMEM((2, rows, wide), low), dma((2,)),
        pltpu.VMEM((total, cols), low),
        pltpu.VMEM((counts, chunk, cols), low),
    ] + line_scratch(counts, (total, cols), low)
    scratch += [pltpu.VMEM(long, low), pltpu.VMEM(long, low)] + line_scratch(counts + extra, long, low)
    operands = [d_attn, w_out, queries, kv, probs, rms, cos, sin, act_t, w_qkv, ffn, x_low, attn, gain,
                gain_grad, mixed_all]
    kernel = functools.partial(tail_kernel, rows, heads, per)
    specs = [vm] * (len(operands) - 1) + [pl.BlockSpec(memory_space=pl.ANY)]
    return kernel_call(kernel, out_shape, operands, specs, scratch, cid, "tail",
                       late=(2, 3, 4, 8, 9, 11, 12))


LANES = 128


def acts_move(
    tokens, seg_ids, gain_attn, w_query, kv_weight, w_out, gain_ffn, w_gate, w_up, w_down, d_out
):
    small = jnp.stack([gain_attn, gain_ffn, seg_ids.astype(gain_ffn.dtype), gain_attn]).astype(jnp.float32)

    qkv, x_low, act_one_t, w_qkv, rms, cos, sin, mask, g_parts = opening(
        tokens, small, w_query, kv_weight, d_out, 1
    )
    g_low = g_parts.reshape(x_low.shape)
    attn, mixed_all, kv, probs, queries, pair_rms, d_hidden = attend(
        qkv, rms, cos, sin, mask, w_out, g_low, w_down, 2
    )
    hidden, d_gate, d_up, act_two_t, dots = ffn_scatter(x_low, attn, small, w_gate, w_up, d_hidden, 4)
    d_norm, grad_gain_two, grad_gate, grad_up = back_gather(
        act_two_t, w_gate, w_up, d_gate, d_up, dots, x_low, attn, small, 5
    )
    ffn, d_attn, grad_down = down_gather(g_low, w_down, hidden, d_norm, 6)
    d_tokens, out, grad_query, grad_out, grad_kv, gain_tiles = tail(
        d_attn,
        w_out,
        queries,
        kv,
        probs,
        pair_rms,
        cos,
        sin,
        act_one_t,
        w_qkv,
        ffn,
        x_low,
        attn,
        small,
        grad_gain_two,
        mixed_all,
        7,
    )
    gains = jnp.sum(gain_tiles, axis=0).reshape(2, -1)
    wider = jnp.float32
    return (
        out,
        d_tokens.astype(wider),
        gains[0],
        grad_query.astype(wider),
        grad_kv.astype(wider),
        grad_out.astype(wider),
        gains[1],
        grad_gate.astype(wider),
        grad_up.astype(wider),
        grad_down.astype(wider),
    )


def solution(mesh):
    in_specs = (
        P(("dp", "seq"), None),
        P("dp"),
        P(("dp", "seq")),
        P(("dp", "seq"), "tensor"),
        P(("dp", "seq"), None),
        P("tensor", ("dp", "seq")),
        P(("dp", "seq")),
        P(("dp", "seq"), "tensor"),
        P(("dp", "seq"), "tensor"),
        P("tensor", ("dp", "seq")),
        P(("dp", "seq"), None),
    )
    out_specs = (
        P(("dp", "seq"), None),
        P(("dp", "seq"), None),
        P(("dp", "seq")),
        P(("dp", "seq"), "tensor"),
        P(("dp", "seq"), None),
        P("tensor", ("dp", "seq")),
        P(("dp", "seq")),
        P(("dp", "seq"), "tensor"),
        P(("dp", "seq"), "tensor"),
        P("tensor", ("dp", "seq")),
    )

    def shards(*arrays):
        tokens = arrays[0]
        sizes = tuple(mesh.shape[name] for name in ("dp", "seq", "tensor"))
        count = tokens.shape[0] * sizes[0] * sizes[1]
        plan = acts_move if sizes == (4, 2, 4) and count <= tokens.shape[1] else weights_move
        return plan(*arrays)

    return jax.shard_map(shards, mesh=mesh, in_specs=in_specs, out_specs=out_specs, check_vma=False)
```

```python
import functools
import math

import jax
import jax.numpy as jnp
from jax import lax
from jax.experimental import pallas as pl
from jax.experimental.pallas import tpu as pltpu
from jax.sharding import PartitionSpec as P

HD = 256


EPS = 1e-06
NEG = -1e30


def place_tables(segs):
    length = segs.shape[0]
    index = jnp.arange(length, dtype=jnp.int32)
    flags = jnp.concatenate([jnp.ones((1,), dtype=bool), segs[1:] != segs[:-1]])
    starts = lax.cummax(jnp.where(flags, index, jnp.zeros_like(index)), axis=0)
    places = index - starts
    half_size = HD // 2
    freqs = jnp.exp(jnp.arange(half_size, dtype=jnp.float32) * (-math.log(10000.0) / half_size))
    angles = places.astype(jnp.float32)[:, None] * freqs[None, :]
    return (places, jnp.cos(angles), jnp.sin(angles))


def rotate(vector, cos_table, sin_table):
    half_size = vector.shape[-1] // 2
    leading = vector[..., :half_size]
    trailing = vector[..., half_size:]
    return jnp.concatenate(
        [leading * cos_table - trailing * sin_table, trailing * cos_table + leading * sin_table],
        axis=-1,
    )


def rotate_back(vector, cos_table, sin_table):
    half_size = vector.shape[-1] // 2
    leading = vector[..., :half_size]
    trailing = vector[..., half_size:]
    return jnp.concatenate(
        [leading * cos_table + trailing * sin_table, trailing * cos_table - leading * sin_table],
        axis=-1,
    )


def matmul(left, right):
    return jnp.dot(left, right, preferred_element_type=jnp.float32)


def matmul_nt(left, right):
    return lax.dot_general(
        left, right, (((1,), (1,)), ((), ())), preferred_element_type=jnp.float32
    )


def matmul_tn(left, right):
    return lax.dot_general(
        left, right, (((0,), (0,)), ((), ())), preferred_element_type=jnp.float32
    )


def gelu_tanh(values):
    return jax.nn.gelu(values, approximate=True)


def norm_back(d_act, normed, rms_val, gain_val):
    scaled = d_act * gain_val
    return rms_val * (scaled - normed * jnp.mean(scaled * normed, axis=-1, keepdims=True))


def weights_move(
    tokens, seg_ids, gain_attn, w_query, kv_weight, w_out, gain_ffn, w_gate, w_up, w_down, d_out
):
    rows = tokens.shape[0]
    scale_factor = 1.0 / math.sqrt(HD)
    offset = lax.axis_index("seq") * rows
    places, cos_table, sin_table = place_tables(seg_ids)
    own_places = lax.dynamic_slice_in_dim(places, offset, rows, 0)
    own_segs = lax.dynamic_slice_in_dim(seg_ids, offset, rows, 0)
    own_cos = lax.dynamic_slice_in_dim(cos_table, offset, rows, 0)
    own_sin = lax.dynamic_slice_in_dim(sin_table, offset, rows, 0)
    allowed = (own_segs[:, None] == seg_ids[None, :]) & (own_places[:, None] >= places[None, :])
    full_query, full_out, full_kv, full_gain_one = (
        lax.all_gather(w_query, ("dp", "seq"), axis=0, tiled=True),
        lax.all_gather(w_out, ("dp", "seq"), axis=1, tiled=True),
        lax.all_gather(kv_weight, ("dp", "seq"), axis=0, tiled=True),
        lax.all_gather(gain_attn, ("dp", "seq"), axis=0, tiled=True),
    )
    gain_one = full_gain_one.astype(jnp.float32)
    inputs = tokens.astype(jnp.float32)
    rms_one = lax.rsqrt(jnp.mean(inputs * inputs, axis=-1, keepdims=True) + EPS)
    norm_one = inputs * rms_one
    act_one = (norm_one * gain_one).astype(jnp.bfloat16)
    query_pre = matmul(act_one, full_query)
    heads = query_pre.shape[1] // HD
    kv_pre = matmul(act_one, full_kv)
    queries = (
        rotate(query_pre.reshape(rows, heads, HD), own_cos[:, None, :], own_sin[:, None, :])
        * scale_factor
    ).astype(jnp.bfloat16)
    own_kv = jnp.concatenate(
        [rotate(kv_pre[:, :HD], own_cos, own_sin), kv_pre[:, HD:]], axis=1
    ).astype(jnp.bfloat16)
    all_kv = lax.all_gather(own_kv, "seq", axis=0, tiled=True)
    keys = all_kv[:, :HD]
    values_all = all_kv[:, HD:]
    scores = jnp.einsum("rhd,kd->hrk", queries, keys, preferred_element_type=jnp.float32)
    scores = jnp.where(allowed[None], scores, NEG)
    top_score = jnp.max(scores, axis=-1, keepdims=True)
    expd = jnp.exp(scores - top_score)
    total = jnp.sum(expd, axis=-1, keepdims=True)
    log_total = top_score + jnp.log(total)
    probs_low = (expd / total).astype(jnp.bfloat16)
    mixed = (
        jnp.einsum("hrk,kd->rhd", probs_low, values_all, preferred_element_type=jnp.float32)
        .reshape(rows, heads * HD)
        .astype(jnp.bfloat16)
    )
    attn = lax.psum(matmul(mixed, full_out), "tensor")
    resid = inputs + attn
    full_gate, full_up, full_down, full_gain_two = (
        lax.all_gather(w_gate, ("dp", "seq"), axis=0, tiled=True),
        lax.all_gather(w_up, ("dp", "seq"), axis=0, tiled=True),
        lax.all_gather(w_down, ("dp", "seq"), axis=1, tiled=True),
        lax.all_gather(gain_ffn, ("dp", "seq"), axis=0, tiled=True),
    )
    gain_two = full_gain_two.astype(jnp.float32)
    rms_two = lax.rsqrt(jnp.mean(resid * resid, axis=-1, keepdims=True) + EPS)
    norm_two = resid * rms_two
    act_two = (norm_two * gain_two).astype(jnp.bfloat16)
    gate = matmul(act_two, full_gate)
    up_val = matmul(act_two, full_up)
    gelu_val, gelu_pull = jax.vjp(gelu_tanh, gate)
    hidden = (gelu_val * up_val).astype(jnp.bfloat16)
    ffn = lax.psum(matmul(hidden, full_down).astype(jnp.bfloat16), "tensor").astype(jnp.float32)
    out = (resid + ffn).astype(jnp.bfloat16)
    back_gate, back_up, back_down = (
        lax.all_gather(w_gate, ("dp", "seq"), axis=0, tiled=True),
        lax.all_gather(w_up, ("dp", "seq"), axis=0, tiled=True),
        lax.all_gather(w_down, ("dp", "seq"), axis=1, tiled=True),
    )
    d_hidden = matmul_nt(d_out, back_down)
    grad_down = matmul_tn(hidden, d_out)
    d_gate = gelu_pull(d_hidden * up_val)[0].astype(jnp.bfloat16)
    d_up = (d_hidden * gelu_val).astype(jnp.bfloat16)
    grad_gate = matmul_tn(act_two, d_gate)
    grad_up = matmul_tn(act_two, d_up)
    d_act_two = lax.psum(matmul_nt(d_gate, back_gate) + matmul_nt(d_up, back_up), "tensor")
    grad_gain_two = jnp.sum(d_act_two * norm_two, axis=0)
    d_resid = d_out.astype(jnp.float32) + norm_back(d_act_two, norm_two, rms_two, gain_two)
    ffn_grads = (
        lax.psum_scatter(
            grad_gate.astype(jnp.bfloat16), ("dp", "seq"), scatter_dimension=0, tiled=True
        ).astype(jnp.float32),
        lax.psum_scatter(
            grad_up.astype(jnp.bfloat16), ("dp", "seq"), scatter_dimension=0, tiled=True
        ).astype(jnp.float32),
        lax.psum_scatter(
            grad_down.astype(jnp.bfloat16), ("dp", "seq"), scatter_dimension=1, tiled=True
        ).astype(jnp.float32),
        lax.psum_scatter(
            grad_gain_two.astype(jnp.bfloat16), ("dp", "seq"), scatter_dimension=0, tiled=True
        ).astype(jnp.float32),
    )
    back_query, back_out, back_kv = (
        lax.all_gather(w_query, ("dp", "seq"), axis=0, tiled=True),
        lax.all_gather(w_out, ("dp", "seq"), axis=1, tiled=True),
        lax.all_gather(kv_weight, ("dp", "seq"), axis=0, tiled=True),
    )
    d_attn = d_resid.astype(jnp.bfloat16)
    grad_out = matmul_tn(mixed, d_attn)
    d_mixed = matmul_nt(d_attn, back_out).astype(jnp.bfloat16).reshape(rows, heads, HD)
    scores_again = jnp.einsum("rhd,kd->hrk", queries, keys, preferred_element_type=jnp.float32)
    probs = jnp.where(allowed[None], jnp.exp(scores_again - log_total), 0.0)
    d_probs = jnp.einsum("rhd,kd->hrk", d_mixed, values_all, preferred_element_type=jnp.float32)
    delta = jnp.sum(probs * d_probs, axis=-1, keepdims=True)
    d_scores = (probs * (d_probs - delta)).astype(jnp.bfloat16)
    d_queries = (
        jnp.einsum("hrk,kd->rhd", d_scores, keys, preferred_element_type=jnp.float32) * scale_factor
    )
    d_query_pre = (
        rotate_back(d_queries, own_cos[:, None, :], own_sin[:, None, :])
        .reshape(rows, heads * HD)
        .astype(jnp.bfloat16)
    )
    d_keys_part = jnp.einsum("hrk,rhd->kd", d_scores, queries, preferred_element_type=jnp.float32)
    d_values_part = jnp.einsum(
        "hrk,rhd->kd", probs.astype(jnp.bfloat16), d_mixed, preferred_element_type=jnp.float32
    )
    own_kv_grad = lax.psum_scatter(
        jnp.concatenate([d_keys_part, d_values_part], axis=1).astype(jnp.bfloat16),
        "seq",
        scatter_dimension=0,
        tiled=True,
    )
    d_act_query = matmul_nt(d_query_pre, back_query)
    d_act_sum, kv_grad = (
        lax.psum(d_act_query.astype(jnp.bfloat16), "tensor").astype(jnp.float32),
        lax.psum(own_kv_grad, "tensor").astype(jnp.float32),
    )
    d_kv_pre = jnp.concatenate(
        [rotate_back(kv_grad[:, :HD], own_cos, own_sin), kv_grad[:, HD:]], axis=1
    ).astype(jnp.bfloat16)
    d_act_one = d_act_sum + matmul_nt(d_kv_pre, back_kv)
    grad_query = matmul_tn(act_one, d_query_pre)
    grad_kv = matmul_tn(act_one, d_kv_pre)
    grad_gain_one = jnp.sum(d_act_one * norm_one, axis=0)
    d_tokens = d_resid + norm_back(d_act_one, norm_one, rms_one, gain_one)
    attn_grads = (
        lax.psum_scatter(
            grad_query.astype(jnp.bfloat16), ("dp", "seq"), scatter_dimension=0, tiled=True
        ).astype(jnp.float32),
        lax.psum_scatter(
            grad_out.astype(jnp.bfloat16), ("dp", "seq"), scatter_dimension=1, tiled=True
        ).astype(jnp.float32),
        lax.psum_scatter(
            grad_kv.astype(jnp.bfloat16), ("dp", "seq"), scatter_dimension=0, tiled=True
        ).astype(jnp.float32),
        lax.psum_scatter(
            grad_gain_one.astype(jnp.bfloat16), ("dp", "seq"), scatter_dimension=0, tiled=True
        ).astype(jnp.float32),
    )
    return (
        out,
        d_tokens,
        attn_grads[3],
        attn_grads[0],
        attn_grads[2],
        attn_grads[1],
        ffn_grads[3],
        ffn_grads[0],
        ffn_grads[1],
        ffn_grads[2],
    )


MESH = pl.DeviceIdType.MESH
VMEM_LIMIT = 66000 * 1024


class Place:
    def __init__(self):
        self.dp = lax.axis_index("dp")
        self.seq = lax.axis_index("seq")
        self.z = lax.axis_index("tensor")
        self.core = lax.rem(self.dp, 2)
        self.chip = lax.div(self.dp, 2)

    def device(self, across, other):
        chip = (self.chip + across) % 2
        seq = (self.seq + across // 2) % 2
        core = (self.core + other) % 2
        return chip * 2 + core, seq, self.z

    def shard(self, across, other):
        dp, seq, _ = self.device(across, other)
        return dp * 2 + seq


def greet(here, peers, line=False):
    barrier = pltpu.get_barrier_semaphore()
    peers = list(peers)
    if line:
        peers += [(here.dp, here.seq, (here.z + step) % 4) for step in range(1, 4)]
    for peer in peers:
        pl.semaphore_signal(barrier, inc=1, device_id=peer, device_id_type=MESH)
    pl.semaphore_wait(barrier, len(peers))


def remote(src, dst, send, recv, peer):
    return pltpu.make_async_remote_copy(
        src_ref=src, dst_ref=dst, send_sem=send, recv_sem=recv, device_id=peer, device_id_type=MESH
    )


class Line:
    def __init__(self, here, counts, refs, place=None):
        self.own, self.out, self.from_end, self.from_mid = refs[:4]
        self.sems = refs[4:10]
        self.counts = counts
        self.chunk = self.from_mid.shape[1]
        self.fold = self.from_end.shape[1] // self.chunk
        self.place = place
        z = here.z
        self.inner = ((z + 1) // 2) % 2
        self.mate = (here.dp, here.seq, z + 1 - 2 * (z % 2))
        self.other = (here.dp, here.seq, 3 - z)

    def rows(self, at):
        at = at if self.place is None else self.place(at)
        return pl.ds(pl.multiple_of(at * self.chunk, self.chunk), self.chunk)

    def inbox(self, at):
        span = pl.ds(pl.multiple_of(at % self.fold * self.chunk, self.chunk), self.chunk)
        return self.from_end.at[at // self.fold, span, :]

    def up(self, at):
        return remote(self.own.at[self.rows(at), :], self.inbox(at), self.sems[0].at[at],
                      self.sems[1].at[at], self.mate)

    def over(self, at):
        return remote(self.out.at[self.rows(at), :], self.from_mid.at[at], self.sems[2].at[at],
                      self.sems[3].at[at], self.other)

    def down(self, at):
        rows = self.rows(at)
        return remote(self.out.at[rows, :], self.out.at[rows, :], self.sems[4].at[at],
                      self.sems[5].at[at], self.mate)

    def launch(self, first, count):
        @pl.when(self.inner == 0)
        def _():
            def send(at, _):
                self.up(first + at).start()
                return 0

            lax.fori_loop(0, count, send, 0)

    def begin(self):
        self.launch(0, self.counts)

    def first(self, at):
        rows = self.rows(at)
        self.up(at).wait_recv()
        total = self.own[rows, :].astype(jnp.float32) + self.inbox(at)[...].astype(jnp.float32)
        self.out[rows, :] = total.astype(self.out.dtype)
        self.over(at).start()

    def second(self, at):
        rows = self.rows(at)
        self.over(at).wait()
        total = self.out[rows, :].astype(jnp.float32) + self.from_mid[at].astype(jnp.float32)
        self.out[rows, :] = total.astype(self.out.dtype)
        self.down(at).start()

    def step(self, at, start=0, count=None):
        count = self.counts if count is None else count

        @pl.when(jnp.logical_and(self.inner == 1, at < count))
        def _():
            self.first(start + at)

        @pl.when(jnp.logical_and(self.inner == 1, jnp.logical_and(at > 1, at < count + 2)))
        def _():
            self.second(start + at - 2)

    def steps(self, first, last, start=0, count=None):
        def rest(at, _):
            self.step(at, start, count)
            return 0

        lax.fori_loop(first, last, rest, 0)

    def settle(self):
        @pl.when(self.inner == 0)
        def _():
            def take(at, _):
                self.up(at).wait_send()
                self.down(at).wait_recv()
                return 0

            lax.fori_loop(0, self.counts, take, 0)

        self.drain()

    def drain(self):
        @pl.when(self.inner == 1)
        def _():
            def drain(at, _):
                self.down(at).wait_send()
                return 0

            lax.fori_loop(0, self.counts, drain, 0)

    def end(self, done=0):
        self.steps(min(done, self.counts + 2), self.counts + 2)
        self.settle()


def line_scratch(counts, shape, low, fold=1):
    chunk = shape[0] // counts
    inbox = pltpu.VMEM((counts // fold, chunk * fold, shape[1]), low)
    return [inbox, pltpu.VMEM((counts, chunk, shape[1]), low)] + [pltpu.SemaphoreType.DMA((counts,))] * 6


def turned(at):
    return 3 - at // 2, 1 - at % 2


def slice_peers(here):
    return [here.device(*turned(at)) for at in range(7)]


def kernel_call(kernel, out_shape, operands, specs, scratch, cid, name, out_specs=None, late=(), early=()):
    vm = pl.BlockSpec(memory_space=pltpu.VMEM)
    hbm = pl.BlockSpec(memory_space=pl.ANY)
    specs = [hbm if at in late else spec for at, spec in enumerate(specs)]
    out_specs = [hbm if at in early else spec for at, spec in enumerate(out_specs or [vm] * len(out_shape))]
    inside = [pltpu.VMEM(operands[at].shape, operands[at].dtype) for at in late]
    inside += [pltpu.VMEM(out_shape[at].shape, out_shape[at].dtype) for at in early]
    inside.append(pltpu.SemaphoreType.DMA((max(1, len(late) + len(early)),)))
    n_in, n_out = len(operands), len(out_shape)

    def body(*refs):
        ins, outs = list(refs[:n_in]), list(refs[n_in : n_in + n_out])
        rest, own = refs[n_in + n_out : -len(inside)], refs[-len(inside) :]
        loads, stores = [], []
        for spot, at in enumerate(late):
            copy = pltpu.make_async_copy(ins[at], own[spot], own[-1].at[spot])
            copy.start()
            loads.append(copy)
            ins[at] = own[spot]
        for number, at in enumerate(early):
            spot = len(late) + number
            stores.append(pltpu.make_async_copy(own[spot], outs[at], own[-1].at[spot]))
            outs[at] = own[spot]
        more = {}
        if late:
            more["late"] = loads
        if early:
            more["early"] = stores
        kernel(*ins, *outs, *rest, **more)
        for copy in stores:
            copy.wait()

    return pl.pallas_call(
        body,
        out_shape=out_shape,
        in_specs=specs,
        out_specs=out_specs,
        scratch_shapes=scratch + inside,
        compiler_params=pltpu.CompilerParams(
            collective_id=cid, has_side_effects=True, vmem_limit_bytes=VMEM_LIMIT
        ),
        name=f"{name}_{cid}",
    )(*operands)


class Tiny:
    def __init__(self, here, src, dst, sems, spread):
        self.here, self.src, self.dst, self.sems, self.spread = here, src, dst, sems, spread
        self.peers = slice_peers(here)
        self.me = here.shard(0, 0)

    def tile(self, shard):
        return self.src.at[shard] if self.spread else self.src

    def copy(self, at):
        return remote(self.tile(self.here.shard(*turned(at))), self.dst.at[self.me], self.sems[0].at[at],
                      self.sems[1].at[at], self.peers[at])

    def begin(self):
        for at in range(7):
            self.copy(at).start()
        self.dst[self.me] = self.tile(self.me)[...]

    def end(self):
        for at in range(7):
            self.copy(at).wait()


class Reduce:
    def __init__(self, here, counts, product, refs, before=None):
        self.counts, self.product, self.before = counts, product, before
        self.held, self.sib_out, self.sib_in, self.from_x, self.from_y = refs[:5]
        self.sib_sems, self.x_sems, self.y_sems = refs[5:7], refs[7:9], refs[9:11]
        self.sib, self.xdev, self.ydev = here.device(0, 1), here.device(1, 0), here.device(2, 0)
        self.steps = 4 * counts
        self.ring = self.sib_out.shape[0]

    def streams(self, stage):
        far = stage // 3
        x_chip = jnp.where(stage == 0, 3, jnp.where(stage == 2, 0, 1))
        y_chip = jnp.where(stage == 0, 3, jnp.where(stage == 2, 0, 2))
        return (x_chip, far), (y_chip, 1 - far)

    def to_sib(self, step, stream):
        stage, at = step // self.counts, step % self.counts
        return remote(self.sib_out.at[step % self.ring, stream], self.sib_in.at[stage, stream, at],
                      self.sib_sems[0].at[stage, stream, at], self.sib_sems[1].at[stage, stream, at], self.sib)

    def to_x(self, hop, at, stage=0):
        return remote(self.held.at[stage, 0, at], self.from_x.at[hop, at], self.x_sems[0].at[hop, at],
                      self.x_sems[1].at[hop, at], self.xdev)

    def to_y(self, hop, at, stage=0):
        return remote(self.held.at[stage, 1, at], self.from_y.at[hop, at], self.y_sems[0].at[hop, at],
                      self.y_sems[1].at[hop, at], self.ydev)

    def compute(self, step):
        stage, at = step // self.counts, step % self.counts
        if self.before:
            for stop in range(3):
                @pl.when(step == stop * self.counts)
                def _():
                    self.before(stop)

        @pl.when(step >= self.ring)
        def _():
            for stream in range(2):
                self.to_sib(step - self.ring, stream).wait_send()

        for stream, (across, half) in enumerate(self.streams(stage)):
            self.sib_out[step % self.ring, stream] = self.product(across, 1, half, at).astype(jnp.bfloat16)
            self.held[stage, stream, at] = self.product(across, 0, half, at).astype(jnp.bfloat16)
        for stream in range(2):
            self.to_sib(step, stream).start()

    def finish(self, step):
        stage, at = step // self.counts, step % self.counts
        for stream in range(2):
            self.to_sib(step, stream).wait_recv()

        def total(stream):
            return self.held[stage, stream, at].astype(jnp.float32) + self.sib_in[stage, stream, at].astype(
                jnp.float32)

        @pl.when(stage < 3)
        def _():
            for stream in range(2):
                self.held[stage, stream, at] = total(stream).astype(jnp.bfloat16)

        @pl.when(stage == 3)
        def _():
            self.to_y(0, at).wait_recv()
            self.held[3, 0, at] = (total(0) + self.from_y[0, at].astype(jnp.float32)).astype(jnp.bfloat16)
            self.to_x(0, at).wait_recv()
            self.held[3, 1, at] = (total(1) + self.from_x[0, at].astype(jnp.float32)).astype(jnp.bfloat16)

        @pl.when(stage != 2)
        def _():
            hop = stage - stage // 3
            self.to_x(hop, at, stage).start()
            self.to_y(hop, at, stage).start()

    def advance(self, step):
        @pl.when(step < self.steps)
        def _():
            self.compute(step)

        @pl.when(jnp.logical_and(step > 0, step <= self.steps))
        def _():
            self.finish(step - 1)

    def run(self, hook=None):
        def body(step, _):
            self.advance(step)

            if hook:
                hook(step)
            return 0

        lax.fori_loop(0, self.steps + 1, body, 0)
        return self.steps + 1

    def end(self, emit):
        def last(at, _):
            values = []
            for half in range(2):
                xs, ys = (1, 2) if half == 0 else (2, 1)
                self.to_x(xs, at).wait_recv()
                self.to_y(ys, at).wait_recv()
                values.append(self.held[2, half, at].astype(jnp.float32) + self.from_x[xs, at].astype(jnp.float32)
                              + self.from_y[ys, at].astype(jnp.float32))
            emit(at, *values)
            for hop in range(3):
                self.to_x(hop, at).wait_send()
                self.to_y(hop, at).wait_send()
            return 0

        lax.fori_loop(0, self.counts, last, 0)

        def drain(at, _):
            for stream in range(2):
                self.to_sib(self.steps - self.ring + at, stream).wait_send()
            return 0

        lax.fori_loop(0, self.ring, drain, 0)


def reduce_scratch(counts, rows, width, ring=4):
    low, dma = jnp.bfloat16, pltpu.SemaphoreType.DMA
    block = pltpu.VMEM((4, 2, counts, rows, width), low)
    landed = pltpu.VMEM((3, counts, rows, width), low)
    sent = pltpu.VMEM((ring, 2, rows, width), low)
    return [block, sent, block, landed, landed] + [dma((4, 2, counts))] * 2 + [dma((3, counts))] * 4


class Spread:
    def __init__(self, here, counts, refs):
        self.counts = counts
        self.got = refs[0]
        self.x_sems, self.y_sems, self.sib_sems = refs[1:3], refs[3:5], refs[5:7]
        self.core = here.core
        self.sib, self.xdev, self.ydev = here.device(0, 1), here.device(1, 0), here.device(2, 0)

    def slot(self, across, half, at):
        return self.got.at[across, self.core, half, at]

    def x_copy(self, hop, at):
        half = jnp.minimum(hop, 1)
        src = self.slot(2 * (hop // 2), half, at)
        dst = self.slot(1 + 2 * (hop // 2), half, at)
        return remote(src, dst, self.x_sems[0].at[hop, at], self.x_sems[1].at[hop, at], self.xdev)

    def y_copy(self, hop, at):
        half = 1 - jnp.minimum(hop, 1)
        src = self.slot(hop // 2, half, at)
        dst = self.slot(2 + hop // 2, half, at)
        return remote(src, dst, self.y_sems[0].at[hop, at], self.y_sems[1].at[hop, at], self.ydev)

    def streams(self, stage):
        some, last, late = jnp.minimum(stage, 1), stage // 3, stage // 2
        return (some + 2 * last, late), (2 * some + last, 1 - late)

    def block(self, at):
        x_stream, y_stream = self.streams(at // 4)
        second = at // 2 % 2
        across = x_stream[0] + second * (y_stream[0] - x_stream[0])
        half = x_stream[1] + second * (y_stream[1] - x_stream[1])
        return across, at % 2, half

    def begin_rows(self):
        for hop in range(2):
            self.x_copy(hop, 0).start()
            self.y_copy(hop, 0).start()
        for stream in range(2):
            self.sib_copy(0, stream, 0).start()

    def receive_rows(self, step):
        stage = step // 4

        @pl.when(jnp.logical_and(step % 4 == 0, jnp.logical_and(stage > 0, stage < 4)))
        def _():
            self.x_copy(stage - 1, 0).wait_recv()
            self.sib_copy(stage, 0, 0).start()
            self.y_copy(stage - 1, 0).wait_recv()
            self.sib_copy(stage, 1, 0).start()

        @pl.when(step == 4)
        def _():
            self.x_copy(2, 0).start()
            self.y_copy(2, 0).start()

        for stream in range(2):
            @pl.when(jnp.logical_and(step % 4 == 2 * stream, step < 16))
            def _(stream=stream):
                self.sib_copy(stage, stream, 0).wait_recv()

    def sib_copy(self, stage, stream, at):
        across, half = self.streams(stage)[stream]
        slot = self.slot(across, half, at)
        spot = (stage, stream, at)
        return remote(slot, slot, self.sib_sems[0].at[spot], self.sib_sems[1].at[spot], self.sib)

    def begin(self):
        def first(at, _):
            self.x_copy(0, at).start()
            self.y_copy(0, at).start()
            return 0

        def own(at, _):
            self.sib_copy(0, 0, at).start()
            self.sib_copy(0, 1, at).start()
            return 0

        lax.fori_loop(0, self.counts, first, 0)
        lax.fori_loop(0, self.counts, own, 0)

    def run(self, blocks, hook=None, done=None):
        counts = self.counts

        def body(step, _):
            stage, at = step // counts, step % counts

            @pl.when(jnp.logical_and(stage > 0, stage < 4))
            def _():
                self.x_copy(stage - 1, at).wait_recv()
                self.sib_copy(stage, 0, at).start()
                self.y_copy(stage - 1, at).wait_recv()
                self.sib_copy(stage, 1, at).start()

            @pl.when(jnp.logical_and(stage > 0, stage < 3))
            def _():
                self.x_copy(stage, at).start()
                self.y_copy(stage, at).start()

            @pl.when(step > 0)
            def _():
                old, spot = (step - 1) // counts, (step - 1) % counts
                for stream, (across, half) in enumerate(self.streams(old)):
                    self.sib_copy(old, stream, spot).wait_recv()
                    blocks(across, half, spot)
                if done:
                    done(old, spot)

            if hook:
                hook(step)
            return 0

        lax.fori_loop(0, 4 * counts + 1, body, 0)
        return 4 * counts + 1

    def end(self):
        def drain(at, _):
            for hop in range(3):
                self.x_copy(hop, at).wait_send()
                self.y_copy(hop, at).wait_send()
            for stage in range(4):
                self.sib_copy(stage, 0, at).wait_send()
                self.sib_copy(stage, 1, at).wait_send()
            return 0

        lax.fori_loop(0, self.counts, drain, 0)


def spread_scratch(counts, rows, width):
    dma = pltpu.SemaphoreType.DMA
    return [pltpu.VMEM((4, 2, 2, counts, rows, width), jnp.bfloat16)] + [dma((3, counts))] * 4 + [
        dma((4, 2, counts))] * 2


def row_span(here, across, other, rows):
    return pl.ds(pl.multiple_of(here.shard(across, other) * rows, rows), rows)


def dot_nt(left, right):
    return lax.dot_general(left, right, (((1,), (1,)), ((), ())), preferred_element_type=jnp.float32)


def dot_tn(left, right):
    return lax.dot_general(left, right, (((0,), (0,)), ((), ())), preferred_element_type=jnp.float32)


def dot_nn(left, right):
    return jnp.dot(left, right, preferred_element_type=jnp.float32)


def products(here, act, weight, nt, rows, width, counts):
    def product(across, other, half, at):
        cols = pl.ds(pl.multiple_of((half * counts + at) * width, width), width)
        block = act[row_span(here, across, other, rows), :]
        return dot_nt(block, weight[cols, :]) if nt else dot_nn(block, weight[:, cols])

    return product


def diagonal():
    return (lax.broadcasted_iota(jnp.int32, (LANES, LANES), 0) ==
            lax.broadcasted_iota(jnp.int32, (LANES, LANES), 1)).astype(jnp.float32)


def to_tile(tile, first, column, eye):
    for at in range(column.shape[0] // LANES):
        spread = column[at * LANES : (at + 1) * LANES, :] * eye
        tile[first + at : first + at + 1, :] = jnp.sum(spread, axis=0, keepdims=True)


def from_tile(row, eye):
    return jnp.sum(eye * row, axis=1, keepdims=True)


def make_tables(here, rows, segs, cos, sin, mask):
    eye = diagonal()
    tiles = rows // LANES
    freqs = jnp.exp(lax.broadcasted_iota(jnp.int32, (1, LANES), 1).astype(jnp.float32) * (-math.log(10000.0) / LANES))
    lane = lax.broadcasted_iota(jnp.int32, (1, LANES), 1)
    line = lax.broadcasted_iota(jnp.int32, (LANES, 1), 0)

    def ids_of(row):
        return segs[2:3, pl.ds(pl.multiple_of(row * LANES, LANES), LANES)]

    def row_of(side, at):
        return ((here.seq + side) % 2) * tiles + at

    for side in range(2):
        for at in range(tiles):
            row = row_of(side, at)
            ids = from_tile(ids_of(row), eye)
            before = jnp.zeros((LANES, 1), jnp.float32)
            for other in range(2 * tiles):
                smaller = ids_of(other) < ids
                before += jnp.sum(smaller.astype(jnp.float32), axis=-1, keepdims=True)
            index = row * LANES + line
            angles = (index.astype(jnp.float32) - before) * freqs
            span = slice(at * LANES, (at + 1) * LANES)
            cos[side, span, :] = jnp.cos(angles)
            sin[side, span, :] = jnp.sin(angles)
            if side == 0:
                for key_side in range(2):
                    for key_at in range(tiles):
                        key_row = row_of(key_side, key_at)
                        same = ids_of(key_row) == ids
                        allowed = jnp.logical_and(same, key_row * LANES + lane <= index)
                        first = key_side * rows + key_at * LANES
                        mask[span, first : first + LANES] = allowed.astype(jnp.float32)


def open_kernel(rows, width, counts, tokens, gain, w_query, kv_weight, cot, qkv, x_low, act_t, w_qkv, rms, cos, sin,
                mask, g_col, *refs, early):
    here = Place()
    cols, segs = gain.shape[1], gain
    act, turn_send, turn_recv, local_sems, cot_part, g_send, g_recv, z_send, z_recv = refs[:9]
    share = rows // 4
    me = here.shard(0, 0)
    own_rows = pl.ds(pl.multiple_of(me * rows, rows), rows)

    def turn_copy(at):
        across, other = turned(at)
        first = pl.multiple_of(here.shard(across, other) * cols, cols)
        return remote(tokens.at[:, pl.ds(first, cols)], x_low.at[own_rows, :], turn_send.at[at], turn_recv.at[at],
                      here.device(across, other))

    wide = w_query.shape[1]
    local = [
        pltpu.make_async_copy(w_query, w_qkv.at[:, :wide], local_sems.at[0]),
        pltpu.make_async_copy(kv_weight, w_qkv.at[:, wide:], local_sems.at[1]),
        pltpu.make_async_copy(tokens.at[:, pl.ds(pl.multiple_of(me * cols, cols), cols)], x_low.at[own_rows, :],
                              local_sems.at[2]),
    ]
    load = pltpu.make_async_copy(cot.at[pl.ds(pl.multiple_of(here.z * share, share), share), :], cot_part,
                                 local_sems.at[3])
    load.start()
    for copy in local:
        copy.start()

    def g_copy(at):
        across, other = turned(at)
        first = pl.multiple_of(here.shard(across, other) * cols, cols)
        return remote(cot_part.at[:, pl.ds(first, cols)], g_col.at[me, here.z], g_send.at[at], g_recv.at[at],
                      here.device(across, other))

    def own_part():
        return pltpu.make_async_copy(cot_part.at[:, pl.ds(pl.multiple_of(me * cols, cols), cols)],
                                     g_col.at[me, here.z], local_sems.at[4])

    def quarter(way, at, step, peer):
        spot = g_col.at[:, at]
        return remote(spot, spot, z_send.at[way, step], z_recv.at[way, step], (here.dp, here.seq, here.z + peer))

    def pass_on(step):
        @pl.when(jnp.logical_and(here.z < 3, here.z >= step))
        def _():
            quarter(0, here.z - step, step, 1).start()

        @pl.when(jnp.logical_and(here.z > 0, here.z <= 3 - step))
        def _():
            quarter(1, here.z + step, step, -1).start()

    def take_quarters(step):
        @pl.when(here.z > step)
        def _():
            quarter(0, here.z - 1 - step, step, -1).wait_recv()

        @pl.when(here.z < 3 - step)
        def _():
            quarter(1, here.z + 1 + step, step, 1).wait_recv()

    greet(here, slice_peers(here), True)
    load.wait()
    own_part().start()
    for at in range(7):
        g_copy(at).start()
    for at in range(7):
        turn_copy(at).start()
    for copy in local:
        copy.wait()
    early[2].start()

    def squares(at, total):
        values = tokens[:, pl.ds(pl.multiple_of(at * cols, cols), cols)].astype(jnp.float32)
        return total + jnp.sum(values * values, axis=-1, keepdims=True)

    total = lax.fori_loop(0, 8, squares, jnp.zeros((rows, 1), jnp.float32))
    rms[...] = jnp.broadcast_to(lax.rsqrt(total / (8 * cols) + EPS), rms.shape)
    make_tables(here, rows, segs, cos, sin, mask)
    for at in (3, 4, 5):
        early[at].start()

    def prepare(first, count):
        def one(step, _):
            at = first + step
            span = row_span(here, *turned(at), rows)
            value = (x_low[span, :].astype(jnp.float32) * gain[0:1, :]).astype(act.dtype)
            act[span, :] = value
            return 0

        lax.fori_loop(0, count, one, 0)

    def before(stop):
        first, count = ((0, 2), (2, 4), (6, 2))[stop]
        if stop == 0:
            own_part().wait()
            for at in range(7):
                g_copy(at).wait_recv()
        else:
            take_quarters(stop - 1)
        pass_on(stop)
        for at in range(first, min(first + count, 7)):
            turn_copy(at).wait_recv()
        prepare(first, count)
        if stop == 2:
            early[0].start()

    def flip():
        def one(shard, _):
            span = pl.ds(pl.multiple_of(shard * rows, rows), rows)
            act_t[:, span] = act[span, :].T
            return 0

        lax.fori_loop(0, 8, one, 0)

    product = products(here, act, w_qkv, False, rows, width, counts)
    total = Reduce(here, counts, product, refs[9:20], before)
    total.run()
    flip()
    early[1].start()

    def emit(at, first, second):
        for half, value in enumerate((first, second)):
            qkv[:, pl.ds(pl.multiple_of((half * counts + at) * width, width), width)] = value

    total.end(emit)
    take_quarters(2)
    early[6].start()
    for at in range(7):
        turn_copy(at).wait_send()
        g_copy(at).wait_send()
    for step in range(3):
        @pl.when(jnp.logical_and(here.z < 3, here.z >= step))
        def _(step=step):
            quarter(0, here.z - step, step, 1).wait_send()

        @pl.when(jnp.logical_and(here.z > 0, here.z <= 3 - step))
        def _(step=step):
            quarter(1, here.z + step, step, -1).wait_send()


def opening(tokens, gain, w_query, kv_weight, cot, cid, width=256):
    rows = tokens.shape[0]
    cols, wide = w_query.shape
    every = wide + kv_weight.shape[1]
    counts = every // (2 * width)
    low, f32 = jnp.bfloat16, jnp.float32
    dma = pltpu.SemaphoreType.DMA
    vm = pl.BlockSpec(memory_space=pltpu.VMEM)
    hbm = pl.BlockSpec(memory_space=pl.ANY)
    out_shape = [
        jax.ShapeDtypeStruct((rows, every), f32),
        jax.ShapeDtypeStruct((8 * rows, cols), low),
        jax.ShapeDtypeStruct((cols, 8 * rows), low),
        jax.ShapeDtypeStruct((cols, every), low),
        jax.ShapeDtypeStruct((rows, LANES), f32),
        jax.ShapeDtypeStruct((2, rows, LANES), f32),
        jax.ShapeDtypeStruct((2, rows, LANES), f32),
        jax.ShapeDtypeStruct((rows, 2 * rows), f32),
        jax.ShapeDtypeStruct((8, 4, rows // 4, cols), low),
    ]
    scratch = [
        pltpu.VMEM((8 * rows, cols), low), dma((7,)), dma((7,)), dma((5,)),
        pltpu.VMEM((rows // 4, 8 * cols), low), dma((7,)), dma((7,)), dma((2, 3)), dma((2, 3)),
    ]
    scratch += reduce_scratch(counts, rows, width)
    kernel = functools.partial(open_kernel, rows, width, counts)
    return kernel_call(kernel, out_shape, [tokens, gain, w_query, kv_weight, cot],
                       [vm, vm, hbm, hbm, hbm], scratch, cid, "open",
                       early=(1, 2, 3, 5, 6, 7, 8))


def ffn_kernel(rows, width, counts, x_low, attn, gain, w_gate, w_up, d_hidden, hidden, d_gate, d_up, act_t, tile_out,
               *refs, late, early):
    here = Place()
    cols = gain.shape[1]
    act, weight, tiny_own, tiny_all, tiny_send, tiny_recv, dots, local_sems = refs[:8]
    tiny = Tiny(here, tiny_own, tiny_all, (tiny_send, tiny_recv), True)
    half_cols = counts * width
    local = [
        pltpu.make_async_copy(w_gate, weight.at[:, :half_cols], local_sems.at[0]),
        pltpu.make_async_copy(w_up, weight.at[:, half_cols:], local_sems.at[1]),
    ]
    for copy in local:
        copy.start()
    eye = diagonal()
    tiny_own[...] = jnp.zeros_like(tiny_own)

    def prepare(number, _):
        shard = here.shard(*turned(number))
        for at in range(rows // LANES):
            span = pl.ds(pl.multiple_of(shard * rows + at * LANES, LANES), LANES)
            resid = x_low[span, :].astype(jnp.float32) + attn[span, :].astype(jnp.float32)
            act[span, :] = (resid * gain[1:2, :]).astype(act.dtype)
            square = jnp.sum(resid * resid, axis=-1, keepdims=True)
            tiny_own[shard, at : at + 1, :] = jnp.sum(square * eye, axis=0, keepdims=True)
        return 0

    def before(stop):
        if stop == 1:
            lax.fori_loop(2, 6, prepare, 0)
        if stop == 2:
            lax.fori_loop(6, 8, prepare, 0)
            tiny.begin()

    lax.fori_loop(0, 2, prepare, 0)
    greet(here, slice_peers(here))
    for copy in local:
        copy.wait()
    product = products(here, act, weight, False, rows, width, counts)
    total = Reduce(here, counts, product, refs[8:19], before)
    total.run()

    def flip(shard, _):
        span = pl.ds(pl.multiple_of(shard * rows, rows), rows)
        act_t[:, span] = act[span, :].T
        return 0

    lax.fori_loop(0, 8, flip, 0)
    early[0].start()
    tiny.end()
    tiles = rows // LANES
    mean = [from_tile(jnp.sum(tiny_all[:, at, :], axis=0, keepdims=True), eye) for at in range(tiles)]
    scale = lax.rsqrt(jnp.concatenate(mean, axis=0) / (8 * cols) + EPS)
    dots[...] = jnp.zeros_like(dots)
    late[0].wait()
    coeff = math.sqrt(2.0 / math.pi)

    def emit(at, first, second):
        span = pl.ds(pl.multiple_of(at * width, width), width)
        gate, up = first * scale, second * scale
        inner = jnp.tanh(coeff * (gate + 0.044715 * (gate * gate * gate)))
        gelu = 0.5 * gate * (1.0 + inner)
        slope = 0.5 * (1.0 + inner) + 0.5 * gate * (1.0 - inner * inner) * (
            coeff * (1.0 + 3.0 * 0.044715 * gate * gate))
        cot = d_hidden[:, span]
        hidden[:, span] = (gelu * up).astype(hidden.dtype)
        back_gate, back_up = cot * up * slope, cot * gelu
        d_gate[:, span] = (back_gate * scale).astype(d_gate.dtype)
        d_up[:, span] = (back_up * scale).astype(d_up.dtype)
        dots[...] += jnp.sum(back_gate * gate + back_up * up, axis=-1, keepdims=True)

    total.end(emit)
    tile_out[...] = jnp.zeros_like(tile_out)
    to_tile(tile_out, 0, dots[...] * (scale * scale * (1.0 / (8 * cols))), eye)


def ffn_scatter(x_low, attn, gain, w_gate, w_up, d_hidden, cid, width=512):
    rows, half = d_hidden.shape
    cols = gain.shape[1]
    counts = half // width
    low, f32 = jnp.bfloat16, jnp.float32
    dma = pltpu.SemaphoreType.DMA
    vm = pl.BlockSpec(memory_space=pltpu.VMEM)
    hbm = pl.BlockSpec(memory_space=pl.ANY)
    out_shape = [jax.ShapeDtypeStruct((rows, half), low)] * 3 + [
        jax.ShapeDtypeStruct((cols, 8 * rows), low),
        jax.ShapeDtypeStruct((8, LANES), f32),
    ]
    scratch = [
        pltpu.VMEM((8 * rows, cols), low),
        pltpu.VMEM((cols, 2 * half), low),
        pltpu.VMEM((8, 8, LANES), f32),
        pltpu.VMEM((8, 8, LANES), f32),
        dma((7,)), dma((7,)),
        pltpu.VMEM((rows, 1), f32),
        dma((2,)),
    ] + reduce_scratch(counts, rows, width)
    kernel = functools.partial(ffn_kernel, rows, width, counts)
    return kernel_call(kernel, out_shape, [x_low, attn, gain, w_gate, w_up, d_hidden], [vm, vm, vm, hbm, hbm, vm],
                       scratch, cid, "ffn", late=(5,), early=(3,))


def load_own(spread, payload, width, counts, sems):
    copies = []
    for half in range(2):
        for at in range(counts):
            first = at * width + (half * counts * width if len(payload) == 1 else 0)
            src = payload[half % len(payload)].at[:, first : first + width]
            copies.append(pltpu.make_async_copy(src, spread.slot(0, half, at), sems.at[half, at]))
    return copies


def chip_place(here, per):
    def place(at):
        return here.shard(at // (2 * per), at // per % 2) * per + at % per

    return place


def back_kernel(rows, width, counts, act_t, w_gate, w_up, d_gate, d_up, dots, x_low, attn, gain, d_norm, gain_grad,
                grad_gate, grad_up, *refs, late):
    here = Place()
    spread = Spread(here, counts, refs[:7])
    tiny_all, tiny_send, tiny_recv, own_sems, weight, sums, grads, staged, local_sems, out_sems = refs[7:17]
    contrib, rest, rest_sems = refs[17:20]
    line = Line(here, 4, [contrib, d_norm] + list(refs[20:]), chip_place(here, 2))
    tiny = Tiny(here, dots, tiny_all, (tiny_send, tiny_recv), False)
    half_cols = counts * width
    local = [
        pltpu.make_async_copy(w_gate, weight.at[:, :half_cols], local_sems.at[0]),
        pltpu.make_async_copy(w_up, weight.at[:, half_cols:], local_sems.at[1]),
    ]
    own = load_own(spread, (d_gate, d_up), width, counts, own_sems)
    for copy in own + local:
        copy.start()
    greet(here, tiny.peers, True)
    for copy in own:
        copy.wait()
    tiny.begin()
    spread.begin()
    sums[...] = jnp.zeros_like(sums)
    for copy in local + late:
        copy.wait()

    def columns(half, at):
        return pl.ds(pl.multiple_of((half * counts + at) * width, width), width)

    def clear(at, _):
        grads[:, columns(0, at)] = jnp.zeros((grads.shape[0], width), jnp.float32)
        return 0

    lax.fori_loop(0, 2 * counts, clear, 0)

    def blocks(across, half, at):
        cols = columns(half, at)
        gained = grads[:, cols]
        for other in range(2):
            row = row_span(here, across, other, rows)
            block = spread.got[across, (spread.core + other) % 2, half, at]
            sums[row, :] += dot_nt(block, weight[:, cols])
            gained = gained + dot_nn(act_t[:, row], block)
        grads[:, cols] = gained

    def leave(half, at):
        spot = pl.ds(pl.multiple_of(at * width, width), width)
        return pltpu.make_async_copy(staged.at[half], (grad_gate, grad_up)[half].at[:, spot],
                                     out_sems.at[half, at])

    eye = diagonal()
    gain_grad[...] = jnp.zeros_like(gain_grad)

    def close_chip(chip, target):
        def close_shard(other, _):
            shard = here.shard(chip, other)
            span = pl.ds(pl.multiple_of(shard * rows, rows), rows)
            loads = [pltpu.make_async_copy(src.at[span, :], rest.at[at], rest_sems.at[at])
                     for at, src in enumerate((x_low, attn))]
            for copy in loads:
                copy.start()
            for copy in loads:
                copy.wait()
            for at in range(rows // LANES):
                span = pl.ds(pl.multiple_of(shard * rows + at * LANES, LANES), LANES)
                piece = slice(at * LANES, (at + 1) * LANES)
                dot = from_tile(tiny_all[shard, at : at + 1, :], eye)
                resid = rest[0, piece, :].astype(jnp.float32) + rest[1, piece, :].astype(jnp.float32)
                value = sums[span, :]
                target[span, :] = (value * gain[1:2, :] - resid * dot).astype(target.dtype)
                gain_grad[...] += jnp.sum(value * resid, axis=0, keepdims=True)
            return 0

        lax.fori_loop(0, 2, close_shard, 0)

    def done(stage, at):
        @pl.when(jnp.logical_and(stage == 3, at > 0))
        def _():
            leave(0, at - 1).wait()
            leave(1, at - 1).wait()

        @pl.when(stage == 3)
        def _():
            for half in range(2):
                staged[half] = grads[:, columns(half, at)].astype(staged.dtype)
            leave(0, at).start()
            leave(1, at).start()

        @pl.when(jnp.logical_and(at == counts - 1, stage == 0))
        def _():
            close_chip(0, contrib)
            line.launch(0, 4)

        @pl.when(jnp.logical_and(at == counts - 1, stage == 2))
        def _():
            lax.fori_loop(1, 3, lambda chip, _: (close_chip(chip, d_norm), 0)[1], 0)

    def hook(step):
        @pl.when(jnp.logical_and(step >= counts, step < counts + 6))
        def _():
            line.step(step - counts)

    tiny.end()
    spread.run(blocks, hook, done)
    close_chip(3, d_norm)
    line.settle()
    spread.end()

    def drain(at, _):
        leave(0, at).wait()
        leave(1, at).wait()
        return 0

    lax.fori_loop(counts - 1, counts, drain, 0)


def back_gather(act_t, w_gate, w_up, d_gate, d_up, dots, x_low, attn, gain, cid, width=512):
    cols, total = act_t.shape
    rows, half = d_gate.shape
    counts = half // width
    low, f32 = jnp.bfloat16, jnp.float32
    dma = pltpu.SemaphoreType.DMA
    vm = pl.BlockSpec(memory_space=pltpu.VMEM)
    hbm = pl.BlockSpec(memory_space=pl.ANY)
    out_shape = [
        jax.ShapeDtypeStruct((total, cols), low),
        jax.ShapeDtypeStruct((1, cols), f32),
        jax.ShapeDtypeStruct((cols, half), low),
        jax.ShapeDtypeStruct((cols, half), low),
    ]
    scratch = spread_scratch(counts, rows, width) + [
        pltpu.VMEM((8, 8, LANES), f32), dma((7,)), dma((7,)), dma((2, counts)),
        pltpu.VMEM((cols, 2 * half), low),
        pltpu.VMEM((total, cols), f32),
        pltpu.VMEM((cols, 2 * half), f32),
        pltpu.VMEM((2, cols, width), low),
        dma((2,)), dma((2, counts)),
        pltpu.VMEM((total, cols), low),
        pltpu.VMEM((2, rows, cols), low),
        dma((2,)),
    ] + line_scratch(4, (4 * rows // 2, cols), low)
    operands = [act_t, w_gate, w_up, d_gate, d_up, dots, x_low, attn, gain]
    kernel = functools.partial(back_kernel, rows, width, counts)
    return kernel_call(kernel, out_shape, operands, [vm] + [hbm] * 4 + [vm, hbm, hbm, vm], scratch, cid, "back",
                       [vm, vm, hbm, hbm], (0,))


def down_kernel(rows, width, counts, cot, weight, hidden, d_norm, ffn, d_attn, grad, *refs, late):
    here = Place()
    spread = Spread(here, counts, refs[:7])
    own_sems, sums, grads, staged, out_sems, norm_out = refs[7:13]
    place = chip_place(here, 2)
    norm_line = Line(here, 12, [d_norm, norm_out] + list(refs[13:]), lambda at: place(at + 4))
    own = load_own(spread, (hidden,), width, counts, own_sems)
    for copy in own:
        copy.start()
    greet(here, slice_peers(here), True)
    norm_line.begin()
    for copy in own:
        copy.wait()
    spread.begin()
    sums[...] = jnp.zeros_like(sums)
    grads[...] = jnp.zeros_like(grads)
    for copy in late:
        copy.wait()

    def columns(half, at):
        return pl.ds(pl.multiple_of((half * counts + at) * width, width), width)

    def blocks(across, half, at):
        cols = columns(half, at)
        gained = grads[cols, :]
        for other in range(2):
            row = row_span(here, across, other, rows)
            block = spread.got[across, (spread.core + other) % 2, half, at]
            sums[row, :] += dot_nn(block, weight[cols, :])
            gained = gained + dot_tn(block, cot[row, :])
        grads[cols, :] = gained

    def leave(half, at):
        return pltpu.make_async_copy(staged.at[at % 2, half], grad.at[columns(half, at), :], out_sems.at[half, at])

    def done(stage, at):
        @pl.when(jnp.logical_and(stage == 3, at > 1))
        def _():
            leave(0, at - 2).wait()
            leave(1, at - 2).wait()

        @pl.when(stage == 3)
        def _():
            for half in range(2):
                staged[at % 2, half] = grads[columns(half, at), :].astype(staged.dtype)
            leave(0, at).start()
            leave(1, at).start()


    def hook(step):
        @pl.when(step % 3 < 2)
        def _():
            norm_line.step(step // 3 * 2 + step % 3)

    spread.run(blocks, hook, done)
    ffn[...] = sums[...].astype(ffn.dtype)
    norm_line.settle()

    def add_norm(at, _):
        def add(source):
            span = row_span(here, at // 2, at % 2, rows)
            d_attn[span, :] = (cot[span, :].astype(jnp.float32) + source[span, :].astype(jnp.float32)).astype(
                d_attn.dtype)

        @pl.when(at < 2)
        def _():
            add(d_norm)

        @pl.when(at >= 2)
        def _():
            add(norm_out)
        return 0

    lax.fori_loop(0, 8, add_norm, 0)
    spread.end()

    def drain(at, _):
        leave(0, at).wait()
        leave(1, at).wait()
        return 0

    lax.fori_loop(counts - 2, counts, drain, 0)


def down_gather(cot, weight, hidden, d_norm, cid, width=256):
    total, cols = cot.shape
    rows, every = hidden.shape
    counts = every // (2 * width)
    low, f32 = jnp.bfloat16, jnp.float32
    dma = pltpu.SemaphoreType.DMA
    vm = pl.BlockSpec(memory_space=pltpu.VMEM)
    hbm = pl.BlockSpec(memory_space=pl.ANY)
    out_shape = [
        jax.ShapeDtypeStruct((total, cols), low),
        jax.ShapeDtypeStruct((total, cols), low),
        jax.ShapeDtypeStruct(weight.shape, low),
    ]
    scratch = spread_scratch(counts, rows, width) + [
        dma((2, counts)),
        pltpu.VMEM((total, cols), f32),
        pltpu.VMEM(weight.shape, f32),
        pltpu.VMEM((2, 2, width, cols), low),
        dma((2, counts)),
        pltpu.VMEM((total, cols), low),
    ] + line_scratch(12, (12 * rows // 2, cols), low)
    kernel = functools.partial(down_kernel, rows, width, counts)
    return kernel_call(kernel, out_shape, [cot, weight, hidden, d_norm], [vm, vm, hbm, vm], scratch, cid, "down",
                       [vm, vm, hbm], (0, 1))


def attend_kernel(rows, heads, cols, width, counts, qkv, rms, cos, sin, mask, w_out, g_col, w_down, attn, mixed_all,
                  kv, probs, queries, pair_rms, d_hidden, *refs, late, early):
    here = Place()
    spread = Spread(here, 1, refs[:7])
    part, pair_sems, tiny_own, tiny_pair, mixed_sems = refs[7:12]
    product = products(here, g_col, w_down, True, rows, width, counts)
    total = Reduce(here, counts, product, refs[12:23])
    piece = rows // 2

    def place(at):
        across, other, half_at = spread.block(at)
        return here.shard(across, other) * 2 + half_at

    line = Line(here, 16, [part, attn] + list(refs[23:]), place)
    got, core = spread.got, here.core
    greet(here, slice_peers(here), True)
    half = HD // 2
    scale = 1.0 / math.sqrt(HD)
    wide = heads * HD

    def rotated(first):
        lead = qkv[:, first : first + half] * rms[...]
        trail = qkv[:, first + half : first + HD] * rms[...]
        return lead * cos[0] - trail * sin[0], trail * cos[0] + lead * sin[0]

    low_k, high_k = rotated(wide)
    kv[0, :, :half] = low_k.astype(kv.dtype)
    kv[0, :, half:HD] = high_k.astype(kv.dtype)
    for at in range(2):
        first = HD + at * half
        kv[0, :, first : first + half] = (qkv[:, wide + first : wide + first + half] * rms[...]).astype(kv.dtype)
    eye = diagonal()
    tiny_own[...] = jnp.zeros_like(tiny_own)
    to_tile(tiny_own, 0, rms[:, :1], eye)
    pair_rms[0] = rms[...]
    pair = remote(kv.at[0], kv.at[1], pair_sems.at[0], pair_sems.at[1], spread.ydev)
    tiny = remote(tiny_own, tiny_pair, pair_sems.at[2], pair_sems.at[3], spread.ydev)
    for head in range(heads):
        if head == 1:
            pair.start()
            tiny.start()
        lead, trail = rotated(head * HD)
        queries[:, head * HD : head * HD + half] = (lead * scale).astype(queries.dtype)
        queries[:, head * HD + half : (head + 1) * HD] = (trail * scale).astype(queries.dtype)
    early[2].start()
    pair.wait()
    early[0].start()
    for copy in late:
        copy.wait()

    def one_head(head, _):
        query = queries[:, pl.ds(pl.multiple_of(head * HD, HD), HD)]
        scores = jnp.concatenate([dot_nt(query, kv[0, :, :HD]), dot_nt(query, kv[1, :, :HD])], axis=1)
        scores = jnp.where(mask[...] > 0, scores, NEG)
        expd = jnp.exp(scores - jnp.max(scores, axis=-1, keepdims=True))
        prob = expd / jnp.sum(expd, axis=-1, keepdims=True)
        probs[head] = prob
        prob_low = prob.astype(jnp.bfloat16)
        mixed = dot_nn(prob_low[:, :rows], kv[0, :, HD:]) + dot_nn(prob_low[:, rows:], kv[1, :, HD:])
        span = pl.ds(pl.multiple_of(head * HD, HD), HD)
        for half_at in range(2):
            low_mixed = mixed[half_at * piece : (half_at + 1) * piece, :].astype(got.dtype)
            got[0, core, half_at, 0, :, span] = low_mixed
        return 0

    lax.fori_loop(0, heads, one_head, 0)
    early[1].start()
    spread.begin_rows()

    def mixed_copy(at):
        across, other, half_at = spread.block(at)
        span = pl.ds(pl.multiple_of(place(at) * piece, piece), piece)
        return pltpu.make_async_copy(got.at[across, (core + other) % 2, half_at, 0], mixed_all.at[span, :],
                                     mixed_sems.at[at])

    def one_step(step, _):
        spread.receive_rows(step)

        @pl.when(step < 16)
        def _():
            across, other, half_at = spread.block(step)
            value = dot_nn(got[across, (core + other) % 2, half_at, 0], w_out[...])
            part[pl.ds(pl.multiple_of(place(step) * piece, piece), piece), :] = value.astype(part.dtype)
            mixed_copy(step).start()
            line.launch(step, 1)

        @pl.when(step >= 2)
        def _():
            total.advance(step - 2)

        @pl.when(step >= 4)
        def _():
            line.step(step - 4)
        return 0

    lax.fori_loop(0, 20, one_step, 0)
    line.end(16)

    def emit(at, first, second):
        for half_at, value in enumerate((first, second)):
            d_hidden[:, pl.ds(pl.multiple_of((half_at * counts + at) * width, width), width)] = value

    total.end(emit)
    for hop in range(3):
        spread.x_copy(hop, 0).wait_send()
        spread.y_copy(hop, 0).wait_send()
    for stage in range(4):
        for stream in range(2):
            spread.sib_copy(stage, stream, 0).wait_send()
    for at in range(16):
        mixed_copy(at).wait()
    tiny.wait()
    for at in range(rows // LANES):
        values = jnp.broadcast_to(from_tile(tiny_pair[at : at + 1, :], eye), (LANES, LANES))
        pair_rms[1, at * LANES : (at + 1) * LANES, :] = values


def attend(qkv, rms, cos, sin, mask, w_out, g_col, w_down, cid, width=512):
    rows = qkv.shape[0]
    wide, cols = w_out.shape
    heads = wide // HD
    counts = w_down.shape[0] // (2 * width)
    low, f32 = jnp.bfloat16, jnp.float32
    dma = pltpu.SemaphoreType.DMA
    vm = pl.BlockSpec(memory_space=pltpu.VMEM)
    out_shape = [
        jax.ShapeDtypeStruct((8 * rows, cols), low),
        jax.ShapeDtypeStruct((8 * rows, wide), low),
        jax.ShapeDtypeStruct((2, rows, 2 * HD), low),
        jax.ShapeDtypeStruct((heads, rows, 2 * rows), f32),
        jax.ShapeDtypeStruct((rows, wide), low),
        jax.ShapeDtypeStruct((2,) + rms.shape, f32),
        jax.ShapeDtypeStruct((rows, w_down.shape[0]), f32),
    ]
    scratch = spread_scratch(1, rows // 2, wide) + [
        pltpu.VMEM((8 * rows, cols), low), dma((4,)),
        pltpu.VMEM((8, LANES), f32), pltpu.VMEM((8, LANES), f32), dma((16,)),
    ] + reduce_scratch(counts, rows, width) + line_scratch(16, (8 * rows, cols), low)
    kernel = functools.partial(attend_kernel, rows, heads, cols, width, counts)
    operands = [qkv, rms, cos, sin, mask, w_out, g_col, w_down]
    out_specs = [vm, pl.BlockSpec(memory_space=pl.ANY)] + [vm] * 5
    return kernel_call(kernel, out_shape, operands, [vm] * 8, scratch, cid, "attend", out_specs, (4, 5, 6, 7), (2, 3, 4))


def tail_kernel(rows, heads, per, d_attn, w_out, queries, kv, probs, rms, cos, sin, act_t, w_qkv, ffn, x_low,
                attn, gain, gain_grad, mixed_all, d_tok, out, grad_query, grad_out, kv_sum, gain_tiles, *refs, late, early):
    here = Place()
    width = HD
    counts = heads // 2
    part = rows // 2
    refs = list(refs)
    line_counts = 8 * per
    cols = d_attn.shape[1]
    extra = cols // (rows // per)

    def take(count):
        taken_refs = refs[:count]
        del refs[:count]
        return taken_refs

    total_refs = take(11)
    spread = Spread(here, 1, take(7))
    d_mixed, tiny_own, tiny_all, d_kv, give, taken, give_sems, tiny_send, tiny_recv = take(9)
    grad, grad_mixed, gain_sum, tile, tile_send, tile_recv, put_sems, local_sems, mixed_two, mixed_sems = take(10)

    def far(at):
        return at // (2 * per), at // per % 2

    def near(at):
        return spread.block(jnp.minimum(at, line_counts - 1))

    def place_ffn(at):
        return here.shard(*far(at)) * per + at % per

    def place_tok(at):
        across, other, half_at = near(at)
        return jnp.where(at < line_counts, here.shard(across, other) * per + half_at, at)

    ffn_sum, leaving = take(2)
    by_chip = chip_place(here, per)
    line = Line(here, line_counts, [ffn, ffn_sum] + take(8), by_chip)
    contrib, summed = take(2)
    line_tok = Line(here, line_counts + extra, [contrib, summed] + take(8), place_tok)
    tiny = Tiny(here, tiny_own, tiny_all, (tiny_send, tiny_recv), False)
    got, core = spread.got, here.core
    product = products(here, d_attn, w_out, True, rows, width, counts)
    total = Reduce(here, counts, product, total_refs)
    greet(here, tiny.peers, True)
    line.begin()
    grad_mixed[...] = jnp.zeros_like(grad_mixed)

    def mixed_copy(step):
        span = pl.ds(pl.multiple_of(step * rows, rows), rows)
        return pltpu.make_async_copy(mixed_all.at[span, :], mixed_two.at[step % 2], mixed_sems.at[step % 2])

    mixed_copy(0).start()

    def beside(step):
        line.step(step)

        @pl.when(step < 8)
        def _():
            span = pl.ds(pl.multiple_of(step * rows, rows), rows)
            mixed_copy(step).wait()

            @pl.when(step < 7)
            def _():
                mixed_copy(step + 1).start()

            grad_mixed[...] += dot_tn(mixed_two[step % 2], d_attn[span, :])

    done = total.run(beside)
    grad_out[...] = grad_mixed[...].astype(grad_out.dtype)
    early[1].start()

    def land(at, first, second):
        for half_at, value in enumerate((first, second)):
            d_mixed[:, pl.ds(pl.multiple_of((half_at * counts + at) * width, width), width)] = value.astype(
                d_mixed.dtype)

    total.end(land)
    half = HD // 2
    scale = 1.0 / math.sqrt(HD)
    depth = w_qkv.shape[0] * 8
    d_kv[...] = jnp.zeros_like(d_kv)
    for copy in late:
        copy.wait()

    def one_head(head, dots):
        span = pl.ds(pl.multiple_of(head * HD, HD), HD)
        query = queries[:, span]
        cot = d_mixed[:, span]
        prob = probs[head]
        d_prob = jnp.concatenate([dot_nt(cot, kv[0, :, HD:]), dot_nt(cot, kv[1, :, HD:])], axis=1)
        delta = jnp.sum(prob * d_prob, axis=-1, keepdims=True)
        d_score = (prob * (d_prob - delta)).astype(jnp.bfloat16)
        prob_low = prob.astype(jnp.bfloat16)
        d_query = (dot_nn(d_score[:, :rows], kv[0, :, :HD]) + dot_nn(d_score[:, rows:], kv[1, :, :HD])) * scale
        for side in range(2):
            keys = slice(side * rows, (side + 1) * rows)
            d_kv[side, :, :HD] += dot_tn(d_score[:, keys], query)
            d_kv[side, :, HD:] += dot_tn(prob_low[:, keys], cot)
        dots = dots + jnp.sum(d_query * query.astype(jnp.float32), axis=-1, keepdims=True)
        lead, trail = d_query[:, :half], d_query[:, half:]
        first = ((lead * cos[0] + trail * sin[0]) * rms[0]).astype(got.dtype)
        second = ((trail * cos[0] - lead * sin[0]) * rms[0]).astype(got.dtype)
        line.step(done + head)
        for rows_at in range(2):
            piece = slice(rows_at * part, (rows_at + 1) * part)
            got[0, core, rows_at, 0, :, pl.ds(pl.multiple_of(head * HD, HD), half)] = first[piece, :]
            got[0, core, rows_at, 0, :, pl.ds(pl.multiple_of(head * HD + half, half), half)] = second[piece, :]

        return dots

    dots = lax.fori_loop(0, heads, one_head, jnp.zeros((rows, 1), jnp.float32))
    eye = diagonal()
    tiny_own[...] = jnp.zeros_like(tiny_own)
    for side in (1, 0):
        d_key, d_value = d_kv[side, :, :HD], d_kv[side, :, HD:]
        own = jnp.sum(d_key * kv[side, :, :HD].astype(jnp.float32) +
                      d_value * kv[side, :, HD:].astype(jnp.float32), axis=-1, keepdims=True)
        if side == 0:
            own = own + dots * (1.0 / scale)
        own = own * (rms[side] * rms[side] * (1.0 / depth))
        to_tile(tiny_own, side * (rows // LANES), own, eye)
        lead, trail = d_key[:, :half], d_key[:, half:]
        parts = [(lead * cos[side] + trail * sin[side]) * rms[side],
                 (trail * cos[side] - lead * sin[side]) * rms[side],
                 d_value[:, :half] * rms[side], d_value[:, half:] * rms[side]]
        for at, value in enumerate(parts):
            if side == 1:
                give[:, at * half : (at + 1) * half] = value.astype(give.dtype)
            else:
                d_kv[0, :, at * half : (at + 1) * half] = value
    given = remote(give, taken, give_sems.at[0], give_sems.at[1], spread.ydev)
    given.start()
    grad[...] = jnp.zeros_like(grad)
    given.wait()
    for rows_at in range(2):
        piece = slice(rows_at * part, (rows_at + 1) * part)
        value = d_kv[0, piece, :] + taken[piece, :].astype(jnp.float32)
        got[0, core, rows_at, 0, :, heads * HD :] = value.astype(got.dtype)
    tiny.begin()
    spread.begin_rows()
    gain_sum[...] = jnp.zeros_like(gain_sum)
    tiny.end()

    def block_of(at):
        across, other, half_at = near(at)
        shard, partner = here.shard(across, other), here.shard((across + 2) % 4, other)
        block = got[across, (core + other) % 2, half_at, 0]
        first = pl.multiple_of(shard * rows + half_at * part, part)
        for tile_at in range(part // LANES):
            row = pl.ds(pl.multiple_of(first + tile_at * LANES, LANES), LANES)
            low_at = half_at * (part // LANES) + tile_at
            kept = rows // LANES + low_at
            dot = from_tile(tiny_all[shard, pl.ds(low_at, 1), :] + tiny_all[partner, pl.ds(kept, 1), :], eye)
            value = dot_nt(block[tile_at * LANES : (tile_at + 1) * LANES, :], w_qkv[...])
            x_rows = x_low[row, :].astype(jnp.float32)
            contrib[row, :] = (value * gain[0:1, :] - x_rows * dot).astype(contrib.dtype)
            gain_sum[...] += jnp.sum(value * x_rows, axis=0, keepdims=True)
        line_tok.launch(at, 1)

        @pl.when(other == 1)
        def _():
            twin = got[across, core, half_at, 0]
            twin_first = pl.multiple_of(here.shard(across, 0) * rows + half_at * part, part)
            rows_t, twin_t = act_t[:, pl.ds(first, part)], act_t[:, pl.ds(twin_first, part)]
            for at_col in range((heads + 2) * HD // 512):
                span = slice(at_col * 512, (at_col + 1) * 512)
                grad[:, span] += dot_nn(rows_t, block[:, span]) + dot_nn(twin_t, twin[:, span])

    me = here.shard(0, 0)
    columns = pl.ds(pl.multiple_of(me * cols, cols), cols)
    chunk = line.chunk

    def landing(which, at):
        sub = at % per if which == 0 else near(at)[2]
        return (out, d_tok)[which].at[pl.ds(pl.multiple_of(sub * chunk, chunk), chunk), columns]

    def leaver(which, at):
        return (leaving, line_tok.from_end)[which].at[at]

    def put(which, at):
        goal = here.device(*(far(at) if which == 0 else near(at)[:2]))
        return remote(leaver(which, at), landing(which, at), put_sems.at[which, 0, at], put_sems.at[which, 1, at],
                      goal)

    def keep(which, at):
        spot = at % per if which == 0 else near(at)[2]
        return pltpu.make_async_copy(leaver(which, at), landing(which, at), local_sems.at[which, spot])

    def emit(which, at):
        if which == 1:
            row = line_tok.rows(at)
            value = d_attn[row, :].astype(jnp.float32) + summed[row, :].astype(jnp.float32)
            line_tok.from_end[at] = value.astype(out.dtype)
            return
        row = pl.ds(pl.multiple_of(place_ffn(at) * chunk, chunk), chunk)

        def leave(source):
            value = x_low[row, :].astype(jnp.float32) + attn[row, :].astype(jnp.float32)
            leaving[at] = (value + source[row, :].astype(jnp.float32)).astype(out.dtype)

        leave(ffn_sum)

    def is_own(which, at):
        return at < per if which == 0 else jnp.logical_and(at < 4, at % 2 == 0)

    def send(which, at):
        own = is_own(which, at)

        @pl.when(own)
        def _():
            keep(which, at).start()

        @pl.when(jnp.logical_not(own))
        def _():
            put(which, at).start()

    def stage_step(step, _):
        spread.receive_rows(step)

        @pl.when(step < line_counts)
        def _():
            block_of(step)

        @pl.when(step < 5)
        def _():
            line.step(done + heads + step)

        @pl.when(step >= 4)
        def _():
            line_tok.step(step - 4)

        @pl.when(step > 0)
        def _():
            send(0, step - 1)

        @pl.when(line.inner == 0)
        def _():
            line.up(step).wait_send()
            line.down(step).wait_recv()

        emit(0, step)

        @pl.when(jnp.logical_and(line.inner == 1, step > 7))
        def _():
            send(1, step - 8)

        @pl.when(jnp.logical_and(line.inner == 1, step > 6))
        def _():
            emit(1, step - 7)
        return 0

    lax.fori_loop(0, line_counts, stage_step, 0)
    for half_at in range(cols // (rows // per)):
        span = pl.ds(line_counts * (rows // per) + half_at * (rows // per), rows // per)
        source = slice(half_at * (rows // per), (half_at + 1) * (rows // per))
        contrib[span, :] = grad[source, heads * HD :].astype(contrib.dtype)
    line_tok.launch(line_counts, extra)
    grad_query[...] = grad[:, : heads * HD].astype(grad_query.dtype)
    early[0].start()
    for at in range(cols // LANES):
        tile[at : at + 1, :] = gain_sum[:, at * LANES : (at + 1) * LANES]
        spot = cols // LANES + at
        tile[spot : spot + 1, :] = gain_grad[:, at * LANES : (at + 1) * LANES]

    def tile_copy(step):
        return remote(tile, gain_tiles.at[here.z], tile_send.at[step], tile_recv.at[step],
                      (here.dp, here.seq, (here.z + step + 1) % 4))

    send(0, line_counts - 1)
    line.drain()
    for step in range(3):
        tile_copy(step).start()
    gain_tiles[here.z] = tile[...]

    @pl.when(line.inner == 1)
    def _():
        start = line_counts - 4

        def both(at, _):
            line_tok.step(at)

            @pl.when(at < line_counts + 4)
            def _():
                send(1, at - 4)

            @pl.when(at < line_counts + 3)
            def _():
                emit(1, at - 3)
            return 0

        lax.fori_loop(start, line_counts + extra + 2, both, 0)

        def drain(at, _):
            line_tok.down(at).wait_send()
            return 0

        lax.fori_loop(0, line_counts + extra, drain, 0)

    @pl.when(line.inner == 0)
    def _():
        def arrive(at, _):
            line_tok.up(at).wait_send()
            line_tok.down(at).wait_recv()

            @pl.when(jnp.logical_and(at > 0, at <= line_counts))
            def _():
                send(1, at - 1)

            @pl.when(at < line_counts)
            def _():
                emit(1, at)
            return 0

        lax.fori_loop(0, line_counts + extra, arrive, 0)

    for half_at in range(extra):
        span = pl.ds((line_counts + half_at) * chunk, chunk)
        kv_sum[half_at * chunk : (half_at + 1) * chunk, :] = summed[span, :]
    for hop in range(3):
        spread.x_copy(hop, 0).wait_send()
        spread.y_copy(hop, 0).wait_send()
    for stage in range(4):
        spread.sib_copy(stage, 0, 0).wait_send()
        spread.sib_copy(stage, 1, 0).wait_send()

    def finish(at, _):
        for which in range(2):
            own = is_own(which, at)

            @pl.when(own)
            def _():
                keep(which, at).wait()

            @pl.when(jnp.logical_not(own))
            def _():
                put(which, at).wait()
        return 0

    lax.fori_loop(0, line_counts, finish, 0)
    for step in range(3):
        tile_copy(step).wait()


def tail(d_attn, w_out, queries, kv, probs, rms, cos, sin, act_t, w_qkv, ffn, x_low, attn, gain, gain_grad,
         mixed_all, cid,
 per=2):
    total, cols = d_attn.shape
    rows = total // 8
    wide = w_out.shape[0]
    heads = wide // HD
    low, f32 = jnp.bfloat16, jnp.float32
    dma = pltpu.SemaphoreType.DMA
    vm = pl.BlockSpec(memory_space=pltpu.VMEM)
    counts = 8 * per
    chunk = rows // per
    extra = cols // chunk
    long = (total + cols, cols)
    out_shape = [
        jax.ShapeDtypeStruct((rows, 8 * cols), low),
        jax.ShapeDtypeStruct((rows, 8 * cols), low),
        jax.ShapeDtypeStruct((cols, wide), low),
        jax.ShapeDtypeStruct(w_out.shape, low),
        jax.ShapeDtypeStruct((cols, 2 * HD), low),
        jax.ShapeDtypeStruct((4, 8, LANES), f32),
    ]
    scratch = reduce_scratch(heads // 2, rows, HD, 2) + spread_scratch(1, rows // 2, wide + 2 * HD)
    scratch += [
        pltpu.VMEM((rows, wide), low),
        pltpu.VMEM((8, LANES), f32),
        pltpu.VMEM((8, 8, LANES), f32),
        pltpu.VMEM((2, rows, 2 * HD), f32),
        pltpu.VMEM((rows, 2 * HD), low),
        pltpu.VMEM((rows, 2 * HD), low),
        dma((2,)), dma((7,)), dma((7,)),
        pltpu.VMEM(w_qkv.shape, f32),
        pltpu.VMEM(w_out.shape, f32),
        pltpu.VMEM((1, cols), f32),
        pltpu.VMEM((8, LANES), f32),
        dma((3,)), dma((3,)), dma((2, 2, counts)), dma((2, per)),
        pltpu.VMEM((2, rows, wide), low), dma((2,)),
        pltpu.VMEM((total, cols), low),
        pltpu.VMEM((counts, chunk, cols), low),
    ] + line_scratch(counts, (total, cols), low)
    scratch += [pltpu.VMEM(long, low), pltpu.VMEM(long, low)] + line_scratch(counts + extra, long, low)
    operands = [d_attn, w_out, queries, kv, probs, rms, cos, sin, act_t, w_qkv, ffn, x_low, attn, gain,
                gain_grad, mixed_all]
    kernel = functools.partial(tail_kernel, rows, heads, per)
    specs = [vm] * (len(operands) - 1) + [pl.BlockSpec(memory_space=pl.ANY)]
    return kernel_call(kernel, out_shape, operands, specs, scratch, cid, "tail",
                       late=(2, 3, 4, 8, 9, 11, 12), early=(2, 3))


LANES = 128


def acts_move(
    tokens, seg_ids, gain_attn, w_query, kv_weight, w_out, gain_ffn, w_gate, w_up, w_down, d_out
):
    small = jnp.stack([gain_attn, gain_ffn, seg_ids.astype(gain_ffn.dtype), gain_attn]).astype(jnp.float32)

    qkv, x_low, act_one_t, w_qkv, rms, cos, sin, mask, g_parts = opening(
        tokens, small, w_query, kv_weight, d_out, 1
    )
    g_low = g_parts.reshape(x_low.shape)
    attn, mixed_all, kv, probs, queries, pair_rms, d_hidden = attend(
        qkv, rms, cos, sin, mask, w_out, g_low, w_down, 2
    )
    hidden, d_gate, d_up, act_two_t, dots = ffn_scatter(x_low, attn, small, w_gate, w_up, d_hidden, 4)
    d_norm, grad_gain_two, grad_gate, grad_up = back_gather(
        act_two_t, w_gate, w_up, d_gate, d_up, dots, x_low, attn, small, 5
    )
    ffn, d_attn, grad_down = down_gather(g_low, w_down, hidden, d_norm, 6)
    d_tokens, out, grad_query, grad_out, grad_kv, gain_tiles = tail(
        d_attn,
        w_out,
        queries,
        kv,
        probs,
        pair_rms,
        cos,
        sin,
        act_one_t,
        w_qkv,
        ffn,
        x_low,
        attn,
        small,
        grad_gain_two,
        mixed_all,
        7,
    )
    gains = jnp.sum(gain_tiles, axis=0).reshape(2, -1)
    wider = jnp.float32
    return (
        out,
        d_tokens.astype(wider),
        gains[0],
        grad_query.astype(wider),
        grad_kv.astype(wider),
        grad_out.astype(wider),
        gains[1],
        grad_gate.astype(wider),
        grad_up.astype(wider),
        grad_down.astype(wider),
    )


def solution(mesh):
    in_specs = (
        P(("dp", "seq"), None),
        P("dp"),
        P(("dp", "seq")),
        P(("dp", "seq"), "tensor"),
        P(("dp", "seq"), None),
        P("tensor", ("dp", "seq")),
        P(("dp", "seq")),
        P(("dp", "seq"), "tensor"),
        P(("dp", "seq"), "tensor"),
        P("tensor", ("dp", "seq")),
        P(("dp", "seq"), None),
    )
    out_specs = (
        P(("dp", "seq"), None),
        P(("dp", "seq"), None),
        P(("dp", "seq")),
        P(("dp", "seq"), "tensor"),
        P(("dp", "seq"), None),
        P("tensor", ("dp", "seq")),
        P(("dp", "seq")),
        P(("dp", "seq"), "tensor"),
        P(("dp", "seq"), "tensor"),
        P("tensor", ("dp", "seq")),
    )

    def shards(*arrays):
        tokens = arrays[0]
        sizes = tuple(mesh.shape[name] for name in ("dp", "seq", "tensor"))
        count = tokens.shape[0] * sizes[0] * sizes[1]
        plan = acts_move if sizes == (4, 2, 4) and count <= tokens.shape[1] else weights_move
        return plan(*arrays)

    return jax.shard_map(shards, mesh=mesh, in_specs=in_specs, out_specs=out_specs, check_vma=False)
```

```python
import functools
import math

import jax
import jax.numpy as jnp
from jax import lax
from jax.experimental import pallas as pl
from jax.experimental.pallas import tpu as pltpu
from jax.sharding import PartitionSpec as P

HD = 256


EPS = 1e-06
NEG = -1e30


def place_tables(segs):
    length = segs.shape[0]
    index = jnp.arange(length, dtype=jnp.int32)
    flags = jnp.concatenate([jnp.ones((1,), dtype=bool), segs[1:] != segs[:-1]])
    starts = lax.cummax(jnp.where(flags, index, jnp.zeros_like(index)), axis=0)
    places = index - starts
    half_size = HD // 2
    freqs = jnp.exp(jnp.arange(half_size, dtype=jnp.float32) * (-math.log(10000.0) / half_size))
    angles = places.astype(jnp.float32)[:, None] * freqs[None, :]
    return (places, jnp.cos(angles), jnp.sin(angles))


def rotate(vector, cos_table, sin_table):
    half_size = vector.shape[-1] // 2
    leading = vector[..., :half_size]
    trailing = vector[..., half_size:]
    return jnp.concatenate(
        [leading * cos_table - trailing * sin_table, trailing * cos_table + leading * sin_table],
        axis=-1,
    )


def rotate_back(vector, cos_table, sin_table):
    half_size = vector.shape[-1] // 2
    leading = vector[..., :half_size]
    trailing = vector[..., half_size:]
    return jnp.concatenate(
        [leading * cos_table + trailing * sin_table, trailing * cos_table - leading * sin_table],
        axis=-1,
    )


def matmul(left, right):
    return jnp.dot(left, right, preferred_element_type=jnp.float32)


def matmul_nt(left, right):
    return lax.dot_general(
        left, right, (((1,), (1,)), ((), ())), preferred_element_type=jnp.float32
    )


def matmul_tn(left, right):
    return lax.dot_general(
        left, right, (((0,), (0,)), ((), ())), preferred_element_type=jnp.float32
    )


def gelu_tanh(values):
    return jax.nn.gelu(values, approximate=True)


def norm_back(d_act, normed, rms_val, gain_val):
    scaled = d_act * gain_val
    return rms_val * (scaled - normed * jnp.mean(scaled * normed, axis=-1, keepdims=True))


def weights_move(
    tokens, seg_ids, gain_attn, w_query, kv_weight, w_out, gain_ffn, w_gate, w_up, w_down, d_out
):
    rows = tokens.shape[0]
    scale_factor = 1.0 / math.sqrt(HD)
    offset = lax.axis_index("seq") * rows
    places, cos_table, sin_table = place_tables(seg_ids)
    own_places = lax.dynamic_slice_in_dim(places, offset, rows, 0)
    own_segs = lax.dynamic_slice_in_dim(seg_ids, offset, rows, 0)
    own_cos = lax.dynamic_slice_in_dim(cos_table, offset, rows, 0)
    own_sin = lax.dynamic_slice_in_dim(sin_table, offset, rows, 0)
    allowed = (own_segs[:, None] == seg_ids[None, :]) & (own_places[:, None] >= places[None, :])
    full_query, full_out, full_kv, full_gain_one = (
        lax.all_gather(w_query, ("dp", "seq"), axis=0, tiled=True),
        lax.all_gather(w_out, ("dp", "seq"), axis=1, tiled=True),
        lax.all_gather(kv_weight, ("dp", "seq"), axis=0, tiled=True),
        lax.all_gather(gain_attn, ("dp", "seq"), axis=0, tiled=True),
    )
    gain_one = full_gain_one.astype(jnp.float32)
    inputs = tokens.astype(jnp.float32)
    rms_one = lax.rsqrt(jnp.mean(inputs * inputs, axis=-1, keepdims=True) + EPS)
    norm_one = inputs * rms_one
    act_one = (norm_one * gain_one).astype(jnp.bfloat16)
    query_pre = matmul(act_one, full_query)
    heads = query_pre.shape[1] // HD
    kv_pre = matmul(act_one, full_kv)
    queries = (
        rotate(query_pre.reshape(rows, heads, HD), own_cos[:, None, :], own_sin[:, None, :])
        * scale_factor
    ).astype(jnp.bfloat16)
    own_kv = jnp.concatenate(
        [rotate(kv_pre[:, :HD], own_cos, own_sin), kv_pre[:, HD:]], axis=1
    ).astype(jnp.bfloat16)
    all_kv = lax.all_gather(own_kv, "seq", axis=0, tiled=True)
    keys = all_kv[:, :HD]
    values_all = all_kv[:, HD:]
    scores = jnp.einsum("rhd,kd->hrk", queries, keys, preferred_element_type=jnp.float32)
    scores = jnp.where(allowed[None], scores, NEG)
    top_score = jnp.max(scores, axis=-1, keepdims=True)
    expd = jnp.exp(scores - top_score)
    total = jnp.sum(expd, axis=-1, keepdims=True)
    log_total = top_score + jnp.log(total)
    probs_low = (expd / total).astype(jnp.bfloat16)
    mixed = (
        jnp.einsum("hrk,kd->rhd", probs_low, values_all, preferred_element_type=jnp.float32)
        .reshape(rows, heads * HD)
        .astype(jnp.bfloat16)
    )
    attn = lax.psum(matmul(mixed, full_out), "tensor")
    resid = inputs + attn
    full_gate, full_up, full_down, full_gain_two = (
        lax.all_gather(w_gate, ("dp", "seq"), axis=0, tiled=True),
        lax.all_gather(w_up, ("dp", "seq"), axis=0, tiled=True),
        lax.all_gather(w_down, ("dp", "seq"), axis=1, tiled=True),
        lax.all_gather(gain_ffn, ("dp", "seq"), axis=0, tiled=True),
    )
    gain_two = full_gain_two.astype(jnp.float32)
    rms_two = lax.rsqrt(jnp.mean(resid * resid, axis=-1, keepdims=True) + EPS)
    norm_two = resid * rms_two
    act_two = (norm_two * gain_two).astype(jnp.bfloat16)
    gate = matmul(act_two, full_gate)
    up_val = matmul(act_two, full_up)
    gelu_val, gelu_pull = jax.vjp(gelu_tanh, gate)
    hidden = (gelu_val * up_val).astype(jnp.bfloat16)
    ffn = lax.psum(matmul(hidden, full_down).astype(jnp.bfloat16), "tensor").astype(jnp.float32)
    out = (resid + ffn).astype(jnp.bfloat16)
    back_gate, back_up, back_down = (
        lax.all_gather(w_gate, ("dp", "seq"), axis=0, tiled=True),
        lax.all_gather(w_up, ("dp", "seq"), axis=0, tiled=True),
        lax.all_gather(w_down, ("dp", "seq"), axis=1, tiled=True),
    )
    d_hidden = matmul_nt(d_out, back_down)
    grad_down = matmul_tn(hidden, d_out)
    d_gate = gelu_pull(d_hidden * up_val)[0].astype(jnp.bfloat16)
    d_up = (d_hidden * gelu_val).astype(jnp.bfloat16)
    grad_gate = matmul_tn(act_two, d_gate)
    grad_up = matmul_tn(act_two, d_up)
    d_act_two = lax.psum(matmul_nt(d_gate, back_gate) + matmul_nt(d_up, back_up), "tensor")
    grad_gain_two = jnp.sum(d_act_two * norm_two, axis=0)
    d_resid = d_out.astype(jnp.float32) + norm_back(d_act_two, norm_two, rms_two, gain_two)
    ffn_grads = (
        lax.psum_scatter(
            grad_gate.astype(jnp.bfloat16), ("dp", "seq"), scatter_dimension=0, tiled=True
        ).astype(jnp.float32),
        lax.psum_scatter(
            grad_up.astype(jnp.bfloat16), ("dp", "seq"), scatter_dimension=0, tiled=True
        ).astype(jnp.float32),
        lax.psum_scatter(
            grad_down.astype(jnp.bfloat16), ("dp", "seq"), scatter_dimension=1, tiled=True
        ).astype(jnp.float32),
        lax.psum_scatter(
            grad_gain_two.astype(jnp.bfloat16), ("dp", "seq"), scatter_dimension=0, tiled=True
        ).astype(jnp.float32),
    )
    back_query, back_out, back_kv = (
        lax.all_gather(w_query, ("dp", "seq"), axis=0, tiled=True),
        lax.all_gather(w_out, ("dp", "seq"), axis=1, tiled=True),
        lax.all_gather(kv_weight, ("dp", "seq"), axis=0, tiled=True),
    )
    d_attn = d_resid.astype(jnp.bfloat16)
    grad_out = matmul_tn(mixed, d_attn)
    d_mixed = matmul_nt(d_attn, back_out).astype(jnp.bfloat16).reshape(rows, heads, HD)
    scores_again = jnp.einsum("rhd,kd->hrk", queries, keys, preferred_element_type=jnp.float32)
    probs = jnp.where(allowed[None], jnp.exp(scores_again - log_total), 0.0)
    d_probs = jnp.einsum("rhd,kd->hrk", d_mixed, values_all, preferred_element_type=jnp.float32)
    delta = jnp.sum(probs * d_probs, axis=-1, keepdims=True)
    d_scores = (probs * (d_probs - delta)).astype(jnp.bfloat16)
    d_queries = (
        jnp.einsum("hrk,kd->rhd", d_scores, keys, preferred_element_type=jnp.float32) * scale_factor
    )
    d_query_pre = (
        rotate_back(d_queries, own_cos[:, None, :], own_sin[:, None, :])
        .reshape(rows, heads * HD)
        .astype(jnp.bfloat16)
    )
    d_keys_part = jnp.einsum("hrk,rhd->kd", d_scores, queries, preferred_element_type=jnp.float32)
    d_values_part = jnp.einsum(
        "hrk,rhd->kd", probs.astype(jnp.bfloat16), d_mixed, preferred_element_type=jnp.float32
    )
    own_kv_grad = lax.psum_scatter(
        jnp.concatenate([d_keys_part, d_values_part], axis=1).astype(jnp.bfloat16),
        "seq",
        scatter_dimension=0,
        tiled=True,
    )
    d_act_query = matmul_nt(d_query_pre, back_query)
    d_act_sum, kv_grad = (
        lax.psum(d_act_query.astype(jnp.bfloat16), "tensor").astype(jnp.float32),
        lax.psum(own_kv_grad, "tensor").astype(jnp.float32),
    )
    d_kv_pre = jnp.concatenate(
        [rotate_back(kv_grad[:, :HD], own_cos, own_sin), kv_grad[:, HD:]], axis=1
    ).astype(jnp.bfloat16)
    d_act_one = d_act_sum + matmul_nt(d_kv_pre, back_kv)
    grad_query = matmul_tn(act_one, d_query_pre)
    grad_kv = matmul_tn(act_one, d_kv_pre)
    grad_gain_one = jnp.sum(d_act_one * norm_one, axis=0)
    d_tokens = d_resid + norm_back(d_act_one, norm_one, rms_one, gain_one)
    attn_grads = (
        lax.psum_scatter(
            grad_query.astype(jnp.bfloat16), ("dp", "seq"), scatter_dimension=0, tiled=True
        ).astype(jnp.float32),
        lax.psum_scatter(
            grad_out.astype(jnp.bfloat16), ("dp", "seq"), scatter_dimension=1, tiled=True
        ).astype(jnp.float32),
        lax.psum_scatter(
            grad_kv.astype(jnp.bfloat16), ("dp", "seq"), scatter_dimension=0, tiled=True
        ).astype(jnp.float32),
        lax.psum_scatter(
            grad_gain_one.astype(jnp.bfloat16), ("dp", "seq"), scatter_dimension=0, tiled=True
        ).astype(jnp.float32),
    )
    return (
        out,
        d_tokens,
        attn_grads[3],
        attn_grads[0],
        attn_grads[2],
        attn_grads[1],
        ffn_grads[3],
        ffn_grads[0],
        ffn_grads[1],
        ffn_grads[2],
    )


MESH = pl.DeviceIdType.MESH
VMEM_LIMIT = 66000 * 1024


class Place:
    def __init__(self):
        self.dp = lax.axis_index("dp")
        self.seq = lax.axis_index("seq")
        self.z = lax.axis_index("tensor")
        self.core = lax.rem(self.dp, 2)
        self.chip = lax.div(self.dp, 2)

    def device(self, across, other):
        chip = (self.chip + across) % 2
        seq = (self.seq + across // 2) % 2
        core = (self.core + other) % 2
        return chip * 2 + core, seq, self.z

    def shard(self, across, other):
        dp, seq, _ = self.device(across, other)
        return dp * 2 + seq


def greet(here, peers, line=False):
    barrier = pltpu.get_barrier_semaphore()
    peers = list(peers)
    if line:
        peers += [(here.dp, here.seq, (here.z + step) % 4) for step in range(1, 4)]
    for peer in peers:
        pl.semaphore_signal(barrier, inc=1, device_id=peer, device_id_type=MESH)
    pl.semaphore_wait(barrier, len(peers))


def remote(src, dst, send, recv, peer):
    return pltpu.make_async_remote_copy(
        src_ref=src, dst_ref=dst, send_sem=send, recv_sem=recv, device_id=peer, device_id_type=MESH
    )


class Line:
    def __init__(self, here, counts, refs, place=None):
        self.own, self.out, self.from_end, self.from_mid = refs[:4]
        self.sems = refs[4:10]
        self.counts = counts
        self.chunk = self.from_mid.shape[1]
        self.fold = self.from_end.shape[1] // self.chunk
        self.place = place
        z = here.z
        self.inner = ((z + 1) // 2) % 2
        self.mate = (here.dp, here.seq, z + 1 - 2 * (z % 2))
        self.other = (here.dp, here.seq, 3 - z)

    def rows(self, at):
        at = at if self.place is None else self.place(at)
        return pl.ds(pl.multiple_of(at * self.chunk, self.chunk), self.chunk)

    def inbox(self, at):
        span = pl.ds(pl.multiple_of(at % self.fold * self.chunk, self.chunk), self.chunk)
        return self.from_end.at[at // self.fold, span, :]

    def up(self, at):
        return remote(self.own.at[self.rows(at), :], self.inbox(at), self.sems[0].at[at],
                      self.sems[1].at[at], self.mate)

    def over(self, at):
        return remote(self.out.at[self.rows(at), :], self.from_mid.at[at], self.sems[2].at[at],
                      self.sems[3].at[at], self.other)

    def down(self, at):
        rows = self.rows(at)
        return remote(self.out.at[rows, :], self.out.at[rows, :], self.sems[4].at[at],
                      self.sems[5].at[at], self.mate)

    def launch(self, first, count):
        @pl.when(self.inner == 0)
        def _():
            def send(at, _):
                self.up(first + at).start()
                return 0

            lax.fori_loop(0, count, send, 0)

    def begin(self):
        self.launch(0, self.counts)

    def first(self, at):
        rows = self.rows(at)
        self.up(at).wait_recv()
        total = self.own[rows, :].astype(jnp.float32) + self.inbox(at)[...].astype(jnp.float32)
        self.out[rows, :] = total.astype(self.out.dtype)
        self.over(at).start()

    def second(self, at):
        rows = self.rows(at)
        self.over(at).wait()
        total = self.out[rows, :].astype(jnp.float32) + self.from_mid[at].astype(jnp.float32)
        self.out[rows, :] = total.astype(self.out.dtype)
        self.down(at).start()

    def step(self, at, start=0, count=None):
        count = self.counts if count is None else count

        @pl.when(jnp.logical_and(self.inner == 1, at < count))
        def _():
            self.first(start + at)

        @pl.when(jnp.logical_and(self.inner == 1, jnp.logical_and(at > 1, at < count + 2)))
        def _():
            self.second(start + at - 2)

    def steps(self, first, last, start=0, count=None):
        def rest(at, _):
            self.step(at, start, count)
            return 0

        lax.fori_loop(first, last, rest, 0)

    def settle(self):
        @pl.when(self.inner == 0)
        def _():
            def take(at, _):
                self.up(at).wait_send()
                self.down(at).wait_recv()
                return 0

            lax.fori_loop(0, self.counts, take, 0)

        self.drain()

    def drain(self):
        @pl.when(self.inner == 1)
        def _():
            def drain(at, _):
                self.down(at).wait_send()
                return 0

            lax.fori_loop(0, self.counts, drain, 0)

    def end(self, done=0):
        self.steps(min(done, self.counts + 2), self.counts + 2)
        self.settle()


def line_scratch(counts, shape, low, fold=1):
    chunk = shape[0] // counts
    inbox = pltpu.VMEM((counts // fold, chunk * fold, shape[1]), low)
    return [inbox, pltpu.VMEM((counts, chunk, shape[1]), low)] + [pltpu.SemaphoreType.DMA((counts,))] * 6


def turned(at):
    return 3 - at // 2, 1 - at % 2


def slice_peers(here):
    return [here.device(*turned(at)) for at in range(7)]


def kernel_call(kernel, out_shape, operands, specs, scratch, cid, name, out_specs=None, late=(), early=()):
    vm = pl.BlockSpec(memory_space=pltpu.VMEM)
    hbm = pl.BlockSpec(memory_space=pl.ANY)
    specs = [hbm if at in late else spec for at, spec in enumerate(specs)]
    out_specs = [hbm if at in early else spec for at, spec in enumerate(out_specs or [vm] * len(out_shape))]
    inside = [pltpu.VMEM(operands[at].shape, operands[at].dtype) for at in late]
    inside += [pltpu.VMEM(out_shape[at].shape, out_shape[at].dtype) for at in early]
    inside.append(pltpu.SemaphoreType.DMA((max(1, len(late) + len(early)),)))
    n_in, n_out = len(operands), len(out_shape)

    def body(*refs):
        ins, outs = list(refs[:n_in]), list(refs[n_in : n_in + n_out])
        rest, own = refs[n_in + n_out : -len(inside)], refs[-len(inside) :]
        loads, stores = [], []
        for spot, at in enumerate(late):
            copy = pltpu.make_async_copy(ins[at], own[spot], own[-1].at[spot])
            copy.start()
            loads.append(copy)
            ins[at] = own[spot]
        for number, at in enumerate(early):
            spot = len(late) + number
            stores.append(pltpu.make_async_copy(own[spot], outs[at], own[-1].at[spot]))
            outs[at] = own[spot]
        more = {}
        if late:
            more["late"] = loads
        if early:
            more["early"] = stores
        kernel(*ins, *outs, *rest, **more)
        for copy in stores:
            copy.wait()

    return pl.pallas_call(
        body,
        out_shape=out_shape,
        in_specs=specs,
        out_specs=out_specs,
        scratch_shapes=scratch + inside,
        compiler_params=pltpu.CompilerParams(
            collective_id=cid, has_side_effects=True, vmem_limit_bytes=VMEM_LIMIT
        ),
        name=f"{name}_{cid}",
    )(*operands)


class Tiny:
    def __init__(self, here, src, dst, sems, spread):
        self.here, self.src, self.dst, self.sems, self.spread = here, src, dst, sems, spread
        self.peers = slice_peers(here)
        self.me = here.shard(0, 0)

    def tile(self, shard):
        return self.src.at[shard] if self.spread else self.src

    def copy(self, at):
        return remote(self.tile(self.here.shard(*turned(at))), self.dst.at[self.me], self.sems[0].at[at],
                      self.sems[1].at[at], self.peers[at])

    def begin(self):
        for at in range(7):
            self.copy(at).start()
        self.dst[self.me] = self.tile(self.me)[...]

    def end(self):
        for at in range(7):
            self.copy(at).wait()


class Reduce:
    def __init__(self, here, counts, product, refs, before=None):
        self.counts, self.product, self.before = counts, product, before
        self.held, self.sib_out, self.sib_in, self.from_x, self.from_y = refs[:5]
        self.sib_sems, self.x_sems, self.y_sems = refs[5:7], refs[7:9], refs[9:11]
        self.sib, self.xdev, self.ydev = here.device(0, 1), here.device(1, 0), here.device(2, 0)
        self.steps = 4 * counts
        self.ring = self.sib_out.shape[0]

    def streams(self, stage):
        far = stage // 3
        x_chip = jnp.where(stage == 0, 3, jnp.where(stage == 2, 0, 1))
        y_chip = jnp.where(stage == 0, 3, jnp.where(stage == 2, 0, 2))
        return (x_chip, far), (y_chip, 1 - far)

    def to_sib(self, step, stream):
        stage, at = step // self.counts, step % self.counts
        return remote(self.sib_out.at[step % self.ring, stream], self.sib_in.at[stage, stream, at],
                      self.sib_sems[0].at[stage, stream, at], self.sib_sems[1].at[stage, stream, at], self.sib)

    def to_x(self, hop, at, stage=0):
        return remote(self.held.at[stage, 0, at], self.from_x.at[hop, at], self.x_sems[0].at[hop, at],
                      self.x_sems[1].at[hop, at], self.xdev)

    def to_y(self, hop, at, stage=0):
        return remote(self.held.at[stage, 1, at], self.from_y.at[hop, at], self.y_sems[0].at[hop, at],
                      self.y_sems[1].at[hop, at], self.ydev)

    def compute(self, step):
        stage, at = step // self.counts, step % self.counts
        if self.before:
            for stop in range(3):
                @pl.when(step == stop * self.counts)
                def _():
                    self.before(stop)

        @pl.when(step >= self.ring)
        def _():
            for stream in range(2):
                self.to_sib(step - self.ring, stream).wait_send()

        for stream, (across, half) in enumerate(self.streams(stage)):
            self.sib_out[step % self.ring, stream] = self.product(across, 1, half, at).astype(jnp.bfloat16)
            self.held[stage, stream, at] = self.product(across, 0, half, at).astype(jnp.bfloat16)
        for stream in range(2):
            self.to_sib(step, stream).start()

    def finish(self, step):
        stage, at = step // self.counts, step % self.counts
        for stream in range(2):
            self.to_sib(step, stream).wait_recv()

        def total(stream):
            return self.held[stage, stream, at].astype(jnp.float32) + self.sib_in[stage, stream, at].astype(
                jnp.float32)

        @pl.when(stage < 3)
        def _():
            for stream in range(2):
                self.held[stage, stream, at] = total(stream).astype(jnp.bfloat16)

        @pl.when(stage == 3)
        def _():
            self.to_y(0, at).wait_recv()
            self.held[3, 0, at] = (total(0) + self.from_y[0, at].astype(jnp.float32)).astype(jnp.bfloat16)
            self.to_x(0, at).wait_recv()
            self.held[3, 1, at] = (total(1) + self.from_x[0, at].astype(jnp.float32)).astype(jnp.bfloat16)

        @pl.when(stage != 2)
        def _():
            hop = stage - stage // 3
            self.to_x(hop, at, stage).start()
            self.to_y(hop, at, stage).start()

    def advance(self, step):
        @pl.when(step < self.steps)
        def _():
            self.compute(step)

        @pl.when(jnp.logical_and(step > 0, step <= self.steps))
        def _():
            self.finish(step - 1)

    def run(self, hook=None):
        def body(step, _):
            self.advance(step)

            if hook:
                hook(step)
            return 0

        lax.fori_loop(0, self.steps + 1, body, 0)
        return self.steps + 1

    def end(self, emit):
        def last(at, _):
            values = []
            for half in range(2):
                xs, ys = (1, 2) if half == 0 else (2, 1)
                self.to_x(xs, at).wait_recv()
                self.to_y(ys, at).wait_recv()
                values.append(self.held[2, half, at].astype(jnp.float32) + self.from_x[xs, at].astype(jnp.float32)
                              + self.from_y[ys, at].astype(jnp.float32))
            emit(at, *values)
            for hop in range(3):
                self.to_x(hop, at).wait_send()
                self.to_y(hop, at).wait_send()
            return 0

        lax.fori_loop(0, self.counts, last, 0)

        def drain(at, _):
            for stream in range(2):
                self.to_sib(self.steps - self.ring + at, stream).wait_send()
            return 0

        lax.fori_loop(0, self.ring, drain, 0)


def reduce_scratch(counts, rows, width, ring=4):
    low, dma = jnp.bfloat16, pltpu.SemaphoreType.DMA
    block = pltpu.VMEM((4, 2, counts, rows, width), low)
    landed = pltpu.VMEM((3, counts, rows, width), low)
    sent = pltpu.VMEM((ring, 2, rows, width), low)
    return [block, sent, block, landed, landed] + [dma((4, 2, counts))] * 2 + [dma((3, counts))] * 4


class Spread:
    def __init__(self, here, counts, refs):
        self.counts = counts
        self.got = refs[0]
        self.x_sems, self.y_sems, self.sib_sems = refs[1:3], refs[3:5], refs[5:7]
        self.core = here.core
        self.sib, self.xdev, self.ydev = here.device(0, 1), here.device(1, 0), here.device(2, 0)

    def slot(self, across, half, at):
        return self.got.at[across, self.core, half, at]

    def x_copy(self, hop, at):
        half = jnp.minimum(hop, 1)
        src = self.slot(2 * (hop // 2), half, at)
        dst = self.slot(1 + 2 * (hop // 2), half, at)
        return remote(src, dst, self.x_sems[0].at[hop, at], self.x_sems[1].at[hop, at], self.xdev)

    def y_copy(self, hop, at):
        half = 1 - jnp.minimum(hop, 1)
        src = self.slot(hop // 2, half, at)
        dst = self.slot(2 + hop // 2, half, at)
        return remote(src, dst, self.y_sems[0].at[hop, at], self.y_sems[1].at[hop, at], self.ydev)

    def streams(self, stage):
        some, last, late = jnp.minimum(stage, 1), stage // 3, stage // 2
        return (some + 2 * last, late), (2 * some + last, 1 - late)

    def block(self, at):
        x_stream, y_stream = self.streams(at // 4)
        second = at // 2 % 2
        across = x_stream[0] + second * (y_stream[0] - x_stream[0])
        half = x_stream[1] + second * (y_stream[1] - x_stream[1])
        return across, at % 2, half

    def begin_rows(self):
        for hop in range(2):
            self.x_copy(hop, 0).start()
            self.y_copy(hop, 0).start()
        for stream in range(2):
            self.sib_copy(0, stream, 0).start()

    def receive_rows(self, step):
        stage = step // 4

        @pl.when(jnp.logical_and(step % 4 == 0, jnp.logical_and(stage > 0, stage < 4)))
        def _():
            self.x_copy(stage - 1, 0).wait_recv()
            self.sib_copy(stage, 0, 0).start()
            self.y_copy(stage - 1, 0).wait_recv()
            self.sib_copy(stage, 1, 0).start()

        @pl.when(step == 4)
        def _():
            self.x_copy(2, 0).start()
            self.y_copy(2, 0).start()

        for stream in range(2):
            @pl.when(jnp.logical_and(step % 4 == 2 * stream, step < 16))
            def _(stream=stream):
                self.sib_copy(stage, stream, 0).wait_recv()

    def sib_copy(self, stage, stream, at):
        across, half = self.streams(stage)[stream]
        slot = self.slot(across, half, at)
        spot = (stage, stream, at)
        return remote(slot, slot, self.sib_sems[0].at[spot], self.sib_sems[1].at[spot], self.sib)

    def begin(self):
        def first(at, _):
            self.x_copy(0, at).start()
            self.y_copy(0, at).start()
            return 0

        def own(at, _):
            self.sib_copy(0, 0, at).start()
            self.sib_copy(0, 1, at).start()
            return 0

        lax.fori_loop(0, self.counts, first, 0)
        lax.fori_loop(0, self.counts, own, 0)

    def run(self, blocks, hook=None, done=None):
        counts = self.counts

        def body(step, _):
            stage, at = step // counts, step % counts

            @pl.when(jnp.logical_and(stage > 0, stage < 4))
            def _():
                self.x_copy(stage - 1, at).wait_recv()
                self.sib_copy(stage, 0, at).start()
                self.y_copy(stage - 1, at).wait_recv()
                self.sib_copy(stage, 1, at).start()

            @pl.when(jnp.logical_and(stage > 0, stage < 3))
            def _():
                self.x_copy(stage, at).start()
                self.y_copy(stage, at).start()

            @pl.when(step > 0)
            def _():
                old, spot = (step - 1) // counts, (step - 1) % counts
                for stream, (across, half) in enumerate(self.streams(old)):
                    self.sib_copy(old, stream, spot).wait_recv()
                    blocks(across, half, spot)
                if done:
                    done(old, spot)

            if hook:
                hook(step)
            return 0

        lax.fori_loop(0, 4 * counts + 1, body, 0)
        return 4 * counts + 1

    def end(self):
        def drain(at, _):
            for hop in range(3):
                self.x_copy(hop, at).wait_send()
                self.y_copy(hop, at).wait_send()
            for stage in range(4):
                self.sib_copy(stage, 0, at).wait_send()
                self.sib_copy(stage, 1, at).wait_send()
            return 0

        lax.fori_loop(0, self.counts, drain, 0)


def spread_scratch(counts, rows, width):
    dma = pltpu.SemaphoreType.DMA
    return [pltpu.VMEM((4, 2, 2, counts, rows, width), jnp.bfloat16)] + [dma((3, counts))] * 4 + [
        dma((4, 2, counts))] * 2


def row_span(here, across, other, rows):
    return pl.ds(pl.multiple_of(here.shard(across, other) * rows, rows), rows)


def dot_nt(left, right):
    return lax.dot_general(left, right, (((1,), (1,)), ((), ())), preferred_element_type=jnp.float32)


def dot_tn(left, right):
    return lax.dot_general(left, right, (((0,), (0,)), ((), ())), preferred_element_type=jnp.float32)


def dot_nn(left, right):
    return jnp.dot(left, right, preferred_element_type=jnp.float32)


def products(here, act, weight, nt, rows, width, counts):
    def product(across, other, half, at):
        cols = pl.ds(pl.multiple_of((half * counts + at) * width, width), width)
        block = act[row_span(here, across, other, rows), :]
        return dot_nt(block, weight[cols, :]) if nt else dot_nn(block, weight[:, cols])

    return product


def diagonal():
    return (lax.broadcasted_iota(jnp.int32, (LANES, LANES), 0) ==
            lax.broadcasted_iota(jnp.int32, (LANES, LANES), 1)).astype(jnp.float32)


def to_tile(tile, first, column, eye):
    for at in range(column.shape[0] // LANES):
        spread = column[at * LANES : (at + 1) * LANES, :] * eye
        tile[first + at : first + at + 1, :] = jnp.sum(spread, axis=0, keepdims=True)


def from_tile(row, eye):
    return jnp.sum(eye * row, axis=1, keepdims=True)


def make_tables(here, rows, segs, cos, sin, mask):
    eye = diagonal()
    tiles = rows // LANES
    freqs = jnp.exp(lax.broadcasted_iota(jnp.int32, (1, LANES), 1).astype(jnp.float32) * (-math.log(10000.0) / LANES))
    lane = lax.broadcasted_iota(jnp.int32, (1, LANES), 1)
    line = lax.broadcasted_iota(jnp.int32, (LANES, 1), 0)

    def ids_of(row):
        return segs[2:3, pl.ds(pl.multiple_of(row * LANES, LANES), LANES)]

    def row_of(side, at):
        return ((here.seq + side) % 2) * tiles + at

    for side in range(2):
        for at in range(tiles):
            row = row_of(side, at)
            ids = from_tile(ids_of(row), eye)
            before = jnp.zeros((LANES, 1), jnp.float32)
            for other in range(2 * tiles):
                smaller = ids_of(other) < ids
                before += jnp.sum(smaller.astype(jnp.float32), axis=-1, keepdims=True)
            index = row * LANES + line
            angles = (index.astype(jnp.float32) - before) * freqs
            span = slice(at * LANES, (at + 1) * LANES)
            cos[side, span, :] = jnp.cos(angles)
            sin[side, span, :] = jnp.sin(angles)
            if side == 0:
                for key_side in range(2):
                    for key_at in range(tiles):
                        key_row = row_of(key_side, key_at)
                        same = ids_of(key_row) == ids
                        allowed = jnp.logical_and(same, key_row * LANES + lane <= index)
                        first = key_side * rows + key_at * LANES
                        mask[span, first : first + LANES] = allowed.astype(jnp.float32)


def open_kernel(rows, width, counts, tokens, gain_one, gain_two, ids, w_query, kv_weight, cot, qkv, x_low, act_t, w_qkv, rms, cos, sin,
                mask, g_col, gain, *refs, early):
    here = Place()
    gain[...] = jnp.zeros_like(gain)
    gain[0:1, :] = gain_one[...].astype(jnp.float32).reshape(1, -1)
    gain[1:2, :] = gain_two[...].astype(jnp.float32).reshape(1, -1)
    gain[2:3, :] = ids[...].astype(jnp.float32).reshape(1, -1)
    early[7].start()
    cols, segs = gain.shape[1], gain
    act, turn_send, turn_recv, local_sems, cot_part, g_send, g_recv, z_send, z_recv = refs[:9]
    share = rows // 4
    me = here.shard(0, 0)
    own_rows = pl.ds(pl.multiple_of(me * rows, rows), rows)

    def turn_copy(at):
        across, other = turned(at)
        first = pl.multiple_of(here.shard(across, other) * cols, cols)
        return remote(tokens.at[:, pl.ds(first, cols)], x_low.at[own_rows, :], turn_send.at[at], turn_recv.at[at],
                      here.device(across, other))

    wide = w_query.shape[1]
    local = [
        pltpu.make_async_copy(w_query, w_qkv.at[:, :wide], local_sems.at[0]),
        pltpu.make_async_copy(kv_weight, w_qkv.at[:, wide:], local_sems.at[1]),
        pltpu.make_async_copy(tokens.at[:, pl.ds(pl.multiple_of(me * cols, cols), cols)], x_low.at[own_rows, :],
                              local_sems.at[2]),
    ]
    load = pltpu.make_async_copy(cot.at[pl.ds(pl.multiple_of(here.z * share, share), share), :], cot_part,
                                 local_sems.at[3])
    load.start()
    for copy in local:
        copy.start()

    def g_copy(at):
        across, other = turned(at)
        first = pl.multiple_of(here.shard(across, other) * cols, cols)
        return remote(cot_part.at[:, pl.ds(first, cols)], g_col.at[me, here.z], g_send.at[at], g_recv.at[at],
                      here.device(across, other))

    def own_part():
        return pltpu.make_async_copy(cot_part.at[:, pl.ds(pl.multiple_of(me * cols, cols), cols)],
                                     g_col.at[me, here.z], local_sems.at[4])

    def quarter(way, at, step, peer):
        spot = g_col.at[:, at]
        return remote(spot, spot, z_send.at[way, step], z_recv.at[way, step], (here.dp, here.seq, here.z + peer))

    def pass_on(step):
        @pl.when(jnp.logical_and(here.z < 3, here.z >= step))
        def _():
            quarter(0, here.z - step, step, 1).start()

        @pl.when(jnp.logical_and(here.z > 0, here.z <= 3 - step))
        def _():
            quarter(1, here.z + step, step, -1).start()

    def take_quarters(step):
        @pl.when(here.z > step)
        def _():
            quarter(0, here.z - 1 - step, step, -1).wait_recv()

        @pl.when(here.z < 3 - step)
        def _():
            quarter(1, here.z + 1 + step, step, 1).wait_recv()

    greet(here, slice_peers(here), True)
    load.wait()
    own_part().start()
    for at in range(7):
        g_copy(at).start()
    for at in range(7):
        turn_copy(at).start()
    for copy in local:
        copy.wait()
    early[2].start()

    def squares(at, total):
        values = tokens[:, pl.ds(pl.multiple_of(at * cols, cols), cols)].astype(jnp.float32)
        return total + jnp.sum(values * values, axis=-1, keepdims=True)

    total = lax.fori_loop(0, 8, squares, jnp.zeros((rows, 1), jnp.float32))
    rms[...] = jnp.broadcast_to(lax.rsqrt(total / (8 * cols) + EPS), rms.shape)
    make_tables(here, rows, segs, cos, sin, mask)
    for at in (3, 4, 5):
        early[at].start()

    def prepare(first, count):
        def one(step, _):
            at = first + step
            span = row_span(here, *turned(at), rows)
            value = (x_low[span, :].astype(jnp.float32) * gain[0:1, :]).astype(act.dtype)
            act[span, :] = value
            return 0

        lax.fori_loop(0, count, one, 0)

    def before(stop):
        first, count = ((0, 2), (2, 4), (6, 2))[stop]
        if stop == 0:
            own_part().wait()
            for at in range(7):
                g_copy(at).wait_recv()
        else:
            take_quarters(stop - 1)
        pass_on(stop)
        for at in range(first, min(first + count, 7)):
            turn_copy(at).wait_recv()
        prepare(first, count)
        if stop == 2:
            early[0].start()

    def flip():
        def one(shard, _):
            span = pl.ds(pl.multiple_of(shard * rows, rows), rows)
            act_t[:, span] = act[span, :].T
            return 0

        lax.fori_loop(0, 8, one, 0)

    product = products(here, act, w_qkv, False, rows, width, counts)
    total = Reduce(here, counts, product, refs[9:20], before)
    total.run()
    flip()
    early[1].start()

    def emit(at, first, second):
        for half, value in enumerate((first, second)):
            qkv[:, pl.ds(pl.multiple_of((half * counts + at) * width, width), width)] = value

    total.end(emit)
    take_quarters(2)
    early[6].start()
    for at in range(7):
        turn_copy(at).wait_send()
        g_copy(at).wait_send()
    for step in range(3):
        @pl.when(jnp.logical_and(here.z < 3, here.z >= step))
        def _(step=step):
            quarter(0, here.z - step, step, 1).wait_send()

        @pl.when(jnp.logical_and(here.z > 0, here.z <= 3 - step))
        def _(step=step):
            quarter(1, here.z + step, step, -1).wait_send()


def opening(tokens, gain_one, gain_two, ids, w_query, kv_weight, cot, cid, width=256):
    rows = tokens.shape[0]
    cols, wide = w_query.shape
    every = wide + kv_weight.shape[1]
    counts = every // (2 * width)
    low, f32 = jnp.bfloat16, jnp.float32
    dma = pltpu.SemaphoreType.DMA
    vm = pl.BlockSpec(memory_space=pltpu.VMEM)
    hbm = pl.BlockSpec(memory_space=pl.ANY)
    out_shape = [
        jax.ShapeDtypeStruct((rows, every), f32),
        jax.ShapeDtypeStruct((8 * rows, cols), low),
        jax.ShapeDtypeStruct((cols, 8 * rows), low),
        jax.ShapeDtypeStruct((cols, every), low),
        jax.ShapeDtypeStruct((rows, LANES), f32),
        jax.ShapeDtypeStruct((2, rows, LANES), f32),
        jax.ShapeDtypeStruct((2, rows, LANES), f32),
        jax.ShapeDtypeStruct((rows, 2 * rows), f32),
        jax.ShapeDtypeStruct((8, 4, rows // 4, cols), low),
        jax.ShapeDtypeStruct((8, cols), f32),
    ]
    scratch = [
        pltpu.VMEM((8 * rows, cols), low), dma((7,)), dma((7,)), dma((5,)),
        pltpu.VMEM((rows // 4, 8 * cols), low), dma((7,)), dma((7,)), dma((2, 3)), dma((2, 3)),
    ]
    scratch += reduce_scratch(counts, rows, width)
    kernel = functools.partial(open_kernel, rows, width, counts)
    return kernel_call(kernel, out_shape, [tokens, gain_one, gain_two, ids, w_query, kv_weight, cot],
                       [vm, vm, vm, vm, hbm, hbm, hbm], scratch, cid, "open",
                       early=(1, 2, 3, 5, 6, 7, 8, 9))


def ffn_kernel(rows, width, counts, x_low, attn, gain, w_gate, w_up, d_hidden, hidden, d_gate, d_up, act_t, tile_out,
               *refs, late, early):
    here = Place()
    cols = gain.shape[1]
    act, weight, tiny_own, tiny_all, tiny_send, tiny_recv, dots, local_sems = refs[:8]
    tiny = Tiny(here, tiny_own, tiny_all, (tiny_send, tiny_recv), True)
    half_cols = counts * width
    local = [
        pltpu.make_async_copy(w_gate, weight.at[:, :half_cols], local_sems.at[0]),
        pltpu.make_async_copy(w_up, weight.at[:, half_cols:], local_sems.at[1]),
    ]
    for copy in local:
        copy.start()
    eye = diagonal()
    tiny_own[...] = jnp.zeros_like(tiny_own)

    def prepare(number, _):
        shard = here.shard(*turned(number))
        for at in range(rows // LANES):
            span = pl.ds(pl.multiple_of(shard * rows + at * LANES, LANES), LANES)
            resid = x_low[span, :].astype(jnp.float32) + attn[span, :].astype(jnp.float32)
            act[span, :] = (resid * gain[1:2, :]).astype(act.dtype)
            square = jnp.sum(resid * resid, axis=-1, keepdims=True)
            tiny_own[shard, at : at + 1, :] = jnp.sum(square * eye, axis=0, keepdims=True)
        return 0

    def before(stop):
        if stop == 1:
            lax.fori_loop(2, 6, prepare, 0)
        if stop == 2:
            lax.fori_loop(6, 8, prepare, 0)
            tiny.begin()

    lax.fori_loop(0, 2, prepare, 0)
    greet(here, slice_peers(here))
    for copy in local:
        copy.wait()
    product = products(here, act, weight, False, rows, width, counts)
    total = Reduce(here, counts, product, refs[8:19], before)
    total.run()

    def flip(shard, _):
        span = pl.ds(pl.multiple_of(shard * rows, rows), rows)
        act_t[:, span] = act[span, :].T
        return 0

    lax.fori_loop(0, 8, flip, 0)
    early[0].start()
    tiny.end()
    tiles = rows // LANES
    mean = [from_tile(jnp.sum(tiny_all[:, at, :], axis=0, keepdims=True), eye) for at in range(tiles)]
    scale = lax.rsqrt(jnp.concatenate(mean, axis=0) / (8 * cols) + EPS)
    dots[...] = jnp.zeros_like(dots)
    late[0].wait()
    coeff = math.sqrt(2.0 / math.pi)

    def emit(at, first, second):
        span = pl.ds(pl.multiple_of(at * width, width), width)
        gate, up = first * scale, second * scale
        inner = jnp.tanh(coeff * (gate + 0.044715 * (gate * gate * gate)))
        gelu = 0.5 * gate * (1.0 + inner)
        slope = 0.5 * (1.0 + inner) + 0.5 * gate * (1.0 - inner * inner) * (
            coeff * (1.0 + 3.0 * 0.044715 * gate * gate))
        cot = d_hidden[:, span]
        hidden[:, span] = (gelu * up).astype(hidden.dtype)
        back_gate, back_up = cot * up * slope, cot * gelu
        d_gate[:, span] = (back_gate * scale).astype(d_gate.dtype)
        d_up[:, span] = (back_up * scale).astype(d_up.dtype)
        dots[...] += jnp.sum(back_gate * gate + back_up * up, axis=-1, keepdims=True)

    total.end(emit)
    tile_out[...] = jnp.zeros_like(tile_out)
    to_tile(tile_out, 0, dots[...] * (scale * scale * (1.0 / (8 * cols))), eye)


def ffn_scatter(x_low, attn, gain, w_gate, w_up, d_hidden, cid, width=512):
    rows, half = d_hidden.shape
    cols = gain.shape[1]
    counts = half // width
    low, f32 = jnp.bfloat16, jnp.float32
    dma = pltpu.SemaphoreType.DMA
    vm = pl.BlockSpec(memory_space=pltpu.VMEM)
    hbm = pl.BlockSpec(memory_space=pl.ANY)
    out_shape = [jax.ShapeDtypeStruct((rows, half), low)] * 3 + [
        jax.ShapeDtypeStruct((cols, 8 * rows), low),
        jax.ShapeDtypeStruct((8, LANES), f32),
    ]
    scratch = [
        pltpu.VMEM((8 * rows, cols), low),
        pltpu.VMEM((cols, 2 * half), low),
        pltpu.VMEM((8, 8, LANES), f32),
        pltpu.VMEM((8, 8, LANES), f32),
        dma((7,)), dma((7,)),
        pltpu.VMEM((rows, 1), f32),
        dma((2,)),
    ] + reduce_scratch(counts, rows, width)
    kernel = functools.partial(ffn_kernel, rows, width, counts)
    return kernel_call(kernel, out_shape, [x_low, attn, gain, w_gate, w_up, d_hidden], [vm, vm, vm, hbm, hbm, vm],
                       scratch, cid, "ffn", late=(5,), early=(3,))


def load_own(spread, payload, width, counts, sems):
    copies = []
    for half in range(2):
        for at in range(counts):
            first = at * width + (half * counts * width if len(payload) == 1 else 0)
            src = payload[half % len(payload)].at[:, first : first + width]
            copies.append(pltpu.make_async_copy(src, spread.slot(0, half, at), sems.at[half, at]))
    return copies


def chip_place(here, per):
    def place(at):
        return here.shard(at // (2 * per), at // per % 2) * per + at % per

    return place


def back_kernel(rows, width, counts, act_t, w_gate, w_up, d_gate, d_up, dots, x_low, attn, gain, d_norm, gain_grad,
                grad_gate, grad_up, *refs, late):
    here = Place()
    spread = Spread(here, counts, refs[:7])
    tiny_all, tiny_send, tiny_recv, own_sems, weight, sums, grads, staged, local_sems, out_sems = refs[7:17]
    contrib, rest, rest_sems = refs[17:20]
    line = Line(here, 4, [contrib, d_norm] + list(refs[20:]), chip_place(here, 2))
    tiny = Tiny(here, dots, tiny_all, (tiny_send, tiny_recv), False)
    half_cols = counts * width
    local = [
        pltpu.make_async_copy(w_gate, weight.at[:, :half_cols], local_sems.at[0]),
        pltpu.make_async_copy(w_up, weight.at[:, half_cols:], local_sems.at[1]),
    ]
    own = load_own(spread, (d_gate, d_up), width, counts, own_sems)
    for copy in own + local:
        copy.start()
    greet(here, tiny.peers, True)
    for copy in own:
        copy.wait()
    tiny.begin()
    spread.begin()
    sums[...] = jnp.zeros_like(sums)
    for copy in local + late:
        copy.wait()

    def columns(half, at):
        return pl.ds(pl.multiple_of((half * counts + at) * width, width), width)

    def clear(at, _):
        grads[:, columns(0, at)] = jnp.zeros((grads.shape[0], width), jnp.float32)
        return 0

    lax.fori_loop(0, 2 * counts, clear, 0)

    def blocks(across, half, at):
        cols = columns(half, at)
        gained = grads[:, cols]
        for other in range(2):
            row = row_span(here, across, other, rows)
            block = spread.got[across, (spread.core + other) % 2, half, at]
            sums[row, :] += dot_nt(block, weight[:, cols])
            gained = gained + dot_nn(act_t[:, row], block)
        grads[:, cols] = gained

    def leave(half, at):
        spot = pl.ds(pl.multiple_of(at * width, width), width)
        return pltpu.make_async_copy(staged.at[half], (grad_gate, grad_up)[half].at[:, spot],
                                     out_sems.at[half, at])

    eye = diagonal()
    gain_grad[...] = jnp.zeros_like(gain_grad)

    def close_chip(chip, target):
        def close_shard(other, _):
            shard = here.shard(chip, other)
            span = pl.ds(pl.multiple_of(shard * rows, rows), rows)
            loads = [pltpu.make_async_copy(src.at[span, :], rest.at[at], rest_sems.at[at])
                     for at, src in enumerate((x_low, attn))]
            for copy in loads:
                copy.start()
            for copy in loads:
                copy.wait()
            for at in range(rows // LANES):
                span = pl.ds(pl.multiple_of(shard * rows + at * LANES, LANES), LANES)
                piece = slice(at * LANES, (at + 1) * LANES)
                dot = from_tile(tiny_all[shard, at : at + 1, :], eye)
                resid = rest[0, piece, :].astype(jnp.float32) + rest[1, piece, :].astype(jnp.float32)
                value = sums[span, :]
                target[span, :] = (value * gain[1:2, :] - resid * dot).astype(target.dtype)
                gain_grad[...] += jnp.sum(value * resid, axis=0, keepdims=True)
            return 0

        lax.fori_loop(0, 2, close_shard, 0)

    def done(stage, at):
        @pl.when(jnp.logical_and(stage == 3, at > 0))
        def _():
            leave(0, at - 1).wait()
            leave(1, at - 1).wait()

        @pl.when(stage == 3)
        def _():
            for half in range(2):
                staged[half] = grads[:, columns(half, at)].astype(staged.dtype)
            leave(0, at).start()
            leave(1, at).start()

        @pl.when(jnp.logical_and(at == counts - 1, stage == 0))
        def _():
            close_chip(0, contrib)
            line.launch(0, 4)

        @pl.when(jnp.logical_and(at == counts - 1, stage == 2))
        def _():
            lax.fori_loop(1, 3, lambda chip, _: (close_chip(chip, d_norm), 0)[1], 0)

    def hook(step):
        @pl.when(jnp.logical_and(step >= counts, step < counts + 6))
        def _():
            line.step(step - counts)

    tiny.end()
    spread.run(blocks, hook, done)
    close_chip(3, d_norm)
    line.settle()
    spread.end()

    def drain(at, _):
        leave(0, at).wait()
        leave(1, at).wait()
        return 0

    lax.fori_loop(counts - 1, counts, drain, 0)


def back_gather(act_t, w_gate, w_up, d_gate, d_up, dots, x_low, attn, gain, cid, width=512):
    cols, total = act_t.shape
    rows, half = d_gate.shape
    counts = half // width
    low, f32 = jnp.bfloat16, jnp.float32
    dma = pltpu.SemaphoreType.DMA
    vm = pl.BlockSpec(memory_space=pltpu.VMEM)
    hbm = pl.BlockSpec(memory_space=pl.ANY)
    out_shape = [
        jax.ShapeDtypeStruct((total, cols), low),
        jax.ShapeDtypeStruct((1, cols), f32),
        jax.ShapeDtypeStruct((cols, half), low),
        jax.ShapeDtypeStruct((cols, half), low),
    ]
    scratch = spread_scratch(counts, rows, width) + [
        pltpu.VMEM((8, 8, LANES), f32), dma((7,)), dma((7,)), dma((2, counts)),
        pltpu.VMEM((cols, 2 * half), low),
        pltpu.VMEM((total, cols), f32),
        pltpu.VMEM((cols, 2 * half), f32),
        pltpu.VMEM((2, cols, width), low),
        dma((2,)), dma((2, counts)),
        pltpu.VMEM((total, cols), low),
        pltpu.VMEM((2, rows, cols), low),
        dma((2,)),
    ] + line_scratch(4, (4 * rows // 2, cols), low)
    operands = [act_t, w_gate, w_up, d_gate, d_up, dots, x_low, attn, gain]
    kernel = functools.partial(back_kernel, rows, width, counts)
    return kernel_call(kernel, out_shape, operands, [vm] + [hbm] * 4 + [vm, hbm, hbm, vm], scratch, cid, "back",
                       [vm, vm, hbm, hbm], (0,))


def down_kernel(rows, width, counts, cot, weight, hidden, d_norm, ffn, d_attn, grad, *refs, late):
    here = Place()
    spread = Spread(here, counts, refs[:7])
    own_sems, sums, grads, staged, out_sems, norm_out = refs[7:13]
    place = chip_place(here, 2)
    norm_line = Line(here, 12, [d_norm, norm_out] + list(refs[13:]), lambda at: place(at + 4))
    own = load_own(spread, (hidden,), width, counts, own_sems)
    for copy in own:
        copy.start()
    greet(here, slice_peers(here), True)
    norm_line.begin()
    for copy in own:
        copy.wait()
    spread.begin()
    sums[...] = jnp.zeros_like(sums)
    grads[...] = jnp.zeros_like(grads)
    for copy in late:
        copy.wait()

    def columns(half, at):
        return pl.ds(pl.multiple_of((half * counts + at) * width, width), width)

    def blocks(across, half, at):
        cols = columns(half, at)
        gained = grads[cols, :]
        for other in range(2):
            row = row_span(here, across, other, rows)
            block = spread.got[across, (spread.core + other) % 2, half, at]
            sums[row, :] += dot_nn(block, weight[cols, :])
            gained = gained + dot_tn(block, cot[row, :])
        grads[cols, :] = gained

    def leave(half, at):
        return pltpu.make_async_copy(staged.at[at % 2, half], grad.at[columns(half, at), :], out_sems.at[half, at])

    def done(stage, at):
        @pl.when(jnp.logical_and(stage == 3, at > 1))
        def _():
            leave(0, at - 2).wait()
            leave(1, at - 2).wait()

        @pl.when(stage == 3)
        def _():
            for half in range(2):
                staged[at % 2, half] = grads[columns(half, at), :].astype(staged.dtype)
            leave(0, at).start()
            leave(1, at).start()


    def hook(step):
        @pl.when(step % 3 < 2)
        def _():
            norm_line.step(step // 3 * 2 + step % 3)

    spread.run(blocks, hook, done)
    ffn[...] = sums[...].astype(ffn.dtype)
    norm_line.settle()

    def add_norm(at, _):
        def add(source):
            span = row_span(here, at // 2, at % 2, rows)
            d_attn[span, :] = (cot[span, :].astype(jnp.float32) + source[span, :].astype(jnp.float32)).astype(
                d_attn.dtype)

        @pl.when(at < 2)
        def _():
            add(d_norm)

        @pl.when(at >= 2)
        def _():
            add(norm_out)
        return 0

    lax.fori_loop(0, 8, add_norm, 0)
    spread.end()

    def drain(at, _):
        leave(0, at).wait()
        leave(1, at).wait()
        return 0

    lax.fori_loop(counts - 2, counts, drain, 0)


def down_gather(cot, weight, hidden, d_norm, cid, width=256):
    total, cols = cot.shape
    rows, every = hidden.shape
    counts = every // (2 * width)
    low, f32 = jnp.bfloat16, jnp.float32
    dma = pltpu.SemaphoreType.DMA
    vm = pl.BlockSpec(memory_space=pltpu.VMEM)
    hbm = pl.BlockSpec(memory_space=pl.ANY)
    out_shape = [
        jax.ShapeDtypeStruct((total, cols), low),
        jax.ShapeDtypeStruct((total, cols), low),
        jax.ShapeDtypeStruct(weight.shape, low),
    ]
    scratch = spread_scratch(counts, rows, width) + [
        dma((2, counts)),
        pltpu.VMEM((total, cols), f32),
        pltpu.VMEM(weight.shape, f32),
        pltpu.VMEM((2, 2, width, cols), low),
        dma((2, counts)),
        pltpu.VMEM((total, cols), low),
    ] + line_scratch(12, (12 * rows // 2, cols), low)
    kernel = functools.partial(down_kernel, rows, width, counts)
    return kernel_call(kernel, out_shape, [cot, weight, hidden, d_norm], [vm, vm, hbm, vm], scratch, cid, "down",
                       [vm, vm, hbm], (0, 1))


def attend_kernel(rows, heads, cols, width, counts, qkv, rms, cos, sin, mask, w_out, g_col, w_down, attn, mixed_all,
                  kv, probs, queries, pair_rms, d_hidden, *refs, late, early):
    here = Place()
    spread = Spread(here, 1, refs[:7])
    part, pair_sems, tiny_own, tiny_pair, mixed_sems = refs[7:12]
    product = products(here, g_col, w_down, True, rows, width, counts)
    total = Reduce(here, counts, product, refs[12:23])
    piece = rows // 2

    def place(at):
        across, other, half_at = spread.block(at)
        return here.shard(across, other) * 2 + half_at

    line = Line(here, 16, [part, attn] + list(refs[23:]), place)
    got, core = spread.got, here.core
    greet(here, slice_peers(here), True)
    half = HD // 2
    scale = 1.0 / math.sqrt(HD)
    wide = heads * HD

    def rotated(first):
        lead = qkv[:, first : first + half] * rms[...]
        trail = qkv[:, first + half : first + HD] * rms[...]
        return lead * cos[0] - trail * sin[0], trail * cos[0] + lead * sin[0]

    low_k, high_k = rotated(wide)
    kv[0, :, :half] = low_k.astype(kv.dtype)
    kv[0, :, half:HD] = high_k.astype(kv.dtype)
    for at in range(2):
        first = HD + at * half
        kv[0, :, first : first + half] = (qkv[:, wide + first : wide + first + half] * rms[...]).astype(kv.dtype)
    eye = diagonal()
    tiny_own[...] = jnp.zeros_like(tiny_own)
    to_tile(tiny_own, 0, rms[:, :1], eye)
    pair_rms[0] = rms[...]
    pair = remote(kv.at[0], kv.at[1], pair_sems.at[0], pair_sems.at[1], spread.ydev)
    tiny = remote(tiny_own, tiny_pair, pair_sems.at[2], pair_sems.at[3], spread.ydev)
    for head in range(heads):
        if head == 1:
            pair.start()
            tiny.start()
        lead, trail = rotated(head * HD)
        queries[:, head * HD : head * HD + half] = (lead * scale).astype(queries.dtype)
        queries[:, head * HD + half : (head + 1) * HD] = (trail * scale).astype(queries.dtype)
    early[2].start()
    pair.wait()
    early[0].start()
    for copy in late:
        copy.wait()

    def one_head(head, _):
        query = queries[:, pl.ds(pl.multiple_of(head * HD, HD), HD)]
        scores = jnp.concatenate([dot_nt(query, kv[0, :, :HD]), dot_nt(query, kv[1, :, :HD])], axis=1)
        scores = jnp.where(mask[...] > 0, scores, NEG)
        expd = jnp.exp(scores - jnp.max(scores, axis=-1, keepdims=True))
        prob = expd / jnp.sum(expd, axis=-1, keepdims=True)
        probs[head] = prob
        prob_low = prob.astype(jnp.bfloat16)
        mixed = dot_nn(prob_low[:, :rows], kv[0, :, HD:]) + dot_nn(prob_low[:, rows:], kv[1, :, HD:])
        span = pl.ds(pl.multiple_of(head * HD, HD), HD)
        for half_at in range(2):
            low_mixed = mixed[half_at * piece : (half_at + 1) * piece, :].astype(got.dtype)
            got[0, core, half_at, 0, :, span] = low_mixed
        return 0

    lax.fori_loop(0, heads, one_head, 0)
    early[1].start()
    spread.begin_rows()

    def mixed_copy(at):
        across, other, half_at = spread.block(at)
        span = pl.ds(pl.multiple_of(place(at) * piece, piece), piece)
        return pltpu.make_async_copy(got.at[across, (core + other) % 2, half_at, 0], mixed_all.at[span, :],
                                     mixed_sems.at[at])

    def one_step(step, _):
        spread.receive_rows(step)

        @pl.when(step < 16)
        def _():
            across, other, half_at = spread.block(step)
            value = dot_nn(got[across, (core + other) % 2, half_at, 0], w_out[...])
            part[pl.ds(pl.multiple_of(place(step) * piece, piece), piece), :] = value.astype(part.dtype)
            mixed_copy(step).start()
            line.launch(step, 1)

        @pl.when(step >= 2)
        def _():
            total.advance(step - 2)

        @pl.when(step >= 4)
        def _():
            line.step(step - 4)
        return 0

    lax.fori_loop(0, 20, one_step, 0)
    line.end(16)

    def emit(at, first, second):
        for half_at, value in enumerate((first, second)):
            d_hidden[:, pl.ds(pl.multiple_of((half_at * counts + at) * width, width), width)] = value

    total.end(emit)
    for hop in range(3):
        spread.x_copy(hop, 0).wait_send()
        spread.y_copy(hop, 0).wait_send()
    for stage in range(4):
        for stream in range(2):
            spread.sib_copy(stage, stream, 0).wait_send()
    for at in range(16):
        mixed_copy(at).wait()
    tiny.wait()
    for at in range(rows // LANES):
        values = jnp.broadcast_to(from_tile(tiny_pair[at : at + 1, :], eye), (LANES, LANES))
        pair_rms[1, at * LANES : (at + 1) * LANES, :] = values


def attend(qkv, rms, cos, sin, mask, w_out, g_col, w_down, cid, width=512):
    rows = qkv.shape[0]
    wide, cols = w_out.shape
    heads = wide // HD
    counts = w_down.shape[0] // (2 * width)
    low, f32 = jnp.bfloat16, jnp.float32
    dma = pltpu.SemaphoreType.DMA
    vm = pl.BlockSpec(memory_space=pltpu.VMEM)
    out_shape = [
        jax.ShapeDtypeStruct((8 * rows, cols), low),
        jax.ShapeDtypeStruct((8 * rows, wide), low),
        jax.ShapeDtypeStruct((2, rows, 2 * HD), low),
        jax.ShapeDtypeStruct((heads, rows, 2 * rows), f32),
        jax.ShapeDtypeStruct((rows, wide), low),
        jax.ShapeDtypeStruct((2,) + rms.shape, f32),
        jax.ShapeDtypeStruct((rows, w_down.shape[0]), f32),
    ]
    scratch = spread_scratch(1, rows // 2, wide) + [
        pltpu.VMEM((8 * rows, cols), low), dma((4,)),
        pltpu.VMEM((8, LANES), f32), pltpu.VMEM((8, LANES), f32), dma((16,)),
    ] + reduce_scratch(counts, rows, width) + line_scratch(16, (8 * rows, cols), low)
    kernel = functools.partial(attend_kernel, rows, heads, cols, width, counts)
    operands = [qkv, rms, cos, sin, mask, w_out, g_col, w_down]
    out_specs = [vm, pl.BlockSpec(memory_space=pl.ANY)] + [vm] * 5
    return kernel_call(kernel, out_shape, operands, [vm] * 8, scratch, cid, "attend", out_specs, (4, 5, 6, 7), (2, 3, 4))


def tail_kernel(rows, heads, per, d_attn, w_out, queries, kv, probs, rms, cos, sin, act_t, w_qkv, ffn, x_low,
                attn, gain, gain_grad, mixed_all, d_tok, out, grad_query, grad_out, kv_sum, gains, *refs, late, early):
    here = Place()
    width = HD
    counts = heads // 2
    part = rows // 2
    refs = list(refs)
    line_counts = 8 * per
    cols = d_attn.shape[1]
    extra = cols // (rows // per)

    def take(count):
        taken_refs = refs[:count]
        del refs[:count]
        return taken_refs

    total_refs = take(11)
    spread = Spread(here, 1, take(7))
    d_mixed, tiny_own, tiny_all, d_kv, give, taken, give_sems, tiny_send, tiny_recv = take(9)
    grad, grad_mixed, gain_sum, tile, tile_send, tile_recv, put_sems, local_sems, mixed_two, mixed_sems = take(10)

    def far(at):
        return at // (2 * per), at // per % 2

    def near(at):
        return spread.block(jnp.minimum(at, line_counts - 1))

    def place_ffn(at):
        return here.shard(*far(at)) * per + at % per

    def place_tok(at):
        across, other, half_at = near(at)
        return jnp.where(at < line_counts, here.shard(across, other) * per + half_at, at)

    gain_tiles, ffn_sum, leaving = take(3)
    by_chip = chip_place(here, per)
    line = Line(here, line_counts, [ffn, ffn_sum] + take(8), by_chip)
    contrib, summed = take(2)
    line_tok = Line(here, line_counts + extra, [contrib, summed] + take(8), place_tok)
    tiny = Tiny(here, tiny_own, tiny_all, (tiny_send, tiny_recv), False)
    got, core = spread.got, here.core
    product = products(here, d_attn, w_out, True, rows, width, counts)
    total = Reduce(here, counts, product, total_refs)
    greet(here, tiny.peers, True)
    line.begin()
    grad_mixed[...] = jnp.zeros_like(grad_mixed)

    def mixed_copy(step):
        span = pl.ds(pl.multiple_of(step * rows, rows), rows)
        return pltpu.make_async_copy(mixed_all.at[span, :], mixed_two.at[step % 2], mixed_sems.at[step % 2])

    mixed_copy(0).start()

    def beside(step):
        line.step(step)

        @pl.when(step < 8)
        def _():
            span = pl.ds(pl.multiple_of(step * rows, rows), rows)
            mixed_copy(step).wait()

            @pl.when(step < 7)
            def _():
                mixed_copy(step + 1).start()

            grad_mixed[...] += dot_tn(mixed_two[step % 2], d_attn[span, :])

    done = total.run(beside)
    grad_out[...] = grad_mixed[...].astype(grad_out.dtype)
    early[1].start()

    def land(at, first, second):
        for half_at, value in enumerate((first, second)):
            d_mixed[:, pl.ds(pl.multiple_of((half_at * counts + at) * width, width), width)] = value.astype(
                d_mixed.dtype)

    total.end(land)
    half = HD // 2
    scale = 1.0 / math.sqrt(HD)
    depth = w_qkv.shape[0] * 8
    d_kv[...] = jnp.zeros_like(d_kv)
    for copy in late:
        copy.wait()

    def one_head(head, dots):
        span = pl.ds(pl.multiple_of(head * HD, HD), HD)
        query = queries[:, span]
        cot = d_mixed[:, span]
        prob = probs[head]
        d_prob = jnp.concatenate([dot_nt(cot, kv[0, :, HD:]), dot_nt(cot, kv[1, :, HD:])], axis=1)
        delta = jnp.sum(prob * d_prob, axis=-1, keepdims=True)
        d_score = (prob * (d_prob - delta)).astype(jnp.bfloat16)
        prob_low = prob.astype(jnp.bfloat16)
        d_query = (dot_nn(d_score[:, :rows], kv[0, :, :HD]) + dot_nn(d_score[:, rows:], kv[1, :, :HD])) * scale
        for side in range(2):
            keys = slice(side * rows, (side + 1) * rows)
            d_kv[side, :, :HD] += dot_tn(d_score[:, keys], query)
            d_kv[side, :, HD:] += dot_tn(prob_low[:, keys], cot)
        dots = dots + jnp.sum(d_query * query.astype(jnp.float32), axis=-1, keepdims=True)
        lead, trail = d_query[:, :half], d_query[:, half:]
        first = ((lead * cos[0] + trail * sin[0]) * rms[0]).astype(got.dtype)
        second = ((trail * cos[0] - lead * sin[0]) * rms[0]).astype(got.dtype)
        line.step(done + head)
        for rows_at in range(2):
            piece = slice(rows_at * part, (rows_at + 1) * part)
            got[0, core, rows_at, 0, :, pl.ds(pl.multiple_of(head * HD, HD), half)] = first[piece, :]
            got[0, core, rows_at, 0, :, pl.ds(pl.multiple_of(head * HD + half, half), half)] = second[piece, :]

        return dots

    dots = lax.fori_loop(0, heads, one_head, jnp.zeros((rows, 1), jnp.float32))
    eye = diagonal()
    tiny_own[...] = jnp.zeros_like(tiny_own)
    for side in (1, 0):
        d_key, d_value = d_kv[side, :, :HD], d_kv[side, :, HD:]
        own = jnp.sum(d_key * kv[side, :, :HD].astype(jnp.float32) +
                      d_value * kv[side, :, HD:].astype(jnp.float32), axis=-1, keepdims=True)
        if side == 0:
            own = own + dots * (1.0 / scale)
        own = own * (rms[side] * rms[side] * (1.0 / depth))
        to_tile(tiny_own, side * (rows // LANES), own, eye)
        lead, trail = d_key[:, :half], d_key[:, half:]
        parts = [(lead * cos[side] + trail * sin[side]) * rms[side],
                 (trail * cos[side] - lead * sin[side]) * rms[side],
                 d_value[:, :half] * rms[side], d_value[:, half:] * rms[side]]
        for at, value in enumerate(parts):
            if side == 1:
                give[:, at * half : (at + 1) * half] = value.astype(give.dtype)
            else:
                d_kv[0, :, at * half : (at + 1) * half] = value
    given = remote(give, taken, give_sems.at[0], give_sems.at[1], spread.ydev)
    given.start()
    grad[...] = jnp.zeros_like(grad)
    line.steps(done + heads, done + heads + 2)
    given.wait()
    for rows_at in range(2):
        piece = slice(rows_at * part, (rows_at + 1) * part)
        value = d_kv[0, piece, :] + taken[piece, :].astype(jnp.float32)
        got[0, core, rows_at, 0, :, heads * HD :] = value.astype(got.dtype)
    tiny.begin()
    spread.begin_rows()
    gain_sum[...] = jnp.zeros_like(gain_sum)
    tiny.end()

    def block_of(at):
        across, other, half_at = near(at)
        shard, partner = here.shard(across, other), here.shard((across + 2) % 4, other)
        block = got[across, (core + other) % 2, half_at, 0]
        first = pl.multiple_of(shard * rows + half_at * part, part)
        for tile_at in range(part // LANES):
            row = pl.ds(pl.multiple_of(first + tile_at * LANES, LANES), LANES)
            low_at = half_at * (part // LANES) + tile_at
            kept = rows // LANES + low_at
            dot = from_tile(tiny_all[shard, pl.ds(low_at, 1), :] + tiny_all[partner, pl.ds(kept, 1), :], eye)
            value = dot_nt(block[tile_at * LANES : (tile_at + 1) * LANES, :], w_qkv[...])
            x_rows = x_low[row, :].astype(jnp.float32)
            contrib[row, :] = (value * gain[0:1, :] - x_rows * dot).astype(contrib.dtype)
            gain_sum[...] += jnp.sum(value * x_rows, axis=0, keepdims=True)
        line_tok.launch(at, 1)

        @pl.when(other == 1)
        def _():
            twin = got[across, core, half_at, 0]
            twin_first = pl.multiple_of(here.shard(across, 0) * rows + half_at * part, part)
            rows_t, twin_t = act_t[:, pl.ds(first, part)], act_t[:, pl.ds(twin_first, part)]
            for at_col in range((heads + 2) * HD // 512):
                span = slice(at_col * 512, (at_col + 1) * 512)
                grad[:, span] += dot_nn(rows_t, block[:, span]) + dot_nn(twin_t, twin[:, span])

    me = here.shard(0, 0)
    columns = pl.ds(pl.multiple_of(me * cols, cols), cols)
    chunk = line.chunk

    def landing(which, at):
        sub = at % per if which == 0 else near(at)[2]
        return (out, d_tok)[which].at[pl.ds(pl.multiple_of(sub * chunk, chunk), chunk), columns]

    def leaver(which, at):
        return (leaving, line_tok.from_end)[which].at[at]

    def put(which, at):
        goal = here.device(*(far(at) if which == 0 else near(at)[:2]))
        return remote(leaver(which, at), landing(which, at), put_sems.at[which, 0, at], put_sems.at[which, 1, at],
                      goal)

    def keep(which, at):
        spot = at % per if which == 0 else near(at)[2]
        return pltpu.make_async_copy(leaver(which, at), landing(which, at), local_sems.at[which, spot])

    def emit(which, at):
        if which == 1:
            row = line_tok.rows(at)
            value = d_attn[row, :].astype(jnp.float32) + summed[row, :].astype(jnp.float32)
            line_tok.from_end[at] = value.astype(out.dtype)
            return
        row = pl.ds(pl.multiple_of(place_ffn(at) * chunk, chunk), chunk)

        def leave(source):
            value = x_low[row, :].astype(jnp.float32) + attn[row, :].astype(jnp.float32)
            leaving[at] = (value + source[row, :].astype(jnp.float32)).astype(out.dtype)

        leave(ffn_sum)

    def is_own(which, at):
        return at < per if which == 0 else jnp.logical_and(at < 4, at % 2 == 0)

    def send(which, at):
        own = is_own(which, at)

        @pl.when(own)
        def _():
            keep(which, at).start()

        @pl.when(jnp.logical_not(own))
        def _():
            put(which, at).start()

    def stage_step(step, _):
        spread.receive_rows(step)

        @pl.when(step < line_counts)
        def _():
            block_of(step)

        @pl.when(step < 3)
        def _():
            line.step(done + heads + 2 + step)

        @pl.when(step >= 4)
        def _():
            line_tok.step(step - 4)

        @pl.when(step > 0)
        def _():
            send(0, step - 1)

        @pl.when(line.inner == 0)
        def _():
            line.up(step).wait_send()
            line.down(step).wait_recv()

        emit(0, step)

        @pl.when(jnp.logical_and(line.inner == 1, step > 7))
        def _():
            send(1, step - 8)

        @pl.when(jnp.logical_and(line.inner == 1, step > 6))
        def _():
            emit(1, step - 7)
        return 0

    lax.fori_loop(0, line_counts, stage_step, 0)
    for half_at in range(cols // (rows // per)):
        span = pl.ds(line_counts * (rows // per) + half_at * (rows // per), rows // per)
        source = slice(half_at * (rows // per), (half_at + 1) * (rows // per))
        contrib[span, :] = grad[source, heads * HD :].astype(contrib.dtype)
    line_tok.launch(line_counts, extra)
    grad_query[...] = grad[:, : heads * HD].astype(grad_query.dtype)
    early[0].start()
    for at in range(cols // LANES):
        tile[at : at + 1, :] = gain_sum[:, at * LANES : (at + 1) * LANES]
        spot = cols // LANES + at
        tile[spot : spot + 1, :] = gain_grad[:, at * LANES : (at + 1) * LANES]

    def tile_copy(step):
        return remote(tile, gain_tiles.at[here.z], tile_send.at[step], tile_recv.at[step],
                      (here.dp, here.seq, (here.z + step + 1) % 4))

    send(0, line_counts - 1)
    line.drain()
    for step in range(3):
        tile_copy(step).start()
    gain_tiles[here.z] = tile[...]

    @pl.when(line.inner == 1)
    def _():
        start = line_counts - 4

        def both(at, _):
            line_tok.step(at)

            @pl.when(at < line_counts + 4)
            def _():
                send(1, at - 4)

            @pl.when(at < line_counts + 3)
            def _():
                emit(1, at - 3)
            return 0

        lax.fori_loop(start, line_counts + extra + 2, both, 0)

        def drain(at, _):
            line_tok.down(at).wait_send()
            return 0

        lax.fori_loop(0, line_counts + extra, drain, 0)

    @pl.when(line.inner == 0)
    def _():
        def arrive(at, _):
            line_tok.up(at).wait_send()
            line_tok.down(at).wait_recv()

            @pl.when(jnp.logical_and(at > 0, at <= line_counts))
            def _():
                send(1, at - 1)

            @pl.when(at < line_counts)
            def _():
                emit(1, at)
            return 0

        lax.fori_loop(0, line_counts + extra, arrive, 0)

    for half_at in range(extra):
        span = pl.ds((line_counts + half_at) * chunk, chunk)
        kv_sum[half_at * chunk : (half_at + 1) * chunk, :] = summed[span, :]
    for hop in range(3):
        spread.x_copy(hop, 0).wait_send()
        spread.y_copy(hop, 0).wait_send()
    for stage in range(4):
        spread.sib_copy(stage, 0, 0).wait_send()
        spread.sib_copy(stage, 1, 0).wait_send()

    def finish(at, _):
        for which in range(2):
            own = is_own(which, at)

            @pl.when(own)
            def _():
                keep(which, at).wait()

            @pl.when(jnp.logical_not(own))
            def _():
                put(which, at).wait()
        return 0

    lax.fori_loop(0, line_counts, finish, 0)
    for step in range(3):
        tile_copy(step).wait()
    gains[...] = gain_tiles[0] + gain_tiles[1] + gain_tiles[2] + gain_tiles[3]


def tail(d_attn, w_out, queries, kv, probs, rms, cos, sin, act_t, w_qkv, ffn, x_low, attn, gain, gain_grad,
         mixed_all, cid,
 per=2):
    total, cols = d_attn.shape
    rows = total // 8
    wide = w_out.shape[0]
    heads = wide // HD
    low, f32 = jnp.bfloat16, jnp.float32
    dma = pltpu.SemaphoreType.DMA
    vm = pl.BlockSpec(memory_space=pltpu.VMEM)
    counts = 8 * per
    chunk = rows // per
    extra = cols // chunk
    long = (total + cols, cols)
    out_shape = [
        jax.ShapeDtypeStruct((rows, 8 * cols), low),
        jax.ShapeDtypeStruct((rows, 8 * cols), low),
        jax.ShapeDtypeStruct((cols, wide), low),
        jax.ShapeDtypeStruct(w_out.shape, low),
        jax.ShapeDtypeStruct((cols, 2 * HD), low),
        jax.ShapeDtypeStruct((8, LANES), f32),
    ]
    scratch = reduce_scratch(heads // 2, rows, HD, 2) + spread_scratch(1, rows // 2, wide + 2 * HD)
    scratch += [
        pltpu.VMEM((rows, wide), low),
        pltpu.VMEM((8, LANES), f32),
        pltpu.VMEM((8, 8, LANES), f32),
        pltpu.VMEM((2, rows, 2 * HD), f32),
        pltpu.VMEM((rows, 2 * HD), low),
        pltpu.VMEM((rows, 2 * HD), low),
        dma((2,)), dma((7,)), dma((7,)),
        pltpu.VMEM(w_qkv.shape, f32),
        pltpu.VMEM(w_out.shape, f32),
        pltpu.VMEM((1, cols), f32),
        pltpu.VMEM((8, LANES), f32),
        dma((3,)), dma((3,)), dma((2, 2, counts)), dma((2, per)),
        pltpu.VMEM((2, rows, wide), low), dma((2,)),
        pltpu.VMEM((4, 8, LANES), f32),
        pltpu.VMEM((total, cols), low),
        pltpu.VMEM((counts, chunk, cols), low),
    ] + line_scratch(counts, (total, cols), low)
    scratch += [pltpu.VMEM(long, low), pltpu.VMEM(long, low)] + line_scratch(counts + extra, long, low)
    operands = [d_attn, w_out, queries, kv, probs, rms, cos, sin, act_t, w_qkv, ffn, x_low, attn, gain,
                gain_grad, mixed_all]
    kernel = functools.partial(tail_kernel, rows, heads, per)
    specs = [vm] * (len(operands) - 1) + [pl.BlockSpec(memory_space=pl.ANY)]
    return kernel_call(kernel, out_shape, operands, specs, scratch, cid, "tail",
                       late=(2, 3, 4, 8, 9, 11, 12), early=(2, 3))


LANES = 128


def acts_move(
    tokens, seg_ids, gain_attn, w_query, kv_weight, w_out, gain_ffn, w_gate, w_up, w_down, d_out
):
    qkv, x_low, act_one_t, w_qkv, rms, cos, sin, mask, g_parts, small = opening(
        tokens, gain_attn, gain_ffn, seg_ids, w_query, kv_weight, d_out, 1
    )
    g_low = g_parts.reshape(x_low.shape)
    attn, mixed_all, kv, probs, queries, pair_rms, d_hidden = attend(
        qkv, rms, cos, sin, mask, w_out, g_low, w_down, 2
    )
    hidden, d_gate, d_up, act_two_t, dots = ffn_scatter(x_low, attn, small, w_gate, w_up, d_hidden, 4)
    d_norm, grad_gain_two, grad_gate, grad_up = back_gather(
        act_two_t, w_gate, w_up, d_gate, d_up, dots, x_low, attn, small, 5
    )
    ffn, d_attn, grad_down = down_gather(g_low, w_down, hidden, d_norm, 6)
    d_tokens, out, grad_query, grad_out, grad_kv, gain_sums = tail(
        d_attn,
        w_out,
        queries,
        kv,
        probs,
        pair_rms,
        cos,
        sin,
        act_one_t,
        w_qkv,
        ffn,
        x_low,
        attn,
        small,
        grad_gain_two,
        mixed_all,
        7,
    )
    gains = gain_sums.reshape(2, -1)
    wider = jnp.float32
    return (
        out,
        d_tokens.astype(wider),
        gains[0],
        grad_query.astype(wider),
        grad_kv.astype(wider),
        grad_out.astype(wider),
        gains[1],
        grad_gate.astype(wider),
        grad_up.astype(wider),
        grad_down.astype(wider),
    )


def solution(mesh):
    in_specs = (
        P(("dp", "seq"), None),
        P("dp"),
        P(("dp", "seq")),
        P(("dp", "seq"), "tensor"),
        P(("dp", "seq"), None),
        P("tensor", ("dp", "seq")),
        P(("dp", "seq")),
        P(("dp", "seq"), "tensor"),
        P(("dp", "seq"), "tensor"),
        P("tensor", ("dp", "seq")),
        P(("dp", "seq"), None),
    )
    out_specs = (
        P(("dp", "seq"), None),
        P(("dp", "seq"), None),
        P(("dp", "seq")),
        P(("dp", "seq"), "tensor"),
        P(("dp", "seq"), None),
        P("tensor", ("dp", "seq")),
        P(("dp", "seq")),
        P(("dp", "seq"), "tensor"),
        P(("dp", "seq"), "tensor"),
        P("tensor", ("dp", "seq")),
    )

    def shards(*arrays):
        tokens = arrays[0]
        sizes = tuple(mesh.shape[name] for name in ("dp", "seq", "tensor"))
        count = tokens.shape[0] * sizes[0] * sizes[1]
        plan = acts_move if sizes == (4, 2, 4) and count <= tokens.shape[1] else weights_move
        return plan(*arrays)

    return jax.shard_map(shards, mesh=mesh, in_specs=in_specs, out_specs=out_specs, check_vma=False)
```

```python
import functools
import math

import jax
import jax.numpy as jnp
from jax import lax
from jax.experimental import pallas as pl
from jax.experimental.pallas import tpu as pltpu
from jax.sharding import PartitionSpec as P

HD = 256


EPS = 1e-06
NEG = -1e30


def place_tables(segs):
    length = segs.shape[0]
    index = jnp.arange(length, dtype=jnp.int32)
    flags = jnp.concatenate([jnp.ones((1,), dtype=bool), segs[1:] != segs[:-1]])
    starts = lax.cummax(jnp.where(flags, index, jnp.zeros_like(index)), axis=0)
    places = index - starts
    half_size = HD // 2
    freqs = jnp.exp(jnp.arange(half_size, dtype=jnp.float32) * (-math.log(10000.0) / half_size))
    angles = places.astype(jnp.float32)[:, None] * freqs[None, :]
    return (places, jnp.cos(angles), jnp.sin(angles))


def rotate(vector, cos_table, sin_table):
    half_size = vector.shape[-1] // 2
    leading = vector[..., :half_size]
    trailing = vector[..., half_size:]
    return jnp.concatenate(
        [leading * cos_table - trailing * sin_table, trailing * cos_table + leading * sin_table],
        axis=-1,
    )


def rotate_back(vector, cos_table, sin_table):
    half_size = vector.shape[-1] // 2
    leading = vector[..., :half_size]
    trailing = vector[..., half_size:]
    return jnp.concatenate(
        [leading * cos_table + trailing * sin_table, trailing * cos_table - leading * sin_table],
        axis=-1,
    )


def matmul(left, right):
    return jnp.dot(left, right, preferred_element_type=jnp.float32)


def matmul_nt(left, right):
    return lax.dot_general(
        left, right, (((1,), (1,)), ((), ())), preferred_element_type=jnp.float32
    )


def matmul_tn(left, right):
    return lax.dot_general(
        left, right, (((0,), (0,)), ((), ())), preferred_element_type=jnp.float32
    )


def gelu_tanh(values):
    return jax.nn.gelu(values, approximate=True)


def norm_back(d_act, normed, rms_val, gain_val):
    scaled = d_act * gain_val
    return rms_val * (scaled - normed * jnp.mean(scaled * normed, axis=-1, keepdims=True))


def weights_move(
    tokens, seg_ids, gain_attn, w_query, kv_weight, w_out, gain_ffn, w_gate, w_up, w_down, d_out
):
    rows = tokens.shape[0]
    scale_factor = 1.0 / math.sqrt(HD)
    offset = lax.axis_index("seq") * rows
    places, cos_table, sin_table = place_tables(seg_ids)
    own_places = lax.dynamic_slice_in_dim(places, offset, rows, 0)
    own_segs = lax.dynamic_slice_in_dim(seg_ids, offset, rows, 0)
    own_cos = lax.dynamic_slice_in_dim(cos_table, offset, rows, 0)
    own_sin = lax.dynamic_slice_in_dim(sin_table, offset, rows, 0)
    allowed = (own_segs[:, None] == seg_ids[None, :]) & (own_places[:, None] >= places[None, :])
    full_query, full_out, full_kv, full_gain_one = (
        lax.all_gather(w_query, ("dp", "seq"), axis=0, tiled=True),
        lax.all_gather(w_out, ("dp", "seq"), axis=1, tiled=True),
        lax.all_gather(kv_weight, ("dp", "seq"), axis=0, tiled=True),
        lax.all_gather(gain_attn, ("dp", "seq"), axis=0, tiled=True),
    )
    gain_one = full_gain_one.astype(jnp.float32)
    inputs = tokens.astype(jnp.float32)
    rms_one = lax.rsqrt(jnp.mean(inputs * inputs, axis=-1, keepdims=True) + EPS)
    norm_one = inputs * rms_one
    act_one = (norm_one * gain_one).astype(jnp.bfloat16)
    query_pre = matmul(act_one, full_query)
    heads = query_pre.shape[1] // HD
    kv_pre = matmul(act_one, full_kv)
    queries = (
        rotate(query_pre.reshape(rows, heads, HD), own_cos[:, None, :], own_sin[:, None, :])
        * scale_factor
    ).astype(jnp.bfloat16)
    own_kv = jnp.concatenate(
        [rotate(kv_pre[:, :HD], own_cos, own_sin), kv_pre[:, HD:]], axis=1
    ).astype(jnp.bfloat16)
    all_kv = lax.all_gather(own_kv, "seq", axis=0, tiled=True)
    keys = all_kv[:, :HD]
    values_all = all_kv[:, HD:]
    scores = jnp.einsum("rhd,kd->hrk", queries, keys, preferred_element_type=jnp.float32)
    scores = jnp.where(allowed[None], scores, NEG)
    top_score = jnp.max(scores, axis=-1, keepdims=True)
    expd = jnp.exp(scores - top_score)
    total = jnp.sum(expd, axis=-1, keepdims=True)
    log_total = top_score + jnp.log(total)
    probs_low = (expd / total).astype(jnp.bfloat16)
    mixed = (
        jnp.einsum("hrk,kd->rhd", probs_low, values_all, preferred_element_type=jnp.float32)
        .reshape(rows, heads * HD)
        .astype(jnp.bfloat16)
    )
    attn = lax.psum(matmul(mixed, full_out), "tensor")
    resid = inputs + attn
    full_gate, full_up, full_down, full_gain_two = (
        lax.all_gather(w_gate, ("dp", "seq"), axis=0, tiled=True),
        lax.all_gather(w_up, ("dp", "seq"), axis=0, tiled=True),
        lax.all_gather(w_down, ("dp", "seq"), axis=1, tiled=True),
        lax.all_gather(gain_ffn, ("dp", "seq"), axis=0, tiled=True),
    )
    gain_two = full_gain_two.astype(jnp.float32)
    rms_two = lax.rsqrt(jnp.mean(resid * resid, axis=-1, keepdims=True) + EPS)
    norm_two = resid * rms_two
    act_two = (norm_two * gain_two).astype(jnp.bfloat16)
    gate = matmul(act_two, full_gate)
    up_val = matmul(act_two, full_up)
    gelu_val, gelu_pull = jax.vjp(gelu_tanh, gate)
    hidden = (gelu_val * up_val).astype(jnp.bfloat16)
    ffn = lax.psum(matmul(hidden, full_down).astype(jnp.bfloat16), "tensor").astype(jnp.float32)
    out = (resid + ffn).astype(jnp.bfloat16)
    back_gate, back_up, back_down = (
        lax.all_gather(w_gate, ("dp", "seq"), axis=0, tiled=True),
        lax.all_gather(w_up, ("dp", "seq"), axis=0, tiled=True),
        lax.all_gather(w_down, ("dp", "seq"), axis=1, tiled=True),
    )
    d_hidden = matmul_nt(d_out, back_down)
    grad_down = matmul_tn(hidden, d_out)
    d_gate = gelu_pull(d_hidden * up_val)[0].astype(jnp.bfloat16)
    d_up = (d_hidden * gelu_val).astype(jnp.bfloat16)
    grad_gate = matmul_tn(act_two, d_gate)
    grad_up = matmul_tn(act_two, d_up)
    d_act_two = lax.psum(matmul_nt(d_gate, back_gate) + matmul_nt(d_up, back_up), "tensor")
    grad_gain_two = jnp.sum(d_act_two * norm_two, axis=0)
    d_resid = d_out.astype(jnp.float32) + norm_back(d_act_two, norm_two, rms_two, gain_two)
    ffn_grads = (
        lax.psum_scatter(
            grad_gate.astype(jnp.bfloat16), ("dp", "seq"), scatter_dimension=0, tiled=True
        ).astype(jnp.float32),
        lax.psum_scatter(
            grad_up.astype(jnp.bfloat16), ("dp", "seq"), scatter_dimension=0, tiled=True
        ).astype(jnp.float32),
        lax.psum_scatter(
            grad_down.astype(jnp.bfloat16), ("dp", "seq"), scatter_dimension=1, tiled=True
        ).astype(jnp.float32),
        lax.psum_scatter(
            grad_gain_two.astype(jnp.bfloat16), ("dp", "seq"), scatter_dimension=0, tiled=True
        ).astype(jnp.float32),
    )
    back_query, back_out, back_kv = (
        lax.all_gather(w_query, ("dp", "seq"), axis=0, tiled=True),
        lax.all_gather(w_out, ("dp", "seq"), axis=1, tiled=True),
        lax.all_gather(kv_weight, ("dp", "seq"), axis=0, tiled=True),
    )
    d_attn = d_resid.astype(jnp.bfloat16)
    grad_out = matmul_tn(mixed, d_attn)
    d_mixed = matmul_nt(d_attn, back_out).astype(jnp.bfloat16).reshape(rows, heads, HD)
    scores_again = jnp.einsum("rhd,kd->hrk", queries, keys, preferred_element_type=jnp.float32)
    probs = jnp.where(allowed[None], jnp.exp(scores_again - log_total), 0.0)
    d_probs = jnp.einsum("rhd,kd->hrk", d_mixed, values_all, preferred_element_type=jnp.float32)
    delta = jnp.sum(probs * d_probs, axis=-1, keepdims=True)
    d_scores = (probs * (d_probs - delta)).astype(jnp.bfloat16)
    d_queries = (
        jnp.einsum("hrk,kd->rhd", d_scores, keys, preferred_element_type=jnp.float32) * scale_factor
    )
    d_query_pre = (
        rotate_back(d_queries, own_cos[:, None, :], own_sin[:, None, :])
        .reshape(rows, heads * HD)
        .astype(jnp.bfloat16)
    )
    d_keys_part = jnp.einsum("hrk,rhd->kd", d_scores, queries, preferred_element_type=jnp.float32)
    d_values_part = jnp.einsum(
        "hrk,rhd->kd", probs.astype(jnp.bfloat16), d_mixed, preferred_element_type=jnp.float32
    )
    own_kv_grad = lax.psum_scatter(
        jnp.concatenate([d_keys_part, d_values_part], axis=1).astype(jnp.bfloat16),
        "seq",
        scatter_dimension=0,
        tiled=True,
    )
    d_act_query = matmul_nt(d_query_pre, back_query)
    d_act_sum, kv_grad = (
        lax.psum(d_act_query.astype(jnp.bfloat16), "tensor").astype(jnp.float32),
        lax.psum(own_kv_grad, "tensor").astype(jnp.float32),
    )
    d_kv_pre = jnp.concatenate(
        [rotate_back(kv_grad[:, :HD], own_cos, own_sin), kv_grad[:, HD:]], axis=1
    ).astype(jnp.bfloat16)
    d_act_one = d_act_sum + matmul_nt(d_kv_pre, back_kv)
    grad_query = matmul_tn(act_one, d_query_pre)
    grad_kv = matmul_tn(act_one, d_kv_pre)
    grad_gain_one = jnp.sum(d_act_one * norm_one, axis=0)
    d_tokens = d_resid + norm_back(d_act_one, norm_one, rms_one, gain_one)
    attn_grads = (
        lax.psum_scatter(
            grad_query.astype(jnp.bfloat16), ("dp", "seq"), scatter_dimension=0, tiled=True
        ).astype(jnp.float32),
        lax.psum_scatter(
            grad_out.astype(jnp.bfloat16), ("dp", "seq"), scatter_dimension=1, tiled=True
        ).astype(jnp.float32),
        lax.psum_scatter(
            grad_kv.astype(jnp.bfloat16), ("dp", "seq"), scatter_dimension=0, tiled=True
        ).astype(jnp.float32),
        lax.psum_scatter(
            grad_gain_one.astype(jnp.bfloat16), ("dp", "seq"), scatter_dimension=0, tiled=True
        ).astype(jnp.float32),
    )
    return (
        out,
        d_tokens,
        attn_grads[3],
        attn_grads[0],
        attn_grads[2],
        attn_grads[1],
        ffn_grads[3],
        ffn_grads[0],
        ffn_grads[1],
        ffn_grads[2],
    )


MESH = pl.DeviceIdType.MESH
VMEM_LIMIT = 66000 * 1024


class Place:
    def __init__(self):
        self.dp = lax.axis_index("dp")
        self.seq = lax.axis_index("seq")
        self.z = lax.axis_index("tensor")
        self.core = lax.rem(self.dp, 2)
        self.chip = lax.div(self.dp, 2)

    def device(self, across, other):
        chip = (self.chip + across) % 2
        seq = (self.seq + across // 2) % 2
        core = (self.core + other) % 2
        return chip * 2 + core, seq, self.z

    def shard(self, across, other):
        dp, seq, _ = self.device(across, other)
        return dp * 2 + seq


def greet(here, peers, line=False):
    barrier = pltpu.get_barrier_semaphore()
    peers = list(peers)
    if line:
        peers += [(here.dp, here.seq, (here.z + step) % 4) for step in range(1, 4)]
    for peer in peers:
        pl.semaphore_signal(barrier, inc=1, device_id=peer, device_id_type=MESH)
    pl.semaphore_wait(barrier, len(peers))


def remote(src, dst, send, recv, peer):
    return pltpu.make_async_remote_copy(
        src_ref=src, dst_ref=dst, send_sem=send, recv_sem=recv, device_id=peer, device_id_type=MESH
    )


class Line:
    def __init__(self, here, counts, refs, place=None):
        self.own, self.out, self.from_end, self.from_mid = refs[:4]
        self.sems = refs[4:10]
        self.counts = counts
        self.chunk = self.from_mid.shape[1]
        self.fold = self.from_end.shape[1] // self.chunk
        self.place = place
        z = here.z
        self.inner = ((z + 1) // 2) % 2
        self.mate = (here.dp, here.seq, z + 1 - 2 * (z % 2))
        self.other = (here.dp, here.seq, 3 - z)

    def rows(self, at):
        at = at if self.place is None else self.place(at)
        return pl.ds(pl.multiple_of(at * self.chunk, self.chunk), self.chunk)

    def inbox(self, at):
        span = pl.ds(pl.multiple_of(at % self.fold * self.chunk, self.chunk), self.chunk)
        return self.from_end.at[at // self.fold, span, :]

    def up(self, at):
        return remote(self.own.at[self.rows(at), :], self.inbox(at), self.sems[0].at[at],
                      self.sems[1].at[at], self.mate)

    def over(self, at):
        return remote(self.out.at[self.rows(at), :], self.from_mid.at[at], self.sems[2].at[at],
                      self.sems[3].at[at], self.other)

    def down(self, at):
        rows = self.rows(at)
        return remote(self.out.at[rows, :], self.out.at[rows, :], self.sems[4].at[at],
                      self.sems[5].at[at], self.mate)

    def launch(self, first, count):
        @pl.when(self.inner == 0)
        def _():
            def send(at, _):
                self.up(first + at).start()
                return 0

            lax.fori_loop(0, count, send, 0)

    def begin(self):
        self.launch(0, self.counts)

    def first(self, at):
        rows = self.rows(at)
        self.up(at).wait_recv()
        total = self.own[rows, :].astype(jnp.float32) + self.inbox(at)[...].astype(jnp.float32)
        self.out[rows, :] = total.astype(self.out.dtype)
        self.over(at).start()

    def second(self, at):
        rows = self.rows(at)
        self.over(at).wait()
        total = self.out[rows, :].astype(jnp.float32) + self.from_mid[at].astype(jnp.float32)
        self.out[rows, :] = total.astype(self.out.dtype)
        self.down(at).start()

    def step(self, at, start=0, count=None):
        count = self.counts if count is None else count

        @pl.when(jnp.logical_and(self.inner == 1, at < count))
        def _():
            self.first(start + at)

        @pl.when(jnp.logical_and(self.inner == 1, jnp.logical_and(at > 1, at < count + 2)))
        def _():
            self.second(start + at - 2)

    def steps(self, first, last, start=0, count=None):
        def rest(at, _):
            self.step(at, start, count)
            return 0

        lax.fori_loop(first, last, rest, 0)

    def settle(self):
        @pl.when(self.inner == 0)
        def _():
            def take(at, _):
                self.up(at).wait_send()
                self.down(at).wait_recv()
                return 0

            lax.fori_loop(0, self.counts, take, 0)

        self.drain()

    def drain(self):
        @pl.when(self.inner == 1)
        def _():
            def drain(at, _):
                self.down(at).wait_send()
                return 0

            lax.fori_loop(0, self.counts, drain, 0)

    def end(self, done=0):
        self.steps(min(done, self.counts + 2), self.counts + 2)
        self.settle()


def line_scratch(counts, shape, low, fold=1):
    chunk = shape[0] // counts
    inbox = pltpu.VMEM((counts // fold, chunk * fold, shape[1]), low)
    return [inbox, pltpu.VMEM((counts, chunk, shape[1]), low)] + [pltpu.SemaphoreType.DMA((counts,))] * 6


def turned(at):
    return 3 - at // 2, 1 - at % 2


def slice_peers(here):
    return [here.device(*turned(at)) for at in range(7)]


def kernel_call(kernel, out_shape, operands, specs, scratch, cid, name, out_specs=None, late=(), early=()):
    vm = pl.BlockSpec(memory_space=pltpu.VMEM)
    hbm = pl.BlockSpec(memory_space=pl.ANY)
    specs = [hbm if at in late else spec for at, spec in enumerate(specs)]
    out_specs = [hbm if at in early else spec for at, spec in enumerate(out_specs or [vm] * len(out_shape))]
    inside = [pltpu.VMEM(operands[at].shape, operands[at].dtype) for at in late]
    inside += [pltpu.VMEM(out_shape[at].shape, out_shape[at].dtype) for at in early]
    inside.append(pltpu.SemaphoreType.DMA((max(1, len(late) + len(early)),)))
    n_in, n_out = len(operands), len(out_shape)

    def body(*refs):
        ins, outs = list(refs[:n_in]), list(refs[n_in : n_in + n_out])
        rest, own = refs[n_in + n_out : -len(inside)], refs[-len(inside) :]
        loads, stores = [], []
        for spot, at in enumerate(late):
            copy = pltpu.make_async_copy(ins[at], own[spot], own[-1].at[spot])
            copy.start()
            loads.append(copy)
            ins[at] = own[spot]
        for number, at in enumerate(early):
            spot = len(late) + number
            stores.append(pltpu.make_async_copy(own[spot], outs[at], own[-1].at[spot]))
            outs[at] = own[spot]
        more = {}
        if late:
            more["late"] = loads
        if early:
            more["early"] = stores
        kernel(*ins, *outs, *rest, **more)
        for copy in stores:
            copy.wait()

    return pl.pallas_call(
        body,
        out_shape=out_shape,
        in_specs=specs,
        out_specs=out_specs,
        scratch_shapes=scratch + inside,
        compiler_params=pltpu.CompilerParams(
            collective_id=cid, has_side_effects=True, vmem_limit_bytes=VMEM_LIMIT
        ),
        name=f"{name}_{cid}",
    )(*operands)


class Tiny:
    def __init__(self, here, src, dst, sems, spread):
        self.here, self.src, self.dst, self.sems, self.spread = here, src, dst, sems, spread
        self.peers = slice_peers(here)
        self.me = here.shard(0, 0)

    def tile(self, shard):
        return self.src.at[shard] if self.spread else self.src

    def copy(self, at):
        return remote(self.tile(self.here.shard(*turned(at))), self.dst.at[self.me], self.sems[0].at[at],
                      self.sems[1].at[at], self.peers[at])

    def begin(self):
        for at in range(7):
            self.copy(at).start()
        self.dst[self.me] = self.tile(self.me)[...]

    def end(self):
        for at in range(7):
            self.copy(at).wait()


class Reduce:
    def __init__(self, here, counts, product, refs, before=None):
        self.counts, self.product, self.before = counts, product, before
        self.held, self.sib_out, self.sib_in, self.from_x, self.from_y = refs[:5]
        self.sib_sems, self.x_sems, self.y_sems = refs[5:7], refs[7:9], refs[9:11]
        self.sib, self.xdev, self.ydev = here.device(0, 1), here.device(1, 0), here.device(2, 0)
        self.steps = 4 * counts
        self.ring = self.sib_out.shape[0]

    def streams(self, stage):
        far = stage // 3
        x_chip = jnp.where(stage == 0, 3, jnp.where(stage == 2, 0, 1))
        y_chip = jnp.where(stage == 0, 3, jnp.where(stage == 2, 0, 2))
        return (x_chip, far), (y_chip, 1 - far)

    def to_sib(self, step, stream):
        stage, at = step // self.counts, step % self.counts
        return remote(self.sib_out.at[step % self.ring, stream], self.sib_in.at[stage, stream, at],
                      self.sib_sems[0].at[stage, stream, at], self.sib_sems[1].at[stage, stream, at], self.sib)

    def to_x(self, hop, at, stage=0):
        return remote(self.held.at[stage, 0, at], self.from_x.at[hop, at], self.x_sems[0].at[hop, at],
                      self.x_sems[1].at[hop, at], self.xdev)

    def to_y(self, hop, at, stage=0):
        return remote(self.held.at[stage, 1, at], self.from_y.at[hop, at], self.y_sems[0].at[hop, at],
                      self.y_sems[1].at[hop, at], self.ydev)

    def compute(self, step):
        stage, at = step // self.counts, step % self.counts
        if self.before:
            for stop in range(3):
                @pl.when(step == stop * self.counts)
                def _():
                    self.before(stop)

        @pl.when(step >= self.ring)
        def _():
            for stream in range(2):
                self.to_sib(step - self.ring, stream).wait_send()

        for stream, (across, half) in enumerate(self.streams(stage)):
            self.sib_out[step % self.ring, stream] = self.product(across, 1, half, at).astype(jnp.bfloat16)
            self.held[stage, stream, at] = self.product(across, 0, half, at).astype(jnp.bfloat16)
        for stream in range(2):
            self.to_sib(step, stream).start()

    def finish(self, step):
        stage, at = step // self.counts, step % self.counts
        for stream in range(2):
            self.to_sib(step, stream).wait_recv()

        def total(stream):
            return self.held[stage, stream, at].astype(jnp.float32) + self.sib_in[stage, stream, at].astype(
                jnp.float32)

        @pl.when(stage < 3)
        def _():
            for stream in range(2):
                self.held[stage, stream, at] = total(stream).astype(jnp.bfloat16)

        @pl.when(stage == 3)
        def _():
            self.to_y(0, at).wait_recv()
            self.held[3, 0, at] = (total(0) + self.from_y[0, at].astype(jnp.float32)).astype(jnp.bfloat16)
            self.to_x(0, at).wait_recv()
            self.held[3, 1, at] = (total(1) + self.from_x[0, at].astype(jnp.float32)).astype(jnp.bfloat16)

        @pl.when(stage != 2)
        def _():
            hop = stage - stage // 3
            self.to_x(hop, at, stage).start()
            self.to_y(hop, at, stage).start()

    def advance(self, step):
        @pl.when(step < self.steps)
        def _():
            self.compute(step)

        @pl.when(jnp.logical_and(step > 0, step <= self.steps))
        def _():
            self.finish(step - 1)

    def run(self, hook=None):
        def body(step, _):
            self.advance(step)

            if hook:
                hook(step)
            return 0

        lax.fori_loop(0, self.steps + 1, body, 0)
        return self.steps + 1

    def end(self, emit):
        def last(at, _):
            values = []
            for half in range(2):
                xs, ys = (1, 2) if half == 0 else (2, 1)
                self.to_x(xs, at).wait_recv()
                self.to_y(ys, at).wait_recv()
                values.append(self.held[2, half, at].astype(jnp.float32) + self.from_x[xs, at].astype(jnp.float32)
                              + self.from_y[ys, at].astype(jnp.float32))
            emit(at, *values)
            for hop in range(3):
                self.to_x(hop, at).wait_send()
                self.to_y(hop, at).wait_send()
            return 0

        lax.fori_loop(0, self.counts, last, 0)

        def drain(at, _):
            for stream in range(2):
                self.to_sib(self.steps - self.ring + at, stream).wait_send()
            return 0

        lax.fori_loop(0, self.ring, drain, 0)


def reduce_scratch(counts, rows, width, ring=4):
    low, dma = jnp.bfloat16, pltpu.SemaphoreType.DMA
    block = pltpu.VMEM((4, 2, counts, rows, width), low)
    landed = pltpu.VMEM((3, counts, rows, width), low)
    sent = pltpu.VMEM((ring, 2, rows, width), low)
    return [block, sent, block, landed, landed] + [dma((4, 2, counts))] * 2 + [dma((3, counts))] * 4


class Spread:
    def __init__(self, here, counts, refs):
        self.counts = counts
        self.got = refs[0]
        self.x_sems, self.y_sems, self.sib_sems = refs[1:3], refs[3:5], refs[5:7]
        self.core = here.core
        self.sib, self.xdev, self.ydev = here.device(0, 1), here.device(1, 0), here.device(2, 0)

    def slot(self, across, half, at):
        return self.got.at[across, self.core, half, at]

    def x_copy(self, hop, at):
        half = jnp.minimum(hop, 1)
        src = self.slot(2 * (hop // 2), half, at)
        dst = self.slot(1 + 2 * (hop // 2), half, at)
        return remote(src, dst, self.x_sems[0].at[hop, at], self.x_sems[1].at[hop, at], self.xdev)

    def y_copy(self, hop, at):
        half = 1 - jnp.minimum(hop, 1)
        src = self.slot(hop // 2, half, at)
        dst = self.slot(2 + hop // 2, half, at)
        return remote(src, dst, self.y_sems[0].at[hop, at], self.y_sems[1].at[hop, at], self.ydev)

    def streams(self, stage):
        some, last, late = jnp.minimum(stage, 1), stage // 3, stage // 2
        return (some + 2 * last, late), (2 * some + last, 1 - late)

    def block(self, at):
        x_stream, y_stream = self.streams(at // 4)
        second = at // 2 % 2
        across = x_stream[0] + second * (y_stream[0] - x_stream[0])
        half = x_stream[1] + second * (y_stream[1] - x_stream[1])
        return across, at % 2, half

    def begin_rows(self):
        for hop in range(2):
            self.x_copy(hop, 0).start()
            self.y_copy(hop, 0).start()
        for stream in range(2):
            self.sib_copy(0, stream, 0).start()

    def receive_rows(self, step):
        stage = step // 4

        @pl.when(jnp.logical_and(step % 4 == 0, jnp.logical_and(stage > 0, stage < 4)))
        def _():
            self.x_copy(stage - 1, 0).wait_recv()
            self.sib_copy(stage, 0, 0).start()
            self.y_copy(stage - 1, 0).wait_recv()
            self.sib_copy(stage, 1, 0).start()

        @pl.when(step == 4)
        def _():
            self.x_copy(2, 0).start()
            self.y_copy(2, 0).start()

        for stream in range(2):
            @pl.when(jnp.logical_and(step % 4 == 2 * stream, step < 16))
            def _(stream=stream):
                self.sib_copy(stage, stream, 0).wait_recv()

    def sib_copy(self, stage, stream, at):
        across, half = self.streams(stage)[stream]
        slot = self.slot(across, half, at)
        spot = (stage, stream, at)
        return remote(slot, slot, self.sib_sems[0].at[spot], self.sib_sems[1].at[spot], self.sib)

    def begin(self):
        def first(at, _):
            self.x_copy(0, at).start()
            self.y_copy(0, at).start()
            return 0

        def own(at, _):
            self.sib_copy(0, 0, at).start()
            self.sib_copy(0, 1, at).start()
            return 0

        lax.fori_loop(0, self.counts, first, 0)
        lax.fori_loop(0, self.counts, own, 0)

    def run(self, blocks, hook=None, done=None):
        counts = self.counts

        def body(step, _):
            stage, at = step // counts, step % counts

            @pl.when(jnp.logical_and(stage > 0, stage < 4))
            def _():
                self.x_copy(stage - 1, at).wait_recv()
                self.sib_copy(stage, 0, at).start()
                self.y_copy(stage - 1, at).wait_recv()
                self.sib_copy(stage, 1, at).start()

            @pl.when(jnp.logical_and(stage > 0, stage < 3))
            def _():
                self.x_copy(stage, at).start()
                self.y_copy(stage, at).start()

            @pl.when(step > 0)
            def _():
                old, spot = (step - 1) // counts, (step - 1) % counts
                for stream, (across, half) in enumerate(self.streams(old)):
                    self.sib_copy(old, stream, spot).wait_recv()
                    blocks(across, half, spot)
                if done:
                    done(old, spot)

            if hook:
                hook(step)
            return 0

        lax.fori_loop(0, 4 * counts + 1, body, 0)
        return 4 * counts + 1

    def end(self):
        def drain(at, _):
            for hop in range(3):
                self.x_copy(hop, at).wait_send()
                self.y_copy(hop, at).wait_send()
            for stage in range(4):
                self.sib_copy(stage, 0, at).wait_send()
                self.sib_copy(stage, 1, at).wait_send()
            return 0

        lax.fori_loop(0, self.counts, drain, 0)


def spread_scratch(counts, rows, width):
    dma = pltpu.SemaphoreType.DMA
    return [pltpu.VMEM((4, 2, 2, counts, rows, width), jnp.bfloat16)] + [dma((3, counts))] * 4 + [
        dma((4, 2, counts))] * 2


def row_span(here, across, other, rows):
    return pl.ds(pl.multiple_of(here.shard(across, other) * rows, rows), rows)


def dot_nt(left, right):
    return lax.dot_general(left, right, (((1,), (1,)), ((), ())), preferred_element_type=jnp.float32)


def dot_tn(left, right):
    return lax.dot_general(left, right, (((0,), (0,)), ((), ())), preferred_element_type=jnp.float32)


def dot_nn(left, right):
    return jnp.dot(left, right, preferred_element_type=jnp.float32)


def products(here, act, weight, nt, rows, width, counts):
    def product(across, other, half, at):
        cols = pl.ds(pl.multiple_of((half * counts + at) * width, width), width)
        block = act[row_span(here, across, other, rows), :]
        return dot_nt(block, weight[cols, :]) if nt else dot_nn(block, weight[:, cols])

    return product


def diagonal():
    return (lax.broadcasted_iota(jnp.int32, (LANES, LANES), 0) ==
            lax.broadcasted_iota(jnp.int32, (LANES, LANES), 1)).astype(jnp.float32)


def to_tile(tile, first, column, eye):
    for at in range(column.shape[0] // LANES):
        spread = column[at * LANES : (at + 1) * LANES, :] * eye
        tile[first + at : first + at + 1, :] = jnp.sum(spread, axis=0, keepdims=True)


def from_tile(row, eye):
    return jnp.sum(eye * row, axis=1, keepdims=True)


def make_tables(here, rows, segs, cos, sin, mask):
    eye = diagonal()
    tiles = rows // LANES
    freqs = jnp.exp(lax.broadcasted_iota(jnp.int32, (1, LANES), 1).astype(jnp.float32) * (-math.log(10000.0) / LANES))
    lane = lax.broadcasted_iota(jnp.int32, (1, LANES), 1)
    line = lax.broadcasted_iota(jnp.int32, (LANES, 1), 0)

    def ids_of(row):
        return segs[2:3, pl.ds(pl.multiple_of(row * LANES, LANES), LANES)]

    def row_of(side, at):
        return ((here.seq + side) % 2) * tiles + at

    for side in range(2):
        for at in range(tiles):
            row = row_of(side, at)
            ids = from_tile(ids_of(row), eye)
            before = jnp.zeros((LANES, 1), jnp.float32)
            for other in range(2 * tiles):
                smaller = ids_of(other) < ids
                before += jnp.sum(smaller.astype(jnp.float32), axis=-1, keepdims=True)
            index = row * LANES + line
            angles = (index.astype(jnp.float32) - before) * freqs
            span = slice(at * LANES, (at + 1) * LANES)
            cos[side, span, :] = jnp.cos(angles)
            sin[side, span, :] = jnp.sin(angles)
            if side == 0:
                for key_side in range(2):
                    for key_at in range(tiles):
                        key_row = row_of(key_side, key_at)
                        same = ids_of(key_row) == ids
                        allowed = jnp.logical_and(same, key_row * LANES + lane <= index)
                        first = key_side * rows + key_at * LANES
                        mask[span, first : first + LANES] = allowed.astype(jnp.float32)


def open_kernel(rows, width, counts, tokens, gain_one, gain_two, ids, w_query, kv_weight, cot, qkv, x_low, act_t, w_qkv, rms, cos, sin,
                mask, g_col, gain, *refs, early):
    here = Place()
    gain[...] = jnp.zeros_like(gain)
    gain[0:1, :] = gain_one[...].astype(jnp.float32).reshape(1, -1)
    gain[1:2, :] = gain_two[...].astype(jnp.float32).reshape(1, -1)
    gain[2:3, :] = ids[...].astype(jnp.float32).reshape(1, -1)
    early[7].start()
    cols, segs = gain.shape[1], gain
    act, turn_send, turn_recv, local_sems, cot_part, g_send, g_recv, z_send, z_recv = refs[:9]
    share = rows // 4
    me = here.shard(0, 0)
    own_rows = pl.ds(pl.multiple_of(me * rows, rows), rows)

    def turn_copy(at):
        across, other = turned(at)
        first = pl.multiple_of(here.shard(across, other) * cols, cols)
        return remote(tokens.at[:, pl.ds(first, cols)], x_low.at[own_rows, :], turn_send.at[at], turn_recv.at[at],
                      here.device(across, other))

    wide = w_query.shape[1]
    local = [
        pltpu.make_async_copy(w_query, w_qkv.at[:, :wide], local_sems.at[0]),
        pltpu.make_async_copy(kv_weight, w_qkv.at[:, wide:], local_sems.at[1]),
        pltpu.make_async_copy(tokens.at[:, pl.ds(pl.multiple_of(me * cols, cols), cols)], x_low.at[own_rows, :],
                              local_sems.at[2]),
    ]
    load = pltpu.make_async_copy(cot.at[pl.ds(pl.multiple_of(here.z * share, share), share), :], cot_part,
                                 local_sems.at[3])
    load.start()
    for copy in local:
        copy.start()

    def g_copy(at):
        across, other = turned(at)
        first = pl.multiple_of(here.shard(across, other) * cols, cols)
        return remote(cot_part.at[:, pl.ds(first, cols)], g_col.at[me, here.z], g_send.at[at], g_recv.at[at],
                      here.device(across, other))

    def own_part():
        return pltpu.make_async_copy(cot_part.at[:, pl.ds(pl.multiple_of(me * cols, cols), cols)],
                                     g_col.at[me, here.z], local_sems.at[4])

    def quarter(way, at, step, peer):
        spot = g_col.at[:, at]
        return remote(spot, spot, z_send.at[way, step], z_recv.at[way, step], (here.dp, here.seq, here.z + peer))

    def pass_on(step):
        @pl.when(jnp.logical_and(here.z < 3, here.z >= step))
        def _():
            quarter(0, here.z - step, step, 1).start()

        @pl.when(jnp.logical_and(here.z > 0, here.z <= 3 - step))
        def _():
            quarter(1, here.z + step, step, -1).start()

    def take_quarters(step):
        @pl.when(here.z > step)
        def _():
            quarter(0, here.z - 1 - step, step, -1).wait_recv()

        @pl.when(here.z < 3 - step)
        def _():
            quarter(1, here.z + 1 + step, step, 1).wait_recv()

    greet(here, slice_peers(here), True)
    load.wait()
    own_part().start()
    for at in range(7):
        g_copy(at).start()
    for at in range(7):
        turn_copy(at).start()
    for copy in local:
        copy.wait()
    early[2].start()

    def squares(at, total):
        values = tokens[:, pl.ds(pl.multiple_of(at * cols, cols), cols)].astype(jnp.float32)
        return total + jnp.sum(values * values, axis=-1, keepdims=True)

    total = lax.fori_loop(0, 8, squares, jnp.zeros((rows, 1), jnp.float32))
    rms[...] = jnp.broadcast_to(lax.rsqrt(total / (8 * cols) + EPS), rms.shape)
    make_tables(here, rows, segs, cos, sin, mask)
    for at in (3, 4, 5):
        early[at].start()

    def prepare(first, count):
        def one(step, _):
            at = first + step
            span = row_span(here, *turned(at), rows)
            value = (x_low[span, :].astype(jnp.float32) * gain[0:1, :]).astype(act.dtype)
            act[span, :] = value
            return 0

        lax.fori_loop(0, count, one, 0)

    def before(stop):
        first, count = ((0, 2), (2, 4), (6, 2))[stop]
        if stop == 0:
            own_part().wait()
            for at in range(7):
                g_copy(at).wait_recv()
        else:
            take_quarters(stop - 1)
        pass_on(stop)
        for at in range(first, min(first + count, 7)):
            turn_copy(at).wait_recv()
        prepare(first, count)
        if stop == 2:
            early[0].start()

    def flip():
        def one(shard, _):
            span = pl.ds(pl.multiple_of(shard * rows, rows), rows)
            act_t[:, span] = act[span, :].T
            return 0

        lax.fori_loop(0, 8, one, 0)

    product = products(here, act, w_qkv, False, rows, width, counts)
    total = Reduce(here, counts, product, refs[9:20], before)
    total.run()
    flip()
    early[1].start()

    def emit(at, first, second):
        for half, value in enumerate((first, second)):
            qkv[:, pl.ds(pl.multiple_of((half * counts + at) * width, width), width)] = value

    total.end(emit)
    take_quarters(2)
    early[6].start()
    for at in range(7):
        turn_copy(at).wait_send()
        g_copy(at).wait_send()
    for step in range(3):
        @pl.when(jnp.logical_and(here.z < 3, here.z >= step))
        def _(step=step):
            quarter(0, here.z - step, step, 1).wait_send()

        @pl.when(jnp.logical_and(here.z > 0, here.z <= 3 - step))
        def _(step=step):
            quarter(1, here.z + step, step, -1).wait_send()


def opening(tokens, gain_one, gain_two, ids, w_query, kv_weight, cot, cid, width=256):
    rows = tokens.shape[0]
    cols, wide = w_query.shape
    every = wide + kv_weight.shape[1]
    counts = every // (2 * width)
    low, f32 = jnp.bfloat16, jnp.float32
    dma = pltpu.SemaphoreType.DMA
    vm = pl.BlockSpec(memory_space=pltpu.VMEM)
    hbm = pl.BlockSpec(memory_space=pl.ANY)
    out_shape = [
        jax.ShapeDtypeStruct((rows, every), f32),
        jax.ShapeDtypeStruct((8 * rows, cols), low),
        jax.ShapeDtypeStruct((cols, 8 * rows), low),
        jax.ShapeDtypeStruct((cols, every), low),
        jax.ShapeDtypeStruct((rows, LANES), f32),
        jax.ShapeDtypeStruct((2, rows, LANES), f32),
        jax.ShapeDtypeStruct((2, rows, LANES), f32),
        jax.ShapeDtypeStruct((rows, 2 * rows), f32),
        jax.ShapeDtypeStruct((8, 4, rows // 4, cols), low),
        jax.ShapeDtypeStruct((8, cols), f32),
    ]
    scratch = [
        pltpu.VMEM((8 * rows, cols), low), dma((7,)), dma((7,)), dma((5,)),
        pltpu.VMEM((rows // 4, 8 * cols), low), dma((7,)), dma((7,)), dma((2, 3)), dma((2, 3)),
    ]
    scratch += reduce_scratch(counts, rows, width)
    kernel = functools.partial(open_kernel, rows, width, counts)
    return kernel_call(kernel, out_shape, [tokens, gain_one, gain_two, ids, w_query, kv_weight, cot],
                       [vm, vm, vm, vm, hbm, hbm, hbm], scratch, cid, "open",
                       early=(1, 2, 3, 5, 6, 7, 8, 9))


def ffn_kernel(rows, width, counts, x_low, attn, gain, w_gate, w_up, d_hidden, hidden, d_gate, d_up, act_t, tile_out,
               *refs, late, early):
    here = Place()
    cols = gain.shape[1]
    act, weight, tiny_own, tiny_all, tiny_send, tiny_recv, dots, local_sems = refs[:8]
    tiny = Tiny(here, tiny_own, tiny_all, (tiny_send, tiny_recv), True)
    half_cols = counts * width
    local = [
        pltpu.make_async_copy(w_gate, weight.at[:, :half_cols], local_sems.at[0]),
        pltpu.make_async_copy(w_up, weight.at[:, half_cols:], local_sems.at[1]),
    ]
    for copy in local:
        copy.start()
    eye = diagonal()
    tiny_own[...] = jnp.zeros_like(tiny_own)

    def prepare(number, _):
        shard = here.shard(*turned(number))
        for at in range(rows // LANES):
            span = pl.ds(pl.multiple_of(shard * rows + at * LANES, LANES), LANES)
            resid = x_low[span, :].astype(jnp.float32) + attn[span, :].astype(jnp.float32)
            act[span, :] = (resid * gain[1:2, :]).astype(act.dtype)
            square = jnp.sum(resid * resid, axis=-1, keepdims=True)
            tiny_own[shard, at : at + 1, :] = jnp.sum(square * eye, axis=0, keepdims=True)
        return 0

    def before(stop):
        if stop == 1:
            lax.fori_loop(2, 6, prepare, 0)
        if stop == 2:
            lax.fori_loop(6, 8, prepare, 0)
            tiny.begin()

    lax.fori_loop(0, 2, prepare, 0)
    greet(here, slice_peers(here))
    for copy in local:
        copy.wait()
    product = products(here, act, weight, False, rows, width, counts)
    total = Reduce(here, counts, product, refs[8:19], before)
    total.run()

    def flip(shard, _):
        span = pl.ds(pl.multiple_of(shard * rows, rows), rows)
        act_t[:, span] = act[span, :].T
        return 0

    lax.fori_loop(0, 8, flip, 0)
    early[0].start()
    tiny.end()
    tiles = rows // LANES
    mean = [from_tile(jnp.sum(tiny_all[:, at, :], axis=0, keepdims=True), eye) for at in range(tiles)]
    scale = lax.rsqrt(jnp.concatenate(mean, axis=0) / (8 * cols) + EPS)
    dots[...] = jnp.zeros_like(dots)
    late[0].wait()
    coeff = math.sqrt(2.0 / math.pi)

    def emit(at, first, second):
        span = pl.ds(pl.multiple_of(at * width, width), width)
        gate, up = first * scale, second * scale
        inner = jnp.tanh(coeff * (gate + 0.044715 * (gate * gate * gate)))
        gelu = 0.5 * gate * (1.0 + inner)
        slope = 0.5 * (1.0 + inner) + 0.5 * gate * (1.0 - inner * inner) * (
            coeff * (1.0 + 3.0 * 0.044715 * gate * gate))
        cot = d_hidden[:, span]
        hidden[:, span] = (gelu * up).astype(hidden.dtype)
        back_gate, back_up = cot * up * slope, cot * gelu
        d_gate[:, span] = (back_gate * scale).astype(d_gate.dtype)
        d_up[:, span] = (back_up * scale).astype(d_up.dtype)
        dots[...] += jnp.sum(back_gate * gate + back_up * up, axis=-1, keepdims=True)

    total.end(emit)
    tile_out[...] = jnp.zeros_like(tile_out)
    to_tile(tile_out, 0, dots[...] * (scale * scale * (1.0 / (8 * cols))), eye)


def ffn_scatter(x_low, attn, gain, w_gate, w_up, d_hidden, cid, width=512):
    rows, half = d_hidden.shape
    cols = gain.shape[1]
    counts = half // width
    low, f32 = jnp.bfloat16, jnp.float32
    dma = pltpu.SemaphoreType.DMA
    vm = pl.BlockSpec(memory_space=pltpu.VMEM)
    hbm = pl.BlockSpec(memory_space=pl.ANY)
    out_shape = [jax.ShapeDtypeStruct((rows, half), low)] * 3 + [
        jax.ShapeDtypeStruct((cols, 8 * rows), low),
        jax.ShapeDtypeStruct((8, LANES), f32),
    ]
    scratch = [
        pltpu.VMEM((8 * rows, cols), low),
        pltpu.VMEM((cols, 2 * half), low),
        pltpu.VMEM((8, 8, LANES), f32),
        pltpu.VMEM((8, 8, LANES), f32),
        dma((7,)), dma((7,)),
        pltpu.VMEM((rows, 1), f32),
        dma((2,)),
    ] + reduce_scratch(counts, rows, width)
    kernel = functools.partial(ffn_kernel, rows, width, counts)
    return kernel_call(kernel, out_shape, [x_low, attn, gain, w_gate, w_up, d_hidden], [vm, vm, vm, hbm, hbm, vm],
                       scratch, cid, "ffn", late=(5,), early=(3,))


def load_own(spread, payload, width, counts, sems):
    copies = []
    for half in range(2):
        for at in range(counts):
            first = at * width + (half * counts * width if len(payload) == 1 else 0)
            src = payload[half % len(payload)].at[:, first : first + width]
            copies.append(pltpu.make_async_copy(src, spread.slot(0, half, at), sems.at[half, at]))
    return copies


def chip_place(here, per):
    def place(at):
        return here.shard(at // (2 * per), at // per % 2) * per + at % per

    return place


def back_kernel(rows, width, counts, act_t, w_gate, w_up, d_gate, d_up, dots, x_low, attn, gain, d_norm, gain_grad,
                grad_gate, grad_up, *refs, late):
    here = Place()
    spread = Spread(here, counts, refs[:7])
    tiny_all, tiny_send, tiny_recv, own_sems, weight, sums, grads, staged, local_sems, out_sems = refs[7:17]
    contrib, rest, rest_sems = refs[17:20]
    line = Line(here, 4, [contrib, d_norm] + list(refs[20:]), chip_place(here, 2))
    tiny = Tiny(here, dots, tiny_all, (tiny_send, tiny_recv), False)
    half_cols = counts * width
    local = [
        pltpu.make_async_copy(w_gate, weight.at[:, :half_cols], local_sems.at[0]),
        pltpu.make_async_copy(w_up, weight.at[:, half_cols:], local_sems.at[1]),
    ]
    own = load_own(spread, (d_gate, d_up), width, counts, own_sems)
    for copy in own + local:
        copy.start()
    greet(here, tiny.peers, True)
    for copy in own:
        copy.wait()
    tiny.begin()
    spread.begin()
    sums[...] = jnp.zeros_like(sums)
    for copy in local + late:
        copy.wait()

    def columns(half, at):
        return pl.ds(pl.multiple_of((half * counts + at) * width, width), width)

    def clear(at, _):
        grads[:, columns(0, at)] = jnp.zeros((grads.shape[0], width), jnp.float32)
        return 0

    lax.fori_loop(0, 2 * counts, clear, 0)

    def blocks(across, half, at):
        cols = columns(half, at)
        gained = grads[:, cols]
        for other in range(2):
            row = row_span(here, across, other, rows)
            block = spread.got[across, (spread.core + other) % 2, half, at]
            sums[row, :] += dot_nt(block, weight[:, cols])
            gained = gained + dot_nn(act_t[:, row], block)
        grads[:, cols] = gained

    def leave(half, at):
        spot = pl.ds(pl.multiple_of(at * width, width), width)
        return pltpu.make_async_copy(staged.at[half], (grad_gate, grad_up)[half].at[:, spot],
                                     out_sems.at[half, at])

    eye = diagonal()
    gain_grad[...] = jnp.zeros_like(gain_grad)

    def close_chip(chip, target):
        def close_shard(other, _):
            shard = here.shard(chip, other)
            span = pl.ds(pl.multiple_of(shard * rows, rows), rows)
            loads = [pltpu.make_async_copy(src.at[span, :], rest.at[at], rest_sems.at[at])
                     for at, src in enumerate((x_low, attn))]
            for copy in loads:
                copy.start()
            for copy in loads:
                copy.wait()
            for at in range(rows // LANES):
                span = pl.ds(pl.multiple_of(shard * rows + at * LANES, LANES), LANES)
                piece = slice(at * LANES, (at + 1) * LANES)
                dot = from_tile(tiny_all[shard, at : at + 1, :], eye)
                resid = rest[0, piece, :].astype(jnp.float32) + rest[1, piece, :].astype(jnp.float32)
                value = sums[span, :]
                target[span, :] = (value * gain[1:2, :] - resid * dot).astype(target.dtype)
                gain_grad[...] += jnp.sum(value * resid, axis=0, keepdims=True)
            return 0

        lax.fori_loop(0, 2, close_shard, 0)

    def done(stage, at):
        @pl.when(jnp.logical_and(stage == 3, at > 0))
        def _():
            leave(0, at - 1).wait()
            leave(1, at - 1).wait()

        @pl.when(stage == 3)
        def _():
            for half in range(2):
                staged[half] = grads[:, columns(half, at)].astype(staged.dtype)
            leave(0, at).start()
            leave(1, at).start()

        @pl.when(jnp.logical_and(at == counts - 1, stage == 0))
        def _():
            close_chip(0, contrib)
            line.launch(0, 4)

        @pl.when(jnp.logical_and(at == counts - 1, stage == 2))
        def _():
            lax.fori_loop(1, 3, lambda chip, _: (close_chip(chip, d_norm), 0)[1], 0)

    def hook(step):
        @pl.when(jnp.logical_and(step >= counts, step < counts + 6))
        def _():
            line.step(step - counts)

    tiny.end()
    spread.run(blocks, hook, done)
    close_chip(3, d_norm)
    line.settle()
    spread.end()

    def drain(at, _):
        leave(0, at).wait()
        leave(1, at).wait()
        return 0

    lax.fori_loop(counts - 1, counts, drain, 0)


def back_gather(act_t, w_gate, w_up, d_gate, d_up, dots, x_low, attn, gain, cid, width=512):
    cols, total = act_t.shape
    rows, half = d_gate.shape
    counts = half // width
    low, f32 = jnp.bfloat16, jnp.float32
    dma = pltpu.SemaphoreType.DMA
    vm = pl.BlockSpec(memory_space=pltpu.VMEM)
    hbm = pl.BlockSpec(memory_space=pl.ANY)
    out_shape = [
        jax.ShapeDtypeStruct((total, cols), low),
        jax.ShapeDtypeStruct((1, cols), f32),
        jax.ShapeDtypeStruct((cols, half), low),
        jax.ShapeDtypeStruct((cols, half), low),
    ]
    scratch = spread_scratch(counts, rows, width) + [
        pltpu.VMEM((8, 8, LANES), f32), dma((7,)), dma((7,)), dma((2, counts)),
        pltpu.VMEM((cols, 2 * half), low),
        pltpu.VMEM((total, cols), f32),
        pltpu.VMEM((cols, 2 * half), f32),
        pltpu.VMEM((2, cols, width), low),
        dma((2,)), dma((2, counts)),
        pltpu.VMEM((total, cols), low),
        pltpu.VMEM((2, rows, cols), low),
        dma((2,)),
    ] + line_scratch(4, (4 * rows // 2, cols), low)
    operands = [act_t, w_gate, w_up, d_gate, d_up, dots, x_low, attn, gain]
    kernel = functools.partial(back_kernel, rows, width, counts)
    return kernel_call(kernel, out_shape, operands, [vm] + [hbm] * 4 + [vm, hbm, hbm, vm], scratch, cid, "back",
                       [vm, vm, hbm, hbm], (0,))


def down_kernel(rows, width, counts, cot, weight, hidden, d_norm, ffn, d_attn, grad, *refs, late, early):
    here = Place()
    spread = Spread(here, counts, refs[:7])
    own_sems, sums, grads, staged, out_sems, norm_out = refs[7:13]
    place = chip_place(here, 2)
    norm_line = Line(here, 12, [d_norm, norm_out] + list(refs[13:]), lambda at: place(at + 4))
    own = load_own(spread, (hidden,), width, counts, own_sems)
    for copy in own:
        copy.start()
    greet(here, slice_peers(here), True)
    norm_line.begin()
    for copy in own:
        copy.wait()
    spread.begin()
    sums[...] = jnp.zeros_like(sums)
    grads[...] = jnp.zeros_like(grads)
    for copy in late:
        copy.wait()

    def columns(half, at):
        return pl.ds(pl.multiple_of((half * counts + at) * width, width), width)

    def blocks(across, half, at):
        cols = columns(half, at)
        gained = grads[cols, :]
        for other in range(2):
            row = row_span(here, across, other, rows)
            block = spread.got[across, (spread.core + other) % 2, half, at]
            sums[row, :] += dot_nn(block, weight[cols, :])
            gained = gained + dot_tn(block, cot[row, :])
        grads[cols, :] = gained

    def leave(half, at):
        return pltpu.make_async_copy(staged.at[at % 2, half], grad.at[columns(half, at), :], out_sems.at[half, at])

    def done(stage, at):
        @pl.when(jnp.logical_and(stage == 3, at > 1))
        def _():
            leave(0, at - 2).wait()
            leave(1, at - 2).wait()

        @pl.when(stage == 3)
        def _():
            for half in range(2):
                staged[at % 2, half] = grads[columns(half, at), :].astype(staged.dtype)
            leave(0, at).start()
            leave(1, at).start()


    def hook(step):
        @pl.when(step % 3 < 2)
        def _():
            norm_line.step(step // 3 * 2 + step % 3)

    spread.run(blocks, hook, done)
    ffn[...] = sums[...].astype(ffn.dtype)
    early[0].start()
    norm_line.settle()

    def add_norm(at, _):
        def add(source):
            span = row_span(here, at // 2, at % 2, rows)
            d_attn[span, :] = (cot[span, :].astype(jnp.float32) + source[span, :].astype(jnp.float32)).astype(
                d_attn.dtype)

        @pl.when(at < 2)
        def _():
            add(d_norm)

        @pl.when(at >= 2)
        def _():
            add(norm_out)
        return 0

    lax.fori_loop(0, 8, add_norm, 0)
    spread.end()

    def drain(at, _):
        leave(0, at).wait()
        leave(1, at).wait()
        return 0

    lax.fori_loop(counts - 2, counts, drain, 0)


def down_gather(cot, weight, hidden, d_norm, cid, width=256):
    total, cols = cot.shape
    rows, every = hidden.shape
    counts = every // (2 * width)
    low, f32 = jnp.bfloat16, jnp.float32
    dma = pltpu.SemaphoreType.DMA
    vm = pl.BlockSpec(memory_space=pltpu.VMEM)
    hbm = pl.BlockSpec(memory_space=pl.ANY)
    out_shape = [
        jax.ShapeDtypeStruct((total, cols), low),
        jax.ShapeDtypeStruct((total, cols), low),
        jax.ShapeDtypeStruct(weight.shape, low),
    ]
    scratch = spread_scratch(counts, rows, width) + [
        dma((2, counts)),
        pltpu.VMEM((total, cols), f32),
        pltpu.VMEM(weight.shape, f32),
        pltpu.VMEM((2, 2, width, cols), low),
        dma((2, counts)),
        pltpu.VMEM((total, cols), low),
    ] + line_scratch(12, (12 * rows // 2, cols), low)
    kernel = functools.partial(down_kernel, rows, width, counts)
    return kernel_call(kernel, out_shape, [cot, weight, hidden, d_norm], [vm, vm, hbm, vm], scratch, cid, "down",
                       [vm, vm, hbm], (0, 1), (0,))


def attend_kernel(rows, heads, cols, width, counts, qkv, rms, cos, sin, mask, w_out, g_col, w_down, attn, mixed_all,
                  kv, probs, queries, pair_rms, d_hidden, *refs, late, early):
    here = Place()
    spread = Spread(here, 1, refs[:7])
    part, pair_sems, tiny_own, tiny_pair, mixed_sems = refs[7:12]
    product = products(here, g_col, w_down, True, rows, width, counts)
    total = Reduce(here, counts, product, refs[12:23])
    piece = rows // 2

    def place(at):
        across, other, half_at = spread.block(at)
        return here.shard(across, other) * 2 + half_at

    line = Line(here, 16, [part, attn] + list(refs[23:]), place)
    got, core = spread.got, here.core
    greet(here, slice_peers(here), True)
    half = HD // 2
    scale = 1.0 / math.sqrt(HD)
    wide = heads * HD

    def rotated(first):
        lead = qkv[:, first : first + half] * rms[...]
        trail = qkv[:, first + half : first + HD] * rms[...]
        return lead * cos[0] - trail * sin[0], trail * cos[0] + lead * sin[0]

    low_k, high_k = rotated(wide)
    kv[0, :, :half] = low_k.astype(kv.dtype)
    kv[0, :, half:HD] = high_k.astype(kv.dtype)
    for at in range(2):
        first = HD + at * half
        kv[0, :, first : first + half] = (qkv[:, wide + first : wide + first + half] * rms[...]).astype(kv.dtype)
    eye = diagonal()
    tiny_own[...] = jnp.zeros_like(tiny_own)
    to_tile(tiny_own, 0, rms[:, :1], eye)
    pair_rms[0] = rms[...]
    pair = remote(kv.at[0], kv.at[1], pair_sems.at[0], pair_sems.at[1], spread.ydev)
    tiny = remote(tiny_own, tiny_pair, pair_sems.at[2], pair_sems.at[3], spread.ydev)
    for head in range(heads):
        if head == 1:
            pair.start()
            tiny.start()
        lead, trail = rotated(head * HD)
        queries[:, head * HD : head * HD + half] = (lead * scale).astype(queries.dtype)
        queries[:, head * HD + half : (head + 1) * HD] = (trail * scale).astype(queries.dtype)
    early[2].start()
    pair.wait()
    early[0].start()
    for copy in late:
        copy.wait()

    def one_head(head, _):
        query = queries[:, pl.ds(pl.multiple_of(head * HD, HD), HD)]
        scores = jnp.concatenate([dot_nt(query, kv[0, :, :HD]), dot_nt(query, kv[1, :, :HD])], axis=1)
        scores = jnp.where(mask[...] > 0, scores, NEG)
        expd = jnp.exp(scores - jnp.max(scores, axis=-1, keepdims=True))
        prob = expd / jnp.sum(expd, axis=-1, keepdims=True)
        probs[head] = prob
        prob_low = prob.astype(jnp.bfloat16)
        mixed = dot_nn(prob_low[:, :rows], kv[0, :, HD:]) + dot_nn(prob_low[:, rows:], kv[1, :, HD:])
        span = pl.ds(pl.multiple_of(head * HD, HD), HD)
        for half_at in range(2):
            low_mixed = mixed[half_at * piece : (half_at + 1) * piece, :].astype(got.dtype)
            got[0, core, half_at, 0, :, span] = low_mixed
        return 0

    lax.fori_loop(0, heads, one_head, 0)
    early[1].start()
    spread.begin_rows()

    def mixed_copy(at):
        across, other, half_at = spread.block(at)
        span = pl.ds(pl.multiple_of(place(at) * piece, piece), piece)
        return pltpu.make_async_copy(got.at[across, (core + other) % 2, half_at, 0], mixed_all.at[span, :],
                                     mixed_sems.at[at])

    def one_step(step, _):
        spread.receive_rows(step)

        @pl.when(step < 16)
        def _():
            across, other, half_at = spread.block(step)
            value = dot_nn(got[across, (core + other) % 2, half_at, 0], w_out[...])
            part[pl.ds(pl.multiple_of(place(step) * piece, piece), piece), :] = value.astype(part.dtype)
            mixed_copy(step).start()
            line.launch(step, 1)

        @pl.when(step >= 2)
        def _():
            total.advance(step - 2)

        @pl.when(step >= 4)
        def _():
            line.step(step - 4)
        return 0

    lax.fori_loop(0, 20, one_step, 0)
    line.end(16)
    early[3].start()

    def emit(at, first, second):
        for half_at, value in enumerate((first, second)):
            d_hidden[:, pl.ds(pl.multiple_of((half_at * counts + at) * width, width), width)] = value

    total.end(emit)
    for hop in range(3):
        spread.x_copy(hop, 0).wait_send()
        spread.y_copy(hop, 0).wait_send()
    for stage in range(4):
        for stream in range(2):
            spread.sib_copy(stage, stream, 0).wait_send()
    for at in range(16):
        mixed_copy(at).wait()
    tiny.wait()
    for at in range(rows // LANES):
        values = jnp.broadcast_to(from_tile(tiny_pair[at : at + 1, :], eye), (LANES, LANES))
        pair_rms[1, at * LANES : (at + 1) * LANES, :] = values


def attend(qkv, rms, cos, sin, mask, w_out, g_col, w_down, cid, width=512):
    rows = qkv.shape[0]
    wide, cols = w_out.shape
    heads = wide // HD
    counts = w_down.shape[0] // (2 * width)
    low, f32 = jnp.bfloat16, jnp.float32
    dma = pltpu.SemaphoreType.DMA
    vm = pl.BlockSpec(memory_space=pltpu.VMEM)
    out_shape = [
        jax.ShapeDtypeStruct((8 * rows, cols), low),
        jax.ShapeDtypeStruct((8 * rows, wide), low),
        jax.ShapeDtypeStruct((2, rows, 2 * HD), low),
        jax.ShapeDtypeStruct((heads, rows, 2 * rows), f32),
        jax.ShapeDtypeStruct((rows, wide), low),
        jax.ShapeDtypeStruct((2,) + rms.shape, f32),
        jax.ShapeDtypeStruct((rows, w_down.shape[0]), f32),
    ]
    scratch = spread_scratch(1, rows // 2, wide) + [
        pltpu.VMEM((8 * rows, cols), low), dma((4,)),
        pltpu.VMEM((8, LANES), f32), pltpu.VMEM((8, LANES), f32), dma((16,)),
    ] + reduce_scratch(counts, rows, width) + line_scratch(16, (8 * rows, cols), low)
    kernel = functools.partial(attend_kernel, rows, heads, cols, width, counts)
    operands = [qkv, rms, cos, sin, mask, w_out, g_col, w_down]
    out_specs = [vm, pl.BlockSpec(memory_space=pl.ANY)] + [vm] * 5
    return kernel_call(kernel, out_shape, operands, [vm] * 8, scratch, cid, "attend", out_specs, (4, 5, 6, 7), (2, 3, 4, 0))


def tail_kernel(rows, heads, per, d_attn, w_out, queries, kv, probs, rms, cos, sin, act_t, w_qkv, ffn, x_low,
                attn, gain, gain_grad, mixed_all, d_tok, out, grad_query, grad_out, kv_sum, gains, *refs, late, early):
    here = Place()
    width = HD
    counts = heads // 2
    part = rows // 2
    refs = list(refs)
    line_counts = 8 * per
    cols = d_attn.shape[1]
    extra = cols // (rows // per)

    def take(count):
        taken_refs = refs[:count]
        del refs[:count]
        return taken_refs

    total_refs = take(11)
    spread = Spread(here, 1, take(7))
    d_mixed, tiny_own, tiny_all, d_kv, give, taken, give_sems, tiny_send, tiny_recv = take(9)
    grad, grad_mixed, gain_sum, tile, tile_send, tile_recv, put_sems, local_sems, mixed_two, mixed_sems = take(10)

    def far(at):
        return at // (2 * per), at // per % 2

    def near(at):
        return spread.block(jnp.minimum(at, line_counts - 1))

    def place_ffn(at):
        return here.shard(*far(at)) * per + at % per

    def place_tok(at):
        across, other, half_at = near(at)
        return jnp.where(at < line_counts, here.shard(across, other) * per + half_at, at)

    gain_tiles, ffn_sum, leaving = take(3)
    by_chip = chip_place(here, per)
    line = Line(here, line_counts, [ffn, ffn_sum] + take(8), by_chip)
    contrib, summed = take(2)
    line_tok = Line(here, line_counts + extra, [contrib, summed] + take(8), place_tok)
    tiny = Tiny(here, tiny_own, tiny_all, (tiny_send, tiny_recv), False)
    got, core = spread.got, here.core
    product = products(here, d_attn, w_out, True, rows, width, counts)
    total = Reduce(here, counts, product, total_refs)
    greet(here, tiny.peers, True)
    line.begin()
    grad_mixed[...] = jnp.zeros_like(grad_mixed)

    def mixed_copy(step):
        span = pl.ds(pl.multiple_of(step * rows, rows), rows)
        return pltpu.make_async_copy(mixed_all.at[span, :], mixed_two.at[step % 2], mixed_sems.at[step % 2])

    mixed_copy(0).start()

    def beside(step):
        line.step(step)

        @pl.when(step < 8)
        def _():
            span = pl.ds(pl.multiple_of(step * rows, rows), rows)
            mixed_copy(step).wait()

            @pl.when(step < 7)
            def _():
                mixed_copy(step + 1).start()

            grad_mixed[...] += dot_tn(mixed_two[step % 2], d_attn[span, :])

    done = total.run(beside)
    grad_out[...] = grad_mixed[...].astype(grad_out.dtype)
    early[1].start()

    def land(at, first, second):
        for half_at, value in enumerate((first, second)):
            d_mixed[:, pl.ds(pl.multiple_of((half_at * counts + at) * width, width), width)] = value.astype(
                d_mixed.dtype)

    total.end(land)
    half = HD // 2
    scale = 1.0 / math.sqrt(HD)
    depth = w_qkv.shape[0] * 8
    d_kv[...] = jnp.zeros_like(d_kv)
    for copy in late:
        copy.wait()

    def one_head(head, dots):
        span = pl.ds(pl.multiple_of(head * HD, HD), HD)
        query = queries[:, span]
        cot = d_mixed[:, span]
        prob = probs[head]
        d_prob = jnp.concatenate([dot_nt(cot, kv[0, :, HD:]), dot_nt(cot, kv[1, :, HD:])], axis=1)
        delta = jnp.sum(prob * d_prob, axis=-1, keepdims=True)
        d_score = (prob * (d_prob - delta)).astype(jnp.bfloat16)
        prob_low = prob.astype(jnp.bfloat16)
        d_query = (dot_nn(d_score[:, :rows], kv[0, :, :HD]) + dot_nn(d_score[:, rows:], kv[1, :, :HD])) * scale
        for side in range(2):
            keys = slice(side * rows, (side + 1) * rows)
            d_kv[side, :, :HD] += dot_tn(d_score[:, keys], query)
            d_kv[side, :, HD:] += dot_tn(prob_low[:, keys], cot)
        dots = dots + jnp.sum(d_query * query.astype(jnp.float32), axis=-1, keepdims=True)
        lead, trail = d_query[:, :half], d_query[:, half:]
        first = ((lead * cos[0] + trail * sin[0]) * rms[0]).astype(got.dtype)
        second = ((trail * cos[0] - lead * sin[0]) * rms[0]).astype(got.dtype)
        line.step(done + head)
        for rows_at in range(2):
            piece = slice(rows_at * part, (rows_at + 1) * part)
            got[0, core, rows_at, 0, :, pl.ds(pl.multiple_of(head * HD, HD), half)] = first[piece, :]
            got[0, core, rows_at, 0, :, pl.ds(pl.multiple_of(head * HD + half, half), half)] = second[piece, :]

        return dots

    dots = lax.fori_loop(0, heads, one_head, jnp.zeros((rows, 1), jnp.float32))
    eye = diagonal()
    tiny_own[...] = jnp.zeros_like(tiny_own)
    for side in (1, 0):
        d_key, d_value = d_kv[side, :, :HD], d_kv[side, :, HD:]
        own = jnp.sum(d_key * kv[side, :, :HD].astype(jnp.float32) +
                      d_value * kv[side, :, HD:].astype(jnp.float32), axis=-1, keepdims=True)
        if side == 0:
            own = own + dots * (1.0 / scale)
        own = own * (rms[side] * rms[side] * (1.0 / depth))
        to_tile(tiny_own, side * (rows // LANES), own, eye)
        lead, trail = d_key[:, :half], d_key[:, half:]
        parts = [(lead * cos[side] + trail * sin[side]) * rms[side],
                 (trail * cos[side] - lead * sin[side]) * rms[side],
                 d_value[:, :half] * rms[side], d_value[:, half:] * rms[side]]
        for at, value in enumerate(parts):
            if side == 1:
                give[:, at * half : (at + 1) * half] = value.astype(give.dtype)
            else:
                d_kv[0, :, at * half : (at + 1) * half] = value
    given = remote(give, taken, give_sems.at[0], give_sems.at[1], spread.ydev)
    given.start()
    grad[...] = jnp.zeros_like(grad)
    line.steps(done + heads, done + heads + 2)
    given.wait()
    for rows_at in range(2):
        piece = slice(rows_at * part, (rows_at + 1) * part)
        value = d_kv[0, piece, :] + taken[piece, :].astype(jnp.float32)
        got[0, core, rows_at, 0, :, heads * HD :] = value.astype(got.dtype)
    tiny.begin()
    spread.begin_rows()
    gain_sum[...] = jnp.zeros_like(gain_sum)
    tiny.end()

    def block_of(at):
        across, other, half_at = near(at)
        shard, partner = here.shard(across, other), here.shard((across + 2) % 4, other)
        block = got[across, (core + other) % 2, half_at, 0]
        first = pl.multiple_of(shard * rows + half_at * part, part)
        for tile_at in range(part // LANES):
            row = pl.ds(pl.multiple_of(first + tile_at * LANES, LANES), LANES)
            low_at = half_at * (part // LANES) + tile_at
            kept = rows // LANES + low_at
            dot = from_tile(tiny_all[shard, pl.ds(low_at, 1), :] + tiny_all[partner, pl.ds(kept, 1), :], eye)
            value = dot_nt(block[tile_at * LANES : (tile_at + 1) * LANES, :], w_qkv[...])
            x_rows = x_low[row, :].astype(jnp.float32)
            contrib[row, :] = (value * gain[0:1, :] - x_rows * dot).astype(contrib.dtype)
            gain_sum[...] += jnp.sum(value * x_rows, axis=0, keepdims=True)
        line_tok.launch(at, 1)

        @pl.when(other == 1)
        def _():
            twin = got[across, core, half_at, 0]
            twin_first = pl.multiple_of(here.shard(across, 0) * rows + half_at * part, part)
            rows_t, twin_t = act_t[:, pl.ds(first, part)], act_t[:, pl.ds(twin_first, part)]
            for at_col in range((heads + 2) * HD // 512):
                span = slice(at_col * 512, (at_col + 1) * 512)
                grad[:, span] += dot_nn(rows_t, block[:, span]) + dot_nn(twin_t, twin[:, span])

    me = here.shard(0, 0)
    columns = pl.ds(pl.multiple_of(me * cols, cols), cols)
    chunk = line.chunk

    def landing(which, at):
        sub = at % per if which == 0 else near(at)[2]
        return (out, d_tok)[which].at[pl.ds(pl.multiple_of(sub * chunk, chunk), chunk), columns]

    def leaver(which, at):
        return (leaving, line_tok.from_end)[which].at[at]

    def put(which, at):
        goal = here.device(*(far(at) if which == 0 else near(at)[:2]))
        return remote(leaver(which, at), landing(which, at), put_sems.at[which, 0, at], put_sems.at[which, 1, at],
                      goal)

    def keep(which, at):
        spot = at % per if which == 0 else near(at)[2]
        return pltpu.make_async_copy(leaver(which, at), landing(which, at), local_sems.at[which, spot])

    def emit(which, at):
        if which == 1:
            row = line_tok.rows(at)
            value = d_attn[row, :].astype(jnp.float32) + summed[row, :].astype(jnp.float32)
            line_tok.from_end[at] = value.astype(out.dtype)
            return
        row = pl.ds(pl.multiple_of(place_ffn(at) * chunk, chunk), chunk)

        def leave(source):
            value = x_low[row, :].astype(jnp.float32) + attn[row, :].astype(jnp.float32)
            leaving[at] = (value + source[row, :].astype(jnp.float32)).astype(out.dtype)

        leave(ffn_sum)

    def is_own(which, at):
        return at < per if which == 0 else jnp.logical_and(at < 4, at % 2 == 0)

    def send(which, at):
        own = is_own(which, at)

        @pl.when(own)
        def _():
            keep(which, at).start()

        @pl.when(jnp.logical_not(own))
        def _():
            put(which, at).start()

    def stage_step(step, _):
        spread.receive_rows(step)

        @pl.when(step < line_counts)
        def _():
            block_of(step)

        @pl.when(step < 3)
        def _():
            line.step(done + heads + 2 + step)

        @pl.when(step >= 4)
        def _():
            line_tok.step(step - 4)

        @pl.when(step > 0)
        def _():
            send(0, step - 1)

        @pl.when(line.inner == 0)
        def _():
            line.up(step).wait_send()
            line.down(step).wait_recv()

        emit(0, step)

        @pl.when(jnp.logical_and(line.inner == 1, step > 7))
        def _():
            send(1, step - 8)

        @pl.when(jnp.logical_and(line.inner == 1, step > 6))
        def _():
            emit(1, step - 7)
        return 0

    lax.fori_loop(0, line_counts, stage_step, 0)
    for half_at in range(cols // (rows // per)):
        span = pl.ds(line_counts * (rows // per) + half_at * (rows // per), rows // per)
        source = slice(half_at * (rows // per), (half_at + 1) * (rows // per))
        contrib[span, :] = grad[source, heads * HD :].astype(contrib.dtype)
    line_tok.launch(line_counts, extra)
    grad_query[...] = grad[:, : heads * HD].astype(grad_query.dtype)
    early[0].start()
    for at in range(cols // LANES):
        tile[at : at + 1, :] = gain_sum[:, at * LANES : (at + 1) * LANES]
        spot = cols // LANES + at
        tile[spot : spot + 1, :] = gain_grad[:, at * LANES : (at + 1) * LANES]

    def tile_copy(step):
        return remote(tile, gain_tiles.at[here.z], tile_send.at[step], tile_recv.at[step],
                      (here.dp, here.seq, (here.z + step + 1) % 4))

    send(0, line_counts - 1)
    line.drain()
    for step in range(3):
        tile_copy(step).start()
    gain_tiles[here.z] = tile[...]

    @pl.when(line.inner == 1)
    def _():
        start = line_counts - 4

        def both(at, _):
            line_tok.step(at)

            @pl.when(at < line_counts + 4)
            def _():
                send(1, at - 4)

            @pl.when(at < line_counts + 3)
            def _():
                emit(1, at - 3)
            return 0

        lax.fori_loop(start, line_counts + extra + 2, both, 0)

        def drain(at, _):
            line_tok.down(at).wait_send()
            return 0

        lax.fori_loop(0, line_counts + extra, drain, 0)

    @pl.when(line.inner == 0)
    def _():
        def arrive(at, _):
            line_tok.up(at).wait_send()
            line_tok.down(at).wait_recv()

            @pl.when(jnp.logical_and(at > 0, at <= line_counts))
            def _():
                send(1, at - 1)

            @pl.when(at < line_counts)
            def _():
                emit(1, at)
            return 0

        lax.fori_loop(0, line_counts + extra, arrive, 0)

    for half_at in range(extra):
        span = pl.ds((line_counts + half_at) * chunk, chunk)
        kv_sum[half_at * chunk : (half_at + 1) * chunk, :] = summed[span, :]
    for hop in range(3):
        spread.x_copy(hop, 0).wait_send()
        spread.y_copy(hop, 0).wait_send()
    for stage in range(4):
        spread.sib_copy(stage, 0, 0).wait_send()
        spread.sib_copy(stage, 1, 0).wait_send()

    for which in range(2):
        def finish(at, _, which=which):
            own = is_own(which, at)

            @pl.when(own)
            def _():
                keep(which, at).wait()

            @pl.when(jnp.logical_not(own))
            def _():
                put(which, at).wait()
            return 0

        lax.fori_loop(0, line_counts, finish, 0)
        if which == 0:
            early[2].start()
    for step in range(3):
        tile_copy(step).wait()
    gains[...] = gain_tiles[0] + gain_tiles[1] + gain_tiles[2] + gain_tiles[3]


def tail(d_attn, w_out, queries, kv, probs, rms, cos, sin, act_t, w_qkv, ffn, x_low, attn, gain, gain_grad,
         mixed_all, cid,
 per=2):
    total, cols = d_attn.shape
    rows = total // 8
    wide = w_out.shape[0]
    heads = wide // HD
    low, f32 = jnp.bfloat16, jnp.float32
    dma = pltpu.SemaphoreType.DMA
    vm = pl.BlockSpec(memory_space=pltpu.VMEM)
    counts = 8 * per
    chunk = rows // per
    extra = cols // chunk
    long = (total + cols, cols)
    out_shape = [
        jax.ShapeDtypeStruct((rows, 8 * cols), low),
        jax.ShapeDtypeStruct((rows, 8 * cols), low),
        jax.ShapeDtypeStruct((cols, wide), low),
        jax.ShapeDtypeStruct(w_out.shape, low),
        jax.ShapeDtypeStruct((cols, 2 * HD), low),
        jax.ShapeDtypeStruct((8, LANES), f32),
    ]
    scratch = reduce_scratch(heads // 2, rows, HD, 2) + spread_scratch(1, rows // 2, wide + 2 * HD)
    scratch += [
        pltpu.VMEM((rows, wide), low),
        pltpu.VMEM((8, LANES), f32),
        pltpu.VMEM((8, 8, LANES), f32),
        pltpu.VMEM((2, rows, 2 * HD), f32),
        pltpu.VMEM((rows, 2 * HD), low),
        pltpu.VMEM((rows, 2 * HD), low),
        dma((2,)), dma((7,)), dma((7,)),
        pltpu.VMEM(w_qkv.shape, f32),
        pltpu.VMEM(w_out.shape, f32),
        pltpu.VMEM((1, cols), f32),
        pltpu.VMEM((8, LANES), f32),
        dma((3,)), dma((3,)), dma((2, 2, counts)), dma((2, per)),
        pltpu.VMEM((2, rows, wide), low), dma((2,)),
        pltpu.VMEM((4, 8, LANES), f32),
        pltpu.VMEM((total, cols), low),
        pltpu.VMEM((counts, chunk, cols), low),
    ] + line_scratch(counts, (total, cols), low)
    scratch += [pltpu.VMEM(long, low), pltpu.VMEM(long, low)] + line_scratch(counts + extra, long, low)
    operands = [d_attn, w_out, queries, kv, probs, rms, cos, sin, act_t, w_qkv, ffn, x_low, attn, gain,
                gain_grad, mixed_all]
    kernel = functools.partial(tail_kernel, rows, heads, per)
    specs = [vm] * (len(operands) - 1) + [pl.BlockSpec(memory_space=pl.ANY)]
    return kernel_call(kernel, out_shape, operands, specs, scratch, cid, "tail",
                       late=(2, 3, 4, 8, 9, 11, 12), early=(2, 3, 1))


LANES = 128


def acts_move(
    tokens, seg_ids, gain_attn, w_query, kv_weight, w_out, gain_ffn, w_gate, w_up, w_down, d_out
):
    qkv, x_low, act_one_t, w_qkv, rms, cos, sin, mask, g_parts, small = opening(
        tokens, gain_attn, gain_ffn, seg_ids, w_query, kv_weight, d_out, 1
    )
    g_low = g_parts.reshape(x_low.shape)
    attn, mixed_all, kv, probs, queries, pair_rms, d_hidden = attend(
        qkv, rms, cos, sin, mask, w_out, g_low, w_down, 2
    )
    hidden, d_gate, d_up, act_two_t, dots = ffn_scatter(x_low, attn, small, w_gate, w_up, d_hidden, 4)
    d_norm, grad_gain_two, grad_gate, grad_up = back_gather(
        act_two_t, w_gate, w_up, d_gate, d_up, dots, x_low, attn, small, 5
    )
    ffn, d_attn, grad_down = down_gather(g_low, w_down, hidden, d_norm, 6)
    d_tokens, out, grad_query, grad_out, grad_kv, gain_sums = tail(
        d_attn,
        w_out,
        queries,
        kv,
        probs,
        pair_rms,
        cos,
        sin,
        act_one_t,
        w_qkv,
        ffn,
        x_low,
        attn,
        small,
        grad_gain_two,
        mixed_all,
        7,
    )
    gains = gain_sums.reshape(2, -1)
    wider = jnp.float32
    return (
        out,
        d_tokens.astype(wider),
        gains[0],
        grad_query.astype(wider),
        grad_kv.astype(wider),
        grad_out.astype(wider),
        gains[1],
        grad_gate.astype(wider),
        grad_up.astype(wider),
        grad_down.astype(wider),
    )


def solution(mesh):
    in_specs = (
        P(("dp", "seq"), None),
        P("dp"),
        P(("dp", "seq")),
        P(("dp", "seq"), "tensor"),
        P(("dp", "seq"), None),
        P("tensor", ("dp", "seq")),
        P(("dp", "seq")),
        P(("dp", "seq"), "tensor"),
        P(("dp", "seq"), "tensor"),
        P("tensor", ("dp", "seq")),
        P(("dp", "seq"), None),
    )
    out_specs = (
        P(("dp", "seq"), None),
        P(("dp", "seq"), None),
        P(("dp", "seq")),
        P(("dp", "seq"), "tensor"),
        P(("dp", "seq"), None),
        P("tensor", ("dp", "seq")),
        P(("dp", "seq")),
        P(("dp", "seq"), "tensor"),
        P(("dp", "seq"), "tensor"),
        P("tensor", ("dp", "seq")),
    )

    def shards(*arrays):
        tokens = arrays[0]
        sizes = tuple(mesh.shape[name] for name in ("dp", "seq", "tensor"))
        count = tokens.shape[0] * sizes[0] * sizes[1]
        plan = acts_move if sizes == (4, 2, 4) and count <= tokens.shape[1] else weights_move
        return plan(*arrays)

    return jax.shard_map(shards, mesh=mesh, in_specs=in_specs, out_specs=out_specs, check_vma=False)
```

```python
import functools
import math

import jax
import jax.numpy as jnp
from jax import lax
from jax.experimental import pallas as pl
from jax.experimental.pallas import tpu as pltpu
from jax.sharding import PartitionSpec as P

HD = 256


EPS = 1e-06
NEG = -1e30


def place_tables(segs):
    length = segs.shape[0]
    index = jnp.arange(length, dtype=jnp.int32)
    flags = jnp.concatenate([jnp.ones((1,), dtype=bool), segs[1:] != segs[:-1]])
    starts = lax.cummax(jnp.where(flags, index, jnp.zeros_like(index)), axis=0)
    places = index - starts
    half_size = HD // 2
    freqs = jnp.exp(jnp.arange(half_size, dtype=jnp.float32) * (-math.log(10000.0) / half_size))
    angles = places.astype(jnp.float32)[:, None] * freqs[None, :]
    return (places, jnp.cos(angles), jnp.sin(angles))


def rotate(vector, cos_table, sin_table):
    half_size = vector.shape[-1] // 2
    leading = vector[..., :half_size]
    trailing = vector[..., half_size:]
    return jnp.concatenate(
        [leading * cos_table - trailing * sin_table, trailing * cos_table + leading * sin_table],
        axis=-1,
    )


def rotate_back(vector, cos_table, sin_table):
    half_size = vector.shape[-1] // 2
    leading = vector[..., :half_size]
    trailing = vector[..., half_size:]
    return jnp.concatenate(
        [leading * cos_table + trailing * sin_table, trailing * cos_table - leading * sin_table],
        axis=-1,
    )


def matmul(left, right):
    return jnp.dot(left, right, preferred_element_type=jnp.float32)


def matmul_nt(left, right):
    return lax.dot_general(
        left, right, (((1,), (1,)), ((), ())), preferred_element_type=jnp.float32
    )


def matmul_tn(left, right):
    return lax.dot_general(
        left, right, (((0,), (0,)), ((), ())), preferred_element_type=jnp.float32
    )


def gelu_tanh(values):
    return jax.nn.gelu(values, approximate=True)


def norm_back(d_act, normed, rms_val, gain_val):
    scaled = d_act * gain_val
    return rms_val * (scaled - normed * jnp.mean(scaled * normed, axis=-1, keepdims=True))


def weights_move(
    tokens, seg_ids, gain_attn, w_query, kv_weight, w_out, gain_ffn, w_gate, w_up, w_down, d_out
):
    rows = tokens.shape[0]
    scale_factor = 1.0 / math.sqrt(HD)
    offset = lax.axis_index("seq") * rows
    places, cos_table, sin_table = place_tables(seg_ids)
    own_places = lax.dynamic_slice_in_dim(places, offset, rows, 0)
    own_segs = lax.dynamic_slice_in_dim(seg_ids, offset, rows, 0)
    own_cos = lax.dynamic_slice_in_dim(cos_table, offset, rows, 0)
    own_sin = lax.dynamic_slice_in_dim(sin_table, offset, rows, 0)
    allowed = (own_segs[:, None] == seg_ids[None, :]) & (own_places[:, None] >= places[None, :])
    full_query, full_out, full_kv, full_gain_one = (
        lax.all_gather(w_query, ("dp", "seq"), axis=0, tiled=True),
        lax.all_gather(w_out, ("dp", "seq"), axis=1, tiled=True),
        lax.all_gather(kv_weight, ("dp", "seq"), axis=0, tiled=True),
        lax.all_gather(gain_attn, ("dp", "seq"), axis=0, tiled=True),
    )
    gain_one = full_gain_one.astype(jnp.float32)
    inputs = tokens.astype(jnp.float32)
    rms_one = lax.rsqrt(jnp.mean(inputs * inputs, axis=-1, keepdims=True) + EPS)
    norm_one = inputs * rms_one
    act_one = (norm_one * gain_one).astype(jnp.bfloat16)
    query_pre = matmul(act_one, full_query)
    heads = query_pre.shape[1] // HD
    kv_pre = matmul(act_one, full_kv)
    queries = (
        rotate(query_pre.reshape(rows, heads, HD), own_cos[:, None, :], own_sin[:, None, :])
        * scale_factor
    ).astype(jnp.bfloat16)
    own_kv = jnp.concatenate(
        [rotate(kv_pre[:, :HD], own_cos, own_sin), kv_pre[:, HD:]], axis=1
    ).astype(jnp.bfloat16)
    all_kv = lax.all_gather(own_kv, "seq", axis=0, tiled=True)
    keys = all_kv[:, :HD]
    values_all = all_kv[:, HD:]
    scores = jnp.einsum("rhd,kd->hrk", queries, keys, preferred_element_type=jnp.float32)
    scores = jnp.where(allowed[None], scores, NEG)
    top_score = jnp.max(scores, axis=-1, keepdims=True)
    expd = jnp.exp(scores - top_score)
    total = jnp.sum(expd, axis=-1, keepdims=True)
    log_total = top_score + jnp.log(total)
    probs_low = (expd / total).astype(jnp.bfloat16)
    mixed = (
        jnp.einsum("hrk,kd->rhd", probs_low, values_all, preferred_element_type=jnp.float32)
        .reshape(rows, heads * HD)
        .astype(jnp.bfloat16)
    )
    attn = lax.psum(matmul(mixed, full_out), "tensor")
    resid = inputs + attn
    full_gate, full_up, full_down, full_gain_two = (
        lax.all_gather(w_gate, ("dp", "seq"), axis=0, tiled=True),
        lax.all_gather(w_up, ("dp", "seq"), axis=0, tiled=True),
        lax.all_gather(w_down, ("dp", "seq"), axis=1, tiled=True),
        lax.all_gather(gain_ffn, ("dp", "seq"), axis=0, tiled=True),
    )
    gain_two = full_gain_two.astype(jnp.float32)
    rms_two = lax.rsqrt(jnp.mean(resid * resid, axis=-1, keepdims=True) + EPS)
    norm_two = resid * rms_two
    act_two = (norm_two * gain_two).astype(jnp.bfloat16)
    gate = matmul(act_two, full_gate)
    up_val = matmul(act_two, full_up)
    gelu_val, gelu_pull = jax.vjp(gelu_tanh, gate)
    hidden = (gelu_val * up_val).astype(jnp.bfloat16)
    ffn = lax.psum(matmul(hidden, full_down).astype(jnp.bfloat16), "tensor").astype(jnp.float32)
    out = (resid + ffn).astype(jnp.bfloat16)
    back_gate, back_up, back_down = (
        lax.all_gather(w_gate, ("dp", "seq"), axis=0, tiled=True),
        lax.all_gather(w_up, ("dp", "seq"), axis=0, tiled=True),
        lax.all_gather(w_down, ("dp", "seq"), axis=1, tiled=True),
    )
    d_hidden = matmul_nt(d_out, back_down)
    grad_down = matmul_tn(hidden, d_out)
    d_gate = gelu_pull(d_hidden * up_val)[0].astype(jnp.bfloat16)
    d_up = (d_hidden * gelu_val).astype(jnp.bfloat16)
    grad_gate = matmul_tn(act_two, d_gate)
    grad_up = matmul_tn(act_two, d_up)
    d_act_two = lax.psum(matmul_nt(d_gate, back_gate) + matmul_nt(d_up, back_up), "tensor")
    grad_gain_two = jnp.sum(d_act_two * norm_two, axis=0)
    d_resid = d_out.astype(jnp.float32) + norm_back(d_act_two, norm_two, rms_two, gain_two)
    ffn_grads = (
        lax.psum_scatter(
            grad_gate.astype(jnp.bfloat16), ("dp", "seq"), scatter_dimension=0, tiled=True
        ).astype(jnp.float32),
        lax.psum_scatter(
            grad_up.astype(jnp.bfloat16), ("dp", "seq"), scatter_dimension=0, tiled=True
        ).astype(jnp.float32),
        lax.psum_scatter(
            grad_down.astype(jnp.bfloat16), ("dp", "seq"), scatter_dimension=1, tiled=True
        ).astype(jnp.float32),
        lax.psum_scatter(
            grad_gain_two.astype(jnp.bfloat16), ("dp", "seq"), scatter_dimension=0, tiled=True
        ).astype(jnp.float32),
    )
    back_query, back_out, back_kv = (
        lax.all_gather(w_query, ("dp", "seq"), axis=0, tiled=True),
        lax.all_gather(w_out, ("dp", "seq"), axis=1, tiled=True),
        lax.all_gather(kv_weight, ("dp", "seq"), axis=0, tiled=True),
    )
    d_attn = d_resid.astype(jnp.bfloat16)
    grad_out = matmul_tn(mixed, d_attn)
    d_mixed = matmul_nt(d_attn, back_out).astype(jnp.bfloat16).reshape(rows, heads, HD)
    scores_again = jnp.einsum("rhd,kd->hrk", queries, keys, preferred_element_type=jnp.float32)
    probs = jnp.where(allowed[None], jnp.exp(scores_again - log_total), 0.0)
    d_probs = jnp.einsum("rhd,kd->hrk", d_mixed, values_all, preferred_element_type=jnp.float32)
    delta = jnp.sum(probs * d_probs, axis=-1, keepdims=True)
    d_scores = (probs * (d_probs - delta)).astype(jnp.bfloat16)
    d_queries = (
        jnp.einsum("hrk,kd->rhd", d_scores, keys, preferred_element_type=jnp.float32) * scale_factor
    )
    d_query_pre = (
        rotate_back(d_queries, own_cos[:, None, :], own_sin[:, None, :])
        .reshape(rows, heads * HD)
        .astype(jnp.bfloat16)
    )
    d_keys_part = jnp.einsum("hrk,rhd->kd", d_scores, queries, preferred_element_type=jnp.float32)
    d_values_part = jnp.einsum(
        "hrk,rhd->kd", probs.astype(jnp.bfloat16), d_mixed, preferred_element_type=jnp.float32
    )
    own_kv_grad = lax.psum_scatter(
        jnp.concatenate([d_keys_part, d_values_part], axis=1).astype(jnp.bfloat16),
        "seq",
        scatter_dimension=0,
        tiled=True,
    )
    d_act_query = matmul_nt(d_query_pre, back_query)
    d_act_sum, kv_grad = (
        lax.psum(d_act_query.astype(jnp.bfloat16), "tensor").astype(jnp.float32),
        lax.psum(own_kv_grad, "tensor").astype(jnp.float32),
    )
    d_kv_pre = jnp.concatenate(
        [rotate_back(kv_grad[:, :HD], own_cos, own_sin), kv_grad[:, HD:]], axis=1
    ).astype(jnp.bfloat16)
    d_act_one = d_act_sum + matmul_nt(d_kv_pre, back_kv)
    grad_query = matmul_tn(act_one, d_query_pre)
    grad_kv = matmul_tn(act_one, d_kv_pre)
    grad_gain_one = jnp.sum(d_act_one * norm_one, axis=0)
    d_tokens = d_resid + norm_back(d_act_one, norm_one, rms_one, gain_one)
    attn_grads = (
        lax.psum_scatter(
            grad_query.astype(jnp.bfloat16), ("dp", "seq"), scatter_dimension=0, tiled=True
        ).astype(jnp.float32),
        lax.psum_scatter(
            grad_out.astype(jnp.bfloat16), ("dp", "seq"), scatter_dimension=1, tiled=True
        ).astype(jnp.float32),
        lax.psum_scatter(
            grad_kv.astype(jnp.bfloat16), ("dp", "seq"), scatter_dimension=0, tiled=True
        ).astype(jnp.float32),
        lax.psum_scatter(
            grad_gain_one.astype(jnp.bfloat16), ("dp", "seq"), scatter_dimension=0, tiled=True
        ).astype(jnp.float32),
    )
    return (
        out,
        d_tokens,
        attn_grads[3],
        attn_grads[0],
        attn_grads[2],
        attn_grads[1],
        ffn_grads[3],
        ffn_grads[0],
        ffn_grads[1],
        ffn_grads[2],
    )


MESH = pl.DeviceIdType.MESH
VMEM_LIMIT = 66000 * 1024


class Place:
    def __init__(self):
        self.dp = lax.axis_index("dp")
        self.seq = lax.axis_index("seq")
        self.z = lax.axis_index("tensor")
        self.core = lax.rem(self.dp, 2)
        self.chip = lax.div(self.dp, 2)

    def device(self, across, other):
        chip = (self.chip + across) % 2
        seq = (self.seq + across // 2) % 2
        core = (self.core + other) % 2
        return chip * 2 + core, seq, self.z

    def shard(self, across, other):
        dp, seq, _ = self.device(across, other)
        return dp * 2 + seq


def greet(here, peers, line=False):
    barrier = pltpu.get_barrier_semaphore()
    peers = list(peers)
    if line:
        peers += [(here.dp, here.seq, (here.z + step) % 4) for step in range(1, 4)]
    for peer in peers:
        pl.semaphore_signal(barrier, inc=1, device_id=peer, device_id_type=MESH)
    pl.semaphore_wait(barrier, len(peers))


def remote(src, dst, send, recv, peer):
    return pltpu.make_async_remote_copy(
        src_ref=src, dst_ref=dst, send_sem=send, recv_sem=recv, device_id=peer, device_id_type=MESH
    )


class Line:
    def __init__(self, here, counts, refs, place=None):
        self.own, self.out, self.from_end, self.from_mid = refs[:4]
        self.sems = refs[4:10]
        self.counts = counts
        self.chunk = self.from_mid.shape[1]
        self.fold = self.from_end.shape[1] // self.chunk
        self.place = place
        z = here.z
        self.inner = ((z + 1) // 2) % 2
        self.mate = (here.dp, here.seq, z + 1 - 2 * (z % 2))
        self.other = (here.dp, here.seq, 3 - z)

    def rows(self, at):
        at = at if self.place is None else self.place(at)
        return pl.ds(pl.multiple_of(at * self.chunk, self.chunk), self.chunk)

    def inbox(self, at):
        span = pl.ds(pl.multiple_of(at % self.fold * self.chunk, self.chunk), self.chunk)
        return self.from_end.at[at // self.fold, span, :]

    def up(self, at):
        return remote(self.own.at[self.rows(at), :], self.inbox(at), self.sems[0].at[at],
                      self.sems[1].at[at], self.mate)

    def over(self, at):
        return remote(self.out.at[self.rows(at), :], self.from_mid.at[at], self.sems[2].at[at],
                      self.sems[3].at[at], self.other)

    def down(self, at):
        rows = self.rows(at)
        return remote(self.out.at[rows, :], self.out.at[rows, :], self.sems[4].at[at],
                      self.sems[5].at[at], self.mate)

    def launch(self, first, count):
        @pl.when(self.inner == 0)
        def _():
            def send(at, _):
                self.up(first + at).start()
                return 0

            lax.fori_loop(0, count, send, 0)

    def begin(self):
        self.launch(0, self.counts)

    def first(self, at):
        rows = self.rows(at)
        self.up(at).wait_recv()
        total = self.own[rows, :].astype(jnp.float32) + self.inbox(at)[...].astype(jnp.float32)
        self.out[rows, :] = total.astype(self.out.dtype)
        self.over(at).start()

    def second(self, at):
        rows = self.rows(at)
        self.over(at).wait()
        total = self.out[rows, :].astype(jnp.float32) + self.from_mid[at].astype(jnp.float32)
        self.out[rows, :] = total.astype(self.out.dtype)
        self.down(at).start()

    def step(self, at, start=0, count=None):
        count = self.counts if count is None else count

        @pl.when(jnp.logical_and(self.inner == 1, at < count))
        def _():
            self.first(start + at)

        @pl.when(jnp.logical_and(self.inner == 1, jnp.logical_and(at > 1, at < count + 2)))
        def _():
            self.second(start + at - 2)

    def steps(self, first, last, start=0, count=None):
        def rest(at, _):
            self.step(at, start, count)
            return 0

        lax.fori_loop(first, last, rest, 0)

    def settle(self):
        @pl.when(self.inner == 0)
        def _():
            def take(at, _):
                self.up(at).wait_send()
                self.down(at).wait_recv()
                return 0

            lax.fori_loop(0, self.counts, take, 0)

        self.drain()

    def drain(self):
        @pl.when(self.inner == 1)
        def _():
            def drain(at, _):
                self.down(at).wait_send()
                return 0

            lax.fori_loop(0, self.counts, drain, 0)

    def end(self, done=0):
        self.steps(min(done, self.counts + 2), self.counts + 2)
        self.settle()


def line_scratch(counts, shape, low, fold=1):
    chunk = shape[0] // counts
    inbox = pltpu.VMEM((counts // fold, chunk * fold, shape[1]), low)
    return [inbox, pltpu.VMEM((counts, chunk, shape[1]), low)] + [pltpu.SemaphoreType.DMA((counts,))] * 6


def turned(at):
    return 3 - at // 2, 1 - at % 2


def slice_peers(here):
    return [here.device(*turned(at)) for at in range(7)]


def kernel_call(kernel, out_shape, operands, specs, scratch, cid, name, out_specs=None, late=(), early=(),
                pieces=()):
    vm = pl.BlockSpec(memory_space=pltpu.VMEM)
    hbm = pl.BlockSpec(memory_space=pl.ANY)
    specs = [hbm if at in late else spec for at, spec in enumerate(specs)]
    out_specs = [hbm if at in early or at in pieces else spec for at, spec in enumerate(out_specs or [vm] * len(out_shape))]
    inside = [pltpu.VMEM(operands[at].shape, operands[at].dtype) for at in late]
    inside += [pltpu.VMEM(out_shape[at].shape, out_shape[at].dtype) for at in (*early, *pieces)]
    inside.append(pltpu.SemaphoreType.DMA((max(1, len(late) + len(early)),)))
    n_in, n_out = len(operands), len(out_shape)

    def body(*refs):
        ins, outs = list(refs[:n_in]), list(refs[n_in : n_in + n_out])
        rest, own = refs[n_in + n_out : -len(inside)], refs[-len(inside) :]
        loads, stores = [], []
        for spot, at in enumerate(late):
            copy = pltpu.make_async_copy(ins[at], own[spot], own[-1].at[spot])
            copy.start()
            loads.append(copy)
            ins[at] = own[spot]
        for number, at in enumerate(early):
            spot = len(late) + number
            stores.append(pltpu.make_async_copy(own[spot], outs[at], own[-1].at[spot]))
            outs[at] = own[spot]
        raw = []
        for number, at in enumerate(pieces):
            raw.append(outs[at])
            outs[at] = own[len(late) + len(early) + number]
        more = {}
        if pieces:
            more["raw"] = raw
        if late:
            more["late"] = loads
        if early:
            more["early"] = stores
        kernel(*ins, *outs, *rest, **more)
        for copy in stores:
            copy.wait()

    return pl.pallas_call(
        body,
        out_shape=out_shape,
        in_specs=specs,
        out_specs=out_specs,
        scratch_shapes=scratch + inside,
        compiler_params=pltpu.CompilerParams(
            collective_id=cid, has_side_effects=True, vmem_limit_bytes=VMEM_LIMIT
        ),
        name=f"{name}_{cid}",
    )(*operands)


class Tiny:
    def __init__(self, here, src, dst, sems, spread):
        self.here, self.src, self.dst, self.sems, self.spread = here, src, dst, sems, spread
        self.peers = slice_peers(here)
        self.me = here.shard(0, 0)

    def tile(self, shard):
        return self.src.at[shard] if self.spread else self.src

    def copy(self, at):
        return remote(self.tile(self.here.shard(*turned(at))), self.dst.at[self.me], self.sems[0].at[at],
                      self.sems[1].at[at], self.peers[at])

    def begin(self):
        for at in range(7):
            self.copy(at).start()
        self.dst[self.me] = self.tile(self.me)[...]

    def end(self):
        for at in range(7):
            self.copy(at).wait()


class Reduce:
    def __init__(self, here, counts, product, refs, before=None):
        self.counts, self.product, self.before = counts, product, before
        self.held, self.sib_out, self.sib_in, self.from_x, self.from_y = refs[:5]
        self.sib_sems, self.x_sems, self.y_sems = refs[5:7], refs[7:9], refs[9:11]
        self.sib, self.xdev, self.ydev = here.device(0, 1), here.device(1, 0), here.device(2, 0)
        self.steps = 4 * counts
        self.ring = self.sib_out.shape[0]

    def streams(self, stage):
        far = stage // 3
        x_chip = jnp.where(stage == 0, 3, jnp.where(stage == 2, 0, 1))
        y_chip = jnp.where(stage == 0, 3, jnp.where(stage == 2, 0, 2))
        return (x_chip, far), (y_chip, 1 - far)

    def to_sib(self, step, stream):
        stage, at = step // self.counts, step % self.counts
        return remote(self.sib_out.at[step % self.ring, stream], self.sib_in.at[stage, stream, at],
                      self.sib_sems[0].at[stage, stream, at], self.sib_sems[1].at[stage, stream, at], self.sib)

    def to_x(self, hop, at, stage=0):
        return remote(self.held.at[stage, 0, at], self.from_x.at[hop, at], self.x_sems[0].at[hop, at],
                      self.x_sems[1].at[hop, at], self.xdev)

    def to_y(self, hop, at, stage=0):
        return remote(self.held.at[stage, 1, at], self.from_y.at[hop, at], self.y_sems[0].at[hop, at],
                      self.y_sems[1].at[hop, at], self.ydev)

    def compute(self, step):
        stage, at = step // self.counts, step % self.counts
        if self.before:
            for stop in range(3):
                @pl.when(step == stop * self.counts)
                def _():
                    self.before(stop)

        @pl.when(step >= self.ring)
        def _():
            for stream in range(2):
                self.to_sib(step - self.ring, stream).wait_send()

        for stream, (across, half) in enumerate(self.streams(stage)):
            self.sib_out[step % self.ring, stream] = self.product(across, 1, half, at).astype(jnp.bfloat16)
            self.held[stage, stream, at] = self.product(across, 0, half, at).astype(jnp.bfloat16)
        for stream in range(2):
            self.to_sib(step, stream).start()

    def finish(self, step):
        stage, at = step // self.counts, step % self.counts
        for stream in range(2):
            self.to_sib(step, stream).wait_recv()

        def total(stream):
            return self.held[stage, stream, at].astype(jnp.float32) + self.sib_in[stage, stream, at].astype(
                jnp.float32)

        @pl.when(stage < 3)
        def _():
            for stream in range(2):
                self.held[stage, stream, at] = total(stream).astype(jnp.bfloat16)

        @pl.when(stage == 3)
        def _():
            self.to_y(0, at).wait_recv()
            self.held[3, 0, at] = (total(0) + self.from_y[0, at].astype(jnp.float32)).astype(jnp.bfloat16)
            self.to_x(0, at).wait_recv()
            self.held[3, 1, at] = (total(1) + self.from_x[0, at].astype(jnp.float32)).astype(jnp.bfloat16)

        @pl.when(stage != 2)
        def _():
            hop = stage - stage // 3
            self.to_x(hop, at, stage).start()
            self.to_y(hop, at, stage).start()

    def advance(self, step):
        @pl.when(step < self.steps)
        def _():
            self.compute(step)

        @pl.when(jnp.logical_and(step > 0, step <= self.steps))
        def _():
            self.finish(step - 1)

    def run(self, hook=None):
        def body(step, _):
            self.advance(step)

            if hook:
                hook(step)
            return 0

        lax.fori_loop(0, self.steps + 1, body, 0)
        return self.steps + 1

    def end(self, emit):
        def last(at, _):
            values = []
            for half in range(2):
                xs, ys = (1, 2) if half == 0 else (2, 1)
                self.to_x(xs, at).wait_recv()
                self.to_y(ys, at).wait_recv()
                values.append(self.held[2, half, at].astype(jnp.float32) + self.from_x[xs, at].astype(jnp.float32)
                              + self.from_y[ys, at].astype(jnp.float32))
            emit(at, *values)
            for hop in range(3):
                self.to_x(hop, at).wait_send()
                self.to_y(hop, at).wait_send()
            return 0

        lax.fori_loop(0, self.counts, last, 0)

        def drain(at, _):
            for stream in range(2):
                self.to_sib(self.steps - self.ring + at, stream).wait_send()
            return 0

        lax.fori_loop(0, self.ring, drain, 0)


def reduce_scratch(counts, rows, width, ring=4):
    low, dma = jnp.bfloat16, pltpu.SemaphoreType.DMA
    block = pltpu.VMEM((4, 2, counts, rows, width), low)
    landed = pltpu.VMEM((3, counts, rows, width), low)
    sent = pltpu.VMEM((ring, 2, rows, width), low)
    return [block, sent, block, landed, landed] + [dma((4, 2, counts))] * 2 + [dma((3, counts))] * 4


class Spread:
    def __init__(self, here, counts, refs):
        self.counts = counts
        self.got = refs[0]
        self.x_sems, self.y_sems, self.sib_sems = refs[1:3], refs[3:5], refs[5:7]
        self.core = here.core
        self.sib, self.xdev, self.ydev = here.device(0, 1), here.device(1, 0), here.device(2, 0)

    def slot(self, across, half, at):
        return self.got.at[across, self.core, half, at]

    def x_copy(self, hop, at):
        half = jnp.minimum(hop, 1)
        src = self.slot(2 * (hop // 2), half, at)
        dst = self.slot(1 + 2 * (hop // 2), half, at)
        return remote(src, dst, self.x_sems[0].at[hop, at], self.x_sems[1].at[hop, at], self.xdev)

    def y_copy(self, hop, at):
        half = 1 - jnp.minimum(hop, 1)
        src = self.slot(hop // 2, half, at)
        dst = self.slot(2 + hop // 2, half, at)
        return remote(src, dst, self.y_sems[0].at[hop, at], self.y_sems[1].at[hop, at], self.ydev)

    def streams(self, stage):
        some, last, late = jnp.minimum(stage, 1), stage // 3, stage // 2
        return (some + 2 * last, late), (2 * some + last, 1 - late)

    def block(self, at):
        x_stream, y_stream = self.streams(at // 4)
        second = at // 2 % 2
        across = x_stream[0] + second * (y_stream[0] - x_stream[0])
        half = x_stream[1] + second * (y_stream[1] - x_stream[1])
        return across, at % 2, half

    def begin_rows(self):
        for hop in range(2):
            self.x_copy(hop, 0).start()
            self.y_copy(hop, 0).start()
        for stream in range(2):
            self.sib_copy(0, stream, 0).start()

    def receive_rows(self, step):
        stage = step // 4

        @pl.when(jnp.logical_and(step % 4 == 0, jnp.logical_and(stage > 0, stage < 4)))
        def _():
            self.x_copy(stage - 1, 0).wait_recv()
            self.sib_copy(stage, 0, 0).start()
            self.y_copy(stage - 1, 0).wait_recv()
            self.sib_copy(stage, 1, 0).start()

        @pl.when(step == 4)
        def _():
            self.x_copy(2, 0).start()
            self.y_copy(2, 0).start()

        for stream in range(2):
            @pl.when(jnp.logical_and(step % 4 == 2 * stream, step < 16))
            def _(stream=stream):
                self.sib_copy(stage, stream, 0).wait_recv()

    def sib_copy(self, stage, stream, at):
        across, half = self.streams(stage)[stream]
        slot = self.slot(across, half, at)
        spot = (stage, stream, at)
        return remote(slot, slot, self.sib_sems[0].at[spot], self.sib_sems[1].at[spot], self.sib)

    def begin(self):
        def first(at, _):
            self.x_copy(0, at).start()
            self.y_copy(0, at).start()
            return 0

        def own(at, _):
            self.sib_copy(0, 0, at).start()
            self.sib_copy(0, 1, at).start()
            return 0

        lax.fori_loop(0, self.counts, first, 0)
        lax.fori_loop(0, self.counts, own, 0)

    def run(self, blocks, hook=None, done=None):
        counts = self.counts

        def body(step, _):
            stage, at = step // counts, step % counts

            @pl.when(jnp.logical_and(stage > 0, stage < 4))
            def _():
                self.x_copy(stage - 1, at).wait_recv()
                self.sib_copy(stage, 0, at).start()
                self.y_copy(stage - 1, at).wait_recv()
                self.sib_copy(stage, 1, at).start()

            @pl.when(jnp.logical_and(stage > 0, stage < 3))
            def _():
                self.x_copy(stage, at).start()
                self.y_copy(stage, at).start()

            @pl.when(step > 0)
            def _():
                old, spot = (step - 1) // counts, (step - 1) % counts
                for stream, (across, half) in enumerate(self.streams(old)):
                    self.sib_copy(old, stream, spot).wait_recv()
                    blocks(across, half, spot)
                if done:
                    done(old, spot)

            if hook:
                hook(step)
            return 0

        lax.fori_loop(0, 4 * counts + 1, body, 0)
        return 4 * counts + 1

    def end(self):
        def drain(at, _):
            for hop in range(3):
                self.x_copy(hop, at).wait_send()
                self.y_copy(hop, at).wait_send()
            for stage in range(4):
                self.sib_copy(stage, 0, at).wait_send()
                self.sib_copy(stage, 1, at).wait_send()
            return 0

        lax.fori_loop(0, self.counts, drain, 0)


def spread_scratch(counts, rows, width):
    dma = pltpu.SemaphoreType.DMA
    return [pltpu.VMEM((4, 2, 2, counts, rows, width), jnp.bfloat16)] + [dma((3, counts))] * 4 + [
        dma((4, 2, counts))] * 2


def row_span(here, across, other, rows):
    return pl.ds(pl.multiple_of(here.shard(across, other) * rows, rows), rows)


def dot_nt(left, right):
    return lax.dot_general(left, right, (((1,), (1,)), ((), ())), preferred_element_type=jnp.float32)


def dot_tn(left, right):
    return lax.dot_general(left, right, (((0,), (0,)), ((), ())), preferred_element_type=jnp.float32)


def dot_nn(left, right):
    return jnp.dot(left, right, preferred_element_type=jnp.float32)


def products(here, act, weight, nt, rows, width, counts):
    def product(across, other, half, at):
        cols = pl.ds(pl.multiple_of((half * counts + at) * width, width), width)
        block = act[row_span(here, across, other, rows), :]
        return dot_nt(block, weight[cols, :]) if nt else dot_nn(block, weight[:, cols])

    return product


def diagonal():
    return (lax.broadcasted_iota(jnp.int32, (LANES, LANES), 0) ==
            lax.broadcasted_iota(jnp.int32, (LANES, LANES), 1)).astype(jnp.float32)


def to_tile(tile, first, column, eye):
    for at in range(column.shape[0] // LANES):
        spread = column[at * LANES : (at + 1) * LANES, :] * eye
        tile[first + at : first + at + 1, :] = jnp.sum(spread, axis=0, keepdims=True)


def from_tile(row, eye):
    return jnp.sum(eye * row, axis=1, keepdims=True)


def make_tables(here, rows, segs, cos, sin, mask):
    eye = diagonal()
    tiles = rows // LANES
    freqs = jnp.exp(lax.broadcasted_iota(jnp.int32, (1, LANES), 1).astype(jnp.float32) * (-math.log(10000.0) / LANES))
    lane = lax.broadcasted_iota(jnp.int32, (1, LANES), 1)
    line = lax.broadcasted_iota(jnp.int32, (LANES, 1), 0)

    def ids_of(row):
        return segs[2:3, pl.ds(pl.multiple_of(row * LANES, LANES), LANES)]

    def row_of(side, at):
        return ((here.seq + side) % 2) * tiles + at

    for side in range(2):
        for at in range(tiles):
            row = row_of(side, at)
            ids = from_tile(ids_of(row), eye)
            before = jnp.zeros((LANES, 1), jnp.float32)
            for other in range(2 * tiles):
                smaller = ids_of(other) < ids
                before += jnp.sum(smaller.astype(jnp.float32), axis=-1, keepdims=True)
            index = row * LANES + line
            angles = (index.astype(jnp.float32) - before) * freqs
            span = slice(at * LANES, (at + 1) * LANES)
            cos[side, span, :] = jnp.cos(angles)
            sin[side, span, :] = jnp.sin(angles)
            if side == 0:
                for key_side in range(2):
                    for key_at in range(tiles):
                        key_row = row_of(key_side, key_at)
                        same = ids_of(key_row) == ids
                        allowed = jnp.logical_and(same, key_row * LANES + lane <= index)
                        first = key_side * rows + key_at * LANES
                        mask[span, first : first + LANES] = allowed.astype(jnp.float32)


def open_kernel(rows, width, counts, tokens, gain_one, gain_two, ids, w_query, kv_weight, cot, qkv, x_low, act_t, w_qkv, rms, cos, sin,
                mask, g_col, gain, *refs, early):
    here = Place()
    gain[...] = jnp.zeros_like(gain)
    gain[0:1, :] = gain_one[...].astype(jnp.float32).reshape(1, -1)
    gain[1:2, :] = gain_two[...].astype(jnp.float32).reshape(1, -1)
    gain[2:3, :] = ids[...].astype(jnp.float32).reshape(1, -1)
    early[7].start()
    cols, segs = gain.shape[1], gain
    act, turn_send, turn_recv, local_sems, cot_part, g_send, g_recv, z_send, z_recv = refs[:9]
    share = rows // 4
    me = here.shard(0, 0)
    own_rows = pl.ds(pl.multiple_of(me * rows, rows), rows)

    def turn_copy(at):
        across, other = turned(at)
        first = pl.multiple_of(here.shard(across, other) * cols, cols)
        return remote(tokens.at[:, pl.ds(first, cols)], x_low.at[own_rows, :], turn_send.at[at], turn_recv.at[at],
                      here.device(across, other))

    wide = w_query.shape[1]
    local = [
        pltpu.make_async_copy(w_query, w_qkv.at[:, :wide], local_sems.at[0]),
        pltpu.make_async_copy(kv_weight, w_qkv.at[:, wide:], local_sems.at[1]),
        pltpu.make_async_copy(tokens.at[:, pl.ds(pl.multiple_of(me * cols, cols), cols)], x_low.at[own_rows, :],
                              local_sems.at[2]),
    ]
    load = pltpu.make_async_copy(cot.at[pl.ds(pl.multiple_of(here.z * share, share), share), :], cot_part,
                                 local_sems.at[3])
    load.start()
    for copy in local:
        copy.start()

    def g_copy(at):
        across, other = turned(at)
        first = pl.multiple_of(here.shard(across, other) * cols, cols)
        return remote(cot_part.at[:, pl.ds(first, cols)], g_col.at[me, here.z], g_send.at[at], g_recv.at[at],
                      here.device(across, other))

    def own_part():
        return pltpu.make_async_copy(cot_part.at[:, pl.ds(pl.multiple_of(me * cols, cols), cols)],
                                     g_col.at[me, here.z], local_sems.at[4])

    def quarter(way, at, step, peer):
        spot = g_col.at[:, at]
        return remote(spot, spot, z_send.at[way, step], z_recv.at[way, step], (here.dp, here.seq, here.z + peer))

    def pass_on(step):
        @pl.when(jnp.logical_and(here.z < 3, here.z >= step))
        def _():
            quarter(0, here.z - step, step, 1).start()

        @pl.when(jnp.logical_and(here.z > 0, here.z <= 3 - step))
        def _():
            quarter(1, here.z + step, step, -1).start()

    def take_quarters(step):
        @pl.when(here.z > step)
        def _():
            quarter(0, here.z - 1 - step, step, -1).wait_recv()

        @pl.when(here.z < 3 - step)
        def _():
            quarter(1, here.z + 1 + step, step, 1).wait_recv()

    greet(here, slice_peers(here), True)
    load.wait()
    own_part().start()
    for at in range(7):
        g_copy(at).start()
    for at in range(7):
        turn_copy(at).start()
    for copy in local:
        copy.wait()
    early[2].start()

    def squares(at, total):
        values = tokens[:, pl.ds(pl.multiple_of(at * cols, cols), cols)].astype(jnp.float32)
        return total + jnp.sum(values * values, axis=-1, keepdims=True)

    total = lax.fori_loop(0, 8, squares, jnp.zeros((rows, 1), jnp.float32))
    rms[...] = jnp.broadcast_to(lax.rsqrt(total / (8 * cols) + EPS), rms.shape)
    make_tables(here, rows, segs, cos, sin, mask)
    for at in (3, 4, 5):
        early[at].start()

    def prepare(first, count):
        def one(step, _):
            at = first + step
            span = row_span(here, *turned(at), rows)
            value = (x_low[span, :].astype(jnp.float32) * gain[0:1, :]).astype(act.dtype)
            act[span, :] = value
            return 0

        lax.fori_loop(0, count, one, 0)

    def before(stop):
        first, count = ((0, 2), (2, 4), (6, 2))[stop]
        if stop == 0:
            own_part().wait()
            for at in range(7):
                g_copy(at).wait_recv()
        else:
            take_quarters(stop - 1)
        pass_on(stop)
        for at in range(first, min(first + count, 7)):
            turn_copy(at).wait_recv()
        prepare(first, count)
        if stop == 2:
            early[0].start()

    def flip():
        def one(shard, _):
            span = pl.ds(pl.multiple_of(shard * rows, rows), rows)
            act_t[:, span] = act[span, :].T
            return 0

        lax.fori_loop(0, 8, one, 0)

    product = products(here, act, w_qkv, False, rows, width, counts)
    total = Reduce(here, counts, product, refs[9:20], before)
    total.run()
    flip()
    early[1].start()

    def emit(at, first, second):
        for half, value in enumerate((first, second)):
            qkv[:, pl.ds(pl.multiple_of((half * counts + at) * width, width), width)] = value

    total.end(emit)
    take_quarters(2)
    early[6].start()
    for at in range(7):
        turn_copy(at).wait_send()
        g_copy(at).wait_send()
    for step in range(3):
        @pl.when(jnp.logical_and(here.z < 3, here.z >= step))
        def _(step=step):
            quarter(0, here.z - step, step, 1).wait_send()

        @pl.when(jnp.logical_and(here.z > 0, here.z <= 3 - step))
        def _(step=step):
            quarter(1, here.z + step, step, -1).wait_send()


def opening(tokens, gain_one, gain_two, ids, w_query, kv_weight, cot, cid, width=256):
    rows = tokens.shape[0]
    cols, wide = w_query.shape
    every = wide + kv_weight.shape[1]
    counts = every // (2 * width)
    low, f32 = jnp.bfloat16, jnp.float32
    dma = pltpu.SemaphoreType.DMA
    vm = pl.BlockSpec(memory_space=pltpu.VMEM)
    hbm = pl.BlockSpec(memory_space=pl.ANY)
    out_shape = [
        jax.ShapeDtypeStruct((rows, every), f32),
        jax.ShapeDtypeStruct((8 * rows, cols), low),
        jax.ShapeDtypeStruct((cols, 8 * rows), low),
        jax.ShapeDtypeStruct((cols, every), low),
        jax.ShapeDtypeStruct((rows, LANES), f32),
        jax.ShapeDtypeStruct((2, rows, LANES), f32),
        jax.ShapeDtypeStruct((2, rows, LANES), f32),
        jax.ShapeDtypeStruct((rows, 2 * rows), f32),
        jax.ShapeDtypeStruct((8, 4, rows // 4, cols), low),
        jax.ShapeDtypeStruct((8, cols), f32),
    ]
    scratch = [
        pltpu.VMEM((8 * rows, cols), low), dma((7,)), dma((7,)), dma((5,)),
        pltpu.VMEM((rows // 4, 8 * cols), low), dma((7,)), dma((7,)), dma((2, 3)), dma((2, 3)),
    ]
    scratch += reduce_scratch(counts, rows, width)
    kernel = functools.partial(open_kernel, rows, width, counts)
    return kernel_call(kernel, out_shape, [tokens, gain_one, gain_two, ids, w_query, kv_weight, cot],
                       [vm, vm, vm, vm, hbm, hbm, hbm], scratch, cid, "open",
                       early=(1, 2, 3, 5, 6, 7, 8, 9))


def ffn_kernel(rows, width, counts, x_low, attn, gain, w_gate, w_up, d_hidden, hidden, d_gate, d_up, act_t, tile_out,
               *refs, late, early, raw):
    here = Place()
    cols = gain.shape[1]
    act, weight, tiny_own, tiny_all, tiny_send, tiny_recv, dots, local_sems = refs[:8]
    tiny = Tiny(here, tiny_own, tiny_all, (tiny_send, tiny_recv), True)
    half_cols = counts * width
    local = [
        pltpu.make_async_copy(w_gate, weight.at[:, :half_cols], local_sems.at[0]),
        pltpu.make_async_copy(w_up, weight.at[:, half_cols:], local_sems.at[1]),
    ]
    for copy in local:
        copy.start()
    eye = diagonal()
    tiny_own[...] = jnp.zeros_like(tiny_own)

    def prepare(number, _):
        shard = here.shard(*turned(number))
        for at in range(rows // LANES):
            span = pl.ds(pl.multiple_of(shard * rows + at * LANES, LANES), LANES)
            resid = x_low[span, :].astype(jnp.float32) + attn[span, :].astype(jnp.float32)
            act[span, :] = (resid * gain[1:2, :]).astype(act.dtype)
            square = jnp.sum(resid * resid, axis=-1, keepdims=True)
            tiny_own[shard, at : at + 1, :] = jnp.sum(square * eye, axis=0, keepdims=True)
        return 0

    def before(stop):
        if stop == 1:
            lax.fori_loop(2, 6, prepare, 0)
        if stop == 2:
            lax.fori_loop(6, 8, prepare, 0)
            tiny.begin()

    lax.fori_loop(0, 2, prepare, 0)
    greet(here, slice_peers(here))
    for copy in local:
        copy.wait()
    product = products(here, act, weight, False, rows, width, counts)
    total = Reduce(here, counts, product, refs[8:19], before)
    leave_sems = refs[19]
    total.run()

    def flip(shard, _):
        span = pl.ds(pl.multiple_of(shard * rows, rows), rows)
        act_t[:, span] = act[span, :].T
        return 0

    lax.fori_loop(0, 8, flip, 0)
    early[0].start()
    tiny.end()
    tiles = rows // LANES
    mean = [from_tile(jnp.sum(tiny_all[:, at, :], axis=0, keepdims=True), eye) for at in range(tiles)]
    scale = lax.rsqrt(jnp.concatenate(mean, axis=0) / (8 * cols) + EPS)
    dots[...] = jnp.zeros_like(dots)
    late[0].wait()
    coeff = math.sqrt(2.0 / math.pi)

    def leave(which, at):
        span = pl.ds(pl.multiple_of(at * width, width), width)
        return pltpu.make_async_copy((hidden, d_gate, d_up)[which].at[:, span], raw[which].at[:, span],
                                     leave_sems.at[which, at])

    def emit(at, first, second):
        span = pl.ds(pl.multiple_of(at * width, width), width)
        gate, up = first * scale, second * scale
        inner = jnp.tanh(coeff * (gate + 0.044715 * (gate * gate * gate)))
        gelu = 0.5 * gate * (1.0 + inner)
        slope = 0.5 * (1.0 + inner) + 0.5 * gate * (1.0 - inner * inner) * (
            coeff * (1.0 + 3.0 * 0.044715 * gate * gate))
        cot = d_hidden[:, span]
        hidden[:, span] = (gelu * up).astype(hidden.dtype)
        back_gate, back_up = cot * up * slope, cot * gelu
        d_gate[:, span] = (back_gate * scale).astype(d_gate.dtype)
        d_up[:, span] = (back_up * scale).astype(d_up.dtype)
        dots[...] += jnp.sum(back_gate * gate + back_up * up, axis=-1, keepdims=True)
        for which in range(3):
            leave(which, at).start()

    total.end(emit)
    tile_out[...] = jnp.zeros_like(tile_out)
    for at in range(counts):
        for which in range(3):
            leave(which, at).wait()
    to_tile(tile_out, 0, dots[...] * (scale * scale * (1.0 / (8 * cols))), eye)


def ffn_scatter(x_low, attn, gain, w_gate, w_up, d_hidden, cid, width=512):
    rows, half = d_hidden.shape
    cols = gain.shape[1]
    counts = half // width
    low, f32 = jnp.bfloat16, jnp.float32
    dma = pltpu.SemaphoreType.DMA
    vm = pl.BlockSpec(memory_space=pltpu.VMEM)
    hbm = pl.BlockSpec(memory_space=pl.ANY)
    out_shape = [jax.ShapeDtypeStruct((rows, half), low)] * 3 + [
        jax.ShapeDtypeStruct((cols, 8 * rows), low),
        jax.ShapeDtypeStruct((8, LANES), f32),
    ]
    scratch = [
        pltpu.VMEM((8 * rows, cols), low),
        pltpu.VMEM((cols, 2 * half), low),
        pltpu.VMEM((8, 8, LANES), f32),
        pltpu.VMEM((8, 8, LANES), f32),
        dma((7,)), dma((7,)),
        pltpu.VMEM((rows, 1), f32),
        dma((2,)),
    ] + reduce_scratch(counts, rows, width) + [dma((3, counts))]
    kernel = functools.partial(ffn_kernel, rows, width, counts)
    return kernel_call(kernel, out_shape, [x_low, attn, gain, w_gate, w_up, d_hidden], [vm, vm, vm, hbm, hbm, vm],
                       scratch, cid, "ffn", late=(5,), early=(3,),
                       pieces=(0, 1, 2))


def load_own(spread, payload, width, counts, sems):
    copies = []
    for half in range(2):
        for at in range(counts):
            first = at * width + (half * counts * width if len(payload) == 1 else 0)
            src = payload[half % len(payload)].at[:, first : first + width]
            copies.append(pltpu.make_async_copy(src, spread.slot(0, half, at), sems.at[half, at]))
    return copies


def chip_place(here, per):
    def place(at):
        return here.shard(at // (2 * per), at // per % 2) * per + at % per

    return place


def back_kernel(rows, width, counts, act_t, w_gate, w_up, d_gate, d_up, dots, x_low, attn, gain, d_norm, gain_grad,
                grad_gate, grad_up, *refs, late):
    here = Place()
    spread = Spread(here, counts, refs[:7])
    tiny_all, tiny_send, tiny_recv, own_sems, weight, sums, grads, staged, local_sems, out_sems = refs[7:17]
    contrib, rest, rest_sems = refs[17:20]
    line = Line(here, 4, [contrib, d_norm] + list(refs[20:]), chip_place(here, 2))
    tiny = Tiny(here, dots, tiny_all, (tiny_send, tiny_recv), False)
    half_cols = counts * width
    local = [
        pltpu.make_async_copy(w_gate, weight.at[:, :half_cols], local_sems.at[0]),
        pltpu.make_async_copy(w_up, weight.at[:, half_cols:], local_sems.at[1]),
    ]
    own = load_own(spread, (d_gate, d_up), width, counts, own_sems)
    for copy in own + local:
        copy.start()
    greet(here, tiny.peers, True)
    for copy in own:
        copy.wait()
    tiny.begin()
    spread.begin()
    sums[...] = jnp.zeros_like(sums)
    for copy in local + late:
        copy.wait()

    def columns(half, at):
        return pl.ds(pl.multiple_of((half * counts + at) * width, width), width)

    def clear(at, _):
        grads[:, columns(0, at)] = jnp.zeros((grads.shape[0], width), jnp.float32)
        return 0

    lax.fori_loop(0, 2 * counts, clear, 0)

    def blocks(across, half, at):
        cols = columns(half, at)
        gained = grads[:, cols]
        for other in range(2):
            row = row_span(here, across, other, rows)
            block = spread.got[across, (spread.core + other) % 2, half, at]
            sums[row, :] += dot_nt(block, weight[:, cols])
            gained = gained + dot_nn(act_t[:, row], block)
        grads[:, cols] = gained

    def leave(half, at):
        spot = pl.ds(pl.multiple_of(at * width, width), width)
        return pltpu.make_async_copy(staged.at[half], (grad_gate, grad_up)[half].at[:, spot],
                                     out_sems.at[half, at])

    eye = diagonal()
    gain_grad[...] = jnp.zeros_like(gain_grad)

    def close_chip(chip, target):
        def close_shard(other, _):
            shard = here.shard(chip, other)
            span = pl.ds(pl.multiple_of(shard * rows, rows), rows)
            loads = [pltpu.make_async_copy(src.at[span, :], rest.at[at], rest_sems.at[at])
                     for at, src in enumerate((x_low, attn))]
            for copy in loads:
                copy.start()
            for copy in loads:
                copy.wait()
            for at in range(rows // LANES):
                span = pl.ds(pl.multiple_of(shard * rows + at * LANES, LANES), LANES)
                piece = slice(at * LANES, (at + 1) * LANES)
                dot = from_tile(tiny_all[shard, at : at + 1, :], eye)
                resid = rest[0, piece, :].astype(jnp.float32) + rest[1, piece, :].astype(jnp.float32)
                value = sums[span, :]
                target[span, :] = (value * gain[1:2, :] - resid * dot).astype(target.dtype)
                gain_grad[...] += jnp.sum(value * resid, axis=0, keepdims=True)
            return 0

        lax.fori_loop(0, 2, close_shard, 0)

    def done(stage, at):
        @pl.when(jnp.logical_and(stage == 3, at > 0))
        def _():
            leave(0, at - 1).wait()
            leave(1, at - 1).wait()

        @pl.when(stage == 3)
        def _():
            for half in range(2):
                staged[half] = grads[:, columns(half, at)].astype(staged.dtype)
            leave(0, at).start()
            leave(1, at).start()

        @pl.when(jnp.logical_and(at == counts - 1, stage == 0))
        def _():
            close_chip(0, contrib)
            line.launch(0, 4)

        @pl.when(jnp.logical_and(at == counts - 1, stage == 2))
        def _():
            lax.fori_loop(1, 3, lambda chip, _: (close_chip(chip, d_norm), 0)[1], 0)

    def hook(step):
        @pl.when(jnp.logical_and(step >= counts, step < counts + 6))
        def _():
            line.step(step - counts)

    tiny.end()
    spread.run(blocks, hook, done)
    close_chip(3, d_norm)
    line.settle()
    spread.end()

    def drain(at, _):
        leave(0, at).wait()
        leave(1, at).wait()
        return 0

    lax.fori_loop(counts - 1, counts, drain, 0)


def back_gather(act_t, w_gate, w_up, d_gate, d_up, dots, x_low, attn, gain, cid, width=512):
    cols, total = act_t.shape
    rows, half = d_gate.shape
    counts = half // width
    low, f32 = jnp.bfloat16, jnp.float32
    dma = pltpu.SemaphoreType.DMA
    vm = pl.BlockSpec(memory_space=pltpu.VMEM)
    hbm = pl.BlockSpec(memory_space=pl.ANY)
    out_shape = [
        jax.ShapeDtypeStruct((total, cols), low),
        jax.ShapeDtypeStruct((1, cols), f32),
        jax.ShapeDtypeStruct((cols, half), low),
        jax.ShapeDtypeStruct((cols, half), low),
    ]
    scratch = spread_scratch(counts, rows, width) + [
        pltpu.VMEM((8, 8, LANES), f32), dma((7,)), dma((7,)), dma((2, counts)),
        pltpu.VMEM((cols, 2 * half), low),
        pltpu.VMEM((total, cols), f32),
        pltpu.VMEM((cols, 2 * half), f32),
        pltpu.VMEM((2, cols, width), low),
        dma((2,)), dma((2, counts)),
        pltpu.VMEM((total, cols), low),
        pltpu.VMEM((2, rows, cols), low),
        dma((2,)),
    ] + line_scratch(4, (4 * rows // 2, cols), low)
    operands = [act_t, w_gate, w_up, d_gate, d_up, dots, x_low, attn, gain]
    kernel = functools.partial(back_kernel, rows, width, counts)
    return kernel_call(kernel, out_shape, operands, [vm] + [hbm] * 4 + [vm, hbm, hbm, vm], scratch, cid, "back",
                       [vm, vm, hbm, hbm], (0,))


def down_kernel(rows, width, counts, cot, weight, hidden, d_norm, ffn, d_attn, grad, *refs, late, early):
    here = Place()
    spread = Spread(here, counts, refs[:7])
    own_sems, sums, grads, staged, out_sems, norm_out = refs[7:13]
    place = chip_place(here, 2)
    norm_line = Line(here, 12, [d_norm, norm_out] + list(refs[13:]), lambda at: place(at + 4))
    own = load_own(spread, (hidden,), width, counts, own_sems)
    for copy in own:
        copy.start()
    greet(here, slice_peers(here), True)
    norm_line.begin()
    for copy in own:
        copy.wait()
    spread.begin()
    sums[...] = jnp.zeros_like(sums)
    grads[...] = jnp.zeros_like(grads)
    for copy in late:
        copy.wait()

    def columns(half, at):
        return pl.ds(pl.multiple_of((half * counts + at) * width, width), width)

    def blocks(across, half, at):
        cols = columns(half, at)
        gained = grads[cols, :]
        for other in range(2):
            row = row_span(here, across, other, rows)
            block = spread.got[across, (spread.core + other) % 2, half, at]
            sums[row, :] += dot_nn(block, weight[cols, :])
            gained = gained + dot_tn(block, cot[row, :])
        grads[cols, :] = gained

    def leave(half, at):
        return pltpu.make_async_copy(staged.at[at % 2, half], grad.at[columns(half, at), :], out_sems.at[half, at])

    def done(stage, at):
        @pl.when(jnp.logical_and(stage == 3, at > 1))
        def _():
            leave(0, at - 2).wait()
            leave(1, at - 2).wait()

        @pl.when(stage == 3)
        def _():
            for half in range(2):
                staged[at % 2, half] = grads[columns(half, at), :].astype(staged.dtype)
            leave(0, at).start()
            leave(1, at).start()


    def hook(step):
        @pl.when(step % 3 < 2)
        def _():
            norm_line.step(step // 3 * 2 + step % 3)

    spread.run(blocks, hook, done)
    ffn[...] = sums[...].astype(ffn.dtype)
    early[0].start()
    norm_line.settle()

    def add_norm(at, _):
        def add(source):
            span = row_span(here, at // 2, at % 2, rows)
            d_attn[span, :] = (cot[span, :].astype(jnp.float32) + source[span, :].astype(jnp.float32)).astype(
                d_attn.dtype)

        @pl.when(at < 2)
        def _():
            add(d_norm)

        @pl.when(at >= 2)
        def _():
            add(norm_out)
        return 0

    lax.fori_loop(0, 8, add_norm, 0)
    spread.end()

    def drain(at, _):
        leave(0, at).wait()
        leave(1, at).wait()
        return 0

    lax.fori_loop(counts - 2, counts, drain, 0)


def down_gather(cot, weight, hidden, d_norm, cid, width=256):
    total, cols = cot.shape
    rows, every = hidden.shape
    counts = every // (2 * width)
    low, f32 = jnp.bfloat16, jnp.float32
    dma = pltpu.SemaphoreType.DMA
    vm = pl.BlockSpec(memory_space=pltpu.VMEM)
    hbm = pl.BlockSpec(memory_space=pl.ANY)
    out_shape = [
        jax.ShapeDtypeStruct((total, cols), low),
        jax.ShapeDtypeStruct((total, cols), low),
        jax.ShapeDtypeStruct(weight.shape, low),
    ]
    scratch = spread_scratch(counts, rows, width) + [
        dma((2, counts)),
        pltpu.VMEM((total, cols), f32),
        pltpu.VMEM(weight.shape, f32),
        pltpu.VMEM((2, 2, width, cols), low),
        dma((2, counts)),
        pltpu.VMEM((total, cols), low),
    ] + line_scratch(12, (12 * rows // 2, cols), low)
    kernel = functools.partial(down_kernel, rows, width, counts)
    return kernel_call(kernel, out_shape, [cot, weight, hidden, d_norm], [vm, vm, hbm, vm], scratch, cid, "down",
                       [vm, vm, hbm], (0, 1), (0,))


def attend_kernel(rows, heads, cols, width, counts, qkv, rms, cos, sin, mask, w_out, g_col, w_down, attn, mixed_all,
                  kv, probs, queries, pair_rms, d_hidden, *refs, late, early, raw):
    here = Place()
    spread = Spread(here, 1, refs[:7])
    part, pair_sems, tiny_own, tiny_pair, mixed_sems = refs[7:12]
    product = products(here, g_col, w_down, True, rows, width, counts)
    total = Reduce(here, counts, product, refs[12:23])
    piece = rows // 2

    def place(at):
        across, other, half_at = spread.block(at)
        return here.shard(across, other) * 2 + half_at

    line = Line(here, 16, [part, attn] + list(refs[23:31]), place)
    got, core = spread.got, here.core
    greet(here, slice_peers(here), True)
    half = HD // 2
    scale = 1.0 / math.sqrt(HD)
    wide = heads * HD

    def rotated(first):
        lead = qkv[:, first : first + half] * rms[...]
        trail = qkv[:, first + half : first + HD] * rms[...]
        return lead * cos[0] - trail * sin[0], trail * cos[0] + lead * sin[0]

    low_k, high_k = rotated(wide)
    kv[0, :, :half] = low_k.astype(kv.dtype)
    kv[0, :, half:HD] = high_k.astype(kv.dtype)
    for at in range(2):
        first = HD + at * half
        kv[0, :, first : first + half] = (qkv[:, wide + first : wide + first + half] * rms[...]).astype(kv.dtype)
    eye = diagonal()
    tiny_own[...] = jnp.zeros_like(tiny_own)
    to_tile(tiny_own, 0, rms[:, :1], eye)
    pair_rms[0] = rms[...]
    pair = remote(kv.at[0], kv.at[1], pair_sems.at[0], pair_sems.at[1], spread.ydev)
    tiny = remote(tiny_own, tiny_pair, pair_sems.at[2], pair_sems.at[3], spread.ydev)
    for head in range(heads):
        if head == 1:
            pair.start()
            tiny.start()
        lead, trail = rotated(head * HD)
        queries[:, head * HD : head * HD + half] = (lead * scale).astype(queries.dtype)
        queries[:, head * HD + half : (head + 1) * HD] = (trail * scale).astype(queries.dtype)
    early[2].start()
    pair.wait()
    early[0].start()
    for copy in late:
        copy.wait()

    def one_head(head, _):
        query = queries[:, pl.ds(pl.multiple_of(head * HD, HD), HD)]
        scores = jnp.concatenate([dot_nt(query, kv[0, :, :HD]), dot_nt(query, kv[1, :, :HD])], axis=1)
        scores = jnp.where(mask[...] > 0, scores, NEG)
        expd = jnp.exp(scores - jnp.max(scores, axis=-1, keepdims=True))
        prob = expd / jnp.sum(expd, axis=-1, keepdims=True)
        probs[head] = prob
        prob_low = prob.astype(jnp.bfloat16)
        mixed = dot_nn(prob_low[:, :rows], kv[0, :, HD:]) + dot_nn(prob_low[:, rows:], kv[1, :, HD:])
        span = pl.ds(pl.multiple_of(head * HD, HD), HD)
        for half_at in range(2):
            low_mixed = mixed[half_at * piece : (half_at + 1) * piece, :].astype(got.dtype)
            got[0, core, half_at, 0, :, span] = low_mixed
        return 0

    lax.fori_loop(0, heads, one_head, 0)
    early[1].start()
    spread.begin_rows()

    def mixed_copy(at):
        across, other, half_at = spread.block(at)
        span = pl.ds(pl.multiple_of(place(at) * piece, piece), piece)
        return pltpu.make_async_copy(got.at[across, (core + other) % 2, half_at, 0], mixed_all.at[span, :],
                                     mixed_sems.at[at])

    def one_step(step, _):
        spread.receive_rows(step)

        @pl.when(step < 16)
        def _():
            across, other, half_at = spread.block(step)
            value = dot_nn(got[across, (core + other) % 2, half_at, 0], w_out[...])
            part[pl.ds(pl.multiple_of(place(step) * piece, piece), piece), :] = value.astype(part.dtype)
            mixed_copy(step).start()
            line.launch(step, 1)

        @pl.when(step >= 2)
        def _():
            total.advance(step - 2)

        @pl.when(step >= 4)
        def _():
            line.step(step - 4)
        return 0

    lax.fori_loop(0, 20, one_step, 0)
    line.end(16)
    early[3].start()

    leave_sems = refs[31]

    def leave(half_at, at):
        span = pl.ds(pl.multiple_of((half_at * counts + at) * width, width), width)
        return pltpu.make_async_copy(d_hidden.at[:, span], raw[0].at[:, span], leave_sems.at[half_at, at])

    def emit(at, first, second):
        for half_at, value in enumerate((first, second)):
            d_hidden[:, pl.ds(pl.multiple_of((half_at * counts + at) * width, width), width)] = value
            leave(half_at, at).start()

    total.end(emit)
    for hop in range(3):
        spread.x_copy(hop, 0).wait_send()
        spread.y_copy(hop, 0).wait_send()
    for stage in range(4):
        for stream in range(2):
            spread.sib_copy(stage, stream, 0).wait_send()
    for at in range(16):
        mixed_copy(at).wait()
    for at in range(counts):
        for half_at in range(2):
            leave(half_at, at).wait()
    tiny.wait()
    for at in range(rows // LANES):
        values = jnp.broadcast_to(from_tile(tiny_pair[at : at + 1, :], eye), (LANES, LANES))
        pair_rms[1, at * LANES : (at + 1) * LANES, :] = values


def attend(qkv, rms, cos, sin, mask, w_out, g_col, w_down, cid, width=512):
    rows = qkv.shape[0]
    wide, cols = w_out.shape
    heads = wide // HD
    counts = w_down.shape[0] // (2 * width)
    low, f32 = jnp.bfloat16, jnp.float32
    dma = pltpu.SemaphoreType.DMA
    vm = pl.BlockSpec(memory_space=pltpu.VMEM)
    out_shape = [
        jax.ShapeDtypeStruct((8 * rows, cols), low),
        jax.ShapeDtypeStruct((8 * rows, wide), low),
        jax.ShapeDtypeStruct((2, rows, 2 * HD), low),
        jax.ShapeDtypeStruct((heads, rows, 2 * rows), f32),
        jax.ShapeDtypeStruct((rows, wide), low),
        jax.ShapeDtypeStruct((2,) + rms.shape, f32),
        jax.ShapeDtypeStruct((rows, w_down.shape[0]), f32),
    ]
    scratch = spread_scratch(1, rows // 2, wide) + [
        pltpu.VMEM((8 * rows, cols), low), dma((4,)),
        pltpu.VMEM((8, LANES), f32), pltpu.VMEM((8, LANES), f32), dma((16,)),
    ] + reduce_scratch(counts, rows, width) + line_scratch(16, (8 * rows, cols), low) + [dma((2, counts))]
    kernel = functools.partial(attend_kernel, rows, heads, cols, width, counts)
    operands = [qkv, rms, cos, sin, mask, w_out, g_col, w_down]
    out_specs = [vm, pl.BlockSpec(memory_space=pl.ANY)] + [vm] * 5
    return kernel_call(kernel, out_shape, operands, [vm] * 8, scratch, cid, "attend", out_specs, (4, 5, 6, 7), (2, 3, 4, 0), (6,))


def tail_kernel(rows, heads, per, d_attn, w_out, queries, kv, probs, rms, cos, sin, act_t, w_qkv, ffn, x_low,
                attn, gain, gain_grad, mixed_all, d_tok, out, grad_query, grad_out, kv_sum, gains, *refs, late, early):
    here = Place()
    width = HD
    counts = heads // 2
    part = rows // 2
    refs = list(refs)
    line_counts = 8 * per
    cols = d_attn.shape[1]
    extra = cols // (rows // per)

    def take(count):
        taken_refs = refs[:count]
        del refs[:count]
        return taken_refs

    total_refs = take(11)
    spread = Spread(here, 1, take(7))
    d_mixed, tiny_own, tiny_all, d_kv, give, taken, give_sems, tiny_send, tiny_recv = take(9)
    grad, grad_mixed, gain_sum, tile, tile_send, tile_recv, put_sems, local_sems, mixed_two, mixed_sems = take(10)

    def far(at):
        return at // (2 * per), at // per % 2

    def near(at):
        return spread.block(jnp.minimum(at, line_counts - 1))

    def place_ffn(at):
        return here.shard(*far(at)) * per + at % per

    def place_tok(at):
        across, other, half_at = near(at)
        return jnp.where(at < line_counts, here.shard(across, other) * per + half_at, at)

    gain_tiles, ffn_sum, leaving = take(3)
    by_chip = chip_place(here, per)
    line = Line(here, line_counts, [ffn, ffn_sum] + take(8), by_chip)
    contrib, summed = take(2)
    line_tok = Line(here, line_counts + extra, [contrib, summed] + take(8), place_tok)
    tiny = Tiny(here, tiny_own, tiny_all, (tiny_send, tiny_recv), False)
    got, core = spread.got, here.core
    product = products(here, d_attn, w_out, True, rows, width, counts)
    total = Reduce(here, counts, product, total_refs)
    greet(here, tiny.peers, True)
    line.begin()
    grad_mixed[...] = jnp.zeros_like(grad_mixed)

    def mixed_copy(step):
        span = pl.ds(pl.multiple_of(step * rows, rows), rows)
        return pltpu.make_async_copy(mixed_all.at[span, :], mixed_two.at[step % 2], mixed_sems.at[step % 2])

    mixed_copy(0).start()

    def beside(step):
        line.step(step)

        @pl.when(step < 8)
        def _():
            span = pl.ds(pl.multiple_of(step * rows, rows), rows)
            mixed_copy(step).wait()

            @pl.when(step < 7)
            def _():
                mixed_copy(step + 1).start()

            grad_mixed[...] += dot_tn(mixed_two[step % 2], d_attn[span, :])

    done = total.run(beside)
    grad_out[...] = grad_mixed[...].astype(grad_out.dtype)
    early[1].start()

    def land(at, first, second):
        for half_at, value in enumerate((first, second)):
            d_mixed[:, pl.ds(pl.multiple_of((half_at * counts + at) * width, width), width)] = value.astype(
                d_mixed.dtype)

    total.end(land)
    half = HD // 2
    scale = 1.0 / math.sqrt(HD)
    depth = w_qkv.shape[0] * 8
    d_kv[...] = jnp.zeros_like(d_kv)
    for copy in late:
        copy.wait()

    def one_head(head, dots):
        span = pl.ds(pl.multiple_of(head * HD, HD), HD)
        query = queries[:, span]
        cot = d_mixed[:, span]
        prob = probs[head]
        d_prob = jnp.concatenate([dot_nt(cot, kv[0, :, HD:]), dot_nt(cot, kv[1, :, HD:])], axis=1)
        delta = jnp.sum(prob * d_prob, axis=-1, keepdims=True)
        d_score = (prob * (d_prob - delta)).astype(jnp.bfloat16)
        prob_low = prob.astype(jnp.bfloat16)
        d_query = (dot_nn(d_score[:, :rows], kv[0, :, :HD]) + dot_nn(d_score[:, rows:], kv[1, :, :HD])) * scale
        for side in range(2):
            keys = slice(side * rows, (side + 1) * rows)
            d_kv[side, :, :HD] += dot_tn(d_score[:, keys], query)
            d_kv[side, :, HD:] += dot_tn(prob_low[:, keys], cot)
        dots = dots + jnp.sum(d_query * query.astype(jnp.float32), axis=-1, keepdims=True)
        lead, trail = d_query[:, :half], d_query[:, half:]
        first = ((lead * cos[0] + trail * sin[0]) * rms[0]).astype(got.dtype)
        second = ((trail * cos[0] - lead * sin[0]) * rms[0]).astype(got.dtype)
        line.step(done + head)
        for rows_at in range(2):
            piece = slice(rows_at * part, (rows_at + 1) * part)
            got[0, core, rows_at, 0, :, pl.ds(pl.multiple_of(head * HD, HD), half)] = first[piece, :]
            got[0, core, rows_at, 0, :, pl.ds(pl.multiple_of(head * HD + half, half), half)] = second[piece, :]

        return dots

    dots = lax.fori_loop(0, heads, one_head, jnp.zeros((rows, 1), jnp.float32))
    eye = diagonal()
    tiny_own[...] = jnp.zeros_like(tiny_own)
    for side in (1, 0):
        d_key, d_value = d_kv[side, :, :HD], d_kv[side, :, HD:]
        own = jnp.sum(d_key * kv[side, :, :HD].astype(jnp.float32) +
                      d_value * kv[side, :, HD:].astype(jnp.float32), axis=-1, keepdims=True)
        if side == 0:
            own = own + dots * (1.0 / scale)
        own = own * (rms[side] * rms[side] * (1.0 / depth))
        to_tile(tiny_own, side * (rows // LANES), own, eye)
        lead, trail = d_key[:, :half], d_key[:, half:]
        parts = [(lead * cos[side] + trail * sin[side]) * rms[side],
                 (trail * cos[side] - lead * sin[side]) * rms[side],
                 d_value[:, :half] * rms[side], d_value[:, half:] * rms[side]]
        for at, value in enumerate(parts):
            if side == 1:
                give[:, at * half : (at + 1) * half] = value.astype(give.dtype)
            else:
                d_kv[0, :, at * half : (at + 1) * half] = value
    given = remote(give, taken, give_sems.at[0], give_sems.at[1], spread.ydev)
    given.start()
    grad[...] = jnp.zeros_like(grad)
    line.steps(done + heads, done + heads + 2)
    given.wait()
    for rows_at in range(2):
        piece = slice(rows_at * part, (rows_at + 1) * part)
        value = d_kv[0, piece, :] + taken[piece, :].astype(jnp.float32)
        got[0, core, rows_at, 0, :, heads * HD :] = value.astype(got.dtype)
    tiny.begin()
    spread.begin_rows()
    gain_sum[...] = jnp.zeros_like(gain_sum)
    tiny.end()

    def block_of(at):
        across, other, half_at = near(at)
        shard, partner = here.shard(across, other), here.shard((across + 2) % 4, other)
        block = got[across, (core + other) % 2, half_at, 0]
        first = pl.multiple_of(shard * rows + half_at * part, part)
        for tile_at in range(part // LANES):
            row = pl.ds(pl.multiple_of(first + tile_at * LANES, LANES), LANES)
            low_at = half_at * (part // LANES) + tile_at
            kept = rows // LANES + low_at
            dot = from_tile(tiny_all[shard, pl.ds(low_at, 1), :] + tiny_all[partner, pl.ds(kept, 1), :], eye)
            value = dot_nt(block[tile_at * LANES : (tile_at + 1) * LANES, :], w_qkv[...])
            x_rows = x_low[row, :].astype(jnp.float32)
            contrib[row, :] = (value * gain[0:1, :] - x_rows * dot).astype(contrib.dtype)
            gain_sum[...] += jnp.sum(value * x_rows, axis=0, keepdims=True)
        line_tok.launch(at, 1)

        @pl.when(other == 1)
        def _():
            twin = got[across, core, half_at, 0]
            twin_first = pl.multiple_of(here.shard(across, 0) * rows + half_at * part, part)
            rows_t, twin_t = act_t[:, pl.ds(first, part)], act_t[:, pl.ds(twin_first, part)]
            for at_col in range((heads + 2) * HD // 512):
                span = slice(at_col * 512, (at_col + 1) * 512)
                grad[:, span] += dot_nn(rows_t, block[:, span]) + dot_nn(twin_t, twin[:, span])

    me = here.shard(0, 0)
    columns = pl.ds(pl.multiple_of(me * cols, cols), cols)
    chunk = line.chunk

    def landing(which, at):
        sub = at % per if which == 0 else near(at)[2]
        return (out, d_tok)[which].at[pl.ds(pl.multiple_of(sub * chunk, chunk), chunk), columns]

    def leaver(which, at):
        return (leaving, line_tok.from_end)[which].at[at]

    def put(which, at):
        goal = here.device(*(far(at) if which == 0 else near(at)[:2]))
        return remote(leaver(which, at), landing(which, at), put_sems.at[which, 0, at], put_sems.at[which, 1, at],
                      goal)

    def keep(which, at):
        spot = at % per if which == 0 else near(at)[2]
        return pltpu.make_async_copy(leaver(which, at), landing(which, at), local_sems.at[which, spot])

    def emit(which, at):
        if which == 1:
            row = line_tok.rows(at)
            value = d_attn[row, :].astype(jnp.float32) + summed[row, :].astype(jnp.float32)
            line_tok.from_end[at] = value.astype(out.dtype)
            return
        row = pl.ds(pl.multiple_of(place_ffn(at) * chunk, chunk), chunk)

        def leave(source):
            value = x_low[row, :].astype(jnp.float32) + attn[row, :].astype(jnp.float32)
            leaving[at] = (value + source[row, :].astype(jnp.float32)).astype(out.dtype)

        leave(ffn_sum)

    def is_own(which, at):
        return at < per if which == 0 else jnp.logical_and(at < 4, at % 2 == 0)

    def send(which, at):
        own = is_own(which, at)

        @pl.when(own)
        def _():
            keep(which, at).start()

        @pl.when(jnp.logical_not(own))
        def _():
            put(which, at).start()

    def stage_step(step, _):
        spread.receive_rows(step)

        @pl.when(step < line_counts)
        def _():
            block_of(step)

        @pl.when(step < 3)
        def _():
            line.step(done + heads + 2 + step)

        @pl.when(step >= 4)
        def _():
            line_tok.step(step - 4)

        @pl.when(step > 0)
        def _():
            send(0, step - 1)

        @pl.when(line.inner == 0)
        def _():
            line.up(step).wait_send()
            line.down(step).wait_recv()

        emit(0, step)

        @pl.when(jnp.logical_and(line.inner == 1, step > 7))
        def _():
            send(1, step - 8)

        @pl.when(jnp.logical_and(line.inner == 1, step > 6))
        def _():
            emit(1, step - 7)
        return 0

    lax.fori_loop(0, line_counts, stage_step, 0)
    for half_at in range(cols // (rows // per)):
        span = pl.ds(line_counts * (rows // per) + half_at * (rows // per), rows // per)
        source = slice(half_at * (rows // per), (half_at + 1) * (rows // per))
        contrib[span, :] = grad[source, heads * HD :].astype(contrib.dtype)
    line_tok.launch(line_counts, extra)
    grad_query[...] = grad[:, : heads * HD].astype(grad_query.dtype)
    early[0].start()
    for at in range(cols // LANES):
        tile[at : at + 1, :] = gain_sum[:, at * LANES : (at + 1) * LANES]
        spot = cols // LANES + at
        tile[spot : spot + 1, :] = gain_grad[:, at * LANES : (at + 1) * LANES]

    def tile_copy(step):
        return remote(tile, gain_tiles.at[here.z], tile_send.at[step], tile_recv.at[step],
                      (here.dp, here.seq, (here.z + step + 1) % 4))

    send(0, line_counts - 1)
    line.drain()
    for step in range(3):
        tile_copy(step).start()
    gain_tiles[here.z] = tile[...]

    @pl.when(line.inner == 1)
    def _():
        start = line_counts - 4

        def both(at, _):
            line_tok.step(at)

            @pl.when(at < line_counts + 4)
            def _():
                send(1, at - 4)

            @pl.when(at < line_counts + 3)
            def _():
                emit(1, at - 3)
            return 0

        lax.fori_loop(start, line_counts + extra + 2, both, 0)

        def drain(at, _):
            line_tok.down(at).wait_send()
            return 0

        lax.fori_loop(0, line_counts + extra, drain, 0)

    @pl.when(line.inner == 0)
    def _():
        def arrive(at, _):
            line_tok.up(at).wait_send()
            line_tok.down(at).wait_recv()

            @pl.when(jnp.logical_and(at > 0, at <= line_counts))
            def _():
                send(1, at - 1)

            @pl.when(at < line_counts)
            def _():
                emit(1, at)
            return 0

        lax.fori_loop(0, line_counts + extra, arrive, 0)

    for half_at in range(extra):
        span = pl.ds((line_counts + half_at) * chunk, chunk)
        kv_sum[half_at * chunk : (half_at + 1) * chunk, :] = summed[span, :]
    for hop in range(3):
        spread.x_copy(hop, 0).wait_send()
        spread.y_copy(hop, 0).wait_send()
    for stage in range(4):
        spread.sib_copy(stage, 0, 0).wait_send()
        spread.sib_copy(stage, 1, 0).wait_send()

    for which in range(2):
        def finish(at, _, which=which):
            own = is_own(which, at)

            @pl.when(own)
            def _():
                keep(which, at).wait()

            @pl.when(jnp.logical_not(own))
            def _():
                put(which, at).wait()
            return 0

        lax.fori_loop(0, line_counts, finish, 0)
        if which == 0:
            early[2].start()
    for step in range(3):
        tile_copy(step).wait()
    gains[...] = gain_tiles[0] + gain_tiles[1] + gain_tiles[2] + gain_tiles[3]


def tail(d_attn, w_out, queries, kv, probs, rms, cos, sin, act_t, w_qkv, ffn, x_low, attn, gain, gain_grad,
         mixed_all, cid,
 per=2):
    total, cols = d_attn.shape
    rows = total // 8
    wide = w_out.shape[0]
    heads = wide // HD
    low, f32 = jnp.bfloat16, jnp.float32
    dma = pltpu.SemaphoreType.DMA
    vm = pl.BlockSpec(memory_space=pltpu.VMEM)
    counts = 8 * per
    chunk = rows // per
    extra = cols // chunk
    long = (total + cols, cols)
    out_shape = [
        jax.ShapeDtypeStruct((rows, 8 * cols), low),
        jax.ShapeDtypeStruct((rows, 8 * cols), low),
        jax.ShapeDtypeStruct((cols, wide), low),
        jax.ShapeDtypeStruct(w_out.shape, low),
        jax.ShapeDtypeStruct((cols, 2 * HD), low),
        jax.ShapeDtypeStruct((8, LANES), f32),
    ]
    scratch = reduce_scratch(heads // 2, rows, HD, 2) + spread_scratch(1, rows // 2, wide + 2 * HD)
    scratch += [
        pltpu.VMEM((rows, wide), low),
        pltpu.VMEM((8, LANES), f32),
        pltpu.VMEM((8, 8, LANES), f32),
        pltpu.VMEM((2, rows, 2 * HD), f32),
        pltpu.VMEM((rows, 2 * HD), low),
        pltpu.VMEM((rows, 2 * HD), low),
        dma((2,)), dma((7,)), dma((7,)),
        pltpu.VMEM(w_qkv.shape, f32),
        pltpu.VMEM(w_out.shape, f32),
        pltpu.VMEM((1, cols), f32),
        pltpu.VMEM((8, LANES), f32),
        dma((3,)), dma((3,)), dma((2, 2, counts)), dma((2, per)),
        pltpu.VMEM((2, rows, wide), low), dma((2,)),
        pltpu.VMEM((4, 8, LANES), f32),
        pltpu.VMEM((total, cols), low),
        pltpu.VMEM((counts, chunk, cols), low),
    ] + line_scratch(counts, (total, cols), low)
    scratch += [pltpu.VMEM(long, low), pltpu.VMEM(long, low)] + line_scratch(counts + extra, long, low)
    operands = [d_attn, w_out, queries, kv, probs, rms, cos, sin, act_t, w_qkv, ffn, x_low, attn, gain,
                gain_grad, mixed_all]
    kernel = functools.partial(tail_kernel, rows, heads, per)
    specs = [vm] * (len(operands) - 1) + [pl.BlockSpec(memory_space=pl.ANY)]
    return kernel_call(kernel, out_shape, operands, specs, scratch, cid, "tail",
                       late=(2, 3, 4, 8, 9, 11, 12), early=(2, 3, 1))


LANES = 128


def acts_move(
    tokens, seg_ids, gain_attn, w_query, kv_weight, w_out, gain_ffn, w_gate, w_up, w_down, d_out
):
    qkv, x_low, act_one_t, w_qkv, rms, cos, sin, mask, g_parts, small = opening(
        tokens, gain_attn, gain_ffn, seg_ids, w_query, kv_weight, d_out, 1
    )
    g_low = g_parts.reshape(x_low.shape)
    attn, mixed_all, kv, probs, queries, pair_rms, d_hidden = attend(
        qkv, rms, cos, sin, mask, w_out, g_low, w_down, 2
    )
    hidden, d_gate, d_up, act_two_t, dots = ffn_scatter(x_low, attn, small, w_gate, w_up, d_hidden, 4)
    d_norm, grad_gain_two, grad_gate, grad_up = back_gather(
        act_two_t, w_gate, w_up, d_gate, d_up, dots, x_low, attn, small, 5
    )
    ffn, d_attn, grad_down = down_gather(g_low, w_down, hidden, d_norm, 6)
    d_tokens, out, grad_query, grad_out, grad_kv, gain_sums = tail(
        d_attn,
        w_out,
        queries,
        kv,
        probs,
        pair_rms,
        cos,
        sin,
        act_one_t,
        w_qkv,
        ffn,
        x_low,
        attn,
        small,
        grad_gain_two,
        mixed_all,
        7,
    )
    gains = gain_sums.reshape(2, -1)
    wider = jnp.float32
    return (
        out,
        d_tokens.astype(wider),
        gains[0],
        grad_query.astype(wider),
        grad_kv.astype(wider),
        grad_out.astype(wider),
        gains[1],
        grad_gate.astype(wider),
        grad_up.astype(wider),
        grad_down.astype(wider),
    )


def solution(mesh):
    in_specs = (
        P(("dp", "seq"), None),
        P("dp"),
        P(("dp", "seq")),
        P(("dp", "seq"), "tensor"),
        P(("dp", "seq"), None),
        P("tensor", ("dp", "seq")),
        P(("dp", "seq")),
        P(("dp", "seq"), "tensor"),
        P(("dp", "seq"), "tensor"),
        P("tensor", ("dp", "seq")),
        P(("dp", "seq"), None),
    )
    out_specs = (
        P(("dp", "seq"), None),
        P(("dp", "seq"), None),
        P(("dp", "seq")),
        P(("dp", "seq"), "tensor"),
        P(("dp", "seq"), None),
        P("tensor", ("dp", "seq")),
        P(("dp", "seq")),
        P(("dp", "seq"), "tensor"),
        P(("dp", "seq"), "tensor"),
        P("tensor", ("dp", "seq")),
    )

    def shards(*arrays):
        tokens = arrays[0]
        sizes = tuple(mesh.shape[name] for name in ("dp", "seq", "tensor"))
        count = tokens.shape[0] * sizes[0] * sizes[1]
        plan = acts_move if sizes == (4, 2, 4) and count <= tokens.shape[1] else weights_move
        return plan(*arrays)

    return jax.shard_map(shards, mesh=mesh, in_specs=in_specs, out_specs=out_specs, check_vma=False)
```

```python
import functools
import math

import jax
import jax.numpy as jnp
from jax import lax
from jax.experimental import pallas as pl
from jax.experimental.pallas import tpu as pltpu
from jax.sharding import PartitionSpec as P

HD = 256


EPS = 1e-06
NEG = -1e30


def place_tables(segs):
    length = segs.shape[0]
    index = jnp.arange(length, dtype=jnp.int32)
    flags = jnp.concatenate([jnp.ones((1,), dtype=bool), segs[1:] != segs[:-1]])
    starts = lax.cummax(jnp.where(flags, index, jnp.zeros_like(index)), axis=0)
    places = index - starts
    half_size = HD // 2
    freqs = jnp.exp(jnp.arange(half_size, dtype=jnp.float32) * (-math.log(10000.0) / half_size))
    angles = places.astype(jnp.float32)[:, None] * freqs[None, :]
    return (places, jnp.cos(angles), jnp.sin(angles))


def rotate(vector, cos_table, sin_table):
    half_size = vector.shape[-1] // 2
    leading = vector[..., :half_size]
    trailing = vector[..., half_size:]
    return jnp.concatenate(
        [leading * cos_table - trailing * sin_table, trailing * cos_table + leading * sin_table],
        axis=-1,
    )


def rotate_back(vector, cos_table, sin_table):
    half_size = vector.shape[-1] // 2
    leading = vector[..., :half_size]
    trailing = vector[..., half_size:]
    return jnp.concatenate(
        [leading * cos_table + trailing * sin_table, trailing * cos_table - leading * sin_table],
        axis=-1,
    )


def matmul(left, right):
    return jnp.dot(left, right, preferred_element_type=jnp.float32)


def matmul_nt(left, right):
    return lax.dot_general(
        left, right, (((1,), (1,)), ((), ())), preferred_element_type=jnp.float32
    )


def matmul_tn(left, right):
    return lax.dot_general(
        left, right, (((0,), (0,)), ((), ())), preferred_element_type=jnp.float32
    )


def gelu_tanh(values):
    return jax.nn.gelu(values, approximate=True)


def norm_back(d_act, normed, rms_val, gain_val):
    scaled = d_act * gain_val
    return rms_val * (scaled - normed * jnp.mean(scaled * normed, axis=-1, keepdims=True))


def weights_move(
    tokens, seg_ids, gain_attn, w_query, kv_weight, w_out, gain_ffn, w_gate, w_up, w_down, d_out
):
    rows = tokens.shape[0]
    scale_factor = 1.0 / math.sqrt(HD)
    offset = lax.axis_index("seq") * rows
    places, cos_table, sin_table = place_tables(seg_ids)
    own_places = lax.dynamic_slice_in_dim(places, offset, rows, 0)
    own_segs = lax.dynamic_slice_in_dim(seg_ids, offset, rows, 0)
    own_cos = lax.dynamic_slice_in_dim(cos_table, offset, rows, 0)
    own_sin = lax.dynamic_slice_in_dim(sin_table, offset, rows, 0)
    allowed = (own_segs[:, None] == seg_ids[None, :]) & (own_places[:, None] >= places[None, :])
    full_query, full_out, full_kv, full_gain_one = (
        lax.all_gather(w_query, ("dp", "seq"), axis=0, tiled=True),
        lax.all_gather(w_out, ("dp", "seq"), axis=1, tiled=True),
        lax.all_gather(kv_weight, ("dp", "seq"), axis=0, tiled=True),
        lax.all_gather(gain_attn, ("dp", "seq"), axis=0, tiled=True),
    )
    gain_one = full_gain_one.astype(jnp.float32)
    inputs = tokens.astype(jnp.float32)
    rms_one = lax.rsqrt(jnp.mean(inputs * inputs, axis=-1, keepdims=True) + EPS)
    norm_one = inputs * rms_one
    act_one = (norm_one * gain_one).astype(jnp.bfloat16)
    query_pre = matmul(act_one, full_query)
    heads = query_pre.shape[1] // HD
    kv_pre = matmul(act_one, full_kv)
    queries = (
        rotate(query_pre.reshape(rows, heads, HD), own_cos[:, None, :], own_sin[:, None, :])
        * scale_factor
    ).astype(jnp.bfloat16)
    own_kv = jnp.concatenate(
        [rotate(kv_pre[:, :HD], own_cos, own_sin), kv_pre[:, HD:]], axis=1
    ).astype(jnp.bfloat16)
    all_kv = lax.all_gather(own_kv, "seq", axis=0, tiled=True)
    keys = all_kv[:, :HD]
    values_all = all_kv[:, HD:]
    scores = jnp.einsum("rhd,kd->hrk", queries, keys, preferred_element_type=jnp.float32)
    scores = jnp.where(allowed[None], scores, NEG)
    top_score = jnp.max(scores, axis=-1, keepdims=True)
    expd = jnp.exp(scores - top_score)
    total = jnp.sum(expd, axis=-1, keepdims=True)
    log_total = top_score + jnp.log(total)
    probs_low = (expd / total).astype(jnp.bfloat16)
    mixed = (
        jnp.einsum("hrk,kd->rhd", probs_low, values_all, preferred_element_type=jnp.float32)
        .reshape(rows, heads * HD)
        .astype(jnp.bfloat16)
    )
    attn = lax.psum(matmul(mixed, full_out), "tensor")
    resid = inputs + attn
    full_gate, full_up, full_down, full_gain_two = (
        lax.all_gather(w_gate, ("dp", "seq"), axis=0, tiled=True),
        lax.all_gather(w_up, ("dp", "seq"), axis=0, tiled=True),
        lax.all_gather(w_down, ("dp", "seq"), axis=1, tiled=True),
        lax.all_gather(gain_ffn, ("dp", "seq"), axis=0, tiled=True),
    )
    gain_two = full_gain_two.astype(jnp.float32)
    rms_two = lax.rsqrt(jnp.mean(resid * resid, axis=-1, keepdims=True) + EPS)
    norm_two = resid * rms_two
    act_two = (norm_two * gain_two).astype(jnp.bfloat16)
    gate = matmul(act_two, full_gate)
    up_val = matmul(act_two, full_up)
    gelu_val, gelu_pull = jax.vjp(gelu_tanh, gate)
    hidden = (gelu_val * up_val).astype(jnp.bfloat16)
    ffn = lax.psum(matmul(hidden, full_down).astype(jnp.bfloat16), "tensor").astype(jnp.float32)
    out = (resid + ffn).astype(jnp.bfloat16)
    back_gate, back_up, back_down = (
        lax.all_gather(w_gate, ("dp", "seq"), axis=0, tiled=True),
        lax.all_gather(w_up, ("dp", "seq"), axis=0, tiled=True),
        lax.all_gather(w_down, ("dp", "seq"), axis=1, tiled=True),
    )
    d_hidden = matmul_nt(d_out, back_down)
    grad_down = matmul_tn(hidden, d_out)
    d_gate = gelu_pull(d_hidden * up_val)[0].astype(jnp.bfloat16)
    d_up = (d_hidden * gelu_val).astype(jnp.bfloat16)
    grad_gate = matmul_tn(act_two, d_gate)
    grad_up = matmul_tn(act_two, d_up)
    d_act_two = lax.psum(matmul_nt(d_gate, back_gate) + matmul_nt(d_up, back_up), "tensor")
    grad_gain_two = jnp.sum(d_act_two * norm_two, axis=0)
    d_resid = d_out.astype(jnp.float32) + norm_back(d_act_two, norm_two, rms_two, gain_two)
    ffn_grads = (
        lax.psum_scatter(
            grad_gate.astype(jnp.bfloat16), ("dp", "seq"), scatter_dimension=0, tiled=True
        ).astype(jnp.float32),
        lax.psum_scatter(
            grad_up.astype(jnp.bfloat16), ("dp", "seq"), scatter_dimension=0, tiled=True
        ).astype(jnp.float32),
        lax.psum_scatter(
            grad_down.astype(jnp.bfloat16), ("dp", "seq"), scatter_dimension=1, tiled=True
        ).astype(jnp.float32),
        lax.psum_scatter(
            grad_gain_two.astype(jnp.bfloat16), ("dp", "seq"), scatter_dimension=0, tiled=True
        ).astype(jnp.float32),
    )
    back_query, back_out, back_kv = (
        lax.all_gather(w_query, ("dp", "seq"), axis=0, tiled=True),
        lax.all_gather(w_out, ("dp", "seq"), axis=1, tiled=True),
        lax.all_gather(kv_weight, ("dp", "seq"), axis=0, tiled=True),
    )
    d_attn = d_resid.astype(jnp.bfloat16)
    grad_out = matmul_tn(mixed, d_attn)
    d_mixed = matmul_nt(d_attn, back_out).astype(jnp.bfloat16).reshape(rows, heads, HD)
    scores_again = jnp.einsum("rhd,kd->hrk", queries, keys, preferred_element_type=jnp.float32)
    probs = jnp.where(allowed[None], jnp.exp(scores_again - log_total), 0.0)
    d_probs = jnp.einsum("rhd,kd->hrk", d_mixed, values_all, preferred_element_type=jnp.float32)
    delta = jnp.sum(probs * d_probs, axis=-1, keepdims=True)
    d_scores = (probs * (d_probs - delta)).astype(jnp.bfloat16)
    d_queries = (
        jnp.einsum("hrk,kd->rhd", d_scores, keys, preferred_element_type=jnp.float32) * scale_factor
    )
    d_query_pre = (
        rotate_back(d_queries, own_cos[:, None, :], own_sin[:, None, :])
        .reshape(rows, heads * HD)
        .astype(jnp.bfloat16)
    )
    d_keys_part = jnp.einsum("hrk,rhd->kd", d_scores, queries, preferred_element_type=jnp.float32)
    d_values_part = jnp.einsum(
        "hrk,rhd->kd", probs.astype(jnp.bfloat16), d_mixed, preferred_element_type=jnp.float32
    )
    own_kv_grad = lax.psum_scatter(
        jnp.concatenate([d_keys_part, d_values_part], axis=1).astype(jnp.bfloat16),
        "seq",
        scatter_dimension=0,
        tiled=True,
    )
    d_act_query = matmul_nt(d_query_pre, back_query)
    d_act_sum, kv_grad = (
        lax.psum(d_act_query.astype(jnp.bfloat16), "tensor").astype(jnp.float32),
        lax.psum(own_kv_grad, "tensor").astype(jnp.float32),
    )
    d_kv_pre = jnp.concatenate(
        [rotate_back(kv_grad[:, :HD], own_cos, own_sin), kv_grad[:, HD:]], axis=1
    ).astype(jnp.bfloat16)
    d_act_one = d_act_sum + matmul_nt(d_kv_pre, back_kv)
    grad_query = matmul_tn(act_one, d_query_pre)
    grad_kv = matmul_tn(act_one, d_kv_pre)
    grad_gain_one = jnp.sum(d_act_one * norm_one, axis=0)
    d_tokens = d_resid + norm_back(d_act_one, norm_one, rms_one, gain_one)
    attn_grads = (
        lax.psum_scatter(
            grad_query.astype(jnp.bfloat16), ("dp", "seq"), scatter_dimension=0, tiled=True
        ).astype(jnp.float32),
        lax.psum_scatter(
            grad_out.astype(jnp.bfloat16), ("dp", "seq"), scatter_dimension=1, tiled=True
        ).astype(jnp.float32),
        lax.psum_scatter(
            grad_kv.astype(jnp.bfloat16), ("dp", "seq"), scatter_dimension=0, tiled=True
        ).astype(jnp.float32),
        lax.psum_scatter(
            grad_gain_one.astype(jnp.bfloat16), ("dp", "seq"), scatter_dimension=0, tiled=True
        ).astype(jnp.float32),
    )
    return (
        out,
        d_tokens,
        attn_grads[3],
        attn_grads[0],
        attn_grads[2],
        attn_grads[1],
        ffn_grads[3],
        ffn_grads[0],
        ffn_grads[1],
        ffn_grads[2],
    )


MESH = pl.DeviceIdType.MESH
VMEM_LIMIT = 66000 * 1024


class Place:
    def __init__(self):
        self.dp = lax.axis_index("dp")
        self.seq = lax.axis_index("seq")
        self.z = lax.axis_index("tensor")
        self.core = lax.rem(self.dp, 2)
        self.chip = lax.div(self.dp, 2)

    def device(self, across, other):
        chip = (self.chip + across) % 2
        seq = (self.seq + across // 2) % 2
        core = (self.core + other) % 2
        return chip * 2 + core, seq, self.z

    def shard(self, across, other):
        dp, seq, _ = self.device(across, other)
        return dp * 2 + seq


def greet(here, peers, line=False):
    barrier = pltpu.get_barrier_semaphore()
    peers = list(peers)
    if line:
        peers += [(here.dp, here.seq, (here.z + step) % 4) for step in range(1, 4)]
    for peer in peers:
        pl.semaphore_signal(barrier, inc=1, device_id=peer, device_id_type=MESH)
    pl.semaphore_wait(barrier, len(peers))


def remote(src, dst, send, recv, peer):
    return pltpu.make_async_remote_copy(
        src_ref=src, dst_ref=dst, send_sem=send, recv_sem=recv, device_id=peer, device_id_type=MESH
    )


class Line:
    def __init__(self, here, counts, refs, place=None):
        self.own, self.out, self.from_end, self.from_mid = refs[:4]
        self.sems = refs[4:10]
        self.counts = counts
        self.chunk = self.from_mid.shape[1]
        self.fold = self.from_end.shape[1] // self.chunk
        self.place = place
        z = here.z
        self.inner = ((z + 1) // 2) % 2
        self.mate = (here.dp, here.seq, z + 1 - 2 * (z % 2))
        self.other = (here.dp, here.seq, 3 - z)

    def rows(self, at):
        at = at if self.place is None else self.place(at)
        return pl.ds(pl.multiple_of(at * self.chunk, self.chunk), self.chunk)

    def inbox(self, at):
        span = pl.ds(pl.multiple_of(at % self.fold * self.chunk, self.chunk), self.chunk)
        return self.from_end.at[at // self.fold, span, :]

    def up(self, at):
        return remote(self.own.at[self.rows(at), :], self.inbox(at), self.sems[0].at[at],
                      self.sems[1].at[at], self.mate)

    def over(self, at):
        return remote(self.out.at[self.rows(at), :], self.from_mid.at[at], self.sems[2].at[at],
                      self.sems[3].at[at], self.other)

    def down(self, at):
        rows = self.rows(at)
        return remote(self.out.at[rows, :], self.out.at[rows, :], self.sems[4].at[at],
                      self.sems[5].at[at], self.mate)

    def launch(self, first, count):
        @pl.when(self.inner == 0)
        def _():
            def send(at, _):
                self.up(first + at).start()
                return 0

            lax.fori_loop(0, count, send, 0)

    def begin(self):
        self.launch(0, self.counts)

    def first(self, at):
        rows = self.rows(at)
        self.up(at).wait_recv()
        total = self.own[rows, :].astype(jnp.float32) + self.inbox(at)[...].astype(jnp.float32)
        self.out[rows, :] = total.astype(self.out.dtype)
        self.over(at).start()

    def second(self, at):
        rows = self.rows(at)
        self.over(at).wait()
        total = self.out[rows, :].astype(jnp.float32) + self.from_mid[at].astype(jnp.float32)
        self.out[rows, :] = total.astype(self.out.dtype)
        self.down(at).start()

    def step(self, at, start=0, count=None):
        count = self.counts if count is None else count

        @pl.when(jnp.logical_and(self.inner == 1, at < count))
        def _():
            self.first(start + at)

        @pl.when(jnp.logical_and(self.inner == 1, jnp.logical_and(at > 1, at < count + 2)))
        def _():
            self.second(start + at - 2)

    def steps(self, first, last, start=0, count=None):
        def rest(at, _):
            self.step(at, start, count)
            return 0

        lax.fori_loop(first, last, rest, 0)

    def settle(self):
        @pl.when(self.inner == 0)
        def _():
            def take(at, _):
                self.up(at).wait_send()
                self.down(at).wait_recv()
                return 0

            lax.fori_loop(0, self.counts, take, 0)

        self.drain()

    def drain(self):
        @pl.when(self.inner == 1)
        def _():
            def drain(at, _):
                self.down(at).wait_send()
                return 0

            lax.fori_loop(0, self.counts, drain, 0)

    def end(self, done=0):
        self.steps(min(done, self.counts + 2), self.counts + 2)
        self.settle()


def line_scratch(counts, shape, low, fold=1):
    chunk = shape[0] // counts
    inbox = pltpu.VMEM((counts // fold, chunk * fold, shape[1]), low)
    return [inbox, pltpu.VMEM((counts, chunk, shape[1]), low)] + [pltpu.SemaphoreType.DMA((counts,))] * 6


def turned(at):
    return 3 - at // 2, 1 - at % 2


def slice_peers(here):
    return [here.device(*turned(at)) for at in range(7)]


def kernel_call(kernel, out_shape, operands, specs, scratch, cid, name, out_specs=None, late=(), early=()):
    vm = pl.BlockSpec(memory_space=pltpu.VMEM)
    hbm = pl.BlockSpec(memory_space=pl.ANY)
    specs = [hbm if at in late else spec for at, spec in enumerate(specs)]
    out_specs = [hbm if at in early else spec for at, spec in enumerate(out_specs or [vm] * len(out_shape))]
    inside = [pltpu.VMEM(operands[at].shape, operands[at].dtype) for at in late]
    inside += [pltpu.VMEM(out_shape[at].shape, out_shape[at].dtype) for at in early]
    inside.append(pltpu.SemaphoreType.DMA((max(1, len(late) + len(early)),)))
    n_in, n_out = len(operands), len(out_shape)

    def body(*refs):
        ins, outs = list(refs[:n_in]), list(refs[n_in : n_in + n_out])
        rest, own = refs[n_in + n_out : -len(inside)], refs[-len(inside) :]
        loads, stores = [], []
        for spot, at in enumerate(late):
            copy = pltpu.make_async_copy(ins[at], own[spot], own[-1].at[spot])
            copy.start()
            loads.append(copy)
            ins[at] = own[spot]
        for number, at in enumerate(early):
            spot = len(late) + number
            stores.append(pltpu.make_async_copy(own[spot], outs[at], own[-1].at[spot]))
            outs[at] = own[spot]
        more = {}
        if late:
            more["late"] = loads
        if early:
            more["early"] = stores
        kernel(*ins, *outs, *rest, **more)
        for copy in stores:
            copy.wait()

    return pl.pallas_call(
        body,
        out_shape=out_shape,
        in_specs=specs,
        out_specs=out_specs,
        scratch_shapes=scratch + inside,
        compiler_params=pltpu.CompilerParams(
            collective_id=cid, has_side_effects=True, vmem_limit_bytes=VMEM_LIMIT
        ),
        name=f"{name}_{cid}",
    )(*operands)


class Tiny:
    def __init__(self, here, src, dst, sems, spread):
        self.here, self.src, self.dst, self.sems, self.spread = here, src, dst, sems, spread
        self.peers = slice_peers(here)
        self.me = here.shard(0, 0)

    def tile(self, shard):
        return self.src.at[shard] if self.spread else self.src

    def copy(self, at):
        return remote(self.tile(self.here.shard(*turned(at))), self.dst.at[self.me], self.sems[0].at[at],
                      self.sems[1].at[at], self.peers[at])

    def begin(self):
        for at in range(7):
            self.copy(at).start()
        self.dst[self.me] = self.tile(self.me)[...]

    def end(self):
        for at in range(7):
            self.copy(at).wait()


class Reduce:
    def __init__(self, here, counts, product, refs, before=None):
        self.counts, self.product, self.before = counts, product, before
        self.held, self.sib_out, self.sib_in, self.from_x, self.from_y = refs[:5]
        self.sib_sems, self.x_sems, self.y_sems = refs[5:7], refs[7:9], refs[9:11]
        self.sib, self.xdev, self.ydev = here.device(0, 1), here.device(1, 0), here.device(2, 0)
        self.steps = 4 * counts
        self.ring = self.sib_out.shape[0]

    def streams(self, stage):
        far = stage // 3
        x_chip = jnp.where(stage == 0, 3, jnp.where(stage == 2, 0, 1))
        y_chip = jnp.where(stage == 0, 3, jnp.where(stage == 2, 0, 2))
        return (x_chip, far), (y_chip, 1 - far)

    def to_sib(self, step, stream):
        stage, at = step // self.counts, step % self.counts
        return remote(self.sib_out.at[step % self.ring, stream], self.sib_in.at[stage, stream, at],
                      self.sib_sems[0].at[stage, stream, at], self.sib_sems[1].at[stage, stream, at], self.sib)

    def to_x(self, hop, at, stage=0):
        return remote(self.held.at[stage, 0, at], self.from_x.at[hop, at], self.x_sems[0].at[hop, at],
                      self.x_sems[1].at[hop, at], self.xdev)

    def to_y(self, hop, at, stage=0):
        return remote(self.held.at[stage, 1, at], self.from_y.at[hop, at], self.y_sems[0].at[hop, at],
                      self.y_sems[1].at[hop, at], self.ydev)

    def compute(self, step):
        stage, at = step // self.counts, step % self.counts
        if self.before:
            for stop in range(3):
                @pl.when(step == stop * self.counts)
                def _():
                    self.before(stop)

        @pl.when(step >= self.ring)
        def _():
            for stream in range(2):
                self.to_sib(step - self.ring, stream).wait_send()

        for stream, (across, half) in enumerate(self.streams(stage)):
            self.sib_out[step % self.ring, stream] = self.product(across, 1, half, at).astype(jnp.bfloat16)
            self.held[stage, stream, at] = self.product(across, 0, half, at).astype(jnp.bfloat16)
        for stream in range(2):
            self.to_sib(step, stream).start()

    def finish(self, step):
        stage, at = step // self.counts, step % self.counts
        for stream in range(2):
            self.to_sib(step, stream).wait_recv()

        def total(stream):
            return self.held[stage, stream, at].astype(jnp.float32) + self.sib_in[stage, stream, at].astype(
                jnp.float32)

        @pl.when(stage < 3)
        def _():
            for stream in range(2):
                self.held[stage, stream, at] = total(stream).astype(jnp.bfloat16)

        @pl.when(stage == 3)
        def _():
            self.to_y(0, at).wait_recv()
            self.held[3, 0, at] = (total(0) + self.from_y[0, at].astype(jnp.float32)).astype(jnp.bfloat16)
            self.to_x(0, at).wait_recv()
            self.held[3, 1, at] = (total(1) + self.from_x[0, at].astype(jnp.float32)).astype(jnp.bfloat16)

        @pl.when(stage != 2)
        def _():
            hop = stage - stage // 3
            self.to_x(hop, at, stage).start()
            self.to_y(hop, at, stage).start()

    def advance(self, step):
        @pl.when(step < self.steps)
        def _():
            self.compute(step)

        @pl.when(jnp.logical_and(step > 0, step <= self.steps))
        def _():
            self.finish(step - 1)

    def run(self, hook=None):
        def body(step, _):
            self.advance(step)

            if hook:
                hook(step)
            return 0

        lax.fori_loop(0, self.steps + 1, body, 0)
        return self.steps + 1

    def end(self, emit):
        def last(at, _):
            values = []
            for half in range(2):
                xs, ys = (1, 2) if half == 0 else (2, 1)
                self.to_x(xs, at).wait_recv()
                self.to_y(ys, at).wait_recv()
                values.append(self.held[2, half, at].astype(jnp.float32) + self.from_x[xs, at].astype(jnp.float32)
                              + self.from_y[ys, at].astype(jnp.float32))
            emit(at, *values)
            for hop in range(3):
                self.to_x(hop, at).wait_send()
                self.to_y(hop, at).wait_send()
            return 0

        lax.fori_loop(0, self.counts, last, 0)

        def drain(at, _):
            for stream in range(2):
                self.to_sib(self.steps - self.ring + at, stream).wait_send()
            return 0

        lax.fori_loop(0, self.ring, drain, 0)


def reduce_scratch(counts, rows, width, ring=4):
    low, dma = jnp.bfloat16, pltpu.SemaphoreType.DMA
    block = pltpu.VMEM((4, 2, counts, rows, width), low)
    landed = pltpu.VMEM((3, counts, rows, width), low)
    sent = pltpu.VMEM((ring, 2, rows, width), low)
    return [block, sent, block, landed, landed] + [dma((4, 2, counts))] * 2 + [dma((3, counts))] * 4


class Spread:
    def __init__(self, here, counts, refs):
        self.counts = counts
        self.got = refs[0]
        self.x_sems, self.y_sems, self.sib_sems = refs[1:3], refs[3:5], refs[5:7]
        self.core = here.core
        self.sib, self.xdev, self.ydev = here.device(0, 1), here.device(1, 0), here.device(2, 0)

    def slot(self, across, half, at):
        return self.got.at[across, self.core, half, at]

    def x_copy(self, hop, at):
        half = jnp.minimum(hop, 1)
        src = self.slot(2 * (hop // 2), half, at)
        dst = self.slot(1 + 2 * (hop // 2), half, at)
        return remote(src, dst, self.x_sems[0].at[hop, at], self.x_sems[1].at[hop, at], self.xdev)

    def y_copy(self, hop, at):
        half = 1 - jnp.minimum(hop, 1)
        src = self.slot(hop // 2, half, at)
        dst = self.slot(2 + hop // 2, half, at)
        return remote(src, dst, self.y_sems[0].at[hop, at], self.y_sems[1].at[hop, at], self.ydev)

    def streams(self, stage):
        some, last, late = jnp.minimum(stage, 1), stage // 3, stage // 2
        return (some + 2 * last, late), (2 * some + last, 1 - late)

    def block(self, at):
        x_stream, y_stream = self.streams(at // 4)
        second = at // 2 % 2
        across = x_stream[0] + second * (y_stream[0] - x_stream[0])
        half = x_stream[1] + second * (y_stream[1] - x_stream[1])
        return across, at % 2, half

    def begin_rows(self):
        for hop in range(2):
            self.x_copy(hop, 0).start()
            self.y_copy(hop, 0).start()
        for stream in range(2):
            self.sib_copy(0, stream, 0).start()

    def receive_rows(self, step):
        stage = step // 4

        @pl.when(jnp.logical_and(step % 4 == 0, jnp.logical_and(stage > 0, stage < 4)))
        def _():
            self.x_copy(stage - 1, 0).wait_recv()
            self.sib_copy(stage, 0, 0).start()
            self.y_copy(stage - 1, 0).wait_recv()
            self.sib_copy(stage, 1, 0).start()

        @pl.when(step == 4)
        def _():
            self.x_copy(2, 0).start()
            self.y_copy(2, 0).start()

        for stream in range(2):
            @pl.when(jnp.logical_and(step % 4 == 2 * stream, step < 16))
            def _(stream=stream):
                self.sib_copy(stage, stream, 0).wait_recv()

    def sib_copy(self, stage, stream, at):
        across, half = self.streams(stage)[stream]
        slot = self.slot(across, half, at)
        spot = (stage, stream, at)
        return remote(slot, slot, self.sib_sems[0].at[spot], self.sib_sems[1].at[spot], self.sib)

    def begin(self):
        def first(at, _):
            self.x_copy(0, at).start()
            self.y_copy(0, at).start()
            return 0

        def own(at, _):
            self.sib_copy(0, 0, at).start()
            self.sib_copy(0, 1, at).start()
            return 0

        lax.fori_loop(0, self.counts, first, 0)
        lax.fori_loop(0, self.counts, own, 0)

    def run(self, blocks, hook=None, done=None):
        counts = self.counts

        def body(step, _):
            stage, at = step // counts, step % counts

            @pl.when(jnp.logical_and(stage > 0, stage < 4))
            def _():
                self.x_copy(stage - 1, at).wait_recv()
                self.sib_copy(stage, 0, at).start()
                self.y_copy(stage - 1, at).wait_recv()
                self.sib_copy(stage, 1, at).start()

            @pl.when(jnp.logical_and(stage > 0, stage < 3))
            def _():
                self.x_copy(stage, at).start()
                self.y_copy(stage, at).start()

            @pl.when(step > 0)
            def _():
                old, spot = (step - 1) // counts, (step - 1) % counts
                for stream, (across, half) in enumerate(self.streams(old)):
                    self.sib_copy(old, stream, spot).wait_recv()
                    blocks(across, half, spot)
                if done:
                    done(old, spot)

            if hook:
                hook(step)
            return 0

        lax.fori_loop(0, 4 * counts + 1, body, 0)
        return 4 * counts + 1

    def end(self):
        def drain(at, _):
            for hop in range(3):
                self.x_copy(hop, at).wait_send()
                self.y_copy(hop, at).wait_send()
            for stage in range(4):
                self.sib_copy(stage, 0, at).wait_send()
                self.sib_copy(stage, 1, at).wait_send()
            return 0

        lax.fori_loop(0, self.counts, drain, 0)


def spread_scratch(counts, rows, width):
    dma = pltpu.SemaphoreType.DMA
    return [pltpu.VMEM((4, 2, 2, counts, rows, width), jnp.bfloat16)] + [dma((3, counts))] * 4 + [
        dma((4, 2, counts))] * 2


def row_span(here, across, other, rows):
    return pl.ds(pl.multiple_of(here.shard(across, other) * rows, rows), rows)


def dot_nt(left, right):
    return lax.dot_general(left, right, (((1,), (1,)), ((), ())), preferred_element_type=jnp.float32)


def dot_tn(left, right):
    return lax.dot_general(left, right, (((0,), (0,)), ((), ())), preferred_element_type=jnp.float32)


def dot_nn(left, right):
    return jnp.dot(left, right, preferred_element_type=jnp.float32)


def products(here, act, weight, nt, rows, width, counts):
    def product(across, other, half, at):
        cols = pl.ds(pl.multiple_of((half * counts + at) * width, width), width)
        block = act[row_span(here, across, other, rows), :]
        return dot_nt(block, weight[cols, :]) if nt else dot_nn(block, weight[:, cols])

    return product


def diagonal():
    return (lax.broadcasted_iota(jnp.int32, (LANES, LANES), 0) ==
            lax.broadcasted_iota(jnp.int32, (LANES, LANES), 1)).astype(jnp.float32)


def to_tile(tile, first, column, eye):
    for at in range(column.shape[0] // LANES):
        spread = column[at * LANES : (at + 1) * LANES, :] * eye
        tile[first + at : first + at + 1, :] = jnp.sum(spread, axis=0, keepdims=True)


def from_tile(row, eye):
    return jnp.sum(eye * row, axis=1, keepdims=True)


def make_tables(here, rows, segs, cos, sin, mask):
    eye = diagonal()
    tiles = rows // LANES
    freqs = jnp.exp(lax.broadcasted_iota(jnp.int32, (1, LANES), 1).astype(jnp.float32) * (-math.log(10000.0) / LANES))
    lane = lax.broadcasted_iota(jnp.int32, (1, LANES), 1)
    line = lax.broadcasted_iota(jnp.int32, (LANES, 1), 0)

    def ids_of(row):
        return segs[2:3, pl.ds(pl.multiple_of(row * LANES, LANES), LANES)]

    def row_of(side, at):
        return ((here.seq + side) % 2) * tiles + at

    for side in range(2):
        for at in range(tiles):
            row = row_of(side, at)
            ids = from_tile(ids_of(row), eye)
            before = jnp.zeros((LANES, 1), jnp.float32)
            for other in range(2 * tiles):
                smaller = ids_of(other) < ids
                before += jnp.sum(smaller.astype(jnp.float32), axis=-1, keepdims=True)
            index = row * LANES + line
            angles = (index.astype(jnp.float32) - before) * freqs
            span = slice(at * LANES, (at + 1) * LANES)
            cos[side, span, :] = jnp.cos(angles)
            sin[side, span, :] = jnp.sin(angles)
            if side == 0:
                for key_side in range(2):
                    for key_at in range(tiles):
                        key_row = row_of(key_side, key_at)
                        same = ids_of(key_row) == ids
                        allowed = jnp.logical_and(same, key_row * LANES + lane <= index)
                        first = key_side * rows + key_at * LANES
                        mask[span, first : first + LANES] = allowed.astype(jnp.float32)


def open_kernel(rows, width, counts, tokens, gain_one, gain_two, ids, w_query, kv_weight, cot, qkv, x_low, act_t, w_qkv, rms, cos, sin,
                mask, g_col, gain, *refs, early):
    here = Place()
    gain[...] = jnp.zeros_like(gain)
    gain[0:1, :] = gain_one[...].astype(jnp.float32).reshape(1, -1)
    gain[1:2, :] = gain_two[...].astype(jnp.float32).reshape(1, -1)
    gain[2:3, :] = ids[...].astype(jnp.float32).reshape(1, -1)
    early[7].start()
    cols, segs = gain.shape[1], gain
    act, turn_send, turn_recv, local_sems, cot_part, g_send, g_recv, z_send, z_recv = refs[:9]
    share = rows // 4
    me = here.shard(0, 0)
    own_rows = pl.ds(pl.multiple_of(me * rows, rows), rows)

    def turn_copy(at):
        across, other = turned(at)
        first = pl.multiple_of(here.shard(across, other) * cols, cols)
        return remote(tokens.at[:, pl.ds(first, cols)], x_low.at[own_rows, :], turn_send.at[at], turn_recv.at[at],
                      here.device(across, other))

    wide = w_query.shape[1]
    local = [
        pltpu.make_async_copy(w_query, w_qkv.at[:, :wide], local_sems.at[0]),
        pltpu.make_async_copy(kv_weight, w_qkv.at[:, wide:], local_sems.at[1]),
        pltpu.make_async_copy(tokens.at[:, pl.ds(pl.multiple_of(me * cols, cols), cols)], x_low.at[own_rows, :],
                              local_sems.at[2]),
    ]
    load = pltpu.make_async_copy(cot.at[pl.ds(pl.multiple_of(here.z * share, share), share), :], cot_part,
                                 local_sems.at[3])
    load.start()
    for copy in local:
        copy.start()

    def g_copy(at):
        across, other = turned(at)
        first = pl.multiple_of(here.shard(across, other) * cols, cols)
        return remote(cot_part.at[:, pl.ds(first, cols)], g_col.at[me, here.z], g_send.at[at], g_recv.at[at],
                      here.device(across, other))

    def own_part():
        return pltpu.make_async_copy(cot_part.at[:, pl.ds(pl.multiple_of(me * cols, cols), cols)],
                                     g_col.at[me, here.z], local_sems.at[4])

    def quarter(way, at, step, peer):
        spot = g_col.at[:, at]
        return remote(spot, spot, z_send.at[way, step], z_recv.at[way, step], (here.dp, here.seq, here.z + peer))

    def pass_on(step):
        @pl.when(jnp.logical_and(here.z < 3, here.z >= step))
        def _():
            quarter(0, here.z - step, step, 1).start()

        @pl.when(jnp.logical_and(here.z > 0, here.z <= 3 - step))
        def _():
            quarter(1, here.z + step, step, -1).start()

    def take_quarters(step):
        @pl.when(here.z > step)
        def _():
            quarter(0, here.z - 1 - step, step, -1).wait_recv()

        @pl.when(here.z < 3 - step)
        def _():
            quarter(1, here.z + 1 + step, step, 1).wait_recv()

    greet(here, slice_peers(here), True)
    load.wait()
    own_part().start()
    for at in range(7):
        g_copy(at).start()
    for at in range(7):
        turn_copy(at).start()
    for copy in local:
        copy.wait()
    early[2].start()

    def squares(at, total):
        values = tokens[:, pl.ds(pl.multiple_of(at * cols, cols), cols)].astype(jnp.float32)
        return total + jnp.sum(values * values, axis=-1, keepdims=True)

    total = lax.fori_loop(0, 8, squares, jnp.zeros((rows, 1), jnp.float32))
    rms[...] = jnp.broadcast_to(lax.rsqrt(total / (8 * cols) + EPS), rms.shape)
    make_tables(here, rows, segs, cos, sin, mask)
    for at in (3, 4, 5):
        early[at].start()

    def prepare(first, count):
        def one(step, _):
            at = first + step
            span = row_span(here, *turned(at), rows)
            value = (x_low[span, :].astype(jnp.float32) * gain[0:1, :]).astype(act.dtype)
            act[span, :] = value
            return 0

        lax.fori_loop(0, count, one, 0)

    def before(stop):
        first, count = ((0, 2), (2, 4), (6, 2))[stop]
        if stop == 0:
            own_part().wait()
            for at in range(7):
                g_copy(at).wait_recv()
        else:
            take_quarters(stop - 1)
        pass_on(stop)
        for at in range(first, min(first + count, 7)):
            turn_copy(at).wait_recv()
        prepare(first, count)
        if stop == 2:
            early[0].start()

    def flip():
        def one(shard, _):
            span = pl.ds(pl.multiple_of(shard * rows, rows), rows)
            act_t[:, span] = act[span, :].T
            return 0

        lax.fori_loop(0, 8, one, 0)

    product = products(here, act, w_qkv, False, rows, width, counts)
    total = Reduce(here, counts, product, refs[9:20], before)
    total.run()
    flip()
    early[1].start()

    def emit(at, first, second):
        for half, value in enumerate((first, second)):
            qkv[:, pl.ds(pl.multiple_of((half * counts + at) * width, width), width)] = value

    total.end(emit)
    take_quarters(2)
    early[6].start()
    for at in range(7):
        turn_copy(at).wait_send()
        g_copy(at).wait_send()
    for step in range(3):
        @pl.when(jnp.logical_and(here.z < 3, here.z >= step))
        def _(step=step):
            quarter(0, here.z - step, step, 1).wait_send()

        @pl.when(jnp.logical_and(here.z > 0, here.z <= 3 - step))
        def _(step=step):
            quarter(1, here.z + step, step, -1).wait_send()


def opening(tokens, gain_one, gain_two, ids, w_query, kv_weight, cot, cid, width=256):
    rows = tokens.shape[0]
    cols, wide = w_query.shape
    every = wide + kv_weight.shape[1]
    counts = every // (2 * width)
    low, f32 = jnp.bfloat16, jnp.float32
    dma = pltpu.SemaphoreType.DMA
    vm = pl.BlockSpec(memory_space=pltpu.VMEM)
    hbm = pl.BlockSpec(memory_space=pl.ANY)
    out_shape = [
        jax.ShapeDtypeStruct((rows, every), f32),
        jax.ShapeDtypeStruct((8 * rows, cols), low),
        jax.ShapeDtypeStruct((cols, 8 * rows), low),
        jax.ShapeDtypeStruct((cols, every), low),
        jax.ShapeDtypeStruct((rows, LANES), f32),
        jax.ShapeDtypeStruct((2, rows, LANES), f32),
        jax.ShapeDtypeStruct((2, rows, LANES), f32),
        jax.ShapeDtypeStruct((rows, 2 * rows), f32),
        jax.ShapeDtypeStruct((8, 4, rows // 4, cols), low),
        jax.ShapeDtypeStruct((8, cols), f32),
    ]
    scratch = [
        pltpu.VMEM((8 * rows, cols), low), dma((7,)), dma((7,)), dma((5,)),
        pltpu.VMEM((rows // 4, 8 * cols), low), dma((7,)), dma((7,)), dma((2, 3)), dma((2, 3)),
    ]
    scratch += reduce_scratch(counts, rows, width)
    kernel = functools.partial(open_kernel, rows, width, counts)
    return kernel_call(kernel, out_shape, [tokens, gain_one, gain_two, ids, w_query, kv_weight, cot],
                       [vm, vm, vm, vm, hbm, hbm, hbm], scratch, cid, "open",
                       early=(1, 2, 3, 5, 6, 7, 8, 9))


def ffn_kernel(rows, width, counts, x_low, attn, gain, w_gate, w_up, d_hidden, hidden, d_gate, d_up, act_t, tile_out,
               *refs, late, early):
    here = Place()
    cols = gain.shape[1]
    act, weight, tiny_own, tiny_all, tiny_send, tiny_recv, dots, local_sems = refs[:8]
    tiny = Tiny(here, tiny_own, tiny_all, (tiny_send, tiny_recv), True)
    half_cols = counts * width
    local = [
        pltpu.make_async_copy(w_gate, weight.at[:, :half_cols], local_sems.at[0]),
        pltpu.make_async_copy(w_up, weight.at[:, half_cols:], local_sems.at[1]),
    ]
    for copy in local:
        copy.start()
    eye = diagonal()
    tiny_own[...] = jnp.zeros_like(tiny_own)

    def prepare(number, _):
        shard = here.shard(*turned(number))
        for at in range(rows // LANES):
            span = pl.ds(pl.multiple_of(shard * rows + at * LANES, LANES), LANES)
            resid = x_low[span, :].astype(jnp.float32) + attn[span, :].astype(jnp.float32)
            act[span, :] = (resid * gain[1:2, :]).astype(act.dtype)
            square = jnp.sum(resid * resid, axis=-1, keepdims=True)
            tiny_own[shard, at : at + 1, :] = jnp.sum(square * eye, axis=0, keepdims=True)
        return 0

    def before(stop):
        if stop == 1:
            lax.fori_loop(2, 6, prepare, 0)
        if stop == 2:
            lax.fori_loop(6, 8, prepare, 0)
            tiny.begin()

    lax.fori_loop(0, 2, prepare, 0)
    greet(here, slice_peers(here))
    for copy in local:
        copy.wait()
    product = products(here, act, weight, False, rows, width, counts)
    total = Reduce(here, counts, product, refs[8:19], before)
    total.run()

    def flip(shard, _):
        span = pl.ds(pl.multiple_of(shard * rows, rows), rows)
        act_t[:, span] = act[span, :].T
        return 0

    lax.fori_loop(0, 8, flip, 0)
    early[0].start()
    tiny.end()
    tiles = rows // LANES
    mean = [from_tile(jnp.sum(tiny_all[:, at, :], axis=0, keepdims=True), eye) for at in range(tiles)]
    scale = lax.rsqrt(jnp.concatenate(mean, axis=0) / (8 * cols) + EPS)
    dots[...] = jnp.zeros_like(dots)
    late[0].wait()
    coeff = math.sqrt(2.0 / math.pi)

    def emit(at, first, second):
        span = pl.ds(pl.multiple_of(at * width, width), width)
        gate, up = first * scale, second * scale
        inner = jnp.tanh(coeff * (gate + 0.044715 * (gate * gate * gate)))
        gelu = 0.5 * gate * (1.0 + inner)
        slope = 0.5 * (1.0 + inner) + 0.5 * gate * (1.0 - inner * inner) * (
            coeff * (1.0 + 3.0 * 0.044715 * gate * gate))
        cot = d_hidden[:, span]
        hidden[:, span] = (gelu * up).astype(hidden.dtype)
        back_gate, back_up = cot * up * slope, cot * gelu
        d_gate[:, span] = (back_gate * scale).astype(d_gate.dtype)
        d_up[:, span] = (back_up * scale).astype(d_up.dtype)
        dots[...] += jnp.sum(back_gate * gate + back_up * up, axis=-1, keepdims=True)

    total.end(emit)
    tile_out[...] = jnp.zeros_like(tile_out)
    to_tile(tile_out, 0, dots[...] * (scale * scale * (1.0 / (8 * cols))), eye)


def ffn_scatter(x_low, attn, gain, w_gate, w_up, d_hidden, cid, width=512):
    rows, half = d_hidden.shape
    cols = gain.shape[1]
    counts = half // width
    low, f32 = jnp.bfloat16, jnp.float32
    dma = pltpu.SemaphoreType.DMA
    vm = pl.BlockSpec(memory_space=pltpu.VMEM)
    hbm = pl.BlockSpec(memory_space=pl.ANY)
    out_shape = [jax.ShapeDtypeStruct((rows, half), low)] * 3 + [
        jax.ShapeDtypeStruct((cols, 8 * rows), low),
        jax.ShapeDtypeStruct((8, LANES), f32),
    ]
    scratch = [
        pltpu.VMEM((8 * rows, cols), low),
        pltpu.VMEM((cols, 2 * half), low),
        pltpu.VMEM((8, 8, LANES), f32),
        pltpu.VMEM((8, 8, LANES), f32),
        dma((7,)), dma((7,)),
        pltpu.VMEM((rows, 1), f32),
        dma((2,)),
    ] + reduce_scratch(counts, rows, width)
    kernel = functools.partial(ffn_kernel, rows, width, counts)
    return kernel_call(kernel, out_shape, [x_low, attn, gain, w_gate, w_up, d_hidden], [vm, vm, vm, hbm, hbm, vm],
                       scratch, cid, "ffn", late=(5,), early=(3,))


def load_own(spread, payload, width, counts, sems):
    copies = []
    for half in range(2):
        for at in range(counts):
            first = at * width + (half * counts * width if len(payload) == 1 else 0)
            src = payload[half % len(payload)].at[:, first : first + width]
            copies.append(pltpu.make_async_copy(src, spread.slot(0, half, at), sems.at[half, at]))
    return copies


def chip_place(here, per):
    def place(at):
        return here.shard(at // (2 * per), at // per % 2) * per + at % per

    return place


def back_kernel(rows, width, counts, act_t, w_gate, w_up, d_gate, d_up, dots, x_low, attn, gain, d_norm, gain_grad,
                grad_gate, grad_up, *refs, late):
    here = Place()
    spread = Spread(here, counts, refs[:7])
    tiny_all, tiny_send, tiny_recv, own_sems, weight, sums, grads, staged, local_sems, out_sems = refs[7:17]
    contrib, rest, rest_sems = refs[17:20]
    line = Line(here, 4, [contrib, d_norm] + list(refs[20:]), chip_place(here, 2))
    tiny = Tiny(here, dots, tiny_all, (tiny_send, tiny_recv), False)
    half_cols = counts * width
    local = [
        pltpu.make_async_copy(w_gate, weight.at[:, :half_cols], local_sems.at[0]),
        pltpu.make_async_copy(w_up, weight.at[:, half_cols:], local_sems.at[1]),
    ]
    own = load_own(spread, (d_gate, d_up), width, counts, own_sems)
    for copy in own + local:
        copy.start()
    greet(here, tiny.peers, True)
    for copy in own:
        copy.wait()
    tiny.begin()
    spread.begin()
    sums[...] = jnp.zeros_like(sums)
    for copy in local + late:
        copy.wait()

    def columns(half, at):
        return pl.ds(pl.multiple_of((half * counts + at) * width, width), width)

    def clear(at, _):
        grads[:, columns(0, at)] = jnp.zeros((grads.shape[0], width), jnp.float32)
        return 0

    lax.fori_loop(0, 2 * counts, clear, 0)

    def blocks(across, half, at):
        cols = columns(half, at)
        gained = grads[:, cols]
        for other in range(2):
            row = row_span(here, across, other, rows)
            block = spread.got[across, (spread.core + other) % 2, half, at]
            sums[row, :] += dot_nt(block, weight[:, cols])
            gained = gained + dot_nn(act_t[:, row], block)
        grads[:, cols] = gained

    def leave(half, at):
        spot = pl.ds(pl.multiple_of(at * width, width), width)
        return pltpu.make_async_copy(staged.at[half], (grad_gate, grad_up)[half].at[:, spot],
                                     out_sems.at[half, at])

    eye = diagonal()
    gain_grad[...] = jnp.zeros_like(gain_grad)

    def close_chip(chip, target):
        def close_shard(other, _):
            shard = here.shard(chip, other)
            span = pl.ds(pl.multiple_of(shard * rows, rows), rows)
            loads = [pltpu.make_async_copy(src.at[span, :], rest.at[at], rest_sems.at[at])
                     for at, src in enumerate((x_low, attn))]
            for copy in loads:
                copy.start()
            for copy in loads:
                copy.wait()
            for at in range(rows // LANES):
                span = pl.ds(pl.multiple_of(shard * rows + at * LANES, LANES), LANES)
                piece = slice(at * LANES, (at + 1) * LANES)
                dot = from_tile(tiny_all[shard, at : at + 1, :], eye)
                resid = rest[0, piece, :].astype(jnp.float32) + rest[1, piece, :].astype(jnp.float32)
                value = sums[span, :]
                target[span, :] = (value * gain[1:2, :] - resid * dot).astype(target.dtype)
                gain_grad[...] += jnp.sum(value * resid, axis=0, keepdims=True)
            return 0

        lax.fori_loop(0, 2, close_shard, 0)

    def done(stage, at):
        @pl.when(jnp.logical_and(stage == 3, at > 0))
        def _():
            leave(0, at - 1).wait()
            leave(1, at - 1).wait()

        @pl.when(stage == 3)
        def _():
            for half in range(2):
                staged[half] = grads[:, columns(half, at)].astype(staged.dtype)
            leave(0, at).start()
            leave(1, at).start()

        @pl.when(jnp.logical_and(at == counts - 1, stage == 0))
        def _():
            close_chip(0, contrib)
            line.launch(0, 4)

        @pl.when(jnp.logical_and(at == counts - 1, stage == 2))
        def _():
            lax.fori_loop(1, 3, lambda chip, _: (close_chip(chip, d_norm), 0)[1], 0)

    def hook(step):
        @pl.when(jnp.logical_and(step >= counts, step < counts + 6))
        def _():
            line.step(step - counts)

    tiny.end()
    spread.run(blocks, hook, done)
    close_chip(3, d_norm)
    line.settle()
    spread.end()

    def drain(at, _):
        leave(0, at).wait()
        leave(1, at).wait()
        return 0

    lax.fori_loop(counts - 1, counts, drain, 0)


def back_gather(act_t, w_gate, w_up, d_gate, d_up, dots, x_low, attn, gain, cid, width=512):
    cols, total = act_t.shape
    rows, half = d_gate.shape
    counts = half // width
    low, f32 = jnp.bfloat16, jnp.float32
    dma = pltpu.SemaphoreType.DMA
    vm = pl.BlockSpec(memory_space=pltpu.VMEM)
    hbm = pl.BlockSpec(memory_space=pl.ANY)
    out_shape = [
        jax.ShapeDtypeStruct((total, cols), low),
        jax.ShapeDtypeStruct((1, cols), f32),
        jax.ShapeDtypeStruct((cols, half), low),
        jax.ShapeDtypeStruct((cols, half), low),
    ]
    scratch = spread_scratch(counts, rows, width) + [
        pltpu.VMEM((8, 8, LANES), f32), dma((7,)), dma((7,)), dma((2, counts)),
        pltpu.VMEM((cols, 2 * half), low),
        pltpu.VMEM((total, cols), f32),
        pltpu.VMEM((cols, 2 * half), f32),
        pltpu.VMEM((2, cols, width), low),
        dma((2,)), dma((2, counts)),
        pltpu.VMEM((total, cols), low),
        pltpu.VMEM((2, rows, cols), low),
        dma((2,)),
    ] + line_scratch(4, (4 * rows // 2, cols), low)
    operands = [act_t, w_gate, w_up, d_gate, d_up, dots, x_low, attn, gain]
    kernel = functools.partial(back_kernel, rows, width, counts)
    return kernel_call(kernel, out_shape, operands, [vm] + [hbm] * 4 + [vm, hbm, hbm, vm], scratch, cid, "back",
                       [vm, vm, hbm, hbm], (0,))


def down_kernel(rows, width, counts, cot, weight, hidden, d_norm, ffn, d_attn, grad, *refs, late, early):
    here = Place()
    spread = Spread(here, counts, refs[:7])
    own_sems, sums, grads, staged, out_sems, norm_out = refs[7:13]
    place = chip_place(here, 2)
    norm_line = Line(here, 12, [d_norm, norm_out] + list(refs[13:]), lambda at: place(at + 4))
    own = load_own(spread, (hidden,), width, counts, own_sems)
    for copy in own:
        copy.start()
    greet(here, slice_peers(here), True)
    norm_line.begin()
    for copy in own:
        copy.wait()
    spread.begin()
    sums[...] = jnp.zeros_like(sums)
    grads[...] = jnp.zeros_like(grads)
    for copy in late:
        copy.wait()

    def columns(half, at):
        return pl.ds(pl.multiple_of((half * counts + at) * width, width), width)

    def blocks(across, half, at):
        cols = columns(half, at)
        gained = grads[cols, :]
        for other in range(2):
            row = row_span(here, across, other, rows)
            block = spread.got[across, (spread.core + other) % 2, half, at]
            sums[row, :] += dot_nn(block, weight[cols, :])
            gained = gained + dot_tn(block, cot[row, :])
        grads[cols, :] = gained

    def leave(half, at):
        return pltpu.make_async_copy(staged.at[at % 2, half], grad.at[columns(half, at), :], out_sems.at[half, at])

    def done(stage, at):
        @pl.when(jnp.logical_and(stage == 3, at > 1))
        def _():
            leave(0, at - 2).wait()
            leave(1, at - 2).wait()

        @pl.when(stage == 3)
        def _():
            for half in range(2):
                staged[at % 2, half] = grads[columns(half, at), :].astype(staged.dtype)
            leave(0, at).start()
            leave(1, at).start()


    def hook(step):
        @pl.when(step % 3 < 2)
        def _():
            norm_line.step(step // 3 * 2 + step % 3)

    spread.run(blocks, hook, done)
    ffn[...] = sums[...].astype(ffn.dtype)
    early[0].start()
    norm_line.settle()

    def add_norm(at, _):
        def add(source):
            span = row_span(here, at // 2, at % 2, rows)
            d_attn[span, :] = (cot[span, :].astype(jnp.float32) + source[span, :].astype(jnp.float32)).astype(
                d_attn.dtype)

        @pl.when(at < 2)
        def _():
            add(d_norm)

        @pl.when(at >= 2)
        def _():
            add(norm_out)
        return 0

    lax.fori_loop(0, 8, add_norm, 0)
    spread.end()

    def drain(at, _):
        leave(0, at).wait()
        leave(1, at).wait()
        return 0

    lax.fori_loop(counts - 2, counts, drain, 0)


def down_gather(cot, weight, hidden, d_norm, cid, width=256):
    total, cols = cot.shape
    rows, every = hidden.shape
    counts = every // (2 * width)
    low, f32 = jnp.bfloat16, jnp.float32
    dma = pltpu.SemaphoreType.DMA
    vm = pl.BlockSpec(memory_space=pltpu.VMEM)
    hbm = pl.BlockSpec(memory_space=pl.ANY)
    out_shape = [
        jax.ShapeDtypeStruct((total, cols), low),
        jax.ShapeDtypeStruct((total, cols), low),
        jax.ShapeDtypeStruct(weight.shape, low),
    ]
    scratch = spread_scratch(counts, rows, width) + [
        dma((2, counts)),
        pltpu.VMEM((total, cols), f32),
        pltpu.VMEM(weight.shape, f32),
        pltpu.VMEM((2, 2, width, cols), low),
        dma((2, counts)),
        pltpu.VMEM((total, cols), low),
    ] + line_scratch(12, (12 * rows // 2, cols), low)
    kernel = functools.partial(down_kernel, rows, width, counts)
    return kernel_call(kernel, out_shape, [cot, weight, hidden, d_norm], [vm, vm, hbm, vm], scratch, cid, "down",
                       [vm, vm, hbm], (0, 1), (0,))


def attend_kernel(rows, heads, cols, width, counts, qkv, rms, cos, sin, mask, w_out, g_col, w_down, attn, mixed_all,
                  kv, probs, queries, pair_rms, d_hidden, *refs, late, early):
    here = Place()
    spread = Spread(here, 1, refs[:7])
    part, pair_sems, tiny_own, tiny_pair, mixed_sems = refs[7:12]
    product = products(here, g_col, w_down, True, rows, width, counts)
    total = Reduce(here, counts, product, refs[12:23])
    piece = rows // 2

    def place(at):
        across, other, half_at = spread.block(at)
        return here.shard(across, other) * 2 + half_at

    line = Line(here, 16, [part, attn] + list(refs[23:]), place)
    got, core = spread.got, here.core
    greet(here, slice_peers(here), True)
    half = HD // 2
    scale = 1.0 / math.sqrt(HD)
    wide = heads * HD

    def rotated(first):
        lead = qkv[:, first : first + half] * rms[...]
        trail = qkv[:, first + half : first + HD] * rms[...]
        return lead * cos[0] - trail * sin[0], trail * cos[0] + lead * sin[0]

    low_k, high_k = rotated(wide)
    kv[0, :, :half] = low_k.astype(kv.dtype)
    kv[0, :, half:HD] = high_k.astype(kv.dtype)
    for at in range(2):
        first = HD + at * half
        kv[0, :, first : first + half] = (qkv[:, wide + first : wide + first + half] * rms[...]).astype(kv.dtype)
    eye = diagonal()
    tiny_own[...] = jnp.zeros_like(tiny_own)
    to_tile(tiny_own, 0, rms[:, :1], eye)
    pair_rms[0] = rms[...]
    pair = remote(kv.at[0], kv.at[1], pair_sems.at[0], pair_sems.at[1], spread.ydev)
    tiny = remote(tiny_own, tiny_pair, pair_sems.at[2], pair_sems.at[3], spread.ydev)
    for head in range(heads):
        if head == 1:
            pair.start()
            tiny.start()
        lead, trail = rotated(head * HD)
        queries[:, head * HD : head * HD + half] = (lead * scale).astype(queries.dtype)
        queries[:, head * HD + half : (head + 1) * HD] = (trail * scale).astype(queries.dtype)
    early[2].start()
    pair.wait()
    early[0].start()
    for copy in late:
        copy.wait()

    def one_head(head, _):
        query = queries[:, pl.ds(pl.multiple_of(head * HD, HD), HD)]
        scores = jnp.concatenate([dot_nt(query, kv[0, :, :HD]), dot_nt(query, kv[1, :, :HD])], axis=1)
        scores = jnp.where(mask[...] > 0, scores, NEG)
        expd = jnp.exp(scores - jnp.max(scores, axis=-1, keepdims=True))
        prob = expd / jnp.sum(expd, axis=-1, keepdims=True)
        probs[head] = prob
        prob_low = prob.astype(jnp.bfloat16)
        mixed = dot_nn(prob_low[:, :rows], kv[0, :, HD:]) + dot_nn(prob_low[:, rows:], kv[1, :, HD:])
        span = pl.ds(pl.multiple_of(head * HD, HD), HD)
        for half_at in range(2):
            low_mixed = mixed[half_at * piece : (half_at + 1) * piece, :].astype(got.dtype)
            got[0, core, half_at, 0, :, span] = low_mixed
        return 0

    lax.fori_loop(0, heads, one_head, 0)
    early[1].start()
    spread.begin_rows()

    def mixed_copy(at):
        across, other, half_at = spread.block(at)
        span = pl.ds(pl.multiple_of(place(at) * piece, piece), piece)
        return pltpu.make_async_copy(got.at[across, (core + other) % 2, half_at, 0], mixed_all.at[span, :],
                                     mixed_sems.at[at])

    def one_step(step, _):
        spread.receive_rows(step)

        @pl.when(step < 16)
        def _():
            across, other, half_at = spread.block(step)
            value = dot_nn(got[across, (core + other) % 2, half_at, 0], w_out[...])
            part[pl.ds(pl.multiple_of(place(step) * piece, piece), piece), :] = value.astype(part.dtype)
            mixed_copy(step).start()
            line.launch(step, 1)

        @pl.when(step >= 2)
        def _():
            total.advance(step - 2)

        @pl.when(step >= 2)
        def _():
            line.step(step - 2)
        return 0

    lax.fori_loop(0, 20, one_step, 0)
    line.end(18)
    early[3].start()

    def emit(at, first, second):
        for half_at, value in enumerate((first, second)):
            d_hidden[:, pl.ds(pl.multiple_of((half_at * counts + at) * width, width), width)] = value

    total.end(emit)
    for hop in range(3):
        spread.x_copy(hop, 0).wait_send()
        spread.y_copy(hop, 0).wait_send()
    for stage in range(4):
        for stream in range(2):
            spread.sib_copy(stage, stream, 0).wait_send()
    for at in range(16):
        mixed_copy(at).wait()
    tiny.wait()
    for at in range(rows // LANES):
        values = jnp.broadcast_to(from_tile(tiny_pair[at : at + 1, :], eye), (LANES, LANES))
        pair_rms[1, at * LANES : (at + 1) * LANES, :] = values


def attend(qkv, rms, cos, sin, mask, w_out, g_col, w_down, cid, width=512):
    rows = qkv.shape[0]
    wide, cols = w_out.shape
    heads = wide // HD
    counts = w_down.shape[0] // (2 * width)
    low, f32 = jnp.bfloat16, jnp.float32
    dma = pltpu.SemaphoreType.DMA
    vm = pl.BlockSpec(memory_space=pltpu.VMEM)
    out_shape = [
        jax.ShapeDtypeStruct((8 * rows, cols), low),
        jax.ShapeDtypeStruct((8 * rows, wide), low),
        jax.ShapeDtypeStruct((2, rows, 2 * HD), low),
        jax.ShapeDtypeStruct((heads, rows, 2 * rows), f32),
        jax.ShapeDtypeStruct((rows, wide), low),
        jax.ShapeDtypeStruct((2,) + rms.shape, f32),
        jax.ShapeDtypeStruct((rows, w_down.shape[0]), f32),
    ]
    scratch = spread_scratch(1, rows // 2, wide) + [
        pltpu.VMEM((8 * rows, cols), low), dma((4,)),
        pltpu.VMEM((8, LANES), f32), pltpu.VMEM((8, LANES), f32), dma((16,)),
    ] + reduce_scratch(counts, rows, width) + line_scratch(16, (8 * rows, cols), low)
    kernel = functools.partial(attend_kernel, rows, heads, cols, width, counts)
    operands = [qkv, rms, cos, sin, mask, w_out, g_col, w_down]
    out_specs = [vm, pl.BlockSpec(memory_space=pl.ANY)] + [vm] * 5
    return kernel_call(kernel, out_shape, operands, [vm] * 8, scratch, cid, "attend", out_specs, (4, 5, 6, 7), (2, 3, 4, 0))


def tail_kernel(rows, heads, per, d_attn, w_out, queries, kv, probs, rms, cos, sin, act_t, w_qkv, ffn, x_low,
                attn, gain, gain_grad, mixed_all, d_tok, out, grad_query, grad_out, kv_sum, gains, *refs, late, early):
    here = Place()
    width = HD
    counts = heads // 2
    part = rows // 2
    refs = list(refs)
    line_counts = 8 * per
    cols = d_attn.shape[1]
    extra = cols // (rows // per)

    def take(count):
        taken_refs = refs[:count]
        del refs[:count]
        return taken_refs

    total_refs = take(11)
    spread = Spread(here, 1, take(7))
    d_mixed, tiny_own, tiny_all, d_kv, give, taken, give_sems, tiny_send, tiny_recv = take(9)
    grad, grad_mixed, gain_sum, tile, tile_send, tile_recv, put_sems, local_sems, mixed_two, mixed_sems = take(10)

    def far(at):
        return at // (2 * per), at // per % 2

    def near(at):
        return spread.block(jnp.minimum(at, line_counts - 1))

    def place_ffn(at):
        return here.shard(*far(at)) * per + at % per

    def place_tok(at):
        across, other, half_at = near(at)
        return jnp.where(at < line_counts, here.shard(across, other) * per + half_at, at)

    gain_tiles, ffn_sum, leaving = take(3)
    by_chip = chip_place(here, per)
    line = Line(here, line_counts, [ffn, ffn_sum] + take(8), by_chip)
    contrib, summed = take(2)
    line_tok = Line(here, line_counts + extra, [contrib, summed] + take(8), place_tok)
    tiny = Tiny(here, tiny_own, tiny_all, (tiny_send, tiny_recv), False)
    got, core = spread.got, here.core
    product = products(here, d_attn, w_out, True, rows, width, counts)
    total = Reduce(here, counts, product, total_refs)
    greet(here, tiny.peers, True)
    line.begin()
    grad_mixed[...] = jnp.zeros_like(grad_mixed)

    def mixed_copy(step):
        span = pl.ds(pl.multiple_of(step * rows, rows), rows)
        return pltpu.make_async_copy(mixed_all.at[span, :], mixed_two.at[step % 2], mixed_sems.at[step % 2])

    mixed_copy(0).start()

    def beside(step):
        line.step(step)

        @pl.when(step < 8)
        def _():
            span = pl.ds(pl.multiple_of(step * rows, rows), rows)
            mixed_copy(step).wait()

            @pl.when(step < 7)
            def _():
                mixed_copy(step + 1).start()

            grad_mixed[...] += dot_tn(mixed_two[step % 2], d_attn[span, :])

    done = total.run(beside)
    grad_out[...] = grad_mixed[...].astype(grad_out.dtype)
    early[1].start()

    def land(at, first, second):
        for half_at, value in enumerate((first, second)):
            d_mixed[:, pl.ds(pl.multiple_of((half_at * counts + at) * width, width), width)] = value.astype(
                d_mixed.dtype)

    total.end(land)
    half = HD // 2
    scale = 1.0 / math.sqrt(HD)
    depth = w_qkv.shape[0] * 8
    d_kv[...] = jnp.zeros_like(d_kv)
    for copy in late:
        copy.wait()

    def one_head(head, dots):
        span = pl.ds(pl.multiple_of(head * HD, HD), HD)
        query = queries[:, span]
        cot = d_mixed[:, span]
        prob = probs[head]
        d_prob = jnp.concatenate([dot_nt(cot, kv[0, :, HD:]), dot_nt(cot, kv[1, :, HD:])], axis=1)
        delta = jnp.sum(prob * d_prob, axis=-1, keepdims=True)
        d_score = (prob * (d_prob - delta)).astype(jnp.bfloat16)
        prob_low = prob.astype(jnp.bfloat16)
        d_query = (dot_nn(d_score[:, :rows], kv[0, :, :HD]) + dot_nn(d_score[:, rows:], kv[1, :, :HD])) * scale
        for side in range(2):
            keys = slice(side * rows, (side + 1) * rows)
            d_kv[side, :, :HD] += dot_tn(d_score[:, keys], query)
            d_kv[side, :, HD:] += dot_tn(prob_low[:, keys], cot)
        dots = dots + jnp.sum(d_query * query.astype(jnp.float32), axis=-1, keepdims=True)
        lead, trail = d_query[:, :half], d_query[:, half:]
        first = ((lead * cos[0] + trail * sin[0]) * rms[0]).astype(got.dtype)
        second = ((trail * cos[0] - lead * sin[0]) * rms[0]).astype(got.dtype)
        line.step(done + head)
        for rows_at in range(2):
            piece = slice(rows_at * part, (rows_at + 1) * part)
            got[0, core, rows_at, 0, :, pl.ds(pl.multiple_of(head * HD, HD), half)] = first[piece, :]
            got[0, core, rows_at, 0, :, pl.ds(pl.multiple_of(head * HD + half, half), half)] = second[piece, :]

        return dots

    dots = lax.fori_loop(0, heads, one_head, jnp.zeros((rows, 1), jnp.float32))
    eye = diagonal()
    tiny_own[...] = jnp.zeros_like(tiny_own)
    for side in (1, 0):
        d_key, d_value = d_kv[side, :, :HD], d_kv[side, :, HD:]
        own = jnp.sum(d_key * kv[side, :, :HD].astype(jnp.float32) +
                      d_value * kv[side, :, HD:].astype(jnp.float32), axis=-1, keepdims=True)
        if side == 0:
            own = own + dots * (1.0 / scale)
        own = own * (rms[side] * rms[side] * (1.0 / depth))
        to_tile(tiny_own, side * (rows // LANES), own, eye)
        lead, trail = d_key[:, :half], d_key[:, half:]
        parts = [(lead * cos[side] + trail * sin[side]) * rms[side],
                 (trail * cos[side] - lead * sin[side]) * rms[side],
                 d_value[:, :half] * rms[side], d_value[:, half:] * rms[side]]
        for at, value in enumerate(parts):
            if side == 1:
                give[:, at * half : (at + 1) * half] = value.astype(give.dtype)
            else:
                d_kv[0, :, at * half : (at + 1) * half] = value
    given = remote(give, taken, give_sems.at[0], give_sems.at[1], spread.ydev)
    given.start()
    grad[...] = jnp.zeros_like(grad)
    line.steps(done + heads, done + heads + 2)
    given.wait()
    for rows_at in range(2):
        piece = slice(rows_at * part, (rows_at + 1) * part)
        value = d_kv[0, piece, :] + taken[piece, :].astype(jnp.float32)
        got[0, core, rows_at, 0, :, heads * HD :] = value.astype(got.dtype)
    tiny.begin()
    spread.begin_rows()
    gain_sum[...] = jnp.zeros_like(gain_sum)
    tiny.end()

    def block_of(at):
        across, other, half_at = near(at)
        shard, partner = here.shard(across, other), here.shard((across + 2) % 4, other)
        block = got[across, (core + other) % 2, half_at, 0]
        first = pl.multiple_of(shard * rows + half_at * part, part)
        for tile_at in range(part // LANES):
            row = pl.ds(pl.multiple_of(first + tile_at * LANES, LANES), LANES)
            low_at = half_at * (part // LANES) + tile_at
            kept = rows // LANES + low_at
            dot = from_tile(tiny_all[shard, pl.ds(low_at, 1), :] + tiny_all[partner, pl.ds(kept, 1), :], eye)
            value = dot_nt(block[tile_at * LANES : (tile_at + 1) * LANES, :], w_qkv[...])
            x_rows = x_low[row, :].astype(jnp.float32)
            contrib[row, :] = (value * gain[0:1, :] - x_rows * dot).astype(contrib.dtype)
            gain_sum[...] += jnp.sum(value * x_rows, axis=0, keepdims=True)
        line_tok.launch(at, 1)

        @pl.when(other == 1)
        def _():
            twin = got[across, core, half_at, 0]
            twin_first = pl.multiple_of(here.shard(across, 0) * rows + half_at * part, part)
            rows_t, twin_t = act_t[:, pl.ds(first, part)], act_t[:, pl.ds(twin_first, part)]
            for at_col in range((heads + 2) * HD // 512):
                span = slice(at_col * 512, (at_col + 1) * 512)
                grad[:, span] += dot_nn(rows_t, block[:, span]) + dot_nn(twin_t, twin[:, span])

    me = here.shard(0, 0)
    columns = pl.ds(pl.multiple_of(me * cols, cols), cols)
    chunk = line.chunk

    def landing(which, at):
        sub = at % per if which == 0 else near(at)[2]
        return (out, d_tok)[which].at[pl.ds(pl.multiple_of(sub * chunk, chunk), chunk), columns]

    def leaver(which, at):
        return (leaving, line_tok.from_end)[which].at[at]

    def put(which, at):
        goal = here.device(*(far(at) if which == 0 else near(at)[:2]))
        return remote(leaver(which, at), landing(which, at), put_sems.at[which, 0, at], put_sems.at[which, 1, at],
                      goal)

    def keep(which, at):
        spot = at % per if which == 0 else near(at)[2]
        return pltpu.make_async_copy(leaver(which, at), landing(which, at), local_sems.at[which, spot])

    def emit(which, at):
        if which == 1:
            row = line_tok.rows(at)
            value = d_attn[row, :].astype(jnp.float32) + summed[row, :].astype(jnp.float32)
            line_tok.from_end[at] = value.astype(out.dtype)
            return
        row = pl.ds(pl.multiple_of(place_ffn(at) * chunk, chunk), chunk)

        def leave(source):
            value = x_low[row, :].astype(jnp.float32) + attn[row, :].astype(jnp.float32)
            leaving[at] = (value + source[row, :].astype(jnp.float32)).astype(out.dtype)

        leave(ffn_sum)

    def is_own(which, at):
        return at < per if which == 0 else jnp.logical_and(at < 4, at % 2 == 0)

    def send(which, at):
        own = is_own(which, at)

        @pl.when(own)
        def _():
            keep(which, at).start()

        @pl.when(jnp.logical_not(own))
        def _():
            put(which, at).start()

    def stage_step(step, _):
        spread.receive_rows(step)

        @pl.when(step < line_counts)
        def _():
            block_of(step)

        @pl.when(step < 3)
        def _():
            line.step(done + heads + 2 + step)

        @pl.when(step >= 4)
        def _():
            line_tok.step(step - 4)

        @pl.when(step > 0)
        def _():
            send(0, step - 1)

        @pl.when(line.inner == 0)
        def _():
            line.up(step).wait_send()
            line.down(step).wait_recv()

        emit(0, step)

        @pl.when(jnp.logical_and(line.inner == 1, step > 7))
        def _():
            send(1, step - 8)

        @pl.when(jnp.logical_and(line.inner == 1, step > 6))
        def _():
            emit(1, step - 7)
        return 0

    lax.fori_loop(0, line_counts, stage_step, 0)
    for half_at in range(cols // (rows // per)):
        span = pl.ds(line_counts * (rows // per) + half_at * (rows // per), rows // per)
        source = slice(half_at * (rows // per), (half_at + 1) * (rows // per))
        contrib[span, :] = grad[source, heads * HD :].astype(contrib.dtype)
    line_tok.launch(line_counts, extra)
    grad_query[...] = grad[:, : heads * HD].astype(grad_query.dtype)
    early[0].start()
    for at in range(cols // LANES):
        tile[at : at + 1, :] = gain_sum[:, at * LANES : (at + 1) * LANES]
        spot = cols // LANES + at
        tile[spot : spot + 1, :] = gain_grad[:, at * LANES : (at + 1) * LANES]

    def tile_copy(step):
        return remote(tile, gain_tiles.at[here.z], tile_send.at[step], tile_recv.at[step],
                      (here.dp, here.seq, (here.z + step + 1) % 4))

    send(0, line_counts - 1)
    line.drain()
    for step in range(3):
        tile_copy(step).start()
    gain_tiles[here.z] = tile[...]

    @pl.when(line.inner == 1)
    def _():
        start = line_counts - 4

        def both(at, _):
            line_tok.step(at)

            @pl.when(at < line_counts + 4)
            def _():
                send(1, at - 4)

            @pl.when(at < line_counts + 3)
            def _():
                emit(1, at - 3)
            return 0

        lax.fori_loop(start, line_counts + extra + 2, both, 0)

        def drain(at, _):
            line_tok.down(at).wait_send()
            return 0

        lax.fori_loop(0, line_counts + extra, drain, 0)

    @pl.when(line.inner == 0)
    def _():
        def arrive(at, _):
            line_tok.up(at).wait_send()
            line_tok.down(at).wait_recv()

            @pl.when(jnp.logical_and(at > 0, at <= line_counts))
            def _():
                send(1, at - 1)

            @pl.when(at < line_counts)
            def _():
                emit(1, at)
            return 0

        lax.fori_loop(0, line_counts + extra, arrive, 0)

    for half_at in range(extra):
        span = pl.ds((line_counts + half_at) * chunk, chunk)
        kv_sum[half_at * chunk : (half_at + 1) * chunk, :] = summed[span, :]
    for hop in range(3):
        spread.x_copy(hop, 0).wait_send()
        spread.y_copy(hop, 0).wait_send()
    for stage in range(4):
        spread.sib_copy(stage, 0, 0).wait_send()
        spread.sib_copy(stage, 1, 0).wait_send()

    for which in range(2):
        def finish(at, _, which=which):
            own = is_own(which, at)

            @pl.when(own)
            def _():
                keep(which, at).wait()

            @pl.when(jnp.logical_not(own))
            def _():
                put(which, at).wait()
            return 0

        lax.fori_loop(0, line_counts, finish, 0)
        if which == 0:
            early[2].start()
    for step in range(3):
        tile_copy(step).wait()
    gains[...] = gain_tiles[0] + gain_tiles[1] + gain_tiles[2] + gain_tiles[3]


def tail(d_attn, w_out, queries, kv, probs, rms, cos, sin, act_t, w_qkv, ffn, x_low, attn, gain, gain_grad,
         mixed_all, cid,
 per=2):
    total, cols = d_attn.shape
    rows = total // 8
    wide = w_out.shape[0]
    heads = wide // HD
    low, f32 = jnp.bfloat16, jnp.float32
    dma = pltpu.SemaphoreType.DMA
    vm = pl.BlockSpec(memory_space=pltpu.VMEM)
    counts = 8 * per
    chunk = rows // per
    extra = cols // chunk
    long = (total + cols, cols)
    out_shape = [
        jax.ShapeDtypeStruct((rows, 8 * cols), low),
        jax.ShapeDtypeStruct((rows, 8 * cols), low),
        jax.ShapeDtypeStruct((cols, wide), low),
        jax.ShapeDtypeStruct(w_out.shape, low),
        jax.ShapeDtypeStruct((cols, 2 * HD), low),
        jax.ShapeDtypeStruct((8, LANES), f32),
    ]
    scratch = reduce_scratch(heads // 2, rows, HD, 2) + spread_scratch(1, rows // 2, wide + 2 * HD)
    scratch += [
        pltpu.VMEM((rows, wide), low),
        pltpu.VMEM((8, LANES), f32),
        pltpu.VMEM((8, 8, LANES), f32),
        pltpu.VMEM((2, rows, 2 * HD), f32),
        pltpu.VMEM((rows, 2 * HD), low),
        pltpu.VMEM((rows, 2 * HD), low),
        dma((2,)), dma((7,)), dma((7,)),
        pltpu.VMEM(w_qkv.shape, f32),
        pltpu.VMEM(w_out.shape, f32),
        pltpu.VMEM((1, cols), f32),
        pltpu.VMEM((8, LANES), f32),
        dma((3,)), dma((3,)), dma((2, 2, counts)), dma((2, per)),
        pltpu.VMEM((2, rows, wide), low), dma((2,)),
        pltpu.VMEM((4, 8, LANES), f32),
        pltpu.VMEM((total, cols), low),
        pltpu.VMEM((counts, chunk, cols), low),
    ] + line_scratch(counts, (total, cols), low)
    scratch += [pltpu.VMEM(long, low), pltpu.VMEM(long, low)] + line_scratch(counts + extra, long, low)
    operands = [d_attn, w_out, queries, kv, probs, rms, cos, sin, act_t, w_qkv, ffn, x_low, attn, gain,
                gain_grad, mixed_all]
    kernel = functools.partial(tail_kernel, rows, heads, per)
    specs = [vm] * (len(operands) - 1) + [pl.BlockSpec(memory_space=pl.ANY)]
    return kernel_call(kernel, out_shape, operands, specs, scratch, cid, "tail",
                       late=(2, 3, 4, 8, 9, 11, 12), early=(2, 3, 1))


LANES = 128


def acts_move(
    tokens, seg_ids, gain_attn, w_query, kv_weight, w_out, gain_ffn, w_gate, w_up, w_down, d_out
):
    qkv, x_low, act_one_t, w_qkv, rms, cos, sin, mask, g_parts, small = opening(
        tokens, gain_attn, gain_ffn, seg_ids, w_query, kv_weight, d_out, 1
    )
    g_low = g_parts.reshape(x_low.shape)
    attn, mixed_all, kv, probs, queries, pair_rms, d_hidden = attend(
        qkv, rms, cos, sin, mask, w_out, g_low, w_down, 2
    )
    hidden, d_gate, d_up, act_two_t, dots = ffn_scatter(x_low, attn, small, w_gate, w_up, d_hidden, 4)
    d_norm, grad_gain_two, grad_gate, grad_up = back_gather(
        act_two_t, w_gate, w_up, d_gate, d_up, dots, x_low, attn, small, 5
    )
    ffn, d_attn, grad_down = down_gather(g_low, w_down, hidden, d_norm, 6)
    d_tokens, out, grad_query, grad_out, grad_kv, gain_sums = tail(
        d_attn,
        w_out,
        queries,
        kv,
        probs,
        pair_rms,
        cos,
        sin,
        act_one_t,
        w_qkv,
        ffn,
        x_low,
        attn,
        small,
        grad_gain_two,
        mixed_all,
        7,
    )
    gains = gain_sums.reshape(2, -1)
    wider = jnp.float32
    return (
        out,
        d_tokens.astype(wider),
        gains[0],
        grad_query.astype(wider),
        grad_kv.astype(wider),
        grad_out.astype(wider),
        gains[1],
        grad_gate.astype(wider),
        grad_up.astype(wider),
        grad_down.astype(wider),
    )


def solution(mesh):
    in_specs = (
        P(("dp", "seq"), None),
        P("dp"),
        P(("dp", "seq")),
        P(("dp", "seq"), "tensor"),
        P(("dp", "seq"), None),
        P("tensor", ("dp", "seq")),
        P(("dp", "seq")),
        P(("dp", "seq"), "tensor"),
        P(("dp", "seq"), "tensor"),
        P("tensor", ("dp", "seq")),
        P(("dp", "seq"), None),
    )
    out_specs = (
        P(("dp", "seq"), None),
        P(("dp", "seq"), None),
        P(("dp", "seq")),
        P(("dp", "seq"), "tensor"),
        P(("dp", "seq"), None),
        P("tensor", ("dp", "seq")),
        P(("dp", "seq")),
        P(("dp", "seq"), "tensor"),
        P(("dp", "seq"), "tensor"),
        P("tensor", ("dp", "seq")),
    )

    def shards(*arrays):
        tokens = arrays[0]
        sizes = tuple(mesh.shape[name] for name in ("dp", "seq", "tensor"))
        count = tokens.shape[0] * sizes[0] * sizes[1]
        plan = acts_move if sizes == (4, 2, 4) and count <= tokens.shape[1] else weights_move
        return plan(*arrays)

    return jax.shard_map(shards, mesh=mesh, in_specs=in_specs, out_specs=out_specs, check_vma=False)
```
